16 devices in a mesh: cp: 16 (over z, y, x, core).
Axes of the slice: x: 2, y: 2, z: 2, core: 2. Of those that a mesh axis runs over, the one named last changes fastest.
Arguments:
- query: bfloat16 [8, 1024, 16, 128], P(None, 'cp')
- key_in: bfloat16 [8, 1024, 16, 128], P(None, 'cp')
- value: bfloat16 [8, 1024, 16, 128], P(None, 'cp')
- bias_u: bfloat16 [16, 128], replicated
- bias_w: bfloat16 [16, 128], replicated
- rel_k: bfloat16 [1024, 16, 128], replicated
- d_out: bfloat16 [8, 1024, 16, 128], P(None, 'cp')
Outputs:
- output 1: bfloat16 [8, 1024, 16, 128], P(None, 'cp')
- output 2: bfloat16 [8, 1024, 16, 128], P(None, 'cp')
- output 3: bfloat16 [8, 1024, 16, 128], P(None, 'cp')
- output 4: bfloat16 [8, 1024, 16, 128], P(None, 'cp')
- output 5: float32 [16, 128], replicated
- output 6: float32 [16, 128], replicated
- output 7: float32 [1024, 16, 128], replicated
All inputs are finite; a program needn't handle non-finite values.
Results may differ from the reference program's by a relative error of at most 0.00858762.
Values are sent between devices in bfloat16 or wider.
A program may use at most 1 GiB of HBM per device.

```python
import jax
import jax.numpy as jnp
from jax import lax

BATCH = 8
SEQ_DEV = 64
SEQ = 1024
HEADS = 16
HEAD = 128
FREQS = 64


def rel_table(rng_key):
    distance = jnp.arange(SEQ, dtype=jnp.float32)[:, None]
    inv_freq = 1.0 / (10000.0 ** (jnp.arange(FREQS, dtype=jnp.float32) / FREQS))
    angles = distance * inv_freq[None, :]
    sinusoid = jnp.concatenate([jnp.sin(angles), jnp.cos(angles)], axis=1)
    rel_proj = jax.random.normal(rng_key, (2 * FREQS, HEADS * HEAD), jnp.float32) * FREQS ** -0.5
    return jnp.dot(sinusoid, rel_proj).reshape(SEQ, HEADS, HEAD).astype(jnp.bfloat16)


def setup_inputs(seed: int = 0) -> dict:
    rng_keys = jax.random.split(jax.random.key(seed), 7)
    act_shape = (BATCH, SEQ, HEADS, HEAD)
    query = jax.random.normal(rng_keys[0], act_shape, jnp.float32)
    key_in = jax.random.normal(rng_keys[1], act_shape, jnp.float32)
    value = jax.random.normal(rng_keys[2], act_shape, jnp.float32)
    d_out = jax.random.normal(rng_keys[3], act_shape, jnp.float32)
    bias_u = 0.5 * jax.random.normal(rng_keys[4], (HEADS, HEAD), jnp.float32)
    bias_w = 0.5 * jax.random.normal(rng_keys[5], (HEADS, HEAD), jnp.float32)
    return {
        'query': query.astype(jnp.bfloat16),
        'key_in': key_in.astype(jnp.bfloat16),
        'value': value.astype(jnp.bfloat16),
        'bias_u': bias_u.astype(jnp.bfloat16),
        'bias_w': bias_w.astype(jnp.bfloat16),
        'rel_k': rel_table(rng_keys[6]),
        'd_out': d_out.astype(jnp.bfloat16),
    }


def reference(query, key_in, value, bias_u, bias_w, rel_k, d_out):
    inv_sqrt = HEAD ** -0.5
    n_blocks = SEQ // SEQ_DEV
    q_u = (query.astype(jnp.float32) + bias_u.astype(jnp.float32)).astype(jnp.bfloat16)
    q_w = (query.astype(jnp.float32) + bias_w.astype(jnp.float32)).astype(jnp.bfloat16)
    pos_row = jnp.arange(SEQ_DEV)[:, None]
    pos_col = jnp.arange(SEQ)[None, :]

    def per_head(head_args):
        qu_h, qw_h, key_h, val_h, dout_h, rel_h = head_args

        def per_row(row_carry, row_args):
            qu_r, qw_r, key_r, val_r, dout_r = row_args

            def per_block(blk_carry, blk_idx):
                dk_acc, dv_acc, drel_acc, du_acc, dw_acc = blk_carry
                start = blk_idx * SEQ_DEV
                qu_b = lax.dynamic_slice_in_dim(qu_r, start, SEQ_DEV, 0)
                qw_b = lax.dynamic_slice_in_dim(qw_r, start, SEQ_DEV, 0)
                dout_b = lax.dynamic_slice_in_dim(dout_r, start, SEQ_DEV, 0)
                pos_q = start + pos_row
                causal = pos_col <= pos_q
                dist_idx = jnp.clip(pos_q - pos_col, 0, SEQ - 1)
                content = jnp.dot(qu_b, key_r.T, preferred_element_type=jnp.float32)
                by_dist = jnp.dot(qw_b, rel_h.T, preferred_element_type=jnp.float32)
                rel_part = jnp.take_along_axis(by_dist, dist_idx, axis=1)
                logits = jnp.where(causal, (content + rel_part) * inv_sqrt, -jnp.inf)
                attn_p = jax.nn.softmax(logits, axis=-1)
                probs_b = attn_p.astype(jnp.bfloat16)
                out_b = jnp.dot(probs_b, val_r, preferred_element_type=jnp.float32).astype(jnp.bfloat16)
                d_probs = jnp.dot(dout_b, val_r.T, preferred_element_type=jnp.float32)
                row_dot = jnp.sum(d_probs * attn_p, axis=-1, keepdims=True)
                d_logit = (attn_p * (d_probs - row_dot) * inv_sqrt).astype(jnp.bfloat16)
                d_dist = jnp.where(causal, jnp.take_along_axis(d_logit, dist_idx, axis=1), 0.0).astype(jnp.bfloat16)
                dq_cont = jnp.dot(d_logit, key_r, preferred_element_type=jnp.float32)
                dq_rel = jnp.dot(d_dist, rel_h, preferred_element_type=jnp.float32)
                dq_b = (dq_cont + dq_rel).astype(jnp.bfloat16)
                dk_acc = dk_acc + jnp.dot(d_logit.T, qu_b, preferred_element_type=jnp.float32)
                dv_acc = dv_acc + jnp.dot(probs_b.T, dout_b, preferred_element_type=jnp.float32)
                drel_acc = drel_acc + jnp.dot(d_dist.T, qw_b, preferred_element_type=jnp.float32)
                du_acc = du_acc + jnp.sum(dq_cont, axis=0)
                dw_acc = dw_acc + jnp.sum(dq_rel, axis=0)
                return (dk_acc, dv_acc, drel_acc, du_acc, dw_acc), (out_b, dq_b)

            drel_acc, du_acc, dw_acc = row_carry
            zeros_seq = jnp.zeros((SEQ, HEAD), jnp.float32)
            blk_out, blk_ys = lax.scan(per_block, (zeros_seq, zeros_seq, drel_acc, du_acc, dw_acc), jnp.arange(n_blocks))
            dk_acc, dv_acc, drel_acc, du_acc, dw_acc = blk_out
            out_r, dq_r = blk_ys
            row_outs = (out_r.reshape(SEQ, HEAD), dq_r.reshape(SEQ, HEAD), dk_acc.astype(jnp.bfloat16), dv_acc.astype(jnp.bfloat16))
            return (drel_acc, du_acc, dw_acc), row_outs

        zeros_dim = jnp.zeros((HEAD,), jnp.float32)
        head_carry, row_outs = lax.scan(per_row, (jnp.zeros((SEQ, HEAD), jnp.float32), zeros_dim, zeros_dim), (qu_h, qw_h, key_h, val_h, dout_h))
        drel_h, du_h, dw_h = head_carry
        return row_outs + (du_h, dw_h, drel_h)

    def by_head(tensor):
        return jnp.transpose(tensor, (2, 0, 1, 3))

    def by_pos(tensor):
        return jnp.transpose(tensor, (1, 2, 0, 3))

    head_outs = lax.map(per_head, (by_head(q_u), by_head(q_w), by_head(key_in), by_head(value), by_head(d_out), jnp.transpose(rel_k, (1, 0, 2))))
    out_h, dq_h, dk_h, dv_h, du_h, dw_h, drel_h = head_outs
    return (by_pos(out_h), by_pos(dq_h), by_pos(dk_h), by_pos(dv_h), du_h, dw_h, jnp.transpose(drel_h, (1, 0, 2)))
```

```python
import functools

import jax
import jax.numpy as jnp
from jax import lax
from jax.experimental import pallas as pl
from jax.experimental.pallas import tpu as pltpu
from jax.sharding import PartitionSpec as P

MESH = pl.DeviceIdType.MESH
BF16, F32 = jnp.bfloat16, jnp.float32
LOG2E = 1.4426950408889634

N_DEV = 16
PAIR = 2
N_PAIR = 8
SLOTS = 4
ROWS = 64
SEQ = N_DEV * ROWS
HEAD = 128
QB = 256
N_QB = SEQ // QB
PARTS = ((0, 171), (171, 171), (342, 171), (513, 171), (684, 170), (854, 170))
HOPS = ((1, 2, 4), (2, 4, 1), (4, 1, 2)) * 2
N_PART = len(PARTS)


def dot(lhs, rhs):
    return jnp.dot(lhs, rhs, preferred_element_type=F32)


def flip8(x):
    rows, cols = x.shape
    idx = 7 - lax.broadcasted_iota(jnp.int32, (rows // 8, 8, cols), 1)
    return jnp.take_along_axis(x.reshape(rows // 8, 8, cols), idx, axis=1).reshape(rows, cols)


def eye_rev(dtype):
    total = lax.broadcasted_iota(jnp.int32, (HEAD, HEAD), 0) + lax.broadcasted_iota(jnp.int32, (HEAD, HEAD), 1)
    return jnp.where(total == HEAD - 1, 1.0, 0.0).astype(dtype)


def kernel(q_in, k_in, v_in, g_in, r_in, u_in, w_in,
           o_out, dq_out, dk_out, dv_out, dr0_out, dr1_out, dr2_out, dr3_out, dr4_out, dr5_out, du_out, dw_out,
           buf, r_buf, dr_rx, dr_fin, dr_acc,
           s_ref, e_ref, dp_ref, pb_ref, ds_ref, dd_ref,
           a_s, c_s, g_s, k_s, v_s, rev_s, kt_s, vt_s, rt_s, at_s, ct_s, gt_s,
           dkt, dvt, stage,
           in_send, in_recv, out_send, out_recv, own_sem, r_sem, x_send, x_recv, ring_send, ring_recv, fw_send, fw_recv, b_send, b_recv):
    me = lax.axis_index("cp")
    core = me % 2
    chip = me // 2
    partner = me + 1 - 2 * core
    scale = HEAD ** -0.5

    r_copy = pltpu.make_async_copy(r_in.at[:, chip], r_buf, r_sem)
    r_copy.start()

    barrier = pltpu.get_barrier_semaphore()

    def say(step, carry):
        pl.semaphore_signal(barrier, inc=1, device_id=((me + step) % N_DEV,), device_id_type=MESH)
        return carry

    lax.fori_loop(1, N_DEV, say, 0)
    pl.semaphore_wait(barrier, N_DEV - 1)

    ins = (q_in, k_in, g_in, v_in)
    my_rows = pl.ds(pl.multiple_of(me * ROWS, ROWS), ROWS)

    def send_in(slot):
        for t, src in enumerate(ins):
            pltpu.make_async_copy(src.at[core * SLOTS + slot, :, chip], buf.at[t, slot, my_rows], in_recv.at[t, slot]).start()

        def to(step, carry):
            peer = me ^ step
            for t, src in enumerate(ins):
                pltpu.make_async_remote_copy(
                    src_ref=src.at[(peer % 2) * SLOTS + slot, :, peer // 2], dst_ref=buf.at[t, slot, my_rows],
                    send_sem=in_send, recv_sem=in_recv.at[t, slot], device_id=(peer,), device_id_type=MESH).start()
            return carry
        lax.fori_loop(1, N_DEV, to, 0)

    for slot in range(SLOTS):
        send_in(slot)

    r_copy.wait()
    pair_tab = pltpu.einshape("abc->bac", r_buf[...])
    rev = eye_rev(BF16)
    for hh in range(PAIR):
        for blk in range(SEQ // HEAD):
            part = pair_tab[hh, SEQ - HEAD * (blk + 1):SEQ - HEAD * blk]
            flipped = dot(rev, part).astype(BF16)
            rev_s[hh, HEAD * blk:HEAD * (blk + 1), :] = flipped
            rt_s[hh, :, HEAD * blk:HEAD * (blk + 1)] = flipped.T
    dr_acc[...] = jnp.zeros_like(dr_acc)

    u_all = u_in[chip].astype(F32)
    w_all = w_in[chip].astype(F32)

    acts = (o_out, dq_out, dk_out, dv_out)

    def send_out(slot, which):
        for t in which:
            pltpu.make_async_copy(buf.at[t, slot, my_rows], acts[t].at[core * SLOTS + slot, :, chip], out_recv.at[t]).start()

        def to(step, carry):
            peer = me ^ step
            peer_rows = pl.ds(pl.multiple_of(peer * ROWS, ROWS), ROWS)
            for t in which:
                pltpu.make_async_remote_copy(
                    src_ref=buf.at[t, slot, peer_rows], dst_ref=acts[t].at[core * SLOTS + slot, :, chip],
                    send_sem=out_send, recv_sem=out_recv.at[t], device_id=(peer,), device_id_type=MESH).start()
            return carry
        lax.fori_loop(1, N_DEV, to, 0)

    def slot_body(slot, carry):
        for t in range(4):
            pltpu.make_async_copy(buf.at[t, slot], buf.at[t, slot], in_recv.at[t, slot]).wait()
        q2 = pltpu.einshape("abc->bac", buf[0, slot])
        for hh in range(PAIR):
            q32 = q2[hh].astype(F32)
            a = (q32 + u_all[hh:hh + 1]).astype(BF16)
            c = (q32 + w_all[hh:hh + 1]).astype(BF16)
            a_s[hh] = a
            c_s[hh] = c
            at_s[hh] = a.T
            ct_s[hh] = flip8(c.astype(F32)).astype(BF16).T
        k2 = pltpu.einshape("abc->bac", buf[1, slot])
        k_s[...] = k2
        g2 = pltpu.einshape("abc->bac", buf[2, slot])
        g_s[...] = g2
        v2 = pltpu.einshape("abc->bac", buf[3, slot])
        v_s[...] = v2
        for hh in range(PAIR):
            kt_s[hh] = k2[hh].T
            gt_s[hh] = g2[hh].T
            vt_s[hh] = v2[hh].T

        def head_body(hh, carry):
            for qb in reversed(range(N_QB)):
                i0 = QB * qb
                width = i0 + QB
                rows = slice(i0, i0 + QB)
                s_ref[:, :width] = dot(a_s[hh, rows, :], kt_s[hh, :, :width])
                e_ref[:, :width] = dot(c_s[hh, rows, :], rt_s[hh, :, SEQ - width:])
                dp_ref[:, :width] = dot(g_s[hh, rows, :], vt_s[hh, :, :width])
                for g in range(QB // 16):
                    r0 = 16 * g
                    group = slice(r0, r0 + 16)
                    rel = pltpu.roll(e_ref[group, :width], i0 + 1 + r0, 1, stride=1, stride_axis=0)
                    s = s_ref[group, :width] + rel
                    ahead = lax.broadcasted_iota(jnp.int32, (16, width), 1) - lax.broadcasted_iota(jnp.int32, (16, width), 0)
                    s = jnp.where(ahead <= i0 + r0, s, -jnp.inf)
                    top = jnp.max(s, axis=1, keepdims=True)
                    p = jnp.exp2((s - top) * (scale * LOG2E))
                    p = p * (1.0 / jnp.sum(p, axis=1, keepdims=True))
                    pb_ref[group, :width] = p.astype(BF16)
                    dp = dp_ref[group, :width]
                    row_dot = jnp.sum(p * dp, axis=1, keepdims=True)
                    ds = (p * (dp - row_dot) * scale).astype(BF16)
                    ds_ref[group, :width] = ds
                    flipped = flip8(ds.astype(F32))
                    half = [pltpu.roll(flipped[8 * j:8 * j + 8], QB - 8 - r0 - 8 * j, 1, stride=1, stride_axis=0) for j in range(2)]
                    dd_ref[group, :width] = jnp.concatenate(half, axis=0).astype(BF16)
                pb = pb_ref[:, :width]
                ds = ds_ref[:, :width]
                dd = dd_ref[:, :width]
                stage[0, hh, rows, :] = dot(pb, v_s[hh, :width, :]).astype(BF16)
                dqc = dot(ds, k_s[hh, :width, :])
                dqr = flip8(dot(dd, rev_s[hh, SEQ - width:, :]))
                stage[1, hh, rows, :] = (dqc + dqr).astype(BF16)
                dr_acc[hh, HEAD:HEAD + 1, :HEAD] += jnp.sum(dqc, axis=0, keepdims=True)
                dr_acc[hh, HEAD + 1:HEAD + 2, :HEAD] += jnp.sum(dqr, axis=0, keepdims=True)
                dk_new = dot(at_s[hh, :, rows], ds)
                dv_new = dot(gt_s[hh, :, rows], pb)
                if qb == N_QB - 1:
                    dkt[...] = dk_new
                    dvt[...] = dv_new
                else:
                    dkt[:, :width] += dk_new
                    dvt[:, :width] += dv_new
                dr_acc[hh, :HEAD, SEQ - width:] += dot(ct_s[hh, :, rows], dd)
            stage[2, hh] = dkt[...].astype(BF16).T
            stage[3, hh] = dvt[...].astype(BF16).T
            return carry

        lax.fori_loop(0, PAIR, head_body, 0)
        for t in range(4):
            buf[t, slot] = pltpu.einshape("abc->bac", stage[t])

        @pl.when(slot < SLOTS - 1)
        def _():
            send_out(slot, range(4))
        return carry

    lax.fori_loop(0, SLOTS, slot_body, 0)

    swap = pltpu.make_async_remote_copy(
        src_ref=dr_acc.at[1 - core], dst_ref=dr_rx, send_sem=x_send, recv_sem=x_recv, device_id=(partner,), device_id_type=MESH)
    swap.start()
    swap.wait()
    head = 2 * chip + core
    total = dr_acc[core] + dr_rx[...]
    rev32 = eye_rev(F32)
    for blk in range(SEQ // HEAD):
        part = total[:HEAD, SEQ - HEAD * (blk + 1):SEQ - HEAD * blk]
        turned = lax.dot_general(rev32, part, (((1,), (1,)), ((), ())), precision=lax.Precision.HIGHEST, preferred_element_type=F32)
        dr_fin[HEAD * blk:HEAD * (blk + 1)] = turned.reshape(HEAD, 1, HEAD)
    dr_fin[SEQ] = total[HEAD:HEAD + 1, :HEAD]
    dr_fin[SEQ + 1] = total[HEAD + 1:HEAD + 2, :HEAD]

    def wait_for(ref, sem):
        pltpu.make_async_copy(ref, ref, sem).wait()

    parts = (dr0_out, dr1_out, dr2_out, dr3_out, dr4_out, dr5_out)

    def block(m, bits):
        if bits == 0:
            start, rows = PARTS[m]
            return dr_fin.at[start:start + rows]
        return parts[m].at[:, 2 * (chip ^ bits) + core]

    def forward(m, bits):
        dst = parts[m].at[:, 2 * (chip ^ bits) + core]
        pltpu.make_async_remote_copy(src_ref=block(m, bits), dst_ref=dst, send_sem=fw_send.at[m], recv_sem=fw_recv.at[m],
                                     device_id=(partner,), device_id_type=MESH).start()

    held = [[0] for _ in range(N_PART)]
    for m in range(N_PART):
        pltpu.make_async_copy(block(m, 0), parts[m].at[:, head], own_sem.at[m]).start()
    for hop in range(3):
        for m in range(N_PART):
            bit = HOPS[m][hop]
            peer = me ^ (2 * bit)
            for bits in held[m]:
                pltpu.make_async_remote_copy(
                    src_ref=block(m, bits), dst_ref=parts[m].at[:, 2 * (chip ^ bits) + core], send_sem=ring_send.at[m],
                    recv_sem=ring_recv.at[hop, m], device_id=(peer,), device_id_type=MESH).start()
        for m in range(N_PART):
            for bits in (held[m] if hop == 0 else held[m][len(held[m]) // 2:]):
                forward(m, bits)
        if hop == 0:
            for j, dst in enumerate((du_out, dw_out)):
                pltpu.make_async_copy(dr_fin.at[SEQ + j], dst.at[head], b_recv.at[j]).start()
                for step in range(1, N_DEV):
                    pltpu.make_async_remote_copy(
                        src_ref=dr_fin.at[SEQ + j], dst_ref=dst.at[head], send_sem=b_send.at[j], recv_sem=b_recv.at[j],
                        device_id=(me ^ step,), device_id_type=MESH).start()
        send_out(SLOTS - 1, ((0, 1), (2,), (3,))[hop])
        for m in range(N_PART):
            count = len(held[m])
            wait_for(parts[m].at[:, :count], ring_recv.at[hop, m])
            held[m] = held[m] + [bits ^ HOPS[m][hop] for bits in held[m]]
    for m in range(N_PART):
        for bits in held[m][4:]:
            forward(m, bits)

    for t, dst in enumerate(acts):
        wait_for(dst, out_recv.at[t])
    for j, dst in enumerate((du_out, dw_out)):
        wait_for(dst, b_recv.at[j])
        wait_for(dst.at[:N_DEV - 1], b_send.at[j])
    wait_for(buf.at[:, :, :SEQ - ROWS], in_send)
    wait_for(buf.at[:, :, :SEQ - ROWS], out_send)
    for m in range(N_PART):
        wait_for(parts[m].at[:, head], own_sem.at[m])
        wait_for(parts[m].at[:, :N_PAIR - 1], ring_send.at[m])
        wait_for(parts[m].at[:, :N_PAIR], fw_send.at[m])
        wait_for(parts[m].at[:, :N_PAIR], fw_recv.at[m])


def writer(*refs):
    ins, (o, dq, dk, dv, dr, du, dw, sem) = refs[:6 + N_PART], refs[6 + N_PART:]
    pairs = list(zip(ins[:4] + ins[-2:], (o, dq, dk, dv, du, dw)))
    for part, (start, rows) in zip(ins[4:-2], PARTS):
        pairs.append((part, dr.at[start:start + rows]))
    copies = [pltpu.make_async_copy(src, dst, sem.at[j]) for j, (src, dst) in enumerate(pairs)]
    for copy in copies:
        copy.start()
    for copy in copies:
        copy.wait()


def solution(mesh):
    n_dev = mesh.shape["cp"]
    seq_spec = P(None, "cp", None, None)

    def local(query, key_in, value, bias_u, bias_w, rel_k, d_out):
        n_batch, rows, n_heads, head_dim = query.shape
        pairs = (n_batch, rows, N_PAIR, PAIR, head_dim)
        vm = pltpu.VMEM
        dma = pltpu.SemaphoreType.DMA
        whole = pl.BlockSpec(memory_space=pl.ANY)
        near = pl.BlockSpec(memory_space=pltpu.VMEM)
        act = jax.ShapeDtypeStruct(pairs, BF16)
        vec = jax.ShapeDtypeStruct((n_heads, 1, head_dim), F32)
        tok = (PAIR, SEQ, HEAD)
        tok_t = (PAIR, HEAD, SEQ)
        outs = pl.pallas_call(
            kernel,
            name="rel_attn",
            out_shape=(act, act, act, act,
                       *[jax.ShapeDtypeStruct((rows, n_heads, 1, head_dim), F32) for _, rows in PARTS],
                       vec, vec),
            in_specs=[whole] * 5 + [near] * 2,
            out_specs=[whole] * (6 + N_PART),
            scratch_shapes=[
                vm((4, SLOTS, SEQ, PAIR, HEAD), BF16),
                vm((SEQ, PAIR, HEAD), BF16), vm((HEAD + 8, SEQ), F32), vm((SEQ + 2, 1, HEAD), F32), vm((PAIR, HEAD + 8, SEQ), F32),
                vm((QB, SEQ), F32), vm((QB, SEQ), F32), vm((QB, SEQ), F32),
                vm((QB, SEQ), BF16), vm((QB, SEQ), BF16), vm((QB, SEQ), BF16),
                vm(tok, BF16), vm(tok, BF16), vm(tok, BF16), vm(tok, BF16), vm(tok, BF16), vm(tok, BF16),
                vm(tok_t, BF16), vm(tok_t, BF16), vm(tok_t, BF16), vm(tok_t, BF16), vm(tok_t, BF16), vm(tok_t, BF16),
                vm((HEAD, SEQ), F32), vm((HEAD, SEQ), F32), vm((4, PAIR, SEQ, HEAD), BF16),
                dma, dma((4, SLOTS)), dma, dma((4,)), dma((N_PART,)), dma, dma, dma, dma((N_PART,)), dma((3, N_PART)), dma((N_PART,)), dma((N_PART,)), dma((2,)), dma((2,)),
            ],
            compiler_params=pltpu.CompilerParams(collective_id=0, has_side_effects=True, vmem_limit_bytes=36 * 1024 * 1024),
        )(query.reshape(pairs), key_in.reshape(pairs), value.reshape(pairs), d_out.reshape(pairs),
          rel_k.reshape(SEQ, N_PAIR, PAIR, head_dim), bias_u.reshape(N_PAIR, PAIR, head_dim), bias_w.reshape(N_PAIR, PAIR, head_dim))
        o, dq, dk, dv, dr, du, dw = pl.pallas_call(
            writer,
            name="writer",
            out_shape=(act, act, act, act, jax.ShapeDtypeStruct((SEQ, n_heads, 1, head_dim), F32), vec, vec),
            in_specs=[whole] * (6 + N_PART),
            out_specs=[whole] * 7,
            scratch_shapes=[dma((6 + N_PART,))],
            compiler_params=pltpu.CompilerParams(vmem_limit_bytes=1024 * 1024),
        )(*outs)
        full = query.shape
        return (o.reshape(full), dq.reshape(full), dk.reshape(full), dv.reshape(full),
                du.reshape(bias_u.shape), dw.reshape(bias_w.shape), dr.reshape(rel_k.shape))

    return jax.shard_map(local, mesh=mesh,
                         in_specs=(seq_spec, seq_spec, seq_spec, P(), P(), P(), seq_spec),
                         out_specs=(seq_spec, seq_spec, seq_spec, seq_spec, P(), P(), P()),
                         check_vma=False)
```

```python
import functools

import jax
import jax.numpy as jnp
from jax import lax
from jax.experimental import pallas as pl
from jax.experimental.pallas import tpu as pltpu
from jax.sharding import PartitionSpec as P

MESH = pl.DeviceIdType.MESH
BF16, F32 = jnp.bfloat16, jnp.float32
LOG2E = 1.4426950408889634

N_DEV = 16
PAIR = 2
N_PAIR = 8
SLOTS = 4
ROWS = 64
SEQ = N_DEV * ROWS
HEAD = 128
QB = 256
N_QB = SEQ // QB
PARTS = ((0, 171), (171, 171), (342, 171), (513, 171), (684, 170), (854, 170))
HOPS = ((1, 2, 4), (2, 4, 1), (4, 1, 2)) * 2
N_PART = len(PARTS)
TURNS = ((1, 3, 5, 7, 6, 2, 4), (7, 5, 3, 1, 2, 6, 4))


def dot(lhs, rhs):
    return jnp.dot(lhs, rhs, preferred_element_type=F32)


def flip8(x):
    rows, cols = x.shape
    idx = 7 - lax.broadcasted_iota(jnp.int32, (rows // 8, 8, cols), 1)
    return jnp.take_along_axis(x.reshape(rows // 8, 8, cols), idx, axis=1).reshape(rows, cols)


def eye_rev(dtype):
    total = lax.broadcasted_iota(jnp.int32, (HEAD, HEAD), 0) + lax.broadcasted_iota(jnp.int32, (HEAD, HEAD), 1)
    return jnp.where(total == HEAD - 1, 1.0, 0.0).astype(dtype)


def kernel(q_in, k_in, v_in, g_in, r_in, u_in, w_in,
           o_out, dq_out, dk_out, dv_out, dr0_out, dr1_out, dr2_out, dr3_out, dr4_out, dr5_out, du_out, dw_out,
           buf, r_buf, dr_rx, dr_fin, dr_acc,
           s_ref, e_ref, dp_ref, pb_ref, ds_ref, dd_ref,
           a_s, c_s, g_s, k_s, v_s, rev_s, kt_s, vt_s, rt_s, at_s, ct_s, gt_s,
           dkt, dvt, stage,
           in_send, in_recv, out_send, out_recv, own_sem, r_sem, x_send, x_recv, ring_send, ring_recv, fw_send, fw_recv, b_send, b_recv):
    me = lax.axis_index("cp")
    core = me % 2
    chip = me // 2
    partner = me + 1 - 2 * core
    scale = HEAD ** -0.5

    r_copy = pltpu.make_async_copy(r_in.at[:, chip], r_buf, r_sem)
    r_copy.start()

    barrier = pltpu.get_barrier_semaphore()

    def say(step, carry):
        pl.semaphore_signal(barrier, inc=1, device_id=((me + step) % N_DEV,), device_id_type=MESH)
        return carry

    lax.fori_loop(1, N_DEV, say, 0)
    pl.semaphore_wait(barrier, N_DEV - 1)

    ins = (q_in, k_in, g_in, v_in)
    my_rows = pl.ds(pl.multiple_of(me * ROWS, ROWS), ROWS)

    def peers():
        for near_turn, far_turn in zip(*TURNS):
            turn = jnp.where(core == 0, near_turn, far_turn)
            yield me ^ (2 * turn)
            yield me ^ (2 * turn + 1)
        yield partner

    def send_in(slot):
        for t, src in enumerate(ins):
            pltpu.make_async_copy(src.at[core * SLOTS + slot, :, chip], buf.at[t, slot, my_rows], in_recv.at[t, slot]).start()

        for peer in peers():
            for t, src in enumerate(ins):
                pltpu.make_async_remote_copy(
                    src_ref=src.at[(peer % 2) * SLOTS + slot, :, peer // 2], dst_ref=buf.at[t, slot, my_rows],
                    send_sem=in_send, recv_sem=in_recv.at[t, slot], device_id=(peer,), device_id_type=MESH).start()

    def send_slot(slot, carry):
        send_in(slot)
        return carry

    lax.fori_loop(0, SLOTS, send_slot, 0)

    r_copy.wait()
    pair_tab = pltpu.einshape("abc->bac", r_buf[...])
    rev = eye_rev(BF16)
    for hh in range(PAIR):
        for blk in range(SEQ // HEAD):
            part = pair_tab[hh, SEQ - HEAD * (blk + 1):SEQ - HEAD * blk]
            flipped = dot(rev, part).astype(BF16)
            rev_s[hh, HEAD * blk:HEAD * (blk + 1), :] = flipped
            rt_s[hh, :, HEAD * blk:HEAD * (blk + 1)] = flipped.T
    dr_acc[...] = jnp.zeros_like(dr_acc)

    u_all = u_in[chip].astype(F32)
    w_all = w_in[chip].astype(F32)

    acts = (o_out, dq_out, dk_out, dv_out)

    def send_out(slot, which):
        for t in which:
            pltpu.make_async_copy(buf.at[t, slot, my_rows], acts[t].at[core * SLOTS + slot, :, chip], out_recv.at[t]).start()

        for peer in peers():
            peer_rows = pl.ds(pl.multiple_of(peer * ROWS, ROWS), ROWS)
            for t in which:
                pltpu.make_async_remote_copy(
                    src_ref=buf.at[t, slot, peer_rows], dst_ref=acts[t].at[core * SLOTS + slot, :, chip],
                    send_sem=out_send, recv_sem=out_recv.at[t], device_id=(peer,), device_id_type=MESH).start()

    def slot_body(slot, carry):
        for t in range(4):
            pltpu.make_async_copy(buf.at[t, slot], buf.at[t, slot], in_recv.at[t, slot]).wait()
        q2 = pltpu.einshape("abc->bac", buf[0, slot])
        for hh in range(PAIR):
            q32 = q2[hh].astype(F32)
            a = (q32 + u_all[hh:hh + 1]).astype(BF16)
            c = (q32 + w_all[hh:hh + 1]).astype(BF16)
            a_s[hh] = a
            c_s[hh] = c
            at_s[hh] = a.T
            ct_s[hh] = flip8(c.astype(F32)).astype(BF16).T
        k2 = pltpu.einshape("abc->bac", buf[1, slot])
        k_s[...] = k2
        g2 = pltpu.einshape("abc->bac", buf[2, slot])
        g_s[...] = g2
        v2 = pltpu.einshape("abc->bac", buf[3, slot])
        v_s[...] = v2
        for hh in range(PAIR):
            kt_s[hh] = k2[hh].T
            gt_s[hh] = g2[hh].T
            vt_s[hh] = v2[hh].T

        def head_body(hh, carry):
            for qb in reversed(range(N_QB)):
                i0 = QB * qb
                width = i0 + QB
                rows = slice(i0, i0 + QB)
                s_ref[:, :width] = dot(a_s[hh, rows, :], kt_s[hh, :, :width])
                e_ref[:, :width] = dot(c_s[hh, rows, :], rt_s[hh, :, SEQ - width:])
                dp_ref[:, :width] = dot(g_s[hh, rows, :], vt_s[hh, :, :width])
                for g in range(QB // 16):
                    r0 = 16 * g
                    group = slice(r0, r0 + 16)
                    rel = pltpu.roll(e_ref[group, :width], i0 + 1 + r0, 1, stride=1, stride_axis=0)
                    s = s_ref[group, :width] + rel
                    ahead = lax.broadcasted_iota(jnp.int32, (16, width), 1) - lax.broadcasted_iota(jnp.int32, (16, width), 0)
                    s = jnp.where(ahead <= i0 + r0, s, -jnp.inf)
                    top = jnp.max(s, axis=1, keepdims=True)
                    p = jnp.exp2((s - top) * (scale * LOG2E))
                    p = p * (1.0 / jnp.sum(p, axis=1, keepdims=True))
                    pb_ref[group, :width] = p.astype(BF16)
                    dp = dp_ref[group, :width]
                    row_dot = jnp.sum(p * dp, axis=1, keepdims=True)
                    ds = (p * (dp - row_dot) * scale).astype(BF16)
                    ds_ref[group, :width] = ds
                    flipped = flip8(ds.astype(F32))
                    half = [pltpu.roll(flipped[8 * j:8 * j + 8], QB - 8 - r0 - 8 * j, 1, stride=1, stride_axis=0) for j in range(2)]
                    dd_ref[group, :width] = jnp.concatenate(half, axis=0).astype(BF16)
                pb = pb_ref[:, :width]
                ds = ds_ref[:, :width]
                dd = dd_ref[:, :width]
                stage[0, hh, rows, :] = dot(pb, v_s[hh, :width, :]).astype(BF16)
                dqc = dot(ds, k_s[hh, :width, :])
                dqr = flip8(dot(dd, rev_s[hh, SEQ - width:, :]))
                stage[1, hh, rows, :] = (dqc + dqr).astype(BF16)
                dr_acc[hh, HEAD:HEAD + 1, :HEAD] += jnp.sum(dqc, axis=0, keepdims=True)
                dr_acc[hh, HEAD + 1:HEAD + 2, :HEAD] += jnp.sum(dqr, axis=0, keepdims=True)
                dk_new = dot(at_s[hh, :, rows], ds)
                dv_new = dot(gt_s[hh, :, rows], pb)
                if qb == N_QB - 1:
                    dkt[...] = dk_new
                    dvt[...] = dv_new
                else:
                    dkt[:, :width] += dk_new
                    dvt[:, :width] += dv_new
                dr_acc[hh, :HEAD, SEQ - width:] += dot(ct_s[hh, :, rows], dd)
            stage[2, hh] = dkt[...].astype(BF16).T
            stage[3, hh] = dvt[...].astype(BF16).T
            return carry

        lax.fori_loop(0, PAIR, head_body, 0)
        for t in range(4):
            buf[t, slot] = pltpu.einshape("abc->bac", stage[t])

        @pl.when(slot < SLOTS - 1)
        def _():
            send_out(slot, range(4))
        return carry

    lax.fori_loop(0, SLOTS, slot_body, 0)

    swap = pltpu.make_async_remote_copy(
        src_ref=dr_acc.at[1 - core], dst_ref=dr_rx, send_sem=x_send, recv_sem=x_recv, device_id=(partner,), device_id_type=MESH)
    swap.start()
    swap.wait()
    head = 2 * chip + core
    total = dr_acc[core] + dr_rx[...]
    rev32 = eye_rev(F32)
    for blk in range(SEQ // HEAD):
        part = total[:HEAD, SEQ - HEAD * (blk + 1):SEQ - HEAD * blk]
        turned = lax.dot_general(rev32, part, (((1,), (1,)), ((), ())), precision=lax.Precision.HIGHEST, preferred_element_type=F32)
        dr_fin[HEAD * blk:HEAD * (blk + 1)] = turned.reshape(HEAD, 1, HEAD)
    dr_fin[SEQ] = total[HEAD:HEAD + 1, :HEAD]
    dr_fin[SEQ + 1] = total[HEAD + 1:HEAD + 2, :HEAD]

    def wait_for(ref, sem):
        pltpu.make_async_copy(ref, ref, sem).wait()

    parts = (dr0_out, dr1_out, dr2_out, dr3_out, dr4_out, dr5_out)

    def block(m, bits):
        if bits == 0:
            start, rows = PARTS[m]
            return dr_fin.at[start:start + rows]
        return parts[m].at[:, 2 * (chip ^ bits) + core]

    def forward(m, bits):
        dst = parts[m].at[:, 2 * (chip ^ bits) + core]
        pltpu.make_async_remote_copy(src_ref=block(m, bits), dst_ref=dst, send_sem=fw_send.at[m], recv_sem=fw_recv.at[m],
                                     device_id=(partner,), device_id_type=MESH).start()

    held = [[0] for _ in range(N_PART)]
    for m in range(N_PART):
        pltpu.make_async_copy(block(m, 0), parts[m].at[:, head], own_sem.at[m]).start()
    for hop in range(3):
        for m in range(N_PART):
            bit = HOPS[m][hop]
            peer = me ^ (2 * bit)
            for bits in held[m]:
                pltpu.make_async_remote_copy(
                    src_ref=block(m, bits), dst_ref=parts[m].at[:, 2 * (chip ^ bits) + core], send_sem=ring_send.at[m],
                    recv_sem=ring_recv.at[hop, m], device_id=(peer,), device_id_type=MESH).start()
        for m in range(N_PART):
            for bits in (held[m] if hop == 0 else held[m][len(held[m]) // 2:]):
                forward(m, bits)
        if hop == 0:
            for j, dst in enumerate((du_out, dw_out)):
                pltpu.make_async_copy(dr_fin.at[SEQ + j], dst.at[head], b_recv.at[j]).start()
                for step in range(1, N_DEV):
                    pltpu.make_async_remote_copy(
                        src_ref=dr_fin.at[SEQ + j], dst_ref=dst.at[head], send_sem=b_send.at[j], recv_sem=b_recv.at[j],
                        device_id=(me ^ step,), device_id_type=MESH).start()
        send_out(SLOTS - 1, ((0, 1), (2,), (3,))[hop])
        for m in range(N_PART):
            count = len(held[m])
            wait_for(parts[m].at[:, :count], ring_recv.at[hop, m])
            held[m] = held[m] + [bits ^ HOPS[m][hop] for bits in held[m]]
    for m in range(N_PART):
        for bits in held[m][4:]:
            forward(m, bits)

    for t, dst in enumerate(acts):
        wait_for(dst, out_recv.at[t])
    for j, dst in enumerate((du_out, dw_out)):
        wait_for(dst, b_recv.at[j])
        wait_for(dst.at[:N_DEV - 1], b_send.at[j])
    wait_for(buf.at[:, :, :SEQ - ROWS], in_send)
    wait_for(buf.at[:, :, :SEQ - ROWS], out_send)
    for m in range(N_PART):
        wait_for(parts[m].at[:, head], own_sem.at[m])
        wait_for(parts[m].at[:, :N_PAIR - 1], ring_send.at[m])
        wait_for(parts[m].at[:, :N_PAIR], fw_send.at[m])
        wait_for(parts[m].at[:, :N_PAIR], fw_recv.at[m])


def writer(*refs):
    ins, (o, dq, dk, dv, dr, du, dw, sem) = refs[:6 + N_PART], refs[6 + N_PART:]
    pairs = list(zip(ins[:4] + ins[-2:], (o, dq, dk, dv, du, dw)))
    for part, (start, rows) in zip(ins[4:-2], PARTS):
        pairs.append((part, dr.at[start:start + rows]))
    copies = [pltpu.make_async_copy(src, dst, sem.at[j]) for j, (src, dst) in enumerate(pairs)]
    for copy in copies:
        copy.start()
    for copy in copies:
        copy.wait()


def solution(mesh):
    n_dev = mesh.shape["cp"]
    seq_spec = P(None, "cp", None, None)

    def local(query, key_in, value, bias_u, bias_w, rel_k, d_out):
        n_batch, rows, n_heads, head_dim = query.shape
        pairs = (n_batch, rows, N_PAIR, PAIR, head_dim)
        vm = pltpu.VMEM
        dma = pltpu.SemaphoreType.DMA
        whole = pl.BlockSpec(memory_space=pl.ANY)
        near = pl.BlockSpec(memory_space=pltpu.VMEM)
        act = jax.ShapeDtypeStruct(pairs, BF16)
        vec = jax.ShapeDtypeStruct((n_heads, 1, head_dim), F32)
        tok = (PAIR, SEQ, HEAD)
        tok_t = (PAIR, HEAD, SEQ)
        outs = pl.pallas_call(
            kernel,
            name="rel_attn",
            out_shape=(act, act, act, act,
                       *[jax.ShapeDtypeStruct((rows, n_heads, 1, head_dim), F32) for _, rows in PARTS],
                       vec, vec),
            in_specs=[whole] * 5 + [near] * 2,
            out_specs=[whole] * (6 + N_PART),
            scratch_shapes=[
                vm((4, SLOTS, SEQ, PAIR, HEAD), BF16),
                vm((SEQ, PAIR, HEAD), BF16), vm((HEAD + 8, SEQ), F32), vm((SEQ + 2, 1, HEAD), F32), vm((PAIR, HEAD + 8, SEQ), F32),
                vm((QB, SEQ), F32), vm((QB, SEQ), F32), vm((QB, SEQ), F32),
                vm((QB, SEQ), BF16), vm((QB, SEQ), BF16), vm((QB, SEQ), BF16),
                vm(tok, BF16), vm(tok, BF16), vm(tok, BF16), vm(tok, BF16), vm(tok, BF16), vm(tok, BF16),
                vm(tok_t, BF16), vm(tok_t, BF16), vm(tok_t, BF16), vm(tok_t, BF16), vm(tok_t, BF16), vm(tok_t, BF16),
                vm((HEAD, SEQ), F32), vm((HEAD, SEQ), F32), vm((4, PAIR, SEQ, HEAD), BF16),
                dma, dma((4, SLOTS)), dma, dma((4,)), dma((N_PART,)), dma, dma, dma, dma((N_PART,)), dma((3, N_PART)), dma((N_PART,)), dma((N_PART,)), dma((2,)), dma((2,)),
            ],
            compiler_params=pltpu.CompilerParams(collective_id=0, has_side_effects=True, vmem_limit_bytes=36 * 1024 * 1024),
        )(query.reshape(pairs), key_in.reshape(pairs), value.reshape(pairs), d_out.reshape(pairs),
          rel_k.reshape(SEQ, N_PAIR, PAIR, head_dim), bias_u.reshape(N_PAIR, PAIR, head_dim), bias_w.reshape(N_PAIR, PAIR, head_dim))
        o, dq, dk, dv, dr, du, dw = pl.pallas_call(
            writer,
            name="writer",
            out_shape=(act, act, act, act, jax.ShapeDtypeStruct((SEQ, n_heads, 1, head_dim), F32), vec, vec),
            in_specs=[whole] * (6 + N_PART),
            out_specs=[whole] * 7,
            scratch_shapes=[dma((6 + N_PART,))],
            compiler_params=pltpu.CompilerParams(vmem_limit_bytes=1024 * 1024),
        )(*outs)
        full = query.shape
        return (o.reshape(full), dq.reshape(full), dk.reshape(full), dv.reshape(full),
                du.reshape(bias_u.shape), dw.reshape(bias_w.shape), dr.reshape(rel_k.shape))

    return jax.shard_map(local, mesh=mesh,
                         in_specs=(seq_spec, seq_spec, seq_spec, P(), P(), P(), seq_spec),
                         out_specs=(seq_spec, seq_spec, seq_spec, seq_spec, P(), P(), P()),
                         check_vma=False)
```

```python
import functools

import jax
import jax.numpy as jnp
from jax import lax
from jax.experimental import pallas as pl
from jax.experimental.pallas import tpu as pltpu
from jax.sharding import PartitionSpec as P

MESH = pl.DeviceIdType.MESH
BF16, F32 = jnp.bfloat16, jnp.float32
LOG2E = 1.4426950408889634

N_DEV = 16
PAIR = 2
N_PAIR = 8
SLOTS = 4
ROWS = 64
SEQ = N_DEV * ROWS
HEAD = 128
QB = 256
N_QB = SEQ // QB
PARTS = ((0, 171), (171, 171), (342, 171), (513, 171), (684, 170), (854, 170))
HOPS = ((1, 2, 4), (2, 4, 1), (4, 1, 2)) * 2
N_PART = len(PARTS)
TURNS = ((1, 3, 5, 7, 6, 2, 4), (7, 5, 3, 1, 2, 6, 4))


def dot(lhs, rhs):
    return jnp.dot(lhs, rhs, preferred_element_type=F32)


def flip8(x):
    rows, cols = x.shape
    idx = 7 - lax.broadcasted_iota(jnp.int32, (rows // 8, 8, cols), 1)
    return jnp.take_along_axis(x.reshape(rows // 8, 8, cols), idx, axis=1).reshape(rows, cols)


def eye_rev(dtype):
    total = lax.broadcasted_iota(jnp.int32, (HEAD, HEAD), 0) + lax.broadcasted_iota(jnp.int32, (HEAD, HEAD), 1)
    return jnp.where(total == HEAD - 1, 1.0, 0.0).astype(dtype)


def kernel(q_in, k_in, v_in, g_in, r_in, u_in, w_in,
           o_out, dq_out, dk_out, dv_out, dr0_out, dr1_out, dr2_out, dr3_out, dr4_out, dr5_out, du_out, dw_out,
           buf, r_buf, u_buf, w_buf, dr_rx, dr_fin, dr_acc,
           s_ref, e_ref, dp_ref, pb_ref, ds_ref, dd_ref,
           a_s, c_s, g_s, k_s, v_s, rev_s, kt_s, vt_s, rt_s, at_s, ct_s, gt_s,
           dkt, dvt, stage,
           in_send, in_recv, out_send, out_recv, own_sem, r_sem, x_send, x_recv, ring_send, ring_recv, fw_send, fw_recv, b_send, b_recv):
    me = lax.axis_index("cp")
    core = me % 2
    chip = me // 2
    partner = me + 1 - 2 * core
    scale = HEAD ** -0.5

    tables = [pltpu.make_async_copy(src, dst, r_sem.at[j]) for j, (src, dst) in enumerate(
        ((r_in.at[:, chip], r_buf), (u_in.at[chip], u_buf), (w_in.at[chip], w_buf)))]
    for copy in tables:
        copy.start()

    barrier = pltpu.get_barrier_semaphore()

    def say(step, carry):
        pl.semaphore_signal(barrier, inc=1, device_id=((me + step) % N_DEV,), device_id_type=MESH)
        return carry

    lax.fori_loop(1, N_DEV, say, 0)
    pl.semaphore_wait(barrier, N_DEV - 1)

    ins = (q_in, k_in, g_in, v_in)
    my_rows = pl.ds(pl.multiple_of(me * ROWS, ROWS), ROWS)

    def peers():
        for near_turn, far_turn in zip(*TURNS):
            turn = jnp.where(core == 0, near_turn, far_turn)
            yield me ^ (2 * turn)
            yield me ^ (2 * turn + 1)
        yield partner

    def send_in(slot):
        for t, src in enumerate(ins):
            pltpu.make_async_copy(src.at[core * SLOTS + slot, :, chip], buf.at[t, slot, my_rows], in_recv.at[t, slot]).start()

        for peer in peers():
            for t, src in enumerate(ins):
                pltpu.make_async_remote_copy(
                    src_ref=src.at[(peer % 2) * SLOTS + slot, :, peer // 2], dst_ref=buf.at[t, slot, my_rows],
                    send_sem=in_send, recv_sem=in_recv.at[t, slot], device_id=(peer,), device_id_type=MESH).start()

    def send_slot(slot, carry):
        send_in(slot)
        return carry

    lax.fori_loop(0, SLOTS, send_slot, 0)

    for copy in tables:
        copy.wait()
    pair_tab = pltpu.einshape("abc->bac", r_buf[...])
    rev = eye_rev(BF16)
    for hh in range(PAIR):
        for blk in range(SEQ // HEAD):
            part = pair_tab[hh, SEQ - HEAD * (blk + 1):SEQ - HEAD * blk]
            flipped = dot(rev, part).astype(BF16)
            rev_s[hh, HEAD * blk:HEAD * (blk + 1), :] = flipped
            rt_s[hh, :, HEAD * blk:HEAD * (blk + 1)] = flipped.T
    dr_acc[...] = jnp.zeros_like(dr_acc)

    u_all = u_buf[...].astype(F32)
    w_all = w_buf[...].astype(F32)

    acts = (o_out, dq_out, dk_out, dv_out)

    def send_out(slot, which):
        for t in which:
            pltpu.make_async_copy(buf.at[t, slot, my_rows], acts[t].at[core * SLOTS + slot, :, chip], out_recv.at[t]).start()

        for peer in peers():
            peer_rows = pl.ds(pl.multiple_of(peer * ROWS, ROWS), ROWS)
            for t in which:
                pltpu.make_async_remote_copy(
                    src_ref=buf.at[t, slot, peer_rows], dst_ref=acts[t].at[core * SLOTS + slot, :, chip],
                    send_sem=out_send, recv_sem=out_recv.at[t], device_id=(peer,), device_id_type=MESH).start()

    def slot_body(slot, carry):
        for t in range(4):
            pltpu.make_async_copy(buf.at[t, slot], buf.at[t, slot], in_recv.at[t, slot]).wait()
        q2 = pltpu.einshape("abc->bac", buf[0, slot])
        for hh in range(PAIR):
            q32 = q2[hh].astype(F32)
            a = (q32 + u_all[hh:hh + 1]).astype(BF16)
            c = (q32 + w_all[hh:hh + 1]).astype(BF16)
            a_s[hh] = a
            c_s[hh] = c
            at_s[hh] = a.T
            ct_s[hh] = flip8(c.astype(F32)).astype(BF16).T
        k2 = pltpu.einshape("abc->bac", buf[1, slot])
        k_s[...] = k2
        g2 = pltpu.einshape("abc->bac", buf[2, slot])
        g_s[...] = g2
        v2 = pltpu.einshape("abc->bac", buf[3, slot])
        v_s[...] = v2
        for hh in range(PAIR):
            kt_s[hh] = k2[hh].T
            gt_s[hh] = g2[hh].T
            vt_s[hh] = v2[hh].T

        def head_body(hh, carry):
            for qb in reversed(range(N_QB)):
                i0 = QB * qb
                width = i0 + QB
                rows = slice(i0, i0 + QB)
                s_ref[:, :width] = dot(a_s[hh, rows, :], kt_s[hh, :, :width])
                e_ref[:, :width] = dot(c_s[hh, rows, :], rt_s[hh, :, SEQ - width:])
                dp_ref[:, :width] = dot(g_s[hh, rows, :], vt_s[hh, :, :width])
                for g in range(QB // 16):
                    r0 = 16 * g
                    group = slice(r0, r0 + 16)
                    rel = pltpu.roll(e_ref[group, :width], i0 + 1 + r0, 1, stride=1, stride_axis=0)
                    s = s_ref[group, :width] + rel
                    ahead = lax.broadcasted_iota(jnp.int32, (16, width), 1) - lax.broadcasted_iota(jnp.int32, (16, width), 0)
                    s = jnp.where(ahead <= i0 + r0, s, -jnp.inf)
                    top = jnp.max(s, axis=1, keepdims=True)
                    p = jnp.exp2((s - top) * (scale * LOG2E))
                    p = p * (1.0 / jnp.sum(p, axis=1, keepdims=True))
                    pb_ref[group, :width] = p.astype(BF16)
                    dp = dp_ref[group, :width]
                    row_dot = jnp.sum(p * dp, axis=1, keepdims=True)
                    ds = (p * (dp - row_dot) * scale).astype(BF16)
                    ds_ref[group, :width] = ds
                    flipped = flip8(ds.astype(F32))
                    half = [pltpu.roll(flipped[8 * j:8 * j + 8], QB - 8 - r0 - 8 * j, 1, stride=1, stride_axis=0) for j in range(2)]
                    dd_ref[group, :width] = jnp.concatenate(half, axis=0).astype(BF16)
                pb = pb_ref[:, :width]
                ds = ds_ref[:, :width]
                dd = dd_ref[:, :width]
                stage[0, hh, rows, :] = dot(pb, v_s[hh, :width, :]).astype(BF16)
                dqc = dot(ds, k_s[hh, :width, :])
                dqr = flip8(dot(dd, rev_s[hh, SEQ - width:, :]))
                stage[1, hh, rows, :] = (dqc + dqr).astype(BF16)
                dr_acc[hh, HEAD:HEAD + 1, :HEAD] += jnp.sum(dqc, axis=0, keepdims=True)
                dr_acc[hh, HEAD + 1:HEAD + 2, :HEAD] += jnp.sum(dqr, axis=0, keepdims=True)
                dk_new = dot(at_s[hh, :, rows], ds)
                dv_new = dot(gt_s[hh, :, rows], pb)
                if qb == N_QB - 1:
                    dkt[...] = dk_new
                    dvt[...] = dv_new
                else:
                    dkt[:, :width] += dk_new
                    dvt[:, :width] += dv_new
                dr_acc[hh, :HEAD, SEQ - width:] += dot(ct_s[hh, :, rows], dd)
            stage[2, hh] = dkt[...].astype(BF16).T
            stage[3, hh] = dvt[...].astype(BF16).T
            return carry

        lax.fori_loop(0, PAIR, head_body, 0)
        for t in range(4):
            buf[t, slot] = pltpu.einshape("abc->bac", stage[t])

        @pl.when(slot < SLOTS - 1)
        def _():
            send_out(slot, range(4))
        return carry

    lax.fori_loop(0, SLOTS, slot_body, 0)

    swap = pltpu.make_async_remote_copy(
        src_ref=dr_acc.at[1 - core], dst_ref=dr_rx, send_sem=x_send, recv_sem=x_recv, device_id=(partner,), device_id_type=MESH)
    swap.start()
    swap.wait()
    head = 2 * chip + core
    total = dr_acc[core] + dr_rx[...]
    rev32 = eye_rev(F32)
    for blk in range(SEQ // HEAD):
        part = total[:HEAD, SEQ - HEAD * (blk + 1):SEQ - HEAD * blk]
        turned = lax.dot_general(rev32, part, (((1,), (1,)), ((), ())), precision=lax.Precision.HIGHEST, preferred_element_type=F32)
        dr_fin[HEAD * blk:HEAD * (blk + 1)] = turned.reshape(HEAD, 1, HEAD)
    dr_fin[SEQ] = total[HEAD:HEAD + 1, :HEAD]
    dr_fin[SEQ + 1] = total[HEAD + 1:HEAD + 2, :HEAD]

    def wait_for(ref, sem):
        pltpu.make_async_copy(ref, ref, sem).wait()

    parts = (dr0_out, dr1_out, dr2_out, dr3_out, dr4_out, dr5_out)

    def block(m, bits):
        if bits == 0:
            start, rows = PARTS[m]
            return dr_fin.at[start:start + rows]
        return parts[m].at[:, 2 * (chip ^ bits) + core]

    def forward(m, bits):
        dst = parts[m].at[:, 2 * (chip ^ bits) + core]
        pltpu.make_async_remote_copy(src_ref=block(m, bits), dst_ref=dst, send_sem=fw_send.at[m], recv_sem=fw_recv.at[m],
                                     device_id=(partner,), device_id_type=MESH).start()

    held = [[0] for _ in range(N_PART)]
    for m in range(N_PART):
        pltpu.make_async_copy(block(m, 0), parts[m].at[:, head], own_sem.at[m]).start()
    for hop in range(3):
        for m in range(N_PART):
            bit = HOPS[m][hop]
            peer = me ^ (2 * bit)
            for bits in held[m]:
                pltpu.make_async_remote_copy(
                    src_ref=block(m, bits), dst_ref=parts[m].at[:, 2 * (chip ^ bits) + core], send_sem=ring_send.at[m],
                    recv_sem=ring_recv.at[hop, m], device_id=(peer,), device_id_type=MESH).start()
        for m in range(N_PART):
            for bits in (held[m] if hop == 0 else held[m][len(held[m]) // 2:]):
                forward(m, bits)
        if hop == 0:
            for j, dst in enumerate((du_out, dw_out)):
                pltpu.make_async_copy(dr_fin.at[SEQ + j], dst.at[head], b_recv.at[j]).start()
                for step in range(1, N_DEV):
                    pltpu.make_async_remote_copy(
                        src_ref=dr_fin.at[SEQ + j], dst_ref=dst.at[head], send_sem=b_send.at[j], recv_sem=b_recv.at[j],
                        device_id=(me ^ step,), device_id_type=MESH).start()
        send_out(SLOTS - 1, ((0,), (1,), (2, 3))[hop])
        for m in range(N_PART):
            count = len(held[m])
            wait_for(parts[m].at[:, :count], ring_recv.at[hop, m])
            held[m] = held[m] + [bits ^ HOPS[m][hop] for bits in held[m]]
            if hop == 2:
                for bits in held[m][4:]:
                    forward(m, bits)

    for t, dst in enumerate(acts):
        wait_for(dst, out_recv.at[t])
    for j, dst in enumerate((du_out, dw_out)):
        wait_for(dst, b_recv.at[j])
        wait_for(dst.at[:N_DEV - 1], b_send.at[j])
    wait_for(buf.at[:, :, :SEQ - ROWS], in_send)
    wait_for(buf.at[:, :, :SEQ - ROWS], out_send)
    for m in range(N_PART):
        wait_for(parts[m].at[:, head], own_sem.at[m])
        wait_for(parts[m].at[:, :N_PAIR - 1], ring_send.at[m])
        wait_for(parts[m].at[:, :N_PAIR], fw_send.at[m])
        wait_for(parts[m].at[:, :N_PAIR], fw_recv.at[m])


def writer(*refs):
    ins, (o, dq, dk, dv, dr, du, dw, sem) = refs[:6 + N_PART], refs[6 + N_PART:]
    pairs = list(zip(ins[:4] + ins[-2:], (o, dq, dk, dv, du, dw)))
    for part, (start, rows) in zip(ins[4:-2], PARTS):
        pairs.append((part, dr.at[start:start + rows]))
    copies = [pltpu.make_async_copy(src, dst, sem.at[j]) for j, (src, dst) in enumerate(pairs)]
    for copy in copies:
        copy.start()
    for copy in copies:
        copy.wait()


def solution(mesh):
    n_dev = mesh.shape["cp"]
    seq_spec = P(None, "cp", None, None)

    def local(query, key_in, value, bias_u, bias_w, rel_k, d_out):
        n_batch, rows, n_heads, head_dim = query.shape
        pairs = (n_batch, rows, N_PAIR, PAIR, head_dim)
        vm = pltpu.VMEM
        dma = pltpu.SemaphoreType.DMA
        whole = pl.BlockSpec(memory_space=pl.ANY)
        act = jax.ShapeDtypeStruct(pairs, BF16)
        vec = jax.ShapeDtypeStruct((n_heads, 1, head_dim), F32)
        tok = (PAIR, SEQ, HEAD)
        tok_t = (PAIR, HEAD, SEQ)
        outs = pl.pallas_call(
            kernel,
            name="rel_attn",
            out_shape=(act, act, act, act,
                       *[jax.ShapeDtypeStruct((rows, n_heads, 1, head_dim), F32) for _, rows in PARTS],
                       vec, vec),
            in_specs=[pl.BlockSpec(memory_space=pltpu.HBM)] * 7,
            out_specs=[whole] * (6 + N_PART),
            scratch_shapes=[
                vm((4, SLOTS, SEQ, PAIR, HEAD), BF16),
                vm((SEQ, PAIR, HEAD), BF16), vm((PAIR, HEAD), BF16), vm((PAIR, HEAD), BF16), vm((HEAD + 8, SEQ), F32), vm((SEQ + 2, 1, HEAD), F32), vm((PAIR, HEAD + 8, SEQ), F32),
                vm((QB, SEQ), F32), vm((QB, SEQ), F32), vm((QB, SEQ), F32),
                vm((QB, SEQ), BF16), vm((QB, SEQ), BF16), vm((QB, SEQ), BF16),
                vm(tok, BF16), vm(tok, BF16), vm(tok, BF16), vm(tok, BF16), vm(tok, BF16), vm(tok, BF16),
                vm(tok_t, BF16), vm(tok_t, BF16), vm(tok_t, BF16), vm(tok_t, BF16), vm(tok_t, BF16), vm(tok_t, BF16),
                vm((HEAD, SEQ), F32), vm((HEAD, SEQ), F32), vm((4, PAIR, SEQ, HEAD), BF16),
                dma, dma((4, SLOTS)), dma, dma((4,)), dma((N_PART,)), dma((3,)), dma, dma, dma((N_PART,)), dma((3, N_PART)), dma((N_PART,)), dma((N_PART,)), dma((2,)), dma((2,)),
            ],
            compiler_params=pltpu.CompilerParams(collective_id=0, has_side_effects=True, vmem_limit_bytes=36 * 1024 * 1024),
        )(*[pltpu.with_memory_space_constraint(x, pltpu.HBM) for x in (
            query.reshape(pairs), key_in.reshape(pairs), value.reshape(pairs), d_out.reshape(pairs),
            rel_k.reshape(SEQ, N_PAIR, PAIR, head_dim), bias_u.reshape(N_PAIR, PAIR, head_dim), bias_w.reshape(N_PAIR, PAIR, head_dim))])
        o, dq, dk, dv, dr, du, dw = pl.pallas_call(
            writer,
            name="writer",
            out_shape=(act, act, act, act, jax.ShapeDtypeStruct((SEQ, n_heads, 1, head_dim), F32), vec, vec),
            in_specs=[whole] * (6 + N_PART),
            out_specs=[whole] * 7,
            scratch_shapes=[dma((6 + N_PART,))],
            compiler_params=pltpu.CompilerParams(vmem_limit_bytes=1024 * 1024),
        )(*outs)
        full = query.shape
        return (o.reshape(full), dq.reshape(full), dk.reshape(full), dv.reshape(full),
                du.reshape(bias_u.shape), dw.reshape(bias_w.shape), dr.reshape(rel_k.shape))

    return jax.shard_map(local, mesh=mesh,
                         in_specs=(seq_spec, seq_spec, seq_spec, P(), P(), P(), seq_spec),
                         out_specs=(seq_spec, seq_spec, seq_spec, seq_spec, P(), P(), P()),
                         check_vma=False)
```

```python
import jax
import jax.numpy as jnp
from jax import lax
from jax.experimental import pallas as pl
from jax.experimental.pallas import tpu as pltpu
from jax.sharding import PartitionSpec as P

MESH = pl.DeviceIdType.MESH
BF16, F32 = jnp.bfloat16, jnp.float32
LOG2E = 1.4426950408889634

N_DEV = 16
PLANE = 8
PAIR = 2
N_PAIR = 8
SLOTS = 4
ROWS = 64
HALF = PLANE * ROWS
SEQ = 2 * HALF
HEAD = 128
QB = 256
WIN = HALF + QB
PARTS = ((0, 171), (171, 171), (342, 171), (513, 171), (684, 170), (854, 170))
HOPS = ((1, 2, 4), (2, 1, 4), (1, 2, 4), (2, 1, 4), (4, 1, 2), (4, 2, 1))
N_PART = len(PARTS)
TURNS = ((1, 3, 2), (3, 1, 2))


def dot(lhs, rhs):
    return jnp.dot(lhs, rhs, preferred_element_type=F32)


def flip8(x):
    rows, cols = x.shape
    idx = 7 - lax.broadcasted_iota(jnp.int32, (rows // 8, 8, cols), 1)
    return jnp.take_along_axis(x.reshape(rows // 8, 8, cols), idx, axis=1).reshape(rows, cols)


def eye_rev(dtype):
    total = lax.broadcasted_iota(jnp.int32, (HEAD, HEAD), 0) + lax.broadcasted_iota(jnp.int32, (HEAD, HEAD), 1)
    return jnp.where(total == HEAD - 1, 1.0, 0.0).astype(dtype)


def kernel(q_in, k_in, v_in, g_in, r_in, u_in, w_in,
           o_out, dq_out, dk_out, dv_out, dr0_out, dr1_out, dr2_out, dr3_out, dr4_out, dr5_out, du_out, dw_out,
           buf, rbuf, r_buf, u_buf, w_buf, st_tx, st_rx, st_ref, dr_rx, dr_rz, dr_fin, dr_acc,
           s_ref, e_ref, dp_ref, pb_ref, ds_ref, dd_ref,
           a_s, c_s, g_s, k_s, v_s, at_s, ct_s, gt_s, kt_s, vt_s, rev_s, rt_s, dkt, dvt, stage,
           in_send, in_recv, out_send, out_recv, own_sem, r_sem, up_send, up_recv, st_send, st_recv,
           x_send, x_recv, z_send, z_recv, ring_send, ring_recv, fw_send, fw_recv, b_send, b_recv):
    me = lax.axis_index("cp")
    core = me % 2
    chip = me // 2
    col = chip % 4
    z = chip // 4
    partner = me + 1 - 2 * core
    across = me + PLANE * (1 - 2 * z)
    scale = HEAD ** -0.5

    def wait_for(ref, sem):
        pltpu.make_async_copy(ref, ref, sem).wait()

    tables = [pltpu.make_async_copy(src, dst, r_sem.at[j]) for j, (src, dst) in enumerate(
        ((r_in.at[:, pl.ds(2 * col, 2)], r_buf), (u_in.at[pl.ds(2 * col, 2)], u_buf), (w_in.at[pl.ds(2 * col, 2)], w_buf)))]
    for copy in tables:
        copy.start()
    dr_rz[...] = jnp.zeros_like(dr_rz)

    barrier = pltpu.get_barrier_semaphore()

    def say(step, carry):
        pl.semaphore_signal(barrier, inc=1, device_id=((me + step) % N_DEV,), device_id_type=MESH)
        return carry

    lax.fori_loop(1, N_DEV, say, 0)
    pl.semaphore_wait(barrier, N_DEV - 1)

    my_rows = pl.ds(pl.multiple_of((me % PLANE) * ROWS, ROWS), ROWS)

    def peers():
        for near_turn, far_turn in zip(*TURNS):
            turn = jnp.where(core == 0, near_turn, far_turn)
            yield me ^ (2 * turn)
            yield me ^ (2 * turn + 1)
        yield partner

    def send_in(ins, slot):
        for first in (0, 2):
            for t in (first, first + 1):
                pltpu.make_async_copy(ins[t].at[core * SLOTS + slot, :, pl.ds(2 * col, 2)], buf.at[t, slot, my_rows], in_recv.at[t, slot]).start()
            for peer in peers():
                for t in (first, first + 1):
                    pltpu.make_async_remote_copy(
                        src_ref=ins[t].at[(peer % 2) * SLOTS + slot, :, pl.ds(2 * ((peer // 2) % 4), 2)], dst_ref=buf.at[t, slot, my_rows],
                        send_sem=in_send, recv_sem=in_recv.at[t, slot], device_id=(peer,), device_id_type=MESH).start()

    def send_all(ins):
        def send_slot(slot, carry):
            send_in(ins, slot)
            return carry
        lax.fori_loop(0, SLOTS, send_slot, 0)

    @pl.when(z == 0)
    def _():
        send_all((k_in, v_in, q_in, g_in))

    @pl.when(z == 1)
    def _():
        send_all((q_in, g_in, k_in, v_in))

    for copy in tables:
        copy.wait()
    rev = eye_rev(BF16)
    for p in range(2):
        pair_tab = pltpu.einshape("abc->bac", r_buf[:, p])
        for hh in range(PAIR):
            for blk in range(SEQ // HEAD):
                part = pair_tab[hh, SEQ - HEAD * (blk + 1):SEQ - HEAD * blk]
                flipped = dot(rev, part).astype(BF16)
                rev_s[2 * p + hh, HEAD * blk:HEAD * (blk + 1), :] = flipped
                rt_s[2 * p + hh, :, HEAD * blk:HEAD * (blk + 1)] = flipped.T
    dr_acc[...] = jnp.zeros_like(dr_acc)

    acts = (o_out, dq_out, dk_out, dv_out)

    def send_out(slot, which):
        for t in which:
            pltpu.make_async_copy(buf.at[t, slot, my_rows], acts[t].at[core * SLOTS + slot, :, pl.ds(2 * col, 2)], out_recv.at[t]).start()
        for peer in peers():
            peer_rows = pl.ds(pl.multiple_of((peer % PLANE) * ROWS, ROWS), ROWS)
            for t in which:
                pltpu.make_async_remote_copy(
                    src_ref=buf.at[t, slot, peer_rows], dst_ref=acts[t].at[core * SLOTS + slot, :, pl.ds(2 * col, 2)],
                    send_sem=out_send, recv_sem=out_recv.at[t], device_id=(peer,), device_id_type=MESH).start()

    def send_up(slot):
        for j in range(2):
            wait_for(buf.at[j, slot], in_recv.at[j, slot])
            pltpu.make_async_remote_copy(src_ref=buf.at[j, slot], dst_ref=rbuf.at[j, slot], send_sem=up_send.at[slot], recv_sem=up_recv.at[j, slot],
                                         device_id=(across,), device_id_type=MESH).start()

    def unpack(ref, j, slot, p):
        return pltpu.einshape("abc->bac", ref[j, slot, :, p])

    def load_rows(q_ref, q_j, g_ref, g_j, slot, p, start, turned):
        rows = slice(start, start + HALF)
        q2 = unpack(q_ref, q_j, slot, p)
        u = u_buf[p].astype(F32)
        w = w_buf[p].astype(F32)
        for hh in range(PAIR):
            q32 = q2[hh].astype(F32)
            a = (q32 + u[hh:hh + 1]).astype(BF16)
            c = (q32 + w[hh:hh + 1]).astype(BF16)
            a_s[hh, rows, :] = a
            c_s[hh, rows, :] = c
            at_s[hh, :, rows] = a.T
            if turned:
                ct_s[hh, :, rows] = flip8(c.astype(F32)).astype(BF16).T
        g2 = unpack(g_ref, g_j, slot, p)
        g_s[:, rows, :] = g2
        for hh in range(PAIR):
            gt_s[hh, :, rows] = g2[hh].T

    def load_keys(k_ref, k_j, v_ref, v_j, slot, p, start):
        rows = slice(start, start + HALF)
        k2 = unpack(k_ref, k_j, slot, p)
        v2 = unpack(v_ref, v_j, slot, p)
        k_s[:, rows, :] = k2
        v_s[:, rows, :] = v2
        for hh in range(PAIR):
            kt_s[hh, :, rows] = k2[hh].T
            vt_s[hh, :, rows] = v2[hh].T

    def row_block(hh, head, start, i0, lo, fresh, stats):
        width = i0 + QB
        rows = slice(start, start + QB)
        s_ref[:, :width] = dot(a_s[hh, rows, :], kt_s[hh, :, :width])
        e_ref[:, :width] = dot(c_s[hh, rows, :], rt_s[head, :, SEQ - width:])
        dp_ref[:, :width] = dot(g_s[hh, rows, :], vt_s[hh, :, :width])
        for r0 in range(0, QB, 16):
            group = slice(r0, r0 + 16)
            rel = pltpu.roll(e_ref[group, :width], i0 + 1 + r0, 1, stride=1, stride_axis=0)
            s = s_ref[group, :width] + rel
            ahead = lax.broadcasted_iota(jnp.int32, (16, width), 1) - lax.broadcasted_iota(jnp.int32, (16, width), 0)
            s = jnp.where(ahead <= i0 + r0, s, -jnp.inf)
            top = jnp.max(s, axis=1, keepdims=True)
            p = jnp.exp2((s - top) * (scale * LOG2E))
            total = jnp.sum(p, axis=1, keepdims=True)
            p = p * (1.0 / total)
            pb_ref[group, :width] = p.astype(BF16)
            dp = dp_ref[group, :width]
            row_dot = jnp.sum(p * dp, axis=1, keepdims=True)
            ds = (p * (dp - row_dot) * scale).astype(BF16)
            ds_ref[group, :width] = ds
            flipped = flip8(ds.astype(F32))
            half = [pltpu.roll(flipped[8 * j:8 * j + 8], QB - 8 - r0 - 8 * j, 1, stride=1, stride_axis=0) for j in range(2)]
            dd_ref[group, :width] = jnp.concatenate(half, axis=0).astype(BF16)
            if stats:
                lane = lax.broadcasted_iota(jnp.int32, (16, HEAD), 1)
                st_ref[group, :] = jnp.where(lane == 0, top * (scale * LOG2E) + jnp.log2(total), row_dot)
        pb = pb_ref[:, :width]
        ds = ds_ref[:, :width]
        dd = dd_ref[:, :width]
        stage[0, hh, rows, :] = dot(pb, v_s[hh, :width, :]).astype(BF16)
        dqc = dot(ds, k_s[hh, :width, :])
        dqr = flip8(dot(dd, rev_s[head, SEQ - width:, :]))
        stage[1, hh, rows, :] = (dqc + dqr).astype(BF16)
        dr_acc[head, HEAD:HEAD + 1, SEQ - HEAD:] += jnp.sum(dqc, axis=0, keepdims=True)
        dr_acc[head, HEAD + 1:HEAD + 2, SEQ - HEAD:] += jnp.sum(dqr, axis=0, keepdims=True)
        dk_new = dot(at_s[hh, :, rows], ds_ref[:, lo:width])
        dv_new = dot(gt_s[hh, :, rows], pb_ref[:, lo:width])
        if fresh:
            dkt[hh] = dk_new
            dvt[hh] = dv_new
        else:
            dkt[hh, :, :width - lo] += dk_new
            dvt[hh, :, :width - lo] += dv_new
        dr_acc[head, :HEAD, SEQ - width:] += dot(ct_s[hh, :, rows], dd)

    def col_block(hh, head, slot, i0):
        rows = slice(i0, i0 + QB)
        first = WIN - i0
        s_ref[:, :HALF] = dot(a_s[hh, rows, :], kt_s[hh, :, :HALF])
        e_ref[:, :WIN] = dot(c_s[hh, rows, :], rt_s[head, :, first:first + WIN])
        dp_ref[:, :HALF] = dot(g_s[hh, rows, :], vt_s[hh, :, :HALF])
        st_ref[:, :8] = st_rx[slot, head, :, i0 - HALF:i0 - HALF + QB].T
        for r0 in range(0, QB, 16):
            group = slice(r0, r0 + 16)
            rel = pltpu.roll(e_ref[group, :WIN], HALF + 1 + r0, 1, stride=1, stride_axis=0)[:, :HALF]
            log_sum = st_ref[group, 0:1]
            row_dot = st_ref[group, 1:2]
            p = jnp.exp2((s_ref[group, :HALF] + rel) * (scale * LOG2E) - log_sum)
            pb_ref[group, :HALF] = p.astype(BF16)
            ds_ref[group, :HALF] = (p * (dp_ref[group, :HALF] - row_dot) * scale).astype(BF16)
        dkt[hh] += dot(at_s[hh, :, rows], ds_ref[:, :HALF])
        dvt[hh] += dot(gt_s[hh, :, rows], pb_ref[:, :HALF])

    def store_pair(slot, p):
        for hh in range(PAIR):
            stage[2, hh] = dkt[hh].astype(BF16).T
            stage[3, hh] = dvt[hh].astype(BF16).T
        for t in range(4):
            buf[t, slot, :, p] = pltpu.einshape("abc->bac", stage[t])

    def lower_pair(slot, p):
        load_rows(buf, 2, buf, 3, slot, p, 0, True)
        load_rows(rbuf, 0, rbuf, 1, slot, p, HALF, False)
        load_keys(buf, 0, buf, 1, slot, p, 0)

        def own(hh, carry):
            row_block(hh, 2 * p + hh, QB, QB, 0, True, False)
            row_block(hh, 2 * p + hh, 0, 0, 0, False, False)
            return carry

        def theirs(hh, carry):
            head = 2 * p + hh
            wait_for(st_rx.at[slot, head], st_recv.at[slot, head])
            col_block(hh, head, slot, HALF)
            col_block(hh, head, slot, HALF + QB)
            return carry

        lax.fori_loop(0, PAIR, own, 0)
        lax.fori_loop(0, PAIR, theirs, 0)

    def upper_pair(slot, p):
        load_rows(buf, 0, buf, 1, slot, p, 0, True)
        load_keys(rbuf, 0, rbuf, 1, slot, p, 0)
        load_keys(buf, 2, buf, 3, slot, p, HALF)

        def own(hh, carry):
            head = 2 * p + hh
            for blk in (1, 0):
                row_block(hh, head, QB * blk, HALF + QB * blk, HALF, blk == 1, True)
                st_tx[slot, head, :, QB * blk:QB * (blk + 1)] = st_ref[...].T[:8]
            pltpu.make_async_remote_copy(src_ref=st_tx.at[slot, head], dst_ref=st_rx.at[slot, head], send_sem=st_send, recv_sem=st_recv.at[slot, head],
                                         device_id=(across,), device_id_type=MESH).start()
            return carry

        lax.fori_loop(0, PAIR, own, 0)

    send_up(0)

    def slot_body(slot, carry):
        @pl.when(slot < SLOTS - 1)
        def _():
            send_up(slot + 1)
        for j in range(2):
            wait_for(buf.at[2 + j, slot], in_recv.at[2 + j, slot])
            wait_for(rbuf.at[j, slot], up_recv.at[j, slot])
        wait_for(rbuf.at[:, slot], up_send.at[slot])

        def pair_body(p, carry):
            @pl.when(z == 0)
            def _():
                lower_pair(slot, p)

            @pl.when(z == 1)
            def _():
                upper_pair(slot, p)

            store_pair(slot, p)
            return carry

        lax.fori_loop(0, 2, pair_body, 0)

        @pl.when(slot < SLOTS - 2)
        def _():
            send_out(slot, range(4))
        return carry

    lax.fori_loop(0, SLOTS, slot_body, 0)
    send_out(SLOTS - 2, (0,))

    swaps = [pltpu.make_async_remote_copy(
        src_ref=dr_acc.at[2 * p + 1 - core], dst_ref=dr_rx.at[p], send_sem=x_send.at[p], recv_sem=x_recv.at[p],
        device_id=(partner,), device_id_type=MESH) for p in range(2)]
    for swap in swaps:
        swap.start()
    for swap in swaps:
        swap.wait()
    for p in range(2):
        dr_rx[p] = dr_rx[p] + dr_acc[2 * p + core]

    @pl.when(z == 0)
    def _():
        pltpu.make_async_remote_copy(src_ref=dr_rx.at[1, :, HALF:], dst_ref=dr_rz.at[:, HALF:], send_sem=z_send, recv_sem=z_recv,
                                     device_id=(across,), device_id_type=MESH).start()
        wait_for(dr_rz, z_recv)
        wait_for(dr_rz.at[:, HALF:], z_send)

    @pl.when(z == 1)
    def _():
        pltpu.make_async_remote_copy(src_ref=dr_rx.at[0], dst_ref=dr_rz, send_sem=z_send, recv_sem=z_recv,
                                     device_id=(across,), device_id_type=MESH).start()
        wait_for(dr_rz.at[:, HALF:], z_recv)
        wait_for(dr_rz, z_send)

    def head_of(bits):
        other = chip ^ bits
        return 4 * (other % 4) + 2 * (other // 4) + core

    head = head_of(0)
    total = dr_rx[z] + dr_rz[...]
    rev32 = eye_rev(F32)
    for blk in range(SEQ // HEAD):
        part = total[:HEAD, SEQ - HEAD * (blk + 1):SEQ - HEAD * blk]
        turned = lax.dot_general(rev32, part, (((1,), (1,)), ((), ())), precision=lax.Precision.HIGHEST, preferred_element_type=F32)
        dr_fin[HEAD * blk:HEAD * (blk + 1)] = turned.reshape(HEAD, 1, HEAD)
    dr_fin[SEQ] = total[HEAD:HEAD + 1, SEQ - HEAD:]
    dr_fin[SEQ + 1] = total[HEAD + 1:HEAD + 2, SEQ - HEAD:]

    parts = (dr0_out, dr1_out, dr2_out, dr3_out, dr4_out, dr5_out)

    def block(m, bits):
        if bits == 0:
            start, rows = PARTS[m]
            return dr_fin.at[start:start + rows]
        return parts[m].at[:, head_of(bits)]

    def forward(m, bits):
        pltpu.make_async_remote_copy(src_ref=block(m, bits), dst_ref=parts[m].at[:, head_of(bits)], send_sem=fw_send.at[m], recv_sem=fw_recv.at[m],
                                     device_id=(partner,), device_id_type=MESH).start()

    held = [[0] for _ in range(N_PART)]
    for m in range(N_PART):
        pltpu.make_async_copy(block(m, 0), parts[m].at[:, head], own_sem.at[m]).start()
    for hop in range(3):
        for m in range(N_PART):
            bit = HOPS[m][hop]
            for bits in held[m]:
                pltpu.make_async_remote_copy(
                    src_ref=block(m, bits), dst_ref=parts[m].at[:, head_of(bits)], send_sem=ring_send.at[m],
                    recv_sem=ring_recv.at[hop, m], device_id=(me ^ (2 * bit),), device_id_type=MESH).start()
        for m in range(N_PART):
            for bits in (held[m] if hop == 0 else held[m][len(held[m]) // 2:]):
                forward(m, bits)
        if hop == 0:
            for j, dst in enumerate((du_out, dw_out)):
                pltpu.make_async_copy(dr_fin.at[SEQ + j], dst.at[head], b_recv.at[j]).start()
                for step in range(1, N_DEV):
                    pltpu.make_async_remote_copy(
                        src_ref=dr_fin.at[SEQ + j], dst_ref=dst.at[head], send_sem=b_send.at[j], recv_sem=b_recv.at[j],
                        device_id=(me ^ step,), device_id_type=MESH).start()
        if hop == 0:
            send_out(SLOTS - 2, (1,))
        elif hop == 1:
            send_out(SLOTS - 2, (2,))
        else:
            send_out(SLOTS - 2, (3,))
            send_out(SLOTS - 1, range(4))
        for m in range(N_PART):
            count = len(held[m])
            wait_for(parts[m].at[:, :count], ring_recv.at[hop, m])
            held[m] = held[m] + [bits ^ HOPS[m][hop] for bits in held[m]]
            if hop == 2:
                for bits in held[m][4:]:
                    forward(m, bits)

    for t, dst in enumerate(acts):
        wait_for(dst, out_recv.at[t])
    for j, dst in enumerate((du_out, dw_out)):
        wait_for(dst, b_recv.at[j])
        wait_for(dst.at[:N_DEV - 1], b_send.at[j])
    wait_for(buf.at[:, :, :HALF - ROWS], in_send)
    wait_for(buf.at[:, :, :HALF - ROWS], out_send)

    @pl.when(z == 1)
    def _():
        wait_for(st_tx, st_send)

    for m in range(N_PART):
        wait_for(parts[m].at[:, head], own_sem.at[m])
        wait_for(parts[m].at[:, :N_PAIR - 1], ring_send.at[m])
        wait_for(parts[m].at[:, :N_PAIR], fw_send.at[m])
        wait_for(parts[m].at[:, :N_PAIR], fw_recv.at[m])


def writer(*refs):
    ins, (o, dq, dk, dv, dr, du, dw, sem) = refs[:6 + N_PART], refs[6 + N_PART:]
    pairs = list(zip(ins[:4] + ins[-2:], (o, dq, dk, dv, du, dw)))
    for part, (start, rows) in zip(ins[4:-2], PARTS):
        pairs.append((part, dr.at[start:start + rows]))
    copies = [pltpu.make_async_copy(src, dst, sem.at[j]) for j, (src, dst) in enumerate(pairs)]
    for copy in copies:
        copy.start()
    for copy in copies:
        copy.wait()


def solution(mesh):
    seq_spec = P(None, "cp", None, None)

    def local(query, key_in, value, bias_u, bias_w, rel_k, d_out):
        n_batch, rows, n_heads, head_dim = query.shape
        pairs = (n_batch, rows, N_PAIR, PAIR, head_dim)
        vm = pltpu.VMEM
        dma = pltpu.SemaphoreType.DMA
        whole = pl.BlockSpec(memory_space=pl.ANY)
        act = jax.ShapeDtypeStruct(pairs, BF16)
        vec = jax.ShapeDtypeStruct((n_heads, 1, head_dim), F32)
        tok = (PAIR, SEQ, HEAD)
        tok_t = (PAIR, HEAD, SEQ)
        acc = (HEAD + 8, SEQ)
        outs = pl.pallas_call(
            kernel,
            name="rel_attn",
            out_shape=(act, act, act, act,
                       *[jax.ShapeDtypeStruct((part_rows, n_heads, 1, head_dim), F32) for _, part_rows in PARTS],
                       vec, vec),
            in_specs=[pl.BlockSpec(memory_space=pltpu.HBM)] * 7,
            out_specs=[whole] * (6 + N_PART),
            scratch_shapes=[
                vm((4, SLOTS, HALF, 2, PAIR, HEAD), BF16), vm((2, SLOTS, HALF, 2, PAIR, HEAD), BF16),
                vm((SEQ, 2, PAIR, HEAD), BF16), vm((2, PAIR, HEAD), BF16), vm((2, PAIR, HEAD), BF16),
                vm((SLOTS, 4, 8, HALF), F32), vm((SLOTS, 4, 8, HALF), F32), vm((QB, HEAD), F32),
                vm((2,) + acc, F32), vm(acc, F32), vm((SEQ + 2, 1, HEAD), F32), vm((4,) + acc, F32),
                vm((QB, SEQ), F32), vm((QB, SEQ), F32), vm((QB, SEQ), F32),
                vm((QB, SEQ), BF16), vm((QB, SEQ), BF16), vm((QB, SEQ), BF16),
                vm(tok, BF16), vm(tok, BF16), vm(tok, BF16), vm(tok, BF16), vm(tok, BF16),
                vm(tok_t, BF16), vm(tok_t, BF16), vm(tok_t, BF16), vm(tok_t, BF16), vm(tok_t, BF16),
                vm((4, SEQ, HEAD), BF16), vm((4, HEAD, SEQ), BF16),
                vm((PAIR, HEAD, HALF), F32), vm((PAIR, HEAD, HALF), F32), vm((4, PAIR, HALF, HEAD), BF16),
                dma, dma((4, SLOTS)), dma, dma((4,)), dma((N_PART,)), dma((3,)), dma((SLOTS,)), dma((2, SLOTS)), dma, dma((SLOTS, 4)),
                dma((2,)), dma((2,)), dma, dma, dma((N_PART,)), dma((3, N_PART)), dma((N_PART,)), dma((N_PART,)), dma((2,)), dma((2,)),
            ],
            compiler_params=pltpu.CompilerParams(collective_id=0, has_side_effects=True, vmem_limit_bytes=36 * 1024 * 1024),
        )(*[pltpu.with_memory_space_constraint(x, pltpu.HBM) for x in (
            query.reshape(pairs), key_in.reshape(pairs), value.reshape(pairs), d_out.reshape(pairs),
            rel_k.reshape(SEQ, N_PAIR, PAIR, head_dim), bias_u.reshape(N_PAIR, PAIR, head_dim), bias_w.reshape(N_PAIR, PAIR, head_dim))])
        o, dq, dk, dv, dr, du, dw = pl.pallas_call(
            writer,
            name="writer",
            out_shape=(act, act, act, act, jax.ShapeDtypeStruct((SEQ, n_heads, 1, head_dim), F32), vec, vec),
            in_specs=[whole] * (6 + N_PART),
            out_specs=[whole] * 7,
            scratch_shapes=[dma((6 + N_PART,))],
            compiler_params=pltpu.CompilerParams(vmem_limit_bytes=1024 * 1024),
        )(*outs)
        full = query.shape
        return (o.reshape(full), dq.reshape(full), dk.reshape(full), dv.reshape(full),
                du.reshape(bias_u.shape), dw.reshape(bias_w.shape), dr.reshape(rel_k.shape))

    return jax.shard_map(local, mesh=mesh,
                         in_specs=(seq_spec, seq_spec, seq_spec, P(), P(), P(), seq_spec),
                         out_specs=(seq_spec, seq_spec, seq_spec, seq_spec, P(), P(), P()),
                         check_vma=False)
```

```python
import jax
import jax.numpy as jnp
from jax import lax
from jax.experimental import pallas as pl
from jax.experimental.pallas import tpu as pltpu
from jax.sharding import PartitionSpec as P

MESH = pl.DeviceIdType.MESH
BF16, F32 = jnp.bfloat16, jnp.float32
LOG2E = 1.4426950408889634

N_DEV = 16
PLANE = 8
PAIR = 2
N_PAIR = 8
SLOTS = 4
SUBS = 2 * SLOTS
EARLY = 2
ROWS = 64
HALF = PLANE * ROWS
SEQ = 2 * HALF
HEAD = 128
QB = 256
WIN = HALF + QB
N_PART = 4
PART = HALF // N_PART
HOPS = ((1, 2, 4), (2, 1, 4), (1, 2, 4), (2, 1, 4))
TURNS = ((1, 3, 2), (3, 1, 2))


def dot(lhs, rhs):
    return jnp.dot(lhs, rhs, preferred_element_type=F32)


def flip8(x):
    rows, cols = x.shape
    idx = 7 - lax.broadcasted_iota(jnp.int32, (rows // 8, 8, cols), 1)
    return jnp.take_along_axis(x.reshape(rows // 8, 8, cols), idx, axis=1).reshape(rows, cols)


def eye_rev(dtype):
    total = lax.broadcasted_iota(jnp.int32, (HEAD, HEAD), 0) + lax.broadcasted_iota(jnp.int32, (HEAD, HEAD), 1)
    return jnp.where(total == HEAD - 1, 1.0, 0.0).astype(dtype)


def kernel(q_in, k_in, v_in, g_in, r_in, u_in, w_in,
           o_out, dq_out, dk_out, dv_out, dr0_out, dr1_out, dr2_out, dr3_out, du_out, dw_out,
           buf, rbuf, r_buf, u_buf, w_buf, st_tx, st_rx, st_ref, dr_rx, dr_fin, dr_acc,
           s_ref, e_ref, dp_ref, pb_ref, ds_ref, dd_ref,
           a_s, c_s, g_s, k_s, v_s, at_s, ct_s, gt_s, kt_s, vt_s, rev_s, rt_s, dkt, dvt, stage,
           in_send, in_recv, out_send, out_recv, own_sem, r_sem, up_send, up_recv, st_send, st_recv,
           x_send, x_recv, ring_send, ring_recv, fw_send, fw_recv, b_send, b_recv):
    me = lax.axis_index("cp")
    core = me % 2
    chip = me // 2
    col = chip % 4
    z = chip // 4
    partner = me + 1 - 2 * core
    across = me + PLANE * (1 - 2 * z)
    scale = HEAD ** -0.5

    def wait_for(ref, sem):
        pltpu.make_async_copy(ref, ref, sem).wait()

    tables = [pltpu.make_async_copy(src, dst, r_sem.at[j]) for j, (src, dst) in enumerate(
        ((r_in.at[:, pl.ds(2 * col, 2)], r_buf), (u_in.at[pl.ds(2 * col, 2)], u_buf), (w_in.at[pl.ds(2 * col, 2)], w_buf)))]
    for copy in tables:
        copy.start()

    barrier = pltpu.get_barrier_semaphore()

    def say(step, carry):
        pl.semaphore_signal(barrier, inc=1, device_id=((me + step) % N_DEV,), device_id_type=MESH)
        return carry

    lax.fori_loop(1, N_DEV, say, 0)
    pl.semaphore_wait(barrier, N_DEV - 1)

    my_rows = pl.ds(pl.multiple_of((me % PLANE) * ROWS, ROWS), ROWS)

    def peers():
        for near_turn, far_turn in zip(*TURNS):
            turn = jnp.where(core == 0, near_turn, far_turn)
            yield me ^ (2 * turn)
            yield me ^ (2 * turn + 1)
        yield partner

    def send_in(ins, sub):
        pair, row = sub // SLOTS, sub % SLOTS
        for first in (0, 2):
            for t in (first, first + 1):
                pltpu.make_async_copy(ins[t].at[core * SLOTS + row, :, 2 * col + pair], buf.at[t, sub, my_rows], in_recv.at[t, sub]).start()
            for peer in peers():
                for t in (first, first + 1):
                    pltpu.make_async_remote_copy(
                        src_ref=ins[t].at[(peer % 2) * SLOTS + row, :, 2 * ((peer // 2) % 4) + pair], dst_ref=buf.at[t, sub, my_rows],
                        send_sem=in_send, recv_sem=in_recv.at[t, sub], device_id=(peer,), device_id_type=MESH).start()

    def send_all(ins):
        def send_sub(sub, carry):
            send_in(ins, sub)
            return carry
        lax.fori_loop(0, SUBS, send_sub, 0)

    @pl.when(z == 0)
    def _():
        send_all((k_in, v_in, q_in, g_in))

    @pl.when(z == 1)
    def _():
        send_all((q_in, g_in, k_in, v_in))

    for copy in tables:
        copy.wait()
    rev = eye_rev(BF16)
    for p in range(2):
        pair_tab = pltpu.einshape("abc->bac", r_buf[:, p])
        for hh in range(PAIR):
            for blk in range(SEQ // HEAD):
                part = pair_tab[hh, SEQ - HEAD * (blk + 1):SEQ - HEAD * blk]
                flipped = dot(rev, part).astype(BF16)
                rev_s[2 * p + hh, HEAD * blk:HEAD * (blk + 1), :] = flipped
                rt_s[2 * p + hh, :, HEAD * blk:HEAD * (blk + 1)] = flipped.T
    dr_acc[...] = jnp.zeros_like(dr_acc)

    acts = (dk_out, dv_out, o_out, dq_out)

    def send_out(sub, which):
        place = (core * SLOTS + sub % SLOTS, slice(None), 2 * col + sub // SLOTS)
        for t in which:
            pltpu.make_async_copy(buf.at[t, sub, my_rows], acts[t].at[place], out_recv.at[t]).start()
        for peer in peers():
            peer_rows = pl.ds(pl.multiple_of((peer % PLANE) * ROWS, ROWS), ROWS)
            for t in which:
                pltpu.make_async_remote_copy(
                    src_ref=buf.at[t, sub, peer_rows], dst_ref=acts[t].at[place],
                    send_sem=out_send, recv_sem=out_recv.at[t], device_id=(peer,), device_id_type=MESH).start()

    def send_up(sub):
        for j in range(2):
            wait_for(buf.at[j, sub], in_recv.at[j, sub])
            pltpu.make_async_remote_copy(src_ref=buf.at[j, sub], dst_ref=rbuf.at[j, sub], send_sem=up_send.at[sub], recv_sem=up_recv.at[j, sub],
                                         device_id=(across,), device_id_type=MESH).start()

    def unpack(ref, j, sub):
        return pltpu.einshape("abc->bac", ref[j, sub])

    def load_rows(q_ref, q_j, g_ref, g_j, sub, start, turned):
        rows = slice(start, start + HALF)
        p = sub // SLOTS
        q2 = unpack(q_ref, q_j, sub)
        u = u_buf[p].astype(F32)
        w = w_buf[p].astype(F32)
        for hh in range(PAIR):
            q32 = q2[hh].astype(F32)
            a = (q32 + u[hh:hh + 1]).astype(BF16)
            c = (q32 + w[hh:hh + 1]).astype(BF16)
            a_s[hh, rows, :] = a
            c_s[hh, rows, :] = c
            at_s[hh, :, rows] = a.T
            if turned:
                ct_s[hh, :, rows] = flip8(c.astype(F32)).astype(BF16).T
        g2 = unpack(g_ref, g_j, sub)
        g_s[:, rows, :] = g2
        for hh in range(PAIR):
            gt_s[hh, :, rows] = g2[hh].T

    def load_keys(k_ref, k_j, v_ref, v_j, sub, start):
        rows = slice(start, start + HALF)
        k2 = unpack(k_ref, k_j, sub)
        v2 = unpack(v_ref, v_j, sub)
        k_s[:, rows, :] = k2
        v_s[:, rows, :] = v2
        for hh in range(PAIR):
            kt_s[hh, :, rows] = k2[hh].T
            vt_s[hh, :, rows] = v2[hh].T

    def row_block(hh, head, start, i0, lo, fresh, stats):
        width = i0 + QB
        rows = slice(start, start + QB)
        s_ref[:, :width] = dot(a_s[hh, rows, :], kt_s[hh, :, :width])
        e_ref[:, :width] = dot(c_s[hh, rows, :], rt_s[head, :, SEQ - width:])
        dp_ref[:, :width] = dot(g_s[hh, rows, :], vt_s[hh, :, :width])
        for r0 in range(0, QB, 16):
            group = slice(r0, r0 + 16)
            rel = pltpu.roll(e_ref[group, :width], i0 + 1 + r0, 1, stride=1, stride_axis=0)
            s = s_ref[group, :width] + rel
            ahead = lax.broadcasted_iota(jnp.int32, (16, width), 1) - lax.broadcasted_iota(jnp.int32, (16, width), 0)
            s = jnp.where(ahead <= i0 + r0, s, -jnp.inf)
            top = jnp.max(s, axis=1, keepdims=True)
            p = jnp.exp2((s - top) * (scale * LOG2E))
            total = jnp.sum(p, axis=1, keepdims=True)
            p = p * (1.0 / total)
            pb_ref[group, :width] = p.astype(BF16)
            dp = dp_ref[group, :width]
            row_dot = jnp.sum(p * dp, axis=1, keepdims=True)
            ds = (p * (dp - row_dot) * scale).astype(BF16)
            ds_ref[group, :width] = ds
            flipped = flip8(ds.astype(F32))
            half = [pltpu.roll(flipped[8 * j:8 * j + 8], QB - 8 - r0 - 8 * j, 1, stride=1, stride_axis=0) for j in range(2)]
            dd_ref[group, :width] = jnp.concatenate(half, axis=0).astype(BF16)
            if stats:
                lane = lax.broadcasted_iota(jnp.int32, (16, HEAD), 1)
                st_ref[group, :] = jnp.where(lane == 0, top * (scale * LOG2E) + jnp.log2(total), row_dot)
        pb = pb_ref[:, :width]
        ds = ds_ref[:, :width]
        dd = dd_ref[:, :width]
        stage[0, hh, rows, :] = dot(pb, v_s[hh, :width, :]).astype(BF16)
        dqc = dot(ds, k_s[hh, :width, :])
        dqr = flip8(dot(dd, rev_s[head, SEQ - width:, :]))
        stage[1, hh, rows, :] = (dqc + dqr).astype(BF16)
        dr_acc[head, 1, HEAD:HEAD + 1, HALF - HEAD:] += jnp.sum(dqc, axis=0, keepdims=True)
        dr_acc[head, 1, HEAD + 1:HEAD + 2, HALF - HEAD:] += jnp.sum(dqr, axis=0, keepdims=True)
        dk_new = dot(at_s[hh, :, rows], ds_ref[:, lo:width])
        dv_new = dot(gt_s[hh, :, rows], pb_ref[:, lo:width])
        if fresh:
            dkt[hh] = dk_new
            dvt[hh] = dv_new
        else:
            dkt[hh, :, :width - lo] += dk_new
            dvt[hh, :, :width - lo] += dv_new
        dr_new = dot(ct_s[hh, :, rows], dd)
        if width > HALF:
            dr_acc[head, 0, :HEAD, SEQ - width:] += dr_new[:, :width - HALF]
            dr_acc[head, 1, :HEAD, :] += dr_new[:, width - HALF:]
        else:
            dr_acc[head, 1, :HEAD, HALF - width:] += dr_new

    def col_block(hh, head, sub, i0):
        rows = slice(i0, i0 + QB)
        first = WIN - i0
        s_ref[:, :HALF] = dot(a_s[hh, rows, :], kt_s[hh, :, :HALF])
        e_ref[:, :WIN] = dot(c_s[hh, rows, :], rt_s[head, :, first:first + WIN])
        dp_ref[:, :HALF] = dot(g_s[hh, rows, :], vt_s[hh, :, :HALF])
        st_ref[:, :8] = st_rx[sub, hh, :, i0 - HALF:i0 - HALF + QB].T
        for r0 in range(0, QB, 16):
            group = slice(r0, r0 + 16)
            rel = pltpu.roll(e_ref[group, :WIN], HALF + 1 + r0, 1, stride=1, stride_axis=0)[:, :HALF]
            log_sum = st_ref[group, 0:1]
            row_dot = st_ref[group, 1:2]
            p = jnp.exp2((s_ref[group, :HALF] + rel) * (scale * LOG2E) - log_sum)
            pb_ref[group, :HALF] = p.astype(BF16)
            ds_ref[group, :HALF] = (p * (dp_ref[group, :HALF] - row_dot) * scale).astype(BF16)
        dkt[hh] += dot(at_s[hh, :, rows], ds_ref[:, :HALF])
        dvt[hh] += dot(gt_s[hh, :, rows], pb_ref[:, :HALF])

    def store_rows(sub):
        for t in range(2):
            buf[2 + t, sub] = pltpu.einshape("abc->bac", stage[t])

    def store_keys(sub):
        for hh in range(PAIR):
            stage[2, hh] = dkt[hh].astype(BF16).T
            stage[3, hh] = dvt[hh].astype(BF16).T
        for t in range(2):
            buf[t, sub] = pltpu.einshape("abc->bac", stage[2 + t])

    def wait_up(sub):
        for j in range(2):
            wait_for(rbuf.at[j, sub], up_recv.at[j, sub])
        wait_for(rbuf.at[:, sub], up_send.at[sub])

    def wait_in(sub):
        for j in range(2, 4):
            wait_for(buf.at[j, sub], in_recv.at[j, sub])

    def lower_own(sub):
        wait_in(sub)
        load_rows(buf, 2, buf, 3, sub, 0, True)
        load_keys(buf, 0, buf, 1, sub, 0)

        def own(hh, carry):
            head = 2 * (sub // SLOTS) + hh
            row_block(hh, head, QB, QB, 0, True, False)
            row_block(hh, head, 0, 0, 0, False, False)
            return carry

        lax.fori_loop(0, PAIR, own, 0)
        store_rows(sub)

    def lower_theirs(sub):
        wait_up(sub)
        load_rows(rbuf, 0, rbuf, 1, sub, HALF, False)

        def theirs(hh, carry):
            head = 2 * (sub // SLOTS) + hh
            wait_for(st_rx.at[sub, hh], st_recv.at[sub, hh])
            col_block(hh, head, sub, HALF)
            col_block(hh, head, sub, HALF + QB)
            return carry

        lax.fori_loop(0, PAIR, theirs, 0)
        store_keys(sub)

    def upper_own(sub):
        wait_in(sub)
        wait_up(sub)
        load_rows(buf, 0, buf, 1, sub, 0, True)
        load_keys(rbuf, 0, rbuf, 1, sub, 0)
        load_keys(buf, 2, buf, 3, sub, HALF)

        def own(hh, carry):
            head = 2 * (sub // SLOTS) + hh
            for blk in (1, 0):
                row_block(hh, head, QB * blk, HALF + QB * blk, HALF, blk == 1, True)
                st_tx[sub, hh, :, QB * blk:QB * (blk + 1)] = st_ref[...].T[:8]
            pltpu.make_async_remote_copy(src_ref=st_tx.at[sub, hh], dst_ref=st_rx.at[sub, hh], send_sem=st_send, recv_sem=st_recv.at[sub, hh],
                                         device_id=(across,), device_id_type=MESH).start()
            return carry

        lax.fori_loop(0, PAIR, own, 0)
        store_rows(sub)
        store_keys(sub)

    side = 1 - core
    parts = (dr0_out, dr1_out, dr2_out, dr3_out)

    def swap_start(p):
        for n, (device, top, end) in enumerate(((partner, z, 1 - core), (across, 1 - z, core), (across + 1 - 2 * core, 1 - z, 1 - core))):
            pltpu.make_async_remote_copy(src_ref=dr_acc.at[2 * p + top, end], dst_ref=dr_rx.at[p, n], send_sem=x_send.at[p], recv_sem=x_recv.at[p, n],
                                         device_id=(device,), device_id_type=MESH).start()

    def head_of(p, bits):
        other = chip ^ bits
        return 4 * (other % 4) + 2 * p + other // 4

    def block(p, m, bits):
        if bits == 0:
            return dr_fin.at[p, PART * m:PART * (m + 1)]
        return parts[m].at[side, :, head_of(p, bits)]

    def forward(p, m, bits):
        pltpu.make_async_remote_copy(src_ref=block(p, m, bits), dst_ref=parts[m].at[side, :, head_of(p, bits)], send_sem=fw_send.at[p, m],
                                     recv_sem=fw_recv.at[p, m], device_id=(partner,), device_id_type=MESH).start()

    def held(m, hop):
        have = [0]
        for bit in HOPS[m][:hop]:
            have = have + [bits ^ bit for bits in have]
        return have

    def hop_start(p, hop):
        for m in range(N_PART):
            for bits in held(m, hop):
                pltpu.make_async_remote_copy(
                    src_ref=block(p, m, bits), dst_ref=parts[m].at[side, :, head_of(p, bits)], send_sem=ring_send.at[p, m],
                    recv_sem=ring_recv.at[p, hop, m], device_id=(me ^ (2 * HOPS[m][hop]),), device_id_type=MESH).start()

    def hop_wait(p, hop):
        for m in range(N_PART):
            have = held(m, hop + 1)
            wait_for(parts[m].at[0, :, :len(have) // 2], ring_recv.at[p, hop, m])
            for bits in have[len(have) // 2:]:
                forward(p, m, bits)

    def swap_finish(p):
        for n in range(3):
            wait_for(dr_rx.at[p, n], x_recv.at[p, n])
        total = dr_acc[2 * p + z, core] + dr_rx[p, 0] + dr_rx[p, 1] + dr_rx[p, 2]
        rev32 = eye_rev(F32)
        for m in range(N_PART):
            part = total[:HEAD, HALF - HEAD * (m + 1):HALF - HEAD * m]
            turned = lax.dot_general(rev32, part, (((1,), (1,)), ((), ())), precision=lax.Precision.HIGHEST, preferred_element_type=F32)
            dr_fin[p, HEAD * m:HEAD * (m + 1)] = turned.reshape(HEAD, 1, HEAD)
        dr_fin[p, HALF] = total[HEAD:HEAD + 1, HALF - HEAD:]
        dr_fin[p, HALF + 1] = total[HEAD + 1:HEAD + 2, HALF - HEAD:]
        hop_start(p, 0)
        head = head_of(p, 0)
        for m in range(N_PART):
            pltpu.make_async_copy(block(p, m, 0), parts[m].at[side, :, head], own_sem.at[p, m]).start()
            forward(p, m, 0)

        @pl.when(core == 1)
        def _():
            for j, dst in enumerate((du_out, dw_out)):
                pltpu.make_async_copy(dr_fin.at[p, HALF + j], dst.at[head], b_recv.at[j]).start()
                for step in range(1, N_DEV):
                    pltpu.make_async_remote_copy(
                        src_ref=dr_fin.at[p, HALF + j], dst_ref=dst.at[head], send_sem=b_send.at[j], recv_sem=b_recv.at[j],
                        device_id=(me ^ step,), device_id_type=MESH).start()

    send_up(0)

    def sub_body(sub, carry):
        @pl.when(sub < SUBS - 1)
        def _():
            send_up(sub + 1)

        @pl.when(sub == SLOTS)
        def _():
            swap_start(0)

        @pl.when(sub == SLOTS + 2)
        def _():
            swap_finish(0)

        @pl.when((z == 0) & (sub > 0))
        def _():
            lower_theirs(sub - 1)

        @pl.when((z == 0) & (sub < SUBS))
        def _():
            lower_own(sub)

        @pl.when((z == 1) & (sub < SUBS))
        def _():
            upper_own(sub)

        @pl.when(sub < EARLY)
        def _():
            send_out(sub, (2, 3))

        @pl.when((sub > 0) & (sub <= EARLY))
        def _():
            send_out(sub - 1, (0, 1))
        return carry

    lax.fori_loop(0, SUBS + 1, sub_body, 0)

    swap_start(1)
    send_out(EARLY, range(4))
    hop_wait(0, 0)
    hop_start(0, 1)
    swap_finish(1)
    send_out(EARLY + 1, range(4))
    hop_wait(0, 1)
    hop_start(0, 2)
    hop_wait(1, 0)
    hop_start(1, 1)
    send_out(EARLY + 2, range(4))
    hop_wait(1, 1)
    hop_start(1, 2)

    def send_late(sub, carry):
        send_out(sub, range(4))
        return carry

    lax.fori_loop(EARLY + 3, SUBS, send_late, 0)
    hop_wait(0, 2)
    hop_wait(1, 2)

    for t, dst in enumerate(acts):
        wait_for(dst, out_recv.at[t])
    for j, dst in enumerate((du_out, dw_out)):
        wait_for(dst, b_recv.at[j])

        @pl.when(core == 1)
        def _():
            wait_for(dr_fin.at[0, :2 * (N_DEV - 1)], b_send.at[j])
    wait_for(buf.at[:, :, :HALF - ROWS], in_send)
    wait_for(buf.at[:, :, :HALF - ROWS], out_send)

    @pl.when(z == 1)
    def _():
        wait_for(st_tx, st_send)

    for p in range(2):
        wait_for(dr_rx.at[p], x_send.at[p])
        for m in range(N_PART):
            wait_for(dr_fin.at[p, :PART], own_sem.at[p, m])
            wait_for(parts[m].at[0, :, :N_PAIR - 1], ring_send.at[p, m])
            wait_for(parts[m].at[0, :, :N_PAIR], fw_send.at[p, m])
            wait_for(parts[m].at[0, :, :N_PAIR], fw_recv.at[p, m])


def writer(*refs):
    ins, (o, dq, dk, dv, dr, du, dw, sem) = refs[:6 + N_PART], refs[6 + N_PART:]
    pairs = list(zip(ins[:4] + ins[-2:], (o, dq, dk, dv, du, dw)))
    for m, part in enumerate(ins[4:-2]):
        for side in range(2):
            start = HALF * side + PART * m
            pairs.append((part.at[side], dr.at[start:start + PART]))
    copies = [pltpu.make_async_copy(src, dst, sem.at[j]) for j, (src, dst) in enumerate(pairs)]
    for copy in copies:
        copy.start()
    for copy in copies:
        copy.wait()


def solution(mesh):
    seq_spec = P(None, "cp", None, None)

    def local(query, key_in, value, bias_u, bias_w, rel_k, d_out):
        n_batch, rows, n_heads, head_dim = query.shape
        pairs = (n_batch, rows, N_PAIR, PAIR, head_dim)
        vm = pltpu.VMEM
        dma = pltpu.SemaphoreType.DMA
        whole = pl.BlockSpec(memory_space=pl.ANY)
        act = jax.ShapeDtypeStruct(pairs, BF16)
        vec = jax.ShapeDtypeStruct((n_heads, 1, head_dim), F32)
        tok = (PAIR, SEQ, HEAD)
        tok_t = (PAIR, HEAD, SEQ)
        acc = (HEAD + 8, HALF)
        outs = pl.pallas_call(
            kernel,
            name="rel_attn",
            out_shape=(act, act, act, act,
                       *[jax.ShapeDtypeStruct((2, PART, n_heads, 1, head_dim), F32)] * N_PART,
                       vec, vec),
            in_specs=[pl.BlockSpec(memory_space=pltpu.HBM)] * 7,
            out_specs=[whole] * (6 + N_PART),
            scratch_shapes=[
                vm((4, SUBS, HALF, PAIR, HEAD), BF16), vm((2, SUBS, HALF, PAIR, HEAD), BF16),
                vm((SEQ, 2, PAIR, HEAD), BF16), vm((2, PAIR, HEAD), BF16), vm((2, PAIR, HEAD), BF16),
                vm((SUBS, PAIR, 8, HALF), F32), vm((SUBS, PAIR, 8, HALF), F32), vm((QB, HEAD), F32),
                vm((2, 3) + acc, F32), vm((2, HALF + 2, 1, HEAD), F32), vm((4, 2) + acc, F32),
                vm((QB, SEQ), F32), vm((QB, SEQ), F32), vm((QB, SEQ), F32),
                vm((QB, SEQ), BF16), vm((QB, SEQ), BF16), vm((QB, SEQ), BF16),
                vm(tok, BF16), vm(tok, BF16), vm(tok, BF16), vm(tok, BF16), vm(tok, BF16),
                vm(tok_t, BF16), vm(tok_t, BF16), vm(tok_t, BF16), vm(tok_t, BF16), vm(tok_t, BF16),
                vm((4, SEQ, HEAD), BF16), vm((4, HEAD, SEQ), BF16),
                vm((PAIR, HEAD, HALF), F32), vm((PAIR, HEAD, HALF), F32), vm((4, PAIR, HALF, HEAD), BF16),
                dma, dma((4, SUBS)), dma, dma((4,)), dma((2, N_PART)), dma((3,)), dma((SUBS,)), dma((2, SUBS)), dma, dma((SUBS, PAIR)),
                dma((2,)), dma((2, 3)), dma((2, N_PART)), dma((2, 3, N_PART)), dma((2, N_PART)), dma((2, N_PART)), dma((2,)), dma((2,)),
            ],
            compiler_params=pltpu.CompilerParams(collective_id=0, has_side_effects=True, vmem_limit_bytes=36 * 1024 * 1024),
        )(*[pltpu.with_memory_space_constraint(x, pltpu.HBM) for x in (
            query.reshape(pairs), key_in.reshape(pairs), value.reshape(pairs), d_out.reshape(pairs),
            rel_k.reshape(SEQ, N_PAIR, PAIR, head_dim), bias_u.reshape(N_PAIR, PAIR, head_dim), bias_w.reshape(N_PAIR, PAIR, head_dim))])
        o, dq, dk, dv, dr, du, dw = pl.pallas_call(
            writer,
            name="writer",
            out_shape=(act, act, act, act, jax.ShapeDtypeStruct((SEQ, n_heads, 1, head_dim), F32), vec, vec),
            in_specs=[whole] * (6 + N_PART),
            out_specs=[whole] * 7,
            scratch_shapes=[dma((6 + 2 * N_PART,))],
            compiler_params=pltpu.CompilerParams(vmem_limit_bytes=1024 * 1024),
        )(*outs)
        full = query.shape
        return (o.reshape(full), dq.reshape(full), dk.reshape(full), dv.reshape(full),
                du.reshape(bias_u.shape), dw.reshape(bias_w.shape), dr.reshape(rel_k.shape))

    return jax.shard_map(local, mesh=mesh,
                         in_specs=(seq_spec, seq_spec, seq_spec, P(), P(), P(), seq_spec),
                         out_specs=(seq_spec, seq_spec, seq_spec, seq_spec, P(), P(), P()),
                         check_vma=False)
```

```python
import jax
import jax.numpy as jnp
from jax import lax
from jax.experimental import pallas as pl
from jax.experimental.pallas import tpu as pltpu
from jax.sharding import PartitionSpec as P

MESH = pl.DeviceIdType.MESH
BF16, F32 = jnp.bfloat16, jnp.float32
LOG2E = 1.4426950408889634

N_DEV = 16
PLANE = 8
PAIR = 2
N_PAIR = 8
SLOTS = 4
SUBS = 2 * SLOTS
EARLY = 3
ROWS = 64
HALF = PLANE * ROWS
SEQ = 2 * HALF
HEAD = 128
QB = 256
WIN = HALF + QB
N_PART = 4
PART = HALF // N_PART
HOPS = ((1, 2, 4), (2, 1, 4), (1, 2, 4), (2, 1, 4))
TURNS = ((1, 3, 2), (3, 1, 2))


def dot(lhs, rhs):
    return jnp.dot(lhs, rhs, preferred_element_type=F32)


def flip8(x):
    rows, cols = x.shape
    idx = 7 - lax.broadcasted_iota(jnp.int32, (rows // 8, 8, cols), 1)
    return jnp.take_along_axis(x.reshape(rows // 8, 8, cols), idx, axis=1).reshape(rows, cols)


def eye_rev(dtype):
    total = lax.broadcasted_iota(jnp.int32, (HEAD, HEAD), 0) + lax.broadcasted_iota(jnp.int32, (HEAD, HEAD), 1)
    return jnp.where(total == HEAD - 1, 1.0, 0.0).astype(dtype)


def kernel(q_in, k_in, v_in, g_in, r_in, u_in, w_in,
           o_out, dq_out, dk_out, dv_out, dr0_out, dr1_out, dr2_out, dr3_out, du_out, dw_out,
           buf, rbuf, r_buf, u_buf, w_buf, st_tx, st_rx, st_ref, dr_rx, dr_rz, dr_fin, dr_acc,
           s_ref, e_ref, dp_ref, pb_ref, ds_ref, dd_ref,
           a_s, c_s, g_s, k_s, v_s, at_s, ct_s, gt_s, kt_s, vt_s, rev_s, rt_s, dkt, dvt, stage,
           in_send, in_recv, out_send, out_recv, own_sem, r_sem, up_send, up_recv, st_send, st_recv,
           x_send, x_recv, z_send, z_recv, ring_send, ring_recv, fw_send, fw_recv, b_send, b_recv):
    me = lax.axis_index("cp")
    core = me % 2
    chip = me // 2
    col = chip % 4
    z = chip // 4
    partner = me + 1 - 2 * core
    across = me + PLANE * (1 - 2 * z)
    scale = HEAD ** -0.5

    def wait_for(ref, sem):
        pltpu.make_async_copy(ref, ref, sem).wait()

    tables = [pltpu.make_async_copy(src, dst, r_sem.at[j]) for j, (src, dst) in enumerate(
        ((r_in.at[:, pl.ds(2 * col, 2)], r_buf), (u_in.at[pl.ds(2 * col, 2)], u_buf), (w_in.at[pl.ds(2 * col, 2)], w_buf)))]
    for copy in tables:
        copy.start()

    barrier = pltpu.get_barrier_semaphore()

    def say(step, carry):
        pl.semaphore_signal(barrier, inc=1, device_id=((me + step) % N_DEV,), device_id_type=MESH)
        return carry

    lax.fori_loop(1, N_DEV, say, 0)
    pl.semaphore_wait(barrier, N_DEV - 1)

    my_rows = pl.ds(pl.multiple_of((me % PLANE) * ROWS, ROWS), ROWS)

    def peers():
        for near_turn, far_turn in zip(*TURNS):
            turn = jnp.where(core == 0, near_turn, far_turn)
            yield me ^ (2 * turn)
            yield me ^ (2 * turn + 1)
        yield partner

    def send_in(ins, sub):
        pair, row = sub // SLOTS, sub % SLOTS
        for first in (0, 2):
            for t in (first, first + 1):
                pltpu.make_async_copy(ins[t].at[core * SLOTS + row, :, 2 * col + pair], buf.at[t, sub, my_rows], in_recv.at[t, sub]).start()
            for peer in peers():
                for t in (first, first + 1):
                    pltpu.make_async_remote_copy(
                        src_ref=ins[t].at[(peer % 2) * SLOTS + row, :, 2 * ((peer // 2) % 4) + pair], dst_ref=buf.at[t, sub, my_rows],
                        send_sem=in_send, recv_sem=in_recv.at[t, sub], device_id=(peer,), device_id_type=MESH).start()

    def send_all(ins):
        def send_sub(sub, carry):
            send_in(ins, sub)
            return carry
        lax.fori_loop(0, SUBS, send_sub, 0)

    @pl.when(z == 0)
    def _():
        send_all((k_in, v_in, q_in, g_in))

    @pl.when(z == 1)
    def _():
        send_all((q_in, g_in, k_in, v_in))

    for copy in tables:
        copy.wait()
    rev = eye_rev(BF16)
    for p in range(2):
        pair_tab = pltpu.einshape("abc->bac", r_buf[:, p])
        for hh in range(PAIR):
            for blk in range(SEQ // HEAD):
                part = pair_tab[hh, SEQ - HEAD * (blk + 1):SEQ - HEAD * blk]
                flipped = dot(rev, part).astype(BF16)
                rev_s[2 * p + hh, HEAD * blk:HEAD * (blk + 1), :] = flipped
                rt_s[2 * p + hh, :, HEAD * blk:HEAD * (blk + 1)] = flipped.T
    dr_acc[...] = jnp.zeros_like(dr_acc)

    acts = (dk_out, dv_out, o_out, dq_out)

    def send_out(sub, which):
        place = (core * SLOTS + sub % SLOTS, slice(None), 2 * col + sub // SLOTS)
        for t in which:
            pltpu.make_async_copy(buf.at[t, sub, my_rows], acts[t].at[place], out_recv.at[t]).start()
        for peer in peers():
            peer_rows = pl.ds(pl.multiple_of((peer % PLANE) * ROWS, ROWS), ROWS)
            for t in which:
                pltpu.make_async_remote_copy(
                    src_ref=buf.at[t, sub, peer_rows], dst_ref=acts[t].at[place],
                    send_sem=out_send, recv_sem=out_recv.at[t], device_id=(peer,), device_id_type=MESH).start()

    def send_up(sub):
        for j in range(2):
            wait_for(buf.at[j, sub], in_recv.at[j, sub])
            pltpu.make_async_remote_copy(src_ref=buf.at[j, sub], dst_ref=rbuf.at[j, sub], send_sem=up_send.at[sub], recv_sem=up_recv.at[j, sub],
                                         device_id=(across,), device_id_type=MESH).start()

    def unpack(ref, j, sub):
        return pltpu.einshape("abc->bac", ref[j, sub])

    def load_rows(q_ref, q_j, g_ref, g_j, sub, start, turned):
        rows = slice(start, start + HALF)
        p = sub // SLOTS
        q2 = unpack(q_ref, q_j, sub)
        u = u_buf[p].astype(F32)
        w = w_buf[p].astype(F32)
        for hh in range(PAIR):
            q32 = q2[hh].astype(F32)
            a = (q32 + u[hh:hh + 1]).astype(BF16)
            c = (q32 + w[hh:hh + 1]).astype(BF16)
            a_s[hh, rows, :] = a
            c_s[hh, rows, :] = c
            at_s[hh, :, rows] = a.T
            if turned:
                ct_s[hh, :, rows] = flip8(c.astype(F32)).astype(BF16).T
        g2 = unpack(g_ref, g_j, sub)
        g_s[:, rows, :] = g2
        for hh in range(PAIR):
            gt_s[hh, :, rows] = g2[hh].T

    def load_keys(k_ref, k_j, v_ref, v_j, sub, start):
        rows = slice(start, start + HALF)
        k2 = unpack(k_ref, k_j, sub)
        v2 = unpack(v_ref, v_j, sub)
        k_s[:, rows, :] = k2
        v_s[:, rows, :] = v2
        for hh in range(PAIR):
            kt_s[hh, :, rows] = k2[hh].T
            vt_s[hh, :, rows] = v2[hh].T

    def row_block(hh, head, start, i0, lo, fresh, stats):
        width = i0 + QB
        rows = slice(start, start + QB)
        s_ref[:, :width] = dot(a_s[hh, rows, :], kt_s[hh, :, :width])
        e_ref[:, :width] = dot(c_s[hh, rows, :], rt_s[head, :, SEQ - width:])
        dp_ref[:, :width] = dot(g_s[hh, rows, :], vt_s[hh, :, :width])
        for r0 in range(0, QB, 16):
            group = slice(r0, r0 + 16)
            rel = pltpu.roll(e_ref[group, :width], i0 + 1 + r0, 1, stride=1, stride_axis=0)
            s = s_ref[group, :width] + rel
            ahead = lax.broadcasted_iota(jnp.int32, (16, width), 1) - lax.broadcasted_iota(jnp.int32, (16, width), 0)
            s = jnp.where(ahead <= i0 + r0, s, -jnp.inf)
            top = jnp.max(s, axis=1, keepdims=True)
            p = jnp.exp2((s - top) * (scale * LOG2E))
            total = jnp.sum(p, axis=1, keepdims=True)
            p = p * (1.0 / total)
            pb_ref[group, :width] = p.astype(BF16)
            dp = dp_ref[group, :width]
            row_dot = jnp.sum(p * dp, axis=1, keepdims=True)
            ds = (p * (dp - row_dot) * scale).astype(BF16)
            ds_ref[group, :width] = ds
            flipped = flip8(ds.astype(F32))
            half = [pltpu.roll(flipped[8 * j:8 * j + 8], QB - 8 - r0 - 8 * j, 1, stride=1, stride_axis=0) for j in range(2)]
            dd_ref[group, :width] = jnp.concatenate(half, axis=0).astype(BF16)
            if stats:
                lane = lax.broadcasted_iota(jnp.int32, (16, HEAD), 1)
                st_ref[group, :] = jnp.where(lane == 0, top * (scale * LOG2E) + jnp.log2(total), row_dot)
        pb = pb_ref[:, :width]
        ds = ds_ref[:, :width]
        dd = dd_ref[:, :width]
        stage[0, hh, rows, :] = dot(pb, v_s[hh, :width, :]).astype(BF16)
        dqc = dot(ds, k_s[hh, :width, :])
        dqr = flip8(dot(dd, rev_s[head, SEQ - width:, :]))
        stage[1, hh, rows, :] = (dqc + dqr).astype(BF16)
        dr_acc[head, 1, HEAD:HEAD + 1, HALF - HEAD:] += jnp.sum(dqc, axis=0, keepdims=True)
        dr_acc[head, 1, HEAD + 1:HEAD + 2, HALF - HEAD:] += jnp.sum(dqr, axis=0, keepdims=True)
        dk_new = dot(at_s[hh, :, rows], ds_ref[:, lo:width])
        dv_new = dot(gt_s[hh, :, rows], pb_ref[:, lo:width])
        if fresh:
            dkt[hh] = dk_new
            dvt[hh] = dv_new
        else:
            dkt[hh, :, :width - lo] += dk_new
            dvt[hh, :, :width - lo] += dv_new
        dr_new = dot(ct_s[hh, :, rows], dd)
        if width > HALF:
            dr_acc[head, 0, :HEAD, SEQ - width:] += dr_new[:, :width - HALF]
            dr_acc[head, 1, :HEAD, :] += dr_new[:, width - HALF:]
        else:
            dr_acc[head, 1, :HEAD, HALF - width:] += dr_new

    def col_block(hh, head, sub, i0):
        rows = slice(i0, i0 + QB)
        first = WIN - i0
        s_ref[:, :HALF] = dot(a_s[hh, rows, :], kt_s[hh, :, :HALF])
        e_ref[:, :WIN] = dot(c_s[hh, rows, :], rt_s[head, :, first:first + WIN])
        dp_ref[:, :HALF] = dot(g_s[hh, rows, :], vt_s[hh, :, :HALF])
        st_ref[:, :8] = st_rx[sub, hh, :, i0 - HALF:i0 - HALF + QB].T
        for r0 in range(0, QB, 16):
            group = slice(r0, r0 + 16)
            rel = pltpu.roll(e_ref[group, :WIN], HALF + 1 + r0, 1, stride=1, stride_axis=0)[:, :HALF]
            log_sum = st_ref[group, 0:1]
            row_dot = st_ref[group, 1:2]
            p = jnp.exp2((s_ref[group, :HALF] + rel) * (scale * LOG2E) - log_sum)
            pb_ref[group, :HALF] = p.astype(BF16)
            ds_ref[group, :HALF] = (p * (dp_ref[group, :HALF] - row_dot) * scale).astype(BF16)
        dkt[hh] += dot(at_s[hh, :, rows], ds_ref[:, :HALF])
        dvt[hh] += dot(gt_s[hh, :, rows], pb_ref[:, :HALF])

    def store_rows(sub):
        for t in range(2):
            buf[2 + t, sub] = pltpu.einshape("abc->bac", stage[t])

    def store_keys(sub):
        for hh in range(PAIR):
            stage[2, hh] = dkt[hh].astype(BF16).T
            stage[3, hh] = dvt[hh].astype(BF16).T
        for t in range(2):
            buf[t, sub] = pltpu.einshape("abc->bac", stage[2 + t])

    def wait_up(sub):
        for j in range(2):
            wait_for(rbuf.at[j, sub], up_recv.at[j, sub])
        wait_for(rbuf.at[:, sub], up_send.at[sub])

    def wait_in(sub):
        for j in range(2, 4):
            wait_for(buf.at[j, sub], in_recv.at[j, sub])

    def lower_rows(sub):
        wait_in(sub)
        load_rows(buf, 2, buf, 3, sub, 0, True)

    def lower_own(sub):
        load_keys(buf, 0, buf, 1, sub, 0)

        def own(hh, carry):
            head = 2 * (sub // SLOTS) + hh
            row_block(hh, head, QB, QB, 0, True, False)
            row_block(hh, head, 0, 0, 0, False, False)
            return carry

        lax.fori_loop(0, PAIR, own, 0)
        store_rows(sub)

    def lower_theirs(sub):
        wait_up(sub)
        load_rows(rbuf, 0, rbuf, 1, sub, HALF, False)

        def theirs(hh, carry):
            head = 2 * (sub // SLOTS) + hh
            wait_for(st_rx.at[sub, hh], st_recv.at[sub, hh])
            col_block(hh, head, sub, HALF)
            col_block(hh, head, sub, HALF + QB)
            return carry

        lax.fori_loop(0, PAIR, theirs, 0)
        store_keys(sub)

    def upper_own(sub):
        wait_in(sub)
        wait_up(sub)
        load_rows(buf, 0, buf, 1, sub, 0, True)
        load_keys(rbuf, 0, rbuf, 1, sub, 0)
        load_keys(buf, 2, buf, 3, sub, HALF)

        def own(hh, carry):
            head = 2 * (sub // SLOTS) + hh
            for blk in (1, 0):
                row_block(hh, head, QB * blk, HALF + QB * blk, HALF, blk == 1, True)
                st_tx[sub, hh, :, QB * blk:QB * (blk + 1)] = st_ref[...].T[:8]
            pltpu.make_async_remote_copy(src_ref=st_tx.at[sub, hh], dst_ref=st_rx.at[sub, hh], send_sem=st_send, recv_sem=st_recv.at[sub, hh],
                                         device_id=(across,), device_id_type=MESH).start()
            return carry

        lax.fori_loop(0, PAIR, own, 0)
        store_rows(sub)
        store_keys(sub)

    side = 1 - core
    parts = (dr0_out, dr1_out, dr2_out, dr3_out)

    def swap_start(p):
        for n in range(2):
            pltpu.make_async_remote_copy(src_ref=dr_acc.at[2 * p + n, side], dst_ref=dr_rx.at[p, n], send_sem=x_send.at[p], recv_sem=x_recv.at[p, n],
                                         device_id=(partner,), device_id_type=MESH).start()

    def swap_add(p):
        for n in range(2):
            wait_for(dr_rx.at[p, n], x_recv.at[p, n])
            dr_rx[p, n] = dr_rx[p, n] + dr_acc[2 * p + n, core]

    def cross_start(p):
        pltpu.make_async_remote_copy(src_ref=dr_rx.at[p, 1 - z], dst_ref=dr_rz.at[p], send_sem=z_send.at[p], recv_sem=z_recv.at[p],
                                     device_id=(across,), device_id_type=MESH).start()

    def head_of(p, bits):
        other = chip ^ bits
        return 4 * (other % 4) + 2 * p + other // 4

    def block(p, m, bits):
        if bits == 0:
            return dr_fin.at[p, PART * m:PART * (m + 1)]
        return parts[m].at[side, :, head_of(p, bits)]

    def forward(p, m, bits):
        pltpu.make_async_remote_copy(src_ref=block(p, m, bits), dst_ref=parts[m].at[side, :, head_of(p, bits)], send_sem=fw_send.at[p, m],
                                     recv_sem=fw_recv.at[p, m], device_id=(partner,), device_id_type=MESH).start()

    def held(m, hop):
        have = [0]
        for bit in HOPS[m][:hop]:
            have = have + [bits ^ bit for bits in have]
        return have

    def hop_start(p, hop):
        for m in range(N_PART):
            for bits in held(m, hop):
                pltpu.make_async_remote_copy(
                    src_ref=block(p, m, bits), dst_ref=parts[m].at[side, :, head_of(p, bits)], send_sem=ring_send.at[p, m],
                    recv_sem=ring_recv.at[p, hop, m], device_id=(me ^ (2 * HOPS[m][hop]),), device_id_type=MESH).start()

    def hop_wait(p, hop):
        for m in range(N_PART):
            have = held(m, hop + 1)
            wait_for(parts[m].at[0, :, :len(have) // 2], ring_recv.at[p, hop, m])
            for bits in have[len(have) // 2:]:
                forward(p, m, bits)

    def cross_finish(p):
        wait_for(dr_rz.at[p], z_recv.at[p])
        total = dr_rx[p, z] + dr_rz[p]
        rev32 = eye_rev(F32)
        for m in range(N_PART):
            part = total[:HEAD, HALF - HEAD * (m + 1):HALF - HEAD * m]
            turned = lax.dot_general(rev32, part, (((1,), (1,)), ((), ())), precision=lax.Precision.HIGHEST, preferred_element_type=F32)
            dr_fin[p, HEAD * m:HEAD * (m + 1)] = turned.reshape(HEAD, 1, HEAD)
        dr_fin[p, HALF] = total[HEAD:HEAD + 1, HALF - HEAD:]
        dr_fin[p, HALF + 1] = total[HEAD + 1:HEAD + 2, HALF - HEAD:]
        hop_start(p, 0)
        head = head_of(p, 0)
        for m in range(N_PART):
            pltpu.make_async_copy(block(p, m, 0), parts[m].at[side, :, head], own_sem.at[p, m]).start()
            forward(p, m, 0)

        @pl.when(core == 1)
        def _():
            for j, dst in enumerate((du_out, dw_out)):
                pltpu.make_async_copy(dr_fin.at[p, HALF + j], dst.at[head], b_recv.at[j]).start()
                for step in range(1, N_DEV):
                    pltpu.make_async_remote_copy(
                        src_ref=dr_fin.at[p, HALF + j], dst_ref=dst.at[head], send_sem=b_send.at[j], recv_sem=b_recv.at[j],
                        device_id=(me ^ step,), device_id_type=MESH).start()

    send_up(0)

    def sub_body(sub, carry):
        @pl.when(sub < SUBS - 1)
        def _():
            send_up(sub + 1)

        @pl.when(sub == SLOTS)
        def _():
            swap_start(0)

        @pl.when(sub == SUBS - 1)
        def _():
            swap_add(0)
            cross_start(0)

        @pl.when(sub == SUBS)
        def _():
            swap_start(1)
            cross_finish(0)

        @pl.when((z == 0) & (sub < SUBS))
        def _():
            lower_rows(sub)

        @pl.when((z == 0) & (sub > 0))
        def _():
            lower_theirs(sub - 1)

        @pl.when((z == 0) & (sub < SUBS))
        def _():
            lower_own(sub)

        @pl.when((z == 1) & (sub < SUBS))
        def _():
            upper_own(sub)

        @pl.when(sub < EARLY)
        def _():
            send_out(sub, (2, 3))

        @pl.when((sub > 0) & (sub <= EARLY))
        def _():
            send_out(sub - 1, (0, 1))
        return carry

    lax.fori_loop(0, SUBS + 1, sub_body, 0)

    swap_add(1)
    cross_start(1)
    cross_finish(1)
    for p in range(2):
        hop_wait(p, 0)
        hop_start(p, 1)

    def send_late(sub, carry):
        send_out(sub, range(4))
        return carry

    lax.fori_loop(EARLY, EARLY + 2, send_late, 0)
    for p in range(2):
        hop_wait(p, 1)
        hop_start(p, 2)
    lax.fori_loop(EARLY + 2, SUBS, send_late, 0)
    for p in range(2):
        hop_wait(p, 2)

    for t, dst in enumerate(acts):
        wait_for(dst, out_recv.at[t])
    for j, dst in enumerate((du_out, dw_out)):
        wait_for(dst, b_recv.at[j])

        @pl.when(core == 1)
        def _():
            wait_for(dr_fin.at[0, :2 * (N_DEV - 1)], b_send.at[j])
    wait_for(buf.at[:, :, :HALF - ROWS], in_send)
    wait_for(buf.at[:, :, :HALF - ROWS], out_send)

    @pl.when(z == 1)
    def _():
        wait_for(st_tx, st_send)

    for p in range(2):
        wait_for(dr_rx.at[p], x_send.at[p])
        wait_for(dr_rz.at[p], z_send.at[p])
        for m in range(N_PART):
            wait_for(dr_fin.at[p, :PART], own_sem.at[p, m])
            wait_for(parts[m].at[0, :, :N_PAIR - 1], ring_send.at[p, m])
            wait_for(parts[m].at[0, :, :N_PAIR], fw_send.at[p, m])
            wait_for(parts[m].at[0, :, :N_PAIR], fw_recv.at[p, m])


def writer(*refs):
    ins, (o, dq, dk, dv, dr, du, dw, sem) = refs[:6 + N_PART], refs[6 + N_PART:]
    pairs = list(zip(ins[:4] + ins[-2:], (o, dq, dk, dv, du, dw)))
    for m, part in enumerate(ins[4:-2]):
        for side in range(2):
            start = HALF * side + PART * m
            pairs.append((part.at[side], dr.at[start:start + PART]))
    copies = [pltpu.make_async_copy(src, dst, sem.at[j]) for j, (src, dst) in enumerate(pairs)]
    for copy in copies:
        copy.start()
    for copy in copies:
        copy.wait()


def solution(mesh):
    seq_spec = P(None, "cp", None, None)

    def local(query, key_in, value, bias_u, bias_w, rel_k, d_out):
        n_batch, rows, n_heads, head_dim = query.shape
        pairs = (n_batch, rows, N_PAIR, PAIR, head_dim)
        vm = pltpu.VMEM
        dma = pltpu.SemaphoreType.DMA
        whole = pl.BlockSpec(memory_space=pl.ANY)
        act = jax.ShapeDtypeStruct(pairs, BF16)
        vec = jax.ShapeDtypeStruct((n_heads, 1, head_dim), F32)
        tok = (PAIR, SEQ, HEAD)
        tok_t = (PAIR, HEAD, SEQ)
        acc = (HEAD + 8, HALF)
        outs = pl.pallas_call(
            kernel,
            name="rel_attn",
            out_shape=(act, act, act, act,
                       *[jax.ShapeDtypeStruct((2, PART, n_heads, 1, head_dim), F32)] * N_PART,
                       vec, vec),
            in_specs=[pl.BlockSpec(memory_space=pltpu.HBM)] * 7,
            out_specs=[whole] * (6 + N_PART),
            scratch_shapes=[
                vm((4, SUBS, HALF, PAIR, HEAD), BF16), vm((2, SUBS, HALF, PAIR, HEAD), BF16),
                vm((SEQ, 2, PAIR, HEAD), BF16), vm((2, PAIR, HEAD), BF16), vm((2, PAIR, HEAD), BF16),
                vm((SUBS, PAIR, 8, HALF), F32), vm((SUBS, PAIR, 8, HALF), F32), vm((QB, HEAD), F32),
                vm((2, 2) + acc, F32), vm((2,) + acc, F32), vm((2, HALF + 2, 1, HEAD), F32), vm((4, 2) + acc, F32),
                vm((QB, SEQ), F32), vm((QB, SEQ), F32), vm((QB, SEQ), F32),
                vm((QB, SEQ), BF16), vm((QB, SEQ), BF16), vm((QB, SEQ), BF16),
                vm(tok, BF16), vm(tok, BF16), vm(tok, BF16), vm(tok, BF16), vm(tok, BF16),
                vm(tok_t, BF16), vm(tok_t, BF16), vm(tok_t, BF16), vm(tok_t, BF16), vm(tok_t, BF16),
                vm((4, SEQ, HEAD), BF16), vm((4, HEAD, SEQ), BF16),
                vm((PAIR, HEAD, HALF), F32), vm((PAIR, HEAD, HALF), F32), vm((4, PAIR, HALF, HEAD), BF16),
                dma, dma((4, SUBS)), dma, dma((4,)), dma((2, N_PART)), dma((3,)), dma((SUBS,)), dma((2, SUBS)), dma, dma((SUBS, PAIR)),
                dma((2,)), dma((2, 2)), dma((2,)), dma((2,)), dma((2, N_PART)), dma((2, 3, N_PART)), dma((2, N_PART)), dma((2, N_PART)), dma((2,)), dma((2,)),
            ],
            compiler_params=pltpu.CompilerParams(collective_id=0, has_side_effects=True, vmem_limit_bytes=36 * 1024 * 1024),
        )(*[pltpu.with_memory_space_constraint(x, pltpu.HBM) for x in (
            query.reshape(pairs), key_in.reshape(pairs), value.reshape(pairs), d_out.reshape(pairs),
            rel_k.reshape(SEQ, N_PAIR, PAIR, head_dim), bias_u.reshape(N_PAIR, PAIR, head_dim), bias_w.reshape(N_PAIR, PAIR, head_dim))])
        o, dq, dk, dv, dr, du, dw = pl.pallas_call(
            writer,
            name="writer",
            out_shape=(act, act, act, act, jax.ShapeDtypeStruct((SEQ, n_heads, 1, head_dim), F32), vec, vec),
            in_specs=[whole] * (6 + N_PART),
            out_specs=[whole] * 7,
            scratch_shapes=[dma((6 + 2 * N_PART,))],
            compiler_params=pltpu.CompilerParams(vmem_limit_bytes=1024 * 1024),
        )(*outs)
        full = query.shape
        return (o.reshape(full), dq.reshape(full), dk.reshape(full), dv.reshape(full),
                du.reshape(bias_u.shape), dw.reshape(bias_w.shape), dr.reshape(rel_k.shape))

    return jax.shard_map(local, mesh=mesh,
                         in_specs=(seq_spec, seq_spec, seq_spec, P(), P(), P(), seq_spec),
                         out_specs=(seq_spec, seq_spec, seq_spec, seq_spec, P(), P(), P()),
                         check_vma=False)
```

```python
import jax
import jax.numpy as jnp
from jax import lax
from jax.experimental import pallas as pl
from jax.experimental.pallas import tpu as pltpu
from jax.sharding import PartitionSpec as P

MESH = pl.DeviceIdType.MESH
BF16, F32 = jnp.bfloat16, jnp.float32
LOG2E = 1.4426950408889634

N_DEV = 16
PLANE = 8
PAIR = 2
N_PAIR = 8
SLOTS = 4
SUBS = 2 * SLOTS
EARLY = 3
ROWS = 64
HALF = PLANE * ROWS
SEQ = 2 * HALF
HEAD = 128
QB = 256
WIN = HALF + QB
N_PART = 6
PART = 86
FIN = N_PART * PART
HOPS = ((1, 2, 4), (2, 1, 4)) * 3
TURNS = ((1, 3, 2), (3, 1, 2))


def dot(lhs, rhs):
    return jnp.dot(lhs, rhs, preferred_element_type=F32)


def flip8(x):
    rows, cols = x.shape
    idx = 7 - lax.broadcasted_iota(jnp.int32, (rows // 8, 8, cols), 1)
    return jnp.take_along_axis(x.reshape(rows // 8, 8, cols), idx, axis=1).reshape(rows, cols)


def eye_rev(dtype):
    total = lax.broadcasted_iota(jnp.int32, (HEAD, HEAD), 0) + lax.broadcasted_iota(jnp.int32, (HEAD, HEAD), 1)
    return jnp.where(total == HEAD - 1, 1.0, 0.0).astype(dtype)


def kernel(q_in, k_in, v_in, g_in, r_in, u_in, w_in,
           o_out, dq_out, dk_out, dv_out, dr0_out, dr1_out, dr2_out, dr3_out, dr4_out, dr5_out,
           buf, rbuf, r_buf, u_buf, w_buf, st_tx, st_rx, st_ref, dr_rx, dr_rz, dr_fin, dr_acc,
           s_ref, e_ref, dp_ref, pb_ref, ds_ref, dd_ref,
           a_s, c_s, g_s, k_s, v_s, at_s, ct_s, gt_s, kt_s, vt_s, rev_s, rt_s, dkt, dvt, stage,
           in_send, in_recv, out_send, out_recv, own_sem, r_sem, up_send, up_recv, st_send, st_recv,
           x_send, x_recv, z_send, z_recv, ring_send, ring_recv, fw_send, fw_recv):
    me = lax.axis_index("cp")
    core = me % 2
    chip = me // 2
    col = chip % 4
    z = chip // 4
    partner = me + 1 - 2 * core
    across = me + PLANE * (1 - 2 * z)
    scale = HEAD ** -0.5

    def wait_for(ref, sem):
        pltpu.make_async_copy(ref, ref, sem).wait()

    tables = [pltpu.make_async_copy(src, dst, r_sem.at[j]) for j, (src, dst) in enumerate(
        ((r_in.at[:, pl.ds(2 * col, 2)], r_buf), (u_in.at[pl.ds(2 * col, 2)], u_buf), (w_in.at[pl.ds(2 * col, 2)], w_buf)))]
    for copy in tables:
        copy.start()

    barrier = pltpu.get_barrier_semaphore()

    for peer in [across] + [me ^ step for step in range(PLANE - 1, 0, -1)]:
        pl.semaphore_signal(barrier, inc=1, device_id=(peer,), device_id_type=MESH)
    pl.semaphore_wait(barrier, PLANE)

    my_rows = pl.ds(pl.multiple_of((me % PLANE) * ROWS, ROWS), ROWS)

    def peers():
        for near_turn, far_turn in zip(*TURNS):
            turn = jnp.where(core == 0, near_turn, far_turn)
            yield me ^ (2 * turn)
            yield me ^ (2 * turn + 1)
        yield partner

    def send_in(ins, sub):
        pair, row = sub // SLOTS, sub % SLOTS
        for first in (0, 2):
            for t in (first, first + 1):
                pltpu.make_async_copy(ins[t].at[core * SLOTS + row, :, 2 * col + pair], buf.at[t, sub, my_rows], in_recv.at[first // 2, sub]).start()
            for peer in peers():
                for t in (first, first + 1):
                    pltpu.make_async_remote_copy(
                        src_ref=ins[t].at[(peer % 2) * SLOTS + row, :, 2 * ((peer // 2) % 4) + pair], dst_ref=buf.at[t, sub, my_rows],
                        send_sem=in_send, recv_sem=in_recv.at[first // 2, sub], device_id=(peer,), device_id_type=MESH).start()

    def send_all(ins):
        def send_sub(sub, carry):
            send_in(ins, sub)
            return carry
        lax.fori_loop(0, SUBS, send_sub, 0)

    @pl.when(z == 0)
    def _():
        send_all((k_in, v_in, q_in, g_in))

    @pl.when(z == 1)
    def _():
        send_all((q_in, g_in, k_in, v_in))

    for copy in tables:
        copy.wait()
    rev = eye_rev(BF16)
    for p in range(2):
        pair_tab = pltpu.einshape("abc->bac", r_buf[:, p])
        for hh in range(PAIR):
            for blk in range(SEQ // HEAD):
                part = pair_tab[hh, SEQ - HEAD * (blk + 1):SEQ - HEAD * blk]
                flipped = dot(rev, part).astype(BF16)
                rev_s[2 * p + hh, HEAD * blk:HEAD * (blk + 1), :] = flipped
                rt_s[2 * p + hh, :, HEAD * blk:HEAD * (blk + 1)] = flipped.T
    dr_acc[...] = jnp.zeros_like(dr_acc)

    acts = (dk_out, dv_out, o_out, dq_out)

    def send_out(sub, which):
        place = (core * SLOTS + sub % SLOTS, slice(None), 2 * col + sub // SLOTS)
        for t in which:
            pltpu.make_async_copy(buf.at[t, sub, my_rows], acts[t].at[place], out_recv).start()
        for peer in peers():
            peer_rows = pl.ds(pl.multiple_of((peer % PLANE) * ROWS, ROWS), ROWS)
            for t in which:
                pltpu.make_async_remote_copy(
                    src_ref=buf.at[t, sub, peer_rows], dst_ref=acts[t].at[place],
                    send_sem=out_send, recv_sem=out_recv, device_id=(peer,), device_id_type=MESH).start()

    def send_up(sub):
        wait_for(buf.at[0:2, sub], in_recv.at[0, sub])
        for j in range(2):
            pltpu.make_async_remote_copy(src_ref=buf.at[j, sub], dst_ref=rbuf.at[j, sub], send_sem=up_send.at[sub % 4], recv_sem=up_recv.at[sub],
                                         device_id=(across,), device_id_type=MESH).start()

    def unpack(ref, j, sub):
        return pltpu.einshape("abc->bac", ref[j, sub])

    def load_rows(q_ref, q_j, g_ref, g_j, sub, start, turned):
        rows = slice(start, start + HALF)
        p = sub // SLOTS
        q2 = unpack(q_ref, q_j, sub)
        u = u_buf[p].astype(F32)
        w = w_buf[p].astype(F32)
        for hh in range(PAIR):
            q32 = q2[hh].astype(F32)
            a = (q32 + u[hh:hh + 1]).astype(BF16)
            c = (q32 + w[hh:hh + 1]).astype(BF16)
            a_s[hh, rows, :] = a
            c_s[hh, rows, :] = c
            at_s[hh, :, rows] = a.T
            if turned:
                ct_s[hh, :, rows] = flip8(c.astype(F32)).astype(BF16).T
        g2 = unpack(g_ref, g_j, sub)
        g_s[:, rows, :] = g2
        for hh in range(PAIR):
            gt_s[hh, :, rows] = g2[hh].T

    def load_keys(k_ref, k_j, v_ref, v_j, sub, start):
        rows = slice(start, start + HALF)
        k2 = unpack(k_ref, k_j, sub)
        v2 = unpack(v_ref, v_j, sub)
        k_s[:, rows, :] = k2
        v_s[:, rows, :] = v2
        for hh in range(PAIR):
            kt_s[hh, :, rows] = k2[hh].T
            vt_s[hh, :, rows] = v2[hh].T

    def row_block(hh, head, start, i0, lo, fresh, stats):
        width = i0 + QB
        rows = slice(start, start + QB)
        s_ref[:, :width] = dot(a_s[hh, rows, :], kt_s[hh, :, :width])
        e_ref[:, :width] = dot(c_s[hh, rows, :], rt_s[head, :, SEQ - width:])
        dp_ref[:, :width] = dot(g_s[hh, rows, :], vt_s[hh, :, :width])
        for r0 in range(0, QB, 16):
            group = slice(r0, r0 + 16)
            rel = pltpu.roll(e_ref[group, :width], i0 + 1 + r0, 1, stride=1, stride_axis=0)
            s = s_ref[group, :width] + rel
            ahead = lax.broadcasted_iota(jnp.int32, (16, width), 1) - lax.broadcasted_iota(jnp.int32, (16, width), 0)
            s = jnp.where(ahead <= i0 + r0, s, -jnp.inf)
            top = jnp.max(s, axis=1, keepdims=True)
            p = jnp.exp2((s - top) * (scale * LOG2E))
            total = jnp.sum(p, axis=1, keepdims=True)
            p = p * (1.0 / total)
            pb_ref[group, :width] = p.astype(BF16)
            dp = dp_ref[group, :width]
            row_dot = jnp.sum(p * dp, axis=1, keepdims=True)
            ds = (p * (dp - row_dot) * scale).astype(BF16)
            ds_ref[group, :width] = ds
            flipped = flip8(ds.astype(F32))
            half = [pltpu.roll(flipped[8 * j:8 * j + 8], QB - 8 - r0 - 8 * j, 1, stride=1, stride_axis=0) for j in range(2)]
            dd_ref[group, :width] = jnp.concatenate(half, axis=0).astype(BF16)
            if stats:
                lane = lax.broadcasted_iota(jnp.int32, (16, HEAD), 1)
                st_ref[group, :] = jnp.where(lane == 0, top * (scale * LOG2E) + jnp.log2(total), row_dot)
        pb = pb_ref[:, :width]
        ds = ds_ref[:, :width]
        dd = dd_ref[:, :width]
        stage[0, hh, rows, :] = dot(pb, v_s[hh, :width, :]).astype(BF16)
        dqc = dot(ds, k_s[hh, :width, :])
        dqr = flip8(dot(dd, rev_s[head, SEQ - width:, :]))
        stage[1, hh, rows, :] = (dqc + dqr).astype(BF16)
        dr_acc[head, 1, HEAD:HEAD + 1, HALF - HEAD:] += jnp.sum(dqc, axis=0, keepdims=True)
        dr_acc[head, 1, HEAD + 1:HEAD + 2, HALF - HEAD:] += jnp.sum(dqr, axis=0, keepdims=True)
        dk_new = dot(at_s[hh, :, rows], ds_ref[:, lo:width])
        dv_new = dot(gt_s[hh, :, rows], pb_ref[:, lo:width])
        if fresh:
            dkt[hh] = dk_new
            dvt[hh] = dv_new
        else:
            dkt[hh, :, :width - lo] += dk_new
            dvt[hh, :, :width - lo] += dv_new
        dr_new = dot(ct_s[hh, :, rows], dd)
        if width > HALF:
            dr_acc[head, 0, :HEAD, SEQ - width:] += dr_new[:, :width - HALF]
            dr_acc[head, 1, :HEAD, :] += dr_new[:, width - HALF:]
        else:
            dr_acc[head, 1, :HEAD, HALF - width:] += dr_new

    def col_block(hh, head, sub, i0):
        rows = slice(i0, i0 + QB)
        first = WIN - i0
        s_ref[:, :HALF] = dot(a_s[hh, rows, :], kt_s[hh, :, :HALF])
        e_ref[:, :WIN] = dot(c_s[hh, rows, :], rt_s[head, :, first:first + WIN])
        dp_ref[:, :HALF] = dot(g_s[hh, rows, :], vt_s[hh, :, :HALF])
        st_ref[:, :8] = st_rx[sub, hh, :, i0 - HALF:i0 - HALF + QB].T
        for r0 in range(0, QB, 16):
            group = slice(r0, r0 + 16)
            rel = pltpu.roll(e_ref[group, :WIN], HALF + 1 + r0, 1, stride=1, stride_axis=0)[:, :HALF]
            log_sum = st_ref[group, 0:1]
            row_dot = st_ref[group, 1:2]
            p = jnp.exp2((s_ref[group, :HALF] + rel) * (scale * LOG2E) - log_sum)
            pb_ref[group, :HALF] = p.astype(BF16)
            ds_ref[group, :HALF] = (p * (dp_ref[group, :HALF] - row_dot) * scale).astype(BF16)
        dkt[hh] += dot(at_s[hh, :, rows], ds_ref[:, :HALF])
        dvt[hh] += dot(gt_s[hh, :, rows], pb_ref[:, :HALF])

    def store_rows(sub):
        for t in range(2):
            buf[2 + t, sub] = pltpu.einshape("abc->bac", stage[t])

    def store_keys(sub):
        for hh in range(PAIR):
            stage[2, hh] = dkt[hh].astype(BF16).T
            stage[3, hh] = dvt[hh].astype(BF16).T
        for t in range(2):
            buf[t, sub] = pltpu.einshape("abc->bac", stage[2 + t])

    def wait_up(sub):
        wait_for(rbuf.at[:, sub], up_recv.at[sub])
        wait_for(rbuf.at[:, sub], up_send.at[sub % 4])

    def wait_in(sub):
        wait_for(buf.at[2:4, sub], in_recv.at[1, sub])

    def lower_rows(sub):
        wait_in(sub)
        load_rows(buf, 2, buf, 3, sub, 0, True)

    def lower_own(sub):
        load_keys(buf, 0, buf, 1, sub, 0)

        def own(hh, carry):
            head = 2 * (sub // SLOTS) + hh
            row_block(hh, head, QB, QB, 0, True, False)
            row_block(hh, head, 0, 0, 0, False, False)
            return carry

        lax.fori_loop(0, PAIR, own, 0)
        store_rows(sub)

    def lower_theirs(sub):
        wait_up(sub)
        load_rows(rbuf, 0, rbuf, 1, sub, HALF, False)
        wait_for(st_rx.at[sub], st_recv.at[sub])

        def theirs(hh, carry):
            head = 2 * (sub // SLOTS) + hh
            col_block(hh, head, sub, HALF)
            col_block(hh, head, sub, HALF + QB)
            return carry

        lax.fori_loop(0, PAIR, theirs, 0)
        store_keys(sub)

    def upper_own(sub):
        wait_in(sub)
        wait_up(sub)
        load_rows(buf, 0, buf, 1, sub, 0, True)
        load_keys(rbuf, 0, rbuf, 1, sub, 0)
        load_keys(buf, 2, buf, 3, sub, HALF)

        def own(hh, carry):
            head = 2 * (sub // SLOTS) + hh
            for blk in (1, 0):
                row_block(hh, head, QB * blk, HALF + QB * blk, HALF, blk == 1, True)
                st_tx[sub, hh, :, QB * blk:QB * (blk + 1)] = st_ref[...].T[:8]
            pltpu.make_async_remote_copy(src_ref=st_tx.at[sub, hh], dst_ref=st_rx.at[sub, hh], send_sem=st_send, recv_sem=st_recv.at[sub],
                                         device_id=(across,), device_id_type=MESH).start()
            return carry

        lax.fori_loop(0, PAIR, own, 0)
        store_rows(sub)
        store_keys(sub)

    side = 1 - core
    parts = (dr0_out, dr1_out, dr2_out, dr3_out, dr4_out, dr5_out)

    def swap_start(p):
        for n in range(2):
            pltpu.make_async_remote_copy(src_ref=dr_acc.at[2 * p + n, side], dst_ref=dr_rx.at[p, n], send_sem=x_send.at[p], recv_sem=x_recv.at[p],
                                         device_id=(partner,), device_id_type=MESH).start()

    def swap_add(p):
        wait_for(dr_rx.at[p], x_recv.at[p])
        for n in range(2):
            dr_rx[p, n] = dr_rx[p, n] + dr_acc[2 * p + n, core]

    def cross_start(p):
        pltpu.make_async_remote_copy(src_ref=dr_rx.at[p, 1 - z], dst_ref=dr_rz.at[p], send_sem=z_send.at[p], recv_sem=z_recv.at[p],
                                     device_id=(across,), device_id_type=MESH).start()

    def head_of(p, bits):
        other = chip ^ bits
        return 4 * (other % 4) + 2 * p + other // 4

    def block(p, m, bits):
        if bits == 0:
            return dr_fin.at[p, PART * m:PART * (m + 1)]
        return parts[m].at[side, :, head_of(p, bits)]

    def forward(p, m, bits):
        pltpu.make_async_remote_copy(src_ref=block(p, m, bits), dst_ref=parts[m].at[side, :, head_of(p, bits)], send_sem=fw_send.at[p, m // 3],
                                     recv_sem=fw_recv.at[p, m // 3], device_id=(partner,), device_id_type=MESH).start()

    def held(m, hop):
        have = [0]
        for bit in HOPS[m][:hop]:
            have = have + [bits ^ bit for bits in have]
        return have

    def blocks(count):
        return parts[0].at[:, :, :count // 2]

    def hop_start(p, hop):
        for m in range(N_PART):
            for bits in held(m, hop):
                pltpu.make_async_remote_copy(
                    src_ref=block(p, m, bits), dst_ref=parts[m].at[side, :, head_of(p, bits)], send_sem=ring_send.at[p, hop],
                    recv_sem=ring_recv.at[p, hop], device_id=(me ^ (2 * HOPS[m][hop]),), device_id_type=MESH).start()

    def hop_wait(p, hop):
        wait_for(blocks(N_PART << hop), ring_recv.at[p, hop])
        for m in range(N_PART):
            have = held(m, hop + 1)
            for bits in have[len(have) // 2:]:
                forward(p, m, bits)

    def cross_finish(p):
        wait_for(dr_rz.at[p], z_recv.at[p])
        total = dr_rx[p, z] + dr_rz[p]
        rev32 = eye_rev(F32)
        for m in range(HALF // HEAD):
            part = total[:HEAD, HALF - HEAD * (m + 1):HALF - HEAD * m]
            turned = lax.dot_general(rev32, part, (((1,), (1,)), ((), ())), precision=lax.Precision.HIGHEST, preferred_element_type=F32)
            dr_fin[p, HEAD * m:HEAD * (m + 1)] = turned.reshape(HEAD, 1, HEAD)
        dr_fin[p, HALF] = total[HEAD:HEAD + 1, HALF - HEAD:]
        dr_fin[p, HALF + 1] = total[HEAD + 1:HEAD + 2, HALF - HEAD:]
        dr_fin[p, HALF + 2:] = jnp.zeros((FIN - HALF - 2, 1, HEAD), F32)
        hop_start(p, 0)
        for m in range(N_PART):
            pltpu.make_async_copy(block(p, m, 0), parts[m].at[side, :, head_of(p, 0)], own_sem.at[p]).start()
            forward(p, m, 0)

    send_up(0)

    def sub_body(sub, carry):
        @pl.when(sub < SUBS - 1)
        def _():
            send_up(sub + 1)

        @pl.when(sub == SLOTS)
        def _():
            swap_start(0)

        @pl.when(sub == SUBS - 1)
        def _():
            swap_add(0)
            cross_start(0)

        @pl.when(sub == SUBS)
        def _():
            swap_start(1)
            cross_finish(0)

        @pl.when((z == 0) & (sub < SUBS))
        def _():
            lower_rows(sub)

        @pl.when((z == 0) & (sub > 0))
        def _():
            lower_theirs(sub - 1)

        @pl.when((z == 0) & (sub < SUBS))
        def _():
            lower_own(sub)

        @pl.when((z == 1) & (sub < SUBS))
        def _():
            upper_own(sub)

        @pl.when(sub < EARLY)
        def _():
            send_out(sub, (2, 3))

        @pl.when((sub > 0) & (sub <= EARLY))
        def _():
            send_out(sub - 1, (0, 1))
        return carry

    lax.fori_loop(0, SUBS + 1, sub_body, 0)

    swap_add(1)
    cross_start(1)
    cross_finish(1)
    for p in range(2):
        hop_wait(p, 0)
        hop_start(p, 1)

    def send_late(sub, carry):
        send_out(sub, range(4))
        return carry

    lax.fori_loop(EARLY, EARLY + 2, send_late, 0)
    for p in range(2):
        hop_wait(p, 1)
        hop_start(p, 2)
    lax.fori_loop(EARLY + 2, SUBS, send_late, 0)
    for p in range(2):
        hop_wait(p, 2)

    wait_for(buf, out_recv)
    wait_for(buf.at[:, :, :HALF - ROWS], in_send)
    wait_for(buf.at[:, :, :HALF - ROWS], out_send)

    @pl.when(z == 1)
    def _():
        wait_for(st_tx, st_send)

    for p in range(2):
        wait_for(dr_rx.at[p], x_send.at[p])
        wait_for(dr_rz.at[p], z_send.at[p])
        wait_for(blocks(N_PART), own_sem.at[p])
        for hop in range(3):
            wait_for(blocks(N_PART << hop), ring_send.at[p, hop])
        for n in range(2):
            wait_for(blocks(N_PART // 2 * N_PAIR), fw_send.at[p, n])
            wait_for(blocks(N_PART // 2 * N_PAIR), fw_recv.at[p, n])


def writer(*refs):
    ins, (o, dq, dk, dv, dr, du, dw, sem) = refs[:4 + N_PART], refs[4 + N_PART:]
    pairs = list(zip(ins[:4], (o, dq, dk, dv)))
    for m, part in enumerate(ins[4:]):
        rows = min(PART, HALF - PART * m)
        for side in range(2):
            start = HALF * side + PART * m
            pairs.append((part.at[side, :rows], dr.at[start:start + rows]))
    last = HALF - PART * (N_PART - 1)
    pairs += [(ins[-1].at[0, last], du), (ins[-1].at[0, last + 1], dw)]
    copies = [pltpu.make_async_copy(src, dst, sem.at[j]) for j, (src, dst) in enumerate(pairs)]
    for copy in copies:
        copy.start()
    for copy in copies:
        copy.wait()


def solution(mesh):
    seq_spec = P(None, "cp", None, None)

    def local(query, key_in, value, bias_u, bias_w, rel_k, d_out):
        n_batch, rows, n_heads, head_dim = query.shape
        pairs = (n_batch, rows, N_PAIR, PAIR, head_dim)
        vm = pltpu.VMEM
        dma = pltpu.SemaphoreType.DMA
        whole = pl.BlockSpec(memory_space=pl.ANY)
        act = jax.ShapeDtypeStruct(pairs, BF16)
        vec = jax.ShapeDtypeStruct((n_heads, 1, head_dim), F32)
        tok = (PAIR, SEQ, HEAD)
        tok_t = (PAIR, HEAD, SEQ)
        acc = (HEAD + 8, HALF)
        outs = pl.pallas_call(
            kernel,
            name="rel_attn",
            out_shape=(act, act, act, act,
                       *[jax.ShapeDtypeStruct((2, PART, n_heads, 1, head_dim), F32)] * N_PART),
            in_specs=[pl.BlockSpec(memory_space=pltpu.HBM)] * 7,
            out_specs=[whole] * (4 + N_PART),
            scratch_shapes=[
                vm((4, SUBS, HALF, PAIR, HEAD), BF16), vm((2, SUBS, HALF, PAIR, HEAD), BF16),
                vm((SEQ, 2, PAIR, HEAD), BF16), vm((2, PAIR, HEAD), BF16), vm((2, PAIR, HEAD), BF16),
                vm((SUBS, PAIR, 8, HALF), F32), vm((SUBS, PAIR, 8, HALF), F32), vm((QB, HEAD), F32),
                vm((2, 2) + acc, F32), vm((2,) + acc, F32), vm((2, FIN, 1, HEAD), F32), vm((4, 2) + acc, F32),
                vm((QB, SEQ), F32), vm((QB, SEQ), F32), vm((QB, SEQ), F32),
                vm((QB, SEQ), BF16), vm((QB, SEQ), BF16), vm((QB, SEQ), BF16),
                vm(tok, BF16), vm(tok, BF16), vm(tok, BF16), vm(tok, BF16), vm(tok, BF16),
                vm(tok_t, BF16), vm(tok_t, BF16), vm(tok_t, BF16), vm(tok_t, BF16), vm(tok_t, BF16),
                vm((4, SEQ, HEAD), BF16), vm((4, HEAD, SEQ), BF16),
                vm((PAIR, HEAD, HALF), F32), vm((PAIR, HEAD, HALF), F32), vm((4, PAIR, HALF, HEAD), BF16),
                dma, dma((2, SUBS)), dma, dma, dma((2,)), dma((3,)), dma((4,)), dma((SUBS,)), dma, dma((SUBS,)),
                dma((2,)), dma((2,)), dma((2,)), dma((2,)), dma((2, 3)), dma((2, 3)), dma((2, 2)), dma((2, 2)),
            ],
            compiler_params=pltpu.CompilerParams(collective_id=0, has_side_effects=True, vmem_limit_bytes=36 * 1024 * 1024),
        )(*[pltpu.with_memory_space_constraint(x, pltpu.HBM) for x in (
            query.reshape(pairs), key_in.reshape(pairs), value.reshape(pairs), d_out.reshape(pairs),
            rel_k.reshape(SEQ, N_PAIR, PAIR, head_dim), bias_u.reshape(N_PAIR, PAIR, head_dim), bias_w.reshape(N_PAIR, PAIR, head_dim))])
        o, dq, dk, dv, dr, du, dw = pl.pallas_call(
            writer,
            name="writer",
            out_shape=(act, act, act, act, jax.ShapeDtypeStruct((SEQ, n_heads, 1, head_dim), F32), vec, vec),
            in_specs=[whole] * (4 + N_PART),
            out_specs=[whole] * 7,
            scratch_shapes=[dma((6 + 2 * N_PART,))],
            compiler_params=pltpu.CompilerParams(vmem_limit_bytes=1024 * 1024),
        )(*outs)
        full = query.shape
        return (o.reshape(full), dq.reshape(full), dk.reshape(full), dv.reshape(full),
                du.reshape(bias_u.shape), dw.reshape(bias_w.shape), dr.reshape(rel_k.shape))

    return jax.shard_map(local, mesh=mesh,
                         in_specs=(seq_spec, seq_spec, seq_spec, P(), P(), P(), seq_spec),
                         out_specs=(seq_spec, seq_spec, seq_spec, seq_spec, P(), P(), P()),
                         check_vma=False)
```

```python
import jax
import jax.numpy as jnp
from jax import lax
from jax.experimental import pallas as pl
from jax.experimental.pallas import tpu as pltpu
from jax.sharding import PartitionSpec as P

MESH = pl.DeviceIdType.MESH
BF16, F32 = jnp.bfloat16, jnp.float32
LOG2E = 1.4426950408889634

N_DEV = 16
PLANE = 8
PAIR = 2
N_PAIR = 8
SLOTS = 4
SUBS = 2 * SLOTS
EARLY = 3
ROWS = 64
HALF = PLANE * ROWS
SEQ = 2 * HALF
HEAD = 128
QB = 256
WIN = HALF + QB
N_PART = 6
PART = 86
FIN = N_PART * PART
HOPS = ((1, 2, 4), (2, 1, 4)) * 3
TURNS = ((1, 3, 2), (3, 1, 2))


def dot(lhs, rhs):
    return jnp.dot(lhs, rhs, preferred_element_type=F32)


def flip8(x):
    rows, cols = x.shape
    idx = 7 - lax.broadcasted_iota(jnp.int32, (rows // 8, 8, cols), 1)
    return jnp.take_along_axis(x.reshape(rows // 8, 8, cols), idx, axis=1).reshape(rows, cols)


def eye_rev(dtype):
    total = lax.broadcasted_iota(jnp.int32, (HEAD, HEAD), 0) + lax.broadcasted_iota(jnp.int32, (HEAD, HEAD), 1)
    return jnp.where(total == HEAD - 1, 1.0, 0.0).astype(dtype)


def kernel(q_in, k_in, v_in, g_in, r_in, u_in, w_in,
           o_out, dq_out, dk_out, dv_out, dr0_out, dr1_out, dr2_out, dr3_out, dr4_out, dr5_out,
           buf, rbuf, r_buf, u_buf, w_buf, st_tx, st_rx, st_ref, dr_rx, dr_rz, dr_fin, dr_acc,
           s_ref, e_ref, dp_ref, pb_ref, ds_ref, dd_ref,
           a_s, c_s, g_s, k_s, v_s, at_s, ct_s, gt_s, kt_s, vt_s, rev_s, rt_s, dkt, dvt, stage,
           in_send, in_recv, out_send, out_recv, own_sem, r_sem, up_send, up_recv, st_send, st_recv,
           x_send, x_recv, z_send, z_recv, ring_send, ring_recv, fw_send, fw_recv):
    me = lax.axis_index("cp")
    core = me % 2
    chip = me // 2
    col = chip % 4
    z = chip // 4
    partner = me + 1 - 2 * core
    across = me + PLANE * (1 - 2 * z)
    scale = HEAD ** -0.5

    def wait_for(ref, sem):
        pltpu.make_async_copy(ref, ref, sem).wait()

    tables = [pltpu.make_async_copy(src, dst, r_sem.at[j]) for j, (src, dst) in enumerate(
        ((r_in.at[:, pl.ds(2 * col, 2)], r_buf), (u_in.at[pl.ds(2 * col, 2)], u_buf), (w_in.at[pl.ds(2 * col, 2)], w_buf)))]
    for copy in tables:
        copy.start()

    barrier = pltpu.get_barrier_semaphore()

    for peer in [across] + [me ^ step for step in range(PLANE - 1, 0, -1)]:
        pl.semaphore_signal(barrier, inc=1, device_id=(peer,), device_id_type=MESH)
    pl.semaphore_wait(barrier, PLANE)

    my_rows = pl.ds(pl.multiple_of((me % PLANE) * ROWS, ROWS), ROWS)

    def peers():
        for near_turn, far_turn in zip(*TURNS):
            turn = jnp.where(core == 0, near_turn, far_turn)
            yield me ^ (2 * turn)
            yield me ^ (2 * turn + 1)
        yield partner

    def send_in(ins, sub):
        pair, row = sub // SLOTS, sub % SLOTS
        for first in (0, 2):
            for t in (first, first + 1):
                pltpu.make_async_copy(ins[t].at[core * SLOTS + row, :, 2 * col + pair], buf.at[t, sub, my_rows], in_recv.at[first // 2, sub]).start()
            for peer in peers():
                for t in (first, first + 1):
                    pltpu.make_async_remote_copy(
                        src_ref=ins[t].at[(peer % 2) * SLOTS + row, :, 2 * ((peer // 2) % 4) + pair], dst_ref=buf.at[t, sub, my_rows],
                        send_sem=in_send, recv_sem=in_recv.at[first // 2, sub], device_id=(peer,), device_id_type=MESH).start()

    def send_all(ins):
        def send_sub(sub, carry):
            send_in(ins, sub)
            return carry
        lax.fori_loop(0, SUBS, send_sub, 0)

    @pl.when(z == 0)
    def _():
        send_all((k_in, v_in, q_in, g_in))

    @pl.when(z == 1)
    def _():
        send_all((q_in, g_in, k_in, v_in))

    for copy in tables:
        copy.wait()
    rev = eye_rev(BF16)
    for p in range(2):
        pair_tab = pltpu.einshape("abc->bac", r_buf[:, p])
        for hh in range(PAIR):
            for blk in range(SEQ // HEAD):
                part = pair_tab[hh, SEQ - HEAD * (blk + 1):SEQ - HEAD * blk]
                flipped = dot(rev, part).astype(BF16)
                rev_s[2 * p + hh, HEAD * blk:HEAD * (blk + 1), :] = flipped
                rt_s[2 * p + hh, :, HEAD * blk:HEAD * (blk + 1)] = flipped.T
    dr_acc[...] = jnp.zeros_like(dr_acc)

    acts = (dk_out, dv_out, o_out, dq_out)

    def send_out(sub, which):
        place = (core * SLOTS + sub % SLOTS, slice(None), 2 * col + sub // SLOTS)
        for t in which:
            pltpu.make_async_copy(buf.at[t, sub, my_rows], acts[t].at[place], out_recv).start()
        for peer in peers():
            peer_rows = pl.ds(pl.multiple_of((peer % PLANE) * ROWS, ROWS), ROWS)
            for t in which:
                pltpu.make_async_remote_copy(
                    src_ref=buf.at[t, sub, peer_rows], dst_ref=acts[t].at[place],
                    send_sem=out_send, recv_sem=out_recv, device_id=(peer,), device_id_type=MESH).start()

    def send_up(sub):
        wait_for(buf.at[0:2, sub], in_recv.at[0, sub])
        for j in range(2):
            pltpu.make_async_remote_copy(src_ref=buf.at[j, sub], dst_ref=rbuf.at[j, sub], send_sem=up_send.at[sub % 4], recv_sem=up_recv.at[sub],
                                         device_id=(across,), device_id_type=MESH).start()

    def unpack(ref, j, sub):
        return pltpu.einshape("abc->bac", ref[j, sub])

    def load_rows(q_ref, q_j, g_ref, g_j, sub, start, turned):
        rows = slice(start, start + HALF)
        p = sub // SLOTS
        q2 = unpack(q_ref, q_j, sub)
        u = u_buf[p].astype(F32)
        w = w_buf[p].astype(F32)
        for hh in range(PAIR):
            q32 = q2[hh].astype(F32)
            a = (q32 + u[hh:hh + 1]).astype(BF16)
            c = (q32 + w[hh:hh + 1]).astype(BF16)
            a_s[hh, rows, :] = a
            c_s[hh, rows, :] = c
            at_s[hh, :, rows] = a.T
            if turned:
                ct_s[hh, :, rows] = flip8(c.astype(F32)).astype(BF16).T
        g2 = unpack(g_ref, g_j, sub)
        g_s[:, rows, :] = g2
        for hh in range(PAIR):
            gt_s[hh, :, rows] = g2[hh].T

    def load_keys(k_ref, k_j, v_ref, v_j, sub, start):
        rows = slice(start, start + HALF)
        k2 = unpack(k_ref, k_j, sub)
        v2 = unpack(v_ref, v_j, sub)
        k_s[:, rows, :] = k2
        v_s[:, rows, :] = v2
        for hh in range(PAIR):
            kt_s[hh, :, rows] = k2[hh].T
            vt_s[hh, :, rows] = v2[hh].T

    def row_block(hh, head, start, i0, lo, fresh, stats):
        width = i0 + QB
        rows = slice(start, start + QB)
        s_ref[:, :width] = dot(a_s[hh, rows, :], kt_s[hh, :, :width])
        e_ref[:, :width] = dot(c_s[hh, rows, :], rt_s[head, :, SEQ - width:])
        dp_ref[:, :width] = dot(g_s[hh, rows, :], vt_s[hh, :, :width])
        for r0 in range(0, QB, 16):
            group = slice(r0, r0 + 16)
            rel = pltpu.roll(e_ref[group, :width], i0 + 1 + r0, 1, stride=1, stride_axis=0)
            s = s_ref[group, :width] + rel
            ahead = lax.broadcasted_iota(jnp.int32, (16, width), 1) - lax.broadcasted_iota(jnp.int32, (16, width), 0)
            s = jnp.where(ahead <= i0 + r0, s, -jnp.inf)
            top = jnp.max(s, axis=1, keepdims=True)
            p = jnp.exp2((s - top) * (scale * LOG2E))
            total = jnp.sum(p, axis=1, keepdims=True)
            p = p * (1.0 / total)
            pb_ref[group, :width] = p.astype(BF16)
            dp = dp_ref[group, :width]
            row_dot = jnp.sum(p * dp, axis=1, keepdims=True)
            ds = (p * (dp - row_dot) * scale).astype(BF16)
            ds_ref[group, :width] = ds
            flipped = flip8(ds.astype(F32))
            half = [pltpu.roll(flipped[8 * j:8 * j + 8], QB - 8 - r0 - 8 * j, 1, stride=1, stride_axis=0) for j in range(2)]
            dd_ref[group, :width] = jnp.concatenate(half, axis=0).astype(BF16)
            if stats:
                lane = lax.broadcasted_iota(jnp.int32, (16, HEAD), 1)
                st_ref[group, :] = jnp.where(lane == 0, top * (scale * LOG2E) + jnp.log2(total), row_dot)
        pb = pb_ref[:, :width]
        ds = ds_ref[:, :width]
        dd = dd_ref[:, :width]
        stage[0, hh, rows, :] = dot(pb, v_s[hh, :width, :]).astype(BF16)
        dqc = dot(ds, k_s[hh, :width, :])
        dqr = flip8(dot(dd, rev_s[head, SEQ - width:, :]))
        stage[1, hh, rows, :] = (dqc + dqr).astype(BF16)
        dr_acc[head, 1, HEAD:HEAD + 1, HALF - HEAD:] += jnp.sum(dqc, axis=0, keepdims=True)
        dr_acc[head, 1, HEAD + 1:HEAD + 2, HALF - HEAD:] += jnp.sum(dqr, axis=0, keepdims=True)
        dk_new = dot(at_s[hh, :, rows], ds_ref[:, lo:width])
        dv_new = dot(gt_s[hh, :, rows], pb_ref[:, lo:width])
        if fresh:
            dkt[hh] = dk_new
            dvt[hh] = dv_new
        else:
            dkt[hh, :, :width - lo] += dk_new
            dvt[hh, :, :width - lo] += dv_new
        dr_new = dot(ct_s[hh, :, rows], dd)
        if width > HALF:
            dr_acc[head, 0, :HEAD, SEQ - width:] += dr_new[:, :width - HALF]
            dr_acc[head, 1, :HEAD, :] += dr_new[:, width - HALF:]
        else:
            dr_acc[head, 1, :HEAD, HALF - width:] += dr_new

    def col_block(hh, head, sub, i0):
        rows = slice(i0, i0 + QB)
        first = WIN - i0
        s_ref[:, :HALF] = dot(a_s[hh, rows, :], kt_s[hh, :, :HALF])
        e_ref[:, :WIN] = dot(c_s[hh, rows, :], rt_s[head, :, first:first + WIN])
        dp_ref[:, :HALF] = dot(g_s[hh, rows, :], vt_s[hh, :, :HALF])
        st_ref[:, :8] = st_rx[sub, hh, :, i0 - HALF:i0 - HALF + QB].T
        for r0 in range(0, QB, 16):
            group = slice(r0, r0 + 16)
            rel = pltpu.roll(e_ref[group, :WIN], HALF + 1 + r0, 1, stride=1, stride_axis=0)[:, :HALF]
            log_sum = st_ref[group, 0:1]
            row_dot = st_ref[group, 1:2]
            p = jnp.exp2((s_ref[group, :HALF] + rel) * (scale * LOG2E) - log_sum)
            pb_ref[group, :HALF] = p.astype(BF16)
            ds_ref[group, :HALF] = (p * (dp_ref[group, :HALF] - row_dot) * scale).astype(BF16)
        dkt[hh] += dot(at_s[hh, :, rows], ds_ref[:, :HALF])
        dvt[hh] += dot(gt_s[hh, :, rows], pb_ref[:, :HALF])

    def store_rows(sub):
        for t in range(2):
            buf[2 + t, sub] = pltpu.einshape("abc->bac", stage[t])

    def store_keys(sub):
        for hh in range(PAIR):
            stage[2, hh] = dkt[hh].astype(BF16).T
            stage[3, hh] = dvt[hh].astype(BF16).T
        for t in range(2):
            buf[t, sub] = pltpu.einshape("abc->bac", stage[2 + t])

    def wait_up(sub):
        wait_for(rbuf.at[:, sub], up_recv.at[sub])
        wait_for(rbuf.at[:, sub], up_send.at[sub % 4])

    def wait_in(sub):
        wait_for(buf.at[2:4, sub], in_recv.at[1, sub])

    def lower_rows(sub):
        wait_in(sub)
        load_rows(buf, 2, buf, 3, sub, 0, True)

    def lower_own(sub):
        load_keys(buf, 0, buf, 1, sub, 0)

        def own(hh, carry):
            head = 2 * (sub // SLOTS) + hh
            row_block(hh, head, QB, QB, 0, True, False)
            row_block(hh, head, 0, 0, 0, False, False)
            return carry

        lax.fori_loop(0, PAIR, own, 0)
        store_rows(sub)

    def lower_theirs(sub):
        wait_up(sub)
        load_rows(rbuf, 0, rbuf, 1, sub, HALF, False)
        wait_for(st_rx.at[sub], st_recv.at[sub])

        def theirs(hh, carry):
            head = 2 * (sub // SLOTS) + hh
            col_block(hh, head, sub, HALF)
            col_block(hh, head, sub, HALF + QB)
            return carry

        lax.fori_loop(0, PAIR, theirs, 0)
        store_keys(sub)

    def upper_own(sub):
        wait_in(sub)
        wait_up(sub)
        load_rows(buf, 0, buf, 1, sub, 0, True)
        load_keys(rbuf, 0, rbuf, 1, sub, 0)
        load_keys(buf, 2, buf, 3, sub, HALF)

        def own(hh, carry):
            head = 2 * (sub // SLOTS) + hh
            for blk in (1, 0):
                row_block(hh, head, QB * blk, HALF + QB * blk, HALF, blk == 1, True)
                st_tx[sub, hh, :, QB * blk:QB * (blk + 1)] = st_ref[...].T[:8]
            pltpu.make_async_remote_copy(src_ref=st_tx.at[sub, hh], dst_ref=st_rx.at[sub, hh], send_sem=st_send, recv_sem=st_recv.at[sub],
                                         device_id=(across,), device_id_type=MESH).start()
            return carry

        lax.fori_loop(0, PAIR, own, 0)
        store_rows(sub)
        store_keys(sub)

    side = 1 - core
    parts = (dr0_out, dr1_out, dr2_out, dr3_out, dr4_out, dr5_out)

    def swap_start(p):
        for n in range(2):
            pltpu.make_async_remote_copy(src_ref=dr_acc.at[2 * p + n, side], dst_ref=dr_rx.at[p, n], send_sem=x_send.at[p], recv_sem=x_recv.at[p],
                                         device_id=(partner,), device_id_type=MESH).start()

    def swap_add(p):
        wait_for(dr_rx.at[p], x_recv.at[p])
        for n in range(2):
            dr_rx[p, n] = dr_rx[p, n] + dr_acc[2 * p + n, core]

    def cross_start(p):
        pltpu.make_async_remote_copy(src_ref=dr_rx.at[p, 1 - z], dst_ref=dr_rz.at[p], send_sem=z_send.at[p], recv_sem=z_recv.at[p],
                                     device_id=(across,), device_id_type=MESH).start()

    def head_of(p, bits):
        other = chip ^ bits
        return 4 * (other % 4) + 2 * p + other // 4

    def block(p, m, bits):
        if bits == 0:
            return dr_fin.at[p, PART * m:PART * (m + 1)]
        return parts[m].at[side, :, head_of(p, bits)]

    def forward(p, m, bits):
        pltpu.make_async_remote_copy(src_ref=block(p, m, bits), dst_ref=parts[m].at[side, :, head_of(p, bits)], send_sem=fw_send.at[p, m // 3],
                                     recv_sem=fw_recv.at[p, m // 3], device_id=(partner,), device_id_type=MESH).start()

    def held(m, hop):
        have = [0]
        for bit in HOPS[m][:hop]:
            have = have + [bits ^ bit for bits in have]
        return have

    def blocks(count):
        return parts[0].at[:, :, :count // 2]

    def hop_start(p, hop):
        for m in range(N_PART):
            for bits in held(m, hop):
                pltpu.make_async_remote_copy(
                    src_ref=block(p, m, bits), dst_ref=parts[m].at[side, :, head_of(p, bits)], send_sem=ring_send.at[p, hop],
                    recv_sem=ring_recv.at[p, hop], device_id=(me ^ (2 * HOPS[m][hop]),), device_id_type=MESH).start()

    def hop_wait(p, hop):
        wait_for(blocks(N_PART << hop), ring_recv.at[p, hop])
        for m in range(N_PART):
            have = held(m, hop + 1)
            for bits in have[len(have) // 2:]:
                forward(p, m, bits)

    def cross_finish(p):
        wait_for(dr_rz.at[p], z_recv.at[p])
        total = dr_rx[p, z] + dr_rz[p]
        rev32 = eye_rev(F32)
        for m in range(HALF // HEAD):
            part = total[:HEAD, HALF - HEAD * (m + 1):HALF - HEAD * m]
            turned = lax.dot_general(rev32, part, (((1,), (1,)), ((), ())), precision=lax.Precision.HIGHEST, preferred_element_type=F32)
            dr_fin[p, HEAD * m:HEAD * (m + 1)] = turned.reshape(HEAD, 1, HEAD)
        dr_fin[p, HALF] = total[HEAD:HEAD + 1, HALF - HEAD:]
        dr_fin[p, HALF + 1] = total[HEAD + 1:HEAD + 2, HALF - HEAD:]
        dr_fin[p, HALF + 2:] = jnp.zeros((FIN - HALF - 2, 1, HEAD), F32)
        hop_start(p, 0)
        for m in range(N_PART):
            pltpu.make_async_copy(block(p, m, 0), parts[m].at[side, :, head_of(p, 0)], own_sem.at[p]).start()
            forward(p, m, 0)

    send_up(0)

    def sub_body(sub, carry):
        @pl.when(sub < SUBS - 1)
        def _():
            send_up(sub + 1)

        @pl.when(sub == SLOTS)
        def _():
            swap_start(0)

        @pl.when(sub == SUBS - 1)
        def _():
            swap_add(0)
            cross_start(0)

        @pl.when(sub == SUBS)
        def _():
            swap_start(1)
            cross_finish(0)

        @pl.when((z == 0) & (sub < SUBS))
        def _():
            lower_rows(sub)

        @pl.when((z == 0) & (sub > 0))
        def _():
            lower_theirs(sub - 1)

        @pl.when((z == 0) & (sub < SUBS))
        def _():
            lower_own(sub)

        @pl.when((z == 1) & (sub < SUBS))
        def _():
            upper_own(sub)

        @pl.when(sub < EARLY)
        def _():
            send_out(sub, (2, 3))

        @pl.when((sub > 0) & (sub <= EARLY))
        def _():
            send_out(sub - 1, (0, 1))
        return carry

    lax.fori_loop(0, SUBS + 1, sub_body, 0)

    swap_add(1)
    cross_start(1)
    cross_finish(1)
    for p in range(2):
        hop_wait(p, 0)
        hop_start(p, 1)

    def send_late(sub, carry):
        send_out(sub, range(4))
        return carry

    lax.fori_loop(EARLY, EARLY + 2, send_late, 0)
    for p in range(2):
        hop_wait(p, 1)
        hop_start(p, 2)
    lax.fori_loop(EARLY + 2, SUBS, send_late, 0)
    for p in range(2):
        hop_wait(p, 2)

    wait_for(buf, out_recv)
    wait_for(buf.at[:, :, :HALF - ROWS], in_send)
    wait_for(buf.at[:, :, :HALF - ROWS], out_send)

    @pl.when(z == 1)
    def _():
        wait_for(st_tx, st_send)

    for p in range(2):
        wait_for(dr_rx.at[p], x_send.at[p])
        wait_for(dr_rz.at[p], z_send.at[p])
        wait_for(blocks(N_PART), own_sem.at[p])
        for hop in range(3):
            wait_for(blocks(N_PART << hop), ring_send.at[p, hop])
        for n in range(2):
            wait_for(blocks(N_PART // 2 * N_PAIR), fw_send.at[p, n])
            wait_for(blocks(N_PART // 2 * N_PAIR), fw_recv.at[p, n])


def writer(*refs):
    ins, (o, dq, dk, dv, dr, du, dw, sem) = refs[:4 + N_PART], refs[4 + N_PART:]
    pairs = list(zip(ins[:4], (o, dq, dk, dv)))
    for m, part in enumerate(ins[4:]):
        rows = min(PART, HALF - PART * m)
        for side in range(2):
            start = HALF * side + PART * m
            pairs.append((part.at[side, :rows], dr.at[start:start + rows]))
    last = HALF - PART * (N_PART - 1)
    pairs += [(ins[-1].at[0, last], du), (ins[-1].at[0, last + 1], dw)]
    copies = [pltpu.make_async_copy(src, dst, sem.at[j]) for j, (src, dst) in enumerate(pairs)]
    for j, copy in enumerate(copies):
        copy.start(priority=j % 2)
    for copy in copies:
        copy.wait()


def solution(mesh):
    seq_spec = P(None, "cp", None, None)

    def local(query, key_in, value, bias_u, bias_w, rel_k, d_out):
        n_batch, rows, n_heads, head_dim = query.shape
        pairs = (n_batch, rows, N_PAIR, PAIR, head_dim)
        vm = pltpu.VMEM
        dma = pltpu.SemaphoreType.DMA
        whole = pl.BlockSpec(memory_space=pl.ANY)
        act = jax.ShapeDtypeStruct(pairs, BF16)
        vec = jax.ShapeDtypeStruct((n_heads, 1, head_dim), F32)
        tok = (PAIR, SEQ, HEAD)
        tok_t = (PAIR, HEAD, SEQ)
        acc = (HEAD + 8, HALF)
        outs = pl.pallas_call(
            kernel,
            name="rel_attn",
            out_shape=(act, act, act, act,
                       *[jax.ShapeDtypeStruct((2, PART, n_heads, 1, head_dim), F32)] * N_PART),
            in_specs=[pl.BlockSpec(memory_space=pltpu.HBM)] * 7,
            out_specs=[whole] * (4 + N_PART),
            scratch_shapes=[
                vm((4, SUBS, HALF, PAIR, HEAD), BF16), vm((2, SUBS, HALF, PAIR, HEAD), BF16),
                vm((SEQ, 2, PAIR, HEAD), BF16), vm((2, PAIR, HEAD), BF16), vm((2, PAIR, HEAD), BF16),
                vm((SUBS, PAIR, 8, HALF), F32), vm((SUBS, PAIR, 8, HALF), F32), vm((QB, HEAD), F32),
                vm((2, 2) + acc, F32), vm((2,) + acc, F32), vm((2, FIN, 1, HEAD), F32), vm((4, 2) + acc, F32),
                vm((QB, SEQ), F32), vm((QB, SEQ), F32), vm((QB, SEQ), F32),
                vm((QB, SEQ), BF16), vm((QB, SEQ), BF16), vm((QB, SEQ), BF16),
                vm(tok, BF16), vm(tok, BF16), vm(tok, BF16), vm(tok, BF16), vm(tok, BF16),
                vm(tok_t, BF16), vm(tok_t, BF16), vm(tok_t, BF16), vm(tok_t, BF16), vm(tok_t, BF16),
                vm((4, SEQ, HEAD), BF16), vm((4, HEAD, SEQ), BF16),
                vm((PAIR, HEAD, HALF), F32), vm((PAIR, HEAD, HALF), F32), vm((4, PAIR, HALF, HEAD), BF16),
                dma, dma((2, SUBS)), dma, dma, dma((2,)), dma((3,)), dma((4,)), dma((SUBS,)), dma, dma((SUBS,)),
                dma((2,)), dma((2,)), dma((2,)), dma((2,)), dma((2, 3)), dma((2, 3)), dma((2, 2)), dma((2, 2)),
            ],
            compiler_params=pltpu.CompilerParams(collective_id=0, has_side_effects=True, vmem_limit_bytes=36 * 1024 * 1024),
        )(*[pltpu.with_memory_space_constraint(x, pltpu.HBM) for x in (
            query.reshape(pairs), key_in.reshape(pairs), value.reshape(pairs), d_out.reshape(pairs),
            rel_k.reshape(SEQ, N_PAIR, PAIR, head_dim), bias_u.reshape(N_PAIR, PAIR, head_dim), bias_w.reshape(N_PAIR, PAIR, head_dim))])
        o, dq, dk, dv, dr, du, dw = pl.pallas_call(
            writer,
            name="writer",
            out_shape=(act, act, act, act, jax.ShapeDtypeStruct((SEQ, n_heads, 1, head_dim), F32), vec, vec),
            in_specs=[whole] * (4 + N_PART),
            out_specs=[whole] * 7,
            scratch_shapes=[dma((6 + 2 * N_PART,))],
            compiler_params=pltpu.CompilerParams(vmem_limit_bytes=1024 * 1024),
        )(*outs)
        full = query.shape
        return (o.reshape(full), dq.reshape(full), dk.reshape(full), dv.reshape(full),
                du.reshape(bias_u.shape), dw.reshape(bias_w.shape), dr.reshape(rel_k.shape))

    return jax.shard_map(local, mesh=mesh,
                         in_specs=(seq_spec, seq_spec, seq_spec, P(), P(), P(), seq_spec),
                         out_specs=(seq_spec, seq_spec, seq_spec, seq_spec, P(), P(), P()),
                         check_vma=False)
```

```python
import jax
import jax.numpy as jnp
from jax import lax
from jax.experimental import pallas as pl
from jax.experimental.pallas import tpu as pltpu
from jax.sharding import PartitionSpec as P

MESH = pl.DeviceIdType.MESH
BF16, F32 = jnp.bfloat16, jnp.float32
LOG2E = 1.4426950408889634

N_DEV = 16
PLANE = 8
PAIR = 2
N_PAIR = 8
SLOTS = 4
SUBS = 2 * SLOTS
EARLY = 3
ROWS = 64
HALF = PLANE * ROWS
SEQ = 2 * HALF
HEAD = 128
QB = 256
WIN = HALF + QB
N_PART = 6
PART = 86
FIN = N_PART * PART
HOPS = ((1, 2, 4), (2, 1, 4)) * 3
TURNS = ((1, 3, 2), (3, 1, 2))


def dot(lhs, rhs):
    return jnp.dot(lhs, rhs, preferred_element_type=F32)


def flip8(x):
    rows, cols = x.shape
    idx = 7 - lax.broadcasted_iota(jnp.int32, (rows // 8, 8, cols), 1)
    return jnp.take_along_axis(x.reshape(rows // 8, 8, cols), idx, axis=1).reshape(rows, cols)


def eye_rev(dtype):
    total = lax.broadcasted_iota(jnp.int32, (HEAD, HEAD), 0) + lax.broadcasted_iota(jnp.int32, (HEAD, HEAD), 1)
    return jnp.where(total == HEAD - 1, 1.0, 0.0).astype(dtype)


def kernel(q_in, k_in, v_in, g_in, r_in, u_in, w_in,
           o_out, dq_out, dk_out, dv_out, dr0_out, dr1_out, dr2_out, dr3_out, dr4_out, dr5_out,
           buf, rbuf, head_start, r_buf, u_buf, w_buf, st_tx, st_rx, st_ref, dr_rx, dr_rz, dr_fin, dr_acc,
           s_ref, e_ref, dp_ref, pb_ref, ds_ref, dd_ref,
           a_s, c_s, g_s, k_s, v_s, at_s, ct_s, gt_s, kt_s, vt_s, rev_s, rt_s, dkt, dvt, stage,
           in_send, in_recv, out_send, out_recv, own_sem, r_sem, up_send, up_recv, st_send, st_recv,
           x_send, x_recv, z_send, z_recv, first_sem, ring_send, ring_recv, fw_send, fw_recv):
    me = lax.axis_index("cp")
    core = me % 2
    chip = me // 2
    col = chip % 4
    z = chip // 4
    partner = me + 1 - 2 * core
    across = me + PLANE * (1 - 2 * z)
    scale = HEAD ** -0.5

    def wait_for(ref, sem):
        pltpu.make_async_copy(ref, ref, sem).wait()

    tables = [pltpu.make_async_copy(src, dst, r_sem.at[j]) for j, (src, dst) in enumerate(
        ((r_in.at[:, pl.ds(2 * col, 2)], r_buf), (u_in.at[pl.ds(2 * col, 2)], u_buf), (w_in.at[pl.ds(2 * col, 2)], w_buf)))]
    for copy in tables:
        copy.start()

    def bring(ins):
        for t in range(2):
            for step in range(1, PLANE):
                peer = me ^ step
                pltpu.make_async_copy(ins[t].at[(peer % 2) * SLOTS, :, 2 * ((peer // 2) % 4)], head_start.at[t, step - 1], first_sem).start()

    @pl.when(z == 0)
    def _():
        bring((k_in, v_in))

    @pl.when(z == 1)
    def _():
        bring((q_in, g_in))

    barrier = pltpu.get_barrier_semaphore()

    for peer in [across] + [me ^ step for step in range(PLANE - 1, 0, -1)]:
        pl.semaphore_signal(barrier, inc=1, device_id=(peer,), device_id_type=MESH)
    pl.semaphore_wait(barrier, PLANE)
    wait_for(head_start, first_sem)

    my_rows = pl.ds(pl.multiple_of((me % PLANE) * ROWS, ROWS), ROWS)

    def peers():
        for near_turn, far_turn in zip(*TURNS):
            turn = jnp.where(core == 0, near_turn, far_turn)
            yield me ^ (2 * turn)
            yield me ^ (2 * turn + 1)
        yield partner

    def send_in(ins, sub, first_ones=False):
        pair, row = sub // SLOTS, sub % SLOTS
        for first in (0, 2):
            for peer in peers():
                for t in (first, first + 1):
                    if first_ones and first == 0:
                        src = head_start.at[t, (peer ^ me) - 1]
                    else:
                        src = ins[t].at[(peer % 2) * SLOTS + row, :, 2 * ((peer // 2) % 4) + pair]
                    pltpu.make_async_remote_copy(
                        src_ref=src, dst_ref=buf.at[t, sub, my_rows],
                        send_sem=in_send, recv_sem=in_recv.at[first // 2, sub], device_id=(peer,), device_id_type=MESH).start()
            for t in (first, first + 1):
                pltpu.make_async_copy(ins[t].at[core * SLOTS + row, :, 2 * col + pair], buf.at[t, sub, my_rows], in_recv.at[first // 2, sub]).start()

    def send_all(ins):
        def send_sub(sub, carry):
            send_in(ins, sub)
            return carry
        send_in(ins, 0, True)
        lax.fori_loop(1, SUBS, send_sub, 0)

    @pl.when(z == 0)
    def _():
        send_all((k_in, v_in, q_in, g_in))

    @pl.when(z == 1)
    def _():
        send_all((q_in, g_in, k_in, v_in))

    for copy in tables:
        copy.wait()
    rev = eye_rev(BF16)
    for p in range(2):
        pair_tab = pltpu.einshape("abc->bac", r_buf[:, p])
        for hh in range(PAIR):
            for blk in range(SEQ // HEAD):
                part = pair_tab[hh, SEQ - HEAD * (blk + 1):SEQ - HEAD * blk]
                flipped = dot(rev, part).astype(BF16)
                rev_s[2 * p + hh, HEAD * blk:HEAD * (blk + 1), :] = flipped
                rt_s[2 * p + hh, :, HEAD * blk:HEAD * (blk + 1)] = flipped.T
    dr_acc[...] = jnp.zeros_like(dr_acc)

    acts = (dk_out, dv_out, o_out, dq_out)

    def send_out(sub, which):
        place = (core * SLOTS + sub % SLOTS, slice(None), 2 * col + sub // SLOTS)
        for t in which:
            pltpu.make_async_copy(buf.at[t, sub, my_rows], acts[t].at[place], out_recv).start()
        for peer in peers():
            peer_rows = pl.ds(pl.multiple_of((peer % PLANE) * ROWS, ROWS), ROWS)
            for t in which:
                pltpu.make_async_remote_copy(
                    src_ref=buf.at[t, sub, peer_rows], dst_ref=acts[t].at[place],
                    send_sem=out_send, recv_sem=out_recv, device_id=(peer,), device_id_type=MESH).start()

    def send_up(sub):
        wait_for(buf.at[0:2, sub], in_recv.at[0, sub])
        for j in range(2):
            pltpu.make_async_remote_copy(src_ref=buf.at[j, sub], dst_ref=rbuf.at[j, sub], send_sem=up_send.at[sub % 4], recv_sem=up_recv.at[sub],
                                         device_id=(across,), device_id_type=MESH).start()

    def unpack(ref, j, sub):
        return pltpu.einshape("abc->bac", ref[j, sub])

    def load_rows(q_ref, q_j, g_ref, g_j, sub, start, turned):
        rows = slice(start, start + HALF)
        p = sub // SLOTS
        q2 = unpack(q_ref, q_j, sub)
        u = u_buf[p].astype(F32)
        w = w_buf[p].astype(F32)
        for hh in range(PAIR):
            q32 = q2[hh].astype(F32)
            a = (q32 + u[hh:hh + 1]).astype(BF16)
            c = (q32 + w[hh:hh + 1]).astype(BF16)
            a_s[hh, rows, :] = a
            c_s[hh, rows, :] = c
            at_s[hh, :, rows] = a.T
            if turned:
                ct_s[hh, :, rows] = flip8(c.astype(F32)).astype(BF16).T
        g2 = unpack(g_ref, g_j, sub)
        g_s[:, rows, :] = g2
        for hh in range(PAIR):
            gt_s[hh, :, rows] = g2[hh].T

    def load_keys(k_ref, k_j, v_ref, v_j, sub, start):
        rows = slice(start, start + HALF)
        k2 = unpack(k_ref, k_j, sub)
        v2 = unpack(v_ref, v_j, sub)
        k_s[:, rows, :] = k2
        v_s[:, rows, :] = v2
        for hh in range(PAIR):
            kt_s[hh, :, rows] = k2[hh].T
            vt_s[hh, :, rows] = v2[hh].T

    def row_block(hh, head, start, i0, lo, fresh, stats):
        width = i0 + QB
        rows = slice(start, start + QB)
        s_ref[:, :width] = dot(a_s[hh, rows, :], kt_s[hh, :, :width])
        e_ref[:, :width] = dot(c_s[hh, rows, :], rt_s[head, :, SEQ - width:])
        dp_ref[:, :width] = dot(g_s[hh, rows, :], vt_s[hh, :, :width])
        for r0 in range(0, QB, 16):
            group = slice(r0, r0 + 16)
            rel = pltpu.roll(e_ref[group, :width], i0 + 1 + r0, 1, stride=1, stride_axis=0)
            s = s_ref[group, :width] + rel
            ahead = lax.broadcasted_iota(jnp.int32, (16, width), 1) - lax.broadcasted_iota(jnp.int32, (16, width), 0)
            s = jnp.where(ahead <= i0 + r0, s, -jnp.inf)
            top = jnp.max(s, axis=1, keepdims=True)
            p = jnp.exp2((s - top) * (scale * LOG2E))
            total = jnp.sum(p, axis=1, keepdims=True)
            p = p * (1.0 / total)
            pb_ref[group, :width] = p.astype(BF16)
            dp = dp_ref[group, :width]
            row_dot = jnp.sum(p * dp, axis=1, keepdims=True)
            ds = (p * (dp - row_dot) * scale).astype(BF16)
            ds_ref[group, :width] = ds
            flipped = flip8(ds.astype(F32))
            half = [pltpu.roll(flipped[8 * j:8 * j + 8], QB - 8 - r0 - 8 * j, 1, stride=1, stride_axis=0) for j in range(2)]
            dd_ref[group, :width] = jnp.concatenate(half, axis=0).astype(BF16)
            if stats:
                lane = lax.broadcasted_iota(jnp.int32, (16, HEAD), 1)
                st_ref[group, :] = jnp.where(lane == 0, top * (scale * LOG2E) + jnp.log2(total), row_dot)
        pb = pb_ref[:, :width]
        ds = ds_ref[:, :width]
        dd = dd_ref[:, :width]
        stage[0, hh, rows, :] = dot(pb, v_s[hh, :width, :]).astype(BF16)
        dqc = dot(ds, k_s[hh, :width, :])
        dqr = flip8(dot(dd, rev_s[head, SEQ - width:, :]))
        stage[1, hh, rows, :] = (dqc + dqr).astype(BF16)
        dr_acc[head, 1, HEAD:HEAD + 1, HALF - HEAD:] += jnp.sum(dqc, axis=0, keepdims=True)
        dr_acc[head, 1, HEAD + 1:HEAD + 2, HALF - HEAD:] += jnp.sum(dqr, axis=0, keepdims=True)
        dk_new = dot(at_s[hh, :, rows], ds_ref[:, lo:width])
        dv_new = dot(gt_s[hh, :, rows], pb_ref[:, lo:width])
        if fresh:
            dkt[hh] = dk_new
            dvt[hh] = dv_new
        else:
            dkt[hh, :, :width - lo] += dk_new
            dvt[hh, :, :width - lo] += dv_new
        dr_new = dot(ct_s[hh, :, rows], dd)
        if width > HALF:
            dr_acc[head, 0, :HEAD, SEQ - width:] += dr_new[:, :width - HALF]
            dr_acc[head, 1, :HEAD, :] += dr_new[:, width - HALF:]
        else:
            dr_acc[head, 1, :HEAD, HALF - width:] += dr_new

    def col_block(hh, head, sub, i0):
        rows = slice(i0, i0 + QB)
        first = WIN - i0
        s_ref[:, :HALF] = dot(a_s[hh, rows, :], kt_s[hh, :, :HALF])
        e_ref[:, :WIN] = dot(c_s[hh, rows, :], rt_s[head, :, first:first + WIN])
        dp_ref[:, :HALF] = dot(g_s[hh, rows, :], vt_s[hh, :, :HALF])
        st_ref[:, :8] = st_rx[sub, hh, :, i0 - HALF:i0 - HALF + QB].T
        for r0 in range(0, QB, 16):
            group = slice(r0, r0 + 16)
            rel = pltpu.roll(e_ref[group, :WIN], HALF + 1 + r0, 1, stride=1, stride_axis=0)[:, :HALF]
            log_sum = st_ref[group, 0:1]
            row_dot = st_ref[group, 1:2]
            p = jnp.exp2((s_ref[group, :HALF] + rel) * (scale * LOG2E) - log_sum)
            pb_ref[group, :HALF] = p.astype(BF16)
            ds_ref[group, :HALF] = (p * (dp_ref[group, :HALF] - row_dot) * scale).astype(BF16)
        dkt[hh] += dot(at_s[hh, :, rows], ds_ref[:, :HALF])
        dvt[hh] += dot(gt_s[hh, :, rows], pb_ref[:, :HALF])

    def store_rows(sub):
        for t in range(2):
            buf[2 + t, sub] = pltpu.einshape("abc->bac", stage[t])

    def store_keys(sub):
        for hh in range(PAIR):
            stage[2, hh] = dkt[hh].astype(BF16).T
            stage[3, hh] = dvt[hh].astype(BF16).T
        for t in range(2):
            buf[t, sub] = pltpu.einshape("abc->bac", stage[2 + t])

    def wait_up(sub):
        wait_for(rbuf.at[:, sub], up_recv.at[sub])
        wait_for(rbuf.at[:, sub], up_send.at[sub % 4])

    def wait_in(sub):
        wait_for(buf.at[2:4, sub], in_recv.at[1, sub])

    def lower_rows(sub):
        wait_in(sub)
        load_rows(buf, 2, buf, 3, sub, 0, True)

    def lower_own(sub):
        load_keys(buf, 0, buf, 1, sub, 0)

        def own(hh, carry):
            head = 2 * (sub // SLOTS) + hh
            row_block(hh, head, QB, QB, 0, True, False)
            row_block(hh, head, 0, 0, 0, False, False)
            return carry

        lax.fori_loop(0, PAIR, own, 0)
        store_rows(sub)

    def lower_theirs(sub):
        wait_up(sub)
        load_rows(rbuf, 0, rbuf, 1, sub, HALF, False)
        wait_for(st_rx.at[sub], st_recv.at[sub])

        def theirs(hh, carry):
            head = 2 * (sub // SLOTS) + hh
            col_block(hh, head, sub, HALF)
            col_block(hh, head, sub, HALF + QB)
            return carry

        lax.fori_loop(0, PAIR, theirs, 0)
        store_keys(sub)

    def upper_own(sub):
        wait_in(sub)
        wait_up(sub)
        load_rows(buf, 0, buf, 1, sub, 0, True)
        load_keys(rbuf, 0, rbuf, 1, sub, 0)
        load_keys(buf, 2, buf, 3, sub, HALF)

        def own(hh, carry):
            head = 2 * (sub // SLOTS) + hh
            for blk in (1, 0):
                row_block(hh, head, QB * blk, HALF + QB * blk, HALF, blk == 1, True)
                st_tx[sub, hh, :, QB * blk:QB * (blk + 1)] = st_ref[...].T[:8]
            pltpu.make_async_remote_copy(src_ref=st_tx.at[sub, hh], dst_ref=st_rx.at[sub, hh], send_sem=st_send, recv_sem=st_recv.at[sub],
                                         device_id=(across,), device_id_type=MESH).start()
            return carry

        lax.fori_loop(0, PAIR, own, 0)
        store_rows(sub)
        store_keys(sub)

    side = 1 - core
    parts = (dr0_out, dr1_out, dr2_out, dr3_out, dr4_out, dr5_out)

    def swap_start(p):
        for n in range(2):
            pltpu.make_async_remote_copy(src_ref=dr_acc.at[2 * p + n, side], dst_ref=dr_rx.at[p, n], send_sem=x_send.at[p], recv_sem=x_recv.at[p],
                                         device_id=(partner,), device_id_type=MESH).start()

    def swap_add(p):
        wait_for(dr_rx.at[p], x_recv.at[p])
        for n in range(2):
            dr_rx[p, n] = dr_rx[p, n] + dr_acc[2 * p + n, core]

    def cross_start(p):
        pltpu.make_async_remote_copy(src_ref=dr_rx.at[p, 1 - z], dst_ref=dr_rz.at[p], send_sem=z_send.at[p], recv_sem=z_recv.at[p],
                                     device_id=(across,), device_id_type=MESH).start()

    def head_of(p, bits):
        other = chip ^ bits
        return 4 * (other % 4) + 2 * p + other // 4

    def block(p, m, bits):
        if bits == 0:
            return dr_fin.at[p, PART * m:PART * (m + 1)]
        return parts[m].at[side, :, head_of(p, bits)]

    def forward(p, m, bits):
        pltpu.make_async_remote_copy(src_ref=block(p, m, bits), dst_ref=parts[m].at[side, :, head_of(p, bits)], send_sem=fw_send.at[p, m // 3],
                                     recv_sem=fw_recv.at[p, m // 3], device_id=(partner,), device_id_type=MESH).start()

    def held(m, hop):
        have = [0]
        for bit in HOPS[m][:hop]:
            have = have + [bits ^ bit for bits in have]
        return have

    def blocks(count):
        return parts[0].at[:, :, :count // 2]

    def hop_start(p, hop):
        for m in range(N_PART):
            for bits in held(m, hop):
                pltpu.make_async_remote_copy(
                    src_ref=block(p, m, bits), dst_ref=parts[m].at[side, :, head_of(p, bits)], send_sem=ring_send.at[p, hop],
                    recv_sem=ring_recv.at[p, hop], device_id=(me ^ (2 * HOPS[m][hop]),), device_id_type=MESH).start()

    def hop_wait(p, hop):
        wait_for(blocks(N_PART << hop), ring_recv.at[p, hop])
        for m in range(N_PART):
            have = held(m, hop + 1)
            for bits in have[len(have) // 2:]:
                forward(p, m, bits)

    def cross_finish(p):
        wait_for(dr_rz.at[p], z_recv.at[p])
        total = dr_rx[p, z] + dr_rz[p]
        rev32 = eye_rev(F32)
        for m in range(HALF // HEAD):
            part = total[:HEAD, HALF - HEAD * (m + 1):HALF - HEAD * m]
            turned = lax.dot_general(rev32, part, (((1,), (1,)), ((), ())), precision=lax.Precision.HIGHEST, preferred_element_type=F32)
            dr_fin[p, HEAD * m:HEAD * (m + 1)] = turned.reshape(HEAD, 1, HEAD)
        dr_fin[p, HALF] = total[HEAD:HEAD + 1, HALF - HEAD:]
        dr_fin[p, HALF + 1] = total[HEAD + 1:HEAD + 2, HALF - HEAD:]
        dr_fin[p, HALF + 2:] = jnp.zeros((FIN - HALF - 2, 1, HEAD), F32)
        hop_start(p, 0)
        for m in range(N_PART):
            pltpu.make_async_copy(block(p, m, 0), parts[m].at[side, :, head_of(p, 0)], own_sem.at[p]).start()
            forward(p, m, 0)

    send_up(0)

    def sub_body(sub, carry):
        @pl.when(sub < SUBS - 1)
        def _():
            send_up(sub + 1)

        @pl.when(sub == SLOTS)
        def _():
            swap_start(0)

        @pl.when(sub == SUBS - 1)
        def _():
            swap_add(0)
            cross_start(0)

        @pl.when(sub == SUBS)
        def _():
            swap_start(1)
            cross_finish(0)

        @pl.when((z == 0) & (sub < SUBS))
        def _():
            lower_rows(sub)

        @pl.when((z == 0) & (sub > 0))
        def _():
            lower_theirs(sub - 1)

        @pl.when((z == 0) & (sub < SUBS))
        def _():
            lower_own(sub)

        @pl.when((z == 1) & (sub < SUBS))
        def _():
            upper_own(sub)

        @pl.when(sub < EARLY)
        def _():
            send_out(sub, (2, 3))

        @pl.when((sub > 0) & (sub <= EARLY))
        def _():
            send_out(sub - 1, (0, 1))
        return carry

    lax.fori_loop(0, SUBS + 1, sub_body, 0)

    swap_add(1)
    cross_start(1)
    cross_finish(1)
    for p in range(2):
        hop_wait(p, 0)
        hop_start(p, 1)

    def send_late(sub, carry):
        send_out(sub, range(4))
        return carry

    lax.fori_loop(EARLY, EARLY + 2, send_late, 0)
    for p in range(2):
        hop_wait(p, 1)
        hop_start(p, 2)
    lax.fori_loop(EARLY + 2, SUBS, send_late, 0)
    for p in range(2):
        hop_wait(p, 2)

    wait_for(buf, out_recv)
    wait_for(buf.at[:, :, :HALF - ROWS], in_send)
    wait_for(buf.at[:, :, :HALF - ROWS], out_send)

    @pl.when(z == 1)
    def _():
        wait_for(st_tx, st_send)

    for p in range(2):
        wait_for(dr_rx.at[p], x_send.at[p])
        wait_for(dr_rz.at[p], z_send.at[p])
        wait_for(blocks(N_PART), own_sem.at[p])
        for hop in range(3):
            wait_for(blocks(N_PART << hop), ring_send.at[p, hop])
        for n in range(2):
            wait_for(blocks(N_PART // 2 * N_PAIR), fw_send.at[p, n])
            wait_for(blocks(N_PART // 2 * N_PAIR), fw_recv.at[p, n])


def writer(*refs):
    ins, (o, dq, dk, dv, dr, du, dw, sem) = refs[:4 + N_PART], refs[4 + N_PART:]
    pairs = list(zip(ins[:4], (o, dq, dk, dv)))
    for m, part in enumerate(ins[4:]):
        rows = min(PART, HALF - PART * m)
        for side in range(2):
            start = HALF * side + PART * m
            pairs.append((part.at[side, :rows], dr.at[start:start + rows]))
    last = HALF - PART * (N_PART - 1)
    pairs += [(ins[-1].at[0, last], du), (ins[-1].at[0, last + 1], dw)]
    copies = [pltpu.make_async_copy(src, dst, sem.at[j]) for j, (src, dst) in enumerate(pairs)]
    for copy in copies:
        copy.start()
    for copy in copies:
        copy.wait()


def solution(mesh):
    seq_spec = P(None, "cp", None, None)

    def local(query, key_in, value, bias_u, bias_w, rel_k, d_out):
        n_batch, rows, n_heads, head_dim = query.shape
        pairs = (n_batch, rows, N_PAIR, PAIR, head_dim)
        vm = pltpu.VMEM
        dma = pltpu.SemaphoreType.DMA
        whole = pl.BlockSpec(memory_space=pl.ANY)
        act = jax.ShapeDtypeStruct(pairs, BF16)
        vec = jax.ShapeDtypeStruct((n_heads, 1, head_dim), F32)
        tok = (PAIR, SEQ, HEAD)
        tok_t = (PAIR, HEAD, SEQ)
        acc = (HEAD + 8, HALF)
        outs = pl.pallas_call(
            kernel,
            name="rel_attn",
            out_shape=(act, act, act, act,
                       *[jax.ShapeDtypeStruct((2, PART, n_heads, 1, head_dim), F32)] * N_PART),
            in_specs=[pl.BlockSpec(memory_space=pltpu.HBM)] * 7,
            out_specs=[whole] * (4 + N_PART),
            scratch_shapes=[
                vm((4, SUBS, HALF, PAIR, HEAD), BF16), vm((2, SUBS, HALF, PAIR, HEAD), BF16), vm((2, PLANE - 1, ROWS, PAIR, HEAD), BF16),
                vm((SEQ, 2, PAIR, HEAD), BF16), vm((2, PAIR, HEAD), BF16), vm((2, PAIR, HEAD), BF16),
                vm((SUBS, PAIR, 8, HALF), F32), vm((SUBS, PAIR, 8, HALF), F32), vm((QB, HEAD), F32),
                vm((2, 2) + acc, F32), vm((2,) + acc, F32), vm((2, FIN, 1, HEAD), F32), vm((4, 2) + acc, F32),
                vm((QB, SEQ), F32), vm((QB, SEQ), F32), vm((QB, SEQ), F32),
                vm((QB, SEQ), BF16), vm((QB, SEQ), BF16), vm((QB, SEQ), BF16),
                vm(tok, BF16), vm(tok, BF16), vm(tok, BF16), vm(tok, BF16), vm(tok, BF16),
                vm(tok_t, BF16), vm(tok_t, BF16), vm(tok_t, BF16), vm(tok_t, BF16), vm(tok_t, BF16),
                vm((4, SEQ, HEAD), BF16), vm((4, HEAD, SEQ), BF16),
                vm((PAIR, HEAD, HALF), F32), vm((PAIR, HEAD, HALF), F32), vm((4, PAIR, HALF, HEAD), BF16),
                dma, dma((2, SUBS)), dma, dma, dma((2,)), dma((3,)), dma((4,)), dma((SUBS,)), dma, dma((SUBS,)),
                dma((2,)), dma((2,)), dma((2,)), dma((2,)), dma, dma((2, 3)), dma((2, 3)), dma((2, 2)), dma((2, 2)),
            ],
            compiler_params=pltpu.CompilerParams(collective_id=0, has_side_effects=True, vmem_limit_bytes=37 * 1024 * 1024),
        )(*[pltpu.with_memory_space_constraint(x, pltpu.HBM) for x in (
            query.reshape(pairs), key_in.reshape(pairs), value.reshape(pairs), d_out.reshape(pairs),
            rel_k.reshape(SEQ, N_PAIR, PAIR, head_dim), bias_u.reshape(N_PAIR, PAIR, head_dim), bias_w.reshape(N_PAIR, PAIR, head_dim))])
        o, dq, dk, dv, dr, du, dw = pl.pallas_call(
            writer,
            name="writer",
            out_shape=(act, act, act, act, jax.ShapeDtypeStruct((SEQ, n_heads, 1, head_dim), F32), vec, vec),
            in_specs=[whole] * (4 + N_PART),
            out_specs=[whole] * 7,
            scratch_shapes=[dma((6 + 2 * N_PART,))],
            compiler_params=pltpu.CompilerParams(vmem_limit_bytes=1024 * 1024),
        )(*outs)
        full = query.shape
        return (o.reshape(full), dq.reshape(full), dk.reshape(full), dv.reshape(full),
                du.reshape(bias_u.shape), dw.reshape(bias_w.shape), dr.reshape(rel_k.shape))

    return jax.shard_map(local, mesh=mesh,
                         in_specs=(seq_spec, seq_spec, seq_spec, P(), P(), P(), seq_spec),
                         out_specs=(seq_spec, seq_spec, seq_spec, seq_spec, P(), P(), P()),
                         check_vma=False)
```

```python
import jax
import jax.numpy as jnp
from jax import lax
from jax.experimental import pallas as pl
from jax.experimental.pallas import tpu as pltpu
from jax.sharding import PartitionSpec as P

MESH = pl.DeviceIdType.MESH
BF16, F32 = jnp.bfloat16, jnp.float32
LOG2E = 1.4426950408889634

N_DEV = 16
PLANE = 8
PAIR = 2
N_PAIR = 8
SLOTS = 4
SUBS = 2 * SLOTS
EARLY = 4
ROWS = 64
HALF = PLANE * ROWS
SEQ = 2 * HALF
HEAD = 128
QB = 256
WIN = HALF + QB
N_PART = 6
PART = 86
FIN = N_PART * PART
HOPS = ((1, 2, 4), (2, 1, 4)) * 3
TURNS = ((1, 3, 2), (3, 1, 2))


def dot(lhs, rhs):
    return jnp.dot(lhs, rhs, preferred_element_type=F32)


def flip8(x):
    rows, cols = x.shape
    idx = 7 - lax.broadcasted_iota(jnp.int32, (rows // 8, 8, cols), 1)
    return jnp.take_along_axis(x.reshape(rows // 8, 8, cols), idx, axis=1).reshape(rows, cols)


def eye_rev(dtype):
    total = lax.broadcasted_iota(jnp.int32, (HEAD, HEAD), 0) + lax.broadcasted_iota(jnp.int32, (HEAD, HEAD), 1)
    return jnp.where(total == HEAD - 1, 1.0, 0.0).astype(dtype)


def kernel(q_in, k_in, v_in, g_in, r_in, u_in, w_in,
           o_out, dq_out, dk_out, dv_out, dr0_out, dr1_out, dr2_out, dr3_out, dr4_out, dr5_out,
           buf, rbuf, r_buf, u_buf, w_buf, st_tx, st_rx, st_ref, dr_rx, dr_rz, dr_fin, dr_acc,
           s_ref, e_ref, dp_ref, pb_ref, ds_ref, dd_ref,
           a_s, c_s, g_s, k_s, v_s, at_s, ct_s, gt_s, kt_s, vt_s, rev_s, rt_s, dkt, dvt, stage,
           in_send, in_recv, out_send, out_recv, own_sem, r_sem, up_send, up_recv, st_send, st_recv,
           x_send, x_recv, z_send, z_recv, ring_send, ring_recv, fw_send, fw_recv):
    me = lax.axis_index("cp")
    core = me % 2
    chip = me // 2
    col = chip % 4
    z = chip // 4
    partner = me + 1 - 2 * core
    across = me + PLANE * (1 - 2 * z)
    scale = HEAD ** -0.5

    def wait_for(ref, sem):
        pltpu.make_async_copy(ref, ref, sem).wait()

    tables = [pltpu.make_async_copy(src, dst, r_sem.at[j]) for j, (src, dst) in enumerate(
        ((r_in.at[:, pl.ds(2 * col, 2)], r_buf), (u_in.at[pl.ds(2 * col, 2)], u_buf), (w_in.at[pl.ds(2 * col, 2)], w_buf)))]
    for copy in tables:
        copy.start()

    barrier = pltpu.get_barrier_semaphore()

    for peer in [across] + [me ^ step for step in range(PLANE - 1, 0, -1)]:
        pl.semaphore_signal(barrier, inc=1, device_id=(peer,), device_id_type=MESH)
    pl.semaphore_wait(barrier, PLANE)

    my_rows = pl.ds(pl.multiple_of((me % PLANE) * ROWS, ROWS), ROWS)

    def peers():
        for near_turn, far_turn in zip(*TURNS):
            turn = jnp.where(core == 0, near_turn, far_turn)
            yield me ^ (2 * turn)
            yield me ^ (2 * turn + 1)
        yield partner

    def send_in(ins, sub):
        pair, row = sub // SLOTS, sub % SLOTS
        for first in (0, 2):
            for t in (first, first + 1):
                pltpu.make_async_copy(ins[t].at[core * SLOTS + row, :, 2 * col + pair], buf.at[t, sub, my_rows], in_recv.at[first // 2, sub]).start()
            for peer in peers():
                for t in (first, first + 1):
                    pltpu.make_async_remote_copy(
                        src_ref=ins[t].at[(peer % 2) * SLOTS + row, :, 2 * ((peer // 2) % 4) + pair], dst_ref=buf.at[t, sub, my_rows],
                        send_sem=in_send, recv_sem=in_recv.at[first // 2, sub], device_id=(peer,), device_id_type=MESH).start()

    def send_all(ins):
        def send_sub(sub, carry):
            send_in(ins, sub)
            return carry
        lax.fori_loop(0, SUBS, send_sub, 0)

    @pl.when(z == 0)
    def _():
        send_all((k_in, v_in, q_in, g_in))

    @pl.when(z == 1)
    def _():
        send_all((q_in, g_in, k_in, v_in))

    for copy in tables:
        copy.wait()
    rev = eye_rev(BF16)
    for p in range(2):
        pair_tab = pltpu.einshape("abc->bac", r_buf[:, p])
        for hh in range(PAIR):
            for blk in range(SEQ // HEAD):
                part = pair_tab[hh, SEQ - HEAD * (blk + 1):SEQ - HEAD * blk]
                flipped = dot(rev, part).astype(BF16)
                rev_s[2 * p + hh, HEAD * blk:HEAD * (blk + 1), :] = flipped
                rt_s[2 * p + hh, :, HEAD * blk:HEAD * (blk + 1)] = flipped.T
    dr_acc[...] = jnp.zeros_like(dr_acc)

    acts = (dk_out, dv_out, o_out, dq_out)

    def send_out(sub, which):
        place = (core * SLOTS + sub % SLOTS, slice(None), 2 * col + sub // SLOTS)
        for t in which:
            pltpu.make_async_copy(buf.at[t, sub, my_rows], acts[t].at[place], out_recv).start()
        for peer in peers():
            peer_rows = pl.ds(pl.multiple_of((peer % PLANE) * ROWS, ROWS), ROWS)
            for t in which:
                pltpu.make_async_remote_copy(
                    src_ref=buf.at[t, sub, peer_rows], dst_ref=acts[t].at[place],
                    send_sem=out_send, recv_sem=out_recv, device_id=(peer,), device_id_type=MESH).start()

    def send_up(sub):
        wait_for(buf.at[0:2, sub], in_recv.at[0, sub])
        for j in range(2):
            pltpu.make_async_remote_copy(src_ref=buf.at[j, sub], dst_ref=rbuf.at[j, sub], send_sem=up_send.at[sub % 4], recv_sem=up_recv.at[sub],
                                         device_id=(across,), device_id_type=MESH).start()

    def unpack(ref, j, sub):
        return pltpu.einshape("abc->bac", ref[j, sub])

    def load_rows(q_ref, q_j, g_ref, g_j, sub, start, turned):
        rows = slice(start, start + HALF)
        p = sub // SLOTS
        q2 = unpack(q_ref, q_j, sub)
        u = u_buf[p].astype(F32)
        w = w_buf[p].astype(F32)
        for hh in range(PAIR):
            q32 = q2[hh].astype(F32)
            a = (q32 + u[hh:hh + 1]).astype(BF16)
            c = (q32 + w[hh:hh + 1]).astype(BF16)
            a_s[hh, rows, :] = a
            c_s[hh, rows, :] = c
            at_s[hh, :, rows] = a.T
            if turned:
                ct_s[hh, :, rows] = flip8(c.astype(F32)).astype(BF16).T
        g2 = unpack(g_ref, g_j, sub)
        g_s[:, rows, :] = g2
        for hh in range(PAIR):
            gt_s[hh, :, rows] = g2[hh].T

    def load_keys(k_ref, k_j, v_ref, v_j, sub, start):
        rows = slice(start, start + HALF)
        k2 = unpack(k_ref, k_j, sub)
        v2 = unpack(v_ref, v_j, sub)
        k_s[:, rows, :] = k2
        v_s[:, rows, :] = v2
        for hh in range(PAIR):
            kt_s[hh, :, rows] = k2[hh].T
            vt_s[hh, :, rows] = v2[hh].T

    def row_block(hh, head, start, i0, lo, fresh, stats):
        width = i0 + QB
        rows = slice(start, start + QB)
        s_ref[:, :width] = dot(a_s[hh, rows, :], kt_s[hh, :, :width])
        e_ref[:, :width] = dot(c_s[hh, rows, :], rt_s[head, :, SEQ - width:])
        dp_ref[:, :width] = dot(g_s[hh, rows, :], vt_s[hh, :, :width])
        for r0 in range(0, QB, 16):
            group = slice(r0, r0 + 16)
            rel = pltpu.roll(e_ref[group, :width], i0 + 1 + r0, 1, stride=1, stride_axis=0)
            s = s_ref[group, :width] + rel
            ahead = lax.broadcasted_iota(jnp.int32, (16, width), 1) - lax.broadcasted_iota(jnp.int32, (16, width), 0)
            s = jnp.where(ahead <= i0 + r0, s, -jnp.inf)
            top = jnp.max(s, axis=1, keepdims=True)
            p = jnp.exp2((s - top) * (scale * LOG2E))
            total = jnp.sum(p, axis=1, keepdims=True)
            p = p * (1.0 / total)
            pb_ref[group, :width] = p.astype(BF16)
            dp = dp_ref[group, :width]
            row_dot = jnp.sum(p * dp, axis=1, keepdims=True)
            ds = (p * (dp - row_dot) * scale).astype(BF16)
            ds_ref[group, :width] = ds
            flipped = flip8(ds.astype(F32))
            half = [pltpu.roll(flipped[8 * j:8 * j + 8], QB - 8 - r0 - 8 * j, 1, stride=1, stride_axis=0) for j in range(2)]
            dd_ref[group, :width] = jnp.concatenate(half, axis=0).astype(BF16)
            if stats:
                lane = lax.broadcasted_iota(jnp.int32, (16, HEAD), 1)
                st_ref[group, :] = jnp.where(lane == 0, top * (scale * LOG2E) + jnp.log2(total), row_dot)
        pb = pb_ref[:, :width]
        ds = ds_ref[:, :width]
        dd = dd_ref[:, :width]
        stage[0, hh, rows, :] = dot(pb, v_s[hh, :width, :]).astype(BF16)
        dqc = dot(ds, k_s[hh, :width, :])
        dqr = flip8(dot(dd, rev_s[head, SEQ - width:, :]))
        stage[1, hh, rows, :] = (dqc + dqr).astype(BF16)
        dr_acc[head, 1, HEAD:HEAD + 1, HALF - HEAD:] += jnp.sum(dqc, axis=0, keepdims=True)
        dr_acc[head, 1, HEAD + 1:HEAD + 2, HALF - HEAD:] += jnp.sum(dqr, axis=0, keepdims=True)
        dk_new = dot(at_s[hh, :, rows], ds_ref[:, lo:width])
        dv_new = dot(gt_s[hh, :, rows], pb_ref[:, lo:width])
        if fresh:
            dkt[hh] = dk_new
            dvt[hh] = dv_new
        else:
            dkt[hh, :, :width - lo] += dk_new
            dvt[hh, :, :width - lo] += dv_new
        dr_new = dot(ct_s[hh, :, rows], dd)
        if width > HALF:
            dr_acc[head, 0, :HEAD, SEQ - width:] += dr_new[:, :width - HALF]
            dr_acc[head, 1, :HEAD, :] += dr_new[:, width - HALF:]
        else:
            dr_acc[head, 1, :HEAD, HALF - width:] += dr_new

    def col_block(hh, head, sub, i0):
        rows = slice(i0, i0 + QB)
        first = WIN - i0
        s_ref[:, :HALF] = dot(a_s[hh, rows, :], kt_s[hh, :, :HALF])
        e_ref[:, :WIN] = dot(c_s[hh, rows, :], rt_s[head, :, first:first + WIN])
        dp_ref[:, :HALF] = dot(g_s[hh, rows, :], vt_s[hh, :, :HALF])
        st_ref[:, :8] = st_rx[sub, hh, :, i0 - HALF:i0 - HALF + QB].T
        for r0 in range(0, QB, 16):
            group = slice(r0, r0 + 16)
            rel = pltpu.roll(e_ref[group, :WIN], HALF + 1 + r0, 1, stride=1, stride_axis=0)[:, :HALF]
            log_sum = st_ref[group, 0:1]
            row_dot = st_ref[group, 1:2]
            p = jnp.exp2((s_ref[group, :HALF] + rel) * (scale * LOG2E) - log_sum)
            pb_ref[group, :HALF] = p.astype(BF16)
            ds_ref[group, :HALF] = (p * (dp_ref[group, :HALF] - row_dot) * scale).astype(BF16)
        dkt[hh] += dot(at_s[hh, :, rows], ds_ref[:, :HALF])
        dvt[hh] += dot(gt_s[hh, :, rows], pb_ref[:, :HALF])

    def store_rows(sub):
        for t in range(2):
            buf[2 + t, sub] = pltpu.einshape("abc->bac", stage[t])

    def store_keys(sub):
        for hh in range(PAIR):
            stage[2, hh] = dkt[hh].astype(BF16).T
            stage[3, hh] = dvt[hh].astype(BF16).T
        for t in range(2):
            buf[t, sub] = pltpu.einshape("abc->bac", stage[2 + t])

    def wait_up(sub):
        wait_for(rbuf.at[:, sub], up_recv.at[sub])
        wait_for(rbuf.at[:, sub], up_send.at[sub % 4])

    def wait_in(sub):
        wait_for(buf.at[2:4, sub], in_recv.at[1, sub])

    def lower_rows(sub):
        wait_in(sub)
        load_rows(buf, 2, buf, 3, sub, 0, True)

    def lower_own(sub):
        load_keys(buf, 0, buf, 1, sub, 0)

        def own(hh, carry):
            head = 2 * (sub // SLOTS) + hh
            row_block(hh, head, QB, QB, 0, True, False)
            row_block(hh, head, 0, 0, 0, False, False)
            return carry

        lax.fori_loop(0, PAIR, own, 0)
        store_rows(sub)

    def lower_theirs(sub):
        wait_up(sub)
        load_rows(rbuf, 0, rbuf, 1, sub, HALF, False)
        wait_for(st_rx.at[sub], st_recv.at[sub])

        def theirs(hh, carry):
            head = 2 * (sub // SLOTS) + hh
            col_block(hh, head, sub, HALF)
            col_block(hh, head, sub, HALF + QB)
            return carry

        lax.fori_loop(0, PAIR, theirs, 0)
        store_keys(sub)

    def upper_own(sub):
        wait_in(sub)
        wait_up(sub)
        load_rows(buf, 0, buf, 1, sub, 0, True)
        load_keys(rbuf, 0, rbuf, 1, sub, 0)
        load_keys(buf, 2, buf, 3, sub, HALF)

        def own(hh, carry):
            head = 2 * (sub // SLOTS) + hh
            for blk in (1, 0):
                row_block(hh, head, QB * blk, HALF + QB * blk, HALF, blk == 1, True)
                st_tx[sub, hh, :, QB * blk:QB * (blk + 1)] = st_ref[...].T[:8]
            pltpu.make_async_remote_copy(src_ref=st_tx.at[sub, hh], dst_ref=st_rx.at[sub, hh], send_sem=st_send, recv_sem=st_recv.at[sub],
                                         device_id=(across,), device_id_type=MESH).start()
            return carry

        lax.fori_loop(0, PAIR, own, 0)
        store_rows(sub)
        store_keys(sub)

    side = 1 - core
    parts = (dr0_out, dr1_out, dr2_out, dr3_out, dr4_out, dr5_out)

    def swap_start(p):
        for n in range(2):
            pltpu.make_async_remote_copy(src_ref=dr_acc.at[2 * p + n, side], dst_ref=dr_rx.at[p, n], send_sem=x_send.at[p], recv_sem=x_recv.at[p],
                                         device_id=(partner,), device_id_type=MESH).start()

    def swap_add(p):
        wait_for(dr_rx.at[p], x_recv.at[p])
        for n in range(2):
            dr_rx[p, n] = dr_rx[p, n] + dr_acc[2 * p + n, core]

    def cross_start(p):
        pltpu.make_async_remote_copy(src_ref=dr_rx.at[p, 1 - z], dst_ref=dr_rz.at[p], send_sem=z_send.at[p], recv_sem=z_recv.at[p],
                                     device_id=(across,), device_id_type=MESH).start()

    def head_of(p, bits):
        other = chip ^ bits
        return 4 * (other % 4) + 2 * p + other // 4

    def block(p, m, bits):
        if bits == 0:
            return dr_fin.at[p, PART * m:PART * (m + 1)]
        return parts[m].at[side, :, head_of(p, bits)]

    def forward(p, m, bits):
        pltpu.make_async_remote_copy(src_ref=block(p, m, bits), dst_ref=parts[m].at[side, :, head_of(p, bits)], send_sem=fw_send.at[p, m // 3],
                                     recv_sem=fw_recv.at[p, m // 3], device_id=(partner,), device_id_type=MESH).start()

    def held(m, hop):
        have = [0]
        for bit in HOPS[m][:hop]:
            have = have + [bits ^ bit for bits in have]
        return have

    def blocks(count):
        return parts[0].at[:, :, :count // 2]

    def hop_start(p, hop):
        for m in range(N_PART):
            for bits in held(m, hop):
                pltpu.make_async_remote_copy(
                    src_ref=block(p, m, bits), dst_ref=parts[m].at[side, :, head_of(p, bits)], send_sem=ring_send.at[p, hop],
                    recv_sem=ring_recv.at[p, hop], device_id=(me ^ (2 * HOPS[m][hop]),), device_id_type=MESH).start()

    def hop_wait(p, hop):
        wait_for(blocks(N_PART << hop), ring_recv.at[p, hop])
        for m in range(N_PART):
            have = held(m, hop + 1)
            for bits in have[len(have) // 2:]:
                forward(p, m, bits)

    def cross_finish(p):
        wait_for(dr_rz.at[p], z_recv.at[p])
        total = dr_rx[p, z] + dr_rz[p]
        rev32 = eye_rev(F32)
        for m in range(HALF // HEAD):
            part = total[:HEAD, HALF - HEAD * (m + 1):HALF - HEAD * m]
            turned = lax.dot_general(rev32, part, (((1,), (1,)), ((), ())), precision=lax.Precision.HIGHEST, preferred_element_type=F32)
            dr_fin[p, HEAD * m:HEAD * (m + 1)] = turned.reshape(HEAD, 1, HEAD)
        dr_fin[p, HALF] = total[HEAD:HEAD + 1, HALF - HEAD:]
        dr_fin[p, HALF + 1] = total[HEAD + 1:HEAD + 2, HALF - HEAD:]
        dr_fin[p, HALF + 2:] = jnp.zeros((FIN - HALF - 2, 1, HEAD), F32)
        hop_start(p, 0)
        for m in range(N_PART):
            pltpu.make_async_copy(block(p, m, 0), parts[m].at[side, :, head_of(p, 0)], own_sem.at[p]).start()
            forward(p, m, 0)

    send_up(0)

    def sub_body(sub, carry):
        @pl.when(sub < SUBS - 1)
        def _():
            send_up(sub + 1)

        @pl.when(sub == SLOTS)
        def _():
            swap_start(0)

        @pl.when(sub == SUBS - 1)
        def _():
            swap_add(0)
            cross_start(0)

        @pl.when(sub == SUBS)
        def _():
            swap_start(1)
            cross_finish(0)

        @pl.when((z == 0) & (sub < SUBS))
        def _():
            lower_rows(sub)

        @pl.when((z == 0) & (sub > 0))
        def _():
            lower_theirs(sub - 1)

        @pl.when((z == 0) & (sub < SUBS))
        def _():
            lower_own(sub)

        @pl.when((z == 1) & (sub < SUBS))
        def _():
            upper_own(sub)

        @pl.when(sub < EARLY)
        def _():
            send_out(sub, (2, 3))

        @pl.when((sub > 0) & (sub <= EARLY))
        def _():
            send_out(sub - 1, (0, 1))
        return carry

    lax.fori_loop(0, SUBS + 1, sub_body, 0)

    swap_add(1)
    cross_start(1)
    cross_finish(1)
    for p in range(2):
        hop_wait(p, 0)
        hop_start(p, 1)

    def send_late(sub, carry):
        send_out(sub, range(4))
        return carry

    lax.fori_loop(EARLY, EARLY + 2, send_late, 0)
    for p in range(2):
        hop_wait(p, 1)
        hop_start(p, 2)
    lax.fori_loop(EARLY + 2, SUBS, send_late, 0)
    for p in range(2):
        hop_wait(p, 2)

    wait_for(buf, out_recv)
    wait_for(buf.at[:, :, :HALF - ROWS], in_send)
    wait_for(buf.at[:, :, :HALF - ROWS], out_send)

    @pl.when(z == 1)
    def _():
        wait_for(st_tx, st_send)

    for p in range(2):
        wait_for(dr_rx.at[p], x_send.at[p])
        wait_for(dr_rz.at[p], z_send.at[p])
        wait_for(blocks(N_PART), own_sem.at[p])
        for hop in range(3):
            wait_for(blocks(N_PART << hop), ring_send.at[p, hop])
        for n in range(2):
            wait_for(blocks(N_PART // 2 * N_PAIR), fw_send.at[p, n])
            wait_for(blocks(N_PART // 2 * N_PAIR), fw_recv.at[p, n])


def writer(*refs):
    ins, (o, dq, dk, dv, dr, du, dw, sem) = refs[:4 + N_PART], refs[4 + N_PART:]
    pairs = list(zip(ins[:4], (o, dq, dk, dv)))
    for m, part in enumerate(ins[4:]):
        rows = min(PART, HALF - PART * m)
        for side in range(2):
            start = HALF * side + PART * m
            pairs.append((part.at[side, :rows], dr.at[start:start + rows]))
    last = HALF - PART * (N_PART - 1)
    pairs += [(ins[-1].at[0, last], du), (ins[-1].at[0, last + 1], dw)]
    copies = [pltpu.make_async_copy(src, dst, sem.at[j]) for j, (src, dst) in enumerate(pairs)]
    for copy in copies:
        copy.start()
    for copy in copies:
        copy.wait()


def solution(mesh):
    seq_spec = P(None, "cp", None, None)

    def local(query, key_in, value, bias_u, bias_w, rel_k, d_out):
        n_batch, rows, n_heads, head_dim = query.shape
        pairs = (n_batch, rows, N_PAIR, PAIR, head_dim)
        vm = pltpu.VMEM
        dma = pltpu.SemaphoreType.DMA
        whole = pl.BlockSpec(memory_space=pl.ANY)
        act = jax.ShapeDtypeStruct(pairs, BF16)
        vec = jax.ShapeDtypeStruct((n_heads, 1, head_dim), F32)
        tok = (PAIR, SEQ, HEAD)
        tok_t = (PAIR, HEAD, SEQ)
        acc = (HEAD + 8, HALF)
        outs = pl.pallas_call(
            kernel,
            name="rel_attn",
            out_shape=(act, act, act, act,
                       *[jax.ShapeDtypeStruct((2, PART, n_heads, 1, head_dim), F32)] * N_PART),
            in_specs=[pl.BlockSpec(memory_space=pltpu.HBM)] * 7,
            out_specs=[whole] * (4 + N_PART),
            scratch_shapes=[
                vm((4, SUBS, HALF, PAIR, HEAD), BF16), vm((2, SUBS, HALF, PAIR, HEAD), BF16),
                vm((SEQ, 2, PAIR, HEAD), BF16), vm((2, PAIR, HEAD), BF16), vm((2, PAIR, HEAD), BF16),
                vm((SUBS, PAIR, 8, HALF), F32), vm((SUBS, PAIR, 8, HALF), F32), vm((QB, HEAD), F32),
                vm((2, 2) + acc, F32), vm((2,) + acc, F32), vm((2, FIN, 1, HEAD), F32), vm((4, 2) + acc, F32),
                vm((QB, SEQ), F32), vm((QB, SEQ), F32), vm((QB, SEQ), F32),
                vm((QB, SEQ), BF16), vm((QB, SEQ), BF16), vm((QB, SEQ), BF16),
                vm(tok, BF16), vm(tok, BF16), vm(tok, BF16), vm(tok, BF16), vm(tok, BF16),
                vm(tok_t, BF16), vm(tok_t, BF16), vm(tok_t, BF16), vm(tok_t, BF16), vm(tok_t, BF16),
                vm((4, SEQ, HEAD), BF16), vm((4, HEAD, SEQ), BF16),
                vm((PAIR, HEAD, HALF), F32), vm((PAIR, HEAD, HALF), F32), vm((4, PAIR, HALF, HEAD), BF16),
                dma, dma((2, SUBS)), dma, dma, dma((2,)), dma((3,)), dma((4,)), dma((SUBS,)), dma, dma((SUBS,)),
                dma((2,)), dma((2,)), dma((2,)), dma((2,)), dma((2, 3)), dma((2, 3)), dma((2, 2)), dma((2, 2)),
            ],
            compiler_params=pltpu.CompilerParams(collective_id=0, has_side_effects=True, vmem_limit_bytes=36 * 1024 * 1024),
        )(*[pltpu.with_memory_space_constraint(x, pltpu.HBM) for x in (
            query.reshape(pairs), key_in.reshape(pairs), value.reshape(pairs), d_out.reshape(pairs),
            rel_k.reshape(SEQ, N_PAIR, PAIR, head_dim), bias_u.reshape(N_PAIR, PAIR, head_dim), bias_w.reshape(N_PAIR, PAIR, head_dim))])
        o, dq, dk, dv, dr, du, dw = pl.pallas_call(
            writer,
            name="writer",
            out_shape=(act, act, act, act, jax.ShapeDtypeStruct((SEQ, n_heads, 1, head_dim), F32), vec, vec),
            in_specs=[whole] * (4 + N_PART),
            out_specs=[whole] * 7,
            scratch_shapes=[dma((6 + 2 * N_PART,))],
            compiler_params=pltpu.CompilerParams(vmem_limit_bytes=1024 * 1024),
        )(*outs)
        full = query.shape
        return (o.reshape(full), dq.reshape(full), dk.reshape(full), dv.reshape(full),
                du.reshape(bias_u.shape), dw.reshape(bias_w.shape), dr.reshape(rel_k.shape))

    return jax.shard_map(local, mesh=mesh,
                         in_specs=(seq_spec, seq_spec, seq_spec, P(), P(), P(), seq_spec),
                         out_specs=(seq_spec, seq_spec, seq_spec, seq_spec, P(), P(), P()),
                         check_vma=False)
```

```python
import jax
import jax.numpy as jnp
from jax import lax
from jax.experimental import pallas as pl
from jax.experimental.pallas import tpu as pltpu
from jax.sharding import PartitionSpec as P

MESH = pl.DeviceIdType.MESH
BF16, F32 = jnp.bfloat16, jnp.float32
LOG2E = 1.4426950408889634

N_DEV = 16
PLANE = 8
PAIR = 2
N_PAIR = 8
SLOTS = 4
SUBS = 2 * SLOTS
EARLY = 4
ROWS = 64
HALF = PLANE * ROWS
SEQ = 2 * HALF
HEAD = 128
QB = 256
WIN = HALF + QB
N_PART = 6
PART = 86
FIN = N_PART * PART
HOPS = ((2, 1, 4), (2, 1, 4), (1, 2, 4)) * 2
TURNS = ((1, 3, 2), (3, 1, 2))


def dot(lhs, rhs):
    return jnp.dot(lhs, rhs, preferred_element_type=F32)


def flip8(x):
    rows, cols = x.shape
    idx = 7 - lax.broadcasted_iota(jnp.int32, (rows // 8, 8, cols), 1)
    return jnp.take_along_axis(x.reshape(rows // 8, 8, cols), idx, axis=1).reshape(rows, cols)


def eye_rev(dtype):
    total = lax.broadcasted_iota(jnp.int32, (HEAD, HEAD), 0) + lax.broadcasted_iota(jnp.int32, (HEAD, HEAD), 1)
    return jnp.where(total == HEAD - 1, 1.0, 0.0).astype(dtype)


def kernel(q_in, k_in, v_in, g_in, r_in, u_in, w_in,
           o_out, dq_out, dk_out, dv_out, dr0_out, dr1_out, dr2_out, dr3_out, dr4_out, dr5_out,
           buf, rbuf, r_buf, u_buf, w_buf, st_tx, st_rx, st_ref, dr_rx, dr_rz, dr_fin, dr_acc,
           s_ref, e_ref, dp_ref, pb_ref, ds_ref, dd_ref,
           a_s, c_s, g_s, k_s, v_s, at_s, ct_s, gt_s, kt_s, vt_s, rev_s, rt_s, dkt, dvt, stage,
           in_send, in_recv, out_send, out_recv, own_sem, r_sem, up_send, up_recv, st_send, st_recv,
           x_send, x_recv, z_send, z_recv, ring_send, ring_recv, fw_send, fw_recv):
    me = lax.axis_index("cp")
    core = me % 2
    chip = me // 2
    col = chip % 4
    z = chip // 4
    partner = me + 1 - 2 * core
    across = me + PLANE * (1 - 2 * z)
    scale = HEAD ** -0.5

    def wait_for(ref, sem):
        pltpu.make_async_copy(ref, ref, sem).wait()

    tables = [pltpu.make_async_copy(src, dst, r_sem.at[j]) for j, (src, dst) in enumerate(
        ((r_in.at[:, pl.ds(2 * col, 2)], r_buf), (u_in.at[pl.ds(2 * col, 2)], u_buf), (w_in.at[pl.ds(2 * col, 2)], w_buf)))]
    for copy in tables:
        copy.start()

    barrier = pltpu.get_barrier_semaphore()

    for peer in [across] + [me ^ step for step in range(PLANE - 1, 0, -1)]:
        pl.semaphore_signal(barrier, inc=1, device_id=(peer,), device_id_type=MESH)
    pl.semaphore_wait(barrier, PLANE)

    my_rows = pl.ds(pl.multiple_of((me % PLANE) * ROWS, ROWS), ROWS)

    def peers():
        for near_turn, far_turn in zip(*TURNS):
            turn = jnp.where(core == 0, near_turn, far_turn)
            yield me ^ (2 * turn)
            yield me ^ (2 * turn + 1)
        yield partner

    def send_in(ins, sub):
        pair, row = sub // SLOTS, sub % SLOTS
        for first in (0, 2):
            for t in (first, first + 1):
                pltpu.make_async_copy(ins[t].at[core * SLOTS + row, :, 2 * col + pair], buf.at[t, sub, my_rows], in_recv.at[first // 2, sub]).start()
            for peer in peers():
                for t in (first, first + 1):
                    pltpu.make_async_remote_copy(
                        src_ref=ins[t].at[(peer % 2) * SLOTS + row, :, 2 * ((peer // 2) % 4) + pair], dst_ref=buf.at[t, sub, my_rows],
                        send_sem=in_send, recv_sem=in_recv.at[first // 2, sub], device_id=(peer,), device_id_type=MESH).start()

    def send_all(ins):
        def send_sub(sub, carry):
            send_in(ins, sub)
            return carry
        lax.fori_loop(0, SUBS, send_sub, 0)

    @pl.when(z == 0)
    def _():
        send_all((k_in, v_in, q_in, g_in))

    @pl.when(z == 1)
    def _():
        send_all((q_in, g_in, k_in, v_in))

    for copy in tables:
        copy.wait()
    rev = eye_rev(BF16)
    for p in range(2):
        pair_tab = pltpu.einshape("abc->bac", r_buf[:, p])
        for hh in range(PAIR):
            for blk in range(SEQ // HEAD):
                part = pair_tab[hh, SEQ - HEAD * (blk + 1):SEQ - HEAD * blk]
                flipped = dot(rev, part).astype(BF16)
                rev_s[2 * p + hh, HEAD * blk:HEAD * (blk + 1), :] = flipped
                rt_s[2 * p + hh, :, HEAD * blk:HEAD * (blk + 1)] = flipped.T
    dr_acc[...] = jnp.zeros_like(dr_acc)

    acts = (dk_out, dv_out, o_out, dq_out)

    def send_out(sub, which):
        place = (core * SLOTS + sub % SLOTS, slice(None), 2 * col + sub // SLOTS)
        for t in which:
            pltpu.make_async_copy(buf.at[t, sub, my_rows], acts[t].at[place], out_recv).start()
        for peer in peers():
            peer_rows = pl.ds(pl.multiple_of((peer % PLANE) * ROWS, ROWS), ROWS)
            for t in which:
                pltpu.make_async_remote_copy(
                    src_ref=buf.at[t, sub, peer_rows], dst_ref=acts[t].at[place],
                    send_sem=out_send, recv_sem=out_recv, device_id=(peer,), device_id_type=MESH).start()

    def send_up(sub):
        wait_for(buf.at[0:2, sub], in_recv.at[0, sub])
        for j in range(2):
            pltpu.make_async_remote_copy(src_ref=buf.at[j, sub], dst_ref=rbuf.at[j, sub], send_sem=up_send.at[sub % 4], recv_sem=up_recv.at[sub],
                                         device_id=(across,), device_id_type=MESH).start()

    def unpack(ref, j, sub):
        return pltpu.einshape("abc->bac", ref[j, sub])

    def load_rows(q_ref, q_j, g_ref, g_j, sub, start, turned):
        rows = slice(start, start + HALF)
        p = sub // SLOTS
        q2 = unpack(q_ref, q_j, sub)
        u = u_buf[p].astype(F32)
        w = w_buf[p].astype(F32)
        for hh in range(PAIR):
            q32 = q2[hh].astype(F32)
            a = (q32 + u[hh:hh + 1]).astype(BF16)
            c = (q32 + w[hh:hh + 1]).astype(BF16)
            a_s[hh, rows, :] = a
            c_s[hh, rows, :] = c
            at_s[hh, :, rows] = a.T
            if turned:
                ct_s[hh, :, rows] = flip8(c.astype(F32)).astype(BF16).T
        g2 = unpack(g_ref, g_j, sub)
        g_s[:, rows, :] = g2
        for hh in range(PAIR):
            gt_s[hh, :, rows] = g2[hh].T

    def load_keys(k_ref, k_j, v_ref, v_j, sub, start):
        rows = slice(start, start + HALF)
        k2 = unpack(k_ref, k_j, sub)
        v2 = unpack(v_ref, v_j, sub)
        k_s[:, rows, :] = k2
        v_s[:, rows, :] = v2
        for hh in range(PAIR):
            kt_s[hh, :, rows] = k2[hh].T
            vt_s[hh, :, rows] = v2[hh].T

    def row_block(hh, head, start, i0, lo, fresh, stats):
        width = i0 + QB
        rows = slice(start, start + QB)
        s_ref[:, :width] = dot(a_s[hh, rows, :], kt_s[hh, :, :width])
        e_ref[:, :width] = dot(c_s[hh, rows, :], rt_s[head, :, SEQ - width:])
        dp_ref[:, :width] = dot(g_s[hh, rows, :], vt_s[hh, :, :width])
        for r0 in range(0, QB, 16):
            group = slice(r0, r0 + 16)
            rel = pltpu.roll(e_ref[group, :width], i0 + 1 + r0, 1, stride=1, stride_axis=0)
            s = s_ref[group, :width] + rel
            ahead = lax.broadcasted_iota(jnp.int32, (16, width), 1) - lax.broadcasted_iota(jnp.int32, (16, width), 0)
            s = jnp.where(ahead <= i0 + r0, s, -jnp.inf)
            top = jnp.max(s, axis=1, keepdims=True)
            p = jnp.exp2((s - top) * (scale * LOG2E))
            total = jnp.sum(p, axis=1, keepdims=True)
            p = p * (1.0 / total)
            pb_ref[group, :width] = p.astype(BF16)
            dp = dp_ref[group, :width]
            row_dot = jnp.sum(p * dp, axis=1, keepdims=True)
            ds = (p * (dp - row_dot) * scale).astype(BF16)
            ds_ref[group, :width] = ds
            flipped = flip8(ds.astype(F32))
            half = [pltpu.roll(flipped[8 * j:8 * j + 8], QB - 8 - r0 - 8 * j, 1, stride=1, stride_axis=0) for j in range(2)]
            dd_ref[group, :width] = jnp.concatenate(half, axis=0).astype(BF16)
            if stats:
                lane = lax.broadcasted_iota(jnp.int32, (16, HEAD), 1)
                st_ref[group, :] = jnp.where(lane == 0, top * (scale * LOG2E) + jnp.log2(total), row_dot)
        pb = pb_ref[:, :width]
        ds = ds_ref[:, :width]
        dd = dd_ref[:, :width]
        stage[0, hh, rows, :] = dot(pb, v_s[hh, :width, :]).astype(BF16)
        dqc = dot(ds, k_s[hh, :width, :])
        dqr = flip8(dot(dd, rev_s[head, SEQ - width:, :]))
        stage[1, hh, rows, :] = (dqc + dqr).astype(BF16)
        dr_acc[head, 1, HEAD:HEAD + 1, HALF - HEAD:] += jnp.sum(dqc, axis=0, keepdims=True)
        dr_acc[head, 1, HEAD + 1:HEAD + 2, HALF - HEAD:] += jnp.sum(dqr, axis=0, keepdims=True)
        dk_new = dot(at_s[hh, :, rows], ds_ref[:, lo:width])
        dv_new = dot(gt_s[hh, :, rows], pb_ref[:, lo:width])
        if fresh:
            dkt[hh] = dk_new
            dvt[hh] = dv_new
        else:
            dkt[hh, :, :width - lo] += dk_new
            dvt[hh, :, :width - lo] += dv_new
        dr_new = dot(ct_s[hh, :, rows], dd)
        if width > HALF:
            dr_acc[head, 0, :HEAD, SEQ - width:] += dr_new[:, :width - HALF]
            dr_acc[head, 1, :HEAD, :] += dr_new[:, width - HALF:]
        else:
            dr_acc[head, 1, :HEAD, HALF - width:] += dr_new

    def col_block(hh, head, sub, i0):
        rows = slice(i0, i0 + QB)
        first = WIN - i0
        s_ref[:, :HALF] = dot(a_s[hh, rows, :], kt_s[hh, :, :HALF])
        e_ref[:, :WIN] = dot(c_s[hh, rows, :], rt_s[head, :, first:first + WIN])
        dp_ref[:, :HALF] = dot(g_s[hh, rows, :], vt_s[hh, :, :HALF])
        st_ref[:, :8] = st_rx[sub, hh, :, i0 - HALF:i0 - HALF + QB].T
        for r0 in range(0, QB, 16):
            group = slice(r0, r0 + 16)
            rel = pltpu.roll(e_ref[group, :WIN], HALF + 1 + r0, 1, stride=1, stride_axis=0)[:, :HALF]
            log_sum = st_ref[group, 0:1]
            row_dot = st_ref[group, 1:2]
            p = jnp.exp2((s_ref[group, :HALF] + rel) * (scale * LOG2E) - log_sum)
            pb_ref[group, :HALF] = p.astype(BF16)
            ds_ref[group, :HALF] = (p * (dp_ref[group, :HALF] - row_dot) * scale).astype(BF16)
        dkt[hh] += dot(at_s[hh, :, rows], ds_ref[:, :HALF])
        dvt[hh] += dot(gt_s[hh, :, rows], pb_ref[:, :HALF])

    def store_rows(sub):
        for t in range(2):
            buf[2 + t, sub] = pltpu.einshape("abc->bac", stage[t])

    def store_keys(sub):
        for hh in range(PAIR):
            stage[2, hh] = dkt[hh].astype(BF16).T
            stage[3, hh] = dvt[hh].astype(BF16).T
        for t in range(2):
            buf[t, sub] = pltpu.einshape("abc->bac", stage[2 + t])

    def wait_up(sub):
        wait_for(rbuf.at[:, sub], up_recv.at[sub])
        wait_for(rbuf.at[:, sub], up_send.at[sub % 4])

    def wait_in(sub):
        wait_for(buf.at[2:4, sub], in_recv.at[1, sub])

    def lower_rows(sub):
        wait_in(sub)
        load_rows(buf, 2, buf, 3, sub, 0, True)

    def lower_own(sub):
        load_keys(buf, 0, buf, 1, sub, 0)

        def own(hh, carry):
            head = 2 * (sub // SLOTS) + hh
            row_block(hh, head, QB, QB, 0, True, False)
            row_block(hh, head, 0, 0, 0, False, False)
            return carry

        lax.fori_loop(0, PAIR, own, 0)
        store_rows(sub)

    def lower_theirs(sub):
        wait_up(sub)
        load_rows(rbuf, 0, rbuf, 1, sub, HALF, False)
        wait_for(st_rx.at[sub], st_recv.at[sub])

        def theirs(hh, carry):
            head = 2 * (sub // SLOTS) + hh
            col_block(hh, head, sub, HALF)
            col_block(hh, head, sub, HALF + QB)
            return carry

        lax.fori_loop(0, PAIR, theirs, 0)
        store_keys(sub)

    def upper_own(sub):
        wait_in(sub)
        wait_up(sub)
        load_rows(buf, 0, buf, 1, sub, 0, True)
        load_keys(rbuf, 0, rbuf, 1, sub, 0)
        load_keys(buf, 2, buf, 3, sub, HALF)

        def own(hh, carry):
            head = 2 * (sub // SLOTS) + hh
            for blk in (1, 0):
                row_block(hh, head, QB * blk, HALF + QB * blk, HALF, blk == 1, True)
                st_tx[sub, hh, :, QB * blk:QB * (blk + 1)] = st_ref[...].T[:8]
            pltpu.make_async_remote_copy(src_ref=st_tx.at[sub, hh], dst_ref=st_rx.at[sub, hh], send_sem=st_send, recv_sem=st_recv.at[sub],
                                         device_id=(across,), device_id_type=MESH).start()
            return carry

        lax.fori_loop(0, PAIR, own, 0)
        store_rows(sub)
        store_keys(sub)

    side = 1 - core
    parts = (dr0_out, dr1_out, dr2_out, dr3_out, dr4_out, dr5_out)

    def swap_start(p):
        for n in range(2):
            pltpu.make_async_remote_copy(src_ref=dr_acc.at[2 * p + n, side], dst_ref=dr_rx.at[p, n], send_sem=x_send.at[p], recv_sem=x_recv.at[p],
                                         device_id=(partner,), device_id_type=MESH).start()

    def swap_add(p):
        wait_for(dr_rx.at[p], x_recv.at[p])
        for n in range(2):
            dr_rx[p, n] = dr_rx[p, n] + dr_acc[2 * p + n, core]

    def cross_start(p):
        pltpu.make_async_remote_copy(src_ref=dr_rx.at[p, 1 - z], dst_ref=dr_rz.at[p], send_sem=z_send.at[p], recv_sem=z_recv.at[p],
                                     device_id=(across,), device_id_type=MESH).start()

    def head_of(p, bits):
        other = chip ^ bits
        return 4 * (other % 4) + 2 * p + other // 4

    def block(p, m, bits):
        if bits == 0:
            return dr_fin.at[p, PART * m:PART * (m + 1)]
        return parts[m].at[side, :, head_of(p, bits)]

    def forward(p, m, bits):
        pltpu.make_async_remote_copy(src_ref=block(p, m, bits), dst_ref=parts[m].at[side, :, head_of(p, bits)], send_sem=fw_send.at[p, m // 3],
                                     recv_sem=fw_recv.at[p, m // 3], device_id=(partner,), device_id_type=MESH).start()

    def held(m, hop):
        have = [0]
        for bit in HOPS[m][:hop]:
            have = have + [bits ^ bit for bits in have]
        return have

    def blocks(count):
        return parts[0].at[:, :, :count // 2]

    def hop_start(p, hop):
        for m in range(N_PART):
            for bits in held(m, hop):
                pltpu.make_async_remote_copy(
                    src_ref=block(p, m, bits), dst_ref=parts[m].at[side, :, head_of(p, bits)], send_sem=ring_send.at[p, hop],
                    recv_sem=ring_recv.at[p, hop], device_id=(me ^ (2 * HOPS[m][hop]),), device_id_type=MESH).start()

    def hop_wait(p, hop):
        wait_for(blocks(N_PART << hop), ring_recv.at[p, hop])
        for m in range(N_PART):
            have = held(m, hop + 1)
            for bits in have[len(have) // 2:]:
                forward(p, m, bits)

    def cross_finish(p):
        wait_for(dr_rz.at[p], z_recv.at[p])
        total = dr_rx[p, z] + dr_rz[p]
        rev32 = eye_rev(F32)
        for m in range(HALF // HEAD):
            part = total[:HEAD, HALF - HEAD * (m + 1):HALF - HEAD * m]
            turned = lax.dot_general(rev32, part, (((1,), (1,)), ((), ())), precision=lax.Precision.HIGHEST, preferred_element_type=F32)
            dr_fin[p, HEAD * m:HEAD * (m + 1)] = turned.reshape(HEAD, 1, HEAD)
        dr_fin[p, HALF] = total[HEAD:HEAD + 1, HALF - HEAD:]
        dr_fin[p, HALF + 1] = total[HEAD + 1:HEAD + 2, HALF - HEAD:]
        dr_fin[p, HALF + 2:] = jnp.zeros((FIN - HALF - 2, 1, HEAD), F32)
        hop_start(p, 0)
        for m in range(N_PART):
            pltpu.make_async_copy(block(p, m, 0), parts[m].at[side, :, head_of(p, 0)], own_sem.at[p]).start()
            forward(p, m, 0)

    send_up(0)

    def sub_body(sub, carry):
        @pl.when(sub < SUBS - 1)
        def _():
            send_up(sub + 1)

        @pl.when(sub == SLOTS)
        def _():
            swap_start(0)

        @pl.when(sub == SUBS - 1)
        def _():
            swap_add(0)
            cross_start(0)

        @pl.when(sub == SUBS)
        def _():
            swap_start(1)
            cross_finish(0)

        @pl.when((z == 0) & (sub < SUBS))
        def _():
            lower_rows(sub)

        @pl.when((z == 0) & (sub > 0))
        def _():
            lower_theirs(sub - 1)

        @pl.when((z == 0) & (sub < SUBS))
        def _():
            lower_own(sub)

        @pl.when((z == 1) & (sub < SUBS))
        def _():
            upper_own(sub)

        @pl.when(sub < EARLY)
        def _():
            send_out(sub, (2, 3))

        @pl.when((sub > 0) & (sub <= EARLY))
        def _():
            send_out(sub - 1, (0, 1))
        return carry

    lax.fori_loop(0, SUBS + 1, sub_body, 0)

    swap_add(1)
    cross_start(1)
    cross_finish(1)
    for p in range(2):
        hop_wait(p, 0)
        hop_start(p, 1)

    def send_late(sub, carry):
        send_out(sub, range(4))
        return carry

    lax.fori_loop(EARLY, EARLY + 2, send_late, 0)
    for p in range(2):
        hop_wait(p, 1)
        hop_start(p, 2)
    lax.fori_loop(EARLY + 2, SUBS, send_late, 0)
    for p in range(2):
        hop_wait(p, 2)

    wait_for(buf, out_recv)
    wait_for(buf.at[:, :, :HALF - ROWS], in_send)
    wait_for(buf.at[:, :, :HALF - ROWS], out_send)

    @pl.when(z == 1)
    def _():
        wait_for(st_tx, st_send)

    for p in range(2):
        wait_for(dr_rx.at[p], x_send.at[p])
        wait_for(dr_rz.at[p], z_send.at[p])
        wait_for(blocks(N_PART), own_sem.at[p])
        for hop in range(3):
            wait_for(blocks(N_PART << hop), ring_send.at[p, hop])
        for n in range(2):
            wait_for(blocks(N_PART // 2 * N_PAIR), fw_send.at[p, n])
            wait_for(blocks(N_PART // 2 * N_PAIR), fw_recv.at[p, n])


def writer(*refs):
    ins, (o, dq, dk, dv, dr, du, dw, sem) = refs[:4 + N_PART], refs[4 + N_PART:]
    pairs = list(zip(ins[:4], (o, dq, dk, dv)))
    for m, part in enumerate(ins[4:]):
        rows = min(PART, HALF - PART * m)
        for side in range(2):
            start = HALF * side + PART * m
            pairs.append((part.at[side, :rows], dr.at[start:start + rows]))
    last = HALF - PART * (N_PART - 1)
    pairs += [(ins[-1].at[0, last], du), (ins[-1].at[0, last + 1], dw)]
    copies = [pltpu.make_async_copy(src, dst, sem.at[j]) for j, (src, dst) in enumerate(pairs)]
    for copy in copies:
        copy.start()
    for copy in copies:
        copy.wait()


def solution(mesh):
    seq_spec = P(None, "cp", None, None)

    def local(query, key_in, value, bias_u, bias_w, rel_k, d_out):
        n_batch, rows, n_heads, head_dim = query.shape
        pairs = (n_batch, rows, N_PAIR, PAIR, head_dim)
        vm = pltpu.VMEM
        dma = pltpu.SemaphoreType.DMA
        whole = pl.BlockSpec(memory_space=pl.ANY)
        act = jax.ShapeDtypeStruct(pairs, BF16)
        vec = jax.ShapeDtypeStruct((n_heads, 1, head_dim), F32)
        tok = (PAIR, SEQ, HEAD)
        tok_t = (PAIR, HEAD, SEQ)
        acc = (HEAD + 8, HALF)
        outs = pl.pallas_call(
            kernel,
            name="rel_attn",
            out_shape=(act, act, act, act,
                       *[jax.ShapeDtypeStruct((2, PART, n_heads, 1, head_dim), F32)] * N_PART),
            in_specs=[pl.BlockSpec(memory_space=pltpu.HBM)] * 7,
            out_specs=[whole] * (4 + N_PART),
            scratch_shapes=[
                vm((4, SUBS, HALF, PAIR, HEAD), BF16), vm((2, SUBS, HALF, PAIR, HEAD), BF16),
                vm((SEQ, 2, PAIR, HEAD), BF16), vm((2, PAIR, HEAD), BF16), vm((2, PAIR, HEAD), BF16),
                vm((SUBS, PAIR, 8, HALF), F32), vm((SUBS, PAIR, 8, HALF), F32), vm((QB, HEAD), F32),
                vm((2, 2) + acc, F32), vm((2,) + acc, F32), vm((2, FIN, 1, HEAD), F32), vm((4, 2) + acc, F32),
                vm((QB, SEQ), F32), vm((QB, SEQ), F32), vm((QB, SEQ), F32),
                vm((QB, SEQ), BF16), vm((QB, SEQ), BF16), vm((QB, SEQ), BF16),
                vm(tok, BF16), vm(tok, BF16), vm(tok, BF16), vm(tok, BF16), vm(tok, BF16),
                vm(tok_t, BF16), vm(tok_t, BF16), vm(tok_t, BF16), vm(tok_t, BF16), vm(tok_t, BF16),
                vm((4, SEQ, HEAD), BF16), vm((4, HEAD, SEQ), BF16),
                vm((PAIR, HEAD, HALF), F32), vm((PAIR, HEAD, HALF), F32), vm((4, PAIR, HALF, HEAD), BF16),
                dma, dma((2, SUBS)), dma, dma, dma((2,)), dma((3,)), dma((4,)), dma((SUBS,)), dma, dma((SUBS,)),
                dma((2,)), dma((2,)), dma((2,)), dma((2,)), dma((2, 3)), dma((2, 3)), dma((2, 2)), dma((2, 2)),
            ],
            compiler_params=pltpu.CompilerParams(collective_id=0, has_side_effects=True, vmem_limit_bytes=36 * 1024 * 1024),
        )(*[pltpu.with_memory_space_constraint(x, pltpu.HBM) for x in (
            query.reshape(pairs), key_in.reshape(pairs), value.reshape(pairs), d_out.reshape(pairs),
            rel_k.reshape(SEQ, N_PAIR, PAIR, head_dim), bias_u.reshape(N_PAIR, PAIR, head_dim), bias_w.reshape(N_PAIR, PAIR, head_dim))])
        o, dq, dk, dv, dr, du, dw = pl.pallas_call(
            writer,
            name="writer",
            out_shape=(act, act, act, act, jax.ShapeDtypeStruct((SEQ, n_heads, 1, head_dim), F32), vec, vec),
            in_specs=[whole] * (4 + N_PART),
            out_specs=[whole] * 7,
            scratch_shapes=[dma((6 + 2 * N_PART,))],
            compiler_params=pltpu.CompilerParams(vmem_limit_bytes=1024 * 1024),
        )(*outs)
        full = query.shape
        return (o.reshape(full), dq.reshape(full), dk.reshape(full), dv.reshape(full),
                du.reshape(bias_u.shape), dw.reshape(bias_w.shape), dr.reshape(rel_k.shape))

    return jax.shard_map(local, mesh=mesh,
                         in_specs=(seq_spec, seq_spec, seq_spec, P(), P(), P(), seq_spec),
                         out_specs=(seq_spec, seq_spec, seq_spec, seq_spec, P(), P(), P()),
                         check_vma=False)
```

```python
import jax
import jax.numpy as jnp
from jax import lax
from jax.experimental import pallas as pl
from jax.experimental.pallas import tpu as pltpu
from jax.sharding import PartitionSpec as P

MESH = pl.DeviceIdType.MESH
BF16, F32 = jnp.bfloat16, jnp.float32
LOG2E = 1.4426950408889634

N_DEV = 16
PLANE = 8
PAIR = 2
N_PAIR = 8
SLOTS = 4
SUBS = 2 * SLOTS
EARLY = 4
ROWS = 64
HALF = PLANE * ROWS
SEQ = 2 * HALF
HEAD = 128
QB = 256
WIN = HALF + QB
N_PART = 6
PART = 86
FIN = N_PART * PART
HOPS = ((1, 2, 4), (1, 2, 4), (2, 1, 4)) * 2
TURNS = ((1, 3, 2), (3, 1, 2))


def dot(lhs, rhs):
    return jnp.dot(lhs, rhs, preferred_element_type=F32)


def flip8(x):
    rows, cols = x.shape
    idx = 7 - lax.broadcasted_iota(jnp.int32, (rows // 8, 8, cols), 1)
    return jnp.take_along_axis(x.reshape(rows // 8, 8, cols), idx, axis=1).reshape(rows, cols)


def eye_rev(dtype):
    total = lax.broadcasted_iota(jnp.int32, (HEAD, HEAD), 0) + lax.broadcasted_iota(jnp.int32, (HEAD, HEAD), 1)
    return jnp.where(total == HEAD - 1, 1.0, 0.0).astype(dtype)


def kernel(q_in, k_in, v_in, g_in, r_in, u_in, w_in,
           o_out, dq_out, dk_out, dv_out, dr0_out, dr1_out, dr2_out, dr3_out, dr4_out, dr5_out,
           buf, rbuf, r_buf, u_buf, w_buf, st_tx, st_rx, st_ref, dr_rx, dr_rz, dr_fin, dr_acc,
           s_ref, e_ref, dp_ref, pb_ref, ds_ref, dd_ref,
           a_s, c_s, g_s, k_s, v_s, at_s, ct_s, gt_s, kt_s, vt_s, rev_s, rt_s, dkt, dvt, stage,
           in_send, in_recv, out_send, out_recv, own_sem, r_sem, up_send, up_recv, st_send, st_recv,
           x_send, x_recv, z_send, z_recv, ring_send, ring_recv, fw_send, fw_recv):
    me = lax.axis_index("cp")
    core = me % 2
    chip = me // 2
    col = chip % 4
    z = chip // 4
    partner = me + 1 - 2 * core
    across = me + PLANE * (1 - 2 * z)
    scale = HEAD ** -0.5

    def wait_for(ref, sem):
        pltpu.make_async_copy(ref, ref, sem).wait()

    tables = [pltpu.make_async_copy(src, dst, r_sem.at[j]) for j, (src, dst) in enumerate(
        ((r_in.at[:, pl.ds(2 * col, 2)], r_buf), (u_in.at[pl.ds(2 * col, 2)], u_buf), (w_in.at[pl.ds(2 * col, 2)], w_buf)))]
    for copy in tables:
        copy.start()

    barrier = pltpu.get_barrier_semaphore()

    for peer in [across] + [me ^ step for step in range(PLANE - 1, 0, -1)]:
        pl.semaphore_signal(barrier, inc=1, device_id=(peer,), device_id_type=MESH)
    pl.semaphore_wait(barrier, PLANE)

    my_rows = pl.ds(pl.multiple_of((me % PLANE) * ROWS, ROWS), ROWS)

    def peers():
        for near_turn, far_turn in zip(*TURNS):
            turn = jnp.where(core == 0, near_turn, far_turn)
            yield me ^ (2 * turn)
            yield me ^ (2 * turn + 1)
        yield partner

    def send_in(ins, sub):
        pair, row = sub // SLOTS, sub % SLOTS
        for first in (0, 2):
            for t in (first, first + 1):
                pltpu.make_async_copy(ins[t].at[core * SLOTS + row, :, 2 * col + pair], buf.at[t, sub, my_rows], in_recv.at[first // 2, sub]).start()
            for peer in peers():
                for t in (first, first + 1):
                    pltpu.make_async_remote_copy(
                        src_ref=ins[t].at[(peer % 2) * SLOTS + row, :, 2 * ((peer // 2) % 4) + pair], dst_ref=buf.at[t, sub, my_rows],
                        send_sem=in_send, recv_sem=in_recv.at[first // 2, sub], device_id=(peer,), device_id_type=MESH).start()

    def send_all(ins):
        def send_sub(sub, carry):
            send_in(ins, sub)
            return carry
        lax.fori_loop(0, SUBS, send_sub, 0)

    @pl.when(z == 0)
    def _():
        send_all((k_in, v_in, q_in, g_in))

    @pl.when(z == 1)
    def _():
        send_all((q_in, g_in, k_in, v_in))

    for copy in tables:
        copy.wait()
    rev = eye_rev(BF16)
    for p in range(2):
        pair_tab = pltpu.einshape("abc->bac", r_buf[:, p])
        for hh in range(PAIR):
            for blk in range(SEQ // HEAD):
                part = pair_tab[hh, SEQ - HEAD * (blk + 1):SEQ - HEAD * blk]
                flipped = dot(rev, part).astype(BF16)
                rev_s[2 * p + hh, HEAD * blk:HEAD * (blk + 1), :] = flipped
                rt_s[2 * p + hh, :, HEAD * blk:HEAD * (blk + 1)] = flipped.T
    dr_acc[...] = jnp.zeros_like(dr_acc)

    acts = (dk_out, dv_out, o_out, dq_out)

    def send_out(sub, which):
        place = (core * SLOTS + sub % SLOTS, slice(None), 2 * col + sub // SLOTS)
        for t in which:
            pltpu.make_async_copy(buf.at[t, sub, my_rows], acts[t].at[place], out_recv).start()
        for peer in peers():
            peer_rows = pl.ds(pl.multiple_of((peer % PLANE) * ROWS, ROWS), ROWS)
            for t in which:
                pltpu.make_async_remote_copy(
                    src_ref=buf.at[t, sub, peer_rows], dst_ref=acts[t].at[place],
                    send_sem=out_send, recv_sem=out_recv, device_id=(peer,), device_id_type=MESH).start()

    def send_up(sub):
        wait_for(buf.at[0:2, sub], in_recv.at[0, sub])
        for j in range(2):
            pltpu.make_async_remote_copy(src_ref=buf.at[j, sub], dst_ref=rbuf.at[j, sub], send_sem=up_send.at[sub % 4], recv_sem=up_recv.at[sub],
                                         device_id=(across,), device_id_type=MESH).start()

    def unpack(ref, j, sub):
        return pltpu.einshape("abc->bac", ref[j, sub])

    def load_rows(q_ref, q_j, g_ref, g_j, sub, start, turned):
        rows = slice(start, start + HALF)
        p = sub // SLOTS
        q2 = unpack(q_ref, q_j, sub)
        u = u_buf[p].astype(F32)
        w = w_buf[p].astype(F32)
        for hh in range(PAIR):
            q32 = q2[hh].astype(F32)
            a = (q32 + u[hh:hh + 1]).astype(BF16)
            c = (q32 + w[hh:hh + 1]).astype(BF16)
            a_s[hh, rows, :] = a
            c_s[hh, rows, :] = c
            at_s[hh, :, rows] = a.T
            if turned:
                ct_s[hh, :, rows] = flip8(c.astype(F32)).astype(BF16).T
        g2 = unpack(g_ref, g_j, sub)
        g_s[:, rows, :] = g2
        for hh in range(PAIR):
            gt_s[hh, :, rows] = g2[hh].T

    def load_keys(k_ref, k_j, v_ref, v_j, sub, start):
        rows = slice(start, start + HALF)
        k2 = unpack(k_ref, k_j, sub)
        v2 = unpack(v_ref, v_j, sub)
        k_s[:, rows, :] = k2
        v_s[:, rows, :] = v2
        for hh in range(PAIR):
            kt_s[hh, :, rows] = k2[hh].T
            vt_s[hh, :, rows] = v2[hh].T

    def row_block(hh, head, start, i0, lo, fresh, stats):
        width = i0 + QB
        rows = slice(start, start + QB)
        s_ref[:, :width] = dot(a_s[hh, rows, :], kt_s[hh, :, :width])
        e_ref[:, :width] = dot(c_s[hh, rows, :], rt_s[head, :, SEQ - width:])
        dp_ref[:, :width] = dot(g_s[hh, rows, :], vt_s[hh, :, :width])
        for r0 in range(0, QB, 16):
            group = slice(r0, r0 + 16)
            rel = pltpu.roll(e_ref[group, :width], i0 + 1 + r0, 1, stride=1, stride_axis=0)
            s = s_ref[group, :width] + rel
            ahead = lax.broadcasted_iota(jnp.int32, (16, width), 1) - lax.broadcasted_iota(jnp.int32, (16, width), 0)
            s = jnp.where(ahead <= i0 + r0, s, -jnp.inf)
            top = jnp.max(s, axis=1, keepdims=True)
            p = jnp.exp2((s - top) * (scale * LOG2E))
            total = jnp.sum(p, axis=1, keepdims=True)
            p = p * (1.0 / total)
            pb_ref[group, :width] = p.astype(BF16)
            dp = dp_ref[group, :width]
            row_dot = jnp.sum(p * dp, axis=1, keepdims=True)
            ds = (p * (dp - row_dot) * scale).astype(BF16)
            ds_ref[group, :width] = ds
            flipped = flip8(ds.astype(F32))
            half = [pltpu.roll(flipped[8 * j:8 * j + 8], QB - 8 - r0 - 8 * j, 1, stride=1, stride_axis=0) for j in range(2)]
            dd_ref[group, :width] = jnp.concatenate(half, axis=0).astype(BF16)
            if stats:
                lane = lax.broadcasted_iota(jnp.int32, (16, HEAD), 1)
                st_ref[group, :] = jnp.where(lane == 0, top * (scale * LOG2E) + jnp.log2(total), row_dot)
        pb = pb_ref[:, :width]
        ds = ds_ref[:, :width]
        dd = dd_ref[:, :width]
        stage[0, hh, rows, :] = dot(pb, v_s[hh, :width, :]).astype(BF16)
        dqc = dot(ds, k_s[hh, :width, :])
        dqr = flip8(dot(dd, rev_s[head, SEQ - width:, :]))
        stage[1, hh, rows, :] = (dqc + dqr).astype(BF16)
        dr_acc[head, 1, HEAD:HEAD + 1, HALF - HEAD:] += jnp.sum(dqc, axis=0, keepdims=True)
        dr_acc[head, 1, HEAD + 1:HEAD + 2, HALF - HEAD:] += jnp.sum(dqr, axis=0, keepdims=True)
        dk_new = dot(at_s[hh, :, rows], ds_ref[:, lo:width])
        dv_new = dot(gt_s[hh, :, rows], pb_ref[:, lo:width])
        if fresh:
            dkt[hh] = dk_new
            dvt[hh] = dv_new
        else:
            dkt[hh, :, :width - lo] += dk_new
            dvt[hh, :, :width - lo] += dv_new
        dr_new = dot(ct_s[hh, :, rows], dd)
        if width > HALF:
            dr_acc[head, 0, :HEAD, SEQ - width:] += dr_new[:, :width - HALF]
            dr_acc[head, 1, :HEAD, :] += dr_new[:, width - HALF:]
        else:
            dr_acc[head, 1, :HEAD, HALF - width:] += dr_new

    def col_block(hh, head, sub, i0):
        rows = slice(i0, i0 + QB)
        first = WIN - i0
        s_ref[:, :HALF] = dot(a_s[hh, rows, :], kt_s[hh, :, :HALF])
        e_ref[:, :WIN] = dot(c_s[hh, rows, :], rt_s[head, :, first:first + WIN])
        dp_ref[:, :HALF] = dot(g_s[hh, rows, :], vt_s[hh, :, :HALF])
        st_ref[:, :8] = st_rx[sub, hh, :, i0 - HALF:i0 - HALF + QB].T
        for r0 in range(0, QB, 16):
            group = slice(r0, r0 + 16)
            rel = pltpu.roll(e_ref[group, :WIN], HALF + 1 + r0, 1, stride=1, stride_axis=0)[:, :HALF]
            log_sum = st_ref[group, 0:1]
            row_dot = st_ref[group, 1:2]
            p = jnp.exp2((s_ref[group, :HALF] + rel) * (scale * LOG2E) - log_sum)
            pb_ref[group, :HALF] = p.astype(BF16)
            ds_ref[group, :HALF] = (p * (dp_ref[group, :HALF] - row_dot) * scale).astype(BF16)
        dkt[hh] += dot(at_s[hh, :, rows], ds_ref[:, :HALF])
        dvt[hh] += dot(gt_s[hh, :, rows], pb_ref[:, :HALF])

    def store_rows(sub):
        for t in range(2):
            buf[2 + t, sub] = pltpu.einshape("abc->bac", stage[t])

    def store_keys(sub):
        for hh in range(PAIR):
            stage[2, hh] = dkt[hh].astype(BF16).T
            stage[3, hh] = dvt[hh].astype(BF16).T
        for t in range(2):
            buf[t, sub] = pltpu.einshape("abc->bac", stage[2 + t])

    def wait_up(sub):
        wait_for(rbuf.at[:, sub], up_recv.at[sub])
        wait_for(rbuf.at[:, sub], up_send.at[sub % 4])

    def wait_in(sub):
        wait_for(buf.at[2:4, sub], in_recv.at[1, sub])

    def lower_rows(sub):
        wait_in(sub)
        load_rows(buf, 2, buf, 3, sub, 0, True)

    def lower_own(sub):
        load_keys(buf, 0, buf, 1, sub, 0)

        def own(hh, carry):
            head = 2 * (sub // SLOTS) + hh
            row_block(hh, head, QB, QB, 0, True, False)
            row_block(hh, head, 0, 0, 0, False, False)
            return carry

        lax.fori_loop(0, PAIR, own, 0)
        store_rows(sub)

    def lower_theirs(sub):
        wait_up(sub)
        load_rows(rbuf, 0, rbuf, 1, sub, HALF, False)
        wait_for(st_rx.at[sub], st_recv.at[sub])

        def theirs(hh, carry):
            head = 2 * (sub // SLOTS) + hh
            col_block(hh, head, sub, HALF)
            col_block(hh, head, sub, HALF + QB)
            return carry

        lax.fori_loop(0, PAIR, theirs, 0)
        store_keys(sub)

    def upper_own(sub):
        wait_in(sub)
        wait_up(sub)
        load_rows(buf, 0, buf, 1, sub, 0, True)
        load_keys(rbuf, 0, rbuf, 1, sub, 0)
        load_keys(buf, 2, buf, 3, sub, HALF)

        def own(hh, carry):
            head = 2 * (sub // SLOTS) + hh
            for blk in (1, 0):
                row_block(hh, head, QB * blk, HALF + QB * blk, HALF, blk == 1, True)
                st_tx[sub, hh, :, QB * blk:QB * (blk + 1)] = st_ref[...].T[:8]
            pltpu.make_async_remote_copy(src_ref=st_tx.at[sub, hh], dst_ref=st_rx.at[sub, hh], send_sem=st_send, recv_sem=st_recv.at[sub],
                                         device_id=(across,), device_id_type=MESH).start()
            return carry

        lax.fori_loop(0, PAIR, own, 0)
        store_rows(sub)
        store_keys(sub)

    side = 1 - core
    parts = (dr0_out, dr1_out, dr2_out, dr3_out, dr4_out, dr5_out)

    def swap_start(p):
        for n in range(2):
            pltpu.make_async_remote_copy(src_ref=dr_acc.at[2 * p + n, side], dst_ref=dr_rx.at[p, n], send_sem=x_send.at[p], recv_sem=x_recv.at[p],
                                         device_id=(partner,), device_id_type=MESH).start()

    def swap_add(p):
        wait_for(dr_rx.at[p], x_recv.at[p])
        for n in range(2):
            dr_rx[p, n] = dr_rx[p, n] + dr_acc[2 * p + n, core]

    def cross_start(p):
        pltpu.make_async_remote_copy(src_ref=dr_rx.at[p, 1 - z], dst_ref=dr_rz.at[p], send_sem=z_send.at[p], recv_sem=z_recv.at[p],
                                     device_id=(across,), device_id_type=MESH).start()

    def head_of(p, bits):
        other = chip ^ bits
        return 4 * (other % 4) + 2 * p + other // 4

    def block(p, m, bits):
        if bits == 0:
            return dr_fin.at[p, PART * m:PART * (m + 1)]
        return parts[m].at[side, :, head_of(p, bits)]

    def forward(p, m, bits):
        pltpu.make_async_remote_copy(src_ref=block(p, m, bits), dst_ref=parts[m].at[side, :, head_of(p, bits)], send_sem=fw_send.at[p, m // 3],
                                     recv_sem=fw_recv.at[p, m // 3], device_id=(partner,), device_id_type=MESH).start()

    def held(m, hop):
        have = [0]
        for bit in HOPS[m][:hop]:
            have = have + [bits ^ bit for bits in have]
        return have

    def blocks(count):
        return parts[0].at[:, :, :count // 2]

    def hop_start(p, hop):
        for m in range(N_PART):
            for bits in held(m, hop):
                pltpu.make_async_remote_copy(
                    src_ref=block(p, m, bits), dst_ref=parts[m].at[side, :, head_of(p, bits)], send_sem=ring_send.at[p, hop],
                    recv_sem=ring_recv.at[p, hop], device_id=(me ^ (2 * HOPS[m][hop]),), device_id_type=MESH).start()

    def hop_wait(p, hop):
        wait_for(blocks(N_PART << hop), ring_recv.at[p, hop])
        for m in range(N_PART):
            have = held(m, hop + 1)
            for bits in have[len(have) // 2:]:
                forward(p, m, bits)

    def cross_finish(p):
        wait_for(dr_rz.at[p], z_recv.at[p])
        total = dr_rx[p, z] + dr_rz[p]
        rev32 = eye_rev(F32)
        for m in range(HALF // HEAD):
            part = total[:HEAD, HALF - HEAD * (m + 1):HALF - HEAD * m]
            turned = lax.dot_general(rev32, part, (((1,), (1,)), ((), ())), precision=lax.Precision.HIGHEST, preferred_element_type=F32)
            dr_fin[p, HEAD * m:HEAD * (m + 1)] = turned.reshape(HEAD, 1, HEAD)
        dr_fin[p, HALF] = total[HEAD:HEAD + 1, HALF - HEAD:]
        dr_fin[p, HALF + 1] = total[HEAD + 1:HEAD + 2, HALF - HEAD:]
        dr_fin[p, HALF + 2:] = jnp.zeros((FIN - HALF - 2, 1, HEAD), F32)
        hop_start(p, 0)
        for m in range(N_PART):
            pltpu.make_async_copy(block(p, m, 0), parts[m].at[side, :, head_of(p, 0)], own_sem.at[p]).start()
            forward(p, m, 0)

    send_up(0)

    def sub_body(sub, carry):
        @pl.when(sub < SUBS - 1)
        def _():
            send_up(sub + 1)

        @pl.when(sub == SLOTS)
        def _():
            swap_start(0)

        @pl.when(sub == SUBS - 1)
        def _():
            swap_add(0)
            cross_start(0)

        @pl.when(sub == SUBS)
        def _():
            swap_start(1)
            cross_finish(0)

        @pl.when((z == 0) & (sub < SUBS))
        def _():
            lower_rows(sub)

        @pl.when((z == 0) & (sub > 0))
        def _():
            lower_theirs(sub - 1)

        @pl.when((z == 0) & (sub < SUBS))
        def _():
            lower_own(sub)

        @pl.when((z == 1) & (sub < SUBS))
        def _():
            upper_own(sub)

        @pl.when(sub < EARLY)
        def _():
            send_out(sub, (2, 3))

        @pl.when((sub > 0) & (sub <= EARLY))
        def _():
            send_out(sub - 1, (0, 1))
        return carry

    lax.fori_loop(0, SUBS + 1, sub_body, 0)

    swap_add(1)
    cross_start(1)
    cross_finish(1)
    for p in range(2):
        hop_wait(p, 0)
        hop_start(p, 1)

    def send_late(sub, carry):
        send_out(sub, range(4))
        return carry

    lax.fori_loop(EARLY, EARLY + 2, send_late, 0)
    for p in range(2):
        hop_wait(p, 1)
        hop_start(p, 2)
    lax.fori_loop(EARLY + 2, SUBS, send_late, 0)
    for p in range(2):
        hop_wait(p, 2)

    wait_for(buf, out_recv)
    wait_for(buf.at[:, :, :HALF - ROWS], in_send)
    wait_for(buf.at[:, :, :HALF - ROWS], out_send)

    @pl.when(z == 1)
    def _():
        wait_for(st_tx, st_send)

    for p in range(2):
        wait_for(dr_rx.at[p], x_send.at[p])
        wait_for(dr_rz.at[p], z_send.at[p])
        wait_for(blocks(N_PART), own_sem.at[p])
        for hop in range(3):
            wait_for(blocks(N_PART << hop), ring_send.at[p, hop])
        for n in range(2):
            wait_for(blocks(N_PART // 2 * N_PAIR), fw_send.at[p, n])
            wait_for(blocks(N_PART // 2 * N_PAIR), fw_recv.at[p, n])


def writer(*refs):
    ins, (o, dq, dk, dv, dr, du, dw, sem) = refs[:4 + N_PART], refs[4 + N_PART:]
    pairs = list(zip(ins[:4], (o, dq, dk, dv)))
    for m, part in enumerate(ins[4:]):
        rows = min(PART, HALF - PART * m)
        for side in range(2):
            start = HALF * side + PART * m
            pairs.append((part.at[side, :rows], dr.at[start:start + rows]))
    last = HALF - PART * (N_PART - 1)
    pairs += [(ins[-1].at[0, last], du), (ins[-1].at[0, last + 1], dw)]
    copies = [pltpu.make_async_copy(src, dst, sem.at[j]) for j, (src, dst) in enumerate(pairs)]
    for copy in copies:
        copy.start()
    for copy in copies:
        copy.wait()


def solution(mesh):
    seq_spec = P(None, "cp", None, None)

    def local(query, key_in, value, bias_u, bias_w, rel_k, d_out):
        n_batch, rows, n_heads, head_dim = query.shape
        pairs = (n_batch, rows, N_PAIR, PAIR, head_dim)
        vm = pltpu.VMEM
        dma = pltpu.SemaphoreType.DMA
        whole = pl.BlockSpec(memory_space=pl.ANY)
        act = jax.ShapeDtypeStruct(pairs, BF16)
        vec = jax.ShapeDtypeStruct((n_heads, 1, head_dim), F32)
        tok = (PAIR, SEQ, HEAD)
        tok_t = (PAIR, HEAD, SEQ)
        acc = (HEAD + 8, HALF)
        outs = pl.pallas_call(
            kernel,
            name="rel_attn",
            out_shape=(act, act, act, act,
                       *[jax.ShapeDtypeStruct((2, PART, n_heads, 1, head_dim), F32)] * N_PART),
            in_specs=[pl.BlockSpec(memory_space=pltpu.HBM)] * 7,
            out_specs=[whole] * (4 + N_PART),
            scratch_shapes=[
                vm((4, SUBS, HALF, PAIR, HEAD), BF16), vm((2, SUBS, HALF, PAIR, HEAD), BF16),
                vm((SEQ, 2, PAIR, HEAD), BF16), vm((2, PAIR, HEAD), BF16), vm((2, PAIR, HEAD), BF16),
                vm((SUBS, PAIR, 8, HALF), F32), vm((SUBS, PAIR, 8, HALF), F32), vm((QB, HEAD), F32),
                vm((2, 2) + acc, F32), vm((2,) + acc, F32), vm((2, FIN, 1, HEAD), F32), vm((4, 2) + acc, F32),
                vm((QB, SEQ), F32), vm((QB, SEQ), F32), vm((QB, SEQ), F32),
                vm((QB, SEQ), BF16), vm((QB, SEQ), BF16), vm((QB, SEQ), BF16),
                vm(tok, BF16), vm(tok, BF16), vm(tok, BF16), vm(tok, BF16), vm(tok, BF16),
                vm(tok_t, BF16), vm(tok_t, BF16), vm(tok_t, BF16), vm(tok_t, BF16), vm(tok_t, BF16),
                vm((4, SEQ, HEAD), BF16), vm((4, HEAD, SEQ), BF16),
                vm((PAIR, HEAD, HALF), F32), vm((PAIR, HEAD, HALF), F32), vm((4, PAIR, HALF, HEAD), BF16),
                dma, dma((2, SUBS)), dma, dma, dma((2,)), dma((3,)), dma((4,)), dma((SUBS,)), dma, dma((SUBS,)),
                dma((2,)), dma((2,)), dma((2,)), dma((2,)), dma((2, 3)), dma((2, 3)), dma((2, 2)), dma((2, 2)),
            ],
            compiler_params=pltpu.CompilerParams(collective_id=0, has_side_effects=True, vmem_limit_bytes=36 * 1024 * 1024),
        )(*[pltpu.with_memory_space_constraint(x, pltpu.HBM) for x in (
            query.reshape(pairs), key_in.reshape(pairs), value.reshape(pairs), d_out.reshape(pairs),
            rel_k.reshape(SEQ, N_PAIR, PAIR, head_dim), bias_u.reshape(N_PAIR, PAIR, head_dim), bias_w.reshape(N_PAIR, PAIR, head_dim))])
        o, dq, dk, dv, dr, du, dw = pl.pallas_call(
            writer,
            name="writer",
            out_shape=(act, act, act, act, jax.ShapeDtypeStruct((SEQ, n_heads, 1, head_dim), F32), vec, vec),
            in_specs=[whole] * (4 + N_PART),
            out_specs=[whole] * 7,
            scratch_shapes=[dma((6 + 2 * N_PART,))],
            compiler_params=pltpu.CompilerParams(vmem_limit_bytes=1024 * 1024),
        )(*outs)
        full = query.shape
        return (o.reshape(full), dq.reshape(full), dk.reshape(full), dv.reshape(full),
                du.reshape(bias_u.shape), dw.reshape(bias_w.shape), dr.reshape(rel_k.shape))

    return jax.shard_map(local, mesh=mesh,
                         in_specs=(seq_spec, seq_spec, seq_spec, P(), P(), P(), seq_spec),
                         out_specs=(seq_spec, seq_spec, seq_spec, seq_spec, P(), P(), P()),
                         check_vma=False)
```

```python
import jax
import jax.numpy as jnp
from jax import lax
from jax.experimental import pallas as pl
from jax.experimental.pallas import tpu as pltpu
from jax.sharding import PartitionSpec as P

MESH = pl.DeviceIdType.MESH
BF16, F32 = jnp.bfloat16, jnp.float32
LOG2E = 1.4426950408889634

N_DEV = 16
PLANE = 8
PAIR = 2
N_PAIR = 8
SLOTS = 4
SUBS = 2 * SLOTS
EARLY = 3
ROWS = 64
HALF = PLANE * ROWS
SEQ = 2 * HALF
HEAD = 128
QB = 256
WIN = HALF + QB
N_PART = 6
PART = 86
FIN = N_PART * PART
HOPS = ((1, 2, 4), (2, 1, 4)) * 3
TURNS = ((1, 3, 2), (3, 1, 2))


def dot(lhs, rhs):
    return jnp.dot(lhs, rhs, preferred_element_type=F32)


def flip8(x):
    rows, cols = x.shape
    idx = 7 - lax.broadcasted_iota(jnp.int32, (rows // 8, 8, cols), 1)
    return jnp.take_along_axis(x.reshape(rows // 8, 8, cols), idx, axis=1).reshape(rows, cols)


def eye_rev(dtype):
    total = lax.broadcasted_iota(jnp.int32, (HEAD, HEAD), 0) + lax.broadcasted_iota(jnp.int32, (HEAD, HEAD), 1)
    return jnp.where(total == HEAD - 1, 1.0, 0.0).astype(dtype)


def kernel(q_in, k_in, v_in, g_in, r_in, u_in, w_in,
           o_out, dq_out, dk_out, dv_out, dr0_out, dr1_out, dr2_out, dr3_out, dr4_out, dr5_out,
           buf, rbuf, r_buf, u_buf, w_buf, st_tx, st_rx, st_ref, dr_rx, dr_rz, dr_fin, dr_acc,
           s_ref, e_ref, dp_ref, pb_ref, ds_ref, dd_ref,
           a_s, c_s, g_s, k_s, v_s, at_s, ct_s, gt_s, kt_s, vt_s, rev_s, rt_s, dkt, dvt, stage,
           in_send, in_recv, out_send, out_recv, own_sem, r_sem, up_send, up_recv, st_send, st_recv,
           x_send, x_recv, z_send, z_recv, ring_send, ring_recv, fw_send, fw_recv):
    me = lax.axis_index("cp")
    core = me % 2
    chip = me // 2
    col = chip % 4
    z = chip // 4
    partner = me + 1 - 2 * core
    across = me + PLANE * (1 - 2 * z)
    scale = HEAD ** -0.5

    def wait_for(ref, sem):
        pltpu.make_async_copy(ref, ref, sem).wait()

    tables = [pltpu.make_async_copy(src, dst, r_sem.at[j]) for j, (src, dst) in enumerate(
        ((r_in.at[:, pl.ds(2 * col, 2)], r_buf), (u_in.at[pl.ds(2 * col, 2)], u_buf), (w_in.at[pl.ds(2 * col, 2)], w_buf)))]
    for copy in tables:
        copy.start()

    barrier = pltpu.get_barrier_semaphore()

    for peer in [across] + [me ^ step for step in range(PLANE - 1, 0, -1)]:
        pl.semaphore_signal(barrier, inc=1, device_id=(peer,), device_id_type=MESH)
    pl.semaphore_wait(barrier, PLANE)

    my_rows = pl.ds(pl.multiple_of((me % PLANE) * ROWS, ROWS), ROWS)

    def peers():
        for near_turn, far_turn in zip(*TURNS):
            turn = jnp.where(core == 0, near_turn, far_turn)
            yield me ^ (2 * turn)
            yield me ^ (2 * turn + 1)
        yield partner

    def send_in(ins, sub):
        pair, row = sub // SLOTS, sub % SLOTS
        for first in (0, 2):
            for t in (first, first + 1):
                pltpu.make_async_copy(ins[t].at[core * SLOTS + row, :, 2 * col + pair], buf.at[t, sub, my_rows], in_recv.at[first // 2, sub]).start()
            for peer in peers():
                for t in (first, first + 1):
                    pltpu.make_async_remote_copy(
                        src_ref=ins[t].at[(peer % 2) * SLOTS + row, :, 2 * ((peer // 2) % 4) + pair], dst_ref=buf.at[t, sub, my_rows],
                        send_sem=in_send, recv_sem=in_recv.at[first // 2, sub], device_id=(peer,), device_id_type=MESH).start()

    def send_all(ins):
        def send_sub(sub, carry):
            send_in(ins, sub)
            return carry
        lax.fori_loop(0, SUBS, send_sub, 0)

    @pl.when(z == 0)
    def _():
        send_all((k_in, v_in, q_in, g_in))

    @pl.when(z == 1)
    def _():
        send_all((q_in, g_in, k_in, v_in))

    for copy in tables:
        copy.wait()
    rev = eye_rev(BF16)
    for p in range(2):
        pair_tab = pltpu.einshape("abc->bac", r_buf[:, p])
        for hh in range(PAIR):
            for blk in range(SEQ // HEAD):
                part = pair_tab[hh, SEQ - HEAD * (blk + 1):SEQ - HEAD * blk]
                flipped = dot(rev, part).astype(BF16)
                rev_s[2 * p + hh, HEAD * blk:HEAD * (blk + 1), :] = flipped
                rt_s[2 * p + hh, :, HEAD * blk:HEAD * (blk + 1)] = flipped.T
    dr_acc[...] = jnp.zeros_like(dr_acc)

    acts = (dk_out, dv_out, o_out, dq_out)

    def send_out(sub, which):
        place = (core * SLOTS + sub % SLOTS, slice(None), 2 * col + sub // SLOTS)
        for t in which:
            pltpu.make_async_copy(buf.at[t, sub, my_rows], acts[t].at[place], out_recv).start()
        for peer in peers():
            peer_rows = pl.ds(pl.multiple_of((peer % PLANE) * ROWS, ROWS), ROWS)
            for t in which:
                pltpu.make_async_remote_copy(
                    src_ref=buf.at[t, sub, peer_rows], dst_ref=acts[t].at[place],
                    send_sem=out_send, recv_sem=out_recv, device_id=(peer,), device_id_type=MESH).start()

    def send_up(sub):
        wait_for(buf.at[0:2, sub], in_recv.at[0, sub])
        for j in range(2):
            pltpu.make_async_remote_copy(src_ref=buf.at[j, sub], dst_ref=rbuf.at[j, sub], send_sem=up_send.at[sub % 4], recv_sem=up_recv.at[sub],
                                         device_id=(across,), device_id_type=MESH).start()

    def unpack(ref, j, sub):
        return pltpu.einshape("abc->bac", ref[j, sub])

    def load_rows(q_ref, q_j, g_ref, g_j, sub, start, turned):
        rows = slice(start, start + HALF)
        p = sub // SLOTS
        q2 = unpack(q_ref, q_j, sub)
        u = u_buf[p].astype(F32)
        w = w_buf[p].astype(F32)
        for hh in range(PAIR):
            q32 = q2[hh].astype(F32)
            a = (q32 + u[hh:hh + 1]).astype(BF16)
            c = (q32 + w[hh:hh + 1]).astype(BF16)
            a_s[hh, rows, :] = a
            c_s[hh, rows, :] = c
            at_s[hh, :, rows] = a.T
            if turned:
                ct_s[hh, :, rows] = flip8(c.astype(F32)).astype(BF16).T
        g2 = unpack(g_ref, g_j, sub)
        g_s[:, rows, :] = g2
        for hh in range(PAIR):
            gt_s[hh, :, rows] = g2[hh].T

    def load_keys(k_ref, k_j, v_ref, v_j, sub, start):
        rows = slice(start, start + HALF)
        k2 = unpack(k_ref, k_j, sub)
        v2 = unpack(v_ref, v_j, sub)
        k_s[:, rows, :] = k2
        v_s[:, rows, :] = v2
        for hh in range(PAIR):
            kt_s[hh, :, rows] = k2[hh].T
            vt_s[hh, :, rows] = v2[hh].T

    def row_block(hh, head, start, i0, lo, fresh, stats):
        width = i0 + QB
        rows = slice(start, start + QB)
        s_ref[:, :width] = dot(a_s[hh, rows, :], kt_s[hh, :, :width])
        e_ref[:, :width] = dot(c_s[hh, rows, :], rt_s[head, :, SEQ - width:])
        dp_ref[:, :width] = dot(g_s[hh, rows, :], vt_s[hh, :, :width])
        for r0 in range(0, QB, 16):
            group = slice(r0, r0 + 16)
            rel = pltpu.roll(e_ref[group, :width], i0 + 1 + r0, 1, stride=1, stride_axis=0)
            s = s_ref[group, :width] + rel
            ahead = lax.broadcasted_iota(jnp.int32, (16, width), 1) - lax.broadcasted_iota(jnp.int32, (16, width), 0)
            s = jnp.where(ahead <= i0 + r0, s, -jnp.inf)
            top = jnp.max(s, axis=1, keepdims=True)
            p = jnp.exp2((s - top) * (scale * LOG2E))
            total = jnp.sum(p, axis=1, keepdims=True)
            p = p * (1.0 / total)
            pb_ref[group, :width] = p.astype(BF16)
            dp = dp_ref[group, :width]
            row_dot = jnp.sum(p * dp, axis=1, keepdims=True)
            ds = (p * (dp - row_dot) * scale).astype(BF16)
            ds_ref[group, :width] = ds
            flipped = flip8(ds.astype(F32))
            half = [pltpu.roll(flipped[8 * j:8 * j + 8], QB - 8 - r0 - 8 * j, 1, stride=1, stride_axis=0) for j in range(2)]
            dd_ref[group, :width] = jnp.concatenate(half, axis=0).astype(BF16)
            if stats:
                lane = lax.broadcasted_iota(jnp.int32, (16, HEAD), 1)
                st_ref[group, :] = jnp.where(lane == 0, top * (scale * LOG2E) + jnp.log2(total), row_dot)
        pb = pb_ref[:, :width]
        ds = ds_ref[:, :width]
        dd = dd_ref[:, :width]
        stage[0, hh, rows, :] = dot(pb, v_s[hh, :width, :]).astype(BF16)
        dqc = dot(ds, k_s[hh, :width, :])
        dqr = flip8(dot(dd, rev_s[head, SEQ - width:, :]))
        stage[1, hh, rows, :] = (dqc + dqr).astype(BF16)
        dr_acc[head, 1, HEAD:HEAD + 1, HALF - HEAD:] += jnp.sum(dqc, axis=0, keepdims=True)
        dr_acc[head, 1, HEAD + 1:HEAD + 2, HALF - HEAD:] += jnp.sum(dqr, axis=0, keepdims=True)
        dk_new = dot(at_s[hh, :, rows], ds_ref[:, lo:width])
        dv_new = dot(gt_s[hh, :, rows], pb_ref[:, lo:width])
        if fresh:
            dkt[hh] = dk_new
            dvt[hh] = dv_new
        else:
            dkt[hh, :, :width - lo] += dk_new
            dvt[hh, :, :width - lo] += dv_new
        dr_new = dot(ct_s[hh, :, rows], dd)
        if width > HALF:
            dr_acc[head, 0, :HEAD, SEQ - width:] += dr_new[:, :width - HALF]
            dr_acc[head, 1, :HEAD, :] += dr_new[:, width - HALF:]
        else:
            dr_acc[head, 1, :HEAD, HALF - width:] += dr_new

    def col_block(hh, head, sub, i0):
        rows = slice(i0, i0 + QB)
        first = WIN - i0
        s_ref[:, :HALF] = dot(a_s[hh, rows, :], kt_s[hh, :, :HALF])
        e_ref[:, :WIN] = dot(c_s[hh, rows, :], rt_s[head, :, first:first + WIN])
        dp_ref[:, :HALF] = dot(g_s[hh, rows, :], vt_s[hh, :, :HALF])
        st_ref[:, :8] = st_rx[sub, hh, :, i0 - HALF:i0 - HALF + QB].T
        for r0 in range(0, QB, 16):
            group = slice(r0, r0 + 16)
            rel = pltpu.roll(e_ref[group, :WIN], HALF + 1 + r0, 1, stride=1, stride_axis=0)[:, :HALF]
            log_sum = st_ref[group, 0:1]
            row_dot = st_ref[group, 1:2]
            p = jnp.exp2((s_ref[group, :HALF] + rel) * (scale * LOG2E) - log_sum)
            pb_ref[group, :HALF] = p.astype(BF16)
            ds_ref[group, :HALF] = (p * (dp_ref[group, :HALF] - row_dot) * scale).astype(BF16)
        dkt[hh] += dot(at_s[hh, :, rows], ds_ref[:, :HALF])
        dvt[hh] += dot(gt_s[hh, :, rows], pb_ref[:, :HALF])

    def store_rows(sub):
        for t in range(2):
            buf[2 + t, sub] = pltpu.einshape("abc->bac", stage[t])

    def store_keys(sub):
        for hh in range(PAIR):
            stage[2, hh] = dkt[hh].astype(BF16).T
            stage[3, hh] = dvt[hh].astype(BF16).T
        for t in range(2):
            buf[t, sub] = pltpu.einshape("abc->bac", stage[2 + t])

    def wait_up(sub):
        wait_for(rbuf.at[:, sub], up_recv.at[sub])
        wait_for(rbuf.at[:, sub], up_send.at[sub % 4])

    def wait_in(sub):
        wait_for(buf.at[2:4, sub], in_recv.at[1, sub])

    def lower_rows(sub):
        wait_in(sub)
        load_rows(buf, 2, buf, 3, sub, 0, True)

    def lower_own(sub):
        load_keys(buf, 0, buf, 1, sub, 0)

        def own(hh, carry):
            head = 2 * (sub // SLOTS) + hh
            row_block(hh, head, QB, QB, 0, True, False)
            row_block(hh, head, 0, 0, 0, False, False)
            return carry

        lax.fori_loop(0, PAIR, own, 0)
        store_rows(sub)

    def lower_theirs(sub):
        wait_up(sub)
        load_rows(rbuf, 0, rbuf, 1, sub, HALF, False)
        wait_for(st_rx.at[sub], st_recv.at[sub])

        def theirs(hh, carry):
            head = 2 * (sub // SLOTS) + hh
            col_block(hh, head, sub, HALF)
            col_block(hh, head, sub, HALF + QB)
            return carry

        lax.fori_loop(0, PAIR, theirs, 0)
        store_keys(sub)

    def upper_own(sub):
        wait_in(sub)
        wait_up(sub)
        load_rows(buf, 0, buf, 1, sub, 0, True)
        load_keys(rbuf, 0, rbuf, 1, sub, 0)
        load_keys(buf, 2, buf, 3, sub, HALF)

        def own(hh, carry):
            head = 2 * (sub // SLOTS) + hh
            for blk in (1, 0):
                row_block(hh, head, QB * blk, HALF + QB * blk, HALF, blk == 1, True)
                st_tx[sub, hh, :, QB * blk:QB * (blk + 1)] = st_ref[...].T[:8]
            pltpu.make_async_remote_copy(src_ref=st_tx.at[sub, hh], dst_ref=st_rx.at[sub, hh], send_sem=st_send, recv_sem=st_recv.at[sub],
                                         device_id=(across,), device_id_type=MESH).start()
            return carry

        lax.fori_loop(0, PAIR, own, 0)
        store_rows(sub)
        store_keys(sub)

    side = 1 - core
    parts = (dr0_out, dr1_out, dr2_out, dr3_out, dr4_out, dr5_out)

    def swap_start(p):
        for n in range(2):
            pltpu.make_async_remote_copy(src_ref=dr_acc.at[2 * p + n, side], dst_ref=dr_rx.at[p, n], send_sem=x_send.at[p], recv_sem=x_recv.at[p],
                                         device_id=(partner,), device_id_type=MESH).start()

    def swap_add(p):
        wait_for(dr_rx.at[p], x_recv.at[p])
        for n in range(2):
            dr_rx[p, n] = dr_rx[p, n] + dr_acc[2 * p + n, core]

    def cross_start(p):
        pltpu.make_async_remote_copy(src_ref=dr_rx.at[p, 1 - z], dst_ref=dr_rz.at[p], send_sem=z_send.at[p], recv_sem=z_recv.at[p],
                                     device_id=(across,), device_id_type=MESH).start()

    def head_of(p, bits):
        other = chip ^ bits
        return 4 * (other % 4) + 2 * p + other // 4

    def block(p, m, bits):
        if bits == 0:
            return dr_fin.at[p, PART * m:PART * (m + 1)]
        return parts[m].at[side, :, head_of(p, bits)]

    def forward(p, m, bits):
        pltpu.make_async_remote_copy(src_ref=block(p, m, bits), dst_ref=parts[m].at[side, :, head_of(p, bits)], send_sem=fw_send.at[p, m // 3],
                                     recv_sem=fw_recv.at[p, m // 3], device_id=(partner,), device_id_type=MESH).start()

    def held(m, hop):
        have = [0]
        for bit in HOPS[m][:hop]:
            have = have + [bits ^ bit for bits in have]
        return have

    def blocks(count):
        return parts[0].at[:, :, :count // 2]

    def hop_start(p, hop):
        for m in range(N_PART):
            for bits in held(m, hop):
                pltpu.make_async_remote_copy(
                    src_ref=block(p, m, bits), dst_ref=parts[m].at[side, :, head_of(p, bits)], send_sem=ring_send.at[p, hop],
                    recv_sem=ring_recv.at[p, hop], device_id=(me ^ (2 * HOPS[m][hop]),), device_id_type=MESH).start()

    def hop_wait(p, hop):
        wait_for(blocks(N_PART << hop), ring_recv.at[p, hop])
        for m in range(N_PART):
            have = held(m, hop + 1)
            for bits in have[len(have) // 2:]:
                forward(p, m, bits)

    def cross_finish(p):
        wait_for(dr_rz.at[p], z_recv.at[p])
        total = dr_rx[p, z] + dr_rz[p]
        rev32 = eye_rev(F32)
        for m in range(HALF // HEAD):
            part = total[:HEAD, HALF - HEAD * (m + 1):HALF - HEAD * m]
            turned = lax.dot_general(rev32, part, (((1,), (1,)), ((), ())), precision=lax.Precision.HIGHEST, preferred_element_type=F32)
            dr_fin[p, HEAD * m:HEAD * (m + 1)] = turned.reshape(HEAD, 1, HEAD)
        dr_fin[p, HALF] = total[HEAD:HEAD + 1, HALF - HEAD:]
        dr_fin[p, HALF + 1] = total[HEAD + 1:HEAD + 2, HALF - HEAD:]
        dr_fin[p, HALF + 2:] = jnp.zeros((FIN - HALF - 2, 1, HEAD), F32)
        hop_start(p, 0)
        for m in range(N_PART):
            pltpu.make_async_copy(block(p, m, 0), parts[m].at[side, :, head_of(p, 0)], own_sem.at[p]).start()
            forward(p, m, 0)

    send_up(0)

    def sub_body(sub, carry):
        @pl.when(sub < SUBS - 1)
        def _():
            send_up(sub + 1)

        @pl.when(sub == SLOTS)
        def _():
            swap_start(0)

        @pl.when(sub == SUBS - 1)
        def _():
            swap_add(0)
            cross_start(0)

        @pl.when(sub == SUBS)
        def _():
            swap_start(1)
            cross_finish(0)

        @pl.when((z == 0) & (sub < SUBS))
        def _():
            lower_rows(sub)

        @pl.when((z == 0) & (sub > 0))
        def _():
            lower_theirs(sub - 1)

        @pl.when((z == 0) & (sub < SUBS))
        def _():
            lower_own(sub)

        @pl.when((z == 1) & (sub < SUBS))
        def _():
            upper_own(sub)

        @pl.when(sub < EARLY)
        def _():
            send_out(sub, (2, 3))

        @pl.when((sub > 0) & (sub <= EARLY))
        def _():
            send_out(sub - 1, (0, 1))
        return carry

    lax.fori_loop(0, SUBS + 1, sub_body, 0)

    send_out(EARLY, (2, 3))
    swap_add(1)
    cross_start(1)
    cross_finish(1)
    for p in range(2):
        hop_wait(p, 0)
        hop_start(p, 1)

    def send_late(sub, carry):
        send_out(sub, range(4))
        return carry

    send_out(EARLY, (0, 1))
    send_out(EARLY + 1, range(4))
    for p in range(2):
        hop_wait(p, 1)
        hop_start(p, 2)
    lax.fori_loop(EARLY + 2, SUBS, send_late, 0)
    for p in range(2):
        hop_wait(p, 2)

    wait_for(buf, out_recv)
    wait_for(buf.at[:, :, :HALF - ROWS], in_send)
    wait_for(buf.at[:, :, :HALF - ROWS], out_send)

    @pl.when(z == 1)
    def _():
        wait_for(st_tx, st_send)

    for p in range(2):
        wait_for(dr_rx.at[p], x_send.at[p])
        wait_for(dr_rz.at[p], z_send.at[p])
        wait_for(blocks(N_PART), own_sem.at[p])
        for hop in range(3):
            wait_for(blocks(N_PART << hop), ring_send.at[p, hop])
        for n in range(2):
            wait_for(blocks(N_PART // 2 * N_PAIR), fw_send.at[p, n])
            wait_for(blocks(N_PART // 2 * N_PAIR), fw_recv.at[p, n])


def writer(*refs):
    ins, (o, dq, dk, dv, dr, du, dw, sem) = refs[:4 + N_PART], refs[4 + N_PART:]
    pairs = list(zip(ins[:4], (o, dq, dk, dv)))
    for m, part in enumerate(ins[4:]):
        rows = min(PART, HALF - PART * m)
        for side in range(2):
            start = HALF * side + PART * m
            pairs.append((part.at[side, :rows], dr.at[start:start + rows]))
    last = HALF - PART * (N_PART - 1)
    pairs += [(ins[-1].at[0, last], du), (ins[-1].at[0, last + 1], dw)]
    copies = [pltpu.make_async_copy(src, dst, sem.at[j]) for j, (src, dst) in enumerate(pairs)]
    for copy in copies:
        copy.start()
    for copy in copies:
        copy.wait()


def solution(mesh):
    seq_spec = P(None, "cp", None, None)

    def local(query, key_in, value, bias_u, bias_w, rel_k, d_out):
        n_batch, rows, n_heads, head_dim = query.shape
        pairs = (n_batch, rows, N_PAIR, PAIR, head_dim)
        vm = pltpu.VMEM
        dma = pltpu.SemaphoreType.DMA
        whole = pl.BlockSpec(memory_space=pl.ANY)
        act = jax.ShapeDtypeStruct(pairs, BF16)
        vec = jax.ShapeDtypeStruct((n_heads, 1, head_dim), F32)
        tok = (PAIR, SEQ, HEAD)
        tok_t = (PAIR, HEAD, SEQ)
        acc = (HEAD + 8, HALF)
        outs = pl.pallas_call(
            kernel,
            name="rel_attn",
            out_shape=(act, act, act, act,
                       *[jax.ShapeDtypeStruct((2, PART, n_heads, 1, head_dim), F32)] * N_PART),
            in_specs=[pl.BlockSpec(memory_space=pltpu.HBM)] * 7,
            out_specs=[whole] * (4 + N_PART),
            scratch_shapes=[
                vm((4, SUBS, HALF, PAIR, HEAD), BF16), vm((2, SUBS, HALF, PAIR, HEAD), BF16),
                vm((SEQ, 2, PAIR, HEAD), BF16), vm((2, PAIR, HEAD), BF16), vm((2, PAIR, HEAD), BF16),
                vm((SUBS, PAIR, 8, HALF), F32), vm((SUBS, PAIR, 8, HALF), F32), vm((QB, HEAD), F32),
                vm((2, 2) + acc, F32), vm((2,) + acc, F32), vm((2, FIN, 1, HEAD), F32), vm((4, 2) + acc, F32),
                vm((QB, SEQ), F32), vm((QB, SEQ), F32), vm((QB, SEQ), F32),
                vm((QB, SEQ), BF16), vm((QB, SEQ), BF16), vm((QB, SEQ), BF16),
                vm(tok, BF16), vm(tok, BF16), vm(tok, BF16), vm(tok, BF16), vm(tok, BF16),
                vm(tok_t, BF16), vm(tok_t, BF16), vm(tok_t, BF16), vm(tok_t, BF16), vm(tok_t, BF16),
                vm((4, SEQ, HEAD), BF16), vm((4, HEAD, SEQ), BF16),
                vm((PAIR, HEAD, HALF), F32), vm((PAIR, HEAD, HALF), F32), vm((4, PAIR, HALF, HEAD), BF16),
                dma, dma((2, SUBS)), dma, dma, dma((2,)), dma((3,)), dma((4,)), dma((SUBS,)), dma, dma((SUBS,)),
                dma((2,)), dma((2,)), dma((2,)), dma((2,)), dma((2, 3)), dma((2, 3)), dma((2, 2)), dma((2, 2)),
            ],
            compiler_params=pltpu.CompilerParams(collective_id=0, has_side_effects=True, vmem_limit_bytes=36 * 1024 * 1024),
        )(*[pltpu.with_memory_space_constraint(x, pltpu.HBM) for x in (
            query.reshape(pairs), key_in.reshape(pairs), value.reshape(pairs), d_out.reshape(pairs),
            rel_k.reshape(SEQ, N_PAIR, PAIR, head_dim), bias_u.reshape(N_PAIR, PAIR, head_dim), bias_w.reshape(N_PAIR, PAIR, head_dim))])
        o, dq, dk, dv, dr, du, dw = pl.pallas_call(
            writer,
            name="writer",
            out_shape=(act, act, act, act, jax.ShapeDtypeStruct((SEQ, n_heads, 1, head_dim), F32), vec, vec),
            in_specs=[whole] * (4 + N_PART),
            out_specs=[whole] * 7,
            scratch_shapes=[dma((6 + 2 * N_PART,))],
            compiler_params=pltpu.CompilerParams(vmem_limit_bytes=1024 * 1024),
        )(*outs)
        full = query.shape
        return (o.reshape(full), dq.reshape(full), dk.reshape(full), dv.reshape(full),
                du.reshape(bias_u.shape), dw.reshape(bias_w.shape), dr.reshape(rel_k.shape))

    return jax.shard_map(local, mesh=mesh,
                         in_specs=(seq_spec, seq_spec, seq_spec, P(), P(), P(), seq_spec),
                         out_specs=(seq_spec, seq_spec, seq_spec, seq_spec, P(), P(), P()),
                         check_vma=False)
```

```python
import jax
import jax.numpy as jnp
from jax import lax
from jax.experimental import pallas as pl
from jax.experimental.pallas import tpu as pltpu
from jax.sharding import PartitionSpec as P

MESH = pl.DeviceIdType.MESH
BF16, F32 = jnp.bfloat16, jnp.float32
LOG2E = 1.4426950408889634

N_DEV = 16
PLANE = 8
PAIR = 2
N_PAIR = 8
SLOTS = 4
SUBS = 2 * SLOTS
EARLY = 3
ROWS = 64
HALF = PLANE * ROWS
SEQ = 2 * HALF
HEAD = 128
QB = 256
WIN = HALF + QB
N_PART = 6
PART = 86
FIN = N_PART * PART
TIP = 2 * ROWS
FAR = N_PAIR - 2
UNITS = FAR * SLOTS
TURNS = ((1, 3, 2), (3, 1, 2))


def dot(lhs, rhs):
    return jnp.dot(lhs, rhs, preferred_element_type=F32)


def flip8(x):
    rows, cols = x.shape
    idx = 7 - lax.broadcasted_iota(jnp.int32, (rows // 8, 8, cols), 1)
    return jnp.take_along_axis(x.reshape(rows // 8, 8, cols), idx, axis=1).reshape(rows, cols)


def eye_rev(dtype):
    total = lax.broadcasted_iota(jnp.int32, (HEAD, HEAD), 0) + lax.broadcasted_iota(jnp.int32, (HEAD, HEAD), 1)
    return jnp.where(total == HEAD - 1, 1.0, 0.0).astype(dtype)


def kernel(q_in, k_in, v_in, g_in, r_in, u_in, w_in,
           o_out, dq_out, dk_out, dv_out, dr0_out, dr1_out, dr2_out, dr3_out, dr4_out, dr5_out, far_out,
           buf, rbuf, r_buf, u_buf, w_buf, st_tx, st_rx, tip_st, st_ref, dr_rx, dr_rz, dr_fin, dr_acc,
           s_ref, e_ref, dp_ref, pb_ref, ds_ref, dd_ref,
           a_s, c_s, g_s, k_s, v_s, at_s, ct_s, gt_s, kt_s, vt_s, rev_s, rt_s, dkt, dvt, stage,
           in_send, in_recv, out_send, out_recv, own_sem, r_sem, up_send, up_recv, st_send, st_recv,
           x_send, x_recv, z_send, z_recv, ring_send, ring_recv, fw_send, fw_recv,
           far_send, far_recv, tip_sem, tip_near, tip_send, ts_send, ts_recv):
    me = lax.axis_index("cp")
    core = me % 2
    chip = me // 2
    col = chip % 4
    z = chip // 4
    partner = me + 1 - 2 * core
    across = me + PLANE * (1 - 2 * z)
    scale = HEAD ** -0.5

    def wait_for(ref, sem):
        pltpu.make_async_copy(ref, ref, sem).wait()

    y = col // 2
    lower, upper = z == 0, z == 1
    tip = chip == 7 * z
    tip_base = 2 - 2 * z

    tables = [pltpu.make_async_copy(src, dst, r_sem.at[j]) for j, (src, dst) in enumerate(
        ((r_in.at[:, 2 * col], r_buf.at[0]), (r_in.at[:, 2 * col + 1], r_buf.at[1]), (u_in, u_buf), (w_in, w_buf)))]
    for copy in tables:
        copy.start()

    barrier = pltpu.get_barrier_semaphore()

    for peer in [across] + [me ^ step for step in range(PLANE - 1, 0, -1)]:
        pl.semaphore_signal(barrier, inc=1, device_id=(peer,), device_id_type=MESH)
    pl.semaphore_wait(barrier, PLANE)

    my_rows = pl.ds(pl.multiple_of((me % PLANE) * ROWS, ROWS), ROWS)

    def peers():
        for near_turn, far_turn in zip(*TURNS):
            turn = jnp.where(core == 0, near_turn, far_turn)
            yield me ^ (2 * turn)
            yield me ^ (2 * turn + 1)
        yield partner

    def send_in(ins, sub):
        pair, row = sub // SLOTS, sub % SLOTS
        for first in (0, 2):
            for t in (first, first + 1):
                pltpu.make_async_copy(ins[t].at[core * SLOTS + row, :, 2 * col + pair], buf.at[t, sub, my_rows], in_recv.at[first // 2, sub]).start()
            for peer in peers():
                for t in (first, first + 1):
                    pltpu.make_async_remote_copy(
                        src_ref=ins[t].at[(peer % 2) * SLOTS + row, :, 2 * ((peer // 2) % 4) + pair], dst_ref=buf.at[t, sub, my_rows],
                        send_sem=in_send, recv_sem=in_recv.at[first // 2, sub], device_id=(peer,), device_id_type=MESH).start()

    def send_all(ins):
        def send_sub(sub, carry):
            send_in(ins, sub)
            return carry
        lax.fori_loop(0, SUBS, send_sub, 0)

    @pl.when(lower)
    def _():
        send_all((k_in, v_in, q_in, g_in))

    @pl.when(upper)
    def _():
        send_all((q_in, g_in, k_in, v_in))

    @pl.when(tip)
    def _():
        for t, src in enumerate((q_in, k_in, v_in, g_in)):
            for row in range(SLOTS):
                pltpu.make_async_remote_copy(
                    src_ref=src.at[(1 - core) * SLOTS + row, :, pl.ds(tip_base, FAR)], dst_ref=far_out.at[t, row],
                    send_sem=far_send, recv_sem=far_recv, device_id=(partner,), device_id_type=MESH).start()

    for copy in tables:
        copy.wait()
    rev = eye_rev(BF16)
    for p in range(2):
        pair_tab = pltpu.einshape("abc->bac", r_buf[p])
        for hh in range(PAIR):
            for blk in range(SEQ // HEAD):
                part = pair_tab[hh, SEQ - HEAD * (blk + 1):SEQ - HEAD * blk]
                flipped = dot(rev, part).astype(BF16)
                rev_s[2 * p + hh, HEAD * blk:HEAD * (blk + 1), :] = flipped
                rt_s[2 * p + hh, :, HEAD * blk:HEAD * (blk + 1)] = flipped.T
    dr_acc[...] = jnp.zeros_like(dr_acc)

    acts = (dk_out, dv_out, o_out, dq_out)

    def send_out(sub, which):
        place = (core * SLOTS + sub % SLOTS, slice(None), 2 * col + sub // SLOTS)
        for t in which:
            pltpu.make_async_copy(buf.at[t, sub, my_rows], acts[t].at[place], out_recv).start()
        for peer in peers():
            peer_rows = pl.ds(pl.multiple_of((peer % PLANE) * ROWS, ROWS), ROWS)
            to_tip = (peer // 2 == 7 * z) & jnp.logical_not(tip)
            for t in which:
                @pl.when(jnp.logical_not(to_tip & (lower if t >= 2 else upper)))
                def _():
                    pltpu.make_async_remote_copy(
                        src_ref=buf.at[t, sub, peer_rows], dst_ref=acts[t].at[place],
                        send_sem=out_send, recv_sem=out_recv, device_id=(peer,), device_id_type=MESH).start()

    def send_up(sub):
        wait_for(buf.at[0:2, sub], in_recv.at[0, sub])
        for j in range(2):
            pltpu.make_async_remote_copy(src_ref=buf.at[j, sub], dst_ref=rbuf.at[j, sub], send_sem=up_send.at[sub % 4], recv_sem=up_recv.at[sub],
                                         device_id=(across,), device_id_type=MESH).start()

    def unpack(ref, j, sub):
        return pltpu.einshape("abc->bac", ref[j, sub])

    def load_rows(q_ref, q_j, g_ref, g_j, sub, start, turned):
        rows = slice(start, start + HALF)
        p = sub // SLOTS
        q2 = unpack(q_ref, q_j, sub)
        u = u_buf[2 * col + p].astype(F32)
        w = w_buf[2 * col + p].astype(F32)
        for hh in range(PAIR):
            q32 = q2[hh].astype(F32)
            a = (q32 + u[hh:hh + 1]).astype(BF16)
            c = (q32 + w[hh:hh + 1]).astype(BF16)
            a_s[hh, rows, :] = a
            c_s[hh, rows, :] = c
            at_s[hh, :, rows] = a.T
            if turned:
                ct_s[hh, :, rows] = flip8(c.astype(F32)).astype(BF16).T
        g2 = unpack(g_ref, g_j, sub)
        g_s[:, rows, :] = g2
        for hh in range(PAIR):
            gt_s[hh, :, rows] = g2[hh].T

    def load_keys(k_ref, k_j, v_ref, v_j, sub, start):
        rows = slice(start, start + HALF)
        k2 = unpack(k_ref, k_j, sub)
        v2 = unpack(v_ref, v_j, sub)
        k_s[:, rows, :] = k2
        v_s[:, rows, :] = v2
        for hh in range(PAIR):
            kt_s[hh, :, rows] = k2[hh].T
            vt_s[hh, :, rows] = v2[hh].T

    def row_block(hh, head, start, i0, lo, fresh, stats):
        width = i0 + QB
        rows = slice(start, start + QB)
        s_ref[:, :width] = dot(a_s[hh, rows, :], kt_s[hh, :, :width])
        e_ref[:, :width] = dot(c_s[hh, rows, :], rt_s[head, :, SEQ - width:])
        dp_ref[:, :width] = dot(g_s[hh, rows, :], vt_s[hh, :, :width])
        for r0 in range(0, QB, 16):
            group = slice(r0, r0 + 16)
            rel = pltpu.roll(e_ref[group, :width], i0 + 1 + r0, 1, stride=1, stride_axis=0)
            s = s_ref[group, :width] + rel
            ahead = lax.broadcasted_iota(jnp.int32, (16, width), 1) - lax.broadcasted_iota(jnp.int32, (16, width), 0)
            s = jnp.where(ahead <= i0 + r0, s, -jnp.inf)
            top = jnp.max(s, axis=1, keepdims=True)
            p = jnp.exp2((s - top) * (scale * LOG2E))
            total = jnp.sum(p, axis=1, keepdims=True)
            p = p * (1.0 / total)
            pb_ref[group, :width] = p.astype(BF16)
            dp = dp_ref[group, :width]
            row_dot = jnp.sum(p * dp, axis=1, keepdims=True)
            ds = (p * (dp - row_dot) * scale).astype(BF16)
            ds_ref[group, :width] = ds
            flipped = flip8(ds.astype(F32))
            half = [pltpu.roll(flipped[8 * j:8 * j + 8], QB - 8 - r0 - 8 * j, 1, stride=1, stride_axis=0) for j in range(2)]
            dd_ref[group, :width] = jnp.concatenate(half, axis=0).astype(BF16)
            if stats:
                lane = lax.broadcasted_iota(jnp.int32, (16, HEAD), 1)
                st_ref[group, :] = jnp.where(lane == 0, top * (scale * LOG2E) + jnp.log2(total), row_dot)
        pb = pb_ref[:, :width]
        ds = ds_ref[:, :width]
        dd = dd_ref[:, :width]
        stage[0, hh, rows, :] = dot(pb, v_s[hh, :width, :]).astype(BF16)
        dqc = dot(ds, k_s[hh, :width, :])
        dqr = flip8(dot(dd, rev_s[head, SEQ - width:, :]))
        stage[1, hh, rows, :] = (dqc + dqr).astype(BF16)
        dr_acc[head, 1, HEAD:HEAD + 1, HALF - HEAD:] += jnp.sum(dqc, axis=0, keepdims=True)
        dr_acc[head, 1, HEAD + 1:HEAD + 2, HALF - HEAD:] += jnp.sum(dqr, axis=0, keepdims=True)
        dk_new = dot(at_s[hh, :, rows], ds_ref[:, lo:width])
        dv_new = dot(gt_s[hh, :, rows], pb_ref[:, lo:width])
        if fresh:
            dkt[hh] = dk_new
            dvt[hh] = dv_new
        else:
            dkt[hh, :, :width - lo] += dk_new
            dvt[hh, :, :width - lo] += dv_new
        dr_new = dot(ct_s[hh, :, rows], dd)
        if width > HALF:
            dr_acc[head, 0, :HEAD, SEQ - width:] += dr_new[:, :width - HALF]
            dr_acc[head, 1, :HEAD, :] += dr_new[:, width - HALF:]
        else:
            dr_acc[head, 1, :HEAD, HALF - width:] += dr_new

    def col_block(hh, head, sub, i0):
        rows = slice(i0, i0 + QB)
        first = WIN - i0
        s_ref[:, :HALF] = dot(a_s[hh, rows, :], kt_s[hh, :, :HALF])
        e_ref[:, :WIN] = dot(c_s[hh, rows, :], rt_s[head, :, first:first + WIN])
        dp_ref[:, :HALF] = dot(g_s[hh, rows, :], vt_s[hh, :, :HALF])
        st_ref[:, :8] = st_rx[sub, hh, :, i0 - HALF:i0 - HALF + QB].T
        for r0 in range(0, QB, 16):
            group = slice(r0, r0 + 16)
            rel = pltpu.roll(e_ref[group, :WIN], HALF + 1 + r0, 1, stride=1, stride_axis=0)[:, :HALF]
            log_sum = st_ref[group, 0:1]
            row_dot = st_ref[group, 1:2]
            p = jnp.exp2((s_ref[group, :HALF] + rel) * (scale * LOG2E) - log_sum)
            pb_ref[group, :HALF] = p.astype(BF16)
            ds_ref[group, :HALF] = (p * (dp_ref[group, :HALF] - row_dot) * scale).astype(BF16)
        dkt[hh] += dot(at_s[hh, :, rows], ds_ref[:, :HALF])
        dvt[hh] += dot(gt_s[hh, :, rows], pb_ref[:, :HALF])

    def store_rows(sub):
        for t in range(2):
            buf[2 + t, sub] = pltpu.einshape("abc->bac", stage[t])

    def store_keys(sub):
        for hh in range(PAIR):
            stage[2, hh] = dkt[hh].astype(BF16).T
            stage[3, hh] = dvt[hh].astype(BF16).T
        for t in range(2):
            buf[t, sub] = pltpu.einshape("abc->bac", stage[2 + t])

    def wait_up(sub):
        wait_for(rbuf.at[:, sub], up_recv.at[sub])
        wait_for(rbuf.at[:, sub], up_send.at[sub % 4])

    def wait_in(sub):
        wait_for(buf.at[2:4, sub], in_recv.at[1, sub])

    def lower_rows(sub):
        wait_in(sub)
        load_rows(buf, 2, buf, 3, sub, 0, True)

    def lower_own(sub):
        load_keys(buf, 0, buf, 1, sub, 0)

        def own(hh, carry):
            head = 2 * (sub // SLOTS) + hh
            row_block(hh, head, QB, QB, 0, True, False)
            row_block(hh, head, 0, 0, 0, False, False)
            return carry

        lax.fori_loop(0, PAIR, own, 0)
        store_rows(sub)

    def lower_theirs(sub):
        wait_up(sub)
        load_rows(rbuf, 0, rbuf, 1, sub, HALF, False)
        wait_for(st_rx.at[sub], st_recv.at[sub])

        def theirs(hh, carry):
            head = 2 * (sub // SLOTS) + hh
            col_block(hh, head, sub, HALF)
            col_block(hh, head, sub, HALF + QB)
            return carry

        lax.fori_loop(0, PAIR, theirs, 0)
        store_keys(sub)

    def upper_own(sub):
        wait_in(sub)
        wait_up(sub)
        load_rows(buf, 0, buf, 1, sub, 0, True)
        load_keys(rbuf, 0, rbuf, 1, sub, 0)
        load_keys(buf, 2, buf, 3, sub, HALF)

        def own(hh, carry):
            head = 2 * (sub // SLOTS) + hh
            for blk in (1, 0):
                row_block(hh, head, QB * blk, HALF + QB * blk, HALF, blk == 1, True)
                st_tx[sub, hh, :, QB * blk:QB * (blk + 1)] = st_ref[...].T[:8]
            pltpu.make_async_remote_copy(src_ref=st_tx.at[sub, hh], dst_ref=st_rx.at[sub, hh], send_sem=st_send, recv_sem=st_recv.at[sub],
                                         device_id=(across,), device_id_type=MESH).start()

            @pl.when(jnp.logical_not(tip))
            def _():
                pltpu.make_async_remote_copy(src_ref=st_tx.at[sub, hh, :, HALF - TIP:], dst_ref=tip_st.at[col, sub, hh], send_sem=ts_send,
                                             recv_sem=ts_recv, device_id=(N_DEV - 2 + core,), device_id_type=MESH).start()
            return carry

        lax.fori_loop(0, PAIR, own, 0)
        store_rows(sub)
        store_keys(sub)

    side = 1 - core
    parts = (dr0_out, dr1_out, dr2_out, dr3_out, dr4_out, dr5_out)

    def swap_start(p):
        for n in range(2):
            pltpu.make_async_remote_copy(src_ref=dr_acc.at[2 * p + n, side], dst_ref=dr_rx.at[p, n], send_sem=x_send.at[p], recv_sem=x_recv.at[p],
                                         device_id=(partner,), device_id_type=MESH).start()

    def swap_add(p):
        wait_for(dr_rx.at[p], x_recv.at[p])
        for n in range(2):
            dr_rx[p, n] = dr_rx[p, n] + dr_acc[2 * p + n, core]

    def cross_start(p):
        pltpu.make_async_remote_copy(src_ref=dr_rx.at[p, 1 - z], dst_ref=dr_rz.at[p], send_sem=z_send.at[p], recv_sem=z_recv.at[p],
                                     device_id=(across,), device_id_type=MESH).start()

    def head_of(p, bits):
        other = chip ^ bits
        return 4 * (other % 4) + 2 * p + other // 4

    def block(p, m, bits):
        if bits == 0:
            return dr_fin.at[p, PART * m:PART * (m + 1)]
        return parts[m].at[side, :, head_of(p, bits)]

    def forward(p, m, bits):
        pltpu.make_async_remote_copy(src_ref=block(p, m, bits), dst_ref=parts[m].at[side, :, head_of(p, bits)], send_sem=fw_send.at[p, m // 3],
                                     recv_sem=fw_recv.at[p, m // 3], device_id=(partner,), device_id_type=MESH).start()

    def blocks(count):
        return parts[0].at[:, :, :N_PART // 2 * count]

    def pass_on(p, bits, hop, device):
        for m in range(N_PART):
            pltpu.make_async_remote_copy(
                src_ref=block(p, m, bits), dst_ref=parts[m].at[side, :, head_of(p, bits)], send_sem=ring_send.at[p, hop],
                recv_sem=ring_recv.at[p, hop], device_id=(device,), device_id_type=MESH).start()

    def hand_over(p, bits):
        for m in range(N_PART):
            forward(p, m, bits)

    even = chip % 2 == z
    loaded = y != z
    along_x, along_y = me ^ 2, me ^ 4

    def hop_start(p, hop):
        if hop == 0:
            for device in (along_x, along_y, across):
                pass_on(p, 0, 0, device)
        if hop == 1:
            @pl.when(even & loaded)
            def _():
                pass_on(p, 1, 1, along_y)

            @pl.when(jnp.logical_not(even) & loaded)
            def _():
                pass_on(p, 2, 1, along_x)

            pass_on(p, 1, 1, across)
            pass_on(p, 2, 1, across)
        if hop == 2:
            @pl.when(even & loaded)
            def _():
                pass_on(p, 5, 2, along_y)

            @pl.when(jnp.logical_not(even) & loaded)
            def _():
                pass_on(p, 6, 2, along_x)

            @pl.when(even)
            def _():
                pass_on(p, 3, 2, across)
        if hop == 3:
            @pl.when(even)
            def _():
                pass_on(p, 7, 3, across)

    def hop_wait(p, hop):
        if hop == 0:
            wait_for(blocks(3), ring_recv.at[p, 0])
            for bits in (1, 2, 4):
                hand_over(p, bits)
        if hop == 1:
            @pl.when(even)
            def _():
                wait_for(blocks(3), ring_recv.at[p, 1])
                hand_over(p, 3)

            @pl.when(jnp.logical_not(even))
            def _():
                wait_for(blocks(2), ring_recv.at[p, 1])
            for bits in (5, 6):
                hand_over(p, bits)
        if hop == 2:
            wait_for(blocks(1), ring_recv.at[p, 2])
            hand_over(p, 7)
        if hop == 3:
            @pl.when(jnp.logical_not(even))
            def _():
                wait_for(blocks(1), ring_recv.at[p, 3])
                hand_over(p, 3)

    def sent_wait(p):
        wait_for(blocks(3), ring_send.at[p, 0])

        @pl.when(loaded)
        def _():
            wait_for(blocks(3), ring_send.at[p, 1])

        @pl.when(jnp.logical_not(loaded))
        def _():
            wait_for(blocks(2), ring_send.at[p, 1])

        @pl.when(even & loaded)
        def _():
            wait_for(blocks(2), ring_send.at[p, 2])

        @pl.when(even != loaded)
        def _():
            wait_for(blocks(1), ring_send.at[p, 2])

        @pl.when(even)
        def _():
            wait_for(blocks(1), ring_send.at[p, 3])

    def cross_finish(p):
        wait_for(dr_rz.at[p], z_recv.at[p])
        total = dr_rx[p, z] + dr_rz[p]
        rev32 = eye_rev(F32)
        for m in range(HALF // HEAD):
            part = total[:HEAD, HALF - HEAD * (m + 1):HALF - HEAD * m]
            turned = lax.dot_general(rev32, part, (((1,), (1,)), ((), ())), precision=lax.Precision.HIGHEST, preferred_element_type=F32)
            dr_fin[p, HEAD * m:HEAD * (m + 1)] = turned.reshape(HEAD, 1, HEAD)
        dr_fin[p, HALF] = total[HEAD:HEAD + 1, HALF - HEAD:]
        dr_fin[p, HALF + 1] = total[HEAD + 1:HEAD + 2, HALF - HEAD:]
        dr_fin[p, HALF + 2:] = jnp.zeros((FIN - HALF - 2, 1, HEAD), F32)
        hop_start(p, 0)
        for m in range(N_PART):
            pltpu.make_async_copy(block(p, m, 0), parts[m].at[side, :, head_of(p, 0)], own_sem.at[p]).start()
        hand_over(p, 0)

    def tip_load(unit):
        slot, row, far = unit % 2, unit // FAR, unit % FAR
        pair = far + tip_base
        for t, src in enumerate((q_in, k_in, v_in, g_in)):
            pltpu.make_async_copy(src.at[core * SLOTS + row, :, pair], r_buf.at[slot, pl.ds(TIP * t + ROWS * core, ROWS)], tip_sem.at[slot]).start()
            pltpu.make_async_copy(far_out.at[t, row, :, far], r_buf.at[slot, pl.ds(TIP * t + ROWS * (1 - core), ROWS)], tip_sem.at[slot]).start()
        pltpu.make_async_copy(r_in.at[:TIP, pair], r_buf.at[slot, 4 * TIP:5 * TIP], tip_sem.at[slot]).start()

    def tip_done(slot):
        wait_for(r_buf.at[slot, :TIP], tip_near.at[slot])
        wait_for(r_buf.at[slot, :TIP], tip_send.at[slot])

    def tip_group(hh, r0):
        group = slice(TIP * hh + r0, TIP * hh + r0 + 16)
        rel = pltpu.roll(e_ref[group, :TIP], 1 + r0, 1, stride=1, stride_axis=0)
        ahead = lax.broadcasted_iota(jnp.int32, (16, TIP), 1) - lax.broadcasted_iota(jnp.int32, (16, TIP), 0)
        return group, s_ref[group, :TIP] + rel, ahead <= r0

    def tip_rows(hh):
        for r0 in range(0, TIP, 16):
            group, s, seen = tip_group(hh, r0)
            s = jnp.where(seen, s, -jnp.inf)
            top = jnp.max(s, axis=1, keepdims=True)
            p = jnp.exp2((s - top) * (scale * LOG2E))
            p = p * (1.0 / jnp.sum(p, axis=1, keepdims=True))
            pb_ref[group, :TIP] = p.astype(BF16)
            dp = dp_ref[group, :TIP]
            row_dot = jnp.sum(p * dp, axis=1, keepdims=True)
            ds = (p * (dp - row_dot) * scale).astype(BF16)
            ds_ref[group, :TIP] = ds
            flipped = flip8(ds.astype(F32))
            half = [pltpu.roll(flipped[8 * j:8 * j + 8], TIP - 8 - r0 - 8 * j, 1, stride=1, stride_axis=0) for j in range(2)]
            dd_ref[group, :TIP] = jnp.concatenate(half, axis=0).astype(BF16)
        rows = slice(TIP * hh, TIP * (hh + 1))
        stage[0, hh, :TIP, :] = dot(pb_ref[rows, :TIP], v_s[hh, :TIP, :]).astype(BF16)
        dqc = dot(ds_ref[rows, :TIP], k_s[hh, :TIP, :])
        dqr = flip8(dot(dd_ref[rows, :TIP], c_s[hh, :TIP, :]))
        stage[1, hh, :TIP, :] = (dqc + dqr).astype(BF16)

    def tip_keys(hh, stats):
        rows = slice(TIP * hh, TIP * (hh + 1))
        st_ref[rows, :8] = stats.T
        for r0 in range(0, TIP, 16):
            group, s, seen = tip_group(hh, r0)
            p = jnp.where(seen, jnp.exp2(s * (scale * LOG2E) - st_ref[group, 0:1]), 0.0)
            pb_ref[group, :TIP] = p.astype(BF16)
            ds_ref[group, :TIP] = (p * (dp_ref[group, :TIP] - st_ref[group, 1:2]) * scale).astype(BF16)
        over_rows = (((0,), (0,)), ((), ()))
        stage[0, hh, :TIP, :] = lax.dot_general(ds_ref[rows, :TIP], a_s[hh, :TIP, :], over_rows, preferred_element_type=F32).astype(BF16)
        stage[1, hh, :TIP, :] = lax.dot_general(pb_ref[rows, :TIP], g_s[hh, :TIP, :], over_rows, preferred_element_type=F32).astype(BF16)

    def tip_unit(unit, carry):
        slot, row, far = unit % 2, unit // FAR, unit % FAR
        pair = far + tip_base
        wait_for(r_buf.at[slot, :5 * TIP], tip_sem.at[slot])

        @pl.when(unit + 1 < UNITS)
        def _():
            tip_load(unit + 1)

        q2, k2, v2, g2, r2 = [pltpu.einshape("abc->bac", r_buf[slot, TIP * t:TIP * (t + 1)]) for t in range(5)]
        u = u_buf[pair].astype(F32)
        w = w_buf[pair].astype(F32)
        for hh in range(PAIR):
            rows = slice(TIP * hh, TIP * (hh + 1))
            q32 = q2[hh].astype(F32)
            a = (q32 + u[hh:hh + 1]).astype(BF16)
            c = (q32 + w[hh:hh + 1]).astype(BF16)
            falling = dot(eye_rev(BF16), r2[hh]).astype(BF16)
            s_ref[rows, :TIP] = dot(a, k2[hh].T)
            e_ref[rows, :TIP] = dot(c, falling.T)
            dp_ref[rows, :TIP] = dot(g2[hh], v2[hh].T)
            a_s[hh, :TIP, :] = a
            c_s[hh, :TIP, :] = falling
            g_s[hh, :TIP, :] = g2[hh]
            k_s[hh, :TIP, :] = k2[hh]
            v_s[hh, :TIP, :] = v2[hh]

        @pl.when(lower)
        def _():
            for hh in range(PAIR):
                tip_rows(hh)

        @pl.when(upper)
        def _():
            for hh in range(PAIR):
                tip_keys(hh, tip_st[far // 2, (far % 2) * SLOTS + row, hh])

        @pl.when(unit >= 2)
        def _():
            tip_done(slot)

        for n in range(2):
            r_buf[slot, (5 + n) * TIP:(6 + n) * TIP] = pltpu.einshape("abc->bac", stage[n, :, :TIP, :])
        place = (core * SLOTS + row, slice(None), pair)

        def give(results):
            for n, dst in enumerate(results):
                pltpu.make_async_copy(r_buf.at[slot, pl.ds((5 + n) * TIP + ROWS * core, ROWS)], dst.at[place], tip_near.at[slot]).start()
                pltpu.make_async_remote_copy(
                    src_ref=r_buf.at[slot, pl.ds((5 + n) * TIP + ROWS * (1 - core), ROWS)], dst_ref=dst.at[place],
                    send_sem=tip_send.at[slot], recv_sem=out_recv, device_id=(partner,), device_id_type=MESH).start()

        @pl.when(lower)
        def _():
            give((o_out, dq_out))

        @pl.when(upper)
        def _():
            give((dk_out, dv_out))
        return carry

    def tips(third):
        @pl.when(tip)
        def _():
            if third == 0:
                wait_for(far_out, far_recv)

                @pl.when(upper)
                def _():
                    wait_for(tip_st, ts_recv)
                tip_load(0)
            lax.fori_loop(UNITS // 3 * third, UNITS // 3 * (third + 1), tip_unit, 0)
            if third == 2:
                tip_done(0)
                tip_done(1)

    send_up(0)

    def sub_body(sub, carry):
        @pl.when(sub < SUBS - 1)
        def _():
            send_up(sub + 1)

        @pl.when(sub == SLOTS)
        def _():
            swap_start(0)

        @pl.when(sub == SUBS - 1)
        def _():
            swap_add(0)
            cross_start(0)

        @pl.when(sub == SUBS)
        def _():
            swap_start(1)
            cross_finish(0)

        @pl.when(lower & (sub < SUBS))
        def _():
            lower_rows(sub)

        @pl.when(lower & (sub > 0))
        def _():
            lower_theirs(sub - 1)

        @pl.when(lower & (sub < SUBS))
        def _():
            lower_own(sub)

        @pl.when(upper & (sub < SUBS))
        def _():
            upper_own(sub)

        @pl.when(sub < EARLY)
        def _():
            send_out(sub, (2, 3))

        @pl.when((sub > 0) & (sub <= EARLY))
        def _():
            send_out(sub - 1, (0, 1))
        return carry

    lax.fori_loop(0, SUBS + 1, sub_body, 0)

    send_out(EARLY, (2, 3))
    swap_add(1)
    cross_start(1)
    cross_finish(1)
    send_out(EARLY, (0, 1))
    for p in range(2):
        hop_wait(p, 0)
        hop_start(p, 1)
    for p in range(2):
        send_out(EARLY + 1 + p, range(4))
        tips(p)
        hop_wait(p, 1)
        hop_start(p, 2)

    def send_late(sub, carry):
        send_out(sub, range(4))
        return carry

    lax.fori_loop(EARLY + 3, SUBS, send_late, 0)
    tips(2)
    for p in range(2):
        hop_wait(p, 2)
        hop_start(p, 3)
    for p in range(2):
        hop_wait(p, 3)

    wait_for(buf.at[:, :, :HALF - ROWS], in_send)

    @pl.when(tip)
    def _():
        wait_for(buf.at[:, :, :HALF - 3 * ROWS // 2], out_recv)
        wait_for(buf.at[:, :, :HALF - ROWS], out_send)
        wait_for(far_out, far_send)

    @pl.when(jnp.logical_not(tip))
    def _():
        wait_for(buf, out_recv)
        wait_for(buf.at[:, :, :HALF - 2 * ROWS], out_send)

    @pl.when(upper & jnp.logical_not(tip))
    def _():
        wait_for(st_tx.at[:2], ts_send)

    @pl.when(upper)
    def _():
        wait_for(st_tx, st_send)

    for p in range(2):
        wait_for(dr_rx.at[p], x_send.at[p])
        wait_for(dr_rz.at[p], z_send.at[p])
        wait_for(blocks(1), own_sem.at[p])
        sent_wait(p)
        for n in range(2):
            wait_for(blocks(N_PAIR // 2), fw_send.at[p, n])
            wait_for(blocks(N_PAIR // 2), fw_recv.at[p, n])


def writer(*refs):
    ins, (o, dq, dk, dv, dr, du, dw, sem) = refs[:4 + N_PART], refs[4 + N_PART:]
    pairs = list(zip(ins[:4], (o, dq, dk, dv)))
    for m, part in enumerate(ins[4:]):
        rows = min(PART, HALF - PART * m)
        for side in range(2):
            start = HALF * side + PART * m
            pairs.append((part.at[side, :rows], dr.at[start:start + rows]))
    last = HALF - PART * (N_PART - 1)
    pairs += [(ins[-1].at[0, last], du), (ins[-1].at[0, last + 1], dw)]
    copies = [pltpu.make_async_copy(src, dst, sem.at[j]) for j, (src, dst) in enumerate(pairs)]
    for copy in copies:
        copy.start()
    for copy in copies:
        copy.wait()


def solution(mesh):
    seq_spec = P(None, "cp", None, None)

    def local(query, key_in, value, bias_u, bias_w, rel_k, d_out):
        n_batch, rows, n_heads, head_dim = query.shape
        pairs = (n_batch, rows, N_PAIR, PAIR, head_dim)
        vm = pltpu.VMEM
        dma = pltpu.SemaphoreType.DMA
        whole = pl.BlockSpec(memory_space=pl.ANY)
        act = jax.ShapeDtypeStruct(pairs, BF16)
        vec = jax.ShapeDtypeStruct((n_heads, 1, head_dim), F32)
        tok = (PAIR, SEQ, HEAD)
        tok_t = (PAIR, HEAD, SEQ)
        acc = (HEAD + 8, HALF)
        outs = pl.pallas_call(
            kernel,
            name="rel_attn",
            out_shape=(act, act, act, act,
                       *[jax.ShapeDtypeStruct((2, PART, n_heads, 1, head_dim), F32)] * N_PART,
                       jax.ShapeDtypeStruct((4, SLOTS, ROWS, FAR, PAIR, HEAD), BF16)),
            in_specs=[pl.BlockSpec(memory_space=pltpu.HBM)] * 7,
            out_specs=[whole] * (5 + N_PART),
            scratch_shapes=[
                vm((4, SUBS, HALF, PAIR, HEAD), BF16), vm((2, SUBS, HALF, PAIR, HEAD), BF16),
                vm((2, SEQ, PAIR, HEAD), BF16), vm((N_PAIR, PAIR, HEAD), BF16), vm((N_PAIR, PAIR, HEAD), BF16),
                vm((SUBS, PAIR, 8, HALF), F32), vm((SUBS, PAIR, 8, HALF), F32), vm((3, SUBS, PAIR, 8, TIP), F32), vm((QB, HEAD), F32),
                vm((2, 2) + acc, F32), vm((2,) + acc, F32), vm((2, FIN, 1, HEAD), F32), vm((4, 2) + acc, F32),
                vm((QB, SEQ), F32), vm((QB, SEQ), F32), vm((QB, SEQ), F32),
                vm((QB, SEQ), BF16), vm((QB, SEQ), BF16), vm((QB, SEQ), BF16),
                vm(tok, BF16), vm(tok, BF16), vm(tok, BF16), vm(tok, BF16), vm(tok, BF16),
                vm(tok_t, BF16), vm(tok_t, BF16), vm(tok_t, BF16), vm(tok_t, BF16), vm(tok_t, BF16),
                vm((4, SEQ, HEAD), BF16), vm((4, HEAD, SEQ), BF16),
                vm((PAIR, HEAD, HALF), F32), vm((PAIR, HEAD, HALF), F32), vm((4, PAIR, HALF, HEAD), BF16),
                dma, dma((2, SUBS)), dma, dma, dma((2,)), dma((4,)), dma((4,)), dma((SUBS,)), dma, dma((SUBS,)),
                dma((2,)), dma((2,)), dma((2,)), dma((2,)), dma((2, 4)), dma((2, 4)), dma((2, 2)), dma((2, 2)),
                dma, dma, dma((2,)), dma((2,)), dma((2,)), dma, dma,
            ],
            compiler_params=pltpu.CompilerParams(collective_id=0, has_side_effects=True, vmem_limit_bytes=37 * 1024 * 1024),
        )(*[pltpu.with_memory_space_constraint(x, pltpu.HBM) for x in (
            query.reshape(pairs), key_in.reshape(pairs), value.reshape(pairs), d_out.reshape(pairs),
            rel_k.reshape(SEQ, N_PAIR, PAIR, head_dim), bias_u.reshape(N_PAIR, PAIR, head_dim), bias_w.reshape(N_PAIR, PAIR, head_dim))])
        o, dq, dk, dv, dr, du, dw = pl.pallas_call(
            writer,
            name="writer",
            out_shape=(act, act, act, act, jax.ShapeDtypeStruct((SEQ, n_heads, 1, head_dim), F32), vec, vec),
            in_specs=[whole] * (4 + N_PART),
            out_specs=[whole] * 7,
            scratch_shapes=[dma((6 + 2 * N_PART,))],
            compiler_params=pltpu.CompilerParams(vmem_limit_bytes=1024 * 1024),
        )(*outs[:-1])
        full = query.shape
        return (o.reshape(full), dq.reshape(full), dk.reshape(full), dv.reshape(full),
                du.reshape(bias_u.shape), dw.reshape(bias_w.shape), dr.reshape(rel_k.shape))

    return jax.shard_map(local, mesh=mesh,
                         in_specs=(seq_spec, seq_spec, seq_spec, P(), P(), P(), seq_spec),
                         out_specs=(seq_spec, seq_spec, seq_spec, seq_spec, P(), P(), P()),
                         check_vma=False)
```

```python
import jax
import jax.numpy as jnp
from jax import lax
from jax.experimental import pallas as pl
from jax.experimental.pallas import tpu as pltpu
from jax.sharding import PartitionSpec as P

MESH = pl.DeviceIdType.MESH
BF16, F32 = jnp.bfloat16, jnp.float32
LOG2E = 1.4426950408889634

N_DEV = 16
PLANE = 8
PAIR = 2
N_PAIR = 8
SLOTS = 4
SUBS = 2 * SLOTS
EARLY = 3
ROWS = 64
HALF = PLANE * ROWS
SEQ = 2 * HALF
HEAD = 128
QB = 256
WIN = HALF + QB
N_PART = 6
PART = 86
FIN = N_PART * PART
TIP = 2 * ROWS
FAR = N_PAIR - 2
UNITS = FAR * SLOTS
TURNS = ((1, 3, 2), (3, 1, 2))


def dot(lhs, rhs):
    return jnp.dot(lhs, rhs, preferred_element_type=F32)


def flip8(x):
    rows, cols = x.shape
    idx = 7 - lax.broadcasted_iota(jnp.int32, (rows // 8, 8, cols), 1)
    return jnp.take_along_axis(x.reshape(rows // 8, 8, cols), idx, axis=1).reshape(rows, cols)


def eye_rev(dtype):
    total = lax.broadcasted_iota(jnp.int32, (HEAD, HEAD), 0) + lax.broadcasted_iota(jnp.int32, (HEAD, HEAD), 1)
    return jnp.where(total == HEAD - 1, 1.0, 0.0).astype(dtype)


def kernel(q_in, k_in, v_in, g_in, r_in, u_in, w_in,
           o_out, dq_out, dk_out, dv_out, dr0_out, dr1_out, dr2_out, dr3_out, dr4_out, dr5_out, far_out,
           buf, rbuf, r_buf, u_buf, w_buf, st_tx, st_rx, tip_st, st_ref, dr_rx, dr_rz, dr_fin, dr_acc,
           s_ref, e_ref, dp_ref, pb_ref, ds_ref, dd_ref,
           a_s, c_s, g_s, k_s, v_s, at_s, ct_s, gt_s, kt_s, vt_s, rev_s, rt_s, dkt, dvt, stage,
           in_send, in_recv, out_send, out_recv, own_sem, r_sem, up_send, up_recv, st_send, st_recv,
           x_send, x_recv, z_send, z_recv, ring_send, ring_recv, fw_send, fw_recv,
           far_send, far_recv, tip_sem, tip_near, tip_send, ts_send, ts_recv):
    me = lax.axis_index("cp")
    core = me % 2
    chip = me // 2
    col = chip % 4
    z = chip // 4
    partner = me + 1 - 2 * core
    across = me + PLANE * (1 - 2 * z)
    scale = HEAD ** -0.5

    def wait_for(ref, sem):
        pltpu.make_async_copy(ref, ref, sem).wait()

    y = col // 2
    lower, upper = z == 0, z == 1
    tip = chip == 7 * z
    tip_base = 2 - 2 * z

    tables = [pltpu.make_async_copy(src, dst, r_sem.at[j]) for j, (src, dst) in enumerate(
        ((r_in.at[:, 2 * col], r_buf.at[0]), (r_in.at[:, 2 * col + 1], r_buf.at[1]), (u_in, u_buf), (w_in, w_buf)))]
    for copy in tables:
        copy.start()

    barrier = pltpu.get_barrier_semaphore()

    for peer in [across] + [me ^ step for step in range(PLANE - 1, 0, -1)]:
        pl.semaphore_signal(barrier, inc=1, device_id=(peer,), device_id_type=MESH)
    pl.semaphore_wait(barrier, PLANE)

    my_rows = pl.ds(pl.multiple_of((me % PLANE) * ROWS, ROWS), ROWS)

    def peers():
        for near_turn, far_turn in zip(*TURNS):
            turn = jnp.where(core == 0, near_turn, far_turn)
            yield me ^ (2 * turn)
            yield me ^ (2 * turn + 1)
        yield partner

    def send_in(ins, sub):
        pair, row = sub // SLOTS, sub % SLOTS
        for first in (0, 2):
            for t in (first, first + 1):
                pltpu.make_async_copy(ins[t].at[core * SLOTS + row, :, 2 * col + pair], buf.at[t, sub, my_rows], in_recv.at[first // 2, sub]).start()
            for peer in peers():
                for t in (first, first + 1):
                    pltpu.make_async_remote_copy(
                        src_ref=ins[t].at[(peer % 2) * SLOTS + row, :, 2 * ((peer // 2) % 4) + pair], dst_ref=buf.at[t, sub, my_rows],
                        send_sem=in_send, recv_sem=in_recv.at[first // 2, sub], device_id=(peer,), device_id_type=MESH).start()

    def send_all(ins):
        def send_sub(sub, carry):
            send_in(ins, sub)
            return carry
        lax.fori_loop(0, SUBS, send_sub, 0)

    @pl.when(lower)
    def _():
        send_all((k_in, v_in, q_in, g_in))

    @pl.when(upper)
    def _():
        send_all((q_in, g_in, k_in, v_in))

    @pl.when(tip)
    def _():
        for t, src in enumerate((q_in, k_in, v_in, g_in)):
            for row in range(SLOTS):
                pltpu.make_async_remote_copy(
                    src_ref=src.at[(1 - core) * SLOTS + row, :, pl.ds(tip_base, FAR)], dst_ref=far_out.at[t, row],
                    send_sem=far_send, recv_sem=far_recv, device_id=(partner,), device_id_type=MESH).start()

    for copy in tables:
        copy.wait()
    rev = eye_rev(BF16)
    for p in range(2):
        pair_tab = pltpu.einshape("abc->bac", r_buf[p])
        for hh in range(PAIR):
            for blk in range(SEQ // HEAD):
                part = pair_tab[hh, SEQ - HEAD * (blk + 1):SEQ - HEAD * blk]
                flipped = dot(rev, part).astype(BF16)
                rev_s[2 * p + hh, HEAD * blk:HEAD * (blk + 1), :] = flipped
                rt_s[2 * p + hh, :, HEAD * blk:HEAD * (blk + 1)] = flipped.T
    dr_acc[...] = jnp.zeros_like(dr_acc)

    acts = (dk_out, dv_out, o_out, dq_out)

    def send_out(sub, which):
        place = (core * SLOTS + sub % SLOTS, slice(None), 2 * col + sub // SLOTS)
        for t in which:
            pltpu.make_async_copy(buf.at[t, sub, my_rows], acts[t].at[place], out_recv).start()
        for peer in peers():
            peer_rows = pl.ds(pl.multiple_of((peer % PLANE) * ROWS, ROWS), ROWS)
            to_tip = (peer // 2 == 7 * z) & jnp.logical_not(tip)
            for t in which:
                @pl.when(jnp.logical_not(to_tip & (lower if t >= 2 else upper)))
                def _():
                    pltpu.make_async_remote_copy(
                        src_ref=buf.at[t, sub, peer_rows], dst_ref=acts[t].at[place],
                        send_sem=out_send, recv_sem=out_recv, device_id=(peer,), device_id_type=MESH).start()

    def send_up(sub):
        wait_for(buf.at[0:2, sub], in_recv.at[0, sub])
        for j in range(2):
            pltpu.make_async_remote_copy(src_ref=buf.at[j, sub], dst_ref=rbuf.at[j, sub], send_sem=up_send.at[sub % 4], recv_sem=up_recv.at[sub],
                                         device_id=(across,), device_id_type=MESH).start()

    def unpack(ref, j, sub):
        return pltpu.einshape("abc->bac", ref[j, sub])

    def load_rows(q_ref, q_j, g_ref, g_j, sub, start, turned):
        rows = slice(start, start + HALF)
        p = sub // SLOTS
        q2 = unpack(q_ref, q_j, sub)
        u = u_buf[2 * col + p].astype(F32)
        w = w_buf[2 * col + p].astype(F32)
        for hh in range(PAIR):
            q32 = q2[hh].astype(F32)
            a = (q32 + u[hh:hh + 1]).astype(BF16)
            c = (q32 + w[hh:hh + 1]).astype(BF16)
            a_s[hh, rows, :] = a
            c_s[hh, rows, :] = c
            at_s[hh, :, rows] = a.T
            if turned:
                ct_s[hh, :, rows] = flip8(c.astype(F32)).astype(BF16).T
        g2 = unpack(g_ref, g_j, sub)
        g_s[:, rows, :] = g2
        for hh in range(PAIR):
            gt_s[hh, :, rows] = g2[hh].T

    def load_keys(k_ref, k_j, v_ref, v_j, sub, start):
        rows = slice(start, start + HALF)
        k2 = unpack(k_ref, k_j, sub)
        v2 = unpack(v_ref, v_j, sub)
        k_s[:, rows, :] = k2
        v_s[:, rows, :] = v2
        for hh in range(PAIR):
            kt_s[hh, :, rows] = k2[hh].T
            vt_s[hh, :, rows] = v2[hh].T

    def row_block(hh, head, start, i0, lo, fresh, stats):
        width = i0 + QB
        rows = slice(start, start + QB)
        s_ref[:, :width] = dot(a_s[hh, rows, :], kt_s[hh, :, :width])
        e_ref[:, :width] = dot(c_s[hh, rows, :], rt_s[head, :, SEQ - width:])
        dp_ref[:, :width] = dot(g_s[hh, rows, :], vt_s[hh, :, :width])
        for r0 in range(0, QB, 16):
            group = slice(r0, r0 + 16)
            rel = pltpu.roll(e_ref[group, :width], i0 + 1 + r0, 1, stride=1, stride_axis=0)
            s = s_ref[group, :width] + rel
            ahead = lax.broadcasted_iota(jnp.int32, (16, width), 1) - lax.broadcasted_iota(jnp.int32, (16, width), 0)
            s = jnp.where(ahead <= i0 + r0, s, -jnp.inf)
            top = jnp.max(s, axis=1, keepdims=True)
            p = jnp.exp2((s - top) * (scale * LOG2E))
            total = jnp.sum(p, axis=1, keepdims=True)
            p = p * (1.0 / total)
            pb_ref[group, :width] = p.astype(BF16)
            dp = dp_ref[group, :width]
            row_dot = jnp.sum(p * dp, axis=1, keepdims=True)
            ds = (p * (dp - row_dot) * scale).astype(BF16)
            ds_ref[group, :width] = ds
            flipped = flip8(ds.astype(F32))
            half = [pltpu.roll(flipped[8 * j:8 * j + 8], QB - 8 - r0 - 8 * j, 1, stride=1, stride_axis=0) for j in range(2)]
            dd_ref[group, :width] = jnp.concatenate(half, axis=0).astype(BF16)
            if stats:
                lane = lax.broadcasted_iota(jnp.int32, (16, HEAD), 1)
                st_ref[group, :] = jnp.where(lane == 0, top * (scale * LOG2E) + jnp.log2(total), row_dot)
        pb = pb_ref[:, :width]
        ds = ds_ref[:, :width]
        dd = dd_ref[:, :width]
        stage[0, hh, rows, :] = dot(pb, v_s[hh, :width, :]).astype(BF16)
        dqc = dot(ds, k_s[hh, :width, :])
        dqr = flip8(dot(dd, rev_s[head, SEQ - width:, :]))
        stage[1, hh, rows, :] = (dqc + dqr).astype(BF16)
        dr_acc[head, 1, HEAD:HEAD + 1, HALF - HEAD:] += jnp.sum(dqc, axis=0, keepdims=True)
        dr_acc[head, 1, HEAD + 1:HEAD + 2, HALF - HEAD:] += jnp.sum(dqr, axis=0, keepdims=True)
        dk_new = dot(at_s[hh, :, rows], ds_ref[:, lo:width])
        dv_new = dot(gt_s[hh, :, rows], pb_ref[:, lo:width])
        if fresh:
            dkt[hh] = dk_new
            dvt[hh] = dv_new
        else:
            dkt[hh, :, :width - lo] += dk_new
            dvt[hh, :, :width - lo] += dv_new
        dr_new = dot(ct_s[hh, :, rows], dd)
        if width > HALF:
            dr_acc[head, 0, :HEAD, SEQ - width:] += dr_new[:, :width - HALF]
            dr_acc[head, 1, :HEAD, :] += dr_new[:, width - HALF:]
        else:
            dr_acc[head, 1, :HEAD, HALF - width:] += dr_new

    def col_block(hh, head, sub, i0):
        rows = slice(i0, i0 + QB)
        first = WIN - i0
        s_ref[:, :HALF] = dot(a_s[hh, rows, :], kt_s[hh, :, :HALF])
        e_ref[:, :WIN] = dot(c_s[hh, rows, :], rt_s[head, :, first:first + WIN])
        dp_ref[:, :HALF] = dot(g_s[hh, rows, :], vt_s[hh, :, :HALF])
        st_ref[:, :8] = st_rx[sub, hh, :, i0 - HALF:i0 - HALF + QB].T
        for r0 in range(0, QB, 16):
            group = slice(r0, r0 + 16)
            rel = pltpu.roll(e_ref[group, :WIN], HALF + 1 + r0, 1, stride=1, stride_axis=0)[:, :HALF]
            log_sum = st_ref[group, 0:1]
            row_dot = st_ref[group, 1:2]
            p = jnp.exp2((s_ref[group, :HALF] + rel) * (scale * LOG2E) - log_sum)
            pb_ref[group, :HALF] = p.astype(BF16)
            ds_ref[group, :HALF] = (p * (dp_ref[group, :HALF] - row_dot) * scale).astype(BF16)
        dkt[hh] += dot(at_s[hh, :, rows], ds_ref[:, :HALF])
        dvt[hh] += dot(gt_s[hh, :, rows], pb_ref[:, :HALF])

    def store_rows(sub):
        for t in range(2):
            buf[2 + t, sub] = pltpu.einshape("abc->bac", stage[t])

    def store_keys(sub):
        for hh in range(PAIR):
            stage[2, hh] = dkt[hh].astype(BF16).T
            stage[3, hh] = dvt[hh].astype(BF16).T
        for t in range(2):
            buf[t, sub] = pltpu.einshape("abc->bac", stage[2 + t])

    def wait_up(sub):
        wait_for(rbuf.at[:, sub], up_recv.at[sub])
        wait_for(rbuf.at[:, sub], up_send.at[sub % 4])

    def wait_in(sub):
        wait_for(buf.at[2:4, sub], in_recv.at[1, sub])

    def lower_rows(sub):
        wait_in(sub)
        load_rows(buf, 2, buf, 3, sub, 0, True)

    def lower_own(sub):
        load_keys(buf, 0, buf, 1, sub, 0)

        def own(hh, carry):
            head = 2 * (sub // SLOTS) + hh
            row_block(hh, head, QB, QB, 0, True, False)
            row_block(hh, head, 0, 0, 0, False, False)
            return carry

        lax.fori_loop(0, PAIR, own, 0)
        store_rows(sub)

    def lower_theirs(sub):
        wait_up(sub)
        load_rows(rbuf, 0, rbuf, 1, sub, HALF, False)
        wait_for(st_rx.at[sub], st_recv.at[sub])

        def theirs(hh, carry):
            head = 2 * (sub // SLOTS) + hh
            col_block(hh, head, sub, HALF)
            col_block(hh, head, sub, HALF + QB)
            return carry

        lax.fori_loop(0, PAIR, theirs, 0)
        store_keys(sub)

    def upper_own(sub):
        wait_in(sub)
        wait_up(sub)
        load_rows(buf, 0, buf, 1, sub, 0, True)
        load_keys(rbuf, 0, rbuf, 1, sub, 0)
        load_keys(buf, 2, buf, 3, sub, HALF)

        def own(hh, carry):
            head = 2 * (sub // SLOTS) + hh
            for blk in (1, 0):
                row_block(hh, head, QB * blk, HALF + QB * blk, HALF, blk == 1, True)
                st_tx[sub, hh, :, QB * blk:QB * (blk + 1)] = st_ref[...].T[:8]
            pltpu.make_async_remote_copy(src_ref=st_tx.at[sub, hh], dst_ref=st_rx.at[sub, hh], send_sem=st_send, recv_sem=st_recv.at[sub],
                                         device_id=(across,), device_id_type=MESH).start()

            @pl.when(jnp.logical_not(tip))
            def _():
                pltpu.make_async_remote_copy(src_ref=st_tx.at[sub, hh, :, HALF - TIP:], dst_ref=tip_st.at[col, sub, hh], send_sem=ts_send,
                                             recv_sem=ts_recv, device_id=(N_DEV - 2 + core,), device_id_type=MESH).start()
            return carry

        lax.fori_loop(0, PAIR, own, 0)
        store_rows(sub)
        store_keys(sub)

    side = 1 - core
    parts = (dr0_out, dr1_out, dr2_out, dr3_out, dr4_out, dr5_out)

    def swap_start(p):
        for n in range(2):
            pltpu.make_async_remote_copy(src_ref=dr_acc.at[2 * p + n, side], dst_ref=dr_rx.at[p, n], send_sem=x_send.at[p], recv_sem=x_recv.at[p],
                                         device_id=(partner,), device_id_type=MESH).start()

    def swap_add(p):
        wait_for(dr_rx.at[p], x_recv.at[p])
        for n in range(2):
            dr_rx[p, n] = dr_rx[p, n] + dr_acc[2 * p + n, core]

    def cross_start(p):
        pltpu.make_async_remote_copy(src_ref=dr_rx.at[p, 1 - z], dst_ref=dr_rz.at[p], send_sem=z_send.at[p], recv_sem=z_recv.at[p],
                                     device_id=(across,), device_id_type=MESH).start()

    def head_of(p, bits):
        other = chip ^ bits
        return 4 * (other % 4) + 2 * p + other // 4

    def block(p, m, bits):
        if bits == 0:
            return dr_fin.at[p, PART * m:PART * (m + 1)]
        return parts[m].at[side, :, head_of(p, bits)]

    def forward(p, m, bits):
        pltpu.make_async_remote_copy(src_ref=block(p, m, bits), dst_ref=parts[m].at[side, :, head_of(p, bits)], send_sem=fw_send.at[p, m // 3],
                                     recv_sem=fw_recv.at[p, m // 3], device_id=(partner,), device_id_type=MESH).start()

    def blocks(count):
        return parts[0].at[:, :, :N_PART // 2 * count]

    def pass_on(p, bits, hop, device):
        for m in range(N_PART):
            pltpu.make_async_remote_copy(
                src_ref=block(p, m, bits), dst_ref=parts[m].at[side, :, head_of(p, bits)], send_sem=ring_send.at[p, hop],
                recv_sem=ring_recv.at[p, hop], device_id=(device,), device_id_type=MESH).start()

    def hand_over(p, bits):
        for m in range(N_PART):
            forward(p, m, bits)

    even = chip % 2 == z
    loaded = y != z
    along_x, along_y = me ^ 2, me ^ 4

    def hop_start(p, hop):
        if hop == 0:
            for device in (along_x, along_y, across):
                pass_on(p, 0, 0, device)
        if hop == 1:
            @pl.when(even & loaded)
            def _():
                pass_on(p, 1, 1, along_y)

            @pl.when(jnp.logical_not(even) & loaded)
            def _():
                pass_on(p, 2, 1, along_x)

            pass_on(p, 1, 1, across)
            pass_on(p, 2, 1, across)
        if hop == 2:
            @pl.when(even & loaded)
            def _():
                pass_on(p, 5, 2, along_y)

            @pl.when(jnp.logical_not(even) & loaded)
            def _():
                pass_on(p, 6, 2, along_x)

            @pl.when(even)
            def _():
                pass_on(p, 3, 2, across)
        if hop == 3:
            @pl.when(even)
            def _():
                pass_on(p, 7, 3, across)

    def hop_wait(p, hop):
        if hop == 0:
            wait_for(blocks(3), ring_recv.at[p, 0])
            for bits in (1, 2, 4):
                hand_over(p, bits)
        if hop == 1:
            @pl.when(even)
            def _():
                wait_for(blocks(3), ring_recv.at[p, 1])
                hand_over(p, 3)

            @pl.when(jnp.logical_not(even))
            def _():
                wait_for(blocks(2), ring_recv.at[p, 1])
            for bits in (5, 6):
                hand_over(p, bits)
        if hop == 2:
            wait_for(blocks(1), ring_recv.at[p, 2])
            hand_over(p, 7)
        if hop == 3:
            @pl.when(jnp.logical_not(even))
            def _():
                wait_for(blocks(1), ring_recv.at[p, 3])
                hand_over(p, 3)

    def sent_wait(p):
        wait_for(blocks(3), ring_send.at[p, 0])

        @pl.when(loaded)
        def _():
            wait_for(blocks(3), ring_send.at[p, 1])

        @pl.when(jnp.logical_not(loaded))
        def _():
            wait_for(blocks(2), ring_send.at[p, 1])

        @pl.when(even & loaded)
        def _():
            wait_for(blocks(2), ring_send.at[p, 2])

        @pl.when(even != loaded)
        def _():
            wait_for(blocks(1), ring_send.at[p, 2])

        @pl.when(even)
        def _():
            wait_for(blocks(1), ring_send.at[p, 3])

    def cross_finish(p):
        wait_for(dr_rz.at[p], z_recv.at[p])
        total = dr_rx[p, z] + dr_rz[p]
        rev32 = eye_rev(F32)
        for m in range(HALF // HEAD):
            part = total[:HEAD, HALF - HEAD * (m + 1):HALF - HEAD * m]
            turned = lax.dot_general(rev32, part, (((1,), (1,)), ((), ())), precision=lax.Precision.HIGHEST, preferred_element_type=F32)
            dr_fin[p, HEAD * m:HEAD * (m + 1)] = turned.reshape(HEAD, 1, HEAD)
        dr_fin[p, HALF] = total[HEAD:HEAD + 1, HALF - HEAD:]
        dr_fin[p, HALF + 1] = total[HEAD + 1:HEAD + 2, HALF - HEAD:]
        dr_fin[p, HALF + 2:] = jnp.zeros((FIN - HALF - 2, 1, HEAD), F32)
        hop_start(p, 0)
        for m in range(N_PART):
            pltpu.make_async_copy(block(p, m, 0), parts[m].at[side, :, head_of(p, 0)], own_sem.at[p]).start()
        hand_over(p, 0)

    def tip_load(unit):
        slot, row, far = unit % 2, unit // FAR, unit % FAR
        pair = far + tip_base
        for t, src in enumerate((q_in, k_in, v_in, g_in)):
            pltpu.make_async_copy(src.at[core * SLOTS + row, :, pair], r_buf.at[slot, pl.ds(TIP * t + ROWS * core, ROWS)], tip_sem.at[slot]).start()
            pltpu.make_async_copy(far_out.at[t, row, :, far], r_buf.at[slot, pl.ds(TIP * t + ROWS * (1 - core), ROWS)], tip_sem.at[slot]).start()
        pltpu.make_async_copy(r_in.at[:TIP, pair], r_buf.at[slot, 4 * TIP:5 * TIP], tip_sem.at[slot]).start()

    def tip_done(slot):
        wait_for(r_buf.at[slot, :TIP], tip_near.at[slot])
        wait_for(r_buf.at[slot, :TIP], tip_send.at[slot])

    def tip_group(hh, r0):
        group = slice(TIP * hh + r0, TIP * hh + r0 + 16)
        rel = pltpu.roll(e_ref[group, :TIP], 1 + r0, 1, stride=1, stride_axis=0)
        ahead = lax.broadcasted_iota(jnp.int32, (16, TIP), 1) - lax.broadcasted_iota(jnp.int32, (16, TIP), 0)
        return group, s_ref[group, :TIP] + rel, ahead <= r0

    def tip_rows(hh):
        for r0 in range(0, TIP, 16):
            group, s, seen = tip_group(hh, r0)
            s = jnp.where(seen, s, -jnp.inf)
            top = jnp.max(s, axis=1, keepdims=True)
            p = jnp.exp2((s - top) * (scale * LOG2E))
            p = p * (1.0 / jnp.sum(p, axis=1, keepdims=True))
            pb_ref[group, :TIP] = p.astype(BF16)
            dp = dp_ref[group, :TIP]
            row_dot = jnp.sum(p * dp, axis=1, keepdims=True)
            ds = (p * (dp - row_dot) * scale).astype(BF16)
            ds_ref[group, :TIP] = ds
            flipped = flip8(ds.astype(F32))
            half = [pltpu.roll(flipped[8 * j:8 * j + 8], TIP - 8 - r0 - 8 * j, 1, stride=1, stride_axis=0) for j in range(2)]
            dd_ref[group, :TIP] = jnp.concatenate(half, axis=0).astype(BF16)
        rows = slice(TIP * hh, TIP * (hh + 1))
        stage[0, hh, :TIP, :] = dot(pb_ref[rows, :TIP], v_s[hh, :TIP, :]).astype(BF16)
        dqc = dot(ds_ref[rows, :TIP], k_s[hh, :TIP, :])
        dqr = flip8(dot(dd_ref[rows, :TIP], c_s[hh, :TIP, :]))
        stage[1, hh, :TIP, :] = (dqc + dqr).astype(BF16)

    def tip_keys(hh, stats):
        rows = slice(TIP * hh, TIP * (hh + 1))
        st_ref[rows, :8] = stats.T
        for r0 in range(0, TIP, 16):
            group, s, seen = tip_group(hh, r0)
            p = jnp.where(seen, jnp.exp2(s * (scale * LOG2E) - st_ref[group, 0:1]), 0.0)
            pb_ref[group, :TIP] = p.astype(BF16)
            ds_ref[group, :TIP] = (p * (dp_ref[group, :TIP] - st_ref[group, 1:2]) * scale).astype(BF16)
        over_rows = (((0,), (0,)), ((), ()))
        stage[0, hh, :TIP, :] = lax.dot_general(ds_ref[rows, :TIP], a_s[hh, :TIP, :], over_rows, preferred_element_type=F32).astype(BF16)
        stage[1, hh, :TIP, :] = lax.dot_general(pb_ref[rows, :TIP], g_s[hh, :TIP, :], over_rows, preferred_element_type=F32).astype(BF16)

    def tip_unit(unit, carry):
        slot, row, far = unit % 2, unit // FAR, unit % FAR
        pair = far + tip_base
        wait_for(r_buf.at[slot, :5 * TIP], tip_sem.at[slot])

        @pl.when(unit + 1 < UNITS)
        def _():
            tip_load(unit + 1)

        q2, k2, v2, g2, r2 = [pltpu.einshape("abc->bac", r_buf[slot, TIP * t:TIP * (t + 1)]) for t in range(5)]
        u = u_buf[pair].astype(F32)
        w = w_buf[pair].astype(F32)
        for hh in range(PAIR):
            rows = slice(TIP * hh, TIP * (hh + 1))
            q32 = q2[hh].astype(F32)
            a = (q32 + u[hh:hh + 1]).astype(BF16)
            c = (q32 + w[hh:hh + 1]).astype(BF16)
            falling = dot(eye_rev(BF16), r2[hh]).astype(BF16)
            s_ref[rows, :TIP] = dot(a, k2[hh].T)
            e_ref[rows, :TIP] = dot(c, falling.T)
            dp_ref[rows, :TIP] = dot(g2[hh], v2[hh].T)
            a_s[hh, :TIP, :] = a
            c_s[hh, :TIP, :] = falling
            g_s[hh, :TIP, :] = g2[hh]
            k_s[hh, :TIP, :] = k2[hh]
            v_s[hh, :TIP, :] = v2[hh]

        @pl.when(lower)
        def _():
            for hh in range(PAIR):
                tip_rows(hh)

        @pl.when(upper)
        def _():
            for hh in range(PAIR):
                tip_keys(hh, tip_st[far // 2, (far % 2) * SLOTS + row, hh])

        @pl.when(unit >= 2)
        def _():
            tip_done(slot)

        for n in range(2):
            r_buf[slot, (5 + n) * TIP:(6 + n) * TIP] = pltpu.einshape("abc->bac", stage[n, :, :TIP, :])
        place = (core * SLOTS + row, slice(None), pair)

        def give(results):
            for n, dst in enumerate(results):
                pltpu.make_async_copy(r_buf.at[slot, pl.ds((5 + n) * TIP + ROWS * core, ROWS)], dst.at[place], tip_near.at[slot]).start()
                pltpu.make_async_remote_copy(
                    src_ref=r_buf.at[slot, pl.ds((5 + n) * TIP + ROWS * (1 - core), ROWS)], dst_ref=dst.at[place],
                    send_sem=tip_send.at[slot], recv_sem=out_recv, device_id=(partner,), device_id_type=MESH).start()

        @pl.when(lower)
        def _():
            give((o_out, dq_out))

        @pl.when(upper)
        def _():
            give((dk_out, dv_out))
        return carry

    def tips(third):
        @pl.when(tip)
        def _():
            if third == 0:
                wait_for(far_out, far_recv)

                @pl.when(upper)
                def _():
                    wait_for(tip_st, ts_recv)
                tip_load(0)
            lax.fori_loop(UNITS // 3 * third, UNITS // 3 * (third + 1), tip_unit, 0)
            if third == 2:
                tip_done(0)
                tip_done(1)

    send_up(0)

    def sub_body(sub, carry):
        @pl.when(sub < SUBS - 1)
        def _():
            send_up(sub + 1)

        @pl.when(sub == SLOTS)
        def _():
            swap_start(0)

        @pl.when(sub == SUBS - 1)
        def _():
            swap_add(0)
            cross_start(0)

        @pl.when(sub == SUBS)
        def _():
            swap_start(1)
            cross_finish(0)
            swap_add(1)
            cross_start(1)

        @pl.when(lower & (sub < SUBS))
        def _():
            lower_rows(sub)

        @pl.when(lower & (sub > 0))
        def _():
            lower_theirs(sub - 1)

        @pl.when(lower & (sub < SUBS))
        def _():
            lower_own(sub)

        @pl.when(upper & (sub < SUBS))
        def _():
            upper_own(sub)

        @pl.when(sub < EARLY)
        def _():
            send_out(sub, (2, 3))

        @pl.when((sub > 0) & (sub <= EARLY))
        def _():
            send_out(sub - 1, (0, 1))
        return carry

    lax.fori_loop(0, SUBS + 1, sub_body, 0)

    send_out(EARLY, (2, 3))
    cross_finish(1)
    send_out(EARLY, (0, 1))
    for p in range(2):
        hop_wait(p, 0)
        hop_start(p, 1)
    for p in range(2):
        send_out(EARLY + 1 + p, range(4))
        tips(p)
        hop_wait(p, 1)
        hop_start(p, 2)

    def send_late(sub, carry):
        send_out(sub, range(4))
        return carry

    lax.fori_loop(EARLY + 3, SUBS, send_late, 0)
    tips(2)
    for p in range(2):
        hop_wait(p, 2)
        hop_start(p, 3)
    for p in range(2):
        hop_wait(p, 3)

    wait_for(buf.at[:, :, :HALF - ROWS], in_send)

    @pl.when(tip)
    def _():
        wait_for(buf.at[:, :, :HALF - 3 * ROWS // 2], out_recv)
        wait_for(buf.at[:, :, :HALF - ROWS], out_send)
        wait_for(far_out, far_send)

    @pl.when(jnp.logical_not(tip))
    def _():
        wait_for(buf, out_recv)
        wait_for(buf.at[:, :, :HALF - 2 * ROWS], out_send)

    @pl.when(upper & jnp.logical_not(tip))
    def _():
        wait_for(st_tx.at[:2], ts_send)

    @pl.when(upper)
    def _():
        wait_for(st_tx, st_send)

    for p in range(2):
        wait_for(dr_rx.at[p], x_send.at[p])
        wait_for(dr_rz.at[p], z_send.at[p])
        wait_for(blocks(1), own_sem.at[p])
        sent_wait(p)
        for n in range(2):
            wait_for(blocks(N_PAIR // 2), fw_send.at[p, n])
            wait_for(blocks(N_PAIR // 2), fw_recv.at[p, n])


def writer(*refs):
    ins, (o, dq, dk, dv, dr, du, dw, sem) = refs[:4 + N_PART], refs[4 + N_PART:]
    pairs = list(zip(ins[:4], (o, dq, dk, dv)))
    for m, part in enumerate(ins[4:]):
        rows = min(PART, HALF - PART * m)
        for side in range(2):
            start = HALF * side + PART * m
            pairs.append((part.at[side, :rows], dr.at[start:start + rows]))
    last = HALF - PART * (N_PART - 1)
    pairs += [(ins[-1].at[0, last], du), (ins[-1].at[0, last + 1], dw)]
    copies = [pltpu.make_async_copy(src, dst, sem.at[j]) for j, (src, dst) in enumerate(pairs)]
    for copy in copies:
        copy.start()
    for copy in copies:
        copy.wait()


def solution(mesh):
    seq_spec = P(None, "cp", None, None)

    def local(query, key_in, value, bias_u, bias_w, rel_k, d_out):
        n_batch, rows, n_heads, head_dim = query.shape
        pairs = (n_batch, rows, N_PAIR, PAIR, head_dim)
        vm = pltpu.VMEM
        dma = pltpu.SemaphoreType.DMA
        whole = pl.BlockSpec(memory_space=pl.ANY)
        act = jax.ShapeDtypeStruct(pairs, BF16)
        vec = jax.ShapeDtypeStruct((n_heads, 1, head_dim), F32)
        tok = (PAIR, SEQ, HEAD)
        tok_t = (PAIR, HEAD, SEQ)
        acc = (HEAD + 8, HALF)
        outs = pl.pallas_call(
            kernel,
            name="rel_attn",
            out_shape=(act, act, act, act,
                       *[jax.ShapeDtypeStruct((2, PART, n_heads, 1, head_dim), F32)] * N_PART,
                       jax.ShapeDtypeStruct((4, SLOTS, ROWS, FAR, PAIR, HEAD), BF16)),
            in_specs=[pl.BlockSpec(memory_space=pltpu.HBM)] * 7,
            out_specs=[whole] * (5 + N_PART),
            scratch_shapes=[
                vm((4, SUBS, HALF, PAIR, HEAD), BF16), vm((2, SUBS, HALF, PAIR, HEAD), BF16),
                vm((2, SEQ, PAIR, HEAD), BF16), vm((N_PAIR, PAIR, HEAD), BF16), vm((N_PAIR, PAIR, HEAD), BF16),
                vm((SUBS, PAIR, 8, HALF), F32), vm((SUBS, PAIR, 8, HALF), F32), vm((3, SUBS, PAIR, 8, TIP), F32), vm((QB, HEAD), F32),
                vm((2, 2) + acc, F32), vm((2,) + acc, F32), vm((2, FIN, 1, HEAD), F32), vm((4, 2) + acc, F32),
                vm((QB, SEQ), F32), vm((QB, SEQ), F32), vm((QB, SEQ), F32),
                vm((QB, SEQ), BF16), vm((QB, SEQ), BF16), vm((QB, SEQ), BF16),
                vm(tok, BF16), vm(tok, BF16), vm(tok, BF16), vm(tok, BF16), vm(tok, BF16),
                vm(tok_t, BF16), vm(tok_t, BF16), vm(tok_t, BF16), vm(tok_t, BF16), vm(tok_t, BF16),
                vm((4, SEQ, HEAD), BF16), vm((4, HEAD, SEQ), BF16),
                vm((PAIR, HEAD, HALF), F32), vm((PAIR, HEAD, HALF), F32), vm((4, PAIR, HALF, HEAD), BF16),
                dma, dma((2, SUBS)), dma, dma, dma((2,)), dma((4,)), dma((4,)), dma((SUBS,)), dma, dma((SUBS,)),
                dma((2,)), dma((2,)), dma((2,)), dma((2,)), dma((2, 4)), dma((2, 4)), dma((2, 2)), dma((2, 2)),
                dma, dma, dma((2,)), dma((2,)), dma((2,)), dma, dma,
            ],
            compiler_params=pltpu.CompilerParams(collective_id=0, has_side_effects=True, vmem_limit_bytes=37 * 1024 * 1024),
        )(*[pltpu.with_memory_space_constraint(x, pltpu.HBM) for x in (
            query.reshape(pairs), key_in.reshape(pairs), value.reshape(pairs), d_out.reshape(pairs),
            rel_k.reshape(SEQ, N_PAIR, PAIR, head_dim), bias_u.reshape(N_PAIR, PAIR, head_dim), bias_w.reshape(N_PAIR, PAIR, head_dim))])
        o, dq, dk, dv, dr, du, dw = pl.pallas_call(
            writer,
            name="writer",
            out_shape=(act, act, act, act, jax.ShapeDtypeStruct((SEQ, n_heads, 1, head_dim), F32), vec, vec),
            in_specs=[whole] * (4 + N_PART),
            out_specs=[whole] * 7,
            scratch_shapes=[dma((6 + 2 * N_PART,))],
            compiler_params=pltpu.CompilerParams(vmem_limit_bytes=1024 * 1024),
        )(*outs[:-1])
        full = query.shape
        return (o.reshape(full), dq.reshape(full), dk.reshape(full), dv.reshape(full),
                du.reshape(bias_u.shape), dw.reshape(bias_w.shape), dr.reshape(rel_k.shape))

    return jax.shard_map(local, mesh=mesh,
                         in_specs=(seq_spec, seq_spec, seq_spec, P(), P(), P(), seq_spec),
                         out_specs=(seq_spec, seq_spec, seq_spec, seq_spec, P(), P(), P()),
                         check_vma=False)
```

```python
import jax
import jax.numpy as jnp
from jax import lax
from jax.experimental import pallas as pl
from jax.experimental.pallas import tpu as pltpu
from jax.sharding import PartitionSpec as P

MESH = pl.DeviceIdType.MESH
BF16, F32 = jnp.bfloat16, jnp.float32
LOG2E = 1.4426950408889634

N_DEV = 16
PLANE = 8
PAIR = 2
N_PAIR = 8
SLOTS = 4
SUBS = 2 * SLOTS
EARLY = 3
ROWS = 64
HALF = PLANE * ROWS
SEQ = 2 * HALF
HEAD = 128
QB = 256
WIN = HALF + QB
N_PART = 6
PART = 86
FIN = N_PART * PART
TIP = 2 * ROWS
FAR = N_PAIR - 2
UNITS = FAR * SLOTS
TURNS = ((1, 3, 2), (3, 1, 2))


def dot(lhs, rhs):
    return jnp.dot(lhs, rhs, preferred_element_type=F32)


def flip8(x):
    rows, cols = x.shape
    idx = 7 - lax.broadcasted_iota(jnp.int32, (rows // 8, 8, cols), 1)
    return jnp.take_along_axis(x.reshape(rows // 8, 8, cols), idx, axis=1).reshape(rows, cols)


def eye_rev(dtype):
    total = lax.broadcasted_iota(jnp.int32, (HEAD, HEAD), 0) + lax.broadcasted_iota(jnp.int32, (HEAD, HEAD), 1)
    return jnp.where(total == HEAD - 1, 1.0, 0.0).astype(dtype)


def kernel(q_in, k_in, v_in, g_in, r_in, u_in, w_in,
           o_out, dq_out, dk_out, dv_out, dr0_out, dr1_out, dr2_out, dr3_out, dr4_out, dr5_out, far_out,
           buf, rbuf, r_buf, u_buf, w_buf, st_tx, st_rx, tip_st, st_ref, dr_rx, dr_rz, dr_fin, dr_acc,
           s_ref, e_ref, dp_ref, pb_ref, ds_ref, dd_ref,
           a_s, c_s, g_s, k_s, v_s, at_s, ct_s, gt_s, kt_s, vt_s, rev_s, rt_s, dkt, dvt, stage,
           in_send, in_recv, out_send, out_recv, own_sem, r_sem, up_send, up_recv, st_send, st_recv,
           x_send, x_recv, z_send, z_recv, ring_send, ring_recv, fw_send, fw_recv,
           far_send, far_recv, tip_sem, tip_near, tip_send, ts_send, ts_recv):
    me = lax.axis_index("cp")
    core = me % 2
    chip = me // 2
    col = chip % 4
    z = chip // 4
    partner = me + 1 - 2 * core
    across = me + PLANE * (1 - 2 * z)
    scale = HEAD ** -0.5

    def wait_for(ref, sem):
        pltpu.make_async_copy(ref, ref, sem).wait()

    y = col // 2
    lower, upper = z == 0, z == 1
    tip = chip == 7 * z
    tip_base = 2 - 2 * z

    tables = [pltpu.make_async_copy(src, dst, r_sem.at[j]) for j, (src, dst) in enumerate(
        ((r_in.at[:, 2 * col], r_buf.at[0]), (r_in.at[:, 2 * col + 1], r_buf.at[1]), (u_in, u_buf), (w_in, w_buf)))]
    for copy in tables:
        copy.start()

    barrier = pltpu.get_barrier_semaphore()

    for peer in [across] + [me ^ step for step in range(PLANE - 1, 0, -1)]:
        pl.semaphore_signal(barrier, inc=1, device_id=(peer,), device_id_type=MESH)
    pl.semaphore_wait(barrier, PLANE)

    my_rows = pl.ds(pl.multiple_of((me % PLANE) * ROWS, ROWS), ROWS)

    def peers():
        for near_turn, far_turn in zip(*TURNS):
            turn = jnp.where(core == 0, near_turn, far_turn)
            yield me ^ (2 * turn)
            yield me ^ (2 * turn + 1)
        yield partner

    def send_in(ins, sub):
        pair, row = sub // SLOTS, sub % SLOTS
        for first in (0, 2):
            for t in (first, first + 1):
                pltpu.make_async_copy(ins[t].at[core * SLOTS + row, :, 2 * col + pair], buf.at[t, sub, my_rows], in_recv.at[first // 2, sub]).start()
            for peer in peers():
                for t in (first, first + 1):
                    pltpu.make_async_remote_copy(
                        src_ref=ins[t].at[(peer % 2) * SLOTS + row, :, 2 * ((peer // 2) % 4) + pair], dst_ref=buf.at[t, sub, my_rows],
                        send_sem=in_send, recv_sem=in_recv.at[first // 2, sub], device_id=(peer,), device_id_type=MESH).start()

    def send_all(ins):
        def send_sub(sub, carry):
            send_in(ins, sub)
            return carry
        lax.fori_loop(0, SUBS, send_sub, 0)

    @pl.when(lower)
    def _():
        send_all((k_in, v_in, q_in, g_in))

    @pl.when(upper)
    def _():
        send_all((q_in, g_in, k_in, v_in))

    @pl.when(tip)
    def _():
        for t, src in enumerate((q_in, k_in, v_in, g_in)):
            for row in range(SLOTS):
                pltpu.make_async_remote_copy(
                    src_ref=src.at[(1 - core) * SLOTS + row, :, pl.ds(tip_base, FAR)], dst_ref=far_out.at[t, row],
                    send_sem=far_send, recv_sem=far_recv, device_id=(partner,), device_id_type=MESH).start()

    for copy in tables:
        copy.wait()
    rev = eye_rev(BF16)
    for p in range(2):
        pair_tab = pltpu.einshape("abc->bac", r_buf[p])
        for hh in range(PAIR):
            for blk in range(SEQ // HEAD):
                part = pair_tab[hh, SEQ - HEAD * (blk + 1):SEQ - HEAD * blk]
                flipped = dot(rev, part).astype(BF16)
                rev_s[2 * p + hh, HEAD * blk:HEAD * (blk + 1), :] = flipped
                rt_s[2 * p + hh, :, HEAD * blk:HEAD * (blk + 1)] = flipped.T
    dr_acc[...] = jnp.zeros_like(dr_acc)

    acts = (dk_out, dv_out, o_out, dq_out)

    def send_out(sub, which):
        place = (core * SLOTS + sub % SLOTS, slice(None), 2 * col + sub // SLOTS)
        for t in which:
            pltpu.make_async_copy(buf.at[t, sub, my_rows], acts[t].at[place], out_recv).start()
        for peer in peers():
            peer_rows = pl.ds(pl.multiple_of((peer % PLANE) * ROWS, ROWS), ROWS)
            to_tip = (peer // 2 == 7 * z) & jnp.logical_not(tip)
            for t in which:
                @pl.when(jnp.logical_not(to_tip & (lower if t >= 2 else upper)))
                def _():
                    pltpu.make_async_remote_copy(
                        src_ref=buf.at[t, sub, peer_rows], dst_ref=acts[t].at[place],
                        send_sem=out_send, recv_sem=out_recv, device_id=(peer,), device_id_type=MESH).start()

    def send_up(sub):
        wait_for(buf.at[0:2, sub], in_recv.at[0, sub])
        for j in range(2):
            pltpu.make_async_remote_copy(src_ref=buf.at[j, sub], dst_ref=rbuf.at[j, sub], send_sem=up_send.at[sub % 4], recv_sem=up_recv.at[sub],
                                         device_id=(across,), device_id_type=MESH).start()

    def unpack(ref, j, sub):
        return pltpu.einshape("abc->bac", ref[j, sub])

    def load_rows(q_ref, q_j, g_ref, g_j, sub, start, turned):
        rows = slice(start, start + HALF)
        p = sub // SLOTS
        q2 = unpack(q_ref, q_j, sub)
        u = u_buf[2 * col + p].astype(F32)
        w = w_buf[2 * col + p].astype(F32)
        for hh in range(PAIR):
            q32 = q2[hh].astype(F32)
            a = (q32 + u[hh:hh + 1]).astype(BF16)
            c = (q32 + w[hh:hh + 1]).astype(BF16)
            a_s[hh, rows, :] = a
            c_s[hh, rows, :] = c
            at_s[hh, :, rows] = a.T
            if turned:
                ct_s[hh, :, rows] = flip8(c.astype(F32)).astype(BF16).T
        g2 = unpack(g_ref, g_j, sub)
        g_s[:, rows, :] = g2
        for hh in range(PAIR):
            gt_s[hh, :, rows] = g2[hh].T

    def load_keys(k_ref, k_j, v_ref, v_j, sub, start):
        rows = slice(start, start + HALF)
        k2 = unpack(k_ref, k_j, sub)
        v2 = unpack(v_ref, v_j, sub)
        k_s[:, rows, :] = k2
        v_s[:, rows, :] = v2
        for hh in range(PAIR):
            kt_s[hh, :, rows] = k2[hh].T
            vt_s[hh, :, rows] = v2[hh].T

    def row_block(hh, head, start, i0, lo, fresh, stats):
        width = i0 + QB
        rows = slice(start, start + QB)
        s_ref[:, :width] = dot(a_s[hh, rows, :], kt_s[hh, :, :width])
        e_ref[:, :width] = dot(c_s[hh, rows, :], rt_s[head, :, SEQ - width:])
        dp_ref[:, :width] = dot(g_s[hh, rows, :], vt_s[hh, :, :width])
        for r0 in range(0, QB, 16):
            group = slice(r0, r0 + 16)
            rel = pltpu.roll(e_ref[group, :width], i0 + 1 + r0, 1, stride=1, stride_axis=0)
            s = s_ref[group, :width] + rel
            ahead = lax.broadcasted_iota(jnp.int32, (16, width), 1) - lax.broadcasted_iota(jnp.int32, (16, width), 0)
            s = jnp.where(ahead <= i0 + r0, s, -jnp.inf)
            top = jnp.max(s, axis=1, keepdims=True)
            p = jnp.exp2((s - top) * (scale * LOG2E))
            total = jnp.sum(p, axis=1, keepdims=True)
            p = p * (1.0 / total)
            pb_ref[group, :width] = p.astype(BF16)
            dp = dp_ref[group, :width]
            row_dot = jnp.sum(p * dp, axis=1, keepdims=True)
            ds = (p * (dp - row_dot) * scale).astype(BF16)
            ds_ref[group, :width] = ds
            flipped = flip8(ds.astype(F32))
            half = [pltpu.roll(flipped[8 * j:8 * j + 8], QB - 8 - r0 - 8 * j, 1, stride=1, stride_axis=0) for j in range(2)]
            dd_ref[group, :width] = jnp.concatenate(half, axis=0).astype(BF16)
            if stats:
                lane = lax.broadcasted_iota(jnp.int32, (16, HEAD), 1)
                st_ref[group, :] = jnp.where(lane == 0, top * (scale * LOG2E) + jnp.log2(total), row_dot)
        pb = pb_ref[:, :width]
        ds = ds_ref[:, :width]
        dd = dd_ref[:, :width]
        stage[0, hh, rows, :] = dot(pb, v_s[hh, :width, :]).astype(BF16)
        dqc = dot(ds, k_s[hh, :width, :])
        dqr = flip8(dot(dd, rev_s[head, SEQ - width:, :]))
        stage[1, hh, rows, :] = (dqc + dqr).astype(BF16)
        dr_acc[head, 1, HEAD:HEAD + 1, HALF - HEAD:] += jnp.sum(dqc, axis=0, keepdims=True)
        dr_acc[head, 1, HEAD + 1:HEAD + 2, HALF - HEAD:] += jnp.sum(dqr, axis=0, keepdims=True)
        dk_new = dot(at_s[hh, :, rows], ds_ref[:, lo:width])
        dv_new = dot(gt_s[hh, :, rows], pb_ref[:, lo:width])
        if fresh:
            dkt[hh] = dk_new
            dvt[hh] = dv_new
        else:
            dkt[hh, :, :width - lo] += dk_new
            dvt[hh, :, :width - lo] += dv_new
        dr_new = dot(ct_s[hh, :, rows], dd)
        if width > HALF:
            dr_acc[head, 0, :HEAD, SEQ - width:] += dr_new[:, :width - HALF]
            dr_acc[head, 1, :HEAD, :] += dr_new[:, width - HALF:]
        else:
            dr_acc[head, 1, :HEAD, HALF - width:] += dr_new

    def col_block(hh, head, sub, i0):
        rows = slice(i0, i0 + QB)
        first = WIN - i0
        s_ref[:, :HALF] = dot(a_s[hh, rows, :], kt_s[hh, :, :HALF])
        e_ref[:, :WIN] = dot(c_s[hh, rows, :], rt_s[head, :, first:first + WIN])
        dp_ref[:, :HALF] = dot(g_s[hh, rows, :], vt_s[hh, :, :HALF])
        st_ref[:, :8] = st_rx[sub, hh, :, i0 - HALF:i0 - HALF + QB].T
        for r0 in range(0, QB, 16):
            group = slice(r0, r0 + 16)
            rel = pltpu.roll(e_ref[group, :WIN], HALF + 1 + r0, 1, stride=1, stride_axis=0)[:, :HALF]
            log_sum = st_ref[group, 0:1]
            row_dot = st_ref[group, 1:2]
            p = jnp.exp2((s_ref[group, :HALF] + rel) * (scale * LOG2E) - log_sum)
            pb_ref[group, :HALF] = p.astype(BF16)
            ds_ref[group, :HALF] = (p * (dp_ref[group, :HALF] - row_dot) * scale).astype(BF16)
        dkt[hh] += dot(at_s[hh, :, rows], ds_ref[:, :HALF])
        dvt[hh] += dot(gt_s[hh, :, rows], pb_ref[:, :HALF])

    def store_rows(sub):
        for t in range(2):
            buf[2 + t, sub] = pltpu.einshape("abc->bac", stage[t])

    def store_keys(sub):
        for hh in range(PAIR):
            stage[2, hh] = dkt[hh].astype(BF16).T
            stage[3, hh] = dvt[hh].astype(BF16).T
        for t in range(2):
            buf[t, sub] = pltpu.einshape("abc->bac", stage[2 + t])

    def wait_up(sub):
        wait_for(rbuf.at[:, sub], up_recv.at[sub])
        wait_for(rbuf.at[:, sub], up_send.at[sub % 4])

    def wait_in(sub):
        wait_for(buf.at[2:4, sub], in_recv.at[1, sub])

    def lower_rows(sub):
        wait_in(sub)
        load_rows(buf, 2, buf, 3, sub, 0, True)

    def lower_own(sub):
        load_keys(buf, 0, buf, 1, sub, 0)

        def own(hh, carry):
            head = 2 * (sub // SLOTS) + hh
            row_block(hh, head, QB, QB, 0, True, False)
            row_block(hh, head, 0, 0, 0, False, False)
            return carry

        lax.fori_loop(0, PAIR, own, 0)
        store_rows(sub)

    def lower_theirs(sub):
        wait_up(sub)
        load_rows(rbuf, 0, rbuf, 1, sub, HALF, False)
        wait_for(st_rx.at[sub], st_recv.at[sub])

        def theirs(hh, carry):
            head = 2 * (sub // SLOTS) + hh
            col_block(hh, head, sub, HALF)
            col_block(hh, head, sub, HALF + QB)
            return carry

        lax.fori_loop(0, PAIR, theirs, 0)
        store_keys(sub)

    def upper_own(sub):
        wait_in(sub)
        wait_up(sub)
        load_rows(buf, 0, buf, 1, sub, 0, True)
        load_keys(rbuf, 0, rbuf, 1, sub, 0)
        load_keys(buf, 2, buf, 3, sub, HALF)

        def own(hh, carry):
            head = 2 * (sub // SLOTS) + hh
            for blk in (1, 0):
                row_block(hh, head, QB * blk, HALF + QB * blk, HALF, blk == 1, True)
                st_tx[sub, hh, :, QB * blk:QB * (blk + 1)] = st_ref[...].T[:8]
            pltpu.make_async_remote_copy(src_ref=st_tx.at[sub, hh], dst_ref=st_rx.at[sub, hh], send_sem=st_send, recv_sem=st_recv.at[sub],
                                         device_id=(across,), device_id_type=MESH).start()

            @pl.when(jnp.logical_not(tip))
            def _():
                pltpu.make_async_remote_copy(src_ref=st_tx.at[sub, hh, :, HALF - TIP:], dst_ref=tip_st.at[col, sub, hh], send_sem=ts_send,
                                             recv_sem=ts_recv, device_id=(N_DEV - 2 + core,), device_id_type=MESH).start()
            return carry

        lax.fori_loop(0, PAIR, own, 0)
        store_rows(sub)
        store_keys(sub)

    side = 1 - core
    parts = (dr0_out, dr1_out, dr2_out, dr3_out, dr4_out, dr5_out)

    def swap_start(p):
        for n in range(2):
            pltpu.make_async_remote_copy(src_ref=dr_acc.at[2 * p + n, side], dst_ref=dr_rx.at[p, n], send_sem=x_send.at[p], recv_sem=x_recv.at[p],
                                         device_id=(partner,), device_id_type=MESH).start()

    def swap_add(p):
        wait_for(dr_rx.at[p], x_recv.at[p])
        for n in range(2):
            dr_rx[p, n] = dr_rx[p, n] + dr_acc[2 * p + n, core]

    def cross_start(p):
        pltpu.make_async_remote_copy(src_ref=dr_rx.at[p, 1 - z], dst_ref=dr_rz.at[p], send_sem=z_send.at[p], recv_sem=z_recv.at[p],
                                     device_id=(across,), device_id_type=MESH).start()

    def head_of(p, bits):
        other = chip ^ bits
        return 4 * (other % 4) + 2 * p + other // 4

    def block(p, m, bits):
        if bits == 0:
            return dr_fin.at[p, PART * m:PART * (m + 1)]
        return parts[m].at[side, :, head_of(p, bits)]

    def forward(p, m, bits):
        pltpu.make_async_remote_copy(src_ref=block(p, m, bits), dst_ref=parts[m].at[side, :, head_of(p, bits)], send_sem=fw_send.at[p, m // 3],
                                     recv_sem=fw_recv.at[p, m // 3], device_id=(partner,), device_id_type=MESH).start()

    def blocks(count):
        return parts[0].at[:, :, :N_PART // 2 * count]

    def pass_on(p, bits, hop, device):
        for m in range(N_PART):
            pltpu.make_async_remote_copy(
                src_ref=block(p, m, bits), dst_ref=parts[m].at[side, :, head_of(p, bits)], send_sem=ring_send.at[p, hop],
                recv_sem=ring_recv.at[p, hop], device_id=(device,), device_id_type=MESH).start()

    def hand_over(p, bits):
        for m in range(N_PART):
            forward(p, m, bits)

    even = chip % 2 == z
    loaded = y != z
    along_x, along_y = me ^ 2, me ^ 4

    def hop_start(p, hop):
        if hop == 0:
            for device in (along_x, along_y, across):
                pass_on(p, 0, 0, device)
        if hop == 1:
            @pl.when(even & loaded)
            def _():
                pass_on(p, 1, 1, along_y)

            @pl.when(jnp.logical_not(even) & loaded)
            def _():
                pass_on(p, 2, 1, along_x)

            pass_on(p, 1, 1, across)
            pass_on(p, 2, 1, across)
        if hop == 2:
            @pl.when(even & loaded)
            def _():
                pass_on(p, 5, 2, along_y)

            @pl.when(jnp.logical_not(even) & loaded)
            def _():
                pass_on(p, 6, 2, along_x)

            @pl.when(even)
            def _():
                pass_on(p, 3, 2, across)
        if hop == 3:
            @pl.when(even)
            def _():
                pass_on(p, 7, 3, across)

    def hop_wait(p, hop):
        if hop == 0:
            wait_for(blocks(3), ring_recv.at[p, 0])
            for bits in (1, 2, 4):
                hand_over(p, bits)
        if hop == 1:
            @pl.when(even)
            def _():
                wait_for(blocks(3), ring_recv.at[p, 1])
                hand_over(p, 3)

            @pl.when(jnp.logical_not(even))
            def _():
                wait_for(blocks(2), ring_recv.at[p, 1])
            for bits in (5, 6):
                hand_over(p, bits)
        if hop == 2:
            wait_for(blocks(1), ring_recv.at[p, 2])
            hand_over(p, 7)
        if hop == 3:
            @pl.when(jnp.logical_not(even))
            def _():
                wait_for(blocks(1), ring_recv.at[p, 3])
                hand_over(p, 3)

    def sent_wait(p):
        wait_for(blocks(3), ring_send.at[p, 0])

        @pl.when(loaded)
        def _():
            wait_for(blocks(3), ring_send.at[p, 1])

        @pl.when(jnp.logical_not(loaded))
        def _():
            wait_for(blocks(2), ring_send.at[p, 1])

        @pl.when(even & loaded)
        def _():
            wait_for(blocks(2), ring_send.at[p, 2])

        @pl.when(even != loaded)
        def _():
            wait_for(blocks(1), ring_send.at[p, 2])

        @pl.when(even)
        def _():
            wait_for(blocks(1), ring_send.at[p, 3])

    def cross_finish(p):
        wait_for(dr_rz.at[p], z_recv.at[p])
        total = dr_rx[p, z] + dr_rz[p]
        rev32 = eye_rev(F32)
        for m in range(HALF // HEAD):
            part = total[:HEAD, HALF - HEAD * (m + 1):HALF - HEAD * m]
            turned = lax.dot_general(rev32, part, (((1,), (1,)), ((), ())), precision=lax.Precision.HIGHEST, preferred_element_type=F32)
            dr_fin[p, HEAD * m:HEAD * (m + 1)] = turned.reshape(HEAD, 1, HEAD)
        dr_fin[p, HALF] = total[HEAD:HEAD + 1, HALF - HEAD:]
        dr_fin[p, HALF + 1] = total[HEAD + 1:HEAD + 2, HALF - HEAD:]
        dr_fin[p, HALF + 2:] = jnp.zeros((FIN - HALF - 2, 1, HEAD), F32)
        hop_start(p, 0)
        for m in range(N_PART):
            pltpu.make_async_copy(block(p, m, 0), parts[m].at[side, :, head_of(p, 0)], own_sem.at[p]).start()
        hand_over(p, 0)

    def tip_load(unit):
        slot, row, far = unit % 2, unit // FAR, unit % FAR
        pair = far + tip_base
        for t, src in enumerate((q_in, k_in, v_in, g_in)):
            pltpu.make_async_copy(src.at[core * SLOTS + row, :, pair], r_buf.at[slot, pl.ds(TIP * t + ROWS * core, ROWS)], tip_sem.at[slot]).start()
            pltpu.make_async_copy(far_out.at[t, row, :, far], r_buf.at[slot, pl.ds(TIP * t + ROWS * (1 - core), ROWS)], tip_sem.at[slot]).start()
        pltpu.make_async_copy(r_in.at[:TIP, pair], r_buf.at[slot, 4 * TIP:5 * TIP], tip_sem.at[slot]).start()

    def tip_done(slot):
        wait_for(r_buf.at[slot, :TIP], tip_near.at[slot])
        wait_for(r_buf.at[slot, :TIP], tip_send.at[slot])

    def tip_group(hh, r0):
        group = slice(TIP * hh + r0, TIP * hh + r0 + 16)
        rel = pltpu.roll(e_ref[group, :TIP], 1 + r0, 1, stride=1, stride_axis=0)
        ahead = lax.broadcasted_iota(jnp.int32, (16, TIP), 1) - lax.broadcasted_iota(jnp.int32, (16, TIP), 0)
        return group, s_ref[group, :TIP] + rel, ahead <= r0

    def tip_rows(hh):
        for r0 in range(0, TIP, 16):
            group, s, seen = tip_group(hh, r0)
            s = jnp.where(seen, s, -jnp.inf)
            top = jnp.max(s, axis=1, keepdims=True)
            p = jnp.exp2((s - top) * (scale * LOG2E))
            p = p * (1.0 / jnp.sum(p, axis=1, keepdims=True))
            pb_ref[group, :TIP] = p.astype(BF16)
            dp = dp_ref[group, :TIP]
            row_dot = jnp.sum(p * dp, axis=1, keepdims=True)
            ds = (p * (dp - row_dot) * scale).astype(BF16)
            ds_ref[group, :TIP] = ds
            flipped = flip8(ds.astype(F32))
            half = [pltpu.roll(flipped[8 * j:8 * j + 8], TIP - 8 - r0 - 8 * j, 1, stride=1, stride_axis=0) for j in range(2)]
            dd_ref[group, :TIP] = jnp.concatenate(half, axis=0).astype(BF16)
        rows = slice(TIP * hh, TIP * (hh + 1))
        stage[0, hh, :TIP, :] = dot(pb_ref[rows, :TIP], v_s[hh, :TIP, :]).astype(BF16)
        dqc = dot(ds_ref[rows, :TIP], k_s[hh, :TIP, :])
        dqr = flip8(dot(dd_ref[rows, :TIP], c_s[hh, :TIP, :]))
        stage[1, hh, :TIP, :] = (dqc + dqr).astype(BF16)

    def tip_keys(hh, stats):
        rows = slice(TIP * hh, TIP * (hh + 1))
        st_ref[rows, :8] = stats.T
        for r0 in range(0, TIP, 16):
            group, s, seen = tip_group(hh, r0)
            p = jnp.where(seen, jnp.exp2(s * (scale * LOG2E) - st_ref[group, 0:1]), 0.0)
            pb_ref[group, :TIP] = p.astype(BF16)
            ds_ref[group, :TIP] = (p * (dp_ref[group, :TIP] - st_ref[group, 1:2]) * scale).astype(BF16)
        over_rows = (((0,), (0,)), ((), ()))
        stage[0, hh, :TIP, :] = lax.dot_general(ds_ref[rows, :TIP], a_s[hh, :TIP, :], over_rows, preferred_element_type=F32).astype(BF16)
        stage[1, hh, :TIP, :] = lax.dot_general(pb_ref[rows, :TIP], g_s[hh, :TIP, :], over_rows, preferred_element_type=F32).astype(BF16)

    def tip_unit(unit, carry):
        slot, row, far = unit % 2, unit // FAR, unit % FAR
        pair = far + tip_base
        wait_for(r_buf.at[slot, :5 * TIP], tip_sem.at[slot])

        @pl.when(unit + 1 < UNITS)
        def _():
            tip_load(unit + 1)

        q2, k2, v2, g2, r2 = [pltpu.einshape("abc->bac", r_buf[slot, TIP * t:TIP * (t + 1)]) for t in range(5)]
        u = u_buf[pair].astype(F32)
        w = w_buf[pair].astype(F32)
        for hh in range(PAIR):
            rows = slice(TIP * hh, TIP * (hh + 1))
            q32 = q2[hh].astype(F32)
            a = (q32 + u[hh:hh + 1]).astype(BF16)
            c = (q32 + w[hh:hh + 1]).astype(BF16)
            falling = dot(eye_rev(BF16), r2[hh]).astype(BF16)
            s_ref[rows, :TIP] = dot(a, k2[hh].T)
            e_ref[rows, :TIP] = dot(c, falling.T)
            dp_ref[rows, :TIP] = dot(g2[hh], v2[hh].T)
            a_s[hh, :TIP, :] = a
            c_s[hh, :TIP, :] = falling
            g_s[hh, :TIP, :] = g2[hh]
            k_s[hh, :TIP, :] = k2[hh]
            v_s[hh, :TIP, :] = v2[hh]

        @pl.when(lower)
        def _():
            for hh in range(PAIR):
                tip_rows(hh)

        @pl.when(upper)
        def _():
            for hh in range(PAIR):
                tip_keys(hh, tip_st[far // 2, (far % 2) * SLOTS + row, hh])

        @pl.when(unit >= 2)
        def _():
            tip_done(slot)

        for n in range(2):
            r_buf[slot, (5 + n) * TIP:(6 + n) * TIP] = pltpu.einshape("abc->bac", stage[n, :, :TIP, :])
        place = (core * SLOTS + row, slice(None), pair)

        def give(results):
            for n, dst in enumerate(results):
                pltpu.make_async_copy(r_buf.at[slot, pl.ds((5 + n) * TIP + ROWS * core, ROWS)], dst.at[place], tip_near.at[slot]).start()
                pltpu.make_async_remote_copy(
                    src_ref=r_buf.at[slot, pl.ds((5 + n) * TIP + ROWS * (1 - core), ROWS)], dst_ref=dst.at[place],
                    send_sem=tip_send.at[slot], recv_sem=out_recv, device_id=(partner,), device_id_type=MESH).start()

        @pl.when(lower)
        def _():
            give((o_out, dq_out))

        @pl.when(upper)
        def _():
            give((dk_out, dv_out))
        return carry

    def tips(third):
        @pl.when(tip)
        def _():
            if third == 0:
                wait_for(far_out, far_recv)

                @pl.when(upper)
                def _():
                    wait_for(tip_st, ts_recv)
                tip_load(0)
            lax.fori_loop(UNITS // 3 * third, UNITS // 3 * (third + 1), tip_unit, 0)
            if third == 2:
                tip_done(0)
                tip_done(1)

    send_up(0)

    def sub_body(sub, carry):
        @pl.when(sub < SUBS - 1)
        def _():
            send_up(sub + 1)

        @pl.when(sub == SLOTS)
        def _():
            swap_start(0)

        @pl.when(sub == SUBS - 1)
        def _():
            swap_add(0)
            cross_start(0)

        @pl.when(sub == SUBS)
        def _():
            swap_start(1)
            swap_add(1)
            cross_start(1)
            cross_finish(0)

        @pl.when(lower & (sub < SUBS))
        def _():
            lower_rows(sub)

        @pl.when(lower & (sub > 0))
        def _():
            lower_theirs(sub - 1)

        @pl.when(lower & (sub < SUBS))
        def _():
            lower_own(sub)

        @pl.when(upper & (sub < SUBS))
        def _():
            upper_own(sub)

        @pl.when(sub <= EARLY)
        def _():
            send_out(sub, (2, 3))

        @pl.when((sub > 0) & (sub <= EARLY))
        def _():
            send_out(sub - 1, (0, 1))
        return carry

    lax.fori_loop(0, SUBS + 1, sub_body, 0)

    cross_finish(1)
    send_out(EARLY, (0, 1))
    for p in range(2):
        hop_wait(p, 0)
        hop_start(p, 1)
    for p in range(2):
        send_out(EARLY + 1 + p, range(4))
        tips(p)
        hop_wait(p, 1)
        hop_start(p, 2)

    def send_late(sub, carry):
        send_out(sub, range(4))
        return carry

    lax.fori_loop(EARLY + 3, SUBS, send_late, 0)
    tips(2)
    for p in range(2):
        hop_wait(p, 2)
        hop_start(p, 3)
    for p in range(2):
        hop_wait(p, 3)

    wait_for(buf.at[:, :, :HALF - ROWS], in_send)

    @pl.when(tip)
    def _():
        wait_for(buf.at[:, :, :HALF - 3 * ROWS // 2], out_recv)
        wait_for(buf.at[:, :, :HALF - ROWS], out_send)
        wait_for(far_out, far_send)

    @pl.when(jnp.logical_not(tip))
    def _():
        wait_for(buf, out_recv)
        wait_for(buf.at[:, :, :HALF - 2 * ROWS], out_send)

    @pl.when(upper & jnp.logical_not(tip))
    def _():
        wait_for(st_tx.at[:2], ts_send)

    @pl.when(upper)
    def _():
        wait_for(st_tx, st_send)

    for p in range(2):
        wait_for(dr_rx.at[p], x_send.at[p])
        wait_for(dr_rz.at[p], z_send.at[p])
        wait_for(blocks(1), own_sem.at[p])
        sent_wait(p)
        for n in range(2):
            wait_for(blocks(N_PAIR // 2), fw_send.at[p, n])
            wait_for(blocks(N_PAIR // 2), fw_recv.at[p, n])


def writer(*refs):
    ins, (o, dq, dk, dv, dr, du, dw, sem) = refs[:4 + N_PART], refs[4 + N_PART:]
    pairs = list(zip(ins[:4], (o, dq, dk, dv)))
    for m, part in enumerate(ins[4:]):
        rows = min(PART, HALF - PART * m)
        for side in range(2):
            start = HALF * side + PART * m
            pairs.append((part.at[side, :rows], dr.at[start:start + rows]))
    last = HALF - PART * (N_PART - 1)
    pairs += [(ins[-1].at[0, last], du), (ins[-1].at[0, last + 1], dw)]
    copies = [pltpu.make_async_copy(src, dst, sem.at[j]) for j, (src, dst) in enumerate(pairs)]
    for copy in copies:
        copy.start()
    for copy in copies:
        copy.wait()


def solution(mesh):
    seq_spec = P(None, "cp", None, None)

    def local(query, key_in, value, bias_u, bias_w, rel_k, d_out):
        n_batch, rows, n_heads, head_dim = query.shape
        pairs = (n_batch, rows, N_PAIR, PAIR, head_dim)
        vm = pltpu.VMEM
        dma = pltpu.SemaphoreType.DMA
        whole = pl.BlockSpec(memory_space=pl.ANY)
        act = jax.ShapeDtypeStruct(pairs, BF16)
        vec = jax.ShapeDtypeStruct((n_heads, 1, head_dim), F32)
        tok = (PAIR, SEQ, HEAD)
        tok_t = (PAIR, HEAD, SEQ)
        acc = (HEAD + 8, HALF)
        outs = pl.pallas_call(
            kernel,
            name="rel_attn",
            out_shape=(act, act, act, act,
                       *[jax.ShapeDtypeStruct((2, PART, n_heads, 1, head_dim), F32)] * N_PART,
                       jax.ShapeDtypeStruct((4, SLOTS, ROWS, FAR, PAIR, HEAD), BF16)),
            in_specs=[pl.BlockSpec(memory_space=pltpu.HBM)] * 7,
            out_specs=[whole] * (5 + N_PART),
            scratch_shapes=[
                vm((4, SUBS, HALF, PAIR, HEAD), BF16), vm((2, SUBS, HALF, PAIR, HEAD), BF16),
                vm((2, SEQ, PAIR, HEAD), BF16), vm((N_PAIR, PAIR, HEAD), BF16), vm((N_PAIR, PAIR, HEAD), BF16),
                vm((SUBS, PAIR, 8, HALF), F32), vm((SUBS, PAIR, 8, HALF), F32), vm((3, SUBS, PAIR, 8, TIP), F32), vm((QB, HEAD), F32),
                vm((2, 2) + acc, F32), vm((2,) + acc, F32), vm((2, FIN, 1, HEAD), F32), vm((4, 2) + acc, F32),
                vm((QB, SEQ), F32), vm((QB, SEQ), F32), vm((QB, SEQ), F32),
                vm((QB, SEQ), BF16), vm((QB, SEQ), BF16), vm((QB, SEQ), BF16),
                vm(tok, BF16), vm(tok, BF16), vm(tok, BF16), vm(tok, BF16), vm(tok, BF16),
                vm(tok_t, BF16), vm(tok_t, BF16), vm(tok_t, BF16), vm(tok_t, BF16), vm(tok_t, BF16),
                vm((4, SEQ, HEAD), BF16), vm((4, HEAD, SEQ), BF16),
                vm((PAIR, HEAD, HALF), F32), vm((PAIR, HEAD, HALF), F32), vm((4, PAIR, HALF, HEAD), BF16),
                dma, dma((2, SUBS)), dma, dma, dma((2,)), dma((4,)), dma((4,)), dma((SUBS,)), dma, dma((SUBS,)),
                dma((2,)), dma((2,)), dma((2,)), dma((2,)), dma((2, 4)), dma((2, 4)), dma((2, 2)), dma((2, 2)),
                dma, dma, dma((2,)), dma((2,)), dma((2,)), dma, dma,
            ],
            compiler_params=pltpu.CompilerParams(collective_id=0, has_side_effects=True, vmem_limit_bytes=37 * 1024 * 1024),
        )(*[pltpu.with_memory_space_constraint(x, pltpu.HBM) for x in (
            query.reshape(pairs), key_in.reshape(pairs), value.reshape(pairs), d_out.reshape(pairs),
            rel_k.reshape(SEQ, N_PAIR, PAIR, head_dim), bias_u.reshape(N_PAIR, PAIR, head_dim), bias_w.reshape(N_PAIR, PAIR, head_dim))])
        o, dq, dk, dv, dr, du, dw = pl.pallas_call(
            writer,
            name="writer",
            out_shape=(act, act, act, act, jax.ShapeDtypeStruct((SEQ, n_heads, 1, head_dim), F32), vec, vec),
            in_specs=[whole] * (4 + N_PART),
            out_specs=[whole] * 7,
            scratch_shapes=[dma((6 + 2 * N_PART,))],
            compiler_params=pltpu.CompilerParams(vmem_limit_bytes=1024 * 1024),
        )(*outs[:-1])
        full = query.shape
        return (o.reshape(full), dq.reshape(full), dk.reshape(full), dv.reshape(full),
                du.reshape(bias_u.shape), dw.reshape(bias_w.shape), dr.reshape(rel_k.shape))

    return jax.shard_map(local, mesh=mesh,
                         in_specs=(seq_spec, seq_spec, seq_spec, P(), P(), P(), seq_spec),
                         out_specs=(seq_spec, seq_spec, seq_spec, seq_spec, P(), P(), P()),
                         check_vma=False)
```

```python
import jax
import jax.numpy as jnp
from jax import lax
from jax.experimental import pallas as pl
from jax.experimental.pallas import tpu as pltpu
from jax.sharding import PartitionSpec as P

MESH = pl.DeviceIdType.MESH
BF16, F32 = jnp.bfloat16, jnp.float32
LOG2E = 1.4426950408889634

N_DEV = 16
PLANE = 8
PAIR = 2
N_PAIR = 8
SLOTS = 4
SUBS = 2 * SLOTS
EARLY = 3
ROWS = 64
HALF = PLANE * ROWS
SEQ = 2 * HALF
HEAD = 128
QB = 256
WIN = HALF + QB
N_PART = 6
PART = 86
FIN = N_PART * PART
TIP = 2 * ROWS
FAR = N_PAIR - 2
UNITS = FAR * SLOTS
TURNS = ((1, 3, 2), (3, 1, 2))


def dot(lhs, rhs):
    return jnp.dot(lhs, rhs, preferred_element_type=F32)


def flip8(x):
    rows, cols = x.shape
    idx = 7 - lax.broadcasted_iota(jnp.int32, (rows // 8, 8, cols), 1)
    return jnp.take_along_axis(x.reshape(rows // 8, 8, cols), idx, axis=1).reshape(rows, cols)


def eye_rev(dtype):
    total = lax.broadcasted_iota(jnp.int32, (HEAD, HEAD), 0) + lax.broadcasted_iota(jnp.int32, (HEAD, HEAD), 1)
    return jnp.where(total == HEAD - 1, 1.0, 0.0).astype(dtype)


def kernel(q_in, k_in, v_in, g_in, r_in, u_in, w_in,
           o_out, dq_out, dk_out, dv_out, dr0_out, dr1_out, dr2_out, dr3_out, dr4_out, dr5_out, far_out,
           buf, rbuf, r_buf, u_buf, w_buf, st_tx, st_rx, tip_st, st_ref, dr_rx, dr_rz, dr_fin, dr_acc,
           s_ref, e_ref, dp_ref, pb_ref, ds_ref, dd_ref,
           a_s, c_s, g_s, k_s, v_s, at_s, ct_s, gt_s, kt_s, vt_s, rev_s, rt_s, dkt, dvt, stage,
           in_send, in_recv, out_send, out_recv, own_sem, r_sem, up_send, up_recv, st_send, st_recv,
           x_send, x_recv, z_send, z_recv, ring_send, ring_recv, fw_send, fw_recv,
           far_send, far_recv, tip_sem, tip_near, tip_send, ts_send, ts_recv):
    me = lax.axis_index("cp")
    core = me % 2
    chip = me // 2
    col = chip % 4
    z = chip // 4
    partner = me + 1 - 2 * core
    across = me + PLANE * (1 - 2 * z)
    scale = HEAD ** -0.5

    def wait_for(ref, sem):
        pltpu.make_async_copy(ref, ref, sem).wait()

    y = col // 2
    lower, upper = z == 0, z == 1
    tip = chip == 7 * z
    tip_base = 2 - 2 * z

    tables = [pltpu.make_async_copy(src, dst, r_sem.at[j]) for j, (src, dst) in enumerate(
        ((r_in.at[:, 2 * col], r_buf.at[0]), (r_in.at[:, 2 * col + 1], r_buf.at[1]), (u_in, u_buf), (w_in, w_buf)))]
    for copy in tables:
        copy.start()

    barrier = pltpu.get_barrier_semaphore()

    for peer in [across] + [me ^ step for step in range(PLANE - 1, 0, -1)]:
        pl.semaphore_signal(barrier, inc=1, device_id=(peer,), device_id_type=MESH)
    pl.semaphore_wait(barrier, PLANE)

    my_rows = pl.ds(pl.multiple_of((me % PLANE) * ROWS, ROWS), ROWS)

    def peers():
        for near_turn, far_turn in zip(*TURNS):
            turn = jnp.where(core == 0, near_turn, far_turn)
            yield me ^ (2 * turn)
            yield me ^ (2 * turn + 1)
        yield partner

    def send_in(ins, sub):
        pair, row = sub // SLOTS, sub % SLOTS
        for first in (0, 2):
            for t in (first, first + 1):
                pltpu.make_async_copy(ins[t].at[core * SLOTS + row, :, 2 * col + pair], buf.at[t, sub, my_rows], in_recv.at[first // 2, sub]).start()
            for peer in peers():
                for t in (first, first + 1):
                    pltpu.make_async_remote_copy(
                        src_ref=ins[t].at[(peer % 2) * SLOTS + row, :, 2 * ((peer // 2) % 4) + pair], dst_ref=buf.at[t, sub, my_rows],
                        send_sem=in_send, recv_sem=in_recv.at[first // 2, sub], device_id=(peer,), device_id_type=MESH).start()

    def send_all(ins):
        def send_sub(sub, carry):
            send_in(ins, sub)
            return carry
        lax.fori_loop(0, SUBS, send_sub, 0)

    @pl.when(lower)
    def _():
        send_all((k_in, v_in, q_in, g_in))

    @pl.when(upper)
    def _():
        send_all((q_in, g_in, k_in, v_in))

    @pl.when(tip)
    def _():
        for t, src in enumerate((q_in, k_in, v_in, g_in)):
            for row in range(SLOTS):
                pltpu.make_async_remote_copy(
                    src_ref=src.at[(1 - core) * SLOTS + row, :, pl.ds(tip_base, FAR)], dst_ref=far_out.at[t, row],
                    send_sem=far_send, recv_sem=far_recv, device_id=(partner,), device_id_type=MESH).start()

    for copy in tables:
        copy.wait()
    rev = eye_rev(BF16)
    for p in range(2):
        pair_tab = pltpu.einshape("abc->bac", r_buf[p])
        for hh in range(PAIR):
            for blk in range(SEQ // HEAD):
                part = pair_tab[hh, SEQ - HEAD * (blk + 1):SEQ - HEAD * blk]
                flipped = dot(rev, part).astype(BF16)
                rev_s[2 * p + hh, HEAD * blk:HEAD * (blk + 1), :] = flipped
                rt_s[2 * p + hh, :, HEAD * blk:HEAD * (blk + 1)] = flipped.T
    dr_acc[...] = jnp.zeros_like(dr_acc)

    acts = (dk_out, dv_out, o_out, dq_out)

    def send_out(sub, which):
        place = (core * SLOTS + sub % SLOTS, slice(None), 2 * col + sub // SLOTS)
        for t in which:
            pltpu.make_async_copy(buf.at[t, sub, my_rows], acts[t].at[place], out_recv).start()
        for peer in peers():
            peer_rows = pl.ds(pl.multiple_of((peer % PLANE) * ROWS, ROWS), ROWS)
            to_tip = (peer // 2 == 7 * z) & jnp.logical_not(tip)
            for t in which:
                @pl.when(jnp.logical_not(to_tip & (lower if t >= 2 else upper)))
                def _():
                    pltpu.make_async_remote_copy(
                        src_ref=buf.at[t, sub, peer_rows], dst_ref=acts[t].at[place],
                        send_sem=out_send, recv_sem=out_recv, device_id=(peer,), device_id_type=MESH).start()

    def send_up(sub):
        wait_for(buf.at[0:2, sub], in_recv.at[0, sub])
        for j in range(2):
            pltpu.make_async_remote_copy(src_ref=buf.at[j, sub], dst_ref=rbuf.at[j, sub], send_sem=up_send.at[sub % 4], recv_sem=up_recv.at[sub],
                                         device_id=(across,), device_id_type=MESH).start()

    def unpack(ref, j, sub):
        return pltpu.einshape("abc->bac", ref[j, sub])

    def load_rows(q_ref, q_j, g_ref, g_j, sub, start, turned):
        rows = slice(start, start + HALF)
        p = sub // SLOTS
        q2 = unpack(q_ref, q_j, sub)
        u = u_buf[2 * col + p].astype(F32)
        w = w_buf[2 * col + p].astype(F32)
        for hh in range(PAIR):
            q32 = q2[hh].astype(F32)
            a = (q32 + u[hh:hh + 1]).astype(BF16)
            c = (q32 + w[hh:hh + 1]).astype(BF16)
            a_s[hh, rows, :] = a
            c_s[hh, rows, :] = c
            at_s[hh, :, rows] = a.T
            if turned:
                ct_s[hh, :, rows] = flip8(c.astype(F32)).astype(BF16).T
        g2 = unpack(g_ref, g_j, sub)
        g_s[:, rows, :] = g2
        for hh in range(PAIR):
            gt_s[hh, :, rows] = g2[hh].T

    def load_keys(k_ref, k_j, v_ref, v_j, sub, start):
        rows = slice(start, start + HALF)
        k2 = unpack(k_ref, k_j, sub)
        v2 = unpack(v_ref, v_j, sub)
        k_s[:, rows, :] = k2
        v_s[:, rows, :] = v2
        for hh in range(PAIR):
            kt_s[hh, :, rows] = k2[hh].T
            vt_s[hh, :, rows] = v2[hh].T

    def row_block(hh, head, start, i0, lo, fresh, stats):
        width = i0 + QB
        rows = slice(start, start + QB)
        s_ref[:, :width] = dot(a_s[hh, rows, :], kt_s[hh, :, :width])
        e_ref[:, :width] = dot(c_s[hh, rows, :], rt_s[head, :, SEQ - width:])
        dp_ref[:, :width] = dot(g_s[hh, rows, :], vt_s[hh, :, :width])
        for r0 in range(0, QB, 16):
            group = slice(r0, r0 + 16)
            rel = pltpu.roll(e_ref[group, :width], i0 + 1 + r0, 1, stride=1, stride_axis=0)
            s = s_ref[group, :width] + rel
            ahead = lax.broadcasted_iota(jnp.int32, (16, width), 1) - lax.broadcasted_iota(jnp.int32, (16, width), 0)
            s = jnp.where(ahead <= i0 + r0, s, -jnp.inf)
            top = jnp.max(s, axis=1, keepdims=True)
            p = jnp.exp2((s - top) * (scale * LOG2E))
            total = jnp.sum(p, axis=1, keepdims=True)
            p = p * (1.0 / total)
            pb_ref[group, :width] = p.astype(BF16)
            dp = dp_ref[group, :width]
            row_dot = jnp.sum(p * dp, axis=1, keepdims=True)
            ds = (p * (dp - row_dot) * scale).astype(BF16)
            ds_ref[group, :width] = ds
            flipped = flip8(ds.astype(F32))
            half = [pltpu.roll(flipped[8 * j:8 * j + 8], QB - 8 - r0 - 8 * j, 1, stride=1, stride_axis=0) for j in range(2)]
            dd_ref[group, :width] = jnp.concatenate(half, axis=0).astype(BF16)
            if stats:
                lane = lax.broadcasted_iota(jnp.int32, (16, HEAD), 1)
                st_ref[group, :] = jnp.where(lane == 0, top * (scale * LOG2E) + jnp.log2(total), row_dot)
        pb = pb_ref[:, :width]
        ds = ds_ref[:, :width]
        dd = dd_ref[:, :width]
        stage[0, hh, rows, :] = dot(pb, v_s[hh, :width, :]).astype(BF16)
        dqc = dot(ds, k_s[hh, :width, :])
        dqr = flip8(dot(dd, rev_s[head, SEQ - width:, :]))
        stage[1, hh, rows, :] = (dqc + dqr).astype(BF16)
        dr_acc[head, 1, HEAD:HEAD + 1, HALF - HEAD:] += jnp.sum(dqc, axis=0, keepdims=True)
        dr_acc[head, 1, HEAD + 1:HEAD + 2, HALF - HEAD:] += jnp.sum(dqr, axis=0, keepdims=True)
        dk_new = dot(at_s[hh, :, rows], ds_ref[:, lo:width])
        dv_new = dot(gt_s[hh, :, rows], pb_ref[:, lo:width])
        if fresh:
            dkt[hh] = dk_new
            dvt[hh] = dv_new
        else:
            dkt[hh, :, :width - lo] += dk_new
            dvt[hh, :, :width - lo] += dv_new
        dr_new = dot(ct_s[hh, :, rows], dd)
        if width > HALF:
            dr_acc[head, 0, :HEAD, SEQ - width:] += dr_new[:, :width - HALF]
            dr_acc[head, 1, :HEAD, :] += dr_new[:, width - HALF:]
        else:
            dr_acc[head, 1, :HEAD, HALF - width:] += dr_new

    def col_block(hh, head, sub, i0):
        rows = slice(i0, i0 + QB)
        first = WIN - i0
        s_ref[:, :HALF] = dot(a_s[hh, rows, :], kt_s[hh, :, :HALF])
        e_ref[:, :WIN] = dot(c_s[hh, rows, :], rt_s[head, :, first:first + WIN])
        dp_ref[:, :HALF] = dot(g_s[hh, rows, :], vt_s[hh, :, :HALF])
        st_ref[:, :8] = st_rx[sub, hh, :, i0 - HALF:i0 - HALF + QB].T
        for r0 in range(0, QB, 16):
            group = slice(r0, r0 + 16)
            rel = pltpu.roll(e_ref[group, :WIN], HALF + 1 + r0, 1, stride=1, stride_axis=0)[:, :HALF]
            log_sum = st_ref[group, 0:1]
            row_dot = st_ref[group, 1:2]
            p = jnp.exp2((s_ref[group, :HALF] + rel) * (scale * LOG2E) - log_sum)
            pb_ref[group, :HALF] = p.astype(BF16)
            ds_ref[group, :HALF] = (p * (dp_ref[group, :HALF] - row_dot) * scale).astype(BF16)
        dkt[hh] += dot(at_s[hh, :, rows], ds_ref[:, :HALF])
        dvt[hh] += dot(gt_s[hh, :, rows], pb_ref[:, :HALF])

    def store_rows(sub):
        for t in range(2):
            buf[2 + t, sub] = pltpu.einshape("abc->bac", stage[t])

    def store_keys(sub):
        for hh in range(PAIR):
            stage[2, hh] = dkt[hh].astype(BF16).T
            stage[3, hh] = dvt[hh].astype(BF16).T
        for t in range(2):
            buf[t, sub] = pltpu.einshape("abc->bac", stage[2 + t])

    def wait_up(sub):
        wait_for(rbuf.at[:, sub], up_recv.at[sub])
        wait_for(rbuf.at[:, sub], up_send.at[sub % 4])

    def wait_in(sub):
        wait_for(buf.at[2:4, sub], in_recv.at[1, sub])

    def lower_rows(sub):
        wait_in(sub)
        load_rows(buf, 2, buf, 3, sub, 0, True)

    def lower_own(sub):
        load_keys(buf, 0, buf, 1, sub, 0)

        def own(hh, carry):
            head = 2 * (sub // SLOTS) + hh
            row_block(hh, head, QB, QB, 0, True, False)
            row_block(hh, head, 0, 0, 0, False, False)
            return carry

        lax.fori_loop(0, PAIR, own, 0)
        store_rows(sub)

    def lower_theirs(sub):
        wait_up(sub)
        load_rows(rbuf, 0, rbuf, 1, sub, HALF, False)
        wait_for(st_rx.at[sub], st_recv.at[sub % 4])

        def theirs(hh, carry):
            head = 2 * (sub // SLOTS) + hh
            col_block(hh, head, sub, HALF)
            col_block(hh, head, sub, HALF + QB)
            return carry

        lax.fori_loop(0, PAIR, theirs, 0)
        store_keys(sub)

    def upper_own(sub):
        wait_in(sub)
        wait_up(sub)
        load_rows(buf, 0, buf, 1, sub, 0, True)
        load_keys(rbuf, 0, rbuf, 1, sub, 0)
        load_keys(buf, 2, buf, 3, sub, HALF)

        def own(hh, carry):
            head = 2 * (sub // SLOTS) + hh
            for blk in (1, 0):
                row_block(hh, head, QB * blk, HALF + QB * blk, HALF, blk == 1, True)
                st_tx[sub, hh, :, QB * blk:QB * (blk + 1)] = st_ref[...].T[:8]
            pltpu.make_async_remote_copy(src_ref=st_tx.at[sub, hh], dst_ref=st_rx.at[sub, hh], send_sem=st_send, recv_sem=st_recv.at[sub % 4],
                                         device_id=(across,), device_id_type=MESH).start()

            @pl.when(jnp.logical_not(tip))
            def _():
                pltpu.make_async_remote_copy(src_ref=st_tx.at[sub, hh, :, HALF - TIP:], dst_ref=tip_st.at[col, sub, hh], send_sem=ts_send,
                                             recv_sem=ts_recv, device_id=(N_DEV - 2 + core,), device_id_type=MESH).start()
            return carry

        lax.fori_loop(0, PAIR, own, 0)
        store_rows(sub)
        store_keys(sub)

    side = 1 - core
    parts = (dr0_out, dr1_out, dr2_out, dr3_out, dr4_out, dr5_out)

    def swap_start(p):
        for n in range(2):
            pltpu.make_async_remote_copy(src_ref=dr_acc.at[2 * p + n, side], dst_ref=dr_rx.at[p, n], send_sem=x_send, recv_sem=x_recv.at[p],
                                         device_id=(partner,), device_id_type=MESH).start()

    def swap_add(p):
        wait_for(dr_rx.at[p], x_recv.at[p])
        for n in range(2):
            dr_rx[p, n] = dr_rx[p, n] + dr_acc[2 * p + n, core]

    def cross_start(p):
        pltpu.make_async_remote_copy(src_ref=dr_rx.at[p, 1 - z], dst_ref=dr_rz.at[p], send_sem=z_send, recv_sem=z_recv.at[p],
                                     device_id=(across,), device_id_type=MESH).start()

    def head_of(p, bits):
        other = chip ^ bits
        return 4 * (other % 4) + 2 * p + other // 4

    def block(p, m, bits):
        if bits == 0:
            return dr_fin.at[p, PART * m:PART * (m + 1)]
        return parts[m].at[side, :, head_of(p, bits)]

    def forward(p, m, bits):
        pltpu.make_async_remote_copy(src_ref=block(p, m, bits), dst_ref=parts[m].at[side, :, head_of(p, bits)], send_sem=fw_send,
                                     recv_sem=fw_recv, device_id=(partner,), device_id_type=MESH).start()

    def blocks(count):
        return parts[0].at[:, :, :N_PART // 2 * count]

    def pass_on(p, bits, hop, device):
        for m in range(N_PART):
            pltpu.make_async_remote_copy(
                src_ref=block(p, m, bits), dst_ref=parts[m].at[side, :, head_of(p, bits)], send_sem=ring_send,
                recv_sem=ring_recv.at[p, hop], device_id=(device,), device_id_type=MESH).start()

    def hand_over(p, bits):
        for m in range(N_PART):
            forward(p, m, bits)

    even = chip % 2 == z
    loaded = y != z
    along_x, along_y = me ^ 2, me ^ 4

    def hop_start(p, hop):
        if hop == 0:
            for device in (along_x, along_y, across):
                pass_on(p, 0, 0, device)
        if hop == 1:
            @pl.when(even & loaded)
            def _():
                pass_on(p, 1, 1, along_y)

            @pl.when(jnp.logical_not(even) & loaded)
            def _():
                pass_on(p, 2, 1, along_x)

            pass_on(p, 1, 1, across)
            pass_on(p, 2, 1, across)
        if hop == 2:
            @pl.when(even & loaded)
            def _():
                pass_on(p, 5, 2, along_y)

            @pl.when(jnp.logical_not(even) & loaded)
            def _():
                pass_on(p, 6, 2, along_x)

            @pl.when(even)
            def _():
                pass_on(p, 3, 2, across)
        if hop == 3:
            @pl.when(even)
            def _():
                pass_on(p, 7, 3, across)

    def hop_wait(p, hop):
        if hop == 0:
            wait_for(blocks(3), ring_recv.at[p, 0])
            for bits in (1, 2, 4):
                hand_over(p, bits)
        if hop == 1:
            @pl.when(even)
            def _():
                wait_for(blocks(3), ring_recv.at[p, 1])
                hand_over(p, 3)

            @pl.when(jnp.logical_not(even))
            def _():
                wait_for(blocks(2), ring_recv.at[p, 1])
            for bits in (5, 6):
                hand_over(p, bits)
        if hop == 2:
            wait_for(blocks(1), ring_recv.at[p, 2])
            hand_over(p, 7)
        if hop == 3:
            @pl.when(jnp.logical_not(even))
            def _():
                wait_for(blocks(1), ring_recv.at[p, 3])
                hand_over(p, 3)

    def sent_wait():
        @pl.when(even & loaded)
        def _():
            wait_for(buf.at[:3, :, :FIN * 18 // 24], ring_send)

        @pl.when(even != loaded)
        def _():
            wait_for(buf.at[:3, :7, :FIN * 14 // 21], ring_send)

        @pl.when(jnp.logical_not(even | loaded))
        def _():
            wait_for(buf.at[:2, :6, :FIN * 10 // 12], ring_send)

    def cross_finish(p):
        wait_for(dr_rz.at[p], z_recv.at[p])
        total = dr_rx[p, z] + dr_rz[p]
        rev32 = eye_rev(F32)
        for m in range(HALF // HEAD):
            part = total[:HEAD, HALF - HEAD * (m + 1):HALF - HEAD * m]
            turned = lax.dot_general(rev32, part, (((1,), (1,)), ((), ())), precision=lax.Precision.HIGHEST, preferred_element_type=F32)
            dr_fin[p, HEAD * m:HEAD * (m + 1)] = turned.reshape(HEAD, 1, HEAD)
        dr_fin[p, HALF] = total[HEAD:HEAD + 1, HALF - HEAD:]
        dr_fin[p, HALF + 1] = total[HEAD + 1:HEAD + 2, HALF - HEAD:]
        dr_fin[p, HALF + 2:] = jnp.zeros((FIN - HALF - 2, 1, HEAD), F32)
        hop_start(p, 0)
        for m in range(N_PART):
            pltpu.make_async_copy(block(p, m, 0), parts[m].at[side, :, head_of(p, 0)], own_sem).start()
        hand_over(p, 0)

    def tip_load(unit):
        slot, row, far = unit % 2, unit // FAR, unit % FAR
        pair = far + tip_base
        for t, src in enumerate((q_in, k_in, v_in, g_in)):
            pltpu.make_async_copy(src.at[core * SLOTS + row, :, pair], r_buf.at[slot, pl.ds(TIP * t + ROWS * core, ROWS)], tip_sem.at[slot]).start()
            pltpu.make_async_copy(far_out.at[t, row, :, far], r_buf.at[slot, pl.ds(TIP * t + ROWS * (1 - core), ROWS)], tip_sem.at[slot]).start()
        pltpu.make_async_copy(r_in.at[:TIP, pair], r_buf.at[slot, 4 * TIP:5 * TIP], tip_sem.at[slot]).start()

    def tip_done(slot):
        wait_for(r_buf.at[slot, :TIP], tip_near.at[slot])
        wait_for(r_buf.at[slot, :TIP], tip_send.at[slot])

    def tip_group(hh, r0):
        group = slice(TIP * hh + r0, TIP * hh + r0 + 16)
        rel = pltpu.roll(e_ref[group, :TIP], 1 + r0, 1, stride=1, stride_axis=0)
        ahead = lax.broadcasted_iota(jnp.int32, (16, TIP), 1) - lax.broadcasted_iota(jnp.int32, (16, TIP), 0)
        return group, s_ref[group, :TIP] + rel, ahead <= r0

    def tip_rows(hh):
        for r0 in range(0, TIP, 16):
            group, s, seen = tip_group(hh, r0)
            s = jnp.where(seen, s, -jnp.inf)
            top = jnp.max(s, axis=1, keepdims=True)
            p = jnp.exp2((s - top) * (scale * LOG2E))
            p = p * (1.0 / jnp.sum(p, axis=1, keepdims=True))
            pb_ref[group, :TIP] = p.astype(BF16)
            dp = dp_ref[group, :TIP]
            row_dot = jnp.sum(p * dp, axis=1, keepdims=True)
            ds = (p * (dp - row_dot) * scale).astype(BF16)
            ds_ref[group, :TIP] = ds
            flipped = flip8(ds.astype(F32))
            half = [pltpu.roll(flipped[8 * j:8 * j + 8], TIP - 8 - r0 - 8 * j, 1, stride=1, stride_axis=0) for j in range(2)]
            dd_ref[group, :TIP] = jnp.concatenate(half, axis=0).astype(BF16)
        rows = slice(TIP * hh, TIP * (hh + 1))
        stage[0, hh, :TIP, :] = dot(pb_ref[rows, :TIP], v_s[hh, :TIP, :]).astype(BF16)
        dqc = dot(ds_ref[rows, :TIP], k_s[hh, :TIP, :])
        dqr = flip8(dot(dd_ref[rows, :TIP], c_s[hh, :TIP, :]))
        stage[1, hh, :TIP, :] = (dqc + dqr).astype(BF16)

    def tip_keys(hh, stats):
        rows = slice(TIP * hh, TIP * (hh + 1))
        st_ref[rows, :8] = stats.T
        for r0 in range(0, TIP, 16):
            group, s, seen = tip_group(hh, r0)
            p = jnp.where(seen, jnp.exp2(s * (scale * LOG2E) - st_ref[group, 0:1]), 0.0)
            pb_ref[group, :TIP] = p.astype(BF16)
            ds_ref[group, :TIP] = (p * (dp_ref[group, :TIP] - st_ref[group, 1:2]) * scale).astype(BF16)
        over_rows = (((0,), (0,)), ((), ()))
        stage[0, hh, :TIP, :] = lax.dot_general(ds_ref[rows, :TIP], a_s[hh, :TIP, :], over_rows, preferred_element_type=F32).astype(BF16)
        stage[1, hh, :TIP, :] = lax.dot_general(pb_ref[rows, :TIP], g_s[hh, :TIP, :], over_rows, preferred_element_type=F32).astype(BF16)

    def tip_unit(unit, carry):
        slot, row, far = unit % 2, unit // FAR, unit % FAR
        pair = far + tip_base
        wait_for(r_buf.at[slot, :5 * TIP], tip_sem.at[slot])

        @pl.when(unit + 1 < UNITS)
        def _():
            tip_load(unit + 1)

        q2, k2, v2, g2, r2 = [pltpu.einshape("abc->bac", r_buf[slot, TIP * t:TIP * (t + 1)]) for t in range(5)]
        u = u_buf[pair].astype(F32)
        w = w_buf[pair].astype(F32)
        for hh in range(PAIR):
            rows = slice(TIP * hh, TIP * (hh + 1))
            q32 = q2[hh].astype(F32)
            a = (q32 + u[hh:hh + 1]).astype(BF16)
            c = (q32 + w[hh:hh + 1]).astype(BF16)
            falling = dot(eye_rev(BF16), r2[hh]).astype(BF16)
            s_ref[rows, :TIP] = dot(a, k2[hh].T)
            e_ref[rows, :TIP] = dot(c, falling.T)
            dp_ref[rows, :TIP] = dot(g2[hh], v2[hh].T)
            a_s[hh, :TIP, :] = a
            c_s[hh, :TIP, :] = falling
            g_s[hh, :TIP, :] = g2[hh]
            k_s[hh, :TIP, :] = k2[hh]
            v_s[hh, :TIP, :] = v2[hh]

        @pl.when(lower)
        def _():
            for hh in range(PAIR):
                tip_rows(hh)

        @pl.when(upper)
        def _():
            for hh in range(PAIR):
                tip_keys(hh, tip_st[far // 2, (far % 2) * SLOTS + row, hh])

        @pl.when(unit >= 2)
        def _():
            tip_done(slot)

        for n in range(2):
            r_buf[slot, (5 + n) * TIP:(6 + n) * TIP] = pltpu.einshape("abc->bac", stage[n, :, :TIP, :])
        place = (core * SLOTS + row, slice(None), pair)

        def give(results):
            for n, dst in enumerate(results):
                pltpu.make_async_copy(r_buf.at[slot, pl.ds((5 + n) * TIP + ROWS * core, ROWS)], dst.at[place], tip_near.at[slot]).start()
                pltpu.make_async_remote_copy(
                    src_ref=r_buf.at[slot, pl.ds((5 + n) * TIP + ROWS * (1 - core), ROWS)], dst_ref=dst.at[place],
                    send_sem=tip_send.at[slot], recv_sem=out_recv, device_id=(partner,), device_id_type=MESH).start()

        @pl.when(lower)
        def _():
            give((o_out, dq_out))

        @pl.when(upper)
        def _():
            give((dk_out, dv_out))
        return carry

    def tips(third):
        @pl.when(tip)
        def _():
            if third == 0:
                wait_for(far_out, far_recv)

                @pl.when(upper)
                def _():
                    wait_for(tip_st, ts_recv)
                tip_load(0)
            lax.fori_loop(UNITS // 3 * third, UNITS // 3 * (third + 1), tip_unit, 0)
            if third == 2:
                tip_done(0)
                tip_done(1)

    send_up(0)

    def sub_body(sub, carry):
        @pl.when(sub < SUBS - 1)
        def _():
            send_up(sub + 1)

        @pl.when(sub == SLOTS)
        def _():
            swap_start(0)

        @pl.when(sub == SUBS - 1)
        def _():
            swap_add(0)
            cross_start(0)

        @pl.when(sub == SUBS)
        def _():
            swap_start(1)
            swap_add(1)
            cross_start(1)
            cross_finish(0)

        @pl.when(lower & (sub < SUBS))
        def _():
            lower_rows(sub)

        @pl.when(lower & (sub > 0))
        def _():
            lower_theirs(sub - 1)

        @pl.when(lower & (sub < SUBS))
        def _():
            lower_own(sub)

        @pl.when(upper & (sub < SUBS))
        def _():
            upper_own(sub)

        @pl.when(sub <= EARLY)
        def _():
            send_out(sub, (2, 3))

        @pl.when((sub > 0) & (sub <= EARLY))
        def _():
            send_out(sub - 1, (0, 1))
        return carry

    lax.fori_loop(0, SUBS + 1, sub_body, 0)

    cross_finish(1)
    send_out(EARLY, (0, 1))
    for p in range(2):
        hop_wait(p, 0)
        hop_start(p, 1)
    for p in range(2):
        send_out(EARLY + 1 + p, range(4))
        tips(p)
        hop_wait(p, 1)
        hop_start(p, 2)

    def send_late(sub, carry):
        send_out(sub, range(4))
        return carry

    lax.fori_loop(EARLY + 3, SUBS, send_late, 0)
    tips(2)
    for p in range(2):
        hop_wait(p, 2)
        hop_start(p, 3)
    for p in range(2):
        hop_wait(p, 3)

    wait_for(buf.at[:, :, :HALF - ROWS], in_send)

    @pl.when(tip)
    def _():
        wait_for(buf.at[:, :, :HALF - 3 * ROWS // 2], out_recv)
        wait_for(buf.at[:, :, :HALF - ROWS], out_send)
        wait_for(far_out, far_send)

    @pl.when(jnp.logical_not(tip))
    def _():
        wait_for(buf, out_recv)
        wait_for(buf.at[:, :, :HALF - 2 * ROWS], out_send)

    @pl.when(upper & jnp.logical_not(tip))
    def _():
        wait_for(st_tx.at[:2], ts_send)

    @pl.when(upper)
    def _():
        wait_for(st_tx, st_send)

    wait_for(dr_rx, x_send)
    wait_for(dr_rz, z_send)
    wait_for(blocks(2), own_sem)
    sent_wait()
    for sem in (fw_send, fw_recv):
        wait_for(buf.at[:3, :, :FIN * 16 // 24], sem)


def writer(*refs):
    ins, (o, dq, dk, dv, dr, du, dw, sem) = refs[:4 + N_PART], refs[4 + N_PART:]
    pairs = list(zip(ins[:4], (o, dq, dk, dv)))
    for m, part in enumerate(ins[4:]):
        rows = min(PART, HALF - PART * m)
        for side in range(2):
            start = HALF * side + PART * m
            pairs.append((part.at[side, :rows], dr.at[start:start + rows]))
    last = HALF - PART * (N_PART - 1)
    pairs += [(ins[-1].at[0, last], du), (ins[-1].at[0, last + 1], dw)]
    copies = [pltpu.make_async_copy(src, dst, sem.at[j]) for j, (src, dst) in enumerate(pairs)]
    for copy in copies:
        copy.start()
    for copy in copies:
        copy.wait()


def solution(mesh):
    seq_spec = P(None, "cp", None, None)

    def local(query, key_in, value, bias_u, bias_w, rel_k, d_out):
        n_batch, rows, n_heads, head_dim = query.shape
        pairs = (n_batch, rows, N_PAIR, PAIR, head_dim)
        vm = pltpu.VMEM
        dma = pltpu.SemaphoreType.DMA
        whole = pl.BlockSpec(memory_space=pl.ANY)
        act = jax.ShapeDtypeStruct(pairs, BF16)
        vec = jax.ShapeDtypeStruct((n_heads, 1, head_dim), F32)
        tok = (PAIR, SEQ, HEAD)
        tok_t = (PAIR, HEAD, SEQ)
        acc = (HEAD + 8, HALF)
        outs = pl.pallas_call(
            kernel,
            name="rel_attn",
            out_shape=(act, act, act, act,
                       *[jax.ShapeDtypeStruct((2, PART, n_heads, 1, head_dim), F32)] * N_PART,
                       jax.ShapeDtypeStruct((4, SLOTS, ROWS, FAR, PAIR, HEAD), BF16)),
            in_specs=[pl.BlockSpec(memory_space=pltpu.HBM)] * 7,
            out_specs=[whole] * (5 + N_PART),
            scratch_shapes=[
                vm((4, SUBS, HALF, PAIR, HEAD), BF16), vm((2, SUBS, HALF, PAIR, HEAD), BF16),
                vm((2, SEQ, PAIR, HEAD), BF16), vm((N_PAIR, PAIR, HEAD), BF16), vm((N_PAIR, PAIR, HEAD), BF16),
                vm((SUBS, PAIR, 8, HALF), F32), vm((SUBS, PAIR, 8, HALF), F32), vm((3, SUBS, PAIR, 8, TIP), F32), vm((QB, HEAD), F32),
                vm((2, 2) + acc, F32), vm((2,) + acc, F32), vm((2, FIN, 1, HEAD), F32), vm((4, 2) + acc, F32),
                vm((QB, SEQ), F32), vm((QB, SEQ), F32), vm((QB, SEQ), F32),
                vm((QB, SEQ), BF16), vm((QB, SEQ), BF16), vm((QB, SEQ), BF16),
                vm(tok, BF16), vm(tok, BF16), vm(tok, BF16), vm(tok, BF16), vm(tok, BF16),
                vm(tok_t, BF16), vm(tok_t, BF16), vm(tok_t, BF16), vm(tok_t, BF16), vm(tok_t, BF16),
                vm((4, SEQ, HEAD), BF16), vm((4, HEAD, SEQ), BF16),
                vm((PAIR, HEAD, HALF), F32), vm((PAIR, HEAD, HALF), F32), vm((4, PAIR, HALF, HEAD), BF16),
                dma, dma((2, SUBS)), dma, dma, dma, dma((4,)), dma((4,)), dma((SUBS,)), dma, dma((4,)),
                dma, dma((2,)), dma, dma((2,)), dma, dma((2, 4)), dma, dma,
                dma, dma, dma((2,)), dma((2,)), dma((2,)), dma, dma,
            ],
            compiler_params=pltpu.CompilerParams(collective_id=0, has_side_effects=True, vmem_limit_bytes=37 * 1024 * 1024),
        )(*[pltpu.with_memory_space_constraint(x, pltpu.HBM) for x in (
            query.reshape(pairs), key_in.reshape(pairs), value.reshape(pairs), d_out.reshape(pairs),
            rel_k.reshape(SEQ, N_PAIR, PAIR, head_dim), bias_u.reshape(N_PAIR, PAIR, head_dim), bias_w.reshape(N_PAIR, PAIR, head_dim))])
        o, dq, dk, dv, dr, du, dw = pl.pallas_call(
            writer,
            name="writer",
            out_shape=(act, act, act, act, jax.ShapeDtypeStruct((SEQ, n_heads, 1, head_dim), F32), vec, vec),
            in_specs=[whole] * (4 + N_PART),
            out_specs=[whole] * 7,
            scratch_shapes=[dma((6 + 2 * N_PART,))],
            compiler_params=pltpu.CompilerParams(vmem_limit_bytes=1024 * 1024),
        )(*outs[:-1])
        full = query.shape
        return (o.reshape(full), dq.reshape(full), dk.reshape(full), dv.reshape(full),
                du.reshape(bias_u.shape), dw.reshape(bias_w.shape), dr.reshape(rel_k.shape))

    return jax.shard_map(local, mesh=mesh,
                         in_specs=(seq_spec, seq_spec, seq_spec, P(), P(), P(), seq_spec),
                         out_specs=(seq_spec, seq_spec, seq_spec, seq_spec, P(), P(), P()),
                         check_vma=False)
```

```python
import jax
import jax.numpy as jnp
from jax import lax
from jax.experimental import pallas as pl
from jax.experimental.pallas import tpu as pltpu
from jax.sharding import PartitionSpec as P

MESH = pl.DeviceIdType.MESH
BF16, F32 = jnp.bfloat16, jnp.float32
LOG2E = 1.4426950408889634

N_DEV = 16
PLANE = 8
PAIR = 2
N_PAIR = 8
SLOTS = 4
SUBS = 2 * SLOTS
EARLY = 3
ROWS = 64
HALF = PLANE * ROWS
SEQ = 2 * HALF
HEAD = 128
QB = 256
WIN = HALF + QB
N_PART = 6
PART = 86
FIN = N_PART * PART
TIP = 2 * ROWS
FAR = N_PAIR - 2
UNITS = FAR * SLOTS
TURNS = ((1, 3, 2), (3, 1, 2))


def dot(lhs, rhs):
    return jnp.dot(lhs, rhs, preferred_element_type=F32)


def flip8(x):
    rows, cols = x.shape
    idx = 7 - lax.broadcasted_iota(jnp.int32, (rows // 8, 8, cols), 1)
    return jnp.take_along_axis(x.reshape(rows // 8, 8, cols), idx, axis=1).reshape(rows, cols)


def eye_rev(dtype):
    total = lax.broadcasted_iota(jnp.int32, (HEAD, HEAD), 0) + lax.broadcasted_iota(jnp.int32, (HEAD, HEAD), 1)
    return jnp.where(total == HEAD - 1, 1.0, 0.0).astype(dtype)


def kernel(q_in, k_in, v_in, g_in, r_in, u_in, w_in,
           o_out, dq_out, dk_out, dv_out, dr0_out, dr1_out, dr2_out, dr3_out, dr4_out, dr5_out, far_out,
           buf, rbuf, r_buf, u_buf, w_buf, st_tx, st_rx, tip_st, st_ref, dr_rx, dr_rz, dr_fin, dr_acc,
           s_ref, e_ref, dp_ref, pb_ref, ds_ref, dd_ref,
           a_s, c_s, g_s, k_s, v_s, at_s, ct_s, gt_s, kt_s, vt_s, rev_s, rt_s, dkt, dvt, stage,
           in_send, in_recv, out_send, out_recv, own_sem, r_sem, up_send, up_recv, st_send, st_recv,
           x_send, x_recv, z_send, z_recv, ring_send, ring_recv, fw_send, fw_recv,
           far_send, far_recv, tip_sem, tip_near, tip_send, ts_send, ts_recv):
    me = lax.axis_index("cp")
    core = me % 2
    chip = me // 2
    col = chip % 4
    z = chip // 4
    partner = me + 1 - 2 * core
    across = me + PLANE * (1 - 2 * z)
    scale = HEAD ** -0.5

    def wait_for(ref, sem):
        pltpu.make_async_copy(ref, ref, sem).wait()

    y = col // 2
    lower, upper = z == 0, z == 1
    tip = chip == 7 * z
    tip_base = 2 - 2 * z

    tables = [pltpu.make_async_copy(src, dst, r_sem.at[j]) for j, (src, dst) in enumerate(
        ((r_in.at[:, 2 * col], r_buf.at[0]), (r_in.at[:, 2 * col + 1], r_buf.at[1]), (u_in, u_buf), (w_in, w_buf)))]
    for copy in tables:
        copy.start()

    my_rows = pl.ds(pl.multiple_of((me % PLANE) * ROWS, ROWS), ROWS)

    def peers():
        for near_turn, far_turn in zip(*TURNS):
            turn = jnp.where(core == 0, near_turn, far_turn)
            yield me ^ (2 * turn)
            yield me ^ (2 * turn + 1)
        yield partner

    def send_in(ins, sub):
        pair, row = sub // SLOTS, sub % SLOTS
        for first in (0, 2):
            for t in (first, first + 1):
                pltpu.make_async_copy(ins[t].at[core * SLOTS + row, :, 2 * col + pair], buf.at[t, sub, my_rows], in_recv.at[first // 2, sub]).start()
            for peer in peers():
                for t in (first, first + 1):
                    pltpu.make_async_remote_copy(
                        src_ref=ins[t].at[(peer % 2) * SLOTS + row, :, 2 * ((peer // 2) % 4) + pair], dst_ref=buf.at[t, sub, my_rows],
                        send_sem=in_send, recv_sem=in_recv.at[first // 2, sub], device_id=(peer,), device_id_type=MESH).start()

    def send_all(ins):
        def send_sub(sub, carry):
            send_in(ins, sub)
            return carry
        lax.fori_loop(0, SUBS, send_sub, 0)

    @pl.when(lower)
    def _():
        send_all((k_in, v_in, q_in, g_in))

    @pl.when(upper)
    def _():
        send_all((q_in, g_in, k_in, v_in))

    @pl.when(tip)
    def _():
        for t, src in enumerate((q_in, k_in, v_in, g_in)):
            for row in range(SLOTS):
                pltpu.make_async_remote_copy(
                    src_ref=src.at[(1 - core) * SLOTS + row, :, pl.ds(tip_base, FAR)], dst_ref=far_out.at[t, row],
                    send_sem=far_send, recv_sem=far_recv, device_id=(partner,), device_id_type=MESH).start()

    for copy in tables:
        copy.wait()
    rev = eye_rev(BF16)
    for p in range(2):
        pair_tab = pltpu.einshape("abc->bac", r_buf[p])
        for hh in range(PAIR):
            for blk in range(SEQ // HEAD):
                part = pair_tab[hh, SEQ - HEAD * (blk + 1):SEQ - HEAD * blk]
                flipped = dot(rev, part).astype(BF16)
                rev_s[2 * p + hh, HEAD * blk:HEAD * (blk + 1), :] = flipped
                rt_s[2 * p + hh, :, HEAD * blk:HEAD * (blk + 1)] = flipped.T
    dr_acc[...] = jnp.zeros_like(dr_acc)

    acts = (dk_out, dv_out, o_out, dq_out)

    def send_out(sub, which):
        place = (core * SLOTS + sub % SLOTS, slice(None), 2 * col + sub // SLOTS)
        for t in which:
            pltpu.make_async_copy(buf.at[t, sub, my_rows], acts[t].at[place], out_recv).start()
        for peer in peers():
            peer_rows = pl.ds(pl.multiple_of((peer % PLANE) * ROWS, ROWS), ROWS)
            to_tip = (peer // 2 == 7 * z) & jnp.logical_not(tip)
            for t in which:
                @pl.when(jnp.logical_not(to_tip & (lower if t >= 2 else upper)))
                def _():
                    pltpu.make_async_remote_copy(
                        src_ref=buf.at[t, sub, peer_rows], dst_ref=acts[t].at[place],
                        send_sem=out_send, recv_sem=out_recv, device_id=(peer,), device_id_type=MESH).start()

    def send_up(sub):
        wait_for(buf.at[0:2, sub], in_recv.at[0, sub])
        for j in range(2):
            pltpu.make_async_remote_copy(src_ref=buf.at[j, sub], dst_ref=rbuf.at[j, sub], send_sem=up_send.at[sub % 4], recv_sem=up_recv.at[sub],
                                         device_id=(across,), device_id_type=MESH).start()

    def unpack(ref, j, sub):
        return pltpu.einshape("abc->bac", ref[j, sub])

    def load_rows(q_ref, q_j, g_ref, g_j, sub, start, turned):
        rows = slice(start, start + HALF)
        p = sub // SLOTS
        q2 = unpack(q_ref, q_j, sub)
        u = u_buf[2 * col + p].astype(F32)
        w = w_buf[2 * col + p].astype(F32)
        for hh in range(PAIR):
            q32 = q2[hh].astype(F32)
            a = (q32 + u[hh:hh + 1]).astype(BF16)
            c = (q32 + w[hh:hh + 1]).astype(BF16)
            a_s[hh, rows, :] = a
            c_s[hh, rows, :] = c
            at_s[hh, :, rows] = a.T
            if turned:
                ct_s[hh, :, rows] = flip8(c.astype(F32)).astype(BF16).T
        g2 = unpack(g_ref, g_j, sub)
        g_s[:, rows, :] = g2
        for hh in range(PAIR):
            gt_s[hh, :, rows] = g2[hh].T

    def load_keys(k_ref, k_j, v_ref, v_j, sub, start):
        rows = slice(start, start + HALF)
        k2 = unpack(k_ref, k_j, sub)
        v2 = unpack(v_ref, v_j, sub)
        k_s[:, rows, :] = k2
        v_s[:, rows, :] = v2
        for hh in range(PAIR):
            kt_s[hh, :, rows] = k2[hh].T
            vt_s[hh, :, rows] = v2[hh].T

    def row_block(hh, head, start, i0, lo, fresh, stats):
        width = i0 + QB
        rows = slice(start, start + QB)
        s_ref[:, :width] = dot(a_s[hh, rows, :], kt_s[hh, :, :width])
        e_ref[:, :width] = dot(c_s[hh, rows, :], rt_s[head, :, SEQ - width:])
        dp_ref[:, :width] = dot(g_s[hh, rows, :], vt_s[hh, :, :width])
        for r0 in range(0, QB, 16):
            group = slice(r0, r0 + 16)
            rel = pltpu.roll(e_ref[group, :width], i0 + 1 + r0, 1, stride=1, stride_axis=0)
            s = s_ref[group, :width] + rel
            ahead = lax.broadcasted_iota(jnp.int32, (16, width), 1) - lax.broadcasted_iota(jnp.int32, (16, width), 0)
            s = jnp.where(ahead <= i0 + r0, s, -jnp.inf)
            top = jnp.max(s, axis=1, keepdims=True)
            p = jnp.exp2((s - top) * (scale * LOG2E))
            total = jnp.sum(p, axis=1, keepdims=True)
            p = p * (1.0 / total)
            pb_ref[group, :width] = p.astype(BF16)
            dp = dp_ref[group, :width]
            row_dot = jnp.sum(p * dp, axis=1, keepdims=True)
            ds = (p * (dp - row_dot) * scale).astype(BF16)
            ds_ref[group, :width] = ds
            flipped = flip8(ds.astype(F32))
            half = [pltpu.roll(flipped[8 * j:8 * j + 8], QB - 8 - r0 - 8 * j, 1, stride=1, stride_axis=0) for j in range(2)]
            dd_ref[group, :width] = jnp.concatenate(half, axis=0).astype(BF16)
            if stats:
                lane = lax.broadcasted_iota(jnp.int32, (16, HEAD), 1)
                st_ref[group, :] = jnp.where(lane == 0, top * (scale * LOG2E) + jnp.log2(total), row_dot)
        pb = pb_ref[:, :width]
        ds = ds_ref[:, :width]
        dd = dd_ref[:, :width]
        stage[0, hh, rows, :] = dot(pb, v_s[hh, :width, :]).astype(BF16)
        dqc = dot(ds, k_s[hh, :width, :])
        dqr = flip8(dot(dd, rev_s[head, SEQ - width:, :]))
        stage[1, hh, rows, :] = (dqc + dqr).astype(BF16)
        dr_acc[head, 1, HEAD:HEAD + 1, HALF - HEAD:] += jnp.sum(dqc, axis=0, keepdims=True)
        dr_acc[head, 1, HEAD + 1:HEAD + 2, HALF - HEAD:] += jnp.sum(dqr, axis=0, keepdims=True)
        dk_new = dot(at_s[hh, :, rows], ds_ref[:, lo:width])
        dv_new = dot(gt_s[hh, :, rows], pb_ref[:, lo:width])
        if fresh:
            dkt[hh] = dk_new
            dvt[hh] = dv_new
        else:
            dkt[hh, :, :width - lo] += dk_new
            dvt[hh, :, :width - lo] += dv_new
        dr_new = dot(ct_s[hh, :, rows], dd)
        if width > HALF:
            dr_acc[head, 0, :HEAD, SEQ - width:] += dr_new[:, :width - HALF]
            dr_acc[head, 1, :HEAD, :] += dr_new[:, width - HALF:]
        else:
            dr_acc[head, 1, :HEAD, HALF - width:] += dr_new

    def col_block(hh, head, sub, i0):
        rows = slice(i0, i0 + QB)
        first = WIN - i0
        s_ref[:, :HALF] = dot(a_s[hh, rows, :], kt_s[hh, :, :HALF])
        e_ref[:, :WIN] = dot(c_s[hh, rows, :], rt_s[head, :, first:first + WIN])
        dp_ref[:, :HALF] = dot(g_s[hh, rows, :], vt_s[hh, :, :HALF])
        st_ref[:, :8] = st_rx[sub, hh, :, i0 - HALF:i0 - HALF + QB].T
        for r0 in range(0, QB, 16):
            group = slice(r0, r0 + 16)
            rel = pltpu.roll(e_ref[group, :WIN], HALF + 1 + r0, 1, stride=1, stride_axis=0)[:, :HALF]
            log_sum = st_ref[group, 0:1]
            row_dot = st_ref[group, 1:2]
            p = jnp.exp2((s_ref[group, :HALF] + rel) * (scale * LOG2E) - log_sum)
            pb_ref[group, :HALF] = p.astype(BF16)
            ds_ref[group, :HALF] = (p * (dp_ref[group, :HALF] - row_dot) * scale).astype(BF16)
        dkt[hh] += dot(at_s[hh, :, rows], ds_ref[:, :HALF])
        dvt[hh] += dot(gt_s[hh, :, rows], pb_ref[:, :HALF])

    def store_rows(sub):
        for t in range(2):
            buf[2 + t, sub] = pltpu.einshape("abc->bac", stage[t])

    def store_keys(sub):
        for hh in range(PAIR):
            stage[2, hh] = dkt[hh].astype(BF16).T
            stage[3, hh] = dvt[hh].astype(BF16).T
        for t in range(2):
            buf[t, sub] = pltpu.einshape("abc->bac", stage[2 + t])

    def wait_up(sub):
        wait_for(rbuf.at[:, sub], up_recv.at[sub])
        wait_for(rbuf.at[:, sub], up_send.at[sub % 4])

    def wait_in(sub):
        wait_for(buf.at[2:4, sub], in_recv.at[1, sub])

    def lower_rows(sub):
        wait_in(sub)
        load_rows(buf, 2, buf, 3, sub, 0, True)

    def lower_own(sub):
        load_keys(buf, 0, buf, 1, sub, 0)

        def own(hh, carry):
            head = 2 * (sub // SLOTS) + hh
            row_block(hh, head, QB, QB, 0, True, False)
            row_block(hh, head, 0, 0, 0, False, False)
            return carry

        lax.fori_loop(0, PAIR, own, 0)
        store_rows(sub)

    def lower_theirs(sub):
        wait_up(sub)
        load_rows(rbuf, 0, rbuf, 1, sub, HALF, False)
        wait_for(st_rx.at[sub], st_recv.at[sub % 4])

        def theirs(hh, carry):
            head = 2 * (sub // SLOTS) + hh
            col_block(hh, head, sub, HALF)
            col_block(hh, head, sub, HALF + QB)
            return carry

        lax.fori_loop(0, PAIR, theirs, 0)
        store_keys(sub)

    def upper_own(sub):
        wait_in(sub)
        wait_up(sub)
        load_rows(buf, 0, buf, 1, sub, 0, True)
        load_keys(rbuf, 0, rbuf, 1, sub, 0)
        load_keys(buf, 2, buf, 3, sub, HALF)

        def own(hh, carry):
            head = 2 * (sub // SLOTS) + hh
            for blk in (1, 0):
                row_block(hh, head, QB * blk, HALF + QB * blk, HALF, blk == 1, True)
                st_tx[sub, hh, :, QB * blk:QB * (blk + 1)] = st_ref[...].T[:8]
            pltpu.make_async_remote_copy(src_ref=st_tx.at[sub, hh], dst_ref=st_rx.at[sub, hh], send_sem=st_send, recv_sem=st_recv.at[sub % 4],
                                         device_id=(across,), device_id_type=MESH).start()

            @pl.when(jnp.logical_not(tip))
            def _():
                pltpu.make_async_remote_copy(src_ref=st_tx.at[sub, hh, :, HALF - TIP:], dst_ref=tip_st.at[col, sub, hh], send_sem=ts_send,
                                             recv_sem=ts_recv, device_id=(N_DEV - 2 + core,), device_id_type=MESH).start()
            return carry

        lax.fori_loop(0, PAIR, own, 0)
        store_rows(sub)
        store_keys(sub)

    side = 1 - core
    parts = (dr0_out, dr1_out, dr2_out, dr3_out, dr4_out, dr5_out)

    def swap_start(p):
        for n in range(2):
            pltpu.make_async_remote_copy(src_ref=dr_acc.at[2 * p + n, side], dst_ref=dr_rx.at[p, n], send_sem=x_send, recv_sem=x_recv.at[p],
                                         device_id=(partner,), device_id_type=MESH).start()

    def swap_add(p):
        wait_for(dr_rx.at[p], x_recv.at[p])
        for n in range(2):
            dr_rx[p, n] = dr_rx[p, n] + dr_acc[2 * p + n, core]

    def cross_start(p):
        pltpu.make_async_remote_copy(src_ref=dr_rx.at[p, 1 - z], dst_ref=dr_rz.at[p], send_sem=z_send, recv_sem=z_recv.at[p],
                                     device_id=(across,), device_id_type=MESH).start()

    def head_of(p, bits):
        other = chip ^ bits
        return 4 * (other % 4) + 2 * p + other // 4

    def block(p, m, bits):
        if bits == 0:
            return dr_fin.at[p, PART * m:PART * (m + 1)]
        return parts[m].at[side, :, head_of(p, bits)]

    def forward(p, m, bits):
        pltpu.make_async_remote_copy(src_ref=block(p, m, bits), dst_ref=parts[m].at[side, :, head_of(p, bits)], send_sem=fw_send,
                                     recv_sem=fw_recv, device_id=(partner,), device_id_type=MESH).start()

    def blocks(count):
        return parts[0].at[:, :, :N_PART // 2 * count]

    def pass_on(p, bits, hop, device):
        for m in range(N_PART):
            pltpu.make_async_remote_copy(
                src_ref=block(p, m, bits), dst_ref=parts[m].at[side, :, head_of(p, bits)], send_sem=ring_send,
                recv_sem=ring_recv.at[p, hop], device_id=(device,), device_id_type=MESH).start()

    def hand_over(p, bits):
        for m in range(N_PART):
            forward(p, m, bits)

    even = chip % 2 == z
    loaded = y != z
    along_x, along_y = me ^ 2, me ^ 4

    def hop_start(p, hop):
        if hop == 0:
            for device in (along_x, along_y, across):
                pass_on(p, 0, 0, device)
        if hop == 1:
            @pl.when(even & loaded)
            def _():
                pass_on(p, 1, 1, along_y)

            @pl.when(jnp.logical_not(even) & loaded)
            def _():
                pass_on(p, 2, 1, along_x)

            pass_on(p, 1, 1, across)
            pass_on(p, 2, 1, across)
        if hop == 2:
            @pl.when(even & loaded)
            def _():
                pass_on(p, 5, 2, along_y)

            @pl.when(jnp.logical_not(even) & loaded)
            def _():
                pass_on(p, 6, 2, along_x)

            @pl.when(even)
            def _():
                pass_on(p, 3, 2, across)
        if hop == 3:
            @pl.when(even)
            def _():
                pass_on(p, 7, 3, across)

    def hop_wait(p, hop):
        if hop == 0:
            wait_for(blocks(3), ring_recv.at[p, 0])
            for bits in (1, 2, 4):
                hand_over(p, bits)
        if hop == 1:
            @pl.when(even)
            def _():
                wait_for(blocks(3), ring_recv.at[p, 1])
                hand_over(p, 3)

            @pl.when(jnp.logical_not(even))
            def _():
                wait_for(blocks(2), ring_recv.at[p, 1])
            for bits in (5, 6):
                hand_over(p, bits)
        if hop == 2:
            wait_for(blocks(1), ring_recv.at[p, 2])
            hand_over(p, 7)
        if hop == 3:
            @pl.when(jnp.logical_not(even))
            def _():
                wait_for(blocks(1), ring_recv.at[p, 3])
                hand_over(p, 3)

    def sent_wait():
        @pl.when(even & loaded)
        def _():
            wait_for(buf.at[:3, :, :FIN * 18 // 24], ring_send)

        @pl.when(even != loaded)
        def _():
            wait_for(buf.at[:3, :7, :FIN * 14 // 21], ring_send)

        @pl.when(jnp.logical_not(even | loaded))
        def _():
            wait_for(buf.at[:2, :6, :FIN * 10 // 12], ring_send)

    def cross_finish(p):
        wait_for(dr_rz.at[p], z_recv.at[p])
        total = dr_rx[p, z] + dr_rz[p]
        rev32 = eye_rev(F32)
        for m in range(HALF // HEAD):
            part = total[:HEAD, HALF - HEAD * (m + 1):HALF - HEAD * m]
            turned = lax.dot_general(rev32, part, (((1,), (1,)), ((), ())), precision=lax.Precision.HIGHEST, preferred_element_type=F32)
            dr_fin[p, HEAD * m:HEAD * (m + 1)] = turned.reshape(HEAD, 1, HEAD)
        dr_fin[p, HALF] = total[HEAD:HEAD + 1, HALF - HEAD:]
        dr_fin[p, HALF + 1] = total[HEAD + 1:HEAD + 2, HALF - HEAD:]
        dr_fin[p, HALF + 2:] = jnp.zeros((FIN - HALF - 2, 1, HEAD), F32)
        hop_start(p, 0)
        for m in range(N_PART):
            pltpu.make_async_copy(block(p, m, 0), parts[m].at[side, :, head_of(p, 0)], own_sem).start()
        hand_over(p, 0)

    def tip_load(unit):
        slot, row, far = unit % 2, unit // FAR, unit % FAR
        pair = far + tip_base
        for t, src in enumerate((q_in, k_in, v_in, g_in)):
            pltpu.make_async_copy(src.at[core * SLOTS + row, :, pair], r_buf.at[slot, pl.ds(TIP * t + ROWS * core, ROWS)], tip_sem.at[slot]).start()
            pltpu.make_async_copy(far_out.at[t, row, :, far], r_buf.at[slot, pl.ds(TIP * t + ROWS * (1 - core), ROWS)], tip_sem.at[slot]).start()
        pltpu.make_async_copy(r_in.at[:TIP, pair], r_buf.at[slot, 4 * TIP:5 * TIP], tip_sem.at[slot]).start()

    def tip_done(slot):
        wait_for(r_buf.at[slot, :TIP], tip_near.at[slot])
        wait_for(r_buf.at[slot, :TIP], tip_send.at[slot])

    def tip_group(hh, r0):
        group = slice(TIP * hh + r0, TIP * hh + r0 + 16)
        rel = pltpu.roll(e_ref[group, :TIP], 1 + r0, 1, stride=1, stride_axis=0)
        ahead = lax.broadcasted_iota(jnp.int32, (16, TIP), 1) - lax.broadcasted_iota(jnp.int32, (16, TIP), 0)
        return group, s_ref[group, :TIP] + rel, ahead <= r0

    def tip_rows(hh):
        for r0 in range(0, TIP, 16):
            group, s, seen = tip_group(hh, r0)
            s = jnp.where(seen, s, -jnp.inf)
            top = jnp.max(s, axis=1, keepdims=True)
            p = jnp.exp2((s - top) * (scale * LOG2E))
            p = p * (1.0 / jnp.sum(p, axis=1, keepdims=True))
            pb_ref[group, :TIP] = p.astype(BF16)
            dp = dp_ref[group, :TIP]
            row_dot = jnp.sum(p * dp, axis=1, keepdims=True)
            ds = (p * (dp - row_dot) * scale).astype(BF16)
            ds_ref[group, :TIP] = ds
            flipped = flip8(ds.astype(F32))
            half = [pltpu.roll(flipped[8 * j:8 * j + 8], TIP - 8 - r0 - 8 * j, 1, stride=1, stride_axis=0) for j in range(2)]
            dd_ref[group, :TIP] = jnp.concatenate(half, axis=0).astype(BF16)
        rows = slice(TIP * hh, TIP * (hh + 1))
        stage[0, hh, :TIP, :] = dot(pb_ref[rows, :TIP], v_s[hh, :TIP, :]).astype(BF16)
        dqc = dot(ds_ref[rows, :TIP], k_s[hh, :TIP, :])
        dqr = flip8(dot(dd_ref[rows, :TIP], c_s[hh, :TIP, :]))
        stage[1, hh, :TIP, :] = (dqc + dqr).astype(BF16)

    def tip_keys(hh, stats):
        rows = slice(TIP * hh, TIP * (hh + 1))
        st_ref[rows, :8] = stats.T
        for r0 in range(0, TIP, 16):
            group, s, seen = tip_group(hh, r0)
            p = jnp.where(seen, jnp.exp2(s * (scale * LOG2E) - st_ref[group, 0:1]), 0.0)
            pb_ref[group, :TIP] = p.astype(BF16)
            ds_ref[group, :TIP] = (p * (dp_ref[group, :TIP] - st_ref[group, 1:2]) * scale).astype(BF16)
        over_rows = (((0,), (0,)), ((), ()))
        stage[0, hh, :TIP, :] = lax.dot_general(ds_ref[rows, :TIP], a_s[hh, :TIP, :], over_rows, preferred_element_type=F32).astype(BF16)
        stage[1, hh, :TIP, :] = lax.dot_general(pb_ref[rows, :TIP], g_s[hh, :TIP, :], over_rows, preferred_element_type=F32).astype(BF16)

    def tip_unit(unit, carry):
        slot, row, far = unit % 2, unit // FAR, unit % FAR
        pair = far + tip_base
        wait_for(r_buf.at[slot, :5 * TIP], tip_sem.at[slot])

        @pl.when(unit + 1 < UNITS)
        def _():
            tip_load(unit + 1)

        q2, k2, v2, g2, r2 = [pltpu.einshape("abc->bac", r_buf[slot, TIP * t:TIP * (t + 1)]) for t in range(5)]
        u = u_buf[pair].astype(F32)
        w = w_buf[pair].astype(F32)
        for hh in range(PAIR):
            rows = slice(TIP * hh, TIP * (hh + 1))
            q32 = q2[hh].astype(F32)
            a = (q32 + u[hh:hh + 1]).astype(BF16)
            c = (q32 + w[hh:hh + 1]).astype(BF16)
            falling = dot(eye_rev(BF16), r2[hh]).astype(BF16)
            s_ref[rows, :TIP] = dot(a, k2[hh].T)
            e_ref[rows, :TIP] = dot(c, falling.T)
            dp_ref[rows, :TIP] = dot(g2[hh], v2[hh].T)
            a_s[hh, :TIP, :] = a
            c_s[hh, :TIP, :] = falling
            g_s[hh, :TIP, :] = g2[hh]
            k_s[hh, :TIP, :] = k2[hh]
            v_s[hh, :TIP, :] = v2[hh]

        @pl.when(lower)
        def _():
            for hh in range(PAIR):
                tip_rows(hh)

        @pl.when(upper)
        def _():
            for hh in range(PAIR):
                tip_keys(hh, tip_st[far // 2, (far % 2) * SLOTS + row, hh])

        @pl.when(unit >= 2)
        def _():
            tip_done(slot)

        for n in range(2):
            r_buf[slot, (5 + n) * TIP:(6 + n) * TIP] = pltpu.einshape("abc->bac", stage[n, :, :TIP, :])
        place = (core * SLOTS + row, slice(None), pair)

        def give(results):
            for n, dst in enumerate(results):
                pltpu.make_async_copy(r_buf.at[slot, pl.ds((5 + n) * TIP + ROWS * core, ROWS)], dst.at[place], tip_near.at[slot]).start()
                pltpu.make_async_remote_copy(
                    src_ref=r_buf.at[slot, pl.ds((5 + n) * TIP + ROWS * (1 - core), ROWS)], dst_ref=dst.at[place],
                    send_sem=tip_send.at[slot], recv_sem=out_recv, device_id=(partner,), device_id_type=MESH).start()

        @pl.when(lower)
        def _():
            give((o_out, dq_out))

        @pl.when(upper)
        def _():
            give((dk_out, dv_out))
        return carry

    def tips(third):
        @pl.when(tip)
        def _():
            if third == 0:
                wait_for(far_out, far_recv)

                @pl.when(upper)
                def _():
                    wait_for(tip_st, ts_recv)
                tip_load(0)
            lax.fori_loop(UNITS // 3 * third, UNITS // 3 * (third + 1), tip_unit, 0)
            if third == 2:
                tip_done(0)
                tip_done(1)

    send_up(0)

    def sub_body(sub, carry):
        @pl.when(sub < SUBS - 1)
        def _():
            send_up(sub + 1)

        @pl.when(sub == SLOTS)
        def _():
            swap_start(0)

        @pl.when(sub == SUBS - 1)
        def _():
            swap_add(0)
            cross_start(0)

        @pl.when(sub == SUBS)
        def _():
            swap_start(1)
            swap_add(1)
            cross_start(1)
            cross_finish(0)

        @pl.when(lower & (sub < SUBS))
        def _():
            lower_rows(sub)

        @pl.when(lower & (sub > 0))
        def _():
            lower_theirs(sub - 1)

        @pl.when(lower & (sub < SUBS))
        def _():
            lower_own(sub)

        @pl.when(upper & (sub < SUBS))
        def _():
            upper_own(sub)

        @pl.when(sub <= EARLY)
        def _():
            send_out(sub, (2, 3))

        @pl.when((sub > 0) & (sub <= EARLY))
        def _():
            send_out(sub - 1, (0, 1))
        return carry

    lax.fori_loop(0, SUBS + 1, sub_body, 0)

    cross_finish(1)
    send_out(EARLY, (0, 1))
    for p in range(2):
        hop_wait(p, 0)
        hop_start(p, 1)
    for p in range(2):
        send_out(EARLY + 1 + p, range(4))
        tips(p)
        hop_wait(p, 1)
        hop_start(p, 2)

    def send_late(sub, carry):
        send_out(sub, range(4))
        return carry

    lax.fori_loop(EARLY + 3, SUBS, send_late, 0)
    tips(2)
    for p in range(2):
        hop_wait(p, 2)
        hop_start(p, 3)
    for p in range(2):
        hop_wait(p, 3)

    wait_for(buf.at[:, :, :HALF - ROWS], in_send)

    @pl.when(tip)
    def _():
        wait_for(buf.at[:, :, :HALF - 3 * ROWS // 2], out_recv)
        wait_for(buf.at[:, :, :HALF - ROWS], out_send)
        wait_for(far_out, far_send)

    @pl.when(jnp.logical_not(tip))
    def _():
        wait_for(buf, out_recv)
        wait_for(buf.at[:, :, :HALF - 2 * ROWS], out_send)

    @pl.when(upper & jnp.logical_not(tip))
    def _():
        wait_for(st_tx.at[:2], ts_send)

    @pl.when(upper)
    def _():
        wait_for(st_tx, st_send)

    wait_for(dr_rx, x_send)
    wait_for(dr_rz, z_send)
    wait_for(blocks(2), own_sem)
    sent_wait()
    for sem in (fw_send, fw_recv):
        wait_for(buf.at[:3, :, :FIN * 16 // 24], sem)


def writer(*refs):
    ins, (o, dq, dk, dv, dr, du, dw, sem) = refs[:4 + N_PART], refs[4 + N_PART:]
    pairs = list(zip(ins[:4], (o, dq, dk, dv)))
    for m, part in enumerate(ins[4:]):
        rows = min(PART, HALF - PART * m)
        for side in range(2):
            start = HALF * side + PART * m
            pairs.append((part.at[side, :rows], dr.at[start:start + rows]))
    last = HALF - PART * (N_PART - 1)
    pairs += [(ins[-1].at[0, last], du), (ins[-1].at[0, last + 1], dw)]
    copies = [pltpu.make_async_copy(src, dst, sem.at[j]) for j, (src, dst) in enumerate(pairs)]
    for copy in copies:
        copy.start()
    for copy in copies:
        copy.wait()


def solution(mesh):
    seq_spec = P(None, "cp", None, None)

    def local(query, key_in, value, bias_u, bias_w, rel_k, d_out):
        n_batch, rows, n_heads, head_dim = query.shape
        pairs = (n_batch, rows, N_PAIR, PAIR, head_dim)
        vm = pltpu.VMEM
        dma = pltpu.SemaphoreType.DMA
        whole = pl.BlockSpec(memory_space=pl.ANY)
        act = jax.ShapeDtypeStruct(pairs, BF16)
        vec = jax.ShapeDtypeStruct((n_heads, 1, head_dim), F32)
        tok = (PAIR, SEQ, HEAD)
        tok_t = (PAIR, HEAD, SEQ)
        acc = (HEAD + 8, HALF)
        outs = pl.pallas_call(
            kernel,
            name="rel_attn",
            out_shape=(act, act, act, act,
                       *[jax.ShapeDtypeStruct((2, PART, n_heads, 1, head_dim), F32)] * N_PART,
                       jax.ShapeDtypeStruct((4, SLOTS, ROWS, FAR, PAIR, HEAD), BF16)),
            in_specs=[pl.BlockSpec(memory_space=pltpu.HBM)] * 7,
            out_specs=[whole] * (5 + N_PART),
            scratch_shapes=[
                vm((4, SUBS, HALF, PAIR, HEAD), BF16), vm((2, SUBS, HALF, PAIR, HEAD), BF16),
                vm((2, SEQ, PAIR, HEAD), BF16), vm((N_PAIR, PAIR, HEAD), BF16), vm((N_PAIR, PAIR, HEAD), BF16),
                vm((SUBS, PAIR, 8, HALF), F32), vm((SUBS, PAIR, 8, HALF), F32), vm((3, SUBS, PAIR, 8, TIP), F32), vm((QB, HEAD), F32),
                vm((2, 2) + acc, F32), vm((2,) + acc, F32), vm((2, FIN, 1, HEAD), F32), vm((4, 2) + acc, F32),
                vm((QB, SEQ), F32), vm((QB, SEQ), F32), vm((QB, SEQ), F32),
                vm((QB, SEQ), BF16), vm((QB, SEQ), BF16), vm((QB, SEQ), BF16),
                vm(tok, BF16), vm(tok, BF16), vm(tok, BF16), vm(tok, BF16), vm(tok, BF16),
                vm(tok_t, BF16), vm(tok_t, BF16), vm(tok_t, BF16), vm(tok_t, BF16), vm(tok_t, BF16),
                vm((4, SEQ, HEAD), BF16), vm((4, HEAD, SEQ), BF16),
                vm((PAIR, HEAD, HALF), F32), vm((PAIR, HEAD, HALF), F32), vm((4, PAIR, HALF, HEAD), BF16),
                dma, dma((2, SUBS)), dma, dma, dma, dma((4,)), dma((4,)), dma((SUBS,)), dma, dma((4,)),
                dma, dma((2,)), dma, dma((2,)), dma, dma((2, 4)), dma, dma,
                dma, dma, dma((2,)), dma((2,)), dma((2,)), dma, dma,
            ],
            compiler_params=pltpu.CompilerParams(has_side_effects=True, vmem_limit_bytes=37 * 1024 * 1024),
        )(*[pltpu.with_memory_space_constraint(x, pltpu.HBM) for x in (
            query.reshape(pairs), key_in.reshape(pairs), value.reshape(pairs), d_out.reshape(pairs),
            rel_k.reshape(SEQ, N_PAIR, PAIR, head_dim), bias_u.reshape(N_PAIR, PAIR, head_dim), bias_w.reshape(N_PAIR, PAIR, head_dim))])
        o, dq, dk, dv, dr, du, dw = pl.pallas_call(
            writer,
            name="writer",
            out_shape=(act, act, act, act, jax.ShapeDtypeStruct((SEQ, n_heads, 1, head_dim), F32), vec, vec),
            in_specs=[whole] * (4 + N_PART),
            out_specs=[whole] * 7,
            scratch_shapes=[dma((6 + 2 * N_PART,))],
            compiler_params=pltpu.CompilerParams(vmem_limit_bytes=1024 * 1024),
        )(*outs[:-1])
        full = query.shape
        return (o.reshape(full), dq.reshape(full), dk.reshape(full), dv.reshape(full),
                du.reshape(bias_u.shape), dw.reshape(bias_w.shape), dr.reshape(rel_k.shape))

    return jax.shard_map(local, mesh=mesh,
                         in_specs=(seq_spec, seq_spec, seq_spec, P(), P(), P(), seq_spec),
                         out_specs=(seq_spec, seq_spec, seq_spec, seq_spec, P(), P(), P()),
                         check_vma=False)
```

```python
import jax
import jax.numpy as jnp
from jax import lax
from jax.experimental import pallas as pl
from jax.experimental.pallas import tpu as pltpu
from jax.sharding import PartitionSpec as P

MESH = pl.DeviceIdType.MESH
BF16, F32 = jnp.bfloat16, jnp.float32
LOG2E = 1.4426950408889634

N_DEV = 16
PLANE = 8
PAIR = 2
N_PAIR = 8
SLOTS = 4
SUBS = 2 * SLOTS
EARLY = 3
ROWS = 64
HALF = PLANE * ROWS
SEQ = 2 * HALF
HEAD = 128
QB = 256
WIN = HALF + QB
N_PART = 6
PART = 86
FIN = N_PART * PART
TIP = 2 * ROWS
FAR = N_PAIR - 2
UNITS = FAR * SLOTS
TURNS = ((1, 3, 2), (3, 1, 2))


def dot(lhs, rhs):
    return jnp.dot(lhs, rhs, preferred_element_type=F32)


def flip8(x):
    rows, cols = x.shape
    idx = 7 - lax.broadcasted_iota(jnp.int32, (rows // 8, 8, cols), 1)
    return jnp.take_along_axis(x.reshape(rows // 8, 8, cols), idx, axis=1).reshape(rows, cols)


def eye_rev(dtype):
    total = lax.broadcasted_iota(jnp.int32, (HEAD, HEAD), 0) + lax.broadcasted_iota(jnp.int32, (HEAD, HEAD), 1)
    return jnp.where(total == HEAD - 1, 1.0, 0.0).astype(dtype)


def kernel(q_in, k_in, v_in, g_in, r_in, u_in, w_in,
           o_out, dq_out, dk_out, dv_out, dr0_out, dr1_out, dr2_out, dr3_out, dr4_out, dr5_out, far_out,
           buf, rbuf, r_buf, u_buf, w_buf, st_tx, st_rx, tip_st, st_ref, dr_rx, dr_rz, dr_fin, dr_acc,
           s_ref, e_ref, dp_ref, pb_ref, ds_ref, dd_ref,
           a_s, c_s, g_s, k_s, v_s, at_s, ct_s, gt_s, kt_s, vt_s, rev_s, rt_s, dkt, dvt, stage,
           in_send, in_recv, out_send, out_recv, own_sem, r_sem, up_send, up_recv, st_send, st_recv,
           x_send, x_recv, z_send, z_recv, ring_send, ring_recv, fw_send, fw_recv,
           far_send, far_recv, tip_sem, tip_near, tip_send, ts_send, ts_recv):
    me = lax.axis_index("cp")
    core = me % 2
    chip = me // 2
    col = chip % 4
    z = chip // 4
    partner = me + 1 - 2 * core
    across = me + PLANE * (1 - 2 * z)
    scale = HEAD ** -0.5

    def wait_for(ref, sem):
        pltpu.make_async_copy(ref, ref, sem).wait()

    y = col // 2
    lower, upper = z == 0, z == 1
    tip = chip == 7 * z
    tip_base = 2 - 2 * z

    tables = [pltpu.make_async_copy(src, dst, r_sem.at[j]) for j, (src, dst) in enumerate(
        ((r_in.at[:, 2 * col], r_buf.at[0]), (r_in.at[:, 2 * col + 1], r_buf.at[1]), (u_in, u_buf), (w_in, w_buf)))]
    for copy in tables:
        copy.start()

    barrier = pltpu.get_barrier_semaphore()

    for peer in [across] + [me ^ step for step in range(PLANE - 1, 0, -1)]:
        pl.semaphore_signal(barrier, inc=1, device_id=(peer,), device_id_type=MESH)
    pl.semaphore_wait(barrier, PLANE)

    my_rows = pl.ds(pl.multiple_of((me % PLANE) * ROWS, ROWS), ROWS)

    def peers():
        first, second, third = [jnp.where(core == 0, near_turn, far_turn) for near_turn, far_turn in zip(*TURNS)]
        for turn, other in ((first, 0), (third, 0), (first, 1), (third, 1), (second, 0), (second, 1)):
            yield me ^ (2 * turn + other)
        yield partner

    def send_in(ins, sub):
        pair, row = sub // SLOTS, sub % SLOTS
        for first in (0, 2):
            for t in (first, first + 1):
                pltpu.make_async_copy(ins[t].at[core * SLOTS + row, :, 2 * col + pair], buf.at[t, sub, my_rows], in_recv.at[first // 2, sub]).start()
            for peer in peers():
                for t in (first, first + 1):
                    pltpu.make_async_remote_copy(
                        src_ref=ins[t].at[(peer % 2) * SLOTS + row, :, 2 * ((peer // 2) % 4) + pair], dst_ref=buf.at[t, sub, my_rows],
                        send_sem=in_send, recv_sem=in_recv.at[first // 2, sub], device_id=(peer,), device_id_type=MESH).start()

    def send_all(ins):
        def send_sub(sub, carry):
            send_in(ins, sub)
            return carry
        lax.fori_loop(0, SUBS, send_sub, 0)

    @pl.when(lower)
    def _():
        send_all((k_in, v_in, q_in, g_in))

    @pl.when(upper)
    def _():
        send_all((q_in, g_in, k_in, v_in))

    @pl.when(tip)
    def _():
        for t, src in enumerate((q_in, k_in, v_in, g_in)):
            for row in range(SLOTS):
                pltpu.make_async_remote_copy(
                    src_ref=src.at[(1 - core) * SLOTS + row, :, pl.ds(tip_base, FAR)], dst_ref=far_out.at[t, row],
                    send_sem=far_send, recv_sem=far_recv, device_id=(partner,), device_id_type=MESH).start()

    for copy in tables:
        copy.wait()
    rev = eye_rev(BF16)
    for p in range(2):
        pair_tab = pltpu.einshape("abc->bac", r_buf[p])
        for hh in range(PAIR):
            for blk in range(SEQ // HEAD):
                part = pair_tab[hh, SEQ - HEAD * (blk + 1):SEQ - HEAD * blk]
                flipped = dot(rev, part).astype(BF16)
                rev_s[2 * p + hh, HEAD * blk:HEAD * (blk + 1), :] = flipped
                rt_s[2 * p + hh, :, HEAD * blk:HEAD * (blk + 1)] = flipped.T
    dr_acc[...] = jnp.zeros_like(dr_acc)

    acts = (dk_out, dv_out, o_out, dq_out)

    def send_out(sub, which):
        place = (core * SLOTS + sub % SLOTS, slice(None), 2 * col + sub // SLOTS)
        for t in which:
            pltpu.make_async_copy(buf.at[t, sub, my_rows], acts[t].at[place], out_recv).start()
        for peer in peers():
            peer_rows = pl.ds(pl.multiple_of((peer % PLANE) * ROWS, ROWS), ROWS)
            to_tip = (peer // 2 == 7 * z) & jnp.logical_not(tip)
            for t in which:
                @pl.when(jnp.logical_not(to_tip & (lower if t >= 2 else upper)))
                def _():
                    pltpu.make_async_remote_copy(
                        src_ref=buf.at[t, sub, peer_rows], dst_ref=acts[t].at[place],
                        send_sem=out_send, recv_sem=out_recv, device_id=(peer,), device_id_type=MESH).start()

    def send_up(sub):
        wait_for(buf.at[0:2, sub], in_recv.at[0, sub])
        for j in range(2):
            pltpu.make_async_remote_copy(src_ref=buf.at[j, sub], dst_ref=rbuf.at[j, sub], send_sem=up_send.at[sub % 4], recv_sem=up_recv.at[sub],
                                         device_id=(across,), device_id_type=MESH).start()

    def unpack(ref, j, sub):
        return pltpu.einshape("abc->bac", ref[j, sub])

    def load_rows(q_ref, q_j, g_ref, g_j, sub, start, turned):
        rows = slice(start, start + HALF)
        p = sub // SLOTS
        q2 = unpack(q_ref, q_j, sub)
        u = u_buf[2 * col + p].astype(F32)
        w = w_buf[2 * col + p].astype(F32)
        for hh in range(PAIR):
            q32 = q2[hh].astype(F32)
            a = (q32 + u[hh:hh + 1]).astype(BF16)
            c = (q32 + w[hh:hh + 1]).astype(BF16)
            a_s[hh, rows, :] = a
            c_s[hh, rows, :] = c
            at_s[hh, :, rows] = a.T
            if turned:
                ct_s[hh, :, rows] = flip8(c.astype(F32)).astype(BF16).T
        g2 = unpack(g_ref, g_j, sub)
        g_s[:, rows, :] = g2
        for hh in range(PAIR):
            gt_s[hh, :, rows] = g2[hh].T

    def load_keys(k_ref, k_j, v_ref, v_j, sub, start):
        rows = slice(start, start + HALF)
        k2 = unpack(k_ref, k_j, sub)
        v2 = unpack(v_ref, v_j, sub)
        k_s[:, rows, :] = k2
        v_s[:, rows, :] = v2
        for hh in range(PAIR):
            kt_s[hh, :, rows] = k2[hh].T
            vt_s[hh, :, rows] = v2[hh].T

    def row_block(hh, head, start, i0, lo, fresh, stats):
        width = i0 + QB
        rows = slice(start, start + QB)
        s_ref[:, :width] = dot(a_s[hh, rows, :], kt_s[hh, :, :width])
        e_ref[:, :width] = dot(c_s[hh, rows, :], rt_s[head, :, SEQ - width:])
        dp_ref[:, :width] = dot(g_s[hh, rows, :], vt_s[hh, :, :width])
        for r0 in range(0, QB, 16):
            group = slice(r0, r0 + 16)
            rel = pltpu.roll(e_ref[group, :width], i0 + 1 + r0, 1, stride=1, stride_axis=0)
            s = s_ref[group, :width] + rel
            ahead = lax.broadcasted_iota(jnp.int32, (16, width), 1) - lax.broadcasted_iota(jnp.int32, (16, width), 0)
            s = jnp.where(ahead <= i0 + r0, s, -jnp.inf)
            top = jnp.max(s, axis=1, keepdims=True)
            p = jnp.exp2((s - top) * (scale * LOG2E))
            total = jnp.sum(p, axis=1, keepdims=True)
            p = p * (1.0 / total)
            pb_ref[group, :width] = p.astype(BF16)
            dp = dp_ref[group, :width]
            row_dot = jnp.sum(p * dp, axis=1, keepdims=True)
            ds = (p * (dp - row_dot) * scale).astype(BF16)
            ds_ref[group, :width] = ds
            flipped = flip8(ds.astype(F32))
            half = [pltpu.roll(flipped[8 * j:8 * j + 8], QB - 8 - r0 - 8 * j, 1, stride=1, stride_axis=0) for j in range(2)]
            dd_ref[group, :width] = jnp.concatenate(half, axis=0).astype(BF16)
            if stats:
                lane = lax.broadcasted_iota(jnp.int32, (16, HEAD), 1)
                st_ref[group, :] = jnp.where(lane == 0, top * (scale * LOG2E) + jnp.log2(total), row_dot)
        pb = pb_ref[:, :width]
        ds = ds_ref[:, :width]
        dd = dd_ref[:, :width]
        stage[0, hh, rows, :] = dot(pb, v_s[hh, :width, :]).astype(BF16)
        dqc = dot(ds, k_s[hh, :width, :])
        dqr = flip8(dot(dd, rev_s[head, SEQ - width:, :]))
        stage[1, hh, rows, :] = (dqc + dqr).astype(BF16)
        dr_acc[head, 1, HEAD:HEAD + 1, HALF - HEAD:] += jnp.sum(dqc, axis=0, keepdims=True)
        dr_acc[head, 1, HEAD + 1:HEAD + 2, HALF - HEAD:] += jnp.sum(dqr, axis=0, keepdims=True)
        dk_new = dot(at_s[hh, :, rows], ds_ref[:, lo:width])
        dv_new = dot(gt_s[hh, :, rows], pb_ref[:, lo:width])
        if fresh:
            dkt[hh] = dk_new
            dvt[hh] = dv_new
        else:
            dkt[hh, :, :width - lo] += dk_new
            dvt[hh, :, :width - lo] += dv_new
        dr_new = dot(ct_s[hh, :, rows], dd)
        if width > HALF:
            dr_acc[head, 0, :HEAD, SEQ - width:] += dr_new[:, :width - HALF]
            dr_acc[head, 1, :HEAD, :] += dr_new[:, width - HALF:]
        else:
            dr_acc[head, 1, :HEAD, HALF - width:] += dr_new

    def col_block(hh, head, sub, i0):
        rows = slice(i0, i0 + QB)
        first = WIN - i0
        s_ref[:, :HALF] = dot(a_s[hh, rows, :], kt_s[hh, :, :HALF])
        e_ref[:, :WIN] = dot(c_s[hh, rows, :], rt_s[head, :, first:first + WIN])
        dp_ref[:, :HALF] = dot(g_s[hh, rows, :], vt_s[hh, :, :HALF])
        st_ref[:, :8] = st_rx[sub, hh, :, i0 - HALF:i0 - HALF + QB].T
        for r0 in range(0, QB, 16):
            group = slice(r0, r0 + 16)
            rel = pltpu.roll(e_ref[group, :WIN], HALF + 1 + r0, 1, stride=1, stride_axis=0)[:, :HALF]
            log_sum = st_ref[group, 0:1]
            row_dot = st_ref[group, 1:2]
            p = jnp.exp2((s_ref[group, :HALF] + rel) * (scale * LOG2E) - log_sum)
            pb_ref[group, :HALF] = p.astype(BF16)
            ds_ref[group, :HALF] = (p * (dp_ref[group, :HALF] - row_dot) * scale).astype(BF16)
        dkt[hh] += dot(at_s[hh, :, rows], ds_ref[:, :HALF])
        dvt[hh] += dot(gt_s[hh, :, rows], pb_ref[:, :HALF])

    def store_rows(sub):
        for t in range(2):
            buf[2 + t, sub] = pltpu.einshape("abc->bac", stage[t])

    def store_keys(sub):
        for hh in range(PAIR):
            stage[2, hh] = dkt[hh].astype(BF16).T
            stage[3, hh] = dvt[hh].astype(BF16).T
        for t in range(2):
            buf[t, sub] = pltpu.einshape("abc->bac", stage[2 + t])

    def wait_up(sub):
        wait_for(rbuf.at[:, sub], up_recv.at[sub])
        wait_for(rbuf.at[:, sub], up_send.at[sub % 4])

    def wait_in(sub):
        wait_for(buf.at[2:4, sub], in_recv.at[1, sub])

    def lower_rows(sub):
        wait_in(sub)
        load_rows(buf, 2, buf, 3, sub, 0, True)

    def lower_own(sub):
        load_keys(buf, 0, buf, 1, sub, 0)

        def own(hh, carry):
            head = 2 * (sub // SLOTS) + hh
            row_block(hh, head, QB, QB, 0, True, False)
            row_block(hh, head, 0, 0, 0, False, False)
            return carry

        lax.fori_loop(0, PAIR, own, 0)
        store_rows(sub)

    def lower_theirs(sub):
        wait_up(sub)
        load_rows(rbuf, 0, rbuf, 1, sub, HALF, False)
        wait_for(st_rx.at[sub], st_recv.at[sub % 4])

        def theirs(hh, carry):
            head = 2 * (sub // SLOTS) + hh
            col_block(hh, head, sub, HALF)
            col_block(hh, head, sub, HALF + QB)
            return carry

        lax.fori_loop(0, PAIR, theirs, 0)
        store_keys(sub)

    def upper_own(sub):
        wait_in(sub)
        wait_up(sub)
        load_rows(buf, 0, buf, 1, sub, 0, True)
        load_keys(rbuf, 0, rbuf, 1, sub, 0)
        load_keys(buf, 2, buf, 3, sub, HALF)

        def own(hh, carry):
            head = 2 * (sub // SLOTS) + hh
            for blk in (1, 0):
                row_block(hh, head, QB * blk, HALF + QB * blk, HALF, blk == 1, True)
                st_tx[sub, hh, :, QB * blk:QB * (blk + 1)] = st_ref[...].T[:8]
            pltpu.make_async_remote_copy(src_ref=st_tx.at[sub, hh], dst_ref=st_rx.at[sub, hh], send_sem=st_send, recv_sem=st_recv.at[sub % 4],
                                         device_id=(across,), device_id_type=MESH).start()

            @pl.when(jnp.logical_not(tip))
            def _():
                pltpu.make_async_remote_copy(src_ref=st_tx.at[sub, hh, :, HALF - TIP:], dst_ref=tip_st.at[col, sub, hh], send_sem=ts_send,
                                             recv_sem=ts_recv, device_id=(N_DEV - 2 + core,), device_id_type=MESH).start()
            return carry

        lax.fori_loop(0, PAIR, own, 0)
        store_rows(sub)
        store_keys(sub)

    side = 1 - core
    parts = (dr0_out, dr1_out, dr2_out, dr3_out, dr4_out, dr5_out)

    def swap_start(p):
        for n in range(2):
            pltpu.make_async_remote_copy(src_ref=dr_acc.at[2 * p + n, side], dst_ref=dr_rx.at[p, n], send_sem=x_send, recv_sem=x_recv.at[p],
                                         device_id=(partner,), device_id_type=MESH).start()

    def swap_add(p):
        wait_for(dr_rx.at[p], x_recv.at[p])
        for n in range(2):
            dr_rx[p, n] = dr_rx[p, n] + dr_acc[2 * p + n, core]

    def cross_start(p):
        pltpu.make_async_remote_copy(src_ref=dr_rx.at[p, 1 - z], dst_ref=dr_rz.at[p], send_sem=z_send, recv_sem=z_recv.at[p],
                                     device_id=(across,), device_id_type=MESH).start()

    def head_of(p, bits):
        other = chip ^ bits
        return 4 * (other % 4) + 2 * p + other // 4

    def block(p, m, bits):
        if bits == 0:
            return dr_fin.at[p, PART * m:PART * (m + 1)]
        return parts[m].at[side, :, head_of(p, bits)]

    def forward(p, m, bits):
        pltpu.make_async_remote_copy(src_ref=block(p, m, bits), dst_ref=parts[m].at[side, :, head_of(p, bits)], send_sem=fw_send,
                                     recv_sem=fw_recv, device_id=(partner,), device_id_type=MESH).start()

    def blocks(count):
        return parts[0].at[:, :, :N_PART // 2 * count]

    def pass_on(p, bits, hop, device):
        for m in range(N_PART):
            pltpu.make_async_remote_copy(
                src_ref=block(p, m, bits), dst_ref=parts[m].at[side, :, head_of(p, bits)], send_sem=ring_send,
                recv_sem=ring_recv.at[p, hop], device_id=(device,), device_id_type=MESH).start()

    def hand_over(p, bits):
        for m in range(N_PART):
            forward(p, m, bits)

    even = chip % 2 == z
    loaded = y != z
    along_x, along_y = me ^ 2, me ^ 4

    def hop_start(p, hop):
        if hop == 0:
            for device in (along_x, along_y, across):
                pass_on(p, 0, 0, device)
        if hop == 1:
            @pl.when(even & loaded)
            def _():
                pass_on(p, 1, 1, along_y)

            @pl.when(jnp.logical_not(even) & loaded)
            def _():
                pass_on(p, 2, 1, along_x)

            pass_on(p, 1, 1, across)
            pass_on(p, 2, 1, across)
        if hop == 2:
            @pl.when(even & loaded)
            def _():
                pass_on(p, 5, 2, along_y)

            @pl.when(jnp.logical_not(even) & loaded)
            def _():
                pass_on(p, 6, 2, along_x)

            @pl.when(even)
            def _():
                pass_on(p, 3, 2, across)
        if hop == 3:
            @pl.when(even)
            def _():
                pass_on(p, 7, 3, across)

    def hop_wait(p, hop):
        if hop == 0:
            wait_for(blocks(3), ring_recv.at[p, 0])
            for bits in (1, 2, 4):
                hand_over(p, bits)
        if hop == 1:
            @pl.when(even)
            def _():
                wait_for(blocks(3), ring_recv.at[p, 1])
                hand_over(p, 3)

            @pl.when(jnp.logical_not(even))
            def _():
                wait_for(blocks(2), ring_recv.at[p, 1])
            for bits in (5, 6):
                hand_over(p, bits)
        if hop == 2:
            wait_for(blocks(1), ring_recv.at[p, 2])
            hand_over(p, 7)
        if hop == 3:
            @pl.when(jnp.logical_not(even))
            def _():
                wait_for(blocks(1), ring_recv.at[p, 3])
                hand_over(p, 3)

    def sent_wait():
        @pl.when(even & loaded)
        def _():
            wait_for(buf.at[:3, :, :FIN * 18 // 24], ring_send)

        @pl.when(even != loaded)
        def _():
            wait_for(buf.at[:3, :7, :FIN * 14 // 21], ring_send)

        @pl.when(jnp.logical_not(even | loaded))
        def _():
            wait_for(buf.at[:2, :6, :FIN * 10 // 12], ring_send)

    def cross_finish(p):
        wait_for(dr_rz.at[p], z_recv.at[p])
        total = dr_rx[p, z] + dr_rz[p]
        rev32 = eye_rev(F32)
        for m in range(HALF // HEAD):
            part = total[:HEAD, HALF - HEAD * (m + 1):HALF - HEAD * m]
            turned = lax.dot_general(rev32, part, (((1,), (1,)), ((), ())), precision=lax.Precision.HIGHEST, preferred_element_type=F32)
            dr_fin[p, HEAD * m:HEAD * (m + 1)] = turned.reshape(HEAD, 1, HEAD)
        dr_fin[p, HALF] = total[HEAD:HEAD + 1, HALF - HEAD:]
        dr_fin[p, HALF + 1] = total[HEAD + 1:HEAD + 2, HALF - HEAD:]
        dr_fin[p, HALF + 2:] = jnp.zeros((FIN - HALF - 2, 1, HEAD), F32)
        hop_start(p, 0)
        for m in range(N_PART):
            pltpu.make_async_copy(block(p, m, 0), parts[m].at[side, :, head_of(p, 0)], own_sem).start()
        hand_over(p, 0)

    def tip_load(unit):
        slot, row, far = unit % 2, unit // FAR, unit % FAR
        pair = far + tip_base
        for t, src in enumerate((q_in, k_in, v_in, g_in)):
            pltpu.make_async_copy(src.at[core * SLOTS + row, :, pair], r_buf.at[slot, pl.ds(TIP * t + ROWS * core, ROWS)], tip_sem.at[slot]).start()
            pltpu.make_async_copy(far_out.at[t, row, :, far], r_buf.at[slot, pl.ds(TIP * t + ROWS * (1 - core), ROWS)], tip_sem.at[slot]).start()
        pltpu.make_async_copy(r_in.at[:TIP, pair], r_buf.at[slot, 4 * TIP:5 * TIP], tip_sem.at[slot]).start()

    def tip_done(slot):
        wait_for(r_buf.at[slot, :TIP], tip_near.at[slot])
        wait_for(r_buf.at[slot, :TIP], tip_send.at[slot])

    def tip_group(hh, r0):
        group = slice(TIP * hh + r0, TIP * hh + r0 + 16)
        rel = pltpu.roll(e_ref[group, :TIP], 1 + r0, 1, stride=1, stride_axis=0)
        ahead = lax.broadcasted_iota(jnp.int32, (16, TIP), 1) - lax.broadcasted_iota(jnp.int32, (16, TIP), 0)
        return group, s_ref[group, :TIP] + rel, ahead <= r0

    def tip_rows(hh):
        for r0 in range(0, TIP, 16):
            group, s, seen = tip_group(hh, r0)
            s = jnp.where(seen, s, -jnp.inf)
            top = jnp.max(s, axis=1, keepdims=True)
            p = jnp.exp2((s - top) * (scale * LOG2E))
            p = p * (1.0 / jnp.sum(p, axis=1, keepdims=True))
            pb_ref[group, :TIP] = p.astype(BF16)
            dp = dp_ref[group, :TIP]
            row_dot = jnp.sum(p * dp, axis=1, keepdims=True)
            ds = (p * (dp - row_dot) * scale).astype(BF16)
            ds_ref[group, :TIP] = ds
            flipped = flip8(ds.astype(F32))
            half = [pltpu.roll(flipped[8 * j:8 * j + 8], TIP - 8 - r0 - 8 * j, 1, stride=1, stride_axis=0) for j in range(2)]
            dd_ref[group, :TIP] = jnp.concatenate(half, axis=0).astype(BF16)
        rows = slice(TIP * hh, TIP * (hh + 1))
        stage[0, hh, :TIP, :] = dot(pb_ref[rows, :TIP], v_s[hh, :TIP, :]).astype(BF16)
        dqc = dot(ds_ref[rows, :TIP], k_s[hh, :TIP, :])
        dqr = flip8(dot(dd_ref[rows, :TIP], c_s[hh, :TIP, :]))
        stage[1, hh, :TIP, :] = (dqc + dqr).astype(BF16)

    def tip_keys(hh, stats):
        rows = slice(TIP * hh, TIP * (hh + 1))
        st_ref[rows, :8] = stats.T
        for r0 in range(0, TIP, 16):
            group, s, seen = tip_group(hh, r0)
            p = jnp.where(seen, jnp.exp2(s * (scale * LOG2E) - st_ref[group, 0:1]), 0.0)
            pb_ref[group, :TIP] = p.astype(BF16)
            ds_ref[group, :TIP] = (p * (dp_ref[group, :TIP] - st_ref[group, 1:2]) * scale).astype(BF16)
        over_rows = (((0,), (0,)), ((), ()))
        stage[0, hh, :TIP, :] = lax.dot_general(ds_ref[rows, :TIP], a_s[hh, :TIP, :], over_rows, preferred_element_type=F32).astype(BF16)
        stage[1, hh, :TIP, :] = lax.dot_general(pb_ref[rows, :TIP], g_s[hh, :TIP, :], over_rows, preferred_element_type=F32).astype(BF16)

    def tip_unit(unit, carry):
        slot, row, far = unit % 2, unit // FAR, unit % FAR
        pair = far + tip_base
        wait_for(r_buf.at[slot, :5 * TIP], tip_sem.at[slot])

        @pl.when(unit + 1 < UNITS)
        def _():
            tip_load(unit + 1)

        q2, k2, v2, g2, r2 = [pltpu.einshape("abc->bac", r_buf[slot, TIP * t:TIP * (t + 1)]) for t in range(5)]
        u = u_buf[pair].astype(F32)
        w = w_buf[pair].astype(F32)
        for hh in range(PAIR):
            rows = slice(TIP * hh, TIP * (hh + 1))
            q32 = q2[hh].astype(F32)
            a = (q32 + u[hh:hh + 1]).astype(BF16)
            c = (q32 + w[hh:hh + 1]).astype(BF16)
            falling = dot(eye_rev(BF16), r2[hh]).astype(BF16)
            s_ref[rows, :TIP] = dot(a, k2[hh].T)
            e_ref[rows, :TIP] = dot(c, falling.T)
            dp_ref[rows, :TIP] = dot(g2[hh], v2[hh].T)
            a_s[hh, :TIP, :] = a
            c_s[hh, :TIP, :] = falling
            g_s[hh, :TIP, :] = g2[hh]
            k_s[hh, :TIP, :] = k2[hh]
            v_s[hh, :TIP, :] = v2[hh]

        @pl.when(lower)
        def _():
            for hh in range(PAIR):
                tip_rows(hh)

        @pl.when(upper)
        def _():
            for hh in range(PAIR):
                tip_keys(hh, tip_st[far // 2, (far % 2) * SLOTS + row, hh])

        @pl.when(unit >= 2)
        def _():
            tip_done(slot)

        for n in range(2):
            r_buf[slot, (5 + n) * TIP:(6 + n) * TIP] = pltpu.einshape("abc->bac", stage[n, :, :TIP, :])
        place = (core * SLOTS + row, slice(None), pair)

        def give(results):
            for n, dst in enumerate(results):
                pltpu.make_async_copy(r_buf.at[slot, pl.ds((5 + n) * TIP + ROWS * core, ROWS)], dst.at[place], tip_near.at[slot]).start()
                pltpu.make_async_remote_copy(
                    src_ref=r_buf.at[slot, pl.ds((5 + n) * TIP + ROWS * (1 - core), ROWS)], dst_ref=dst.at[place],
                    send_sem=tip_send.at[slot], recv_sem=out_recv, device_id=(partner,), device_id_type=MESH).start()

        @pl.when(lower)
        def _():
            give((o_out, dq_out))

        @pl.when(upper)
        def _():
            give((dk_out, dv_out))
        return carry

    def tips(third):
        @pl.when(tip)
        def _():
            if third == 0:
                wait_for(far_out, far_recv)

                @pl.when(upper)
                def _():
                    wait_for(tip_st, ts_recv)
                tip_load(0)
            lax.fori_loop(UNITS // 3 * third, UNITS // 3 * (third + 1), tip_unit, 0)
            if third == 2:
                tip_done(0)
                tip_done(1)

    send_up(0)

    def sub_body(sub, carry):
        @pl.when(sub < SUBS - 1)
        def _():
            send_up(sub + 1)

        @pl.when(sub == SLOTS)
        def _():
            swap_start(0)

        @pl.when(sub == SUBS - 1)
        def _():
            swap_add(0)
            cross_start(0)

        @pl.when(sub == SUBS)
        def _():
            swap_start(1)
            swap_add(1)
            cross_start(1)
            cross_finish(0)

        @pl.when(lower & (sub < SUBS))
        def _():
            lower_rows(sub)

        @pl.when(lower & (sub > 0))
        def _():
            lower_theirs(sub - 1)

        @pl.when(lower & (sub < SUBS))
        def _():
            lower_own(sub)

        @pl.when(upper & (sub < SUBS))
        def _():
            upper_own(sub)

        @pl.when(sub <= EARLY)
        def _():
            send_out(sub, (2, 3))

        @pl.when((sub > 0) & (sub <= EARLY))
        def _():
            send_out(sub - 1, (0, 1))
        return carry

    lax.fori_loop(0, SUBS + 1, sub_body, 0)

    cross_finish(1)
    send_out(EARLY, (0, 1))
    for p in range(2):
        hop_wait(p, 0)
        hop_start(p, 1)
    for p in range(2):
        send_out(EARLY + 1 + p, range(4))
        tips(p)
        hop_wait(p, 1)
        hop_start(p, 2)

    def send_late(sub, carry):
        send_out(sub, range(4))
        return carry

    lax.fori_loop(EARLY + 3, SUBS, send_late, 0)
    tips(2)
    for p in range(2):
        hop_wait(p, 2)
        hop_start(p, 3)
    for p in range(2):
        hop_wait(p, 3)

    wait_for(buf.at[:, :, :HALF - ROWS], in_send)

    @pl.when(tip)
    def _():
        wait_for(buf.at[:, :, :HALF - 3 * ROWS // 2], out_recv)
        wait_for(buf.at[:, :, :HALF - ROWS], out_send)
        wait_for(far_out, far_send)

    @pl.when(jnp.logical_not(tip))
    def _():
        wait_for(buf, out_recv)
        wait_for(buf.at[:, :, :HALF - 2 * ROWS], out_send)

    @pl.when(upper & jnp.logical_not(tip))
    def _():
        wait_for(st_tx.at[:2], ts_send)

    @pl.when(upper)
    def _():
        wait_for(st_tx, st_send)

    wait_for(dr_rx, x_send)
    wait_for(dr_rz, z_send)
    wait_for(blocks(2), own_sem)
    sent_wait()
    for sem in (fw_send, fw_recv):
        wait_for(buf.at[:3, :, :FIN * 16 // 24], sem)


def writer(*refs):
    ins, (o, dq, dk, dv, dr, du, dw, sem) = refs[:4 + N_PART], refs[4 + N_PART:]
    pairs = list(zip(ins[:4], (o, dq, dk, dv)))
    for m, part in enumerate(ins[4:]):
        rows = min(PART, HALF - PART * m)
        for side in range(2):
            start = HALF * side + PART * m
            pairs.append((part.at[side, :rows], dr.at[start:start + rows]))
    last = HALF - PART * (N_PART - 1)
    pairs += [(ins[-1].at[0, last], du), (ins[-1].at[0, last + 1], dw)]
    copies = [pltpu.make_async_copy(src, dst, sem.at[j]) for j, (src, dst) in enumerate(pairs)]
    for copy in copies:
        copy.start()
    for copy in copies:
        copy.wait()


def solution(mesh):
    seq_spec = P(None, "cp", None, None)

    def local(query, key_in, value, bias_u, bias_w, rel_k, d_out):
        n_batch, rows, n_heads, head_dim = query.shape
        pairs = (n_batch, rows, N_PAIR, PAIR, head_dim)
        vm = pltpu.VMEM
        dma = pltpu.SemaphoreType.DMA
        whole = pl.BlockSpec(memory_space=pl.ANY)
        act = jax.ShapeDtypeStruct(pairs, BF16)
        vec = jax.ShapeDtypeStruct((n_heads, 1, head_dim), F32)
        tok = (PAIR, SEQ, HEAD)
        tok_t = (PAIR, HEAD, SEQ)
        acc = (HEAD + 8, HALF)
        outs = pl.pallas_call(
            kernel,
            name="rel_attn",
            out_shape=(act, act, act, act,
                       *[jax.ShapeDtypeStruct((2, PART, n_heads, 1, head_dim), F32)] * N_PART,
                       jax.ShapeDtypeStruct((4, SLOTS, ROWS, FAR, PAIR, HEAD), BF16)),
            in_specs=[pl.BlockSpec(memory_space=pltpu.HBM)] * 7,
            out_specs=[whole] * (5 + N_PART),
            scratch_shapes=[
                vm((4, SUBS, HALF, PAIR, HEAD), BF16), vm((2, SUBS, HALF, PAIR, HEAD), BF16),
                vm((2, SEQ, PAIR, HEAD), BF16), vm((N_PAIR, PAIR, HEAD), BF16), vm((N_PAIR, PAIR, HEAD), BF16),
                vm((SUBS, PAIR, 8, HALF), F32), vm((SUBS, PAIR, 8, HALF), F32), vm((3, SUBS, PAIR, 8, TIP), F32), vm((QB, HEAD), F32),
                vm((2, 2) + acc, F32), vm((2,) + acc, F32), vm((2, FIN, 1, HEAD), F32), vm((4, 2) + acc, F32),
                vm((QB, SEQ), F32), vm((QB, SEQ), F32), vm((QB, SEQ), F32),
                vm((QB, SEQ), BF16), vm((QB, SEQ), BF16), vm((QB, SEQ), BF16),
                vm(tok, BF16), vm(tok, BF16), vm(tok, BF16), vm(tok, BF16), vm(tok, BF16),
                vm(tok_t, BF16), vm(tok_t, BF16), vm(tok_t, BF16), vm(tok_t, BF16), vm(tok_t, BF16),
                vm((4, SEQ, HEAD), BF16), vm((4, HEAD, SEQ), BF16),
                vm((PAIR, HEAD, HALF), F32), vm((PAIR, HEAD, HALF), F32), vm((4, PAIR, HALF, HEAD), BF16),
                dma, dma((2, SUBS)), dma, dma, dma, dma((4,)), dma((4,)), dma((SUBS,)), dma, dma((4,)),
                dma, dma((2,)), dma, dma((2,)), dma, dma((2, 4)), dma, dma,
                dma, dma, dma((2,)), dma((2,)), dma((2,)), dma, dma,
            ],
            compiler_params=pltpu.CompilerParams(collective_id=0, has_side_effects=True, vmem_limit_bytes=37 * 1024 * 1024),
        )(*[pltpu.with_memory_space_constraint(x, pltpu.HBM) for x in (
            query.reshape(pairs), key_in.reshape(pairs), value.reshape(pairs), d_out.reshape(pairs),
            rel_k.reshape(SEQ, N_PAIR, PAIR, head_dim), bias_u.reshape(N_PAIR, PAIR, head_dim), bias_w.reshape(N_PAIR, PAIR, head_dim))])
        o, dq, dk, dv, dr, du, dw = pl.pallas_call(
            writer,
            name="writer",
            out_shape=(act, act, act, act, jax.ShapeDtypeStruct((SEQ, n_heads, 1, head_dim), F32), vec, vec),
            in_specs=[whole] * (4 + N_PART),
            out_specs=[whole] * 7,
            scratch_shapes=[dma((6 + 2 * N_PART,))],
            compiler_params=pltpu.CompilerParams(vmem_limit_bytes=1024 * 1024),
        )(*outs[:-1])
        full = query.shape
        return (o.reshape(full), dq.reshape(full), dk.reshape(full), dv.reshape(full),
                du.reshape(bias_u.shape), dw.reshape(bias_w.shape), dr.reshape(rel_k.shape))

    return jax.shard_map(local, mesh=mesh,
                         in_specs=(seq_spec, seq_spec, seq_spec, P(), P(), P(), seq_spec),
                         out_specs=(seq_spec, seq_spec, seq_spec, seq_spec, P(), P(), P()),
                         check_vma=False)
```

```python
import jax
import jax.numpy as jnp
from jax import lax
from jax.experimental import pallas as pl
from jax.experimental.pallas import tpu as pltpu
from jax.sharding import PartitionSpec as P

MESH = pl.DeviceIdType.MESH
BF16, F32 = jnp.bfloat16, jnp.float32
LOG2E = 1.4426950408889634

N_DEV = 16
PLANE = 8
PAIR = 2
N_PAIR = 8
SLOTS = 4
SUBS = 2 * SLOTS
EARLY = 3
ROWS = 64
HALF = PLANE * ROWS
SEQ = 2 * HALF
HEAD = 128
QB = 256
WIN = HALF + QB
N_PART = 6
PART = 86
FIN = N_PART * PART
TIP = 2 * ROWS
FAR = N_PAIR - 2
UNITS = FAR * SLOTS
TURNS = ((1, 3, 2), (3, 1, 2))


def dot(lhs, rhs):
    return jnp.dot(lhs, rhs, preferred_element_type=F32)


def flip8(x):
    rows, cols = x.shape
    idx = 7 - lax.broadcasted_iota(jnp.int32, (rows // 8, 8, cols), 1)
    return jnp.take_along_axis(x.reshape(rows // 8, 8, cols), idx, axis=1).reshape(rows, cols)


def eye_rev(dtype):
    total = lax.broadcasted_iota(jnp.int32, (HEAD, HEAD), 0) + lax.broadcasted_iota(jnp.int32, (HEAD, HEAD), 1)
    return jnp.where(total == HEAD - 1, 1.0, 0.0).astype(dtype)


def kernel(q_in, k_in, v_in, g_in, r_in, u_in, w_in,
           o_out, dq_out, dk_out, dv_out, dr0_out, dr1_out, dr2_out, dr3_out, dr4_out, dr5_out, far_out,
           buf, rbuf, r_buf, u_buf, w_buf, st_tx, st_rx, tip_st, st_ref, dr_rx, dr_rz, dr_fin, dr_acc,
           s_ref, e_ref, dp_ref, pb_ref, ds_ref, dd_ref,
           a_s, c_s, g_s, k_s, v_s, at_s, ct_s, gt_s, kt_s, vt_s, rev_s, rt_s, dkt, dvt, stage,
           in_send, in_recv, out_send, out_recv, own_sem, r_sem, up_send, up_recv, st_send, st_recv,
           x_send, x_recv, z_send, z_recv, ring_send, ring_recv, fw_send, fw_recv,
           far_send, far_recv, tip_sem, tip_near, tip_send, ts_send, ts_recv):
    me = lax.axis_index("cp")
    core = me % 2
    chip = me // 2
    col = chip % 4
    z = chip // 4
    partner = me + 1 - 2 * core
    across = me + PLANE * (1 - 2 * z)
    scale = HEAD ** -0.5

    def wait_for(ref, sem):
        pltpu.make_async_copy(ref, ref, sem).wait()

    y = col // 2
    lower, upper = z == 0, z == 1
    tip = chip == 7 * z
    tip_base = 2 - 2 * z

    tables = [pltpu.make_async_copy(src, dst, r_sem.at[j]) for j, (src, dst) in enumerate(
        ((r_in.at[:, 2 * col], r_buf.at[0]), (r_in.at[:, 2 * col + 1], r_buf.at[1]), (u_in, u_buf), (w_in, w_buf)))]
    for copy in tables:
        copy.start()

    barrier = pltpu.get_barrier_semaphore()

    for peer in [across] + [me ^ step for step in range(PLANE - 1, 0, -1)]:
        pl.semaphore_signal(barrier, inc=1, device_id=(peer,), device_id_type=MESH)
    pl.semaphore_wait(barrier, PLANE)

    my_rows = pl.ds(pl.multiple_of((me % PLANE) * ROWS, ROWS), ROWS)

    even = chip % 2 == z
    loaded = y != z

    def peers(late=False):
        near = core == 0
        if late:
            near = near & (even | jnp.logical_not(loaded))
        first, second, third = [jnp.where(near, near_turn, far_turn) for near_turn, far_turn in zip(*TURNS)]
        for turn, other in ((first, 0), (third, 0), (first, 1), (third, 1), (second, 0), (second, 1)):
            yield me ^ (2 * turn + other)
        yield partner

    def send_in(ins, sub):
        pair, row = sub // SLOTS, sub % SLOTS
        for first in (0, 2):
            for t in (first, first + 1):
                pltpu.make_async_copy(ins[t].at[core * SLOTS + row, :, 2 * col + pair], buf.at[t, sub, my_rows], in_recv.at[first // 2, sub]).start()
            for peer in peers():
                for t in (first, first + 1):
                    pltpu.make_async_remote_copy(
                        src_ref=ins[t].at[(peer % 2) * SLOTS + row, :, 2 * ((peer // 2) % 4) + pair], dst_ref=buf.at[t, sub, my_rows],
                        send_sem=in_send, recv_sem=in_recv.at[first // 2, sub], device_id=(peer,), device_id_type=MESH).start()

    def send_all(ins):
        def send_sub(sub, carry):
            send_in(ins, sub)
            return carry
        lax.fori_loop(0, SUBS, send_sub, 0)

    @pl.when(lower)
    def _():
        send_all((k_in, v_in, q_in, g_in))

    @pl.when(upper)
    def _():
        send_all((q_in, g_in, k_in, v_in))

    @pl.when(tip)
    def _():
        for t, src in enumerate((q_in, k_in, v_in, g_in)):
            for row in range(SLOTS):
                pltpu.make_async_remote_copy(
                    src_ref=src.at[(1 - core) * SLOTS + row, :, pl.ds(tip_base, FAR)], dst_ref=far_out.at[t, row],
                    send_sem=far_send, recv_sem=far_recv, device_id=(partner,), device_id_type=MESH).start()

    for copy in tables:
        copy.wait()
    rev = eye_rev(BF16)
    for p in range(2):
        pair_tab = pltpu.einshape("abc->bac", r_buf[p])
        for hh in range(PAIR):
            for blk in range(SEQ // HEAD):
                part = pair_tab[hh, SEQ - HEAD * (blk + 1):SEQ - HEAD * blk]
                flipped = dot(rev, part).astype(BF16)
                rev_s[2 * p + hh, HEAD * blk:HEAD * (blk + 1), :] = flipped
                rt_s[2 * p + hh, :, HEAD * blk:HEAD * (blk + 1)] = flipped.T
    dr_acc[...] = jnp.zeros_like(dr_acc)

    acts = (dk_out, dv_out, o_out, dq_out)

    def send_out(sub, which, late=False):
        place = (core * SLOTS + sub % SLOTS, slice(None), 2 * col + sub // SLOTS)
        for t in which:
            pltpu.make_async_copy(buf.at[t, sub, my_rows], acts[t].at[place], out_recv).start()
        for peer in peers(late):
            peer_rows = pl.ds(pl.multiple_of((peer % PLANE) * ROWS, ROWS), ROWS)
            to_tip = (peer // 2 == 7 * z) & jnp.logical_not(tip)
            for t in which:
                @pl.when(jnp.logical_not(to_tip & (lower if t >= 2 else upper)))
                def _():
                    pltpu.make_async_remote_copy(
                        src_ref=buf.at[t, sub, peer_rows], dst_ref=acts[t].at[place],
                        send_sem=out_send, recv_sem=out_recv, device_id=(peer,), device_id_type=MESH).start()

    def send_up(sub):
        wait_for(buf.at[0:2, sub], in_recv.at[0, sub])
        for j in range(2):
            pltpu.make_async_remote_copy(src_ref=buf.at[j, sub], dst_ref=rbuf.at[j, sub], send_sem=up_send.at[sub % 4], recv_sem=up_recv.at[sub],
                                         device_id=(across,), device_id_type=MESH).start()

    def unpack(ref, j, sub):
        return pltpu.einshape("abc->bac", ref[j, sub])

    def load_rows(q_ref, q_j, g_ref, g_j, sub, start, turned):
        rows = slice(start, start + HALF)
        p = sub // SLOTS
        q2 = unpack(q_ref, q_j, sub)
        u = u_buf[2 * col + p].astype(F32)
        w = w_buf[2 * col + p].astype(F32)
        for hh in range(PAIR):
            q32 = q2[hh].astype(F32)
            a = (q32 + u[hh:hh + 1]).astype(BF16)
            c = (q32 + w[hh:hh + 1]).astype(BF16)
            a_s[hh, rows, :] = a
            c_s[hh, rows, :] = c
            at_s[hh, :, rows] = a.T
            if turned:
                ct_s[hh, :, rows] = flip8(c.astype(F32)).astype(BF16).T
        g2 = unpack(g_ref, g_j, sub)
        g_s[:, rows, :] = g2
        for hh in range(PAIR):
            gt_s[hh, :, rows] = g2[hh].T

    def load_keys(k_ref, k_j, v_ref, v_j, sub, start):
        rows = slice(start, start + HALF)
        k2 = unpack(k_ref, k_j, sub)
        v2 = unpack(v_ref, v_j, sub)
        k_s[:, rows, :] = k2
        v_s[:, rows, :] = v2
        for hh in range(PAIR):
            kt_s[hh, :, rows] = k2[hh].T
            vt_s[hh, :, rows] = v2[hh].T

    def row_block(hh, head, start, i0, lo, fresh, stats):
        width = i0 + QB
        rows = slice(start, start + QB)
        s_ref[:, :width] = dot(a_s[hh, rows, :], kt_s[hh, :, :width])
        e_ref[:, :width] = dot(c_s[hh, rows, :], rt_s[head, :, SEQ - width:])
        dp_ref[:, :width] = dot(g_s[hh, rows, :], vt_s[hh, :, :width])
        for r0 in range(0, QB, 16):
            group = slice(r0, r0 + 16)
            rel = pltpu.roll(e_ref[group, :width], i0 + 1 + r0, 1, stride=1, stride_axis=0)
            s = s_ref[group, :width] + rel
            ahead = lax.broadcasted_iota(jnp.int32, (16, width), 1) - lax.broadcasted_iota(jnp.int32, (16, width), 0)
            s = jnp.where(ahead <= i0 + r0, s, -jnp.inf)
            top = jnp.max(s, axis=1, keepdims=True)
            p = jnp.exp2((s - top) * (scale * LOG2E))
            total = jnp.sum(p, axis=1, keepdims=True)
            p = p * (1.0 / total)
            pb_ref[group, :width] = p.astype(BF16)
            dp = dp_ref[group, :width]
            row_dot = jnp.sum(p * dp, axis=1, keepdims=True)
            ds = (p * (dp - row_dot) * scale).astype(BF16)
            ds_ref[group, :width] = ds
            flipped = flip8(ds.astype(F32))
            half = [pltpu.roll(flipped[8 * j:8 * j + 8], QB - 8 - r0 - 8 * j, 1, stride=1, stride_axis=0) for j in range(2)]
            dd_ref[group, :width] = jnp.concatenate(half, axis=0).astype(BF16)
            if stats:
                lane = lax.broadcasted_iota(jnp.int32, (16, HEAD), 1)
                st_ref[group, :] = jnp.where(lane == 0, top * (scale * LOG2E) + jnp.log2(total), row_dot)
        pb = pb_ref[:, :width]
        ds = ds_ref[:, :width]
        dd = dd_ref[:, :width]
        stage[0, hh, rows, :] = dot(pb, v_s[hh, :width, :]).astype(BF16)
        dqc = dot(ds, k_s[hh, :width, :])
        dqr = flip8(dot(dd, rev_s[head, SEQ - width:, :]))
        stage[1, hh, rows, :] = (dqc + dqr).astype(BF16)
        dr_acc[head, 1, HEAD:HEAD + 1, HALF - HEAD:] += jnp.sum(dqc, axis=0, keepdims=True)
        dr_acc[head, 1, HEAD + 1:HEAD + 2, HALF - HEAD:] += jnp.sum(dqr, axis=0, keepdims=True)
        dk_new = dot(at_s[hh, :, rows], ds_ref[:, lo:width])
        dv_new = dot(gt_s[hh, :, rows], pb_ref[:, lo:width])
        if fresh:
            dkt[hh] = dk_new
            dvt[hh] = dv_new
        else:
            dkt[hh, :, :width - lo] += dk_new
            dvt[hh, :, :width - lo] += dv_new
        dr_new = dot(ct_s[hh, :, rows], dd)
        if width > HALF:
            dr_acc[head, 0, :HEAD, SEQ - width:] += dr_new[:, :width - HALF]
            dr_acc[head, 1, :HEAD, :] += dr_new[:, width - HALF:]
        else:
            dr_acc[head, 1, :HEAD, HALF - width:] += dr_new

    def col_block(hh, head, sub, i0):
        rows = slice(i0, i0 + QB)
        first = WIN - i0
        s_ref[:, :HALF] = dot(a_s[hh, rows, :], kt_s[hh, :, :HALF])
        e_ref[:, :WIN] = dot(c_s[hh, rows, :], rt_s[head, :, first:first + WIN])
        dp_ref[:, :HALF] = dot(g_s[hh, rows, :], vt_s[hh, :, :HALF])
        st_ref[:, :8] = st_rx[sub, hh, :, i0 - HALF:i0 - HALF + QB].T
        for r0 in range(0, QB, 16):
            group = slice(r0, r0 + 16)
            rel = pltpu.roll(e_ref[group, :WIN], HALF + 1 + r0, 1, stride=1, stride_axis=0)[:, :HALF]
            log_sum = st_ref[group, 0:1]
            row_dot = st_ref[group, 1:2]
            p = jnp.exp2((s_ref[group, :HALF] + rel) * (scale * LOG2E) - log_sum)
            pb_ref[group, :HALF] = p.astype(BF16)
            ds_ref[group, :HALF] = (p * (dp_ref[group, :HALF] - row_dot) * scale).astype(BF16)
        dkt[hh] += dot(at_s[hh, :, rows], ds_ref[:, :HALF])
        dvt[hh] += dot(gt_s[hh, :, rows], pb_ref[:, :HALF])

    def store_rows(sub):
        for t in range(2):
            buf[2 + t, sub] = pltpu.einshape("abc->bac", stage[t])

    def store_keys(sub):
        for hh in range(PAIR):
            stage[2, hh] = dkt[hh].astype(BF16).T
            stage[3, hh] = dvt[hh].astype(BF16).T
        for t in range(2):
            buf[t, sub] = pltpu.einshape("abc->bac", stage[2 + t])

    def wait_up(sub):
        wait_for(rbuf.at[:, sub], up_recv.at[sub])
        wait_for(rbuf.at[:, sub], up_send.at[sub % 4])

    def wait_in(sub):
        wait_for(buf.at[2:4, sub], in_recv.at[1, sub])

    def lower_rows(sub):
        wait_in(sub)
        load_rows(buf, 2, buf, 3, sub, 0, True)

    def lower_own(sub):
        load_keys(buf, 0, buf, 1, sub, 0)

        def own(hh, carry):
            head = 2 * (sub // SLOTS) + hh
            row_block(hh, head, QB, QB, 0, True, False)
            row_block(hh, head, 0, 0, 0, False, False)
            return carry

        lax.fori_loop(0, PAIR, own, 0)
        store_rows(sub)

    def lower_theirs(sub):
        wait_up(sub)
        load_rows(rbuf, 0, rbuf, 1, sub, HALF, False)
        wait_for(st_rx.at[sub], st_recv.at[sub % 4])

        def theirs(hh, carry):
            head = 2 * (sub // SLOTS) + hh
            col_block(hh, head, sub, HALF)
            col_block(hh, head, sub, HALF + QB)
            return carry

        lax.fori_loop(0, PAIR, theirs, 0)
        store_keys(sub)

    def upper_own(sub):
        wait_in(sub)
        wait_up(sub)
        load_rows(buf, 0, buf, 1, sub, 0, True)
        load_keys(rbuf, 0, rbuf, 1, sub, 0)
        load_keys(buf, 2, buf, 3, sub, HALF)

        def own(hh, carry):
            head = 2 * (sub // SLOTS) + hh
            for blk in (1, 0):
                row_block(hh, head, QB * blk, HALF + QB * blk, HALF, blk == 1, True)
                st_tx[sub, hh, :, QB * blk:QB * (blk + 1)] = st_ref[...].T[:8]
            pltpu.make_async_remote_copy(src_ref=st_tx.at[sub, hh], dst_ref=st_rx.at[sub, hh], send_sem=st_send, recv_sem=st_recv.at[sub % 4],
                                         device_id=(across,), device_id_type=MESH).start()

            @pl.when(jnp.logical_not(tip))
            def _():
                pltpu.make_async_remote_copy(src_ref=st_tx.at[sub, hh, :, HALF - TIP:], dst_ref=tip_st.at[col, sub, hh], send_sem=ts_send,
                                             recv_sem=ts_recv, device_id=(N_DEV - 2 + core,), device_id_type=MESH).start()
            return carry

        lax.fori_loop(0, PAIR, own, 0)
        store_rows(sub)
        store_keys(sub)

    side = 1 - core
    parts = (dr0_out, dr1_out, dr2_out, dr3_out, dr4_out, dr5_out)

    def swap_start(p):
        for n in range(2):
            pltpu.make_async_remote_copy(src_ref=dr_acc.at[2 * p + n, side], dst_ref=dr_rx.at[p, n], send_sem=x_send, recv_sem=x_recv.at[p],
                                         device_id=(partner,), device_id_type=MESH).start()

    def swap_add(p):
        wait_for(dr_rx.at[p], x_recv.at[p])
        for n in range(2):
            dr_rx[p, n] = dr_rx[p, n] + dr_acc[2 * p + n, core]

    def cross_start(p):
        pltpu.make_async_remote_copy(src_ref=dr_rx.at[p, 1 - z], dst_ref=dr_rz.at[p], send_sem=z_send, recv_sem=z_recv.at[p],
                                     device_id=(across,), device_id_type=MESH).start()

    def head_of(p, bits):
        other = chip ^ bits
        return 4 * (other % 4) + 2 * p + other // 4

    def block(p, m, bits):
        if bits == 0:
            return dr_fin.at[p, PART * m:PART * (m + 1)]
        return parts[m].at[side, :, head_of(p, bits)]

    def forward(p, m, bits):
        pltpu.make_async_remote_copy(src_ref=block(p, m, bits), dst_ref=parts[m].at[side, :, head_of(p, bits)], send_sem=fw_send,
                                     recv_sem=fw_recv, device_id=(partner,), device_id_type=MESH).start()

    def blocks(count):
        return parts[0].at[:, :, :N_PART // 2 * count]

    def pass_on(p, bits, hop, device):
        for m in range(N_PART):
            pltpu.make_async_remote_copy(
                src_ref=block(p, m, bits), dst_ref=parts[m].at[side, :, head_of(p, bits)], send_sem=ring_send,
                recv_sem=ring_recv.at[p, hop], device_id=(device,), device_id_type=MESH).start()

    def hand_over(p, bits):
        for m in range(N_PART):
            forward(p, m, bits)

    along_x, along_y = me ^ 2, me ^ 4

    def hop_start(p, hop):
        if hop == 0:
            for device in (along_x, along_y, across):
                pass_on(p, 0, 0, device)
        if hop == 1:
            @pl.when(even & loaded)
            def _():
                pass_on(p, 1, 1, along_y)

            @pl.when(jnp.logical_not(even) & loaded)
            def _():
                pass_on(p, 2, 1, along_x)

            pass_on(p, 1, 1, across)
            pass_on(p, 2, 1, across)
        if hop == 2:
            @pl.when(even & loaded)
            def _():
                pass_on(p, 5, 2, along_y)

            @pl.when(jnp.logical_not(even) & loaded)
            def _():
                pass_on(p, 6, 2, along_x)

            @pl.when(even)
            def _():
                pass_on(p, 3, 2, across)
        if hop == 3:
            @pl.when(even)
            def _():
                pass_on(p, 7, 3, across)

    def hop_wait(p, hop):
        if hop == 0:
            wait_for(blocks(3), ring_recv.at[p, 0])
            for bits in (1, 2, 4):
                hand_over(p, bits)
        if hop == 1:
            @pl.when(even)
            def _():
                wait_for(blocks(3), ring_recv.at[p, 1])
                hand_over(p, 3)

            @pl.when(jnp.logical_not(even))
            def _():
                wait_for(blocks(2), ring_recv.at[p, 1])
            for bits in (5, 6):
                hand_over(p, bits)
        if hop == 2:
            wait_for(blocks(1), ring_recv.at[p, 2])
            hand_over(p, 7)
        if hop == 3:
            @pl.when(jnp.logical_not(even))
            def _():
                wait_for(blocks(1), ring_recv.at[p, 3])
                hand_over(p, 3)

    def sent_wait():
        @pl.when(even & loaded)
        def _():
            wait_for(buf.at[:3, :, :FIN * 18 // 24], ring_send)

        @pl.when(even != loaded)
        def _():
            wait_for(buf.at[:3, :7, :FIN * 14 // 21], ring_send)

        @pl.when(jnp.logical_not(even | loaded))
        def _():
            wait_for(buf.at[:2, :6, :FIN * 10 // 12], ring_send)

    def cross_finish(p):
        wait_for(dr_rz.at[p], z_recv.at[p])
        total = dr_rx[p, z] + dr_rz[p]
        rev32 = eye_rev(F32)
        for m in range(HALF // HEAD):
            part = total[:HEAD, HALF - HEAD * (m + 1):HALF - HEAD * m]
            turned = lax.dot_general(rev32, part, (((1,), (1,)), ((), ())), precision=lax.Precision.HIGHEST, preferred_element_type=F32)
            dr_fin[p, HEAD * m:HEAD * (m + 1)] = turned.reshape(HEAD, 1, HEAD)
        dr_fin[p, HALF] = total[HEAD:HEAD + 1, HALF - HEAD:]
        dr_fin[p, HALF + 1] = total[HEAD + 1:HEAD + 2, HALF - HEAD:]
        dr_fin[p, HALF + 2:] = jnp.zeros((FIN - HALF - 2, 1, HEAD), F32)
        hop_start(p, 0)
        for m in range(N_PART):
            pltpu.make_async_copy(block(p, m, 0), parts[m].at[side, :, head_of(p, 0)], own_sem).start()
        hand_over(p, 0)

    def tip_load(unit):
        slot, row, far = unit % 2, unit // FAR, unit % FAR
        pair = far + tip_base
        for t, src in enumerate((q_in, k_in, v_in, g_in)):
            pltpu.make_async_copy(src.at[core * SLOTS + row, :, pair], r_buf.at[slot, pl.ds(TIP * t + ROWS * core, ROWS)], tip_sem.at[slot]).start()
            pltpu.make_async_copy(far_out.at[t, row, :, far], r_buf.at[slot, pl.ds(TIP * t + ROWS * (1 - core), ROWS)], tip_sem.at[slot]).start()
        pltpu.make_async_copy(r_in.at[:TIP, pair], r_buf.at[slot, 4 * TIP:5 * TIP], tip_sem.at[slot]).start()

    def tip_done(slot):
        wait_for(r_buf.at[slot, :TIP], tip_near.at[slot])
        wait_for(r_buf.at[slot, :TIP], tip_send.at[slot])

    def tip_group(hh, r0):
        group = slice(TIP * hh + r0, TIP * hh + r0 + 16)
        rel = pltpu.roll(e_ref[group, :TIP], 1 + r0, 1, stride=1, stride_axis=0)
        ahead = lax.broadcasted_iota(jnp.int32, (16, TIP), 1) - lax.broadcasted_iota(jnp.int32, (16, TIP), 0)
        return group, s_ref[group, :TIP] + rel, ahead <= r0

    def tip_rows(hh):
        for r0 in range(0, TIP, 16):
            group, s, seen = tip_group(hh, r0)
            s = jnp.where(seen, s, -jnp.inf)
            top = jnp.max(s, axis=1, keepdims=True)
            p = jnp.exp2((s - top) * (scale * LOG2E))
            p = p * (1.0 / jnp.sum(p, axis=1, keepdims=True))
            pb_ref[group, :TIP] = p.astype(BF16)
            dp = dp_ref[group, :TIP]
            row_dot = jnp.sum(p * dp, axis=1, keepdims=True)
            ds = (p * (dp - row_dot) * scale).astype(BF16)
            ds_ref[group, :TIP] = ds
            flipped = flip8(ds.astype(F32))
            half = [pltpu.roll(flipped[8 * j:8 * j + 8], TIP - 8 - r0 - 8 * j, 1, stride=1, stride_axis=0) for j in range(2)]
            dd_ref[group, :TIP] = jnp.concatenate(half, axis=0).astype(BF16)
        rows = slice(TIP * hh, TIP * (hh + 1))
        stage[0, hh, :TIP, :] = dot(pb_ref[rows, :TIP], v_s[hh, :TIP, :]).astype(BF16)
        dqc = dot(ds_ref[rows, :TIP], k_s[hh, :TIP, :])
        dqr = flip8(dot(dd_ref[rows, :TIP], c_s[hh, :TIP, :]))
        stage[1, hh, :TIP, :] = (dqc + dqr).astype(BF16)

    def tip_keys(hh, stats):
        rows = slice(TIP * hh, TIP * (hh + 1))
        st_ref[rows, :8] = stats.T
        for r0 in range(0, TIP, 16):
            group, s, seen = tip_group(hh, r0)
            p = jnp.where(seen, jnp.exp2(s * (scale * LOG2E) - st_ref[group, 0:1]), 0.0)
            pb_ref[group, :TIP] = p.astype(BF16)
            ds_ref[group, :TIP] = (p * (dp_ref[group, :TIP] - st_ref[group, 1:2]) * scale).astype(BF16)
        over_rows = (((0,), (0,)), ((), ()))
        stage[0, hh, :TIP, :] = lax.dot_general(ds_ref[rows, :TIP], a_s[hh, :TIP, :], over_rows, preferred_element_type=F32).astype(BF16)
        stage[1, hh, :TIP, :] = lax.dot_general(pb_ref[rows, :TIP], g_s[hh, :TIP, :], over_rows, preferred_element_type=F32).astype(BF16)

    def tip_unit(unit, carry):
        slot, row, far = unit % 2, unit // FAR, unit % FAR
        pair = far + tip_base
        wait_for(r_buf.at[slot, :5 * TIP], tip_sem.at[slot])

        @pl.when(unit + 1 < UNITS)
        def _():
            tip_load(unit + 1)

        q2, k2, v2, g2, r2 = [pltpu.einshape("abc->bac", r_buf[slot, TIP * t:TIP * (t + 1)]) for t in range(5)]
        u = u_buf[pair].astype(F32)
        w = w_buf[pair].astype(F32)
        for hh in range(PAIR):
            rows = slice(TIP * hh, TIP * (hh + 1))
            q32 = q2[hh].astype(F32)
            a = (q32 + u[hh:hh + 1]).astype(BF16)
            c = (q32 + w[hh:hh + 1]).astype(BF16)
            falling = dot(eye_rev(BF16), r2[hh]).astype(BF16)
            s_ref[rows, :TIP] = dot(a, k2[hh].T)
            e_ref[rows, :TIP] = dot(c, falling.T)
            dp_ref[rows, :TIP] = dot(g2[hh], v2[hh].T)
            a_s[hh, :TIP, :] = a
            c_s[hh, :TIP, :] = falling
            g_s[hh, :TIP, :] = g2[hh]
            k_s[hh, :TIP, :] = k2[hh]
            v_s[hh, :TIP, :] = v2[hh]

        @pl.when(lower)
        def _():
            for hh in range(PAIR):
                tip_rows(hh)

        @pl.when(upper)
        def _():
            for hh in range(PAIR):
                tip_keys(hh, tip_st[far // 2, (far % 2) * SLOTS + row, hh])

        @pl.when(unit >= 2)
        def _():
            tip_done(slot)

        for n in range(2):
            r_buf[slot, (5 + n) * TIP:(6 + n) * TIP] = pltpu.einshape("abc->bac", stage[n, :, :TIP, :])
        place = (core * SLOTS + row, slice(None), pair)

        def give(results):
            for n, dst in enumerate(results):
                pltpu.make_async_copy(r_buf.at[slot, pl.ds((5 + n) * TIP + ROWS * core, ROWS)], dst.at[place], tip_near.at[slot]).start()
                pltpu.make_async_remote_copy(
                    src_ref=r_buf.at[slot, pl.ds((5 + n) * TIP + ROWS * (1 - core), ROWS)], dst_ref=dst.at[place],
                    send_sem=tip_send.at[slot], recv_sem=out_recv, device_id=(partner,), device_id_type=MESH).start()

        @pl.when(lower)
        def _():
            give((o_out, dq_out))

        @pl.when(upper)
        def _():
            give((dk_out, dv_out))
        return carry

    def tips(third):
        @pl.when(tip)
        def _():
            if third == 0:
                wait_for(far_out, far_recv)

                @pl.when(upper)
                def _():
                    wait_for(tip_st, ts_recv)
                tip_load(0)
            lax.fori_loop(UNITS // 3 * third, UNITS // 3 * (third + 1), tip_unit, 0)
            if third == 2:
                tip_done(0)
                tip_done(1)

    send_up(0)

    def sub_body(sub, carry):
        @pl.when(sub < SUBS - 1)
        def _():
            send_up(sub + 1)

        @pl.when(sub == SLOTS)
        def _():
            swap_start(0)

        @pl.when(sub == SUBS - 1)
        def _():
            swap_add(0)
            cross_start(0)

        @pl.when(sub == SUBS)
        def _():
            swap_start(1)
            swap_add(1)
            cross_start(1)
            cross_finish(0)

        @pl.when(lower & (sub < SUBS))
        def _():
            lower_rows(sub)

        @pl.when(lower & (sub > 0))
        def _():
            lower_theirs(sub - 1)

        @pl.when(lower & (sub < SUBS))
        def _():
            lower_own(sub)

        @pl.when(upper & (sub < SUBS))
        def _():
            upper_own(sub)

        @pl.when(sub <= EARLY)
        def _():
            send_out(sub, (2, 3))

        @pl.when((sub > 0) & (sub <= EARLY))
        def _():
            send_out(sub - 1, (0, 1))
        return carry

    lax.fori_loop(0, SUBS + 1, sub_body, 0)

    cross_finish(1)
    send_out(EARLY, (0, 1))
    for p in range(2):
        hop_wait(p, 0)
        hop_start(p, 1)
    for p in range(2):
        send_out(EARLY + 1 + p, range(4))
        tips(p)
        hop_wait(p, 1)
        hop_start(p, 2)

    def send_late(sub, carry):
        send_out(sub, range(4), True)
        return carry

    lax.fori_loop(EARLY + 3, SUBS, send_late, 0)
    tips(2)
    for p in range(2):
        hop_wait(p, 2)
        hop_start(p, 3)
    for p in range(2):
        hop_wait(p, 3)

    wait_for(buf.at[:, :, :HALF - ROWS], in_send)

    @pl.when(tip)
    def _():
        wait_for(buf.at[:, :, :HALF - 3 * ROWS // 2], out_recv)
        wait_for(buf.at[:, :, :HALF - ROWS], out_send)
        wait_for(far_out, far_send)

    @pl.when(jnp.logical_not(tip))
    def _():
        wait_for(buf, out_recv)
        wait_for(buf.at[:, :, :HALF - 2 * ROWS], out_send)

    @pl.when(upper & jnp.logical_not(tip))
    def _():
        wait_for(st_tx.at[:2], ts_send)

    @pl.when(upper)
    def _():
        wait_for(st_tx, st_send)

    wait_for(dr_rx, x_send)
    wait_for(dr_rz, z_send)
    wait_for(blocks(2), own_sem)
    sent_wait()
    for sem in (fw_send, fw_recv):
        wait_for(buf.at[:3, :, :FIN * 16 // 24], sem)


def writer(*refs):
    ins, (o, dq, dk, dv, dr, du, dw, sem) = refs[:4 + N_PART], refs[4 + N_PART:]
    pairs = list(zip(ins[:4], (o, dq, dk, dv)))
    for m, part in enumerate(ins[4:]):
        rows = min(PART, HALF - PART * m)
        for side in range(2):
            start = HALF * side + PART * m
            pairs.append((part.at[side, :rows], dr.at[start:start + rows]))
    last = HALF - PART * (N_PART - 1)
    pairs += [(ins[-1].at[0, last], du), (ins[-1].at[0, last + 1], dw)]
    copies = [pltpu.make_async_copy(src, dst, sem.at[j]) for j, (src, dst) in enumerate(pairs)]
    for copy in copies:
        copy.start()
    for copy in copies:
        copy.wait()


def solution(mesh):
    seq_spec = P(None, "cp", None, None)

    def local(query, key_in, value, bias_u, bias_w, rel_k, d_out):
        n_batch, rows, n_heads, head_dim = query.shape
        pairs = (n_batch, rows, N_PAIR, PAIR, head_dim)
        vm = pltpu.VMEM
        dma = pltpu.SemaphoreType.DMA
        whole = pl.BlockSpec(memory_space=pl.ANY)
        act = jax.ShapeDtypeStruct(pairs, BF16)
        vec = jax.ShapeDtypeStruct((n_heads, 1, head_dim), F32)
        tok = (PAIR, SEQ, HEAD)
        tok_t = (PAIR, HEAD, SEQ)
        acc = (HEAD + 8, HALF)
        outs = pl.pallas_call(
            kernel,
            name="rel_attn",
            out_shape=(act, act, act, act,
                       *[jax.ShapeDtypeStruct((2, PART, n_heads, 1, head_dim), F32)] * N_PART,
                       jax.ShapeDtypeStruct((4, SLOTS, ROWS, FAR, PAIR, HEAD), BF16)),
            in_specs=[pl.BlockSpec(memory_space=pltpu.HBM)] * 7,
            out_specs=[whole] * (5 + N_PART),
            scratch_shapes=[
                vm((4, SUBS, HALF, PAIR, HEAD), BF16), vm((2, SUBS, HALF, PAIR, HEAD), BF16),
                vm((2, SEQ, PAIR, HEAD), BF16), vm((N_PAIR, PAIR, HEAD), BF16), vm((N_PAIR, PAIR, HEAD), BF16),
                vm((SUBS, PAIR, 8, HALF), F32), vm((SUBS, PAIR, 8, HALF), F32), vm((3, SUBS, PAIR, 8, TIP), F32), vm((QB, HEAD), F32),
                vm((2, 2) + acc, F32), vm((2,) + acc, F32), vm((2, FIN, 1, HEAD), F32), vm((4, 2) + acc, F32),
                vm((QB, SEQ), F32), vm((QB, SEQ), F32), vm((QB, SEQ), F32),
                vm((QB, SEQ), BF16), vm((QB, SEQ), BF16), vm((QB, SEQ), BF16),
                vm(tok, BF16), vm(tok, BF16), vm(tok, BF16), vm(tok, BF16), vm(tok, BF16),
                vm(tok_t, BF16), vm(tok_t, BF16), vm(tok_t, BF16), vm(tok_t, BF16), vm(tok_t, BF16),
                vm((4, SEQ, HEAD), BF16), vm((4, HEAD, SEQ), BF16),
                vm((PAIR, HEAD, HALF), F32), vm((PAIR, HEAD, HALF), F32), vm((4, PAIR, HALF, HEAD), BF16),
                dma, dma((2, SUBS)), dma, dma, dma, dma((4,)), dma((4,)), dma((SUBS,)), dma, dma((4,)),
                dma, dma((2,)), dma, dma((2,)), dma, dma((2, 4)), dma, dma,
                dma, dma, dma((2,)), dma((2,)), dma((2,)), dma, dma,
            ],
            compiler_params=pltpu.CompilerParams(collective_id=0, has_side_effects=True, vmem_limit_bytes=37 * 1024 * 1024),
        )(*[pltpu.with_memory_space_constraint(x, pltpu.HBM) for x in (
            query.reshape(pairs), key_in.reshape(pairs), value.reshape(pairs), d_out.reshape(pairs),
            rel_k.reshape(SEQ, N_PAIR, PAIR, head_dim), bias_u.reshape(N_PAIR, PAIR, head_dim), bias_w.reshape(N_PAIR, PAIR, head_dim))])
        o, dq, dk, dv, dr, du, dw = pl.pallas_call(
            writer,
            name="writer",
            out_shape=(act, act, act, act, jax.ShapeDtypeStruct((SEQ, n_heads, 1, head_dim), F32), vec, vec),
            in_specs=[whole] * (4 + N_PART),
            out_specs=[whole] * 7,
            scratch_shapes=[dma((6 + 2 * N_PART,))],
            compiler_params=pltpu.CompilerParams(vmem_limit_bytes=1024 * 1024),
        )(*outs[:-1])
        full = query.shape
        return (o.reshape(full), dq.reshape(full), dk.reshape(full), dv.reshape(full),
                du.reshape(bias_u.shape), dw.reshape(bias_w.shape), dr.reshape(rel_k.shape))

    return jax.shard_map(local, mesh=mesh,
                         in_specs=(seq_spec, seq_spec, seq_spec, P(), P(), P(), seq_spec),
                         out_specs=(seq_spec, seq_spec, seq_spec, seq_spec, P(), P(), P()),
                         check_vma=False)
```

```python
import jax
import jax.numpy as jnp
from jax import lax
from jax.experimental import pallas as pl
from jax.experimental.pallas import tpu as pltpu
from jax.sharding import PartitionSpec as P

MESH = pl.DeviceIdType.MESH
BF16, F32 = jnp.bfloat16, jnp.float32
LOG2E = 1.4426950408889634

N_DEV = 16
PLANE = 8
PAIR = 2
N_PAIR = 8
SLOTS = 4
SUBS = 2 * SLOTS
EARLY = 3
ROWS = 64
HALF = PLANE * ROWS
SEQ = 2 * HALF
HEAD = 128
QB = 256
WIN = HALF + QB
N_PART = 6
PART = 86
FIN = N_PART * PART
TIP = 2 * ROWS
FAR = N_PAIR - 2
UNITS = FAR * SLOTS
TURNS = ((1, 3, 2), (3, 1, 2))


def dot(lhs, rhs):
    return jnp.dot(lhs, rhs, preferred_element_type=F32)


def flip8(x):
    rows, cols = x.shape
    idx = 7 - lax.broadcasted_iota(jnp.int32, (rows // 8, 8, cols), 1)
    return jnp.take_along_axis(x.reshape(rows // 8, 8, cols), idx, axis=1).reshape(rows, cols)


def eye_rev(dtype):
    total = lax.broadcasted_iota(jnp.int32, (HEAD, HEAD), 0) + lax.broadcasted_iota(jnp.int32, (HEAD, HEAD), 1)
    return jnp.where(total == HEAD - 1, 1.0, 0.0).astype(dtype)


def kernel(q_in, k_in, v_in, g_in, r_in, u_in, w_in,
           o_out, dq_out, dk_out, dv_out, dr0_out, dr1_out, dr2_out, dr3_out, dr4_out, dr5_out, far_out,
           buf, rbuf, r_buf, u_buf, w_buf, st_tx, st_rx, tip_st, st_ref, dr_rx, dr_rz, dr_fin, dr_acc,
           s_ref, e_ref, dp_ref, pb_ref, ds_ref, dd_ref,
           a_s, c_s, g_s, k_s, v_s, at_s, ct_s, gt_s, kt_s, vt_s, rev_s, rt_s, dkt, dvt, stage,
           in_send, in_recv, out_send, out_recv, own_sem, r_sem, up_send, up_recv, st_send, st_recv,
           x_send, x_recv, z_send, z_recv, ring_send, ring_recv, fw_send, fw_recv,
           far_send, far_recv, tip_sem, tip_near, tip_send, ts_send, ts_recv):
    me = lax.axis_index("cp")
    core = me % 2
    chip = me // 2
    col = chip % 4
    z = chip // 4
    partner = me + 1 - 2 * core
    across = me + PLANE * (1 - 2 * z)
    scale = HEAD ** -0.5

    def wait_for(ref, sem):
        pltpu.make_async_copy(ref, ref, sem).wait()

    y = col // 2
    lower, upper = z == 0, z == 1
    tip = chip == 7 * z
    tip_base = 2 - 2 * z

    tables = [pltpu.make_async_copy(src, dst, r_sem.at[j]) for j, (src, dst) in enumerate(
        ((r_in.at[:, 2 * col], r_buf.at[0]), (r_in.at[:, 2 * col + 1], r_buf.at[1]), (u_in, u_buf), (w_in, w_buf)))]
    for copy in tables:
        copy.start()

    barrier = pltpu.get_barrier_semaphore()

    for peer in [across] + [me ^ step for step in range(PLANE - 1, 0, -1)]:
        pl.semaphore_signal(barrier, inc=1, device_id=(peer,), device_id_type=MESH)
    pl.semaphore_wait(barrier, PLANE)

    my_rows = pl.ds(pl.multiple_of((me % PLANE) * ROWS, ROWS), ROWS)

    even = chip % 2 == z
    loaded = y != z

    def peers(late=False):
        near = core == 0
        if late:
            near = jnp.logical_not(near) & (even | jnp.logical_not(loaded))
        first, second, third = [jnp.where(near, near_turn, far_turn) for near_turn, far_turn in zip(*TURNS)]
        for turn, other in ((first, 0), (third, 0), (first, 1), (third, 1), (second, 0), (second, 1)):
            yield me ^ (2 * turn + other)
        yield partner

    def send_in(ins, sub):
        pair, row = sub // SLOTS, sub % SLOTS
        for first in (0, 2):
            for t in (first, first + 1):
                pltpu.make_async_copy(ins[t].at[core * SLOTS + row, :, 2 * col + pair], buf.at[t, sub, my_rows], in_recv.at[first // 2, sub]).start()
            for peer in peers():
                for t in (first, first + 1):
                    pltpu.make_async_remote_copy(
                        src_ref=ins[t].at[(peer % 2) * SLOTS + row, :, 2 * ((peer // 2) % 4) + pair], dst_ref=buf.at[t, sub, my_rows],
                        send_sem=in_send, recv_sem=in_recv.at[first // 2, sub], device_id=(peer,), device_id_type=MESH).start()

    def send_all(ins):
        def send_sub(sub, carry):
            send_in(ins, sub)
            return carry
        lax.fori_loop(0, SUBS, send_sub, 0)

    @pl.when(lower)
    def _():
        send_all((k_in, v_in, q_in, g_in))

    @pl.when(upper)
    def _():
        send_all((q_in, g_in, k_in, v_in))

    @pl.when(tip)
    def _():
        for t, src in enumerate((q_in, k_in, v_in, g_in)):
            for row in range(SLOTS):
                pltpu.make_async_remote_copy(
                    src_ref=src.at[(1 - core) * SLOTS + row, :, pl.ds(tip_base, FAR)], dst_ref=far_out.at[t, row],
                    send_sem=far_send, recv_sem=far_recv, device_id=(partner,), device_id_type=MESH).start()

    for copy in tables:
        copy.wait()
    rev = eye_rev(BF16)
    for p in range(2):
        pair_tab = pltpu.einshape("abc->bac", r_buf[p])
        for hh in range(PAIR):
            for blk in range(SEQ // HEAD):
                part = pair_tab[hh, SEQ - HEAD * (blk + 1):SEQ - HEAD * blk]
                flipped = dot(rev, part).astype(BF16)
                rev_s[2 * p + hh, HEAD * blk:HEAD * (blk + 1), :] = flipped
                rt_s[2 * p + hh, :, HEAD * blk:HEAD * (blk + 1)] = flipped.T
    dr_acc[...] = jnp.zeros_like(dr_acc)

    acts = (dk_out, dv_out, o_out, dq_out)

    def send_out(sub, which, late=False):
        place = (core * SLOTS + sub % SLOTS, slice(None), 2 * col + sub // SLOTS)
        for t in which:
            pltpu.make_async_copy(buf.at[t, sub, my_rows], acts[t].at[place], out_recv).start()
        for peer in peers(late):
            peer_rows = pl.ds(pl.multiple_of((peer % PLANE) * ROWS, ROWS), ROWS)
            to_tip = (peer // 2 == 7 * z) & jnp.logical_not(tip)
            for t in which:
                @pl.when(jnp.logical_not(to_tip & (lower if t >= 2 else upper)))
                def _():
                    pltpu.make_async_remote_copy(
                        src_ref=buf.at[t, sub, peer_rows], dst_ref=acts[t].at[place],
                        send_sem=out_send, recv_sem=out_recv, device_id=(peer,), device_id_type=MESH).start()

    def send_up(sub):
        wait_for(buf.at[0:2, sub], in_recv.at[0, sub])
        for j in range(2):
            pltpu.make_async_remote_copy(src_ref=buf.at[j, sub], dst_ref=rbuf.at[j, sub], send_sem=up_send.at[sub % 4], recv_sem=up_recv.at[sub],
                                         device_id=(across,), device_id_type=MESH).start()

    def unpack(ref, j, sub):
        return pltpu.einshape("abc->bac", ref[j, sub])

    def load_rows(q_ref, q_j, g_ref, g_j, sub, start, turned):
        rows = slice(start, start + HALF)
        p = sub // SLOTS
        q2 = unpack(q_ref, q_j, sub)
        u = u_buf[2 * col + p].astype(F32)
        w = w_buf[2 * col + p].astype(F32)
        for hh in range(PAIR):
            q32 = q2[hh].astype(F32)
            a = (q32 + u[hh:hh + 1]).astype(BF16)
            c = (q32 + w[hh:hh + 1]).astype(BF16)
            a_s[hh, rows, :] = a
            c_s[hh, rows, :] = c
            at_s[hh, :, rows] = a.T
            if turned:
                ct_s[hh, :, rows] = flip8(c.astype(F32)).astype(BF16).T
        g2 = unpack(g_ref, g_j, sub)
        g_s[:, rows, :] = g2
        for hh in range(PAIR):
            gt_s[hh, :, rows] = g2[hh].T

    def load_keys(k_ref, k_j, v_ref, v_j, sub, start):
        rows = slice(start, start + HALF)
        k2 = unpack(k_ref, k_j, sub)
        v2 = unpack(v_ref, v_j, sub)
        k_s[:, rows, :] = k2
        v_s[:, rows, :] = v2
        for hh in range(PAIR):
            kt_s[hh, :, rows] = k2[hh].T
            vt_s[hh, :, rows] = v2[hh].T

    def row_block(hh, head, start, i0, lo, fresh, stats):
        width = i0 + QB
        rows = slice(start, start + QB)
        s_ref[:, :width] = dot(a_s[hh, rows, :], kt_s[hh, :, :width])
        e_ref[:, :width] = dot(c_s[hh, rows, :], rt_s[head, :, SEQ - width:])
        dp_ref[:, :width] = dot(g_s[hh, rows, :], vt_s[hh, :, :width])
        for r0 in range(0, QB, 16):
            group = slice(r0, r0 + 16)
            rel = pltpu.roll(e_ref[group, :width], i0 + 1 + r0, 1, stride=1, stride_axis=0)
            s = s_ref[group, :width] + rel
            ahead = lax.broadcasted_iota(jnp.int32, (16, width), 1) - lax.broadcasted_iota(jnp.int32, (16, width), 0)
            s = jnp.where(ahead <= i0 + r0, s, -jnp.inf)
            top = jnp.max(s, axis=1, keepdims=True)
            p = jnp.exp2((s - top) * (scale * LOG2E))
            total = jnp.sum(p, axis=1, keepdims=True)
            p = p * (1.0 / total)
            pb_ref[group, :width] = p.astype(BF16)
            dp = dp_ref[group, :width]
            row_dot = jnp.sum(p * dp, axis=1, keepdims=True)
            ds = (p * (dp - row_dot) * scale).astype(BF16)
            ds_ref[group, :width] = ds
            flipped = flip8(ds.astype(F32))
            half = [pltpu.roll(flipped[8 * j:8 * j + 8], QB - 8 - r0 - 8 * j, 1, stride=1, stride_axis=0) for j in range(2)]
            dd_ref[group, :width] = jnp.concatenate(half, axis=0).astype(BF16)
            if stats:
                lane = lax.broadcasted_iota(jnp.int32, (16, HEAD), 1)
                st_ref[group, :] = jnp.where(lane == 0, top * (scale * LOG2E) + jnp.log2(total), row_dot)
        pb = pb_ref[:, :width]
        ds = ds_ref[:, :width]
        dd = dd_ref[:, :width]
        stage[0, hh, rows, :] = dot(pb, v_s[hh, :width, :]).astype(BF16)
        dqc = dot(ds, k_s[hh, :width, :])
        dqr = flip8(dot(dd, rev_s[head, SEQ - width:, :]))
        stage[1, hh, rows, :] = (dqc + dqr).astype(BF16)
        dr_acc[head, 1, HEAD:HEAD + 1, HALF - HEAD:] += jnp.sum(dqc, axis=0, keepdims=True)
        dr_acc[head, 1, HEAD + 1:HEAD + 2, HALF - HEAD:] += jnp.sum(dqr, axis=0, keepdims=True)
        dk_new = dot(at_s[hh, :, rows], ds_ref[:, lo:width])
        dv_new = dot(gt_s[hh, :, rows], pb_ref[:, lo:width])
        if fresh:
            dkt[hh] = dk_new
            dvt[hh] = dv_new
        else:
            dkt[hh, :, :width - lo] += dk_new
            dvt[hh, :, :width - lo] += dv_new
        dr_new = dot(ct_s[hh, :, rows], dd)
        if width > HALF:
            dr_acc[head, 0, :HEAD, SEQ - width:] += dr_new[:, :width - HALF]
            dr_acc[head, 1, :HEAD, :] += dr_new[:, width - HALF:]
        else:
            dr_acc[head, 1, :HEAD, HALF - width:] += dr_new

    def col_block(hh, head, sub, i0):
        rows = slice(i0, i0 + QB)
        first = WIN - i0
        s_ref[:, :HALF] = dot(a_s[hh, rows, :], kt_s[hh, :, :HALF])
        e_ref[:, :WIN] = dot(c_s[hh, rows, :], rt_s[head, :, first:first + WIN])
        dp_ref[:, :HALF] = dot(g_s[hh, rows, :], vt_s[hh, :, :HALF])
        st_ref[:, :8] = st_rx[sub, hh, :, i0 - HALF:i0 - HALF + QB].T
        for r0 in range(0, QB, 16):
            group = slice(r0, r0 + 16)
            rel = pltpu.roll(e_ref[group, :WIN], HALF + 1 + r0, 1, stride=1, stride_axis=0)[:, :HALF]
            log_sum = st_ref[group, 0:1]
            row_dot = st_ref[group, 1:2]
            p = jnp.exp2((s_ref[group, :HALF] + rel) * (scale * LOG2E) - log_sum)
            pb_ref[group, :HALF] = p.astype(BF16)
            ds_ref[group, :HALF] = (p * (dp_ref[group, :HALF] - row_dot) * scale).astype(BF16)
        dkt[hh] += dot(at_s[hh, :, rows], ds_ref[:, :HALF])
        dvt[hh] += dot(gt_s[hh, :, rows], pb_ref[:, :HALF])

    def store_rows(sub):
        for t in range(2):
            buf[2 + t, sub] = pltpu.einshape("abc->bac", stage[t])

    def store_keys(sub):
        for hh in range(PAIR):
            stage[2, hh] = dkt[hh].astype(BF16).T
            stage[3, hh] = dvt[hh].astype(BF16).T
        for t in range(2):
            buf[t, sub] = pltpu.einshape("abc->bac", stage[2 + t])

    def wait_up(sub):
        wait_for(rbuf.at[:, sub], up_recv.at[sub])
        wait_for(rbuf.at[:, sub], up_send.at[sub % 4])

    def wait_in(sub):
        wait_for(buf.at[2:4, sub], in_recv.at[1, sub])

    def lower_rows(sub):
        wait_in(sub)
        load_rows(buf, 2, buf, 3, sub, 0, True)

    def lower_own(sub):
        load_keys(buf, 0, buf, 1, sub, 0)

        def own(hh, carry):
            head = 2 * (sub // SLOTS) + hh
            row_block(hh, head, QB, QB, 0, True, False)
            row_block(hh, head, 0, 0, 0, False, False)
            return carry

        lax.fori_loop(0, PAIR, own, 0)
        store_rows(sub)

    def lower_theirs(sub):
        wait_up(sub)
        load_rows(rbuf, 0, rbuf, 1, sub, HALF, False)
        wait_for(st_rx.at[sub], st_recv.at[sub % 4])

        def theirs(hh, carry):
            head = 2 * (sub // SLOTS) + hh
            col_block(hh, head, sub, HALF)
            col_block(hh, head, sub, HALF + QB)
            return carry

        lax.fori_loop(0, PAIR, theirs, 0)
        store_keys(sub)

    def upper_own(sub):
        wait_in(sub)
        wait_up(sub)
        load_rows(buf, 0, buf, 1, sub, 0, True)
        load_keys(rbuf, 0, rbuf, 1, sub, 0)
        load_keys(buf, 2, buf, 3, sub, HALF)

        def own(hh, carry):
            head = 2 * (sub // SLOTS) + hh
            for blk in (1, 0):
                row_block(hh, head, QB * blk, HALF + QB * blk, HALF, blk == 1, True)
                st_tx[sub, hh, :, QB * blk:QB * (blk + 1)] = st_ref[...].T[:8]
            pltpu.make_async_remote_copy(src_ref=st_tx.at[sub, hh], dst_ref=st_rx.at[sub, hh], send_sem=st_send, recv_sem=st_recv.at[sub % 4],
                                         device_id=(across,), device_id_type=MESH).start()

            @pl.when(jnp.logical_not(tip))
            def _():
                pltpu.make_async_remote_copy(src_ref=st_tx.at[sub, hh, :, HALF - TIP:], dst_ref=tip_st.at[col, sub, hh], send_sem=ts_send,
                                             recv_sem=ts_recv, device_id=(N_DEV - 2 + core,), device_id_type=MESH).start()
            return carry

        lax.fori_loop(0, PAIR, own, 0)
        store_rows(sub)
        store_keys(sub)

    side = 1 - core
    parts = (dr0_out, dr1_out, dr2_out, dr3_out, dr4_out, dr5_out)

    def swap_start(p):
        for n in range(2):
            pltpu.make_async_remote_copy(src_ref=dr_acc.at[2 * p + n, side], dst_ref=dr_rx.at[p, n], send_sem=x_send, recv_sem=x_recv.at[p],
                                         device_id=(partner,), device_id_type=MESH).start()

    def swap_add(p):
        wait_for(dr_rx.at[p], x_recv.at[p])
        for n in range(2):
            dr_rx[p, n] = dr_rx[p, n] + dr_acc[2 * p + n, core]

    def cross_start(p):
        pltpu.make_async_remote_copy(src_ref=dr_rx.at[p, 1 - z], dst_ref=dr_rz.at[p], send_sem=z_send, recv_sem=z_recv.at[p],
                                     device_id=(across,), device_id_type=MESH).start()

    def head_of(p, bits):
        other = chip ^ bits
        return 4 * (other % 4) + 2 * p + other // 4

    def block(p, m, bits):
        if bits == 0:
            return dr_fin.at[p, PART * m:PART * (m + 1)]
        return parts[m].at[side, :, head_of(p, bits)]

    def forward(p, m, bits):
        pltpu.make_async_remote_copy(src_ref=block(p, m, bits), dst_ref=parts[m].at[side, :, head_of(p, bits)], send_sem=fw_send,
                                     recv_sem=fw_recv, device_id=(partner,), device_id_type=MESH).start()

    def blocks(count):
        return parts[0].at[:, :, :N_PART // 2 * count]

    def pass_on(p, bits, hop, device):
        for m in range(N_PART):
            pltpu.make_async_remote_copy(
                src_ref=block(p, m, bits), dst_ref=parts[m].at[side, :, head_of(p, bits)], send_sem=ring_send,
                recv_sem=ring_recv.at[p, hop], device_id=(device,), device_id_type=MESH).start()

    def hand_over(p, bits):
        for m in range(N_PART):
            forward(p, m, bits)

    along_x, along_y = me ^ 2, me ^ 4

    def hop_start(p, hop):
        if hop == 0:
            for device in (along_x, along_y, across):
                pass_on(p, 0, 0, device)
        if hop == 1:
            @pl.when(even & loaded)
            def _():
                pass_on(p, 1, 1, along_y)

            @pl.when(jnp.logical_not(even) & loaded)
            def _():
                pass_on(p, 2, 1, along_x)

            pass_on(p, 1, 1, across)
            pass_on(p, 2, 1, across)
        if hop == 2:
            @pl.when(even & loaded)
            def _():
                pass_on(p, 5, 2, along_y)

            @pl.when(jnp.logical_not(even) & loaded)
            def _():
                pass_on(p, 6, 2, along_x)

            @pl.when(even)
            def _():
                pass_on(p, 3, 2, across)
        if hop == 3:
            @pl.when(even)
            def _():
                pass_on(p, 7, 3, across)

    def hop_wait(p, hop):
        if hop == 0:
            wait_for(blocks(3), ring_recv.at[p, 0])
            for bits in (1, 2, 4):
                hand_over(p, bits)
        if hop == 1:
            @pl.when(even)
            def _():
                wait_for(blocks(3), ring_recv.at[p, 1])
                hand_over(p, 3)

            @pl.when(jnp.logical_not(even))
            def _():
                wait_for(blocks(2), ring_recv.at[p, 1])
            for bits in (5, 6):
                hand_over(p, bits)
        if hop == 2:
            wait_for(blocks(1), ring_recv.at[p, 2])
            hand_over(p, 7)
        if hop == 3:
            @pl.when(jnp.logical_not(even))
            def _():
                wait_for(blocks(1), ring_recv.at[p, 3])
                hand_over(p, 3)

    def sent_wait():
        @pl.when(even & loaded)
        def _():
            wait_for(buf.at[:3, :, :FIN * 18 // 24], ring_send)

        @pl.when(even != loaded)
        def _():
            wait_for(buf.at[:3, :7, :FIN * 14 // 21], ring_send)

        @pl.when(jnp.logical_not(even | loaded))
        def _():
            wait_for(buf.at[:2, :6, :FIN * 10 // 12], ring_send)

    def cross_finish(p):
        wait_for(dr_rz.at[p], z_recv.at[p])
        total = dr_rx[p, z] + dr_rz[p]
        rev32 = eye_rev(F32)
        for m in range(HALF // HEAD):
            part = total[:HEAD, HALF - HEAD * (m + 1):HALF - HEAD * m]
            turned = lax.dot_general(rev32, part, (((1,), (1,)), ((), ())), precision=lax.Precision.HIGHEST, preferred_element_type=F32)
            dr_fin[p, HEAD * m:HEAD * (m + 1)] = turned.reshape(HEAD, 1, HEAD)
        dr_fin[p, HALF] = total[HEAD:HEAD + 1, HALF - HEAD:]
        dr_fin[p, HALF + 1] = total[HEAD + 1:HEAD + 2, HALF - HEAD:]
        dr_fin[p, HALF + 2:] = jnp.zeros((FIN - HALF - 2, 1, HEAD), F32)
        hop_start(p, 0)
        for m in range(N_PART):
            pltpu.make_async_copy(block(p, m, 0), parts[m].at[side, :, head_of(p, 0)], own_sem).start()
        hand_over(p, 0)

    def tip_load(unit):
        slot, row, far = unit % 2, unit // FAR, unit % FAR
        pair = far + tip_base
        for t, src in enumerate((q_in, k_in, v_in, g_in)):
            pltpu.make_async_copy(src.at[core * SLOTS + row, :, pair], r_buf.at[slot, pl.ds(TIP * t + ROWS * core, ROWS)], tip_sem.at[slot]).start()
            pltpu.make_async_copy(far_out.at[t, row, :, far], r_buf.at[slot, pl.ds(TIP * t + ROWS * (1 - core), ROWS)], tip_sem.at[slot]).start()
        pltpu.make_async_copy(r_in.at[:TIP, pair], r_buf.at[slot, 4 * TIP:5 * TIP], tip_sem.at[slot]).start()

    def tip_done(slot):
        wait_for(r_buf.at[slot, :TIP], tip_near.at[slot])
        wait_for(r_buf.at[slot, :TIP], tip_send.at[slot])

    def tip_group(hh, r0):
        group = slice(TIP * hh + r0, TIP * hh + r0 + 16)
        rel = pltpu.roll(e_ref[group, :TIP], 1 + r0, 1, stride=1, stride_axis=0)
        ahead = lax.broadcasted_iota(jnp.int32, (16, TIP), 1) - lax.broadcasted_iota(jnp.int32, (16, TIP), 0)
        return group, s_ref[group, :TIP] + rel, ahead <= r0

    def tip_rows(hh):
        for r0 in range(0, TIP, 16):
            group, s, seen = tip_group(hh, r0)
            s = jnp.where(seen, s, -jnp.inf)
            top = jnp.max(s, axis=1, keepdims=True)
            p = jnp.exp2((s - top) * (scale * LOG2E))
            p = p * (1.0 / jnp.sum(p, axis=1, keepdims=True))
            pb_ref[group, :TIP] = p.astype(BF16)
            dp = dp_ref[group, :TIP]
            row_dot = jnp.sum(p * dp, axis=1, keepdims=True)
            ds = (p * (dp - row_dot) * scale).astype(BF16)
            ds_ref[group, :TIP] = ds
            flipped = flip8(ds.astype(F32))
            half = [pltpu.roll(flipped[8 * j:8 * j + 8], TIP - 8 - r0 - 8 * j, 1, stride=1, stride_axis=0) for j in range(2)]
            dd_ref[group, :TIP] = jnp.concatenate(half, axis=0).astype(BF16)
        rows = slice(TIP * hh, TIP * (hh + 1))
        stage[0, hh, :TIP, :] = dot(pb_ref[rows, :TIP], v_s[hh, :TIP, :]).astype(BF16)
        dqc = dot(ds_ref[rows, :TIP], k_s[hh, :TIP, :])
        dqr = flip8(dot(dd_ref[rows, :TIP], c_s[hh, :TIP, :]))
        stage[1, hh, :TIP, :] = (dqc + dqr).astype(BF16)

    def tip_keys(hh, stats):
        rows = slice(TIP * hh, TIP * (hh + 1))
        st_ref[rows, :8] = stats.T
        for r0 in range(0, TIP, 16):
            group, s, seen = tip_group(hh, r0)
            p = jnp.where(seen, jnp.exp2(s * (scale * LOG2E) - st_ref[group, 0:1]), 0.0)
            pb_ref[group, :TIP] = p.astype(BF16)
            ds_ref[group, :TIP] = (p * (dp_ref[group, :TIP] - st_ref[group, 1:2]) * scale).astype(BF16)
        over_rows = (((0,), (0,)), ((), ()))
        stage[0, hh, :TIP, :] = lax.dot_general(ds_ref[rows, :TIP], a_s[hh, :TIP, :], over_rows, preferred_element_type=F32).astype(BF16)
        stage[1, hh, :TIP, :] = lax.dot_general(pb_ref[rows, :TIP], g_s[hh, :TIP, :], over_rows, preferred_element_type=F32).astype(BF16)

    def tip_unit(unit, carry):
        slot, row, far = unit % 2, unit // FAR, unit % FAR
        pair = far + tip_base
        wait_for(r_buf.at[slot, :5 * TIP], tip_sem.at[slot])

        @pl.when(unit + 1 < UNITS)
        def _():
            tip_load(unit + 1)

        q2, k2, v2, g2, r2 = [pltpu.einshape("abc->bac", r_buf[slot, TIP * t:TIP * (t + 1)]) for t in range(5)]
        u = u_buf[pair].astype(F32)
        w = w_buf[pair].astype(F32)
        for hh in range(PAIR):
            rows = slice(TIP * hh, TIP * (hh + 1))
            q32 = q2[hh].astype(F32)
            a = (q32 + u[hh:hh + 1]).astype(BF16)
            c = (q32 + w[hh:hh + 1]).astype(BF16)
            falling = dot(eye_rev(BF16), r2[hh]).astype(BF16)
            s_ref[rows, :TIP] = dot(a, k2[hh].T)
            e_ref[rows, :TIP] = dot(c, falling.T)
            dp_ref[rows, :TIP] = dot(g2[hh], v2[hh].T)
            a_s[hh, :TIP, :] = a
            c_s[hh, :TIP, :] = falling
            g_s[hh, :TIP, :] = g2[hh]
            k_s[hh, :TIP, :] = k2[hh]
            v_s[hh, :TIP, :] = v2[hh]

        @pl.when(lower)
        def _():
            for hh in range(PAIR):
                tip_rows(hh)

        @pl.when(upper)
        def _():
            for hh in range(PAIR):
                tip_keys(hh, tip_st[far // 2, (far % 2) * SLOTS + row, hh])

        @pl.when(unit >= 2)
        def _():
            tip_done(slot)

        for n in range(2):
            r_buf[slot, (5 + n) * TIP:(6 + n) * TIP] = pltpu.einshape("abc->bac", stage[n, :, :TIP, :])
        place = (core * SLOTS + row, slice(None), pair)

        def give(results):
            for n, dst in enumerate(results):
                pltpu.make_async_copy(r_buf.at[slot, pl.ds((5 + n) * TIP + ROWS * core, ROWS)], dst.at[place], tip_near.at[slot]).start()
                pltpu.make_async_remote_copy(
                    src_ref=r_buf.at[slot, pl.ds((5 + n) * TIP + ROWS * (1 - core), ROWS)], dst_ref=dst.at[place],
                    send_sem=tip_send.at[slot], recv_sem=out_recv, device_id=(partner,), device_id_type=MESH).start()

        @pl.when(lower)
        def _():
            give((o_out, dq_out))

        @pl.when(upper)
        def _():
            give((dk_out, dv_out))
        return carry

    def tips(third):
        @pl.when(tip)
        def _():
            if third == 0:
                wait_for(far_out, far_recv)

                @pl.when(upper)
                def _():
                    wait_for(tip_st, ts_recv)
                tip_load(0)
            lax.fori_loop(UNITS // 3 * third, UNITS // 3 * (third + 1), tip_unit, 0)
            if third == 2:
                tip_done(0)
                tip_done(1)

    send_up(0)

    def sub_body(sub, carry):
        @pl.when(sub < SUBS - 1)
        def _():
            send_up(sub + 1)

        @pl.when(sub == SLOTS)
        def _():
            swap_start(0)

        @pl.when(sub == SUBS - 1)
        def _():
            swap_add(0)
            cross_start(0)

        @pl.when(sub == SUBS)
        def _():
            swap_start(1)
            swap_add(1)
            cross_start(1)
            cross_finish(0)

        @pl.when(lower & (sub < SUBS))
        def _():
            lower_rows(sub)

        @pl.when(lower & (sub > 0))
        def _():
            lower_theirs(sub - 1)

        @pl.when(lower & (sub < SUBS))
        def _():
            lower_own(sub)

        @pl.when(upper & (sub < SUBS))
        def _():
            upper_own(sub)

        @pl.when(sub <= EARLY)
        def _():
            send_out(sub, (2, 3))

        @pl.when((sub > 0) & (sub <= EARLY))
        def _():
            send_out(sub - 1, (0, 1))
        return carry

    lax.fori_loop(0, SUBS + 1, sub_body, 0)

    cross_finish(1)
    send_out(EARLY, (0, 1))
    for p in range(2):
        hop_wait(p, 0)
        hop_start(p, 1)
    for p in range(2):
        send_out(EARLY + 1 + p, range(4))
        tips(p)
        hop_wait(p, 1)
        hop_start(p, 2)

    def send_late(sub, carry):
        send_out(sub, range(4), True)
        return carry

    lax.fori_loop(EARLY + 3, SUBS, send_late, 0)
    tips(2)
    for p in range(2):
        hop_wait(p, 2)
        hop_start(p, 3)
    for p in range(2):
        hop_wait(p, 3)

    wait_for(buf.at[:, :, :HALF - ROWS], in_send)

    @pl.when(tip)
    def _():
        wait_for(buf.at[:, :, :HALF - 3 * ROWS // 2], out_recv)
        wait_for(buf.at[:, :, :HALF - ROWS], out_send)
        wait_for(far_out, far_send)

    @pl.when(jnp.logical_not(tip))
    def _():
        wait_for(buf, out_recv)
        wait_for(buf.at[:, :, :HALF - 2 * ROWS], out_send)

    @pl.when(upper & jnp.logical_not(tip))
    def _():
        wait_for(st_tx.at[:2], ts_send)

    @pl.when(upper)
    def _():
        wait_for(st_tx, st_send)

    wait_for(dr_rx, x_send)
    wait_for(dr_rz, z_send)
    wait_for(blocks(2), own_sem)
    sent_wait()
    for sem in (fw_send, fw_recv):
        wait_for(buf.at[:3, :, :FIN * 16 // 24], sem)


def writer(*refs):
    ins, (o, dq, dk, dv, dr, du, dw, sem) = refs[:4 + N_PART], refs[4 + N_PART:]
    pairs = list(zip(ins[:4], (o, dq, dk, dv)))
    for m, part in enumerate(ins[4:]):
        rows = min(PART, HALF - PART * m)
        for side in range(2):
            start = HALF * side + PART * m
            pairs.append((part.at[side, :rows], dr.at[start:start + rows]))
    last = HALF - PART * (N_PART - 1)
    pairs += [(ins[-1].at[0, last], du), (ins[-1].at[0, last + 1], dw)]
    copies = [pltpu.make_async_copy(src, dst, sem.at[j]) for j, (src, dst) in enumerate(pairs)]
    for copy in copies:
        copy.start()
    for copy in copies:
        copy.wait()


def solution(mesh):
    seq_spec = P(None, "cp", None, None)

    def local(query, key_in, value, bias_u, bias_w, rel_k, d_out):
        n_batch, rows, n_heads, head_dim = query.shape
        pairs = (n_batch, rows, N_PAIR, PAIR, head_dim)
        vm = pltpu.VMEM
        dma = pltpu.SemaphoreType.DMA
        whole = pl.BlockSpec(memory_space=pl.ANY)
        act = jax.ShapeDtypeStruct(pairs, BF16)
        vec = jax.ShapeDtypeStruct((n_heads, 1, head_dim), F32)
        tok = (PAIR, SEQ, HEAD)
        tok_t = (PAIR, HEAD, SEQ)
        acc = (HEAD + 8, HALF)
        outs = pl.pallas_call(
            kernel,
            name="rel_attn",
            out_shape=(act, act, act, act,
                       *[jax.ShapeDtypeStruct((2, PART, n_heads, 1, head_dim), F32)] * N_PART,
                       jax.ShapeDtypeStruct((4, SLOTS, ROWS, FAR, PAIR, HEAD), BF16)),
            in_specs=[pl.BlockSpec(memory_space=pltpu.HBM)] * 7,
            out_specs=[whole] * (5 + N_PART),
            scratch_shapes=[
                vm((4, SUBS, HALF, PAIR, HEAD), BF16), vm((2, SUBS, HALF, PAIR, HEAD), BF16),
                vm((2, SEQ, PAIR, HEAD), BF16), vm((N_PAIR, PAIR, HEAD), BF16), vm((N_PAIR, PAIR, HEAD), BF16),
                vm((SUBS, PAIR, 8, HALF), F32), vm((SUBS, PAIR, 8, HALF), F32), vm((3, SUBS, PAIR, 8, TIP), F32), vm((QB, HEAD), F32),
                vm((2, 2) + acc, F32), vm((2,) + acc, F32), vm((2, FIN, 1, HEAD), F32), vm((4, 2) + acc, F32),
                vm((QB, SEQ), F32), vm((QB, SEQ), F32), vm((QB, SEQ), F32),
                vm((QB, SEQ), BF16), vm((QB, SEQ), BF16), vm((QB, SEQ), BF16),
                vm(tok, BF16), vm(tok, BF16), vm(tok, BF16), vm(tok, BF16), vm(tok, BF16),
                vm(tok_t, BF16), vm(tok_t, BF16), vm(tok_t, BF16), vm(tok_t, BF16), vm(tok_t, BF16),
                vm((4, SEQ, HEAD), BF16), vm((4, HEAD, SEQ), BF16),
                vm((PAIR, HEAD, HALF), F32), vm((PAIR, HEAD, HALF), F32), vm((4, PAIR, HALF, HEAD), BF16),
                dma, dma((2, SUBS)), dma, dma, dma, dma((4,)), dma((4,)), dma((SUBS,)), dma, dma((4,)),
                dma, dma((2,)), dma, dma((2,)), dma, dma((2, 4)), dma, dma,
                dma, dma, dma((2,)), dma((2,)), dma((2,)), dma, dma,
            ],
            compiler_params=pltpu.CompilerParams(collective_id=0, has_side_effects=True, vmem_limit_bytes=37 * 1024 * 1024),
        )(*[pltpu.with_memory_space_constraint(x, pltpu.HBM) for x in (
            query.reshape(pairs), key_in.reshape(pairs), value.reshape(pairs), d_out.reshape(pairs),
            rel_k.reshape(SEQ, N_PAIR, PAIR, head_dim), bias_u.reshape(N_PAIR, PAIR, head_dim), bias_w.reshape(N_PAIR, PAIR, head_dim))])
        o, dq, dk, dv, dr, du, dw = pl.pallas_call(
            writer,
            name="writer",
            out_shape=(act, act, act, act, jax.ShapeDtypeStruct((SEQ, n_heads, 1, head_dim), F32), vec, vec),
            in_specs=[whole] * (4 + N_PART),
            out_specs=[whole] * 7,
            scratch_shapes=[dma((6 + 2 * N_PART,))],
            compiler_params=pltpu.CompilerParams(vmem_limit_bytes=1024 * 1024),
        )(*outs[:-1])
        full = query.shape
        return (o.reshape(full), dq.reshape(full), dk.reshape(full), dv.reshape(full),
                du.reshape(bias_u.shape), dw.reshape(bias_w.shape), dr.reshape(rel_k.shape))

    return jax.shard_map(local, mesh=mesh,
                         in_specs=(seq_spec, seq_spec, seq_spec, P(), P(), P(), seq_spec),
                         out_specs=(seq_spec, seq_spec, seq_spec, seq_spec, P(), P(), P()),
                         check_vma=False)
```

```python
import jax
import jax.numpy as jnp
from jax import lax
from jax.experimental import pallas as pl
from jax.experimental.pallas import tpu as pltpu
from jax.sharding import PartitionSpec as P

MESH = pl.DeviceIdType.MESH
BF16, F32 = jnp.bfloat16, jnp.float32
LOG2E = 1.4426950408889634

N_DEV = 16
PLANE = 8
PAIR = 2
N_PAIR = 8
SLOTS = 4
SUBS = 2 * SLOTS
EARLY = 3
ROWS = 64
HALF = PLANE * ROWS
SEQ = 2 * HALF
HEAD = 128
QB = 256
WIN = HALF + QB
N_PART = 6
PART = 86
FIN = N_PART * PART
TIP = 2 * ROWS
FAR = N_PAIR - 2
UNITS = FAR * SLOTS
TURNS = ((1, 3, 2), (3, 1, 2))


def dot(lhs, rhs):
    return jnp.dot(lhs, rhs, preferred_element_type=F32)


def flip8(x):
    rows, cols = x.shape
    idx = 7 - lax.broadcasted_iota(jnp.int32, (rows // 8, 8, cols), 1)
    return jnp.take_along_axis(x.reshape(rows // 8, 8, cols), idx, axis=1).reshape(rows, cols)


def eye_rev(dtype):
    total = lax.broadcasted_iota(jnp.int32, (HEAD, HEAD), 0) + lax.broadcasted_iota(jnp.int32, (HEAD, HEAD), 1)
    return jnp.where(total == HEAD - 1, 1.0, 0.0).astype(dtype)


def kernel(q_in, k_in, v_in, g_in, r_in, u_in, w_in,
           o_out, dq_out, dk_out, dv_out, dr0_out, dr1_out, dr2_out, dr3_out, dr4_out, dr5_out, far_out,
           buf, rbuf, r_buf, u_buf, w_buf, st_tx, st_rx, tip_st, st_ref, dr_rx, dr_rz, dr_fin, dr_acc,
           s_ref, e_ref, dp_ref, pb_ref, ds_ref, dd_ref,
           a_s, c_s, g_s, k_s, v_s, at_s, ct_s, gt_s, kt_s, vt_s, rev_s, rt_s, dkt, dvt, stage,
           in_send, in_recv, out_send, out_recv, own_sem, r_sem, up_send, up_recv, st_send, st_recv,
           x_send, x_recv, z_send, z_recv, ring_send, ring_recv, fw_send, fw_recv,
           far_send, far_recv, tip_sem, tip_near, tip_send, ts_send, ts_recv):
    me = lax.axis_index("cp")
    core = me % 2
    chip = me // 2
    col = chip % 4
    z = chip // 4
    partner = me + 1 - 2 * core
    across = me + PLANE * (1 - 2 * z)
    scale = HEAD ** -0.5

    def wait_for(ref, sem):
        pltpu.make_async_copy(ref, ref, sem).wait()

    y = col // 2
    lower, upper = z == 0, z == 1
    tip = chip == 7 * z
    tip_base = 2 - 2 * z

    tables = [pltpu.make_async_copy(src, dst, r_sem.at[j]) for j, (src, dst) in enumerate(
        ((r_in.at[:, 2 * col], r_buf.at[0]), (r_in.at[:, 2 * col + 1], r_buf.at[1]), (u_in, u_buf), (w_in, w_buf)))]
    for copy in tables:
        copy.start()

    barrier = pltpu.get_barrier_semaphore()

    for peer in [across] + [me ^ step for step in range(PLANE - 1, 0, -1)]:
        pl.semaphore_signal(barrier, inc=1, device_id=(peer,), device_id_type=MESH)
    pl.semaphore_wait(barrier, PLANE)

    my_rows = pl.ds(pl.multiple_of((me % PLANE) * ROWS, ROWS), ROWS)

    even = chip % 2 == z
    loaded = y != z

    def peers(late=False):
        near, last = core == 0, 0
        if late:
            last = jnp.where(near & loaded & jnp.logical_not(even), 1, 0)
            near = jnp.logical_not(near) & (even | jnp.logical_not(loaded))
        first, second, third = [jnp.where(near, near_turn, far_turn) for near_turn, far_turn in zip(*TURNS)]
        for turn, other in ((first, 0), (third, 0), (first, 1), (third, 1), (second, last), (second, 1 - last)):
            yield me ^ (2 * turn + other)
        yield partner

    def send_in(ins, sub):
        pair, row = sub // SLOTS, sub % SLOTS
        for first in (0, 2):
            for t in (first, first + 1):
                pltpu.make_async_copy(ins[t].at[core * SLOTS + row, :, 2 * col + pair], buf.at[t, sub, my_rows], in_recv.at[first // 2, sub]).start()
            for peer in peers():
                for t in (first, first + 1):
                    pltpu.make_async_remote_copy(
                        src_ref=ins[t].at[(peer % 2) * SLOTS + row, :, 2 * ((peer // 2) % 4) + pair], dst_ref=buf.at[t, sub, my_rows],
                        send_sem=in_send, recv_sem=in_recv.at[first // 2, sub], device_id=(peer,), device_id_type=MESH).start()

    def send_all(ins):
        def send_sub(sub, carry):
            send_in(ins, sub)
            return carry
        lax.fori_loop(0, SUBS, send_sub, 0)

    @pl.when(lower)
    def _():
        send_all((k_in, v_in, q_in, g_in))

    @pl.when(upper)
    def _():
        send_all((q_in, g_in, k_in, v_in))

    @pl.when(tip)
    def _():
        for t, src in enumerate((q_in, k_in, v_in, g_in)):
            for row in range(SLOTS):
                pltpu.make_async_remote_copy(
                    src_ref=src.at[(1 - core) * SLOTS + row, :, pl.ds(tip_base, FAR)], dst_ref=far_out.at[t, row],
                    send_sem=far_send, recv_sem=far_recv, device_id=(partner,), device_id_type=MESH).start()

    for copy in tables:
        copy.wait()
    rev = eye_rev(BF16)
    for p in range(2):
        pair_tab = pltpu.einshape("abc->bac", r_buf[p])
        for hh in range(PAIR):
            for blk in range(SEQ // HEAD):
                part = pair_tab[hh, SEQ - HEAD * (blk + 1):SEQ - HEAD * blk]
                flipped = dot(rev, part).astype(BF16)
                rev_s[2 * p + hh, HEAD * blk:HEAD * (blk + 1), :] = flipped
                rt_s[2 * p + hh, :, HEAD * blk:HEAD * (blk + 1)] = flipped.T
    dr_acc[...] = jnp.zeros_like(dr_acc)

    acts = (dk_out, dv_out, o_out, dq_out)

    def send_out(sub, which, late=False):
        place = (core * SLOTS + sub % SLOTS, slice(None), 2 * col + sub // SLOTS)
        for t in which:
            pltpu.make_async_copy(buf.at[t, sub, my_rows], acts[t].at[place], out_recv).start()
        for peer in peers(late):
            peer_rows = pl.ds(pl.multiple_of((peer % PLANE) * ROWS, ROWS), ROWS)
            to_tip = (peer // 2 == 7 * z) & jnp.logical_not(tip)
            for t in which:
                @pl.when(jnp.logical_not(to_tip & (lower if t >= 2 else upper)))
                def _():
                    pltpu.make_async_remote_copy(
                        src_ref=buf.at[t, sub, peer_rows], dst_ref=acts[t].at[place],
                        send_sem=out_send, recv_sem=out_recv, device_id=(peer,), device_id_type=MESH).start()

    def send_up(sub):
        wait_for(buf.at[0:2, sub], in_recv.at[0, sub])
        for j in range(2):
            pltpu.make_async_remote_copy(src_ref=buf.at[j, sub], dst_ref=rbuf.at[j, sub], send_sem=up_send.at[sub % 4], recv_sem=up_recv.at[sub],
                                         device_id=(across,), device_id_type=MESH).start()

    def unpack(ref, j, sub):
        return pltpu.einshape("abc->bac", ref[j, sub])

    def load_rows(q_ref, q_j, g_ref, g_j, sub, start, turned):
        rows = slice(start, start + HALF)
        p = sub // SLOTS
        q2 = unpack(q_ref, q_j, sub)
        u = u_buf[2 * col + p].astype(F32)
        w = w_buf[2 * col + p].astype(F32)
        for hh in range(PAIR):
            q32 = q2[hh].astype(F32)
            a = (q32 + u[hh:hh + 1]).astype(BF16)
            c = (q32 + w[hh:hh + 1]).astype(BF16)
            a_s[hh, rows, :] = a
            c_s[hh, rows, :] = c
            at_s[hh, :, rows] = a.T
            if turned:
                ct_s[hh, :, rows] = flip8(c.astype(F32)).astype(BF16).T
        g2 = unpack(g_ref, g_j, sub)
        g_s[:, rows, :] = g2
        for hh in range(PAIR):
            gt_s[hh, :, rows] = g2[hh].T

    def load_keys(k_ref, k_j, v_ref, v_j, sub, start):
        rows = slice(start, start + HALF)
        k2 = unpack(k_ref, k_j, sub)
        v2 = unpack(v_ref, v_j, sub)
        k_s[:, rows, :] = k2
        v_s[:, rows, :] = v2
        for hh in range(PAIR):
            kt_s[hh, :, rows] = k2[hh].T
            vt_s[hh, :, rows] = v2[hh].T

    def row_block(hh, head, start, i0, lo, fresh, stats):
        width = i0 + QB
        rows = slice(start, start + QB)
        s_ref[:, :width] = dot(a_s[hh, rows, :], kt_s[hh, :, :width])
        e_ref[:, :width] = dot(c_s[hh, rows, :], rt_s[head, :, SEQ - width:])
        dp_ref[:, :width] = dot(g_s[hh, rows, :], vt_s[hh, :, :width])
        for r0 in range(0, QB, 16):
            group = slice(r0, r0 + 16)
            rel = pltpu.roll(e_ref[group, :width], i0 + 1 + r0, 1, stride=1, stride_axis=0)
            s = s_ref[group, :width] + rel
            ahead = lax.broadcasted_iota(jnp.int32, (16, width), 1) - lax.broadcasted_iota(jnp.int32, (16, width), 0)
            s = jnp.where(ahead <= i0 + r0, s, -jnp.inf)
            top = jnp.max(s, axis=1, keepdims=True)
            p = jnp.exp2((s - top) * (scale * LOG2E))
            total = jnp.sum(p, axis=1, keepdims=True)
            p = p * (1.0 / total)
            pb_ref[group, :width] = p.astype(BF16)
            dp = dp_ref[group, :width]
            row_dot = jnp.sum(p * dp, axis=1, keepdims=True)
            ds = (p * (dp - row_dot) * scale).astype(BF16)
            ds_ref[group, :width] = ds
            flipped = flip8(ds.astype(F32))
            half = [pltpu.roll(flipped[8 * j:8 * j + 8], QB - 8 - r0 - 8 * j, 1, stride=1, stride_axis=0) for j in range(2)]
            dd_ref[group, :width] = jnp.concatenate(half, axis=0).astype(BF16)
            if stats:
                lane = lax.broadcasted_iota(jnp.int32, (16, HEAD), 1)
                st_ref[group, :] = jnp.where(lane == 0, top * (scale * LOG2E) + jnp.log2(total), row_dot)
        pb = pb_ref[:, :width]
        ds = ds_ref[:, :width]
        dd = dd_ref[:, :width]
        stage[0, hh, rows, :] = dot(pb, v_s[hh, :width, :]).astype(BF16)
        dqc = dot(ds, k_s[hh, :width, :])
        dqr = flip8(dot(dd, rev_s[head, SEQ - width:, :]))
        stage[1, hh, rows, :] = (dqc + dqr).astype(BF16)
        dr_acc[head, 1, HEAD:HEAD + 1, HALF - HEAD:] += jnp.sum(dqc, axis=0, keepdims=True)
        dr_acc[head, 1, HEAD + 1:HEAD + 2, HALF - HEAD:] += jnp.sum(dqr, axis=0, keepdims=True)
        dk_new = dot(at_s[hh, :, rows], ds_ref[:, lo:width])
        dv_new = dot(gt_s[hh, :, rows], pb_ref[:, lo:width])
        if fresh:
            dkt[hh] = dk_new
            dvt[hh] = dv_new
        else:
            dkt[hh, :, :width - lo] += dk_new
            dvt[hh, :, :width - lo] += dv_new
        dr_new = dot(ct_s[hh, :, rows], dd)
        if width > HALF:
            dr_acc[head, 0, :HEAD, SEQ - width:] += dr_new[:, :width - HALF]
            dr_acc[head, 1, :HEAD, :] += dr_new[:, width - HALF:]
        else:
            dr_acc[head, 1, :HEAD, HALF - width:] += dr_new

    def col_block(hh, head, sub, i0):
        rows = slice(i0, i0 + QB)
        first = WIN - i0
        s_ref[:, :HALF] = dot(a_s[hh, rows, :], kt_s[hh, :, :HALF])
        e_ref[:, :WIN] = dot(c_s[hh, rows, :], rt_s[head, :, first:first + WIN])
        dp_ref[:, :HALF] = dot(g_s[hh, rows, :], vt_s[hh, :, :HALF])
        st_ref[:, :8] = st_rx[sub, hh, :, i0 - HALF:i0 - HALF + QB].T
        for r0 in range(0, QB, 16):
            group = slice(r0, r0 + 16)
            rel = pltpu.roll(e_ref[group, :WIN], HALF + 1 + r0, 1, stride=1, stride_axis=0)[:, :HALF]
            log_sum = st_ref[group, 0:1]
            row_dot = st_ref[group, 1:2]
            p = jnp.exp2((s_ref[group, :HALF] + rel) * (scale * LOG2E) - log_sum)
            pb_ref[group, :HALF] = p.astype(BF16)
            ds_ref[group, :HALF] = (p * (dp_ref[group, :HALF] - row_dot) * scale).astype(BF16)
        dkt[hh] += dot(at_s[hh, :, rows], ds_ref[:, :HALF])
        dvt[hh] += dot(gt_s[hh, :, rows], pb_ref[:, :HALF])

    def store_rows(sub):
        for t in range(2):
            buf[2 + t, sub] = pltpu.einshape("abc->bac", stage[t])

    def store_keys(sub):
        for hh in range(PAIR):
            stage[2, hh] = dkt[hh].astype(BF16).T
            stage[3, hh] = dvt[hh].astype(BF16).T
        for t in range(2):
            buf[t, sub] = pltpu.einshape("abc->bac", stage[2 + t])

    def wait_up(sub):
        wait_for(rbuf.at[:, sub], up_recv.at[sub])
        wait_for(rbuf.at[:, sub], up_send.at[sub % 4])

    def wait_in(sub):
        wait_for(buf.at[2:4, sub], in_recv.at[1, sub])

    def lower_rows(sub):
        wait_in(sub)
        load_rows(buf, 2, buf, 3, sub, 0, True)

    def lower_own(sub):
        load_keys(buf, 0, buf, 1, sub, 0)

        def own(hh, carry):
            head = 2 * (sub // SLOTS) + hh
            row_block(hh, head, QB, QB, 0, True, False)
            row_block(hh, head, 0, 0, 0, False, False)
            return carry

        lax.fori_loop(0, PAIR, own, 0)
        store_rows(sub)

    def lower_theirs(sub):
        wait_up(sub)
        load_rows(rbuf, 0, rbuf, 1, sub, HALF, False)
        wait_for(st_rx.at[sub], st_recv.at[sub % 4])

        def theirs(hh, carry):
            head = 2 * (sub // SLOTS) + hh
            col_block(hh, head, sub, HALF)
            col_block(hh, head, sub, HALF + QB)
            return carry

        lax.fori_loop(0, PAIR, theirs, 0)
        store_keys(sub)

    def upper_own(sub):
        wait_in(sub)
        wait_up(sub)
        load_rows(buf, 0, buf, 1, sub, 0, True)
        load_keys(rbuf, 0, rbuf, 1, sub, 0)
        load_keys(buf, 2, buf, 3, sub, HALF)

        def own(hh, carry):
            head = 2 * (sub // SLOTS) + hh
            for blk in (1, 0):
                row_block(hh, head, QB * blk, HALF + QB * blk, HALF, blk == 1, True)
                st_tx[sub, hh, :, QB * blk:QB * (blk + 1)] = st_ref[...].T[:8]
            pltpu.make_async_remote_copy(src_ref=st_tx.at[sub, hh], dst_ref=st_rx.at[sub, hh], send_sem=st_send, recv_sem=st_recv.at[sub % 4],
                                         device_id=(across,), device_id_type=MESH).start()

            @pl.when(jnp.logical_not(tip))
            def _():
                pltpu.make_async_remote_copy(src_ref=st_tx.at[sub, hh, :, HALF - TIP:], dst_ref=tip_st.at[col, sub, hh], send_sem=ts_send,
                                             recv_sem=ts_recv, device_id=(N_DEV - 2 + core,), device_id_type=MESH).start()
            return carry

        lax.fori_loop(0, PAIR, own, 0)
        store_rows(sub)
        store_keys(sub)

    side = 1 - core
    parts = (dr0_out, dr1_out, dr2_out, dr3_out, dr4_out, dr5_out)

    def swap_start(p):
        for n in range(2):
            pltpu.make_async_remote_copy(src_ref=dr_acc.at[2 * p + n, side], dst_ref=dr_rx.at[p, n], send_sem=x_send, recv_sem=x_recv.at[p],
                                         device_id=(partner,), device_id_type=MESH).start()

    def swap_add(p):
        wait_for(dr_rx.at[p], x_recv.at[p])
        for n in range(2):
            dr_rx[p, n] = dr_rx[p, n] + dr_acc[2 * p + n, core]

    def cross_start(p):
        pltpu.make_async_remote_copy(src_ref=dr_rx.at[p, 1 - z], dst_ref=dr_rz.at[p], send_sem=z_send, recv_sem=z_recv.at[p],
                                     device_id=(across,), device_id_type=MESH).start()

    def head_of(p, bits):
        other = chip ^ bits
        return 4 * (other % 4) + 2 * p + other // 4

    def block(p, m, bits):
        if bits == 0:
            return dr_fin.at[p, PART * m:PART * (m + 1)]
        return parts[m].at[side, :, head_of(p, bits)]

    def forward(p, m, bits):
        pltpu.make_async_remote_copy(src_ref=block(p, m, bits), dst_ref=parts[m].at[side, :, head_of(p, bits)], send_sem=fw_send,
                                     recv_sem=fw_recv, device_id=(partner,), device_id_type=MESH).start()

    def blocks(count):
        return parts[0].at[:, :, :N_PART // 2 * count]

    def pass_on(p, bits, hop, device):
        for m in range(N_PART):
            pltpu.make_async_remote_copy(
                src_ref=block(p, m, bits), dst_ref=parts[m].at[side, :, head_of(p, bits)], send_sem=ring_send,
                recv_sem=ring_recv.at[p, hop], device_id=(device,), device_id_type=MESH).start()

    def hand_over(p, bits):
        for m in range(N_PART):
            forward(p, m, bits)

    along_x, along_y = me ^ 2, me ^ 4

    def hop_start(p, hop):
        if hop == 0:
            for device in (along_x, along_y, across):
                pass_on(p, 0, 0, device)
        if hop == 1:
            @pl.when(even & loaded)
            def _():
                pass_on(p, 1, 1, along_y)

            @pl.when(jnp.logical_not(even) & loaded)
            def _():
                pass_on(p, 2, 1, along_x)

            pass_on(p, 1, 1, across)
            pass_on(p, 2, 1, across)
        if hop == 2:
            @pl.when(even & loaded)
            def _():
                pass_on(p, 5, 2, along_y)

            @pl.when(jnp.logical_not(even) & loaded)
            def _():
                pass_on(p, 6, 2, along_x)

            @pl.when(even)
            def _():
                pass_on(p, 3, 2, across)
        if hop == 3:
            @pl.when(even)
            def _():
                pass_on(p, 7, 3, across)

    def hop_wait(p, hop):
        if hop == 0:
            wait_for(blocks(3), ring_recv.at[p, 0])
            for bits in (1, 2, 4):
                hand_over(p, bits)
        if hop == 1:
            @pl.when(even)
            def _():
                wait_for(blocks(3), ring_recv.at[p, 1])
                hand_over(p, 3)

            @pl.when(jnp.logical_not(even))
            def _():
                wait_for(blocks(2), ring_recv.at[p, 1])
            for bits in (5, 6):
                hand_over(p, bits)
        if hop == 2:
            wait_for(blocks(1), ring_recv.at[p, 2])
            hand_over(p, 7)
        if hop == 3:
            @pl.when(jnp.logical_not(even))
            def _():
                wait_for(blocks(1), ring_recv.at[p, 3])
                hand_over(p, 3)

    def sent_wait():
        @pl.when(even & loaded)
        def _():
            wait_for(buf.at[:3, :, :FIN * 18 // 24], ring_send)

        @pl.when(even != loaded)
        def _():
            wait_for(buf.at[:3, :7, :FIN * 14 // 21], ring_send)

        @pl.when(jnp.logical_not(even | loaded))
        def _():
            wait_for(buf.at[:2, :6, :FIN * 10 // 12], ring_send)

    def cross_finish(p):
        wait_for(dr_rz.at[p], z_recv.at[p])
        total = dr_rx[p, z] + dr_rz[p]
        rev32 = eye_rev(F32)
        for m in range(HALF // HEAD):
            part = total[:HEAD, HALF - HEAD * (m + 1):HALF - HEAD * m]
            turned = lax.dot_general(rev32, part, (((1,), (1,)), ((), ())), precision=lax.Precision.HIGHEST, preferred_element_type=F32)
            dr_fin[p, HEAD * m:HEAD * (m + 1)] = turned.reshape(HEAD, 1, HEAD)
        dr_fin[p, HALF] = total[HEAD:HEAD + 1, HALF - HEAD:]
        dr_fin[p, HALF + 1] = total[HEAD + 1:HEAD + 2, HALF - HEAD:]
        dr_fin[p, HALF + 2:] = jnp.zeros((FIN - HALF - 2, 1, HEAD), F32)
        hop_start(p, 0)
        for m in range(N_PART):
            pltpu.make_async_copy(block(p, m, 0), parts[m].at[side, :, head_of(p, 0)], own_sem).start()
        hand_over(p, 0)

    def tip_load(unit):
        slot, row, far = unit % 2, unit // FAR, unit % FAR
        pair = far + tip_base
        for t, src in enumerate((q_in, k_in, v_in, g_in)):
            pltpu.make_async_copy(src.at[core * SLOTS + row, :, pair], r_buf.at[slot, pl.ds(TIP * t + ROWS * core, ROWS)], tip_sem.at[slot]).start()
            pltpu.make_async_copy(far_out.at[t, row, :, far], r_buf.at[slot, pl.ds(TIP * t + ROWS * (1 - core), ROWS)], tip_sem.at[slot]).start()
        pltpu.make_async_copy(r_in.at[:TIP, pair], r_buf.at[slot, 4 * TIP:5 * TIP], tip_sem.at[slot]).start()

    def tip_done(slot):
        wait_for(r_buf.at[slot, :TIP], tip_near.at[slot])
        wait_for(r_buf.at[slot, :TIP], tip_send.at[slot])

    def tip_group(hh, r0):
        group = slice(TIP * hh + r0, TIP * hh + r0 + 16)
        rel = pltpu.roll(e_ref[group, :TIP], 1 + r0, 1, stride=1, stride_axis=0)
        ahead = lax.broadcasted_iota(jnp.int32, (16, TIP), 1) - lax.broadcasted_iota(jnp.int32, (16, TIP), 0)
        return group, s_ref[group, :TIP] + rel, ahead <= r0

    def tip_rows(hh):
        for r0 in range(0, TIP, 16):
            group, s, seen = tip_group(hh, r0)
            s = jnp.where(seen, s, -jnp.inf)
            top = jnp.max(s, axis=1, keepdims=True)
            p = jnp.exp2((s - top) * (scale * LOG2E))
            p = p * (1.0 / jnp.sum(p, axis=1, keepdims=True))
            pb_ref[group, :TIP] = p.astype(BF16)
            dp = dp_ref[group, :TIP]
            row_dot = jnp.sum(p * dp, axis=1, keepdims=True)
            ds = (p * (dp - row_dot) * scale).astype(BF16)
            ds_ref[group, :TIP] = ds
            flipped = flip8(ds.astype(F32))
            half = [pltpu.roll(flipped[8 * j:8 * j + 8], TIP - 8 - r0 - 8 * j, 1, stride=1, stride_axis=0) for j in range(2)]
            dd_ref[group, :TIP] = jnp.concatenate(half, axis=0).astype(BF16)
        rows = slice(TIP * hh, TIP * (hh + 1))
        stage[0, hh, :TIP, :] = dot(pb_ref[rows, :TIP], v_s[hh, :TIP, :]).astype(BF16)
        dqc = dot(ds_ref[rows, :TIP], k_s[hh, :TIP, :])
        dqr = flip8(dot(dd_ref[rows, :TIP], c_s[hh, :TIP, :]))
        stage[1, hh, :TIP, :] = (dqc + dqr).astype(BF16)

    def tip_keys(hh, stats):
        rows = slice(TIP * hh, TIP * (hh + 1))
        st_ref[rows, :8] = stats.T
        for r0 in range(0, TIP, 16):
            group, s, seen = tip_group(hh, r0)
            p = jnp.where(seen, jnp.exp2(s * (scale * LOG2E) - st_ref[group, 0:1]), 0.0)
            pb_ref[group, :TIP] = p.astype(BF16)
            ds_ref[group, :TIP] = (p * (dp_ref[group, :TIP] - st_ref[group, 1:2]) * scale).astype(BF16)
        over_rows = (((0,), (0,)), ((), ()))
        stage[0, hh, :TIP, :] = lax.dot_general(ds_ref[rows, :TIP], a_s[hh, :TIP, :], over_rows, preferred_element_type=F32).astype(BF16)
        stage[1, hh, :TIP, :] = lax.dot_general(pb_ref[rows, :TIP], g_s[hh, :TIP, :], over_rows, preferred_element_type=F32).astype(BF16)

    def tip_unit(unit, carry):
        slot, row, far = unit % 2, unit // FAR, unit % FAR
        pair = far + tip_base
        wait_for(r_buf.at[slot, :5 * TIP], tip_sem.at[slot])

        @pl.when(unit + 1 < UNITS)
        def _():
            tip_load(unit + 1)

        q2, k2, v2, g2, r2 = [pltpu.einshape("abc->bac", r_buf[slot, TIP * t:TIP * (t + 1)]) for t in range(5)]
        u = u_buf[pair].astype(F32)
        w = w_buf[pair].astype(F32)
        for hh in range(PAIR):
            rows = slice(TIP * hh, TIP * (hh + 1))
            q32 = q2[hh].astype(F32)
            a = (q32 + u[hh:hh + 1]).astype(BF16)
            c = (q32 + w[hh:hh + 1]).astype(BF16)
            falling = dot(eye_rev(BF16), r2[hh]).astype(BF16)
            s_ref[rows, :TIP] = dot(a, k2[hh].T)
            e_ref[rows, :TIP] = dot(c, falling.T)
            dp_ref[rows, :TIP] = dot(g2[hh], v2[hh].T)
            a_s[hh, :TIP, :] = a
            c_s[hh, :TIP, :] = falling
            g_s[hh, :TIP, :] = g2[hh]
            k_s[hh, :TIP, :] = k2[hh]
            v_s[hh, :TIP, :] = v2[hh]

        @pl.when(lower)
        def _():
            for hh in range(PAIR):
                tip_rows(hh)

        @pl.when(upper)
        def _():
            for hh in range(PAIR):
                tip_keys(hh, tip_st[far // 2, (far % 2) * SLOTS + row, hh])

        @pl.when(unit >= 2)
        def _():
            tip_done(slot)

        for n in range(2):
            r_buf[slot, (5 + n) * TIP:(6 + n) * TIP] = pltpu.einshape("abc->bac", stage[n, :, :TIP, :])
        place = (core * SLOTS + row, slice(None), pair)

        def give(results):
            for n, dst in enumerate(results):
                pltpu.make_async_copy(r_buf.at[slot, pl.ds((5 + n) * TIP + ROWS * core, ROWS)], dst.at[place], tip_near.at[slot]).start()
                pltpu.make_async_remote_copy(
                    src_ref=r_buf.at[slot, pl.ds((5 + n) * TIP + ROWS * (1 - core), ROWS)], dst_ref=dst.at[place],
                    send_sem=tip_send.at[slot], recv_sem=out_recv, device_id=(partner,), device_id_type=MESH).start()

        @pl.when(lower)
        def _():
            give((o_out, dq_out))

        @pl.when(upper)
        def _():
            give((dk_out, dv_out))
        return carry

    def tips(third):
        @pl.when(tip)
        def _():
            if third == 0:
                wait_for(far_out, far_recv)

                @pl.when(upper)
                def _():
                    wait_for(tip_st, ts_recv)
                tip_load(0)
            lax.fori_loop(UNITS // 3 * third, UNITS // 3 * (third + 1), tip_unit, 0)
            if third == 2:
                tip_done(0)
                tip_done(1)

    send_up(0)

    def sub_body(sub, carry):
        @pl.when(sub < SUBS - 1)
        def _():
            send_up(sub + 1)

        @pl.when(sub == SLOTS)
        def _():
            swap_start(0)

        @pl.when(sub == SUBS - 1)
        def _():
            swap_add(0)
            cross_start(0)

        @pl.when(sub == SUBS)
        def _():
            swap_start(1)
            swap_add(1)
            cross_start(1)
            cross_finish(0)

        @pl.when(lower & (sub < SUBS))
        def _():
            lower_rows(sub)

        @pl.when(lower & (sub > 0))
        def _():
            lower_theirs(sub - 1)

        @pl.when(lower & (sub < SUBS))
        def _():
            lower_own(sub)

        @pl.when(upper & (sub < SUBS))
        def _():
            upper_own(sub)

        @pl.when(sub <= EARLY)
        def _():
            send_out(sub, (2, 3))

        @pl.when((sub > 0) & (sub <= EARLY))
        def _():
            send_out(sub - 1, (0, 1))
        return carry

    lax.fori_loop(0, SUBS + 1, sub_body, 0)

    cross_finish(1)
    send_out(EARLY, (0, 1))
    for p in range(2):
        hop_wait(p, 0)
        hop_start(p, 1)
    for p in range(2):
        send_out(EARLY + 1 + p, range(4))
        tips(p)
        hop_wait(p, 1)
        hop_start(p, 2)

    def send_late(sub, carry):
        send_out(sub, range(4), True)
        return carry

    lax.fori_loop(EARLY + 3, SUBS, send_late, 0)
    tips(2)
    for p in range(2):
        hop_wait(p, 2)
        hop_start(p, 3)
    for p in range(2):
        hop_wait(p, 3)

    wait_for(buf.at[:, :, :HALF - ROWS], in_send)

    @pl.when(tip)
    def _():
        wait_for(buf.at[:, :, :HALF - 3 * ROWS // 2], out_recv)
        wait_for(buf.at[:, :, :HALF - ROWS], out_send)
        wait_for(far_out, far_send)

    @pl.when(jnp.logical_not(tip))
    def _():
        wait_for(buf, out_recv)
        wait_for(buf.at[:, :, :HALF - 2 * ROWS], out_send)

    @pl.when(upper & jnp.logical_not(tip))
    def _():
        wait_for(st_tx.at[:2], ts_send)

    @pl.when(upper)
    def _():
        wait_for(st_tx, st_send)

    wait_for(dr_rx, x_send)
    wait_for(dr_rz, z_send)
    wait_for(blocks(2), own_sem)
    sent_wait()
    for sem in (fw_send, fw_recv):
        wait_for(buf.at[:3, :, :FIN * 16 // 24], sem)


def writer(*refs):
    ins, (o, dq, dk, dv, dr, du, dw, sem) = refs[:4 + N_PART], refs[4 + N_PART:]
    pairs = list(zip(ins[:4], (o, dq, dk, dv)))
    for m, part in enumerate(ins[4:]):
        rows = min(PART, HALF - PART * m)
        for side in range(2):
            start = HALF * side + PART * m
            pairs.append((part.at[side, :rows], dr.at[start:start + rows]))
    last = HALF - PART * (N_PART - 1)
    pairs += [(ins[-1].at[0, last], du), (ins[-1].at[0, last + 1], dw)]
    copies = [pltpu.make_async_copy(src, dst, sem.at[j]) for j, (src, dst) in enumerate(pairs)]
    for copy in copies:
        copy.start()
    for copy in copies:
        copy.wait()


def solution(mesh):
    seq_spec = P(None, "cp", None, None)

    def local(query, key_in, value, bias_u, bias_w, rel_k, d_out):
        n_batch, rows, n_heads, head_dim = query.shape
        pairs = (n_batch, rows, N_PAIR, PAIR, head_dim)
        vm = pltpu.VMEM
        dma = pltpu.SemaphoreType.DMA
        whole = pl.BlockSpec(memory_space=pl.ANY)
        act = jax.ShapeDtypeStruct(pairs, BF16)
        vec = jax.ShapeDtypeStruct((n_heads, 1, head_dim), F32)
        tok = (PAIR, SEQ, HEAD)
        tok_t = (PAIR, HEAD, SEQ)
        acc = (HEAD + 8, HALF)
        outs = pl.pallas_call(
            kernel,
            name="rel_attn",
            out_shape=(act, act, act, act,
                       *[jax.ShapeDtypeStruct((2, PART, n_heads, 1, head_dim), F32)] * N_PART,
                       jax.ShapeDtypeStruct((4, SLOTS, ROWS, FAR, PAIR, HEAD), BF16)),
            in_specs=[pl.BlockSpec(memory_space=pltpu.HBM)] * 7,
            out_specs=[whole] * (5 + N_PART),
            scratch_shapes=[
                vm((4, SUBS, HALF, PAIR, HEAD), BF16), vm((2, SUBS, HALF, PAIR, HEAD), BF16),
                vm((2, SEQ, PAIR, HEAD), BF16), vm((N_PAIR, PAIR, HEAD), BF16), vm((N_PAIR, PAIR, HEAD), BF16),
                vm((SUBS, PAIR, 8, HALF), F32), vm((SUBS, PAIR, 8, HALF), F32), vm((3, SUBS, PAIR, 8, TIP), F32), vm((QB, HEAD), F32),
                vm((2, 2) + acc, F32), vm((2,) + acc, F32), vm((2, FIN, 1, HEAD), F32), vm((4, 2) + acc, F32),
                vm((QB, SEQ), F32), vm((QB, SEQ), F32), vm((QB, SEQ), F32),
                vm((QB, SEQ), BF16), vm((QB, SEQ), BF16), vm((QB, SEQ), BF16),
                vm(tok, BF16), vm(tok, BF16), vm(tok, BF16), vm(tok, BF16), vm(tok, BF16),
                vm(tok_t, BF16), vm(tok_t, BF16), vm(tok_t, BF16), vm(tok_t, BF16), vm(tok_t, BF16),
                vm((4, SEQ, HEAD), BF16), vm((4, HEAD, SEQ), BF16),
                vm((PAIR, HEAD, HALF), F32), vm((PAIR, HEAD, HALF), F32), vm((4, PAIR, HALF, HEAD), BF16),
                dma, dma((2, SUBS)), dma, dma, dma, dma((4,)), dma((4,)), dma((SUBS,)), dma, dma((4,)),
                dma, dma((2,)), dma, dma((2,)), dma, dma((2, 4)), dma, dma,
                dma, dma, dma((2,)), dma((2,)), dma((2,)), dma, dma,
            ],
            compiler_params=pltpu.CompilerParams(collective_id=0, has_side_effects=True, vmem_limit_bytes=37 * 1024 * 1024),
        )(*[pltpu.with_memory_space_constraint(x, pltpu.HBM) for x in (
            query.reshape(pairs), key_in.reshape(pairs), value.reshape(pairs), d_out.reshape(pairs),
            rel_k.reshape(SEQ, N_PAIR, PAIR, head_dim), bias_u.reshape(N_PAIR, PAIR, head_dim), bias_w.reshape(N_PAIR, PAIR, head_dim))])
        o, dq, dk, dv, dr, du, dw = pl.pallas_call(
            writer,
            name="writer",
            out_shape=(act, act, act, act, jax.ShapeDtypeStruct((SEQ, n_heads, 1, head_dim), F32), vec, vec),
            in_specs=[whole] * (4 + N_PART),
            out_specs=[whole] * 7,
            scratch_shapes=[dma((6 + 2 * N_PART,))],
            compiler_params=pltpu.CompilerParams(vmem_limit_bytes=1024 * 1024),
        )(*outs[:-1])
        full = query.shape
        return (o.reshape(full), dq.reshape(full), dk.reshape(full), dv.reshape(full),
                du.reshape(bias_u.shape), dw.reshape(bias_w.shape), dr.reshape(rel_k.shape))

    return jax.shard_map(local, mesh=mesh,
                         in_specs=(seq_spec, seq_spec, seq_spec, P(), P(), P(), seq_spec),
                         out_specs=(seq_spec, seq_spec, seq_spec, seq_spec, P(), P(), P()),
                         check_vma=False)
```

```python
import jax
import jax.numpy as jnp
from jax import lax
from jax.experimental import pallas as pl
from jax.experimental.pallas import tpu as pltpu
from jax.sharding import PartitionSpec as P

MESH = pl.DeviceIdType.MESH
BF16, F32 = jnp.bfloat16, jnp.float32
LOG2E = 1.4426950408889634

N_DEV = 16
PLANE = 8
PAIR = 2
N_PAIR = 8
SLOTS = 4
SUBS = 2 * SLOTS
EARLY = 3
ROWS = 64
HALF = PLANE * ROWS
SEQ = 2 * HALF
HEAD = 128
QB = 256
WIN = HALF + QB
N_PART = 6
PART = 86
FIN = N_PART * PART
TIP = 2 * ROWS
FAR = N_PAIR - 2
UNITS = FAR * SLOTS
TURNS = ((1, 3, 2), (3, 1, 2))


def dot(lhs, rhs):
    return jnp.dot(lhs, rhs, preferred_element_type=F32)


def flip8(x):
    rows, cols = x.shape
    idx = 7 - lax.broadcasted_iota(jnp.int32, (rows // 8, 8, cols), 1)
    return jnp.take_along_axis(x.reshape(rows // 8, 8, cols), idx, axis=1).reshape(rows, cols)


def eye_rev(dtype):
    total = lax.broadcasted_iota(jnp.int32, (HEAD, HEAD), 0) + lax.broadcasted_iota(jnp.int32, (HEAD, HEAD), 1)
    return jnp.where(total == HEAD - 1, 1.0, 0.0).astype(dtype)


def kernel(q_in, k_in, v_in, g_in, r_in, u_in, w_in,
           o_out, dq_out, dk_out, dv_out, dr0_out, dr1_out, dr2_out, dr3_out, dr4_out, dr5_out, far_out,
           buf, rbuf, r_buf, u_buf, w_buf, st_tx, st_rx, tip_st, st_ref, dr_rx, dr_rz, dr_fin, dr_acc,
           s_ref, e_ref, dp_ref, pb_ref, ds_ref, dd_ref,
           a_s, c_s, g_s, k_s, v_s, at_s, ct_s, gt_s, kt_s, vt_s, rev_s, rt_s, dkt, dvt, stage,
           in_send, in_recv, out_send, out_recv, own_sem, r_sem, up_send, up_recv, st_send, st_recv,
           x_send, x_recv, z_send, z_recv, ring_send, ring_recv, fw_send, fw_recv,
           far_send, far_recv, tip_sem, tip_near, tip_send, ts_send, ts_recv):
    me = lax.axis_index("cp")
    core = me % 2
    chip = me // 2
    col = chip % 4
    z = chip // 4
    partner = me + 1 - 2 * core
    across = me + PLANE * (1 - 2 * z)
    scale = HEAD ** -0.5

    def wait_for(ref, sem):
        pltpu.make_async_copy(ref, ref, sem).wait()

    y = col // 2
    lower, upper = z == 0, z == 1
    tip = chip == 7 * z
    tip_base = 2 - 2 * z

    tables = [pltpu.make_async_copy(src, dst, r_sem.at[j]) for j, (src, dst) in enumerate(
        ((r_in.at[:, 2 * col], r_buf.at[0]), (r_in.at[:, 2 * col + 1], r_buf.at[1]), (u_in, u_buf), (w_in, w_buf)))]
    for copy in tables:
        copy.start()

    barrier = pltpu.get_barrier_semaphore()

    for peer in [across] + [me ^ step for step in range(PLANE - 1, 0, -1)]:
        pl.semaphore_signal(barrier, inc=1, device_id=(peer,), device_id_type=MESH)
    pl.semaphore_wait(barrier, PLANE)

    my_rows = pl.ds(pl.multiple_of((me % PLANE) * ROWS, ROWS), ROWS)

    even = chip % 2 == z
    loaded = y != z

    def peers(late=False):
        near = core == 0
        if late:
            near = jnp.logical_not(near) & (even | jnp.logical_not(loaded))
        first, second, third = [jnp.where(near, near_turn, far_turn) for near_turn, far_turn in zip(*TURNS)]
        for turn, other in ((first, 0), (third, 0), (first, 1), (third, 1), (second, 0), (second, 1)):
            yield me ^ (2 * turn + other)
        yield partner

    def send_in(ins, sub):
        pair, row = sub // SLOTS, sub % SLOTS
        for first in (0, 2):
            for t in (first, first + 1):
                pltpu.make_async_copy(ins[t].at[core * SLOTS + row, :, 2 * col + pair], buf.at[t, sub, my_rows], in_recv.at[first // 2, sub]).start()
            for peer in peers():
                for t in (first, first + 1):
                    pltpu.make_async_remote_copy(
                        src_ref=ins[t].at[(peer % 2) * SLOTS + row, :, 2 * ((peer // 2) % 4) + pair], dst_ref=buf.at[t, sub, my_rows],
                        send_sem=in_send, recv_sem=in_recv.at[first // 2, sub], device_id=(peer,), device_id_type=MESH).start()

    def send_all(ins):
        def send_sub(sub, carry):
            send_in(ins, sub)
            return carry
        lax.fori_loop(0, SUBS, send_sub, 0)

    @pl.when(lower)
    def _():
        send_all((k_in, v_in, q_in, g_in))

    @pl.when(upper)
    def _():
        send_all((q_in, g_in, k_in, v_in))

    @pl.when(tip)
    def _():
        for t, src in enumerate((q_in, k_in, v_in, g_in)):
            for row in range(SLOTS):
                pltpu.make_async_remote_copy(
                    src_ref=src.at[(1 - core) * SLOTS + row, :, pl.ds(tip_base, FAR)], dst_ref=far_out.at[t, row],
                    send_sem=far_send, recv_sem=far_recv, device_id=(partner,), device_id_type=MESH).start()

    for copy in tables:
        copy.wait()
    rev = eye_rev(BF16)
    for p in range(2):
        pair_tab = pltpu.einshape("abc->bac", r_buf[p])
        for hh in range(PAIR):
            for blk in range(SEQ // HEAD):
                part = pair_tab[hh, SEQ - HEAD * (blk + 1):SEQ - HEAD * blk]
                flipped = dot(rev, part).astype(BF16)
                rev_s[2 * p + hh, HEAD * blk:HEAD * (blk + 1), :] = flipped
                rt_s[2 * p + hh, :, HEAD * blk:HEAD * (blk + 1)] = flipped.T
    dr_acc[...] = jnp.zeros_like(dr_acc)

    acts = (dk_out, dv_out, o_out, dq_out)

    def send_out(sub, which, late=False):
        place = (core * SLOTS + sub % SLOTS, slice(None), 2 * col + sub // SLOTS)
        for t in which:
            pltpu.make_async_copy(buf.at[t, sub, my_rows], acts[t].at[place], out_recv).start()
        for peer in peers(late):
            peer_rows = pl.ds(pl.multiple_of((peer % PLANE) * ROWS, ROWS), ROWS)
            to_tip = (peer // 2 == 7 * z) & jnp.logical_not(tip)
            for t in which:
                @pl.when(jnp.logical_not(to_tip & (lower if t >= 2 else upper)))
                def _():
                    pltpu.make_async_remote_copy(
                        src_ref=buf.at[t, sub, peer_rows], dst_ref=acts[t].at[place],
                        send_sem=out_send, recv_sem=out_recv, device_id=(peer,), device_id_type=MESH).start()

    def send_up(sub):
        wait_for(buf.at[0:2, sub], in_recv.at[0, sub])
        for j in range(2):
            pltpu.make_async_remote_copy(src_ref=buf.at[j, sub], dst_ref=rbuf.at[j, sub], send_sem=up_send.at[sub % 4], recv_sem=up_recv.at[sub],
                                         device_id=(across,), device_id_type=MESH).start()

    def unpack(ref, j, sub):
        return pltpu.einshape("abc->bac", ref[j, sub])

    def load_rows(q_ref, q_j, g_ref, g_j, sub, start, turned):
        rows = slice(start, start + HALF)
        p = sub // SLOTS
        q2 = unpack(q_ref, q_j, sub)
        u = u_buf[2 * col + p].astype(F32)
        w = w_buf[2 * col + p].astype(F32)
        for hh in range(PAIR):
            q32 = q2[hh].astype(F32)
            a = (q32 + u[hh:hh + 1]).astype(BF16)
            c = (q32 + w[hh:hh + 1]).astype(BF16)
            a_s[hh, rows, :] = a
            c_s[hh, rows, :] = c
            at_s[hh, :, rows] = a.T
            if turned:
                ct_s[hh, :, rows] = flip8(c.astype(F32)).astype(BF16).T
        g2 = unpack(g_ref, g_j, sub)
        g_s[:, rows, :] = g2
        for hh in range(PAIR):
            gt_s[hh, :, rows] = g2[hh].T

    def load_keys(k_ref, k_j, v_ref, v_j, sub, start):
        rows = slice(start, start + HALF)
        k2 = unpack(k_ref, k_j, sub)
        v2 = unpack(v_ref, v_j, sub)
        k_s[:, rows, :] = k2
        v_s[:, rows, :] = v2
        for hh in range(PAIR):
            kt_s[hh, :, rows] = k2[hh].T
            vt_s[hh, :, rows] = v2[hh].T

    def row_block(hh, head, start, i0, lo, fresh, stats):
        width = i0 + QB
        rows = slice(start, start + QB)
        s_ref[:, :width] = dot(a_s[hh, rows, :], kt_s[hh, :, :width])
        e_ref[:, :width] = dot(c_s[hh, rows, :], rt_s[head, :, SEQ - width:])
        dp_ref[:, :width] = dot(g_s[hh, rows, :], vt_s[hh, :, :width])
        for r0 in range(0, QB, 16):
            group = slice(r0, r0 + 16)
            rel = pltpu.roll(e_ref[group, :width], i0 + 1 + r0, 1, stride=1, stride_axis=0)
            s = s_ref[group, :width] + rel
            ahead = lax.broadcasted_iota(jnp.int32, (16, width), 1) - lax.broadcasted_iota(jnp.int32, (16, width), 0)
            s = jnp.where(ahead <= i0 + r0, s, -jnp.inf)
            top = jnp.max(s, axis=1, keepdims=True)
            p = jnp.exp2((s - top) * (scale * LOG2E))
            total = jnp.sum(p, axis=1, keepdims=True)
            p = p * (1.0 / total)
            pb_ref[group, :width] = p.astype(BF16)
            dp = dp_ref[group, :width]
            row_dot = jnp.sum(p * dp, axis=1, keepdims=True)
            ds = (p * (dp - row_dot) * scale).astype(BF16)
            ds_ref[group, :width] = ds
            flipped = flip8(ds.astype(F32))
            half = [pltpu.roll(flipped[8 * j:8 * j + 8], QB - 8 - r0 - 8 * j, 1, stride=1, stride_axis=0) for j in range(2)]
            dd_ref[group, :width] = jnp.concatenate(half, axis=0).astype(BF16)
            if stats:
                lane = lax.broadcasted_iota(jnp.int32, (16, HEAD), 1)
                st_ref[group, :] = jnp.where(lane == 0, top * (scale * LOG2E) + jnp.log2(total), row_dot)
        pb = pb_ref[:, :width]
        ds = ds_ref[:, :width]
        dd = dd_ref[:, :width]
        stage[0, hh, rows, :] = dot(pb, v_s[hh, :width, :]).astype(BF16)
        dqc = dot(ds, k_s[hh, :width, :])
        dqr = flip8(dot(dd, rev_s[head, SEQ - width:, :]))
        stage[1, hh, rows, :] = (dqc + dqr).astype(BF16)
        dr_acc[head, 1, HEAD:HEAD + 1, HALF - HEAD:] += jnp.sum(dqc, axis=0, keepdims=True)
        dr_acc[head, 1, HEAD + 1:HEAD + 2, HALF - HEAD:] += jnp.sum(dqr, axis=0, keepdims=True)
        dk_new = dot(at_s[hh, :, rows], ds_ref[:, lo:width])
        dv_new = dot(gt_s[hh, :, rows], pb_ref[:, lo:width])
        if fresh:
            dkt[hh] = dk_new
            dvt[hh] = dv_new
        else:
            dkt[hh, :, :width - lo] += dk_new
            dvt[hh, :, :width - lo] += dv_new
        dr_new = dot(ct_s[hh, :, rows], dd)
        if width > HALF:
            dr_acc[head, 0, :HEAD, SEQ - width:] += dr_new[:, :width - HALF]
            dr_acc[head, 1, :HEAD, :] += dr_new[:, width - HALF:]
        else:
            dr_acc[head, 1, :HEAD, HALF - width:] += dr_new

    def col_block(hh, head, sub, i0):
        rows = slice(i0, i0 + QB)
        first = WIN - i0
        s_ref[:, :HALF] = dot(a_s[hh, rows, :], kt_s[hh, :, :HALF])
        e_ref[:, :WIN] = dot(c_s[hh, rows, :], rt_s[head, :, first:first + WIN])
        dp_ref[:, :HALF] = dot(g_s[hh, rows, :], vt_s[hh, :, :HALF])
        st_ref[:, :8] = st_rx[sub, hh, :, i0 - HALF:i0 - HALF + QB].T
        for r0 in range(0, QB, 16):
            group = slice(r0, r0 + 16)
            rel = pltpu.roll(e_ref[group, :WIN], HALF + 1 + r0, 1, stride=1, stride_axis=0)[:, :HALF]
            log_sum = st_ref[group, 0:1]
            row_dot = st_ref[group, 1:2]
            p = jnp.exp2((s_ref[group, :HALF] + rel) * (scale * LOG2E) - log_sum)
            pb_ref[group, :HALF] = p.astype(BF16)
            ds_ref[group, :HALF] = (p * (dp_ref[group, :HALF] - row_dot) * scale).astype(BF16)
        dkt[hh] += dot(at_s[hh, :, rows], ds_ref[:, :HALF])
        dvt[hh] += dot(gt_s[hh, :, rows], pb_ref[:, :HALF])

    def store_rows(sub):
        for t in range(2):
            buf[2 + t, sub] = pltpu.einshape("abc->bac", stage[t])

    def store_keys(sub):
        for hh in range(PAIR):
            stage[2, hh] = dkt[hh].astype(BF16).T
            stage[3, hh] = dvt[hh].astype(BF16).T
        for t in range(2):
            buf[t, sub] = pltpu.einshape("abc->bac", stage[2 + t])

    def wait_up(sub):
        wait_for(rbuf.at[:, sub], up_recv.at[sub])
        wait_for(rbuf.at[:, sub], up_send.at[sub % 4])

    def wait_in(sub):
        wait_for(buf.at[2:4, sub], in_recv.at[1, sub])

    def lower_rows(sub):
        wait_in(sub)
        load_rows(buf, 2, buf, 3, sub, 0, True)

    def lower_own(sub):
        load_keys(buf, 0, buf, 1, sub, 0)

        def own(hh, carry):
            head = 2 * (sub // SLOTS) + hh
            row_block(hh, head, QB, QB, 0, True, False)
            row_block(hh, head, 0, 0, 0, False, False)
            return carry

        lax.fori_loop(0, PAIR, own, 0)
        store_rows(sub)

    def lower_theirs(sub):
        wait_up(sub)
        load_rows(rbuf, 0, rbuf, 1, sub, HALF, False)
        wait_for(st_rx.at[sub], st_recv.at[sub % 4])

        def theirs(hh, carry):
            head = 2 * (sub // SLOTS) + hh
            col_block(hh, head, sub, HALF)
            col_block(hh, head, sub, HALF + QB)
            return carry

        lax.fori_loop(0, PAIR, theirs, 0)
        store_keys(sub)

    def upper_own(sub):
        wait_in(sub)
        wait_up(sub)
        load_rows(buf, 0, buf, 1, sub, 0, True)
        load_keys(rbuf, 0, rbuf, 1, sub, 0)
        load_keys(buf, 2, buf, 3, sub, HALF)

        def own(hh, carry):
            head = 2 * (sub // SLOTS) + hh
            for blk in (1, 0):
                row_block(hh, head, QB * blk, HALF + QB * blk, HALF, blk == 1, True)
                st_tx[sub, hh, :, QB * blk:QB * (blk + 1)] = st_ref[...].T[:8]
            pltpu.make_async_remote_copy(src_ref=st_tx.at[sub, hh], dst_ref=st_rx.at[sub, hh], send_sem=st_send, recv_sem=st_recv.at[sub % 4],
                                         device_id=(across,), device_id_type=MESH).start()

            @pl.when(jnp.logical_not(tip))
            def _():
                pltpu.make_async_remote_copy(src_ref=st_tx.at[sub, hh, :, HALF - TIP:], dst_ref=tip_st.at[col, sub, hh], send_sem=ts_send,
                                             recv_sem=ts_recv, device_id=(N_DEV - 2 + core,), device_id_type=MESH).start()
            return carry

        lax.fori_loop(0, PAIR, own, 0)
        store_rows(sub)
        store_keys(sub)

    side = 1 - core
    parts = (dr0_out, dr1_out, dr2_out, dr3_out, dr4_out, dr5_out)

    def swap_start(p):
        for n in range(2):
            pltpu.make_async_remote_copy(src_ref=dr_acc.at[2 * p + n, side], dst_ref=dr_rx.at[p, n], send_sem=x_send, recv_sem=x_recv.at[p],
                                         device_id=(partner,), device_id_type=MESH).start()

    def swap_add(p):
        wait_for(dr_rx.at[p], x_recv.at[p])
        for n in range(2):
            dr_rx[p, n] = dr_rx[p, n] + dr_acc[2 * p + n, core]

    def cross_start(p):
        pltpu.make_async_remote_copy(src_ref=dr_rx.at[p, 1 - z], dst_ref=dr_rz.at[p], send_sem=z_send, recv_sem=z_recv.at[p],
                                     device_id=(across,), device_id_type=MESH).start()

    def head_of(p, bits):
        other = chip ^ bits
        return 4 * (other % 4) + 2 * p + other // 4

    def block(p, m, bits):
        if bits == 0:
            return dr_fin.at[p, PART * m:PART * (m + 1)]
        return parts[m].at[side, :, head_of(p, bits)]

    def forward(p, m, bits):
        pltpu.make_async_remote_copy(src_ref=block(p, m, bits), dst_ref=parts[m].at[side, :, head_of(p, bits)], send_sem=fw_send,
                                     recv_sem=fw_recv, device_id=(partner,), device_id_type=MESH).start()

    def blocks(count):
        return parts[0].at[:, :, :N_PART // 2 * count]

    def pass_on(p, bits, hop, device):
        for m in range(N_PART):
            pltpu.make_async_remote_copy(
                src_ref=block(p, m, bits), dst_ref=parts[m].at[side, :, head_of(p, bits)], send_sem=ring_send,
                recv_sem=ring_recv.at[p, hop], device_id=(device,), device_id_type=MESH).start()

    def hand_over(p, bits):
        for m in range(N_PART):
            forward(p, m, bits)

    along_x, along_y = me ^ 2, me ^ 4

    def hop_start(p, hop):
        if hop == 0:
            for device in (along_x, along_y, across):
                pass_on(p, 0, 0, device)
        if hop == 1:
            @pl.when(even & loaded)
            def _():
                pass_on(p, 1, 1, along_y)

            @pl.when(jnp.logical_not(even) & loaded)
            def _():
                pass_on(p, 2, 1, along_x)

            pass_on(p, 1, 1, across)
            pass_on(p, 2, 1, across)
        if hop == 2:
            @pl.when(even & loaded)
            def _():
                pass_on(p, 5, 2, along_y)

            @pl.when(jnp.logical_not(even) & loaded)
            def _():
                pass_on(p, 6, 2, along_x)

            @pl.when(even)
            def _():
                pass_on(p, 3, 2, across)
        if hop == 3:
            @pl.when(even)
            def _():
                pass_on(p, 7, 3, across)

    def hop_wait(p, hop):
        if hop == 0:
            wait_for(blocks(3), ring_recv.at[p, 0])
            for bits in (1, 2, 4):
                hand_over(p, bits)
        if hop == 1:
            @pl.when(even)
            def _():
                wait_for(blocks(3), ring_recv.at[p, 1])
                hand_over(p, 3)

            @pl.when(jnp.logical_not(even))
            def _():
                wait_for(blocks(2), ring_recv.at[p, 1])
            for bits in (5, 6):
                hand_over(p, bits)
        if hop == 2:
            wait_for(blocks(1), ring_recv.at[p, 2])
            hand_over(p, 7)
        if hop == 3:
            @pl.when(jnp.logical_not(even))
            def _():
                wait_for(blocks(1), ring_recv.at[p, 3])
                hand_over(p, 3)

    def sent_wait():
        @pl.when(even & loaded)
        def _():
            wait_for(buf.at[:3, :, :FIN * 18 // 24], ring_send)

        @pl.when(even != loaded)
        def _():
            wait_for(buf.at[:3, :7, :FIN * 14 // 21], ring_send)

        @pl.when(jnp.logical_not(even | loaded))
        def _():
            wait_for(buf.at[:2, :6, :FIN * 10 // 12], ring_send)

    def cross_finish(p):
        wait_for(dr_rz.at[p], z_recv.at[p])
        total = dr_rx[p, z] + dr_rz[p]
        rev32 = eye_rev(F32)
        for m in range(HALF // HEAD):
            part = total[:HEAD, HALF - HEAD * (m + 1):HALF - HEAD * m]
            turned = lax.dot_general(rev32, part, (((1,), (1,)), ((), ())), precision=lax.Precision.HIGHEST, preferred_element_type=F32)
            dr_fin[p, HEAD * m:HEAD * (m + 1)] = turned.reshape(HEAD, 1, HEAD)
        dr_fin[p, HALF] = total[HEAD:HEAD + 1, HALF - HEAD:]
        dr_fin[p, HALF + 1] = total[HEAD + 1:HEAD + 2, HALF - HEAD:]
        dr_fin[p, HALF + 2:] = jnp.zeros((FIN - HALF - 2, 1, HEAD), F32)
        hop_start(p, 0)
        for m in range(N_PART):
            pltpu.make_async_copy(block(p, m, 0), parts[m].at[side, :, head_of(p, 0)], own_sem).start()
        hand_over(p, 0)

    def tip_load(unit):
        slot, row, far = unit % 2, unit // FAR, unit % FAR
        pair = far + tip_base
        for t, src in enumerate((q_in, k_in, v_in, g_in)):
            pltpu.make_async_copy(src.at[core * SLOTS + row, :, pair], r_buf.at[slot, pl.ds(TIP * t + ROWS * core, ROWS)], tip_sem.at[slot]).start()
            pltpu.make_async_copy(far_out.at[t, row, :, far], r_buf.at[slot, pl.ds(TIP * t + ROWS * (1 - core), ROWS)], tip_sem.at[slot]).start()
        pltpu.make_async_copy(r_in.at[:TIP, pair], r_buf.at[slot, 4 * TIP:5 * TIP], tip_sem.at[slot]).start()

    def tip_done(slot):
        wait_for(r_buf.at[slot, :TIP], tip_near.at[slot])
        wait_for(r_buf.at[slot, :TIP], tip_send.at[slot])

    def tip_group(hh, r0):
        group = slice(TIP * hh + r0, TIP * hh + r0 + 16)
        rel = pltpu.roll(e_ref[group, :TIP], 1 + r0, 1, stride=1, stride_axis=0)
        ahead = lax.broadcasted_iota(jnp.int32, (16, TIP), 1) - lax.broadcasted_iota(jnp.int32, (16, TIP), 0)
        return group, s_ref[group, :TIP] + rel, ahead <= r0

    def tip_rows(hh):
        for r0 in range(0, TIP, 16):
            group, s, seen = tip_group(hh, r0)
            s = jnp.where(seen, s, -jnp.inf)
            top = jnp.max(s, axis=1, keepdims=True)
            p = jnp.exp2((s - top) * (scale * LOG2E))
            p = p * (1.0 / jnp.sum(p, axis=1, keepdims=True))
            pb_ref[group, :TIP] = p.astype(BF16)
            dp = dp_ref[group, :TIP]
            row_dot = jnp.sum(p * dp, axis=1, keepdims=True)
            ds = (p * (dp - row_dot) * scale).astype(BF16)
            ds_ref[group, :TIP] = ds
            flipped = flip8(ds.astype(F32))
            half = [pltpu.roll(flipped[8 * j:8 * j + 8], TIP - 8 - r0 - 8 * j, 1, stride=1, stride_axis=0) for j in range(2)]
            dd_ref[group, :TIP] = jnp.concatenate(half, axis=0).astype(BF16)
        rows = slice(TIP * hh, TIP * (hh + 1))
        stage[0, hh, :TIP, :] = dot(pb_ref[rows, :TIP], v_s[hh, :TIP, :]).astype(BF16)
        dqc = dot(ds_ref[rows, :TIP], k_s[hh, :TIP, :])
        dqr = flip8(dot(dd_ref[rows, :TIP], c_s[hh, :TIP, :]))
        stage[1, hh, :TIP, :] = (dqc + dqr).astype(BF16)

    def tip_keys(hh, stats):
        rows = slice(TIP * hh, TIP * (hh + 1))
        st_ref[rows, :8] = stats.T
        for r0 in range(0, TIP, 16):
            group, s, seen = tip_group(hh, r0)
            p = jnp.where(seen, jnp.exp2(s * (scale * LOG2E) - st_ref[group, 0:1]), 0.0)
            pb_ref[group, :TIP] = p.astype(BF16)
            ds_ref[group, :TIP] = (p * (dp_ref[group, :TIP] - st_ref[group, 1:2]) * scale).astype(BF16)
        over_rows = (((0,), (0,)), ((), ()))
        stage[0, hh, :TIP, :] = lax.dot_general(ds_ref[rows, :TIP], a_s[hh, :TIP, :], over_rows, preferred_element_type=F32).astype(BF16)
        stage[1, hh, :TIP, :] = lax.dot_general(pb_ref[rows, :TIP], g_s[hh, :TIP, :], over_rows, preferred_element_type=F32).astype(BF16)

    def tip_unit(unit, carry):
        slot, row, far = unit % 2, unit // FAR, unit % FAR
        pair = far + tip_base
        wait_for(r_buf.at[slot, :5 * TIP], tip_sem.at[slot])

        @pl.when(unit + 1 < UNITS)
        def _():
            tip_load(unit + 1)

        q2, k2, v2, g2, r2 = [pltpu.einshape("abc->bac", r_buf[slot, TIP * t:TIP * (t + 1)]) for t in range(5)]
        u = u_buf[pair].astype(F32)
        w = w_buf[pair].astype(F32)
        for hh in range(PAIR):
            rows = slice(TIP * hh, TIP * (hh + 1))
            q32 = q2[hh].astype(F32)
            a = (q32 + u[hh:hh + 1]).astype(BF16)
            c = (q32 + w[hh:hh + 1]).astype(BF16)
            falling = dot(eye_rev(BF16), r2[hh]).astype(BF16)
            s_ref[rows, :TIP] = dot(a, k2[hh].T)
            e_ref[rows, :TIP] = dot(c, falling.T)
            dp_ref[rows, :TIP] = dot(g2[hh], v2[hh].T)
            a_s[hh, :TIP, :] = a
            c_s[hh, :TIP, :] = falling
            g_s[hh, :TIP, :] = g2[hh]
            k_s[hh, :TIP, :] = k2[hh]
            v_s[hh, :TIP, :] = v2[hh]

        @pl.when(lower)
        def _():
            for hh in range(PAIR):
                tip_rows(hh)

        @pl.when(upper)
        def _():
            for hh in range(PAIR):
                tip_keys(hh, tip_st[far // 2, (far % 2) * SLOTS + row, hh])

        @pl.when(unit >= 2)
        def _():
            tip_done(slot)

        for n in range(2):
            r_buf[slot, (5 + n) * TIP:(6 + n) * TIP] = pltpu.einshape("abc->bac", stage[n, :, :TIP, :])
        place = (core * SLOTS + row, slice(None), pair)

        def give(results):
            for n, dst in enumerate(results):
                pltpu.make_async_copy(r_buf.at[slot, pl.ds((5 + n) * TIP + ROWS * core, ROWS)], dst.at[place], tip_near.at[slot]).start()
                pltpu.make_async_remote_copy(
                    src_ref=r_buf.at[slot, pl.ds((5 + n) * TIP + ROWS * (1 - core), ROWS)], dst_ref=dst.at[place],
                    send_sem=tip_send.at[slot], recv_sem=out_recv, device_id=(partner,), device_id_type=MESH).start()

        @pl.when(lower)
        def _():
            give((o_out, dq_out))

        @pl.when(upper)
        def _():
            give((dk_out, dv_out))
        return carry

    def tips(third):
        @pl.when(tip)
        def _():
            if third == 0:
                wait_for(far_out, far_recv)

                @pl.when(upper)
                def _():
                    wait_for(tip_st, ts_recv)
                tip_load(0)
            lax.fori_loop(UNITS // 3 * third, UNITS // 3 * (third + 1), tip_unit, 0)
            if third == 2:
                tip_done(0)
                tip_done(1)

    send_up(0)

    def sub_body(sub, carry):
        @pl.when(sub < SUBS - 1)
        def _():
            send_up(sub + 1)

        @pl.when(sub == SLOTS)
        def _():
            swap_start(0)

        @pl.when(sub == SUBS - 1)
        def _():
            swap_add(0)
            cross_start(0)

        @pl.when(sub == SUBS)
        def _():
            swap_start(1)
            swap_add(1)
            cross_start(1)
            cross_finish(0)

        @pl.when(lower & (sub < SUBS))
        def _():
            lower_rows(sub)

        @pl.when(lower & (sub > 0))
        def _():
            lower_theirs(sub - 1)

        @pl.when(lower & (sub < SUBS))
        def _():
            lower_own(sub)

        @pl.when(upper & (sub < SUBS))
        def _():
            upper_own(sub)

        @pl.when(sub <= EARLY)
        def _():
            send_out(sub, (2, 3))

        @pl.when((sub > 0) & (sub <= EARLY))
        def _():
            send_out(sub - 1, (0, 1))
        return carry

    lax.fori_loop(0, SUBS + 1, sub_body, 0)

    cross_finish(1)
    send_out(EARLY, (0, 1))
    send_out(EARLY + 1, (2, 3))
    for p in range(2):
        hop_wait(p, 0)
        hop_start(p, 1)
    for p in range(2):
        send_out(EARLY + 1 + p, range(2 * (p + 1)))
        tips(p)
        hop_wait(p, 1)
        hop_start(p, 2)

    def send_late(sub, carry):
        send_out(sub, range(4), True)
        return carry

    lax.fori_loop(EARLY + 3, SUBS, send_late, 0)
    tips(2)
    for p in range(2):
        hop_wait(p, 2)
        hop_start(p, 3)
    for p in range(2):
        hop_wait(p, 3)

    wait_for(buf.at[:, :, :HALF - ROWS], in_send)

    @pl.when(tip)
    def _():
        wait_for(buf.at[:, :, :HALF - 3 * ROWS // 2], out_recv)
        wait_for(buf.at[:, :, :HALF - ROWS], out_send)
        wait_for(far_out, far_send)

    @pl.when(jnp.logical_not(tip))
    def _():
        wait_for(buf, out_recv)
        wait_for(buf.at[:, :, :HALF - 2 * ROWS], out_send)

    @pl.when(upper & jnp.logical_not(tip))
    def _():
        wait_for(st_tx.at[:2], ts_send)

    @pl.when(upper)
    def _():
        wait_for(st_tx, st_send)

    wait_for(dr_rx, x_send)
    wait_for(dr_rz, z_send)
    wait_for(blocks(2), own_sem)
    sent_wait()
    for sem in (fw_send, fw_recv):
        wait_for(buf.at[:3, :, :FIN * 16 // 24], sem)


def writer(*refs):
    ins, (o, dq, dk, dv, dr, du, dw, sem) = refs[:4 + N_PART], refs[4 + N_PART:]
    pairs = list(zip(ins[:4], (o, dq, dk, dv)))
    for m, part in enumerate(ins[4:]):
        rows = min(PART, HALF - PART * m)
        for side in range(2):
            start = HALF * side + PART * m
            pairs.append((part.at[side, :rows], dr.at[start:start + rows]))
    last = HALF - PART * (N_PART - 1)
    pairs += [(ins[-1].at[0, last], du), (ins[-1].at[0, last + 1], dw)]
    copies = [pltpu.make_async_copy(src, dst, sem.at[j]) for j, (src, dst) in enumerate(pairs)]
    for copy in copies:
        copy.start()
    for copy in copies:
        copy.wait()


def solution(mesh):
    seq_spec = P(None, "cp", None, None)

    def local(query, key_in, value, bias_u, bias_w, rel_k, d_out):
        n_batch, rows, n_heads, head_dim = query.shape
        pairs = (n_batch, rows, N_PAIR, PAIR, head_dim)
        vm = pltpu.VMEM
        dma = pltpu.SemaphoreType.DMA
        whole = pl.BlockSpec(memory_space=pl.ANY)
        act = jax.ShapeDtypeStruct(pairs, BF16)
        vec = jax.ShapeDtypeStruct((n_heads, 1, head_dim), F32)
        tok = (PAIR, SEQ, HEAD)
        tok_t = (PAIR, HEAD, SEQ)
        acc = (HEAD + 8, HALF)
        outs = pl.pallas_call(
            kernel,
            name="rel_attn",
            out_shape=(act, act, act, act,
                       *[jax.ShapeDtypeStruct((2, PART, n_heads, 1, head_dim), F32)] * N_PART,
                       jax.ShapeDtypeStruct((4, SLOTS, ROWS, FAR, PAIR, HEAD), BF16)),
            in_specs=[pl.BlockSpec(memory_space=pltpu.HBM)] * 7,
            out_specs=[whole] * (5 + N_PART),
            scratch_shapes=[
                vm((4, SUBS, HALF, PAIR, HEAD), BF16), vm((2, SUBS, HALF, PAIR, HEAD), BF16),
                vm((2, SEQ, PAIR, HEAD), BF16), vm((N_PAIR, PAIR, HEAD), BF16), vm((N_PAIR, PAIR, HEAD), BF16),
                vm((SUBS, PAIR, 8, HALF), F32), vm((SUBS, PAIR, 8, HALF), F32), vm((3, SUBS, PAIR, 8, TIP), F32), vm((QB, HEAD), F32),
                vm((2, 2) + acc, F32), vm((2,) + acc, F32), vm((2, FIN, 1, HEAD), F32), vm((4, 2) + acc, F32),
                vm((QB, SEQ), F32), vm((QB, SEQ), F32), vm((QB, SEQ), F32),
                vm((QB, SEQ), BF16), vm((QB, SEQ), BF16), vm((QB, SEQ), BF16),
                vm(tok, BF16), vm(tok, BF16), vm(tok, BF16), vm(tok, BF16), vm(tok, BF16),
                vm(tok_t, BF16), vm(tok_t, BF16), vm(tok_t, BF16), vm(tok_t, BF16), vm(tok_t, BF16),
                vm((4, SEQ, HEAD), BF16), vm((4, HEAD, SEQ), BF16),
                vm((PAIR, HEAD, HALF), F32), vm((PAIR, HEAD, HALF), F32), vm((4, PAIR, HALF, HEAD), BF16),
                dma, dma((2, SUBS)), dma, dma, dma, dma((4,)), dma((4,)), dma((SUBS,)), dma, dma((4,)),
                dma, dma((2,)), dma, dma((2,)), dma, dma((2, 4)), dma, dma,
                dma, dma, dma((2,)), dma((2,)), dma((2,)), dma, dma,
            ],
            compiler_params=pltpu.CompilerParams(collective_id=0, has_side_effects=True, vmem_limit_bytes=37 * 1024 * 1024),
        )(*[pltpu.with_memory_space_constraint(x, pltpu.HBM) for x in (
            query.reshape(pairs), key_in.reshape(pairs), value.reshape(pairs), d_out.reshape(pairs),
            rel_k.reshape(SEQ, N_PAIR, PAIR, head_dim), bias_u.reshape(N_PAIR, PAIR, head_dim), bias_w.reshape(N_PAIR, PAIR, head_dim))])
        o, dq, dk, dv, dr, du, dw = pl.pallas_call(
            writer,
            name="writer",
            out_shape=(act, act, act, act, jax.ShapeDtypeStruct((SEQ, n_heads, 1, head_dim), F32), vec, vec),
            in_specs=[whole] * (4 + N_PART),
            out_specs=[whole] * 7,
            scratch_shapes=[dma((6 + 2 * N_PART,))],
            compiler_params=pltpu.CompilerParams(vmem_limit_bytes=1024 * 1024),
        )(*outs[:-1])
        full = query.shape
        return (o.reshape(full), dq.reshape(full), dk.reshape(full), dv.reshape(full),
                du.reshape(bias_u.shape), dw.reshape(bias_w.shape), dr.reshape(rel_k.shape))

    return jax.shard_map(local, mesh=mesh,
                         in_specs=(seq_spec, seq_spec, seq_spec, P(), P(), P(), seq_spec),
                         out_specs=(seq_spec, seq_spec, seq_spec, seq_spec, P(), P(), P()),
                         check_vma=False)
```

```python
import jax
import jax.numpy as jnp
from jax import lax
from jax.experimental import pallas as pl
from jax.experimental.pallas import tpu as pltpu
from jax.sharding import PartitionSpec as P

MESH = pl.DeviceIdType.MESH
BF16, F32 = jnp.bfloat16, jnp.float32
LOG2E = 1.4426950408889634

N_DEV = 16
PLANE = 8
PAIR = 2
N_PAIR = 8
SLOTS = 4
SUBS = 2 * SLOTS
EARLY = 3
ROWS = 64
HALF = PLANE * ROWS
SEQ = 2 * HALF
HEAD = 128
QB = 256
WIN = HALF + QB
N_PART = 6
PART = 86
FIN = N_PART * PART
TIP = 2 * ROWS
FAR = N_PAIR - 2
UNITS = FAR * SLOTS
TURNS = ((1, 3, 2), (3, 1, 2))


def dot(lhs, rhs):
    return jnp.dot(lhs, rhs, preferred_element_type=F32)


def flip8(x):
    rows, cols = x.shape
    idx = 7 - lax.broadcasted_iota(jnp.int32, (rows // 8, 8, cols), 1)
    return jnp.take_along_axis(x.reshape(rows // 8, 8, cols), idx, axis=1).reshape(rows, cols)


def eye_rev(dtype):
    total = lax.broadcasted_iota(jnp.int32, (HEAD, HEAD), 0) + lax.broadcasted_iota(jnp.int32, (HEAD, HEAD), 1)
    return jnp.where(total == HEAD - 1, 1.0, 0.0).astype(dtype)


def kernel(q_in, k_in, v_in, g_in, r_in, u_in, w_in,
           o_out, dq_out, dk_out, dv_out, dr0_out, dr1_out, dr2_out, dr3_out, dr4_out, dr5_out, far_out,
           buf, rbuf, r_buf, u_buf, w_buf, st_tx, st_rx, tip_st, st_ref, dr_rx, dr_rz, dr_fin, dr_acc,
           s_ref, e_ref, dp_ref, pb_ref, ds_ref, dd_ref,
           a_s, c_s, g_s, k_s, v_s, at_s, ct_s, gt_s, kt_s, vt_s, rev_s, rt_s, dkt, dvt, stage,
           in_send, in_recv, out_send, out_recv, own_sem, r_sem, up_send, up_recv, st_send, st_recv,
           x_send, x_recv, z_send, z_recv, ring_send, ring_recv, fw_send, fw_recv,
           far_send, far_recv, tip_sem, tip_near, tip_send, ts_send, ts_recv):
    me = lax.axis_index("cp")
    core = me % 2
    chip = me // 2
    col = chip % 4
    z = chip // 4
    partner = me + 1 - 2 * core
    across = me + PLANE * (1 - 2 * z)
    scale = HEAD ** -0.5

    def wait_for(ref, sem):
        pltpu.make_async_copy(ref, ref, sem).wait()

    y = col // 2
    lower, upper = z == 0, z == 1
    tip = chip == 7 * z
    tip_base = 2 - 2 * z

    tables = [pltpu.make_async_copy(src, dst, r_sem.at[j]) for j, (src, dst) in enumerate(
        ((r_in.at[:, 2 * col], r_buf.at[0]), (r_in.at[:, 2 * col + 1], r_buf.at[1]), (u_in, u_buf), (w_in, w_buf)))]
    for copy in tables:
        copy.start()

    barrier = pltpu.get_barrier_semaphore()

    for peer in [across] + [me ^ step for step in range(PLANE - 1, 0, -1)]:
        pl.semaphore_signal(barrier, inc=1, device_id=(peer,), device_id_type=MESH)
    pl.semaphore_wait(barrier, PLANE)

    my_rows = pl.ds(pl.multiple_of((me % PLANE) * ROWS, ROWS), ROWS)

    even = chip % 2 == z
    loaded = y != z

    def peers(late_sub=None):
        near = core == 0
        if late_sub is not None:
            near = jnp.logical_not(near) & (even | jnp.logical_not(loaded) | (late_sub < SUBS - 1))
        first, second, third = [jnp.where(near, near_turn, far_turn) for near_turn, far_turn in zip(*TURNS)]
        for turn, other in ((first, 0), (third, 0), (first, 1), (third, 1), (second, 0), (second, 1)):
            yield me ^ (2 * turn + other)
        yield partner

    def send_in(ins, sub):
        pair, row = sub // SLOTS, sub % SLOTS
        for first in (0, 2):
            for t in (first, first + 1):
                pltpu.make_async_copy(ins[t].at[core * SLOTS + row, :, 2 * col + pair], buf.at[t, sub, my_rows], in_recv.at[first // 2, sub]).start()
            for peer in peers():
                for t in (first, first + 1):
                    pltpu.make_async_remote_copy(
                        src_ref=ins[t].at[(peer % 2) * SLOTS + row, :, 2 * ((peer // 2) % 4) + pair], dst_ref=buf.at[t, sub, my_rows],
                        send_sem=in_send, recv_sem=in_recv.at[first // 2, sub], device_id=(peer,), device_id_type=MESH).start()

    def send_all(ins):
        def send_sub(sub, carry):
            send_in(ins, sub)
            return carry
        lax.fori_loop(0, SUBS, send_sub, 0)

    @pl.when(lower)
    def _():
        send_all((k_in, v_in, q_in, g_in))

    @pl.when(upper)
    def _():
        send_all((q_in, g_in, k_in, v_in))

    @pl.when(tip)
    def _():
        for t, src in enumerate((q_in, k_in, v_in, g_in)):
            for row in range(SLOTS):
                pltpu.make_async_remote_copy(
                    src_ref=src.at[(1 - core) * SLOTS + row, :, pl.ds(tip_base, FAR)], dst_ref=far_out.at[t, row],
                    send_sem=far_send, recv_sem=far_recv, device_id=(partner,), device_id_type=MESH).start()

    for copy in tables:
        copy.wait()
    rev = eye_rev(BF16)
    for p in range(2):
        pair_tab = pltpu.einshape("abc->bac", r_buf[p])
        for hh in range(PAIR):
            for blk in range(SEQ // HEAD):
                part = pair_tab[hh, SEQ - HEAD * (blk + 1):SEQ - HEAD * blk]
                flipped = dot(rev, part).astype(BF16)
                rev_s[2 * p + hh, HEAD * blk:HEAD * (blk + 1), :] = flipped
                rt_s[2 * p + hh, :, HEAD * blk:HEAD * (blk + 1)] = flipped.T
    dr_acc[...] = jnp.zeros_like(dr_acc)

    acts = (dk_out, dv_out, o_out, dq_out)

    def send_out(sub, which, late_sub=None):
        place = (core * SLOTS + sub % SLOTS, slice(None), 2 * col + sub // SLOTS)
        for t in which:
            pltpu.make_async_copy(buf.at[t, sub, my_rows], acts[t].at[place], out_recv).start()
        for peer in peers(late_sub):
            peer_rows = pl.ds(pl.multiple_of((peer % PLANE) * ROWS, ROWS), ROWS)
            to_tip = (peer // 2 == 7 * z) & jnp.logical_not(tip)
            for t in which:
                @pl.when(jnp.logical_not(to_tip & (lower if t >= 2 else upper)))
                def _():
                    pltpu.make_async_remote_copy(
                        src_ref=buf.at[t, sub, peer_rows], dst_ref=acts[t].at[place],
                        send_sem=out_send, recv_sem=out_recv, device_id=(peer,), device_id_type=MESH).start()

    def send_up(sub):
        wait_for(buf.at[0:2, sub], in_recv.at[0, sub])
        for j in range(2):
            pltpu.make_async_remote_copy(src_ref=buf.at[j, sub], dst_ref=rbuf.at[j, sub], send_sem=up_send.at[sub % 4], recv_sem=up_recv.at[sub],
                                         device_id=(across,), device_id_type=MESH).start()

    def unpack(ref, j, sub):
        return pltpu.einshape("abc->bac", ref[j, sub])

    def load_rows(q_ref, q_j, g_ref, g_j, sub, start, turned):
        rows = slice(start, start + HALF)
        p = sub // SLOTS
        q2 = unpack(q_ref, q_j, sub)
        u = u_buf[2 * col + p].astype(F32)
        w = w_buf[2 * col + p].astype(F32)
        for hh in range(PAIR):
            q32 = q2[hh].astype(F32)
            a = (q32 + u[hh:hh + 1]).astype(BF16)
            c = (q32 + w[hh:hh + 1]).astype(BF16)
            a_s[hh, rows, :] = a
            c_s[hh, rows, :] = c
            at_s[hh, :, rows] = a.T
            if turned:
                ct_s[hh, :, rows] = flip8(c.astype(F32)).astype(BF16).T
        g2 = unpack(g_ref, g_j, sub)
        g_s[:, rows, :] = g2
        for hh in range(PAIR):
            gt_s[hh, :, rows] = g2[hh].T

    def load_keys(k_ref, k_j, v_ref, v_j, sub, start):
        rows = slice(start, start + HALF)
        k2 = unpack(k_ref, k_j, sub)
        v2 = unpack(v_ref, v_j, sub)
        k_s[:, rows, :] = k2
        v_s[:, rows, :] = v2
        for hh in range(PAIR):
            kt_s[hh, :, rows] = k2[hh].T
            vt_s[hh, :, rows] = v2[hh].T

    def row_block(hh, head, start, i0, lo, fresh, stats):
        width = i0 + QB
        rows = slice(start, start + QB)
        s_ref[:, :width] = dot(a_s[hh, rows, :], kt_s[hh, :, :width])
        e_ref[:, :width] = dot(c_s[hh, rows, :], rt_s[head, :, SEQ - width:])
        dp_ref[:, :width] = dot(g_s[hh, rows, :], vt_s[hh, :, :width])
        for r0 in range(0, QB, 16):
            group = slice(r0, r0 + 16)
            rel = pltpu.roll(e_ref[group, :width], i0 + 1 + r0, 1, stride=1, stride_axis=0)
            s = s_ref[group, :width] + rel
            ahead = lax.broadcasted_iota(jnp.int32, (16, width), 1) - lax.broadcasted_iota(jnp.int32, (16, width), 0)
            s = jnp.where(ahead <= i0 + r0, s, -jnp.inf)
            top = jnp.max(s, axis=1, keepdims=True)
            p = jnp.exp2((s - top) * (scale * LOG2E))
            total = jnp.sum(p, axis=1, keepdims=True)
            p = p * (1.0 / total)
            pb_ref[group, :width] = p.astype(BF16)
            dp = dp_ref[group, :width]
            row_dot = jnp.sum(p * dp, axis=1, keepdims=True)
            ds = (p * (dp - row_dot) * scale).astype(BF16)
            ds_ref[group, :width] = ds
            flipped = flip8(ds.astype(F32))
            half = [pltpu.roll(flipped[8 * j:8 * j + 8], QB - 8 - r0 - 8 * j, 1, stride=1, stride_axis=0) for j in range(2)]
            dd_ref[group, :width] = jnp.concatenate(half, axis=0).astype(BF16)
            if stats:
                lane = lax.broadcasted_iota(jnp.int32, (16, HEAD), 1)
                st_ref[group, :] = jnp.where(lane == 0, top * (scale * LOG2E) + jnp.log2(total), row_dot)
        pb = pb_ref[:, :width]
        ds = ds_ref[:, :width]
        dd = dd_ref[:, :width]
        stage[0, hh, rows, :] = dot(pb, v_s[hh, :width, :]).astype(BF16)
        dqc = dot(ds, k_s[hh, :width, :])
        dqr = flip8(dot(dd, rev_s[head, SEQ - width:, :]))
        stage[1, hh, rows, :] = (dqc + dqr).astype(BF16)
        dr_acc[head, 1, HEAD:HEAD + 1, HALF - HEAD:] += jnp.sum(dqc, axis=0, keepdims=True)
        dr_acc[head, 1, HEAD + 1:HEAD + 2, HALF - HEAD:] += jnp.sum(dqr, axis=0, keepdims=True)
        dk_new = dot(at_s[hh, :, rows], ds_ref[:, lo:width])
        dv_new = dot(gt_s[hh, :, rows], pb_ref[:, lo:width])
        if fresh:
            dkt[hh] = dk_new
            dvt[hh] = dv_new
        else:
            dkt[hh, :, :width - lo] += dk_new
            dvt[hh, :, :width - lo] += dv_new
        dr_new = dot(ct_s[hh, :, rows], dd)
        if width > HALF:
            dr_acc[head, 0, :HEAD, SEQ - width:] += dr_new[:, :width - HALF]
            dr_acc[head, 1, :HEAD, :] += dr_new[:, width - HALF:]
        else:
            dr_acc[head, 1, :HEAD, HALF - width:] += dr_new

    def col_block(hh, head, sub, i0):
        rows = slice(i0, i0 + QB)
        first = WIN - i0
        s_ref[:, :HALF] = dot(a_s[hh, rows, :], kt_s[hh, :, :HALF])
        e_ref[:, :WIN] = dot(c_s[hh, rows, :], rt_s[head, :, first:first + WIN])
        dp_ref[:, :HALF] = dot(g_s[hh, rows, :], vt_s[hh, :, :HALF])
        st_ref[:, :8] = st_rx[sub, hh, :, i0 - HALF:i0 - HALF + QB].T
        for r0 in range(0, QB, 16):
            group = slice(r0, r0 + 16)
            rel = pltpu.roll(e_ref[group, :WIN], HALF + 1 + r0, 1, stride=1, stride_axis=0)[:, :HALF]
            log_sum = st_ref[group, 0:1]
            row_dot = st_ref[group, 1:2]
            p = jnp.exp2((s_ref[group, :HALF] + rel) * (scale * LOG2E) - log_sum)
            pb_ref[group, :HALF] = p.astype(BF16)
            ds_ref[group, :HALF] = (p * (dp_ref[group, :HALF] - row_dot) * scale).astype(BF16)
        dkt[hh] += dot(at_s[hh, :, rows], ds_ref[:, :HALF])
        dvt[hh] += dot(gt_s[hh, :, rows], pb_ref[:, :HALF])

    def store_rows(sub):
        for t in range(2):
            buf[2 + t, sub] = pltpu.einshape("abc->bac", stage[t])

    def store_keys(sub):
        for hh in range(PAIR):
            stage[2, hh] = dkt[hh].astype(BF16).T
            stage[3, hh] = dvt[hh].astype(BF16).T
        for t in range(2):
            buf[t, sub] = pltpu.einshape("abc->bac", stage[2 + t])

    def wait_up(sub):
        wait_for(rbuf.at[:, sub], up_recv.at[sub])
        wait_for(rbuf.at[:, sub], up_send.at[sub % 4])

    def wait_in(sub):
        wait_for(buf.at[2:4, sub], in_recv.at[1, sub])

    def lower_rows(sub):
        wait_in(sub)
        load_rows(buf, 2, buf, 3, sub, 0, True)

    def lower_own(sub):
        load_keys(buf, 0, buf, 1, sub, 0)

        def own(hh, carry):
            head = 2 * (sub // SLOTS) + hh
            row_block(hh, head, QB, QB, 0, True, False)
            row_block(hh, head, 0, 0, 0, False, False)
            return carry

        lax.fori_loop(0, PAIR, own, 0)
        store_rows(sub)

    def lower_theirs(sub):
        wait_up(sub)
        load_rows(rbuf, 0, rbuf, 1, sub, HALF, False)
        wait_for(st_rx.at[sub], st_recv.at[sub % 4])

        def theirs(hh, carry):
            head = 2 * (sub // SLOTS) + hh
            col_block(hh, head, sub, HALF)
            col_block(hh, head, sub, HALF + QB)
            return carry

        lax.fori_loop(0, PAIR, theirs, 0)
        store_keys(sub)

    def upper_own(sub):
        wait_in(sub)
        wait_up(sub)
        load_rows(buf, 0, buf, 1, sub, 0, True)
        load_keys(rbuf, 0, rbuf, 1, sub, 0)
        load_keys(buf, 2, buf, 3, sub, HALF)

        def own(hh, carry):
            head = 2 * (sub // SLOTS) + hh
            for blk in (1, 0):
                row_block(hh, head, QB * blk, HALF + QB * blk, HALF, blk == 1, True)
                st_tx[sub, hh, :, QB * blk:QB * (blk + 1)] = st_ref[...].T[:8]
            pltpu.make_async_remote_copy(src_ref=st_tx.at[sub, hh], dst_ref=st_rx.at[sub, hh], send_sem=st_send, recv_sem=st_recv.at[sub % 4],
                                         device_id=(across,), device_id_type=MESH).start()

            @pl.when(jnp.logical_not(tip))
            def _():
                pltpu.make_async_remote_copy(src_ref=st_tx.at[sub, hh, :, HALF - TIP:], dst_ref=tip_st.at[col, sub, hh], send_sem=ts_send,
                                             recv_sem=ts_recv, device_id=(N_DEV - 2 + core,), device_id_type=MESH).start()
            return carry

        lax.fori_loop(0, PAIR, own, 0)
        store_rows(sub)
        store_keys(sub)

    side = 1 - core
    parts = (dr0_out, dr1_out, dr2_out, dr3_out, dr4_out, dr5_out)

    def swap_start(p):
        for n in range(2):
            pltpu.make_async_remote_copy(src_ref=dr_acc.at[2 * p + n, side], dst_ref=dr_rx.at[p, n], send_sem=x_send, recv_sem=x_recv.at[p],
                                         device_id=(partner,), device_id_type=MESH).start()

    def swap_add(p):
        wait_for(dr_rx.at[p], x_recv.at[p])
        for n in range(2):
            dr_rx[p, n] = dr_rx[p, n] + dr_acc[2 * p + n, core]

    def cross_start(p):
        pltpu.make_async_remote_copy(src_ref=dr_rx.at[p, 1 - z], dst_ref=dr_rz.at[p], send_sem=z_send, recv_sem=z_recv.at[p],
                                     device_id=(across,), device_id_type=MESH).start()

    def head_of(p, bits):
        other = chip ^ bits
        return 4 * (other % 4) + 2 * p + other // 4

    def block(p, m, bits):
        if bits == 0:
            return dr_fin.at[p, PART * m:PART * (m + 1)]
        return parts[m].at[side, :, head_of(p, bits)]

    def forward(p, m, bits):
        pltpu.make_async_remote_copy(src_ref=block(p, m, bits), dst_ref=parts[m].at[side, :, head_of(p, bits)], send_sem=fw_send,
                                     recv_sem=fw_recv, device_id=(partner,), device_id_type=MESH).start()

    def blocks(count):
        return parts[0].at[:, :, :N_PART // 2 * count]

    def pass_on(p, bits, hop, device):
        for m in range(N_PART):
            pltpu.make_async_remote_copy(
                src_ref=block(p, m, bits), dst_ref=parts[m].at[side, :, head_of(p, bits)], send_sem=ring_send,
                recv_sem=ring_recv.at[p, hop], device_id=(device,), device_id_type=MESH).start()

    def hand_over(p, bits):
        for m in range(N_PART):
            forward(p, m, bits)

    along_x, along_y = me ^ 2, me ^ 4

    def hop_start(p, hop):
        if hop == 0:
            for device in (along_x, along_y, across):
                pass_on(p, 0, 0, device)
        if hop == 1:
            @pl.when(even & loaded)
            def _():
                pass_on(p, 1, 1, along_y)

            @pl.when(jnp.logical_not(even) & loaded)
            def _():
                pass_on(p, 2, 1, along_x)

            pass_on(p, 1, 1, across)
            pass_on(p, 2, 1, across)
        if hop == 2:
            @pl.when(even & loaded)
            def _():
                pass_on(p, 5, 2, along_y)

            @pl.when(jnp.logical_not(even) & loaded)
            def _():
                pass_on(p, 6, 2, along_x)

            @pl.when(even)
            def _():
                pass_on(p, 3, 2, across)
        if hop == 3:
            @pl.when(even)
            def _():
                pass_on(p, 7, 3, across)

    def hop_wait(p, hop):
        if hop == 0:
            wait_for(blocks(3), ring_recv.at[p, 0])
            for bits in (1, 2, 4):
                hand_over(p, bits)
        if hop == 1:
            @pl.when(even)
            def _():
                wait_for(blocks(3), ring_recv.at[p, 1])
                hand_over(p, 3)

            @pl.when(jnp.logical_not(even))
            def _():
                wait_for(blocks(2), ring_recv.at[p, 1])
            for bits in (5, 6):
                hand_over(p, bits)
        if hop == 2:
            wait_for(blocks(1), ring_recv.at[p, 2])
            hand_over(p, 7)
        if hop == 3:
            @pl.when(jnp.logical_not(even))
            def _():
                wait_for(blocks(1), ring_recv.at[p, 3])
                hand_over(p, 3)

    def sent_wait():
        @pl.when(even & loaded)
        def _():
            wait_for(buf.at[:3, :, :FIN * 18 // 24], ring_send)

        @pl.when(even != loaded)
        def _():
            wait_for(buf.at[:3, :7, :FIN * 14 // 21], ring_send)

        @pl.when(jnp.logical_not(even | loaded))
        def _():
            wait_for(buf.at[:2, :6, :FIN * 10 // 12], ring_send)

    def cross_finish(p):
        wait_for(dr_rz.at[p], z_recv.at[p])
        total = dr_rx[p, z] + dr_rz[p]
        rev32 = eye_rev(F32)
        for m in range(HALF // HEAD):
            part = total[:HEAD, HALF - HEAD * (m + 1):HALF - HEAD * m]
            turned = lax.dot_general(rev32, part, (((1,), (1,)), ((), ())), precision=lax.Precision.HIGHEST, preferred_element_type=F32)
            dr_fin[p, HEAD * m:HEAD * (m + 1)] = turned.reshape(HEAD, 1, HEAD)
        dr_fin[p, HALF] = total[HEAD:HEAD + 1, HALF - HEAD:]
        dr_fin[p, HALF + 1] = total[HEAD + 1:HEAD + 2, HALF - HEAD:]
        dr_fin[p, HALF + 2:] = jnp.zeros((FIN - HALF - 2, 1, HEAD), F32)
        hop_start(p, 0)
        for m in range(N_PART):
            pltpu.make_async_copy(block(p, m, 0), parts[m].at[side, :, head_of(p, 0)], own_sem).start()
        hand_over(p, 0)

    def tip_load(unit):
        slot, row, far = unit % 2, unit // FAR, unit % FAR
        pair = far + tip_base
        for t, src in enumerate((q_in, k_in, v_in, g_in)):
            pltpu.make_async_copy(src.at[core * SLOTS + row, :, pair], r_buf.at[slot, pl.ds(TIP * t + ROWS * core, ROWS)], tip_sem.at[slot]).start()
            pltpu.make_async_copy(far_out.at[t, row, :, far], r_buf.at[slot, pl.ds(TIP * t + ROWS * (1 - core), ROWS)], tip_sem.at[slot]).start()
        pltpu.make_async_copy(r_in.at[:TIP, pair], r_buf.at[slot, 4 * TIP:5 * TIP], tip_sem.at[slot]).start()

    def tip_done(slot):
        wait_for(r_buf.at[slot, :TIP], tip_near.at[slot])
        wait_for(r_buf.at[slot, :TIP], tip_send.at[slot])

    def tip_group(hh, r0):
        group = slice(TIP * hh + r0, TIP * hh + r0 + 16)
        rel = pltpu.roll(e_ref[group, :TIP], 1 + r0, 1, stride=1, stride_axis=0)
        ahead = lax.broadcasted_iota(jnp.int32, (16, TIP), 1) - lax.broadcasted_iota(jnp.int32, (16, TIP), 0)
        return group, s_ref[group, :TIP] + rel, ahead <= r0

    def tip_rows(hh):
        for r0 in range(0, TIP, 16):
            group, s, seen = tip_group(hh, r0)
            s = jnp.where(seen, s, -jnp.inf)
            top = jnp.max(s, axis=1, keepdims=True)
            p = jnp.exp2((s - top) * (scale * LOG2E))
            p = p * (1.0 / jnp.sum(p, axis=1, keepdims=True))
            pb_ref[group, :TIP] = p.astype(BF16)
            dp = dp_ref[group, :TIP]
            row_dot = jnp.sum(p * dp, axis=1, keepdims=True)
            ds = (p * (dp - row_dot) * scale).astype(BF16)
            ds_ref[group, :TIP] = ds
            flipped = flip8(ds.astype(F32))
            half = [pltpu.roll(flipped[8 * j:8 * j + 8], TIP - 8 - r0 - 8 * j, 1, stride=1, stride_axis=0) for j in range(2)]
            dd_ref[group, :TIP] = jnp.concatenate(half, axis=0).astype(BF16)
        rows = slice(TIP * hh, TIP * (hh + 1))
        stage[0, hh, :TIP, :] = dot(pb_ref[rows, :TIP], v_s[hh, :TIP, :]).astype(BF16)
        dqc = dot(ds_ref[rows, :TIP], k_s[hh, :TIP, :])
        dqr = flip8(dot(dd_ref[rows, :TIP], c_s[hh, :TIP, :]))
        stage[1, hh, :TIP, :] = (dqc + dqr).astype(BF16)

    def tip_keys(hh, stats):
        rows = slice(TIP * hh, TIP * (hh + 1))
        st_ref[rows, :8] = stats.T
        for r0 in range(0, TIP, 16):
            group, s, seen = tip_group(hh, r0)
            p = jnp.where(seen, jnp.exp2(s * (scale * LOG2E) - st_ref[group, 0:1]), 0.0)
            pb_ref[group, :TIP] = p.astype(BF16)
            ds_ref[group, :TIP] = (p * (dp_ref[group, :TIP] - st_ref[group, 1:2]) * scale).astype(BF16)
        over_rows = (((0,), (0,)), ((), ()))
        stage[0, hh, :TIP, :] = lax.dot_general(ds_ref[rows, :TIP], a_s[hh, :TIP, :], over_rows, preferred_element_type=F32).astype(BF16)
        stage[1, hh, :TIP, :] = lax.dot_general(pb_ref[rows, :TIP], g_s[hh, :TIP, :], over_rows, preferred_element_type=F32).astype(BF16)

    def tip_unit(unit, carry):
        slot, row, far = unit % 2, unit // FAR, unit % FAR
        pair = far + tip_base
        wait_for(r_buf.at[slot, :5 * TIP], tip_sem.at[slot])

        @pl.when(unit + 1 < UNITS)
        def _():
            tip_load(unit + 1)

        q2, k2, v2, g2, r2 = [pltpu.einshape("abc->bac", r_buf[slot, TIP * t:TIP * (t + 1)]) for t in range(5)]
        u = u_buf[pair].astype(F32)
        w = w_buf[pair].astype(F32)
        for hh in range(PAIR):
            rows = slice(TIP * hh, TIP * (hh + 1))
            q32 = q2[hh].astype(F32)
            a = (q32 + u[hh:hh + 1]).astype(BF16)
            c = (q32 + w[hh:hh + 1]).astype(BF16)
            falling = dot(eye_rev(BF16), r2[hh]).astype(BF16)
            s_ref[rows, :TIP] = dot(a, k2[hh].T)
            e_ref[rows, :TIP] = dot(c, falling.T)
            dp_ref[rows, :TIP] = dot(g2[hh], v2[hh].T)
            a_s[hh, :TIP, :] = a
            c_s[hh, :TIP, :] = falling
            g_s[hh, :TIP, :] = g2[hh]
            k_s[hh, :TIP, :] = k2[hh]
            v_s[hh, :TIP, :] = v2[hh]

        @pl.when(lower)
        def _():
            for hh in range(PAIR):
                tip_rows(hh)

        @pl.when(upper)
        def _():
            for hh in range(PAIR):
                tip_keys(hh, tip_st[far // 2, (far % 2) * SLOTS + row, hh])

        @pl.when(unit >= 2)
        def _():
            tip_done(slot)

        for n in range(2):
            r_buf[slot, (5 + n) * TIP:(6 + n) * TIP] = pltpu.einshape("abc->bac", stage[n, :, :TIP, :])
        place = (core * SLOTS + row, slice(None), pair)

        def give(results):
            for n, dst in enumerate(results):
                pltpu.make_async_copy(r_buf.at[slot, pl.ds((5 + n) * TIP + ROWS * core, ROWS)], dst.at[place], tip_near.at[slot]).start()
                pltpu.make_async_remote_copy(
                    src_ref=r_buf.at[slot, pl.ds((5 + n) * TIP + ROWS * (1 - core), ROWS)], dst_ref=dst.at[place],
                    send_sem=tip_send.at[slot], recv_sem=out_recv, device_id=(partner,), device_id_type=MESH).start()

        @pl.when(lower)
        def _():
            give((o_out, dq_out))

        @pl.when(upper)
        def _():
            give((dk_out, dv_out))
        return carry

    def tips(third):
        @pl.when(tip)
        def _():
            if third == 0:
                wait_for(far_out, far_recv)

                @pl.when(upper)
                def _():
                    wait_for(tip_st, ts_recv)
                tip_load(0)
            lax.fori_loop(UNITS // 3 * third, UNITS // 3 * (third + 1), tip_unit, 0)
            if third == 2:
                tip_done(0)
                tip_done(1)

    send_up(0)

    def sub_body(sub, carry):
        @pl.when(sub < SUBS - 1)
        def _():
            send_up(sub + 1)

        @pl.when(sub == SLOTS)
        def _():
            swap_start(0)

        @pl.when(sub == SUBS - 1)
        def _():
            swap_add(0)
            cross_start(0)

        @pl.when(sub == SUBS)
        def _():
            swap_start(1)
            swap_add(1)
            cross_start(1)
            cross_finish(0)

        @pl.when(lower & (sub < SUBS))
        def _():
            lower_rows(sub)

        @pl.when(lower & (sub > 0))
        def _():
            lower_theirs(sub - 1)

        @pl.when(lower & (sub < SUBS))
        def _():
            lower_own(sub)

        @pl.when(upper & (sub < SUBS))
        def _():
            upper_own(sub)

        @pl.when(sub <= EARLY)
        def _():
            send_out(sub, (2, 3))

        @pl.when((sub > 0) & (sub <= EARLY))
        def _():
            send_out(sub - 1, (0, 1))
        return carry

    lax.fori_loop(0, SUBS + 1, sub_body, 0)

    cross_finish(1)
    send_out(EARLY, (0, 1))
    send_out(EARLY + 1, (2, 3))
    for p in range(2):
        hop_wait(p, 0)
        hop_start(p, 1)
    for p in range(2):
        send_out(EARLY + 1 + p, range(2 * (p + 1)))
        tips(p)
        hop_wait(p, 1)
        hop_start(p, 2)

    def send_late(sub, carry):
        send_out(sub, range(4), sub)
        return carry

    lax.fori_loop(EARLY + 3, SUBS, send_late, 0)
    tips(2)
    for p in range(2):
        hop_wait(p, 2)
        hop_start(p, 3)
    for p in range(2):
        hop_wait(p, 3)

    wait_for(buf.at[:, :, :HALF - ROWS], in_send)

    @pl.when(tip)
    def _():
        wait_for(buf.at[:, :, :HALF - 3 * ROWS // 2], out_recv)
        wait_for(buf.at[:, :, :HALF - ROWS], out_send)
        wait_for(far_out, far_send)

    @pl.when(jnp.logical_not(tip))
    def _():
        wait_for(buf, out_recv)
        wait_for(buf.at[:, :, :HALF - 2 * ROWS], out_send)

    @pl.when(upper & jnp.logical_not(tip))
    def _():
        wait_for(st_tx.at[:2], ts_send)

    @pl.when(upper)
    def _():
        wait_for(st_tx, st_send)

    wait_for(dr_rx, x_send)
    wait_for(dr_rz, z_send)
    wait_for(blocks(2), own_sem)
    sent_wait()
    for sem in (fw_send, fw_recv):
        wait_for(buf.at[:3, :, :FIN * 16 // 24], sem)


def writer(*refs):
    ins, (o, dq, dk, dv, dr, du, dw, sem) = refs[:4 + N_PART], refs[4 + N_PART:]
    pairs = list(zip(ins[:4], (o, dq, dk, dv)))
    for m, part in enumerate(ins[4:]):
        rows = min(PART, HALF - PART * m)
        for side in range(2):
            start = HALF * side + PART * m
            pairs.append((part.at[side, :rows], dr.at[start:start + rows]))
    last = HALF - PART * (N_PART - 1)
    pairs += [(ins[-1].at[0, last], du), (ins[-1].at[0, last + 1], dw)]
    copies = [pltpu.make_async_copy(src, dst, sem.at[j]) for j, (src, dst) in enumerate(pairs)]
    for copy in copies:
        copy.start()
    for copy in copies:
        copy.wait()


def solution(mesh):
    seq_spec = P(None, "cp", None, None)

    def local(query, key_in, value, bias_u, bias_w, rel_k, d_out):
        n_batch, rows, n_heads, head_dim = query.shape
        pairs = (n_batch, rows, N_PAIR, PAIR, head_dim)
        vm = pltpu.VMEM
        dma = pltpu.SemaphoreType.DMA
        whole = pl.BlockSpec(memory_space=pl.ANY)
        act = jax.ShapeDtypeStruct(pairs, BF16)
        vec = jax.ShapeDtypeStruct((n_heads, 1, head_dim), F32)
        tok = (PAIR, SEQ, HEAD)
        tok_t = (PAIR, HEAD, SEQ)
        acc = (HEAD + 8, HALF)
        outs = pl.pallas_call(
            kernel,
            name="rel_attn",
            out_shape=(act, act, act, act,
                       *[jax.ShapeDtypeStruct((2, PART, n_heads, 1, head_dim), F32)] * N_PART,
                       jax.ShapeDtypeStruct((4, SLOTS, ROWS, FAR, PAIR, HEAD), BF16)),
            in_specs=[pl.BlockSpec(memory_space=pltpu.HBM)] * 7,
            out_specs=[whole] * (5 + N_PART),
            scratch_shapes=[
                vm((4, SUBS, HALF, PAIR, HEAD), BF16), vm((2, SUBS, HALF, PAIR, HEAD), BF16),
                vm((2, SEQ, PAIR, HEAD), BF16), vm((N_PAIR, PAIR, HEAD), BF16), vm((N_PAIR, PAIR, HEAD), BF16),
                vm((SUBS, PAIR, 8, HALF), F32), vm((SUBS, PAIR, 8, HALF), F32), vm((3, SUBS, PAIR, 8, TIP), F32), vm((QB, HEAD), F32),
                vm((2, 2) + acc, F32), vm((2,) + acc, F32), vm((2, FIN, 1, HEAD), F32), vm((4, 2) + acc, F32),
                vm((QB, SEQ), F32), vm((QB, SEQ), F32), vm((QB, SEQ), F32),
                vm((QB, SEQ), BF16), vm((QB, SEQ), BF16), vm((QB, SEQ), BF16),
                vm(tok, BF16), vm(tok, BF16), vm(tok, BF16), vm(tok, BF16), vm(tok, BF16),
                vm(tok_t, BF16), vm(tok_t, BF16), vm(tok_t, BF16), vm(tok_t, BF16), vm(tok_t, BF16),
                vm((4, SEQ, HEAD), BF16), vm((4, HEAD, SEQ), BF16),
                vm((PAIR, HEAD, HALF), F32), vm((PAIR, HEAD, HALF), F32), vm((4, PAIR, HALF, HEAD), BF16),
                dma, dma((2, SUBS)), dma, dma, dma, dma((4,)), dma((4,)), dma((SUBS,)), dma, dma((4,)),
                dma, dma((2,)), dma, dma((2,)), dma, dma((2, 4)), dma, dma,
                dma, dma, dma((2,)), dma((2,)), dma((2,)), dma, dma,
            ],
            compiler_params=pltpu.CompilerParams(collective_id=0, has_side_effects=True, vmem_limit_bytes=37 * 1024 * 1024),
        )(*[pltpu.with_memory_space_constraint(x, pltpu.HBM) for x in (
            query.reshape(pairs), key_in.reshape(pairs), value.reshape(pairs), d_out.reshape(pairs),
            rel_k.reshape(SEQ, N_PAIR, PAIR, head_dim), bias_u.reshape(N_PAIR, PAIR, head_dim), bias_w.reshape(N_PAIR, PAIR, head_dim))])
        o, dq, dk, dv, dr, du, dw = pl.pallas_call(
            writer,
            name="writer",
            out_shape=(act, act, act, act, jax.ShapeDtypeStruct((SEQ, n_heads, 1, head_dim), F32), vec, vec),
            in_specs=[whole] * (4 + N_PART),
            out_specs=[whole] * 7,
            scratch_shapes=[dma((6 + 2 * N_PART,))],
            compiler_params=pltpu.CompilerParams(vmem_limit_bytes=1024 * 1024),
        )(*outs[:-1])
        full = query.shape
        return (o.reshape(full), dq.reshape(full), dk.reshape(full), dv.reshape(full),
                du.reshape(bias_u.shape), dw.reshape(bias_w.shape), dr.reshape(rel_k.shape))

    return jax.shard_map(local, mesh=mesh,
                         in_specs=(seq_spec, seq_spec, seq_spec, P(), P(), P(), seq_spec),
                         out_specs=(seq_spec, seq_spec, seq_spec, seq_spec, P(), P(), P()),
                         check_vma=False)
```

```python
import jax
import jax.numpy as jnp
from jax import lax
from jax.experimental import pallas as pl
from jax.experimental.pallas import tpu as pltpu
from jax.sharding import PartitionSpec as P

MESH = pl.DeviceIdType.MESH
BF16, F32 = jnp.bfloat16, jnp.float32
LOG2E = 1.4426950408889634

N_DEV = 16
PLANE = 8
PAIR = 2
N_PAIR = 8
SLOTS = 4
SUBS = 2 * SLOTS
EARLY = 3
ROWS = 64
HALF = PLANE * ROWS
SEQ = 2 * HALF
HEAD = 128
QB = 256
WIN = HALF + QB
N_PART = 6
PART = 86
FIN = N_PART * PART
TIP = 2 * ROWS
FAR = N_PAIR - 2
UNITS = FAR * SLOTS
TURNS = ((1, 3, 2), (3, 1, 2))


def dot(lhs, rhs):
    return jnp.dot(lhs, rhs, preferred_element_type=F32)


def flip8(x):
    rows, cols = x.shape
    idx = 7 - lax.broadcasted_iota(jnp.int32, (rows // 8, 8, cols), 1)
    return jnp.take_along_axis(x.reshape(rows // 8, 8, cols), idx, axis=1).reshape(rows, cols)


def eye_rev(dtype):
    total = lax.broadcasted_iota(jnp.int32, (HEAD, HEAD), 0) + lax.broadcasted_iota(jnp.int32, (HEAD, HEAD), 1)
    return jnp.where(total == HEAD - 1, 1.0, 0.0).astype(dtype)


def kernel(q_in, k_in, v_in, g_in, r_in, u_in, w_in,
           o_out, dq_out, dk_out, dv_out, dr0_out, dr1_out, dr2_out, dr3_out, dr4_out, dr5_out, far_out,
           buf, rbuf, r_buf, u_buf, w_buf, st_tx, st_rx, tip_st, st_ref, dr_rx, dr_rz, dr_fin, dr_acc,
           s_ref, e_ref, dp_ref, pb_ref, ds_ref, dd_ref,
           a_s, c_s, g_s, k_s, v_s, at_s, ct_s, gt_s, kt_s, vt_s, rev_s, rt_s, dkt, dvt, stage,
           in_send, in_recv, out_send, out_recv, own_sem, r_sem, up_send, up_recv, st_send, st_recv,
           x_send, x_recv, z_send, z_recv, ring_send, ring_recv, fw_send, fw_recv,
           far_send, far_recv, tip_sem, tip_near, tip_send, ts_send, ts_recv):
    me = lax.axis_index("cp")
    core = me % 2
    chip = me // 2
    col = chip % 4
    z = chip // 4
    partner = me + 1 - 2 * core
    across = me + PLANE * (1 - 2 * z)
    scale = HEAD ** -0.5

    def wait_for(ref, sem):
        pltpu.make_async_copy(ref, ref, sem).wait()

    y = col // 2
    lower, upper = z == 0, z == 1
    tip = chip == 7 * z
    tip_base = 2 - 2 * z

    tables = [pltpu.make_async_copy(src, dst, r_sem.at[j]) for j, (src, dst) in enumerate(
        ((r_in.at[:, 2 * col], r_buf.at[0]), (r_in.at[:, 2 * col + 1], r_buf.at[1]), (u_in, u_buf), (w_in, w_buf)))]
    for copy in tables:
        copy.start()

    barrier = pltpu.get_barrier_semaphore()

    for peer in [across] + [me ^ step for step in range(PLANE - 1, 0, -1)]:
        pl.semaphore_signal(barrier, inc=1, device_id=(peer,), device_id_type=MESH)
    pl.semaphore_wait(barrier, PLANE)

    my_rows = pl.ds(pl.multiple_of((me % PLANE) * ROWS, ROWS), ROWS)

    even = chip % 2 == z
    loaded = y != z

    def peers(late=False):
        near, last = core == 0, 0
        if late:
            lone = loaded & jnp.logical_not(even)
            last = jnp.where(near & lone & upper, 1, 0)
            near = jnp.where(lone, near & upper, jnp.logical_not(near))
        first, second, third = [jnp.where(near, near_turn, far_turn) for near_turn, far_turn in zip(*TURNS)]
        for turn, other in ((first, 0), (third, 0), (first, 1), (third, 1), (second, last), (second, 1 - last)):
            yield me ^ (2 * turn + other)
        yield partner

    def send_in(ins, sub):
        pair, row = sub // SLOTS, sub % SLOTS
        for first in (0, 2):
            for t in (first, first + 1):
                pltpu.make_async_copy(ins[t].at[core * SLOTS + row, :, 2 * col + pair], buf.at[t, sub, my_rows], in_recv.at[first // 2, sub]).start()
            for peer in peers():
                for t in (first, first + 1):
                    pltpu.make_async_remote_copy(
                        src_ref=ins[t].at[(peer % 2) * SLOTS + row, :, 2 * ((peer // 2) % 4) + pair], dst_ref=buf.at[t, sub, my_rows],
                        send_sem=in_send, recv_sem=in_recv.at[first // 2, sub], device_id=(peer,), device_id_type=MESH).start()

    def send_all(ins):
        def send_sub(sub, carry):
            send_in(ins, sub)
            return carry
        lax.fori_loop(0, SUBS, send_sub, 0)

    @pl.when(lower)
    def _():
        send_all((k_in, v_in, q_in, g_in))

    @pl.when(upper)
    def _():
        send_all((q_in, g_in, k_in, v_in))

    @pl.when(tip)
    def _():
        for t, src in enumerate((q_in, k_in, v_in, g_in)):
            for row in range(SLOTS):
                pltpu.make_async_remote_copy(
                    src_ref=src.at[(1 - core) * SLOTS + row, :, pl.ds(tip_base, FAR)], dst_ref=far_out.at[t, row],
                    send_sem=far_send, recv_sem=far_recv, device_id=(partner,), device_id_type=MESH).start()

    for copy in tables:
        copy.wait()
    rev = eye_rev(BF16)
    for p in range(2):
        pair_tab = pltpu.einshape("abc->bac", r_buf[p])
        for hh in range(PAIR):
            for blk in range(SEQ // HEAD):
                part = pair_tab[hh, SEQ - HEAD * (blk + 1):SEQ - HEAD * blk]
                flipped = dot(rev, part).astype(BF16)
                rev_s[2 * p + hh, HEAD * blk:HEAD * (blk + 1), :] = flipped
                rt_s[2 * p + hh, :, HEAD * blk:HEAD * (blk + 1)] = flipped.T
    dr_acc[...] = jnp.zeros_like(dr_acc)

    acts = (dk_out, dv_out, o_out, dq_out)

    def send_out(sub, which, late=False):
        place = (core * SLOTS + sub % SLOTS, slice(None), 2 * col + sub // SLOTS)
        for t in which:
            pltpu.make_async_copy(buf.at[t, sub, my_rows], acts[t].at[place], out_recv).start()
        for peer in peers(late):
            peer_rows = pl.ds(pl.multiple_of((peer % PLANE) * ROWS, ROWS), ROWS)
            to_tip = (peer // 2 == 7 * z) & jnp.logical_not(tip)
            for t in which:
                @pl.when(jnp.logical_not(to_tip & (lower if t >= 2 else upper)))
                def _():
                    pltpu.make_async_remote_copy(
                        src_ref=buf.at[t, sub, peer_rows], dst_ref=acts[t].at[place],
                        send_sem=out_send, recv_sem=out_recv, device_id=(peer,), device_id_type=MESH).start()

    def send_up(sub):
        wait_for(buf.at[0:2, sub], in_recv.at[0, sub])
        for j in range(2):
            pltpu.make_async_remote_copy(src_ref=buf.at[j, sub], dst_ref=rbuf.at[j, sub], send_sem=up_send.at[sub % 4], recv_sem=up_recv.at[sub],
                                         device_id=(across,), device_id_type=MESH).start()

    def unpack(ref, j, sub):
        return pltpu.einshape("abc->bac", ref[j, sub])

    def load_rows(q_ref, q_j, g_ref, g_j, sub, start, turned):
        rows = slice(start, start + HALF)
        p = sub // SLOTS
        q2 = unpack(q_ref, q_j, sub)
        u = u_buf[2 * col + p].astype(F32)
        w = w_buf[2 * col + p].astype(F32)
        for hh in range(PAIR):
            q32 = q2[hh].astype(F32)
            a = (q32 + u[hh:hh + 1]).astype(BF16)
            c = (q32 + w[hh:hh + 1]).astype(BF16)
            a_s[hh, rows, :] = a
            c_s[hh, rows, :] = c
            at_s[hh, :, rows] = a.T
            if turned:
                ct_s[hh, :, rows] = flip8(c.astype(F32)).astype(BF16).T
        g2 = unpack(g_ref, g_j, sub)
        g_s[:, rows, :] = g2
        for hh in range(PAIR):
            gt_s[hh, :, rows] = g2[hh].T

    def load_keys(k_ref, k_j, v_ref, v_j, sub, start):
        rows = slice(start, start + HALF)
        k2 = unpack(k_ref, k_j, sub)
        v2 = unpack(v_ref, v_j, sub)
        k_s[:, rows, :] = k2
        v_s[:, rows, :] = v2
        for hh in range(PAIR):
            kt_s[hh, :, rows] = k2[hh].T
            vt_s[hh, :, rows] = v2[hh].T

    def row_block(hh, head, start, i0, lo, fresh, stats):
        width = i0 + QB
        rows = slice(start, start + QB)
        s_ref[:, :width] = dot(a_s[hh, rows, :], kt_s[hh, :, :width])
        e_ref[:, :width] = dot(c_s[hh, rows, :], rt_s[head, :, SEQ - width:])
        dp_ref[:, :width] = dot(g_s[hh, rows, :], vt_s[hh, :, :width])
        for r0 in range(0, QB, 16):
            group = slice(r0, r0 + 16)
            rel = pltpu.roll(e_ref[group, :width], i0 + 1 + r0, 1, stride=1, stride_axis=0)
            s = s_ref[group, :width] + rel
            ahead = lax.broadcasted_iota(jnp.int32, (16, width), 1) - lax.broadcasted_iota(jnp.int32, (16, width), 0)
            s = jnp.where(ahead <= i0 + r0, s, -jnp.inf)
            top = jnp.max(s, axis=1, keepdims=True)
            p = jnp.exp2((s - top) * (scale * LOG2E))
            total = jnp.sum(p, axis=1, keepdims=True)
            p = p * (1.0 / total)
            pb_ref[group, :width] = p.astype(BF16)
            dp = dp_ref[group, :width]
            row_dot = jnp.sum(p * dp, axis=1, keepdims=True)
            ds = (p * (dp - row_dot) * scale).astype(BF16)
            ds_ref[group, :width] = ds
            flipped = flip8(ds.astype(F32))
            half = [pltpu.roll(flipped[8 * j:8 * j + 8], QB - 8 - r0 - 8 * j, 1, stride=1, stride_axis=0) for j in range(2)]
            dd_ref[group, :width] = jnp.concatenate(half, axis=0).astype(BF16)
            if stats:
                lane = lax.broadcasted_iota(jnp.int32, (16, HEAD), 1)
                st_ref[group, :] = jnp.where(lane == 0, top * (scale * LOG2E) + jnp.log2(total), row_dot)
        pb = pb_ref[:, :width]
        ds = ds_ref[:, :width]
        dd = dd_ref[:, :width]
        stage[0, hh, rows, :] = dot(pb, v_s[hh, :width, :]).astype(BF16)
        dqc = dot(ds, k_s[hh, :width, :])
        dqr = flip8(dot(dd, rev_s[head, SEQ - width:, :]))
        stage[1, hh, rows, :] = (dqc + dqr).astype(BF16)
        dr_acc[head, 1, HEAD:HEAD + 1, HALF - HEAD:] += jnp.sum(dqc, axis=0, keepdims=True)
        dr_acc[head, 1, HEAD + 1:HEAD + 2, HALF - HEAD:] += jnp.sum(dqr, axis=0, keepdims=True)
        dk_new = dot(at_s[hh, :, rows], ds_ref[:, lo:width])
        dv_new = dot(gt_s[hh, :, rows], pb_ref[:, lo:width])
        if fresh:
            dkt[hh] = dk_new
            dvt[hh] = dv_new
        else:
            dkt[hh, :, :width - lo] += dk_new
            dvt[hh, :, :width - lo] += dv_new
        dr_new = dot(ct_s[hh, :, rows], dd)
        if width > HALF:
            dr_acc[head, 0, :HEAD, SEQ - width:] += dr_new[:, :width - HALF]
            dr_acc[head, 1, :HEAD, :] += dr_new[:, width - HALF:]
        else:
            dr_acc[head, 1, :HEAD, HALF - width:] += dr_new

    def col_block(hh, head, sub, i0):
        rows = slice(i0, i0 + QB)
        first = WIN - i0
        s_ref[:, :HALF] = dot(a_s[hh, rows, :], kt_s[hh, :, :HALF])
        e_ref[:, :WIN] = dot(c_s[hh, rows, :], rt_s[head, :, first:first + WIN])
        dp_ref[:, :HALF] = dot(g_s[hh, rows, :], vt_s[hh, :, :HALF])
        st_ref[:, :8] = st_rx[sub, hh, :, i0 - HALF:i0 - HALF + QB].T
        for r0 in range(0, QB, 16):
            group = slice(r0, r0 + 16)
            rel = pltpu.roll(e_ref[group, :WIN], HALF + 1 + r0, 1, stride=1, stride_axis=0)[:, :HALF]
            log_sum = st_ref[group, 0:1]
            row_dot = st_ref[group, 1:2]
            p = jnp.exp2((s_ref[group, :HALF] + rel) * (scale * LOG2E) - log_sum)
            pb_ref[group, :HALF] = p.astype(BF16)
            ds_ref[group, :HALF] = (p * (dp_ref[group, :HALF] - row_dot) * scale).astype(BF16)
        dkt[hh] += dot(at_s[hh, :, rows], ds_ref[:, :HALF])
        dvt[hh] += dot(gt_s[hh, :, rows], pb_ref[:, :HALF])

    def store_rows(sub):
        for t in range(2):
            buf[2 + t, sub] = pltpu.einshape("abc->bac", stage[t])

    def store_keys(sub):
        for hh in range(PAIR):
            stage[2, hh] = dkt[hh].astype(BF16).T
            stage[3, hh] = dvt[hh].astype(BF16).T
        for t in range(2):
            buf[t, sub] = pltpu.einshape("abc->bac", stage[2 + t])

    def wait_up(sub):
        wait_for(rbuf.at[:, sub], up_recv.at[sub])
        wait_for(rbuf.at[:, sub], up_send.at[sub % 4])

    def wait_in(sub):
        wait_for(buf.at[2:4, sub], in_recv.at[1, sub])

    def lower_rows(sub):
        wait_in(sub)
        load_rows(buf, 2, buf, 3, sub, 0, True)

    def lower_own(sub):
        load_keys(buf, 0, buf, 1, sub, 0)

        def own(hh, carry):
            head = 2 * (sub // SLOTS) + hh
            row_block(hh, head, QB, QB, 0, True, False)
            row_block(hh, head, 0, 0, 0, False, False)
            return carry

        lax.fori_loop(0, PAIR, own, 0)
        store_rows(sub)

    def lower_theirs(sub):
        wait_up(sub)
        load_rows(rbuf, 0, rbuf, 1, sub, HALF, False)
        wait_for(st_rx.at[sub], st_recv.at[sub % 4])

        def theirs(hh, carry):
            head = 2 * (sub // SLOTS) + hh
            col_block(hh, head, sub, HALF)
            col_block(hh, head, sub, HALF + QB)
            return carry

        lax.fori_loop(0, PAIR, theirs, 0)
        store_keys(sub)

    def upper_own(sub):
        wait_in(sub)
        wait_up(sub)
        load_rows(buf, 0, buf, 1, sub, 0, True)
        load_keys(rbuf, 0, rbuf, 1, sub, 0)
        load_keys(buf, 2, buf, 3, sub, HALF)

        def own(hh, carry):
            head = 2 * (sub // SLOTS) + hh
            for blk in (1, 0):
                row_block(hh, head, QB * blk, HALF + QB * blk, HALF, blk == 1, True)
                st_tx[sub, hh, :, QB * blk:QB * (blk + 1)] = st_ref[...].T[:8]
            pltpu.make_async_remote_copy(src_ref=st_tx.at[sub, hh], dst_ref=st_rx.at[sub, hh], send_sem=st_send, recv_sem=st_recv.at[sub % 4],
                                         device_id=(across,), device_id_type=MESH).start()

            @pl.when(jnp.logical_not(tip))
            def _():
                pltpu.make_async_remote_copy(src_ref=st_tx.at[sub, hh, :, HALF - TIP:], dst_ref=tip_st.at[col, sub, hh], send_sem=ts_send,
                                             recv_sem=ts_recv, device_id=(N_DEV - 2 + core,), device_id_type=MESH).start()
            return carry

        lax.fori_loop(0, PAIR, own, 0)
        store_rows(sub)
        store_keys(sub)

    side = 1 - core
    parts = (dr0_out, dr1_out, dr2_out, dr3_out, dr4_out, dr5_out)

    def swap_start(p):
        for n in range(2):
            pltpu.make_async_remote_copy(src_ref=dr_acc.at[2 * p + n, side], dst_ref=dr_rx.at[p, n], send_sem=x_send, recv_sem=x_recv.at[p],
                                         device_id=(partner,), device_id_type=MESH).start()

    def swap_add(p):
        wait_for(dr_rx.at[p], x_recv.at[p])
        for n in range(2):
            dr_rx[p, n] = dr_rx[p, n] + dr_acc[2 * p + n, core]

    def cross_start(p):
        pltpu.make_async_remote_copy(src_ref=dr_rx.at[p, 1 - z], dst_ref=dr_rz.at[p], send_sem=z_send, recv_sem=z_recv.at[p],
                                     device_id=(across,), device_id_type=MESH).start()

    def head_of(p, bits):
        other = chip ^ bits
        return 4 * (other % 4) + 2 * p + other // 4

    def block(p, m, bits):
        if bits == 0:
            return dr_fin.at[p, PART * m:PART * (m + 1)]
        return parts[m].at[side, :, head_of(p, bits)]

    def forward(p, m, bits):
        pltpu.make_async_remote_copy(src_ref=block(p, m, bits), dst_ref=parts[m].at[side, :, head_of(p, bits)], send_sem=fw_send,
                                     recv_sem=fw_recv, device_id=(partner,), device_id_type=MESH).start()

    def blocks(count):
        return parts[0].at[:, :, :N_PART // 2 * count]

    def pass_on(p, bits, hop, device):
        for m in range(N_PART):
            pltpu.make_async_remote_copy(
                src_ref=block(p, m, bits), dst_ref=parts[m].at[side, :, head_of(p, bits)], send_sem=ring_send,
                recv_sem=ring_recv.at[p, hop], device_id=(device,), device_id_type=MESH).start()

    def hand_over(p, bits):
        for m in range(N_PART):
            forward(p, m, bits)

    along_x, along_y = me ^ 2, me ^ 4

    def hop_start(p, hop):
        if hop == 0:
            for device in (along_x, along_y, across):
                pass_on(p, 0, 0, device)
        if hop == 1:
            @pl.when(even & loaded)
            def _():
                pass_on(p, 1, 1, along_y)

            @pl.when(jnp.logical_not(even) & loaded)
            def _():
                pass_on(p, 2, 1, along_x)

            pass_on(p, 1, 1, across)
            pass_on(p, 2, 1, across)
        if hop == 2:
            @pl.when(even & loaded)
            def _():
                pass_on(p, 5, 2, along_y)

            @pl.when(jnp.logical_not(even) & loaded)
            def _():
                pass_on(p, 6, 2, along_x)

            @pl.when(even)
            def _():
                pass_on(p, 3, 2, across)
        if hop == 3:
            @pl.when(even)
            def _():
                pass_on(p, 7, 3, across)

    def hop_wait(p, hop):
        if hop == 0:
            wait_for(blocks(3), ring_recv.at[p, 0])
            for bits in (1, 2, 4):
                hand_over(p, bits)
        if hop == 1:
            @pl.when(even)
            def _():
                wait_for(blocks(3), ring_recv.at[p, 1])
                hand_over(p, 3)

            @pl.when(jnp.logical_not(even))
            def _():
                wait_for(blocks(2), ring_recv.at[p, 1])
            for bits in (5, 6):
                hand_over(p, bits)
        if hop == 2:
            wait_for(blocks(1), ring_recv.at[p, 2])
            hand_over(p, 7)
        if hop == 3:
            @pl.when(jnp.logical_not(even))
            def _():
                wait_for(blocks(1), ring_recv.at[p, 3])
                hand_over(p, 3)

    def sent_wait():
        @pl.when(even & loaded)
        def _():
            wait_for(buf.at[:3, :, :FIN * 18 // 24], ring_send)

        @pl.when(even != loaded)
        def _():
            wait_for(buf.at[:3, :7, :FIN * 14 // 21], ring_send)

        @pl.when(jnp.logical_not(even | loaded))
        def _():
            wait_for(buf.at[:2, :6, :FIN * 10 // 12], ring_send)

    def cross_finish(p):
        wait_for(dr_rz.at[p], z_recv.at[p])
        total = dr_rx[p, z] + dr_rz[p]
        rev32 = eye_rev(F32)
        for m in range(HALF // HEAD):
            part = total[:HEAD, HALF - HEAD * (m + 1):HALF - HEAD * m]
            turned = lax.dot_general(rev32, part, (((1,), (1,)), ((), ())), precision=lax.Precision.HIGHEST, preferred_element_type=F32)
            dr_fin[p, HEAD * m:HEAD * (m + 1)] = turned.reshape(HEAD, 1, HEAD)
        dr_fin[p, HALF] = total[HEAD:HEAD + 1, HALF - HEAD:]
        dr_fin[p, HALF + 1] = total[HEAD + 1:HEAD + 2, HALF - HEAD:]
        dr_fin[p, HALF + 2:] = jnp.zeros((FIN - HALF - 2, 1, HEAD), F32)
        hop_start(p, 0)
        for m in range(N_PART):
            pltpu.make_async_copy(block(p, m, 0), parts[m].at[side, :, head_of(p, 0)], own_sem).start()
        hand_over(p, 0)

    def tip_load(unit):
        slot, row, far = unit % 2, unit // FAR, unit % FAR
        pair = far + tip_base
        for t, src in enumerate((q_in, k_in, v_in, g_in)):
            pltpu.make_async_copy(src.at[core * SLOTS + row, :, pair], r_buf.at[slot, pl.ds(TIP * t + ROWS * core, ROWS)], tip_sem.at[slot]).start()
            pltpu.make_async_copy(far_out.at[t, row, :, far], r_buf.at[slot, pl.ds(TIP * t + ROWS * (1 - core), ROWS)], tip_sem.at[slot]).start()
        pltpu.make_async_copy(r_in.at[:TIP, pair], r_buf.at[slot, 4 * TIP:5 * TIP], tip_sem.at[slot]).start()

    def tip_done(slot):
        wait_for(r_buf.at[slot, :TIP], tip_near.at[slot])
        wait_for(r_buf.at[slot, :TIP], tip_send.at[slot])

    def tip_group(hh, r0):
        group = slice(TIP * hh + r0, TIP * hh + r0 + 16)
        rel = pltpu.roll(e_ref[group, :TIP], 1 + r0, 1, stride=1, stride_axis=0)
        ahead = lax.broadcasted_iota(jnp.int32, (16, TIP), 1) - lax.broadcasted_iota(jnp.int32, (16, TIP), 0)
        return group, s_ref[group, :TIP] + rel, ahead <= r0

    def tip_rows(hh):
        for r0 in range(0, TIP, 16):
            group, s, seen = tip_group(hh, r0)
            s = jnp.where(seen, s, -jnp.inf)
            top = jnp.max(s, axis=1, keepdims=True)
            p = jnp.exp2((s - top) * (scale * LOG2E))
            p = p * (1.0 / jnp.sum(p, axis=1, keepdims=True))
            pb_ref[group, :TIP] = p.astype(BF16)
            dp = dp_ref[group, :TIP]
            row_dot = jnp.sum(p * dp, axis=1, keepdims=True)
            ds = (p * (dp - row_dot) * scale).astype(BF16)
            ds_ref[group, :TIP] = ds
            flipped = flip8(ds.astype(F32))
            half = [pltpu.roll(flipped[8 * j:8 * j + 8], TIP - 8 - r0 - 8 * j, 1, stride=1, stride_axis=0) for j in range(2)]
            dd_ref[group, :TIP] = jnp.concatenate(half, axis=0).astype(BF16)
        rows = slice(TIP * hh, TIP * (hh + 1))
        stage[0, hh, :TIP, :] = dot(pb_ref[rows, :TIP], v_s[hh, :TIP, :]).astype(BF16)
        dqc = dot(ds_ref[rows, :TIP], k_s[hh, :TIP, :])
        dqr = flip8(dot(dd_ref[rows, :TIP], c_s[hh, :TIP, :]))
        stage[1, hh, :TIP, :] = (dqc + dqr).astype(BF16)

    def tip_keys(hh, stats):
        rows = slice(TIP * hh, TIP * (hh + 1))
        st_ref[rows, :8] = stats.T
        for r0 in range(0, TIP, 16):
            group, s, seen = tip_group(hh, r0)
            p = jnp.where(seen, jnp.exp2(s * (scale * LOG2E) - st_ref[group, 0:1]), 0.0)
            pb_ref[group, :TIP] = p.astype(BF16)
            ds_ref[group, :TIP] = (p * (dp_ref[group, :TIP] - st_ref[group, 1:2]) * scale).astype(BF16)
        over_rows = (((0,), (0,)), ((), ()))
        stage[0, hh, :TIP, :] = lax.dot_general(ds_ref[rows, :TIP], a_s[hh, :TIP, :], over_rows, preferred_element_type=F32).astype(BF16)
        stage[1, hh, :TIP, :] = lax.dot_general(pb_ref[rows, :TIP], g_s[hh, :TIP, :], over_rows, preferred_element_type=F32).astype(BF16)

    def tip_unit(unit, carry):
        slot, row, far = unit % 2, unit // FAR, unit % FAR
        pair = far + tip_base
        wait_for(r_buf.at[slot, :5 * TIP], tip_sem.at[slot])

        @pl.when(unit + 1 < UNITS)
        def _():
            tip_load(unit + 1)

        q2, k2, v2, g2, r2 = [pltpu.einshape("abc->bac", r_buf[slot, TIP * t:TIP * (t + 1)]) for t in range(5)]
        u = u_buf[pair].astype(F32)
        w = w_buf[pair].astype(F32)
        for hh in range(PAIR):
            rows = slice(TIP * hh, TIP * (hh + 1))
            q32 = q2[hh].astype(F32)
            a = (q32 + u[hh:hh + 1]).astype(BF16)
            c = (q32 + w[hh:hh + 1]).astype(BF16)
            falling = dot(eye_rev(BF16), r2[hh]).astype(BF16)
            s_ref[rows, :TIP] = dot(a, k2[hh].T)
            e_ref[rows, :TIP] = dot(c, falling.T)
            dp_ref[rows, :TIP] = dot(g2[hh], v2[hh].T)
            a_s[hh, :TIP, :] = a
            c_s[hh, :TIP, :] = falling
            g_s[hh, :TIP, :] = g2[hh]
            k_s[hh, :TIP, :] = k2[hh]
            v_s[hh, :TIP, :] = v2[hh]

        @pl.when(lower)
        def _():
            for hh in range(PAIR):
                tip_rows(hh)

        @pl.when(upper)
        def _():
            for hh in range(PAIR):
                tip_keys(hh, tip_st[far // 2, (far % 2) * SLOTS + row, hh])

        @pl.when(unit >= 2)
        def _():
            tip_done(slot)

        for n in range(2):
            r_buf[slot, (5 + n) * TIP:(6 + n) * TIP] = pltpu.einshape("abc->bac", stage[n, :, :TIP, :])
        place = (core * SLOTS + row, slice(None), pair)

        def give(results):
            for n, dst in enumerate(results):
                pltpu.make_async_copy(r_buf.at[slot, pl.ds((5 + n) * TIP + ROWS * core, ROWS)], dst.at[place], tip_near.at[slot]).start()
                pltpu.make_async_remote_copy(
                    src_ref=r_buf.at[slot, pl.ds((5 + n) * TIP + ROWS * (1 - core), ROWS)], dst_ref=dst.at[place],
                    send_sem=tip_send.at[slot], recv_sem=out_recv, device_id=(partner,), device_id_type=MESH).start()

        @pl.when(lower)
        def _():
            give((o_out, dq_out))

        @pl.when(upper)
        def _():
            give((dk_out, dv_out))
        return carry

    def tips(third):
        @pl.when(tip)
        def _():
            if third == 0:
                wait_for(far_out, far_recv)

                @pl.when(upper)
                def _():
                    wait_for(tip_st, ts_recv)
                tip_load(0)
            lax.fori_loop(UNITS // 3 * third, UNITS // 3 * (third + 1), tip_unit, 0)
            if third == 2:
                tip_done(0)
                tip_done(1)

    send_up(0)

    def sub_body(sub, carry):
        @pl.when(sub < SUBS - 1)
        def _():
            send_up(sub + 1)

        @pl.when(sub == SLOTS)
        def _():
            swap_start(0)

        @pl.when(sub == SUBS - 1)
        def _():
            swap_add(0)
            cross_start(0)

        @pl.when(sub == SUBS)
        def _():
            swap_start(1)
            swap_add(1)
            cross_start(1)
            cross_finish(0)

        @pl.when(lower & (sub < SUBS))
        def _():
            lower_rows(sub)

        @pl.when(lower & (sub > 0))
        def _():
            lower_theirs(sub - 1)

        @pl.when(lower & (sub < SUBS))
        def _():
            lower_own(sub)

        @pl.when(upper & (sub < SUBS))
        def _():
            upper_own(sub)

        @pl.when(sub <= EARLY)
        def _():
            send_out(sub, (2, 3))

        @pl.when((sub > 0) & (sub <= EARLY))
        def _():
            send_out(sub - 1, (0, 1))
        return carry

    lax.fori_loop(0, SUBS + 1, sub_body, 0)

    cross_finish(1)
    send_out(EARLY, (0, 1))
    for p in range(2):
        hop_wait(p, 0)
        hop_start(p, 1)
    for p in range(2):
        send_out(EARLY + 1 + p, range(4))
        tips(p)
        hop_wait(p, 1)
        hop_start(p, 2)

    def send_late(sub, carry):
        send_out(sub, range(4), True)
        return carry

    lax.fori_loop(EARLY + 3, SUBS, send_late, 0)
    tips(2)
    for p in range(2):
        hop_wait(p, 2)
        hop_start(p, 3)
    for p in range(2):
        hop_wait(p, 3)

    wait_for(buf.at[:, :, :HALF - ROWS], in_send)

    @pl.when(tip)
    def _():
        wait_for(buf.at[:, :, :HALF - 3 * ROWS // 2], out_recv)
        wait_for(buf.at[:, :, :HALF - ROWS], out_send)
        wait_for(far_out, far_send)

    @pl.when(jnp.logical_not(tip))
    def _():
        wait_for(buf, out_recv)
        wait_for(buf.at[:, :, :HALF - 2 * ROWS], out_send)

    @pl.when(upper & jnp.logical_not(tip))
    def _():
        wait_for(st_tx.at[:2], ts_send)

    @pl.when(upper)
    def _():
        wait_for(st_tx, st_send)

    wait_for(dr_rx, x_send)
    wait_for(dr_rz, z_send)
    wait_for(blocks(2), own_sem)
    sent_wait()
    for sem in (fw_send, fw_recv):
        wait_for(buf.at[:3, :, :FIN * 16 // 24], sem)


def writer(*refs):
    ins, (o, dq, dk, dv, dr, du, dw, sem) = refs[:4 + N_PART], refs[4 + N_PART:]
    pairs = list(zip(ins[:4], (o, dq, dk, dv)))
    for m, part in enumerate(ins[4:]):
        rows = min(PART, HALF - PART * m)
        for side in range(2):
            start = HALF * side + PART * m
            pairs.append((part.at[side, :rows], dr.at[start:start + rows]))
    last = HALF - PART * (N_PART - 1)
    pairs += [(ins[-1].at[0, last], du), (ins[-1].at[0, last + 1], dw)]
    copies = [pltpu.make_async_copy(src, dst, sem.at[j]) for j, (src, dst) in enumerate(pairs)]
    for copy in copies:
        copy.start()
    for copy in copies:
        copy.wait()


def solution(mesh):
    seq_spec = P(None, "cp", None, None)

    def local(query, key_in, value, bias_u, bias_w, rel_k, d_out):
        n_batch, rows, n_heads, head_dim = query.shape
        pairs = (n_batch, rows, N_PAIR, PAIR, head_dim)
        vm = pltpu.VMEM
        dma = pltpu.SemaphoreType.DMA
        whole = pl.BlockSpec(memory_space=pl.ANY)
        act = jax.ShapeDtypeStruct(pairs, BF16)
        vec = jax.ShapeDtypeStruct((n_heads, 1, head_dim), F32)
        tok = (PAIR, SEQ, HEAD)
        tok_t = (PAIR, HEAD, SEQ)
        acc = (HEAD + 8, HALF)
        outs = pl.pallas_call(
            kernel,
            name="rel_attn",
            out_shape=(act, act, act, act,
                       *[jax.ShapeDtypeStruct((2, PART, n_heads, 1, head_dim), F32)] * N_PART,
                       jax.ShapeDtypeStruct((4, SLOTS, ROWS, FAR, PAIR, HEAD), BF16)),
            in_specs=[pl.BlockSpec(memory_space=pltpu.HBM)] * 7,
            out_specs=[whole] * (5 + N_PART),
            scratch_shapes=[
                vm((4, SUBS, HALF, PAIR, HEAD), BF16), vm((2, SUBS, HALF, PAIR, HEAD), BF16),
                vm((2, SEQ, PAIR, HEAD), BF16), vm((N_PAIR, PAIR, HEAD), BF16), vm((N_PAIR, PAIR, HEAD), BF16),
                vm((SUBS, PAIR, 8, HALF), F32), vm((SUBS, PAIR, 8, HALF), F32), vm((3, SUBS, PAIR, 8, TIP), F32), vm((QB, HEAD), F32),
                vm((2, 2) + acc, F32), vm((2,) + acc, F32), vm((2, FIN, 1, HEAD), F32), vm((4, 2) + acc, F32),
                vm((QB, SEQ), F32), vm((QB, SEQ), F32), vm((QB, SEQ), F32),
                vm((QB, SEQ), BF16), vm((QB, SEQ), BF16), vm((QB, SEQ), BF16),
                vm(tok, BF16), vm(tok, BF16), vm(tok, BF16), vm(tok, BF16), vm(tok, BF16),
                vm(tok_t, BF16), vm(tok_t, BF16), vm(tok_t, BF16), vm(tok_t, BF16), vm(tok_t, BF16),
                vm((4, SEQ, HEAD), BF16), vm((4, HEAD, SEQ), BF16),
                vm((PAIR, HEAD, HALF), F32), vm((PAIR, HEAD, HALF), F32), vm((4, PAIR, HALF, HEAD), BF16),
                dma, dma((2, SUBS)), dma, dma, dma, dma((4,)), dma((4,)), dma((SUBS,)), dma, dma((4,)),
                dma, dma((2,)), dma, dma((2,)), dma, dma((2, 4)), dma, dma,
                dma, dma, dma((2,)), dma((2,)), dma((2,)), dma, dma,
            ],
            compiler_params=pltpu.CompilerParams(collective_id=0, has_side_effects=True, vmem_limit_bytes=37 * 1024 * 1024),
        )(*[pltpu.with_memory_space_constraint(x, pltpu.HBM) for x in (
            query.reshape(pairs), key_in.reshape(pairs), value.reshape(pairs), d_out.reshape(pairs),
            rel_k.reshape(SEQ, N_PAIR, PAIR, head_dim), bias_u.reshape(N_PAIR, PAIR, head_dim), bias_w.reshape(N_PAIR, PAIR, head_dim))])
        o, dq, dk, dv, dr, du, dw = pl.pallas_call(
            writer,
            name="writer",
            out_shape=(act, act, act, act, jax.ShapeDtypeStruct((SEQ, n_heads, 1, head_dim), F32), vec, vec),
            in_specs=[whole] * (4 + N_PART),
            out_specs=[whole] * 7,
            scratch_shapes=[dma((6 + 2 * N_PART,))],
            compiler_params=pltpu.CompilerParams(vmem_limit_bytes=1024 * 1024),
        )(*outs[:-1])
        full = query.shape
        return (o.reshape(full), dq.reshape(full), dk.reshape(full), dv.reshape(full),
                du.reshape(bias_u.shape), dw.reshape(bias_w.shape), dr.reshape(rel_k.shape))

    return jax.shard_map(local, mesh=mesh,
                         in_specs=(seq_spec, seq_spec, seq_spec, P(), P(), P(), seq_spec),
                         out_specs=(seq_spec, seq_spec, seq_spec, seq_spec, P(), P(), P()),
                         check_vma=False)
```

```python
import jax
import jax.numpy as jnp
from jax import lax
from jax.experimental import pallas as pl
from jax.experimental.pallas import tpu as pltpu
from jax.sharding import PartitionSpec as P

MESH = pl.DeviceIdType.MESH
BF16, F32 = jnp.bfloat16, jnp.float32
LOG2E = 1.4426950408889634

N_DEV = 16
BOTH = range(2)
PLANE = 8
PAIR = 2
N_PAIR = 8
SLOTS = 4
SUBS = 2 * SLOTS
EARLY = 3
ROWS = 64
HALF = PLANE * ROWS
SEQ = 2 * HALF
HEAD = 128
QB = 256
WIN = HALF + QB
N_PART = 6
PART = 86
FIN = N_PART * PART
TIP = 2 * ROWS
FAR = N_PAIR - 2
UNITS = FAR * SLOTS
TURNS = ((1, 3, 2), (3, 1, 2))


def dot(lhs, rhs):
    return jnp.dot(lhs, rhs, preferred_element_type=F32)


def flip8(x):
    rows, cols = x.shape
    idx = 7 - lax.broadcasted_iota(jnp.int32, (rows // 8, 8, cols), 1)
    return jnp.take_along_axis(x.reshape(rows // 8, 8, cols), idx, axis=1).reshape(rows, cols)


def eye_rev(dtype):
    total = lax.broadcasted_iota(jnp.int32, (HEAD, HEAD), 0) + lax.broadcasted_iota(jnp.int32, (HEAD, HEAD), 1)
    return jnp.where(total == HEAD - 1, 1.0, 0.0).astype(dtype)


def kernel(q_in, k_in, v_in, g_in, r_in, u_in, w_in,
           o_out, dq_out, dk_out, dv_out, dr0_out, dr1_out, dr2_out, dr3_out, dr4_out, dr5_out, far_out,
           buf, rbuf, r_buf, u_buf, w_buf, st_tx, st_rx, tip_tx, tip_st, st_ref, dr_rx, dr_rz, dr_fin, dr_acc,
           s_ref, e_ref, dp_ref, pb_ref, ds_ref, dd_ref,
           a_s, c_s, g_s, k_s, v_s, at_s, ct_s, gt_s, kt_s, vt_s, rev_s, rt_s, dkt, dvt, stage,
           in_send, in_recv, out_send, out_recv, own_sem, r_sem, up_send, up_recv, st_send, st_recv,
           x_send, x_recv, z_send, z_recv, ring_send, ring_recv, fw_send, fw_recv,
           far_send, far_recv, tip_sem, tip_near, tip_send, ts_send, ts_recv):
    me = lax.axis_index("cp")
    core = me % 2
    chip = me // 2
    col = chip % 4
    z = chip // 4
    partner = me + 1 - 2 * core
    across = me + PLANE * (1 - 2 * z)
    scale = HEAD ** -0.5

    def wait_for(ref, sem):
        pltpu.make_async_copy(ref, ref, sem).wait()

    y = col // 2
    lower, upper = z == 0, z == 1
    tip = chip == 7 * z
    tip_base = 2 - 2 * z

    tables = [pltpu.make_async_copy(src, dst, r_sem.at[j]) for j, (src, dst) in enumerate(
        ((r_in.at[:, 2 * col], r_buf.at[0]), (r_in.at[:, 2 * col + 1], r_buf.at[1]), (u_in, u_buf), (w_in, w_buf)))]
    for copy in tables:
        copy.start()

    barrier = pltpu.get_barrier_semaphore()

    for peer in [across] + [me ^ step for step in range(PLANE - 1, 0, -1)]:
        pl.semaphore_signal(barrier, inc=1, device_id=(peer,), device_id_type=MESH)
    pl.semaphore_wait(barrier, PLANE)

    my_rows = pl.ds(pl.multiple_of((me % PLANE) * ROWS, ROWS), ROWS)

    even = chip % 2 == z
    loaded = y != z

    def peers(late=False):
        near, last = core == 0, 0
        if late:
            lone = loaded & jnp.logical_not(even)
            last = jnp.where(near & lone & upper, 1, 0)
            near = jnp.where(lone, near & upper, jnp.logical_not(near))
        first, second, third = [jnp.where(near, near_turn, far_turn) for near_turn, far_turn in zip(*TURNS)]
        for turn, other in ((first, 0), (third, 0), (first, 1), (third, 1), (second, last), (second, 1 - last)):
            yield me ^ (2 * turn + other)
        yield partner

    def send_in(ins, sub):
        pair, row = sub // SLOTS, sub % SLOTS
        for first in (0, 2):
            for t in (first, first + 1):
                pltpu.make_async_copy(ins[t].at[core * SLOTS + row, :, 2 * col + pair], buf.at[t, sub, my_rows], in_recv.at[first // 2, sub]).start()
            for peer in peers():
                for t in (first, first + 1):
                    pltpu.make_async_remote_copy(
                        src_ref=ins[t].at[(peer % 2) * SLOTS + row, :, 2 * ((peer // 2) % 4) + pair], dst_ref=buf.at[t, sub, my_rows],
                        send_sem=in_send, recv_sem=in_recv.at[first // 2, sub], device_id=(peer,), device_id_type=MESH).start()

    def send_all(ins):
        def send_sub(sub, carry):
            send_in(ins, sub)
            return carry
        lax.fori_loop(0, SUBS, send_sub, 0)

    @pl.when(lower)
    def _():
        send_all((k_in, v_in, q_in, g_in))

    @pl.when(upper)
    def _():
        send_all((q_in, g_in, k_in, v_in))

    @pl.when(tip)
    def _():
        for t, src in enumerate((q_in, k_in, v_in, g_in)):
            for row in range(SLOTS):
                pltpu.make_async_remote_copy(
                    src_ref=src.at[(1 - core) * SLOTS + row, :, pl.ds(tip_base, FAR)], dst_ref=far_out.at[t, row],
                    send_sem=far_send, recv_sem=far_recv, device_id=(partner,), device_id_type=MESH).start()

    for copy in tables:
        copy.wait()
    rev = eye_rev(BF16)
    for p in BOTH:
        pair_tab = pltpu.einshape("abc->bac", r_buf[p])
        for hh in BOTH:
            for blk in range(SEQ // HEAD):
                part = pair_tab[hh, SEQ - HEAD * (blk + 1):SEQ - HEAD * blk]
                flipped = dot(rev, part).astype(BF16)
                rev_s[2 * p + hh, HEAD * blk:HEAD * (blk + 1), :] = flipped
                rt_s[2 * p + hh, :, HEAD * blk:HEAD * (blk + 1)] = flipped.T
    dr_acc[...] = jnp.zeros_like(dr_acc)

    acts = (dk_out, dv_out, o_out, dq_out)

    def send_out(sub, which, late=False):
        place = (core * SLOTS + sub % SLOTS, slice(None), 2 * col + sub // SLOTS)
        for t in which:
            pltpu.make_async_copy(buf.at[t, sub, my_rows], acts[t].at[place], out_recv).start()
        for peer in peers(late):
            peer_rows = pl.ds(pl.multiple_of((peer % PLANE) * ROWS, ROWS), ROWS)
            to_tip = (peer // 2 == 7 * z) & jnp.logical_not(tip)
            for t in which:
                @pl.when(jnp.logical_not(to_tip & (lower if t >= 2 else upper)))
                def _():
                    pltpu.make_async_remote_copy(
                        src_ref=buf.at[t, sub, peer_rows], dst_ref=acts[t].at[place],
                        send_sem=out_send, recv_sem=out_recv, device_id=(peer,), device_id_type=MESH).start()

    def send_up(sub):
        wait_for(buf.at[0:2, sub], in_recv.at[0, sub])
        for j in BOTH:
            pltpu.make_async_remote_copy(src_ref=buf.at[j, sub], dst_ref=rbuf.at[j, sub], send_sem=up_send.at[sub % 4], recv_sem=up_recv.at[sub],
                                         device_id=(across,), device_id_type=MESH).start()

    def unpack(ref, j, sub):
        return pltpu.einshape("abc->bac", ref[j, sub])

    def load_rows(q_ref, q_j, g_ref, g_j, sub, start, turned):
        rows = slice(start, start + HALF)
        p = sub // SLOTS
        q2 = unpack(q_ref, q_j, sub)
        u = u_buf[2 * col + p].astype(F32)
        w = w_buf[2 * col + p].astype(F32)
        for hh in BOTH:
            q32 = q2[hh].astype(F32)
            a = (q32 + u[hh:hh + 1]).astype(BF16)
            c = (q32 + w[hh:hh + 1]).astype(BF16)
            a_s[hh, rows, :] = a
            c_s[hh, rows, :] = c
            at_s[hh, :, rows] = a.T
            if turned:
                ct_s[hh, :, rows] = flip8(c.astype(F32)).astype(BF16).T
        g2 = unpack(g_ref, g_j, sub)
        g_s[:, rows, :] = g2
        for hh in BOTH:
            gt_s[hh, :, rows] = g2[hh].T

    def load_keys(k_ref, k_j, v_ref, v_j, sub, start):
        rows = slice(start, start + HALF)
        k2 = unpack(k_ref, k_j, sub)
        v2 = unpack(v_ref, v_j, sub)
        k_s[:, rows, :] = k2
        v_s[:, rows, :] = v2
        for hh in BOTH:
            kt_s[hh, :, rows] = k2[hh].T
            vt_s[hh, :, rows] = v2[hh].T

    def row_block(hh, head, start, i0, lo, fresh, stats):
        width = i0 + QB
        rows = slice(start, start + QB)
        s_ref[:, :width] = dot(a_s[hh, rows, :], kt_s[hh, :, :width])
        e_ref[:, :width] = dot(c_s[hh, rows, :], rt_s[head, :, SEQ - width:])
        dp_ref[:, :width] = dot(g_s[hh, rows, :], vt_s[hh, :, :width])
        for r0 in range(0, QB, 16):
            group = slice(r0, r0 + 16)
            rel = pltpu.roll(e_ref[group, :width], i0 + 1 + r0, 1, stride=1, stride_axis=0)
            s = s_ref[group, :width] + rel
            ahead = lax.broadcasted_iota(jnp.int32, (16, width), 1) - lax.broadcasted_iota(jnp.int32, (16, width), 0)
            s = jnp.where(ahead <= i0 + r0, s, -jnp.inf)
            top = jnp.max(s, axis=1, keepdims=True)
            p = jnp.exp2((s - top) * (scale * LOG2E))
            total = jnp.sum(p, axis=1, keepdims=True)
            p = p * (1.0 / total)
            pb_ref[group, :width] = p.astype(BF16)
            dp = dp_ref[group, :width]
            row_dot = jnp.sum(p * dp, axis=1, keepdims=True)
            ds = (p * (dp - row_dot) * scale).astype(BF16)
            ds_ref[group, :width] = ds
            flipped = flip8(ds.astype(F32))
            half = [pltpu.roll(flipped[8 * j:8 * j + 8], QB - 8 - r0 - 8 * j, 1, stride=1, stride_axis=0) for j in range(2)]
            dd_ref[group, :width] = jnp.concatenate(half, axis=0).astype(BF16)
            if stats:
                lane = lax.broadcasted_iota(jnp.int32, (16, HEAD), 1)
                st_ref[group, :] = jnp.where(lane == 0, top * (scale * LOG2E) + jnp.log2(total), row_dot)
        pb = pb_ref[:, :width]
        ds = ds_ref[:, :width]
        dd = dd_ref[:, :width]
        stage[0, hh, rows, :] = dot(pb, v_s[hh, :width, :]).astype(BF16)
        dqc = dot(ds, k_s[hh, :width, :])
        dqr = flip8(dot(dd, rev_s[head, SEQ - width:, :]))
        stage[1, hh, rows, :] = (dqc + dqr).astype(BF16)
        dr_acc[head, 1, HEAD:HEAD + 1, HALF - HEAD:] += jnp.sum(dqc, axis=0, keepdims=True)
        dr_acc[head, 1, HEAD + 1:HEAD + 2, HALF - HEAD:] += jnp.sum(dqr, axis=0, keepdims=True)
        dk_new = dot(at_s[hh, :, rows], ds_ref[:, lo:width])
        dv_new = dot(gt_s[hh, :, rows], pb_ref[:, lo:width])
        if fresh:
            dkt[hh] = dk_new
            dvt[hh] = dv_new
        else:
            dkt[hh, :, :width - lo] += dk_new
            dvt[hh, :, :width - lo] += dv_new
        dr_new = dot(ct_s[hh, :, rows], dd)
        if width > HALF:
            dr_acc[head, 0, :HEAD, SEQ - width:] += dr_new[:, :width - HALF]
            dr_acc[head, 1, :HEAD, :] += dr_new[:, width - HALF:]
        else:
            dr_acc[head, 1, :HEAD, HALF - width:] += dr_new

    def col_block(hh, head, sub, i0):
        rows = slice(i0, i0 + QB)
        first = WIN - i0
        s_ref[:, :HALF] = dot(a_s[hh, rows, :], kt_s[hh, :, :HALF])
        e_ref[:, :WIN] = dot(c_s[hh, rows, :], rt_s[head, :, first:first + WIN])
        dp_ref[:, :HALF] = dot(g_s[hh, rows, :], vt_s[hh, :, :HALF])
        st_ref[:, :8] = st_rx[sub, hh, :, i0 - HALF:i0 - HALF + QB].T
        for r0 in range(0, QB, 16):
            group = slice(r0, r0 + 16)
            rel = pltpu.roll(e_ref[group, :WIN], HALF + 1 + r0, 1, stride=1, stride_axis=0)[:, :HALF]
            log_sum = st_ref[group, 0:1]
            row_dot = st_ref[group, 1:2]
            p = jnp.exp2((s_ref[group, :HALF] + rel) * (scale * LOG2E) - log_sum)
            pb_ref[group, :HALF] = p.astype(BF16)
            ds_ref[group, :HALF] = (p * (dp_ref[group, :HALF] - row_dot) * scale).astype(BF16)
        dkt[hh] += dot(at_s[hh, :, rows], ds_ref[:, :HALF])
        dvt[hh] += dot(gt_s[hh, :, rows], pb_ref[:, :HALF])

    def store_rows(sub):
        for t in BOTH:
            buf[2 + t, sub] = pltpu.einshape("abc->bac", stage[t])

    def store_keys(sub):
        for hh in BOTH:
            stage[2, hh] = dkt[hh].astype(BF16).T
            stage[3, hh] = dvt[hh].astype(BF16).T
        for t in BOTH:
            buf[t, sub] = pltpu.einshape("abc->bac", stage[2 + t])

    def wait_up(sub):
        wait_for(rbuf.at[:, sub], up_recv.at[sub])
        wait_for(rbuf.at[:, sub], up_send.at[sub % 4])

    def wait_in(sub):
        wait_for(buf.at[2:4, sub], in_recv.at[1, sub])

    def lower_rows(sub):
        wait_in(sub)
        load_rows(buf, 2, buf, 3, sub, 0, True)

    def lower_own(sub):
        load_keys(buf, 0, buf, 1, sub, 0)

        def own(hh, carry):
            head = 2 * (sub // SLOTS) + hh
            row_block(hh, head, QB, QB, 0, True, False)
            row_block(hh, head, 0, 0, 0, False, False)
            return carry

        lax.fori_loop(0, PAIR, own, 0)
        store_rows(sub)

    def lower_theirs(sub):
        wait_up(sub)
        load_rows(rbuf, 0, rbuf, 1, sub, HALF, False)
        wait_for(st_rx.at[sub], st_recv.at[sub % 4])

        def theirs(hh, carry):
            head = 2 * (sub // SLOTS) + hh
            col_block(hh, head, sub, HALF)
            col_block(hh, head, sub, HALF + QB)
            return carry

        lax.fori_loop(0, PAIR, theirs, 0)
        store_keys(sub)

    def upper_own(sub):
        wait_in(sub)
        wait_up(sub)
        load_rows(buf, 0, buf, 1, sub, 0, True)
        load_keys(rbuf, 0, rbuf, 1, sub, 0)
        load_keys(buf, 2, buf, 3, sub, HALF)

        def own(hh, carry):
            head = 2 * (sub // SLOTS) + hh
            for blk in (1, 0):
                row_block(hh, head, QB * blk, HALF + QB * blk, HALF, blk == 1, True)
                st_tx[sub, hh, :, QB * blk:QB * (blk + 1)] = st_ref[...].T[:8]
            pltpu.make_async_remote_copy(src_ref=st_tx.at[sub, hh], dst_ref=st_rx.at[sub, hh], send_sem=st_send, recv_sem=st_recv.at[sub % 4],
                                         device_id=(across,), device_id_type=MESH).start()
            place = 2 * (sub % 2 * PAIR + hh)
            row_id = lax.broadcasted_iota(jnp.int32, (8, TIP), 0)
            tile = tip_tx[sub // 2]
            for j in BOTH:
                tile = jnp.where(row_id == place + j, st_tx[sub, hh, j:j + 1, HALF - TIP:], tile)
            tip_tx[sub // 2] = tile
            return carry

        lax.fori_loop(0, PAIR, own, 0)

        @pl.when(jnp.logical_not(tip) & (sub % 2 == 1))
        def _():
            pltpu.make_async_remote_copy(src_ref=tip_tx.at[sub // 2], dst_ref=tip_st.at[col, sub // 2], send_sem=ts_send, recv_sem=ts_recv,
                                         device_id=(N_DEV - 2 + core,), device_id_type=MESH).start()
        store_rows(sub)
        store_keys(sub)

    side = 1 - core
    parts = (dr0_out, dr1_out, dr2_out, dr3_out, dr4_out, dr5_out)

    def swap_start(p):
        for n in BOTH:
            pltpu.make_async_remote_copy(src_ref=dr_acc.at[2 * p + n, side], dst_ref=dr_rx.at[p, n], send_sem=x_send, recv_sem=x_recv.at[p],
                                         device_id=(partner,), device_id_type=MESH).start()

    def swap_add(p):
        wait_for(dr_rx.at[p], x_recv.at[p])
        for n in BOTH:
            dr_rx[p, n] = dr_rx[p, n] + dr_acc[2 * p + n, core]

    def cross_start(p):
        pltpu.make_async_remote_copy(src_ref=dr_rx.at[p, 1 - z], dst_ref=dr_rz.at[p], send_sem=z_send, recv_sem=z_recv.at[p],
                                     device_id=(across,), device_id_type=MESH).start()

    def head_of(p, bits):
        other = chip ^ bits
        return 4 * (other % 4) + 2 * p + other // 4

    def block(p, m, bits):
        if bits == 0:
            return dr_fin.at[p, PART * m:PART * (m + 1)]
        return parts[m].at[side, :, head_of(p, bits)]

    def forward(p, m, bits):
        pltpu.make_async_remote_copy(src_ref=block(p, m, bits), dst_ref=parts[m].at[side, :, head_of(p, bits)], send_sem=fw_send,
                                     recv_sem=fw_recv, device_id=(partner,), device_id_type=MESH).start()

    def blocks(count):
        return parts[0].at[:, :, :N_PART // 2 * count]

    def pass_on(p, bits, hop, device):
        for m in range(N_PART):
            pltpu.make_async_remote_copy(
                src_ref=block(p, m, bits), dst_ref=parts[m].at[side, :, head_of(p, bits)], send_sem=ring_send,
                recv_sem=ring_recv.at[p, hop], device_id=(device,), device_id_type=MESH).start()

    def hand_over(p, bits):
        for m in range(N_PART):
            forward(p, m, bits)

    along_x, along_y = me ^ 2, me ^ 4

    def hop_start(p, hop):
        if hop == 0:
            for device in (along_x, along_y, across):
                pass_on(p, 0, 0, device)
        if hop == 1:
            @pl.when(even & loaded)
            def _():
                pass_on(p, 1, 1, along_y)

            @pl.when(jnp.logical_not(even) & loaded)
            def _():
                pass_on(p, 2, 1, along_x)

            pass_on(p, 1, 1, across)
            pass_on(p, 2, 1, across)
        if hop == 2:
            @pl.when(even & loaded)
            def _():
                pass_on(p, 5, 2, along_y)

            @pl.when(jnp.logical_not(even) & loaded)
            def _():
                pass_on(p, 6, 2, along_x)

            @pl.when(even)
            def _():
                pass_on(p, 3, 2, across)
        if hop == 3:
            @pl.when(even)
            def _():
                pass_on(p, 7, 3, across)

    def hop_wait(p, hop):
        if hop == 0:
            wait_for(blocks(3), ring_recv.at[p, 0])
            for bits in (1, 2, 4):
                hand_over(p, bits)
        if hop == 1:
            @pl.when(even)
            def _():
                wait_for(blocks(3), ring_recv.at[p, 1])
                hand_over(p, 3)

            @pl.when(jnp.logical_not(even))
            def _():
                wait_for(blocks(2), ring_recv.at[p, 1])
            for bits in (5, 6):
                hand_over(p, bits)
        if hop == 2:
            wait_for(blocks(1), ring_recv.at[p, 2])
            hand_over(p, 7)
        if hop == 3:
            @pl.when(jnp.logical_not(even))
            def _():
                wait_for(blocks(1), ring_recv.at[p, 3])
                hand_over(p, 3)

    def sent_wait():
        @pl.when(even & loaded)
        def _():
            wait_for(buf.at[:3, :, :FIN * 18 // 24], ring_send)

        @pl.when(even != loaded)
        def _():
            wait_for(buf.at[:3, :7, :FIN * 14 // 21], ring_send)

        @pl.when(jnp.logical_not(even | loaded))
        def _():
            wait_for(buf.at[:2, :6, :FIN * 10 // 12], ring_send)

    def cross_finish(p):
        wait_for(dr_rz.at[p], z_recv.at[p])
        total = dr_rx[p, z] + dr_rz[p]
        rev32 = eye_rev(F32)
        for m in range(HALF // HEAD):
            part = total[:HEAD, HALF - HEAD * (m + 1):HALF - HEAD * m]
            turned = lax.dot_general(rev32, part, (((1,), (1,)), ((), ())), precision=lax.Precision.HIGHEST, preferred_element_type=F32)
            dr_fin[p, HEAD * m:HEAD * (m + 1)] = turned.reshape(HEAD, 1, HEAD)
        dr_fin[p, HALF] = total[HEAD:HEAD + 1, HALF - HEAD:]
        dr_fin[p, HALF + 1] = total[HEAD + 1:HEAD + 2, HALF - HEAD:]
        dr_fin[p, HALF + 2:] = jnp.zeros((FIN - HALF - 2, 1, HEAD), F32)
        hop_start(p, 0)
        for m in range(N_PART):
            pltpu.make_async_copy(block(p, m, 0), parts[m].at[side, :, head_of(p, 0)], own_sem).start()
        hand_over(p, 0)

    def tip_load(unit):
        slot, row, far = unit % 2, unit // FAR, unit % FAR
        pair = far + tip_base
        for t, src in enumerate((q_in, k_in, v_in, g_in)):
            pltpu.make_async_copy(src.at[core * SLOTS + row, :, pair], r_buf.at[slot, pl.ds(TIP * t + ROWS * core, ROWS)], tip_sem.at[slot]).start()
            pltpu.make_async_copy(far_out.at[t, row, :, far], r_buf.at[slot, pl.ds(TIP * t + ROWS * (1 - core), ROWS)], tip_sem.at[slot]).start()
        pltpu.make_async_copy(r_in.at[:TIP, pair], r_buf.at[slot, 4 * TIP:5 * TIP], tip_sem.at[slot]).start()

    def tip_done(slot):
        wait_for(r_buf.at[slot, :TIP], tip_near.at[slot])
        wait_for(r_buf.at[slot, :TIP], tip_send.at[slot])

    def tip_group(hh, r0):
        group = slice(TIP * hh + r0, TIP * hh + r0 + 16)
        rel = pltpu.roll(e_ref[group, :TIP], 1 + r0, 1, stride=1, stride_axis=0)
        ahead = lax.broadcasted_iota(jnp.int32, (16, TIP), 1) - lax.broadcasted_iota(jnp.int32, (16, TIP), 0)
        return group, s_ref[group, :TIP] + rel, ahead <= r0

    def tip_rows(hh):
        for r0 in range(0, TIP, 16):
            group, s, seen = tip_group(hh, r0)
            s = jnp.where(seen, s, -jnp.inf)
            top = jnp.max(s, axis=1, keepdims=True)
            p = jnp.exp2((s - top) * (scale * LOG2E))
            p = p * (1.0 / jnp.sum(p, axis=1, keepdims=True))
            pb_ref[group, :TIP] = p.astype(BF16)
            dp = dp_ref[group, :TIP]
            row_dot = jnp.sum(p * dp, axis=1, keepdims=True)
            ds = (p * (dp - row_dot) * scale).astype(BF16)
            ds_ref[group, :TIP] = ds
            flipped = flip8(ds.astype(F32))
            half = [pltpu.roll(flipped[8 * j:8 * j + 8], TIP - 8 - r0 - 8 * j, 1, stride=1, stride_axis=0) for j in range(2)]
            dd_ref[group, :TIP] = jnp.concatenate(half, axis=0).astype(BF16)
        rows = slice(TIP * hh, TIP * (hh + 1))
        stage[0, hh, :TIP, :] = dot(pb_ref[rows, :TIP], v_s[hh, :TIP, :]).astype(BF16)
        dqc = dot(ds_ref[rows, :TIP], k_s[hh, :TIP, :])
        dqr = flip8(dot(dd_ref[rows, :TIP], c_s[hh, :TIP, :]))
        stage[1, hh, :TIP, :] = (dqc + dqr).astype(BF16)

    def tip_keys(hh, stats, odd):
        rows = slice(TIP * hh, TIP * (hh + 1))
        by_row = stats.T
        even_row, odd_row = [by_row[:, n:n + 2] for n in (2 * hh, 2 * (hh + PAIR))]
        st_ref[rows, :2] = jnp.where(odd == 1, odd_row, even_row)
        for r0 in range(0, TIP, 16):
            group, s, seen = tip_group(hh, r0)
            p = jnp.where(seen, jnp.exp2(s * (scale * LOG2E) - st_ref[group, 0:1]), 0.0)
            pb_ref[group, :TIP] = p.astype(BF16)
            ds_ref[group, :TIP] = (p * (dp_ref[group, :TIP] - st_ref[group, 1:2]) * scale).astype(BF16)
        over_rows = (((0,), (0,)), ((), ()))
        stage[0, hh, :TIP, :] = lax.dot_general(ds_ref[rows, :TIP], a_s[hh, :TIP, :], over_rows, preferred_element_type=F32).astype(BF16)
        stage[1, hh, :TIP, :] = lax.dot_general(pb_ref[rows, :TIP], g_s[hh, :TIP, :], over_rows, preferred_element_type=F32).astype(BF16)

    def tip_unit(unit, carry):
        slot, row, far = unit % 2, unit // FAR, unit % FAR
        pair = far + tip_base
        wait_for(r_buf.at[slot, :5 * TIP], tip_sem.at[slot])

        @pl.when(unit + 1 < UNITS)
        def _():
            tip_load(unit + 1)

        q2, k2, v2, g2, r2 = [pltpu.einshape("abc->bac", r_buf[slot, TIP * t:TIP * (t + 1)]) for t in range(5)]
        u = u_buf[pair].astype(F32)
        w = w_buf[pair].astype(F32)
        for hh in BOTH:
            rows = slice(TIP * hh, TIP * (hh + 1))
            q32 = q2[hh].astype(F32)
            a = (q32 + u[hh:hh + 1]).astype(BF16)
            c = (q32 + w[hh:hh + 1]).astype(BF16)
            falling = dot(eye_rev(BF16), r2[hh]).astype(BF16)
            s_ref[rows, :TIP] = dot(a, k2[hh].T)
            e_ref[rows, :TIP] = dot(c, falling.T)
            dp_ref[rows, :TIP] = dot(g2[hh], v2[hh].T)
            a_s[hh, :TIP, :] = a
            c_s[hh, :TIP, :] = falling
            g_s[hh, :TIP, :] = g2[hh]
            k_s[hh, :TIP, :] = k2[hh]
            v_s[hh, :TIP, :] = v2[hh]

        @pl.when(lower)
        def _():
            for hh in BOTH:
                tip_rows(hh)

        @pl.when(upper)
        def _():
            for hh in BOTH:
                tip_keys(hh, tip_st[far // 2, (far % 2 * SLOTS + row) // 2], row % 2)

        @pl.when(unit >= 2)
        def _():
            tip_done(slot)

        for n in BOTH:
            r_buf[slot, (5 + n) * TIP:(6 + n) * TIP] = pltpu.einshape("abc->bac", stage[n, :, :TIP, :])
        place = (core * SLOTS + row, slice(None), pair)

        def give(results):
            for n, dst in enumerate(results):
                pltpu.make_async_copy(r_buf.at[slot, pl.ds((5 + n) * TIP + ROWS * core, ROWS)], dst.at[place], tip_near.at[slot]).start()
                pltpu.make_async_remote_copy(
                    src_ref=r_buf.at[slot, pl.ds((5 + n) * TIP + ROWS * (1 - core), ROWS)], dst_ref=dst.at[place],
                    send_sem=tip_send.at[slot], recv_sem=out_recv, device_id=(partner,), device_id_type=MESH).start()

        @pl.when(lower)
        def _():
            give((o_out, dq_out))

        @pl.when(upper)
        def _():
            give((dk_out, dv_out))
        return carry

    def tips(third):
        @pl.when(tip)
        def _():
            if third == 0:
                wait_for(far_out, far_recv)

                @pl.when(upper)
                def _():
                    wait_for(tip_st, ts_recv)
                tip_load(0)
            lax.fori_loop(UNITS // 3 * third, UNITS // 3 * (third + 1), tip_unit, 0)
            if third == 2:
                tip_done(0)
                tip_done(1)

    send_up(0)

    def sub_body(sub, carry):
        @pl.when(sub < SUBS - 1)
        def _():
            send_up(sub + 1)

        @pl.when(sub == SLOTS)
        def _():
            swap_start(0)

        @pl.when(sub == SUBS - 1)
        def _():
            swap_add(0)
            cross_start(0)

        @pl.when(sub == SUBS)
        def _():
            swap_start(1)
            swap_add(1)
            cross_start(1)
            cross_finish(0)

        @pl.when(lower & (sub < SUBS))
        def _():
            lower_rows(sub)

        @pl.when(lower & (sub > 0))
        def _():
            lower_theirs(sub - 1)

        @pl.when(lower & (sub < SUBS))
        def _():
            lower_own(sub)

        @pl.when(upper & (sub < SUBS))
        def _():
            upper_own(sub)

        @pl.when(sub <= EARLY)
        def _():
            send_out(sub, (2, 3))

        @pl.when((sub > 0) & (sub <= EARLY))
        def _():
            send_out(sub - 1, (0, 1))
        return carry

    lax.fori_loop(0, SUBS + 1, sub_body, 0)

    cross_finish(1)
    send_out(EARLY, (0, 1))
    for p in BOTH:
        hop_wait(p, 0)
        hop_start(p, 1)
    for p in BOTH:
        send_out(EARLY + 1 + p, range(4))
        tips(p)
        hop_wait(p, 1)
        hop_start(p, 2)

    def send_late(sub, carry):
        send_out(sub, range(4), True)
        return carry

    lax.fori_loop(EARLY + 3, SUBS, send_late, 0)
    tips(2)
    for p in BOTH:
        hop_wait(p, 2)
        hop_start(p, 3)
    for p in BOTH:
        hop_wait(p, 3)

    wait_for(buf.at[:, :, :HALF - ROWS], in_send)

    @pl.when(tip)
    def _():
        wait_for(buf.at[:, :, :HALF - 3 * ROWS // 2], out_recv)
        wait_for(buf.at[:, :, :HALF - ROWS], out_send)
        wait_for(far_out, far_send)

    @pl.when(jnp.logical_not(tip))
    def _():
        wait_for(buf, out_recv)
        wait_for(buf.at[:, :, :HALF - 2 * ROWS], out_send)

    @pl.when(upper & jnp.logical_not(tip))
    def _():
        wait_for(tip_tx, ts_send)

    @pl.when(upper)
    def _():
        wait_for(st_tx, st_send)

    wait_for(dr_rx, x_send)
    wait_for(dr_rz, z_send)
    wait_for(blocks(2), own_sem)
    sent_wait()
    for sem in (fw_send, fw_recv):
        wait_for(buf.at[:3, :, :FIN * 16 // 24], sem)


def writer(*refs):
    ins, (o, dq, dk, dv, dr, du, dw, sem) = refs[:4 + N_PART], refs[4 + N_PART:]
    pairs = list(zip(ins[:4], (o, dq, dk, dv)))
    for m, part in enumerate(ins[4:]):
        rows = min(PART, HALF - PART * m)
        for side in BOTH:
            start = HALF * side + PART * m
            pairs.append((part.at[side, :rows], dr.at[start:start + rows]))
    last = HALF - PART * (N_PART - 1)
    pairs += [(ins[-1].at[0, last], du), (ins[-1].at[0, last + 1], dw)]
    copies = [pltpu.make_async_copy(src, dst, sem.at[j]) for j, (src, dst) in enumerate(pairs)]
    for copy in copies:
        copy.start()
    for copy in copies:
        copy.wait()


def solution(mesh):
    seq_spec = P(None, "cp", None, None)

    def local(query, key_in, value, bias_u, bias_w, rel_k, d_out):
        n_batch, rows, n_heads, head_dim = query.shape
        pairs = (n_batch, rows, N_PAIR, PAIR, head_dim)
        vm = pltpu.VMEM
        dma = pltpu.SemaphoreType.DMA
        whole = pl.BlockSpec(memory_space=pl.ANY)
        act = jax.ShapeDtypeStruct(pairs, BF16)
        vec = jax.ShapeDtypeStruct((n_heads, 1, head_dim), F32)
        tok = (PAIR, SEQ, HEAD)
        tok_t = (PAIR, HEAD, SEQ)
        acc = (HEAD + 8, HALF)
        outs = pl.pallas_call(
            kernel,
            name="rel_attn",
            out_shape=(act, act, act, act,
                       *[jax.ShapeDtypeStruct((2, PART, n_heads, 1, head_dim), F32)] * N_PART,
                       jax.ShapeDtypeStruct((4, SLOTS, ROWS, FAR, PAIR, HEAD), BF16)),
            in_specs=[pl.BlockSpec(memory_space=pltpu.HBM)] * 7,
            out_specs=[whole] * (5 + N_PART),
            scratch_shapes=[
                vm((4, SUBS, HALF, PAIR, HEAD), BF16), vm((2, SUBS, HALF, PAIR, HEAD), BF16),
                vm((2, SEQ, PAIR, HEAD), BF16), vm((N_PAIR, PAIR, HEAD), BF16), vm((N_PAIR, PAIR, HEAD), BF16),
                vm((SUBS, PAIR, 8, HALF), F32), vm((SUBS, PAIR, 8, HALF), F32), vm((SUBS // 2, 8, TIP), F32), vm((3, SUBS // 2, 8, TIP), F32), vm((QB, HEAD), F32),
                vm((2, 2) + acc, F32), vm((2,) + acc, F32), vm((2, FIN, 1, HEAD), F32), vm((4, 2) + acc, F32),
                vm((QB, SEQ), F32), vm((QB, SEQ), F32), vm((QB, SEQ), F32),
                vm((QB, SEQ), BF16), vm((QB, SEQ), BF16), vm((QB, SEQ), BF16),
                vm(tok, BF16), vm(tok, BF16), vm(tok, BF16), vm(tok, BF16), vm(tok, BF16),
                vm(tok_t, BF16), vm(tok_t, BF16), vm(tok_t, BF16), vm(tok_t, BF16), vm(tok_t, BF16),
                vm((4, SEQ, HEAD), BF16), vm((4, HEAD, SEQ), BF16),
                vm((PAIR, HEAD, HALF), F32), vm((PAIR, HEAD, HALF), F32), vm((4, PAIR, HALF, HEAD), BF16),
                dma, dma((2, SUBS)), dma, dma, dma, dma((4,)), dma((4,)), dma((SUBS,)), dma, dma((4,)),
                dma, dma((2,)), dma, dma((2,)), dma, dma((2, 4)), dma, dma,
                dma, dma, dma((2,)), dma((2,)), dma((2,)), dma, dma,
            ],
            compiler_params=pltpu.CompilerParams(collective_id=0, has_side_effects=True, vmem_limit_bytes=37 * 1024 * 1024),
        )(*[pltpu.with_memory_space_constraint(x, pltpu.HBM) for x in (
            query.reshape(pairs), key_in.reshape(pairs), value.reshape(pairs), d_out.reshape(pairs),
            rel_k.reshape(SEQ, N_PAIR, PAIR, head_dim), bias_u.reshape(N_PAIR, PAIR, head_dim), bias_w.reshape(N_PAIR, PAIR, head_dim))])
        o, dq, dk, dv, dr, du, dw = pl.pallas_call(
            writer,
            name="writer",
            out_shape=(act, act, act, act, jax.ShapeDtypeStruct((SEQ, n_heads, 1, head_dim), F32), vec, vec),
            in_specs=[whole] * (4 + N_PART),
            out_specs=[whole] * 7,
            scratch_shapes=[dma((6 + 2 * N_PART,))],
            compiler_params=pltpu.CompilerParams(vmem_limit_bytes=1024 * 1024),
        )(*outs[:-1])
        full = query.shape
        return (o.reshape(full), dq.reshape(full), dk.reshape(full), dv.reshape(full),
                du.reshape(bias_u.shape), dw.reshape(bias_w.shape), dr.reshape(rel_k.shape))

    return jax.shard_map(local, mesh=mesh,
                         in_specs=(seq_spec, seq_spec, seq_spec, P(), P(), P(), seq_spec),
                         out_specs=(seq_spec, seq_spec, seq_spec, seq_spec, P(), P(), P()),
                         check_vma=False)
```

```python
import jax
import jax.numpy as jnp
from jax import lax
from jax.experimental import pallas as pl
from jax.experimental.pallas import tpu as pltpu
from jax.sharding import PartitionSpec as P

MESH = pl.DeviceIdType.MESH
BF16, F32 = jnp.bfloat16, jnp.float32
LOG2E = 1.4426950408889634

N_DEV = 16
BOTH = range(2)
PLANE = 8
PAIR = 2
N_PAIR = 8
SLOTS = 4
SUBS = 2 * SLOTS
EARLY = 3
ROWS = 64
HALF = PLANE * ROWS
SEQ = 2 * HALF
HEAD = 128
QB = 256
WIN = HALF + QB
N_PART = 6
PART = 86
FIN = N_PART * PART
TIP = 2 * ROWS
FAR = N_PAIR - 2
UNITS = FAR * SLOTS
TURNS = ((1, 3, 2), (3, 1, 2))


def dot(lhs, rhs):
    return jnp.dot(lhs, rhs, preferred_element_type=F32)


def flip8(x):
    rows, cols = x.shape
    idx = 7 - lax.broadcasted_iota(jnp.int32, (rows // 8, 8, cols), 1)
    return jnp.take_along_axis(x.reshape(rows // 8, 8, cols), idx, axis=1).reshape(rows, cols)


def eye_rev(dtype):
    total = lax.broadcasted_iota(jnp.int32, (HEAD, HEAD), 0) + lax.broadcasted_iota(jnp.int32, (HEAD, HEAD), 1)
    return jnp.where(total == HEAD - 1, 1.0, 0.0).astype(dtype)


def kernel(q_in, k_in, v_in, g_in, r_in, u_in, w_in,
           o_out, dq_out, dk_out, dv_out, dr0_out, dr1_out, dr2_out, dr3_out, dr4_out, dr5_out, far_out,
           buf, rbuf, r_buf, u_buf, w_buf, st_tx, st_rx, tip_tx, tip_st, st_ref, dr_rx, dr_rz, dr_fin, dr_acc,
           s_ref, e_ref, dp_ref, pb_ref, ds_ref, dd_ref,
           a_s, c_s, g_s, k_s, v_s, at_s, ct_s, gt_s, kt_s, vt_s, rev_s, rt_s, dkt, dvt, stage,
           in_send, in_recv, out_send, out_recv, own_sem, r_sem, up_send, up_recv, st_send, st_recv,
           x_send, x_recv, z_send, z_recv, ring_send, ring_recv, fw_send, fw_recv,
           far_send, far_recv, tip_sem, tip_near, tip_send, ts_send, ts_recv):
    me = lax.axis_index("cp")
    core = me % 2
    chip = me // 2
    col = chip % 4
    z = chip // 4
    partner = me + 1 - 2 * core
    across = me + PLANE * (1 - 2 * z)
    scale = HEAD ** -0.5

    def wait_for(ref, sem):
        pltpu.make_async_copy(ref, ref, sem).wait()

    y = col // 2
    lower, upper = z == 0, z == 1
    tip = chip == 7 * z
    tip_base = 2 - 2 * z

    tables = [pltpu.make_async_copy(src, dst, r_sem.at[j]) for j, (src, dst) in enumerate(
        ((r_in.at[:, 2 * col], r_buf.at[0]), (r_in.at[:, 2 * col + 1], r_buf.at[1]), (u_in, u_buf), (w_in, w_buf)))]
    for copy in tables:
        copy.start()

    barrier = pltpu.get_barrier_semaphore()

    for peer in [across] + [me ^ step for step in range(PLANE - 1, 0, -1)]:
        pl.semaphore_signal(barrier, inc=1, device_id=(peer,), device_id_type=MESH)
    pl.semaphore_wait(barrier, PLANE)

    my_rows = pl.ds(pl.multiple_of((me % PLANE) * ROWS, ROWS), ROWS)

    even = chip % 2 == z
    loaded = y != z
    lone = loaded & jnp.logical_not(even)

    def peers(late=False):
        near = core == 0
        if late:
            near = jnp.logical_not(near | lone)
        first, second, third = [jnp.where(near, near_turn, far_turn) for near_turn, far_turn in zip(*TURNS)]
        for turn, other in ((first, 0), (third, 0), (first, 1), (third, 1), (second, 0), (second, 1)):
            yield me ^ (2 * turn + other)
        yield partner

    def send_in(ins, sub):
        pair, row = sub // SLOTS, sub % SLOTS
        for first in (0, 2):
            for t in (first, first + 1):
                pltpu.make_async_copy(ins[t].at[core * SLOTS + row, :, 2 * col + pair], buf.at[t, sub, my_rows], in_recv.at[first // 2, sub]).start()
            for peer in peers():
                for t in (first, first + 1):
                    pltpu.make_async_remote_copy(
                        src_ref=ins[t].at[(peer % 2) * SLOTS + row, :, 2 * ((peer // 2) % 4) + pair], dst_ref=buf.at[t, sub, my_rows],
                        send_sem=in_send, recv_sem=in_recv.at[first // 2, sub], device_id=(peer,), device_id_type=MESH).start()

    def send_all(ins):
        def send_sub(sub, carry):
            send_in(ins, sub)
            return carry
        lax.fori_loop(0, SUBS, send_sub, 0)

    @pl.when(lower)
    def _():
        send_all((k_in, v_in, q_in, g_in))

    @pl.when(upper)
    def _():
        send_all((q_in, g_in, k_in, v_in))

    @pl.when(tip)
    def _():
        for t, src in enumerate((q_in, k_in, v_in, g_in)):
            for row in range(SLOTS):
                pltpu.make_async_remote_copy(
                    src_ref=src.at[(1 - core) * SLOTS + row, :, pl.ds(tip_base, FAR)], dst_ref=far_out.at[t, row],
                    send_sem=far_send, recv_sem=far_recv, device_id=(partner,), device_id_type=MESH).start()

    for copy in tables:
        copy.wait()
    rev = eye_rev(BF16)
    for p in BOTH:
        pair_tab = pltpu.einshape("abc->bac", r_buf[p])
        for hh in BOTH:
            for blk in range(SEQ // HEAD):
                part = pair_tab[hh, SEQ - HEAD * (blk + 1):SEQ - HEAD * blk]
                flipped = dot(rev, part).astype(BF16)
                rev_s[2 * p + hh, HEAD * blk:HEAD * (blk + 1), :] = flipped
                rt_s[2 * p + hh, :, HEAD * blk:HEAD * (blk + 1)] = flipped.T
    dr_acc[...] = jnp.zeros_like(dr_acc)

    acts = (dk_out, dv_out, o_out, dq_out)

    def send_out(sub, which, late=False):
        place = (core * SLOTS + sub % SLOTS, slice(None), 2 * col + sub // SLOTS)
        for t in which:
            pltpu.make_async_copy(buf.at[t, sub, my_rows], acts[t].at[place], out_recv).start()
        for peer in peers(late):
            peer_rows = pl.ds(pl.multiple_of((peer % PLANE) * ROWS, ROWS), ROWS)
            to_tip = (peer // 2 == 7 * z) & jnp.logical_not(tip)
            for t in which:
                @pl.when(jnp.logical_not(to_tip & (lower if t >= 2 else upper)))
                def _():
                    pltpu.make_async_remote_copy(
                        src_ref=buf.at[t, sub, peer_rows], dst_ref=acts[t].at[place],
                        send_sem=out_send, recv_sem=out_recv, device_id=(peer,), device_id_type=MESH).start()

    def send_up(sub):
        wait_for(buf.at[0:2, sub], in_recv.at[0, sub])
        for j in BOTH:
            pltpu.make_async_remote_copy(src_ref=buf.at[j, sub], dst_ref=rbuf.at[j, sub], send_sem=up_send.at[sub % 4], recv_sem=up_recv.at[sub],
                                         device_id=(across,), device_id_type=MESH).start()

    def unpack(ref, j, sub):
        return pltpu.einshape("abc->bac", ref[j, sub])

    def load_rows(q_ref, q_j, g_ref, g_j, sub, start, turned):
        rows = slice(start, start + HALF)
        p = sub // SLOTS
        q2 = unpack(q_ref, q_j, sub)
        u = u_buf[2 * col + p].astype(F32)
        w = w_buf[2 * col + p].astype(F32)
        for hh in BOTH:
            q32 = q2[hh].astype(F32)
            a = (q32 + u[hh:hh + 1]).astype(BF16)
            c = (q32 + w[hh:hh + 1]).astype(BF16)
            a_s[hh, rows, :] = a
            c_s[hh, rows, :] = c
            at_s[hh, :, rows] = a.T
            if turned:
                ct_s[hh, :, rows] = flip8(c.astype(F32)).astype(BF16).T
        g2 = unpack(g_ref, g_j, sub)
        g_s[:, rows, :] = g2
        for hh in BOTH:
            gt_s[hh, :, rows] = g2[hh].T

    def load_keys(k_ref, k_j, v_ref, v_j, sub, start):
        rows = slice(start, start + HALF)
        k2 = unpack(k_ref, k_j, sub)
        v2 = unpack(v_ref, v_j, sub)
        k_s[:, rows, :] = k2
        v_s[:, rows, :] = v2
        for hh in BOTH:
            kt_s[hh, :, rows] = k2[hh].T
            vt_s[hh, :, rows] = v2[hh].T

    def row_block(hh, head, start, i0, lo, fresh, stats):
        width = i0 + QB
        rows = slice(start, start + QB)
        s_ref[:, :width] = dot(a_s[hh, rows, :], kt_s[hh, :, :width])
        e_ref[:, :width] = dot(c_s[hh, rows, :], rt_s[head, :, SEQ - width:])
        dp_ref[:, :width] = dot(g_s[hh, rows, :], vt_s[hh, :, :width])
        for r0 in range(0, QB, 16):
            group = slice(r0, r0 + 16)
            rel = pltpu.roll(e_ref[group, :width], i0 + 1 + r0, 1, stride=1, stride_axis=0)
            s = s_ref[group, :width] + rel
            ahead = lax.broadcasted_iota(jnp.int32, (16, width), 1) - lax.broadcasted_iota(jnp.int32, (16, width), 0)
            s = jnp.where(ahead <= i0 + r0, s, -jnp.inf)
            top = jnp.max(s, axis=1, keepdims=True)
            p = jnp.exp2((s - top) * (scale * LOG2E))
            total = jnp.sum(p, axis=1, keepdims=True)
            p = p * (1.0 / total)
            pb_ref[group, :width] = p.astype(BF16)
            dp = dp_ref[group, :width]
            row_dot = jnp.sum(p * dp, axis=1, keepdims=True)
            ds = (p * (dp - row_dot) * scale).astype(BF16)
            ds_ref[group, :width] = ds
            flipped = flip8(ds.astype(F32))
            half = [pltpu.roll(flipped[8 * j:8 * j + 8], QB - 8 - r0 - 8 * j, 1, stride=1, stride_axis=0) for j in range(2)]
            dd_ref[group, :width] = jnp.concatenate(half, axis=0).astype(BF16)
            if stats:
                lane = lax.broadcasted_iota(jnp.int32, (16, HEAD), 1)
                st_ref[group, :] = jnp.where(lane == 0, top * (scale * LOG2E) + jnp.log2(total), row_dot)
        pb = pb_ref[:, :width]
        ds = ds_ref[:, :width]
        dd = dd_ref[:, :width]
        stage[0, hh, rows, :] = dot(pb, v_s[hh, :width, :]).astype(BF16)
        dqc = dot(ds, k_s[hh, :width, :])
        dqr = flip8(dot(dd, rev_s[head, SEQ - width:, :]))
        stage[1, hh, rows, :] = (dqc + dqr).astype(BF16)
        dr_acc[head, 1, HEAD:HEAD + 1, HALF - HEAD:] += jnp.sum(dqc, axis=0, keepdims=True)
        dr_acc[head, 1, HEAD + 1:HEAD + 2, HALF - HEAD:] += jnp.sum(dqr, axis=0, keepdims=True)
        dk_new = dot(at_s[hh, :, rows], ds_ref[:, lo:width])
        dv_new = dot(gt_s[hh, :, rows], pb_ref[:, lo:width])
        if fresh:
            dkt[hh] = dk_new
            dvt[hh] = dv_new
        else:
            dkt[hh, :, :width - lo] += dk_new
            dvt[hh, :, :width - lo] += dv_new
        dr_new = dot(ct_s[hh, :, rows], dd)
        if width > HALF:
            dr_acc[head, 0, :HEAD, SEQ - width:] += dr_new[:, :width - HALF]
            dr_acc[head, 1, :HEAD, :] += dr_new[:, width - HALF:]
        else:
            dr_acc[head, 1, :HEAD, HALF - width:] += dr_new

    def col_block(hh, head, sub, i0):
        rows = slice(i0, i0 + QB)
        first = WIN - i0
        s_ref[:, :HALF] = dot(a_s[hh, rows, :], kt_s[hh, :, :HALF])
        e_ref[:, :WIN] = dot(c_s[hh, rows, :], rt_s[head, :, first:first + WIN])
        dp_ref[:, :HALF] = dot(g_s[hh, rows, :], vt_s[hh, :, :HALF])
        st_ref[:, :8] = st_rx[sub, hh, :, i0 - HALF:i0 - HALF + QB].T
        for r0 in range(0, QB, 16):
            group = slice(r0, r0 + 16)
            rel = pltpu.roll(e_ref[group, :WIN], HALF + 1 + r0, 1, stride=1, stride_axis=0)[:, :HALF]
            log_sum = st_ref[group, 0:1]
            row_dot = st_ref[group, 1:2]
            p = jnp.exp2((s_ref[group, :HALF] + rel) * (scale * LOG2E) - log_sum)
            pb_ref[group, :HALF] = p.astype(BF16)
            ds_ref[group, :HALF] = (p * (dp_ref[group, :HALF] - row_dot) * scale).astype(BF16)
        dkt[hh] += dot(at_s[hh, :, rows], ds_ref[:, :HALF])
        dvt[hh] += dot(gt_s[hh, :, rows], pb_ref[:, :HALF])

    def store_rows(sub):
        for t in BOTH:
            buf[2 + t, sub] = pltpu.einshape("abc->bac", stage[t])

    def store_keys(sub):
        for hh in BOTH:
            stage[2, hh] = dkt[hh].astype(BF16).T
            stage[3, hh] = dvt[hh].astype(BF16).T
        for t in BOTH:
            buf[t, sub] = pltpu.einshape("abc->bac", stage[2 + t])

    def wait_up(sub):
        wait_for(rbuf.at[:, sub], up_recv.at[sub])
        wait_for(rbuf.at[:, sub], up_send.at[sub % 4])

    def wait_in(sub):
        wait_for(buf.at[2:4, sub], in_recv.at[1, sub])

    def lower_rows(sub):
        wait_in(sub)
        load_rows(buf, 2, buf, 3, sub, 0, True)

    def lower_own(sub):
        load_keys(buf, 0, buf, 1, sub, 0)

        def own(hh, carry):
            head = 2 * (sub // SLOTS) + hh
            row_block(hh, head, QB, QB, 0, True, False)
            row_block(hh, head, 0, 0, 0, False, False)
            return carry

        lax.fori_loop(0, PAIR, own, 0)
        store_rows(sub)

    def lower_theirs(sub):
        wait_up(sub)
        load_rows(rbuf, 0, rbuf, 1, sub, HALF, False)
        wait_for(st_rx.at[sub], st_recv.at[sub % 4])

        def theirs(hh, carry):
            head = 2 * (sub // SLOTS) + hh
            col_block(hh, head, sub, HALF)
            col_block(hh, head, sub, HALF + QB)
            return carry

        lax.fori_loop(0, PAIR, theirs, 0)
        store_keys(sub)

    def upper_own(sub):
        wait_in(sub)
        wait_up(sub)
        load_rows(buf, 0, buf, 1, sub, 0, True)
        load_keys(rbuf, 0, rbuf, 1, sub, 0)
        load_keys(buf, 2, buf, 3, sub, HALF)

        def own(hh, carry):
            head = 2 * (sub // SLOTS) + hh
            for blk in (1, 0):
                row_block(hh, head, QB * blk, HALF + QB * blk, HALF, blk == 1, True)
                st_tx[sub, hh, :, QB * blk:QB * (blk + 1)] = st_ref[...].T[:8]
            pltpu.make_async_remote_copy(src_ref=st_tx.at[sub, hh], dst_ref=st_rx.at[sub, hh], send_sem=st_send, recv_sem=st_recv.at[sub % 4],
                                         device_id=(across,), device_id_type=MESH).start()
            place = 2 * (sub % 2 * PAIR + hh)
            row_id = lax.broadcasted_iota(jnp.int32, (8, TIP), 0)
            tile = tip_tx[sub // 2]
            for j in BOTH:
                tile = jnp.where(row_id == place + j, st_tx[sub, hh, j:j + 1, HALF - TIP:], tile)
            tip_tx[sub // 2] = tile
            return carry

        lax.fori_loop(0, PAIR, own, 0)

        @pl.when(jnp.logical_not(tip) & (sub % 2 == 1))
        def _():
            pltpu.make_async_remote_copy(src_ref=tip_tx.at[sub // 2], dst_ref=tip_st.at[col, sub // 2], send_sem=ts_send, recv_sem=ts_recv,
                                         device_id=(N_DEV - 2 + core,), device_id_type=MESH).start()
        store_rows(sub)
        store_keys(sub)

    side = 1 - core
    parts = (dr0_out, dr1_out, dr2_out, dr3_out, dr4_out, dr5_out)

    def swap_start(p):
        for n in BOTH:
            pltpu.make_async_remote_copy(src_ref=dr_acc.at[2 * p + n, side], dst_ref=dr_rx.at[p, n], send_sem=x_send, recv_sem=x_recv.at[p],
                                         device_id=(partner,), device_id_type=MESH).start()

    def swap_add(p):
        wait_for(dr_rx.at[p], x_recv.at[p])
        for n in BOTH:
            dr_rx[p, n] = dr_rx[p, n] + dr_acc[2 * p + n, core]

    def cross_start(p):
        pltpu.make_async_remote_copy(src_ref=dr_rx.at[p, 1 - z], dst_ref=dr_rz.at[p], send_sem=z_send, recv_sem=z_recv.at[p],
                                     device_id=(across,), device_id_type=MESH).start()

    def head_of(p, bits):
        other = chip ^ bits
        return 4 * (other % 4) + 2 * p + other // 4

    def block(p, m, bits):
        if bits == 0:
            return dr_fin.at[p, PART * m:PART * (m + 1)]
        return parts[m].at[side, :, head_of(p, bits)]

    def forward(p, m, bits):
        pltpu.make_async_remote_copy(src_ref=block(p, m, bits), dst_ref=parts[m].at[side, :, head_of(p, bits)], send_sem=fw_send,
                                     recv_sem=fw_recv, device_id=(partner,), device_id_type=MESH).start()

    def blocks(count):
        return parts[0].at[:, :, :N_PART // 2 * count]

    def pass_on(p, bits, hop, device):
        for m in range(N_PART):
            pltpu.make_async_remote_copy(
                src_ref=block(p, m, bits), dst_ref=parts[m].at[side, :, head_of(p, bits)], send_sem=ring_send,
                recv_sem=ring_recv.at[p, hop], device_id=(device,), device_id_type=MESH).start()

    def hand_over(p, bits):
        for m in range(N_PART):
            forward(p, m, bits)

    along_x, along_y = me ^ 2, me ^ 4

    def hop_start(p, hop):
        if hop == 0:
            for device in (along_x, along_y, across):
                pass_on(p, 0, 0, device)
        if hop == 1:
            @pl.when(even & loaded)
            def _():
                pass_on(p, 1, 1, along_y)

            @pl.when(jnp.logical_not(even) & loaded)
            def _():
                pass_on(p, 2, 1, along_x)

            pass_on(p, 1, 1, across)
            pass_on(p, 2, 1, across)
        if hop == 2:
            @pl.when(even & loaded)
            def _():
                pass_on(p, 5, 2, along_y)

            @pl.when(jnp.logical_not(even) & loaded)
            def _():
                pass_on(p, 6, 2, along_x)

            @pl.when(even)
            def _():
                pass_on(p, 3, 2, across)
        if hop == 3:
            @pl.when(even)
            def _():
                pass_on(p, 7, 3, across)

    def hop_wait(p, hop):
        if hop == 0:
            wait_for(blocks(3), ring_recv.at[p, 0])
            for bits in (1, 2, 4):
                hand_over(p, bits)
        if hop == 1:
            @pl.when(even)
            def _():
                wait_for(blocks(3), ring_recv.at[p, 1])
                hand_over(p, 3)

            @pl.when(jnp.logical_not(even))
            def _():
                wait_for(blocks(2), ring_recv.at[p, 1])
            for bits in (5, 6):
                hand_over(p, bits)
        if hop == 2:
            wait_for(blocks(1), ring_recv.at[p, 2])
            hand_over(p, 7)
        if hop == 3:
            @pl.when(jnp.logical_not(even))
            def _():
                wait_for(blocks(1), ring_recv.at[p, 3])
                hand_over(p, 3)

    def sent_wait():
        @pl.when(even & loaded)
        def _():
            wait_for(buf.at[:3, :, :FIN * 18 // 24], ring_send)

        @pl.when(even != loaded)
        def _():
            wait_for(buf.at[:3, :7, :FIN * 14 // 21], ring_send)

        @pl.when(jnp.logical_not(even | loaded))
        def _():
            wait_for(buf.at[:2, :6, :FIN * 10 // 12], ring_send)

    def cross_finish(p):
        wait_for(dr_rz.at[p], z_recv.at[p])
        total = dr_rx[p, z] + dr_rz[p]
        rev32 = eye_rev(F32)
        for m in range(HALF // HEAD):
            part = total[:HEAD, HALF - HEAD * (m + 1):HALF - HEAD * m]
            turned = lax.dot_general(rev32, part, (((1,), (1,)), ((), ())), precision=lax.Precision.HIGHEST, preferred_element_type=F32)
            dr_fin[p, HEAD * m:HEAD * (m + 1)] = turned.reshape(HEAD, 1, HEAD)
        dr_fin[p, HALF] = total[HEAD:HEAD + 1, HALF - HEAD:]
        dr_fin[p, HALF + 1] = total[HEAD + 1:HEAD + 2, HALF - HEAD:]
        dr_fin[p, HALF + 2:] = jnp.zeros((FIN - HALF - 2, 1, HEAD), F32)
        hop_start(p, 0)
        for m in range(N_PART):
            pltpu.make_async_copy(block(p, m, 0), parts[m].at[side, :, head_of(p, 0)], own_sem).start()
        hand_over(p, 0)

    def tip_load(unit):
        slot, row, far = unit % 2, unit // FAR, unit % FAR
        pair = far + tip_base
        for t, src in enumerate((q_in, k_in, v_in, g_in)):
            pltpu.make_async_copy(src.at[core * SLOTS + row, :, pair], r_buf.at[slot, pl.ds(TIP * t + ROWS * core, ROWS)], tip_sem.at[slot]).start()
            pltpu.make_async_copy(far_out.at[t, row, :, far], r_buf.at[slot, pl.ds(TIP * t + ROWS * (1 - core), ROWS)], tip_sem.at[slot]).start()
        pltpu.make_async_copy(r_in.at[:TIP, pair], r_buf.at[slot, 4 * TIP:5 * TIP], tip_sem.at[slot]).start()

    def tip_done(slot):
        wait_for(r_buf.at[slot, :TIP], tip_near.at[slot])
        wait_for(r_buf.at[slot, :TIP], tip_send.at[slot])

    def tip_group(hh, r0):
        group = slice(TIP * hh + r0, TIP * hh + r0 + 16)
        rel = pltpu.roll(e_ref[group, :TIP], 1 + r0, 1, stride=1, stride_axis=0)
        ahead = lax.broadcasted_iota(jnp.int32, (16, TIP), 1) - lax.broadcasted_iota(jnp.int32, (16, TIP), 0)
        return group, s_ref[group, :TIP] + rel, ahead <= r0

    def tip_rows(hh):
        for r0 in range(0, TIP, 16):
            group, s, seen = tip_group(hh, r0)
            s = jnp.where(seen, s, -jnp.inf)
            top = jnp.max(s, axis=1, keepdims=True)
            p = jnp.exp2((s - top) * (scale * LOG2E))
            p = p * (1.0 / jnp.sum(p, axis=1, keepdims=True))
            pb_ref[group, :TIP] = p.astype(BF16)
            dp = dp_ref[group, :TIP]
            row_dot = jnp.sum(p * dp, axis=1, keepdims=True)
            ds = (p * (dp - row_dot) * scale).astype(BF16)
            ds_ref[group, :TIP] = ds
            flipped = flip8(ds.astype(F32))
            half = [pltpu.roll(flipped[8 * j:8 * j + 8], TIP - 8 - r0 - 8 * j, 1, stride=1, stride_axis=0) for j in range(2)]
            dd_ref[group, :TIP] = jnp.concatenate(half, axis=0).astype(BF16)
        rows = slice(TIP * hh, TIP * (hh + 1))
        stage[0, hh, :TIP, :] = dot(pb_ref[rows, :TIP], v_s[hh, :TIP, :]).astype(BF16)
        dqc = dot(ds_ref[rows, :TIP], k_s[hh, :TIP, :])
        dqr = flip8(dot(dd_ref[rows, :TIP], c_s[hh, :TIP, :]))
        stage[1, hh, :TIP, :] = (dqc + dqr).astype(BF16)

    def tip_keys(hh, stats, odd):
        rows = slice(TIP * hh, TIP * (hh + 1))
        by_row = stats.T
        even_row, odd_row = [by_row[:, n:n + 2] for n in (2 * hh, 2 * (hh + PAIR))]
        st_ref[rows, :2] = jnp.where(odd == 1, odd_row, even_row)
        for r0 in range(0, TIP, 16):
            group, s, seen = tip_group(hh, r0)
            p = jnp.where(seen, jnp.exp2(s * (scale * LOG2E) - st_ref[group, 0:1]), 0.0)
            pb_ref[group, :TIP] = p.astype(BF16)
            ds_ref[group, :TIP] = (p * (dp_ref[group, :TIP] - st_ref[group, 1:2]) * scale).astype(BF16)
        over_rows = (((0,), (0,)), ((), ()))
        stage[0, hh, :TIP, :] = lax.dot_general(ds_ref[rows, :TIP], a_s[hh, :TIP, :], over_rows, preferred_element_type=F32).astype(BF16)
        stage[1, hh, :TIP, :] = lax.dot_general(pb_ref[rows, :TIP], g_s[hh, :TIP, :], over_rows, preferred_element_type=F32).astype(BF16)

    def tip_unit(unit, carry):
        slot, row, far = unit % 2, unit // FAR, unit % FAR
        pair = far + tip_base
        wait_for(r_buf.at[slot, :5 * TIP], tip_sem.at[slot])

        @pl.when(unit + 1 < UNITS)
        def _():
            tip_load(unit + 1)

        q2, k2, v2, g2, r2 = [pltpu.einshape("abc->bac", r_buf[slot, TIP * t:TIP * (t + 1)]) for t in range(5)]
        u = u_buf[pair].astype(F32)
        w = w_buf[pair].astype(F32)
        for hh in BOTH:
            rows = slice(TIP * hh, TIP * (hh + 1))
            q32 = q2[hh].astype(F32)
            a = (q32 + u[hh:hh + 1]).astype(BF16)
            c = (q32 + w[hh:hh + 1]).astype(BF16)
            falling = dot(eye_rev(BF16), r2[hh]).astype(BF16)
            s_ref[rows, :TIP] = dot(a, k2[hh].T)
            e_ref[rows, :TIP] = dot(c, falling.T)
            dp_ref[rows, :TIP] = dot(g2[hh], v2[hh].T)
            a_s[hh, :TIP, :] = a
            c_s[hh, :TIP, :] = falling
            g_s[hh, :TIP, :] = g2[hh]
            k_s[hh, :TIP, :] = k2[hh]
            v_s[hh, :TIP, :] = v2[hh]

        @pl.when(lower)
        def _():
            for hh in BOTH:
                tip_rows(hh)

        @pl.when(upper)
        def _():
            for hh in BOTH:
                tip_keys(hh, tip_st[far // 2, (far % 2 * SLOTS + row) // 2], row % 2)

        @pl.when(unit >= 2)
        def _():
            tip_done(slot)

        for n in BOTH:
            r_buf[slot, (5 + n) * TIP:(6 + n) * TIP] = pltpu.einshape("abc->bac", stage[n, :, :TIP, :])
        place = (core * SLOTS + row, slice(None), pair)

        def give(results):
            for n, dst in enumerate(results):
                pltpu.make_async_copy(r_buf.at[slot, pl.ds((5 + n) * TIP + ROWS * core, ROWS)], dst.at[place], tip_near.at[slot]).start()
                pltpu.make_async_remote_copy(
                    src_ref=r_buf.at[slot, pl.ds((5 + n) * TIP + ROWS * (1 - core), ROWS)], dst_ref=dst.at[place],
                    send_sem=tip_send.at[slot], recv_sem=out_recv, device_id=(partner,), device_id_type=MESH).start()

        @pl.when(lower)
        def _():
            give((o_out, dq_out))

        @pl.when(upper)
        def _():
            give((dk_out, dv_out))
        return carry

    def tips(third):
        @pl.when(tip)
        def _():
            if third == 0:
                wait_for(far_out, far_recv)

                @pl.when(upper)
                def _():
                    wait_for(tip_st, ts_recv)
                tip_load(0)
            lax.fori_loop(UNITS // 3 * third, UNITS // 3 * (third + 1), tip_unit, 0)
            if third == 2:
                tip_done(0)
                tip_done(1)

    send_up(0)

    def sub_body(sub, carry):
        @pl.when(sub < SUBS - 1)
        def _():
            send_up(sub + 1)

        @pl.when(sub == SLOTS)
        def _():
            swap_start(0)

        @pl.when(sub == SUBS - 1)
        def _():
            swap_add(0)
            cross_start(0)

        @pl.when(sub == SUBS)
        def _():
            swap_start(1)
            swap_add(1)
            cross_start(1)
            cross_finish(0)

        @pl.when(lower & (sub < SUBS))
        def _():
            lower_rows(sub)

        @pl.when(lower & (sub > 0))
        def _():
            lower_theirs(sub - 1)

        @pl.when(lower & (sub < SUBS))
        def _():
            lower_own(sub)

        @pl.when(upper & (sub < SUBS))
        def _():
            upper_own(sub)

        @pl.when(sub <= EARLY)
        def _():
            send_out(sub, (2, 3))

        @pl.when((sub > 0) & (sub <= EARLY))
        def _():
            send_out(sub - 1, (0, 1))
        return carry

    lax.fori_loop(0, SUBS + 1, sub_body, 0)

    cross_finish(1)
    send_out(EARLY, (0, 1))

    @pl.when(lone)
    def _():
        send_out(EARLY + 1, (2, 3))

    for p in BOTH:
        hop_wait(p, 0)
        hop_start(p, 1)

    @pl.when(jnp.logical_not(lone))
    def _():
        send_out(EARLY + 1, (2, 3))

    for p in BOTH:
        send_out(EARLY + 1 + p, range(2 * (p + 1)))
        tips(p)
        hop_wait(p, 1)
        hop_start(p, 2)

    def send_late(sub, carry):
        send_out(sub, range(4), True)
        return carry

    lax.fori_loop(EARLY + 3, SUBS, send_late, 0)
    tips(2)
    for p in BOTH:
        hop_wait(p, 2)
        hop_start(p, 3)
    for p in BOTH:
        hop_wait(p, 3)

    wait_for(buf.at[:, :, :HALF - ROWS], in_send)

    @pl.when(tip)
    def _():
        wait_for(buf.at[:, :, :HALF - 3 * ROWS // 2], out_recv)
        wait_for(buf.at[:, :, :HALF - ROWS], out_send)
        wait_for(far_out, far_send)

    @pl.when(jnp.logical_not(tip))
    def _():
        wait_for(buf, out_recv)
        wait_for(buf.at[:, :, :HALF - 2 * ROWS], out_send)

    @pl.when(upper & jnp.logical_not(tip))
    def _():
        wait_for(tip_tx, ts_send)

    @pl.when(upper)
    def _():
        wait_for(st_tx, st_send)

    wait_for(dr_rx, x_send)
    wait_for(dr_rz, z_send)
    wait_for(blocks(2), own_sem)
    sent_wait()
    for sem in (fw_send, fw_recv):
        wait_for(buf.at[:3, :, :FIN * 16 // 24], sem)


def writer(*refs):
    ins, (o, dq, dk, dv, dr, du, dw, sem) = refs[:4 + N_PART], refs[4 + N_PART:]
    pairs = list(zip(ins[:4], (o, dq, dk, dv)))
    for m, part in enumerate(ins[4:]):
        rows = min(PART, HALF - PART * m)
        for side in BOTH:
            start = HALF * side + PART * m
            pairs.append((part.at[side, :rows], dr.at[start:start + rows]))
    last = HALF - PART * (N_PART - 1)
    pairs += [(ins[-1].at[0, last], du), (ins[-1].at[0, last + 1], dw)]
    copies = [pltpu.make_async_copy(src, dst, sem.at[j]) for j, (src, dst) in enumerate(pairs)]
    for copy in copies:
        copy.start()
    for copy in copies:
        copy.wait()


def solution(mesh):
    seq_spec = P(None, "cp", None, None)

    def local(query, key_in, value, bias_u, bias_w, rel_k, d_out):
        n_batch, rows, n_heads, head_dim = query.shape
        pairs = (n_batch, rows, N_PAIR, PAIR, head_dim)
        vm = pltpu.VMEM
        dma = pltpu.SemaphoreType.DMA
        whole = pl.BlockSpec(memory_space=pl.ANY)
        act = jax.ShapeDtypeStruct(pairs, BF16)
        vec = jax.ShapeDtypeStruct((n_heads, 1, head_dim), F32)
        tok = (PAIR, SEQ, HEAD)
        tok_t = (PAIR, HEAD, SEQ)
        acc = (HEAD + 8, HALF)
        outs = pl.pallas_call(
            kernel,
            name="rel_attn",
            out_shape=(act, act, act, act,
                       *[jax.ShapeDtypeStruct((2, PART, n_heads, 1, head_dim), F32)] * N_PART,
                       jax.ShapeDtypeStruct((4, SLOTS, ROWS, FAR, PAIR, HEAD), BF16)),
            in_specs=[pl.BlockSpec(memory_space=pltpu.HBM)] * 7,
            out_specs=[whole] * (5 + N_PART),
            scratch_shapes=[
                vm((4, SUBS, HALF, PAIR, HEAD), BF16), vm((2, SUBS, HALF, PAIR, HEAD), BF16),
                vm((2, SEQ, PAIR, HEAD), BF16), vm((N_PAIR, PAIR, HEAD), BF16), vm((N_PAIR, PAIR, HEAD), BF16),
                vm((SUBS, PAIR, 8, HALF), F32), vm((SUBS, PAIR, 8, HALF), F32), vm((SUBS // 2, 8, TIP), F32), vm((3, SUBS // 2, 8, TIP), F32), vm((QB, HEAD), F32),
                vm((2, 2) + acc, F32), vm((2,) + acc, F32), vm((2, FIN, 1, HEAD), F32), vm((4, 2) + acc, F32),
                vm((QB, SEQ), F32), vm((QB, SEQ), F32), vm((QB, SEQ), F32),
                vm((QB, SEQ), BF16), vm((QB, SEQ), BF16), vm((QB, SEQ), BF16),
                vm(tok, BF16), vm(tok, BF16), vm(tok, BF16), vm(tok, BF16), vm(tok, BF16),
                vm(tok_t, BF16), vm(tok_t, BF16), vm(tok_t, BF16), vm(tok_t, BF16), vm(tok_t, BF16),
                vm((4, SEQ, HEAD), BF16), vm((4, HEAD, SEQ), BF16),
                vm((PAIR, HEAD, HALF), F32), vm((PAIR, HEAD, HALF), F32), vm((4, PAIR, HALF, HEAD), BF16),
                dma, dma((2, SUBS)), dma, dma, dma, dma((4,)), dma((4,)), dma((SUBS,)), dma, dma((4,)),
                dma, dma((2,)), dma, dma((2,)), dma, dma((2, 4)), dma, dma,
                dma, dma, dma((2,)), dma((2,)), dma((2,)), dma, dma,
            ],
            compiler_params=pltpu.CompilerParams(collective_id=0, has_side_effects=True, vmem_limit_bytes=37 * 1024 * 1024),
        )(*[pltpu.with_memory_space_constraint(x, pltpu.HBM) for x in (
            query.reshape(pairs), key_in.reshape(pairs), value.reshape(pairs), d_out.reshape(pairs),
            rel_k.reshape(SEQ, N_PAIR, PAIR, head_dim), bias_u.reshape(N_PAIR, PAIR, head_dim), bias_w.reshape(N_PAIR, PAIR, head_dim))])
        o, dq, dk, dv, dr, du, dw = pl.pallas_call(
            writer,
            name="writer",
            out_shape=(act, act, act, act, jax.ShapeDtypeStruct((SEQ, n_heads, 1, head_dim), F32), vec, vec),
            in_specs=[whole] * (4 + N_PART),
            out_specs=[whole] * 7,
            scratch_shapes=[dma((6 + 2 * N_PART,))],
            compiler_params=pltpu.CompilerParams(vmem_limit_bytes=1024 * 1024),
        )(*outs[:-1])
        full = query.shape
        return (o.reshape(full), dq.reshape(full), dk.reshape(full), dv.reshape(full),
                du.reshape(bias_u.shape), dw.reshape(bias_w.shape), dr.reshape(rel_k.shape))

    return jax.shard_map(local, mesh=mesh,
                         in_specs=(seq_spec, seq_spec, seq_spec, P(), P(), P(), seq_spec),
                         out_specs=(seq_spec, seq_spec, seq_spec, seq_spec, P(), P(), P()),
                         check_vma=False)
```

```python
import jax
import jax.numpy as jnp
from jax import lax
from jax.experimental import pallas as pl
from jax.experimental.pallas import tpu as pltpu
from jax.sharding import PartitionSpec as P

MESH = pl.DeviceIdType.MESH
BF16, F32 = jnp.bfloat16, jnp.float32
LOG2E = 1.4426950408889634

N_DEV = 16
BOTH = range(2)
PLANE = 8
PAIR = 2
N_PAIR = 8
SLOTS = 4
SUBS = 2 * SLOTS
EARLY = 3
ROWS = 64
HALF = PLANE * ROWS
SEQ = 2 * HALF
HEAD = 128
QB = 256
WIN = HALF + QB
N_PART = 6
PART = 86
FIN = N_PART * PART
TIP = 2 * ROWS
FAR = N_PAIR - 2
UNITS = FAR * SLOTS
TURNS = ((1, 3, 2), (3, 1, 2))


def dot(lhs, rhs):
    return jnp.dot(lhs, rhs, preferred_element_type=F32)


def flip8(x):
    rows, cols = x.shape
    idx = 7 - lax.broadcasted_iota(jnp.int32, (rows // 8, 8, cols), 1)
    return jnp.take_along_axis(x.reshape(rows // 8, 8, cols), idx, axis=1).reshape(rows, cols)


def eye_rev(dtype):
    total = lax.broadcasted_iota(jnp.int32, (HEAD, HEAD), 0) + lax.broadcasted_iota(jnp.int32, (HEAD, HEAD), 1)
    return jnp.where(total == HEAD - 1, 1.0, 0.0).astype(dtype)


def kernel(q_in, k_in, v_in, g_in, r_in, u_in, w_in,
           o_out, dq_out, dk_out, dv_out, dr0_out, dr1_out, dr2_out, dr3_out, dr4_out, dr5_out, far_out,
           buf, rbuf, r_buf, u_buf, w_buf, st_tx, st_rx, tip_tx, tip_st, st_ref, dr_rx, dr_rz, dr_fin, dr_acc,
           s_ref, e_ref, dp_ref, pb_ref, ds_ref, dd_ref,
           a_s, c_s, g_s, k_s, v_s, at_s, ct_s, gt_s, kt_s, vt_s, rev_s, rt_s, dkt, dvt, stage,
           in_send, in_recv, out_send, out_recv, own_sem, r_sem, up_send, up_recv, st_send, st_recv,
           x_send, x_recv, z_send, z_recv, ring_send, ring_recv, fw_send, fw_recv,
           far_send, far_recv, tip_sem, tip_near, tip_send, ts_send, ts_recv):
    me = lax.axis_index("cp")
    core = me % 2
    chip = me // 2
    col = chip % 4
    z = chip // 4
    partner = me + 1 - 2 * core
    across = me + PLANE * (1 - 2 * z)
    scale = HEAD ** -0.5

    def wait_for(ref, sem):
        pltpu.make_async_copy(ref, ref, sem).wait()

    y = col // 2
    lower, upper = z == 0, z == 1
    tip = chip == 7 * z
    tip_base = 2 - 2 * z

    tables = [pltpu.make_async_copy(src, dst, r_sem.at[j]) for j, (src, dst) in enumerate(
        ((r_in.at[:, 2 * col], r_buf.at[0]), (r_in.at[:, 2 * col + 1], r_buf.at[1]), (u_in, u_buf), (w_in, w_buf)))]
    for copy in tables:
        copy.start()

    barrier = pltpu.get_barrier_semaphore()

    for peer in [across] + [me ^ step for step in range(PLANE - 1, 0, -1)]:
        pl.semaphore_signal(barrier, inc=1, device_id=(peer,), device_id_type=MESH)
    pl.semaphore_wait(barrier, PLANE)

    my_rows = pl.ds(pl.multiple_of((me % PLANE) * ROWS, ROWS), ROWS)

    even = chip % 2 == z
    loaded = y != z
    lone = loaded & jnp.logical_not(even)

    def peers(late=False):
        near = core == 0
        if late:
            near = jnp.logical_not(near | lone)
        first, second, third = [jnp.where(near, near_turn, far_turn) for near_turn, far_turn in zip(*TURNS)]
        for turn, other in ((first, 0), (third, 0), (first, 1), (third, 1), (second, 0), (second, 1)):
            yield me ^ (2 * turn + other)
        yield partner

    def send_in(ins, sub):
        pair, row = sub // SLOTS, sub % SLOTS
        for first in (0, 2):
            for t in (first, first + 1):
                pltpu.make_async_copy(ins[t].at[core * SLOTS + row, :, 2 * col + pair], buf.at[t, sub, my_rows], in_recv.at[first // 2, sub]).start()
            for peer in peers():
                for t in (first, first + 1):
                    pltpu.make_async_remote_copy(
                        src_ref=ins[t].at[(peer % 2) * SLOTS + row, :, 2 * ((peer // 2) % 4) + pair], dst_ref=buf.at[t, sub, my_rows],
                        send_sem=in_send, recv_sem=in_recv.at[first // 2, sub], device_id=(peer,), device_id_type=MESH).start()

    def send_all(ins):
        def send_sub(sub, carry):
            send_in(ins, sub)
            return carry
        lax.fori_loop(0, SUBS, send_sub, 0)

    @pl.when(lower)
    def _():
        send_all((k_in, v_in, q_in, g_in))

    @pl.when(upper)
    def _():
        send_all((q_in, g_in, k_in, v_in))

    @pl.when(tip)
    def _():
        for t, src in enumerate((q_in, k_in, v_in, g_in)):
            for row in range(SLOTS):
                pltpu.make_async_remote_copy(
                    src_ref=src.at[(1 - core) * SLOTS + row, :, pl.ds(tip_base, FAR)], dst_ref=far_out.at[t, row],
                    send_sem=far_send, recv_sem=far_recv, device_id=(partner,), device_id_type=MESH).start()

    for copy in tables:
        copy.wait()
    rev = eye_rev(BF16)
    for p in BOTH:
        pair_tab = pltpu.einshape("abc->bac", r_buf[p])
        for hh in BOTH:
            for blk in range(SEQ // HEAD):
                part = pair_tab[hh, SEQ - HEAD * (blk + 1):SEQ - HEAD * blk]
                flipped = dot(rev, part).astype(BF16)
                rev_s[2 * p + hh, HEAD * blk:HEAD * (blk + 1), :] = flipped
                rt_s[2 * p + hh, :, HEAD * blk:HEAD * (blk + 1)] = flipped.T
    dr_acc[...] = jnp.zeros_like(dr_acc)

    acts = (dk_out, dv_out, o_out, dq_out)

    def send_out(sub, which, late=False):
        place = (core * SLOTS + sub % SLOTS, slice(None), 2 * col + sub // SLOTS)
        for t in which:
            pltpu.make_async_copy(buf.at[t, sub, my_rows], acts[t].at[place], out_recv).start()
        for peer in peers(late):
            peer_rows = pl.ds(pl.multiple_of((peer % PLANE) * ROWS, ROWS), ROWS)
            to_tip = (peer // 2 == 7 * z) & jnp.logical_not(tip)
            for t in which:
                @pl.when(jnp.logical_not(to_tip & (lower if t >= 2 else upper)))
                def _():
                    pltpu.make_async_remote_copy(
                        src_ref=buf.at[t, sub, peer_rows], dst_ref=acts[t].at[place],
                        send_sem=out_send, recv_sem=out_recv, device_id=(peer,), device_id_type=MESH).start()

    def send_up(sub):
        wait_for(buf.at[0:2, sub], in_recv.at[0, sub])
        for j in BOTH:
            pltpu.make_async_remote_copy(src_ref=buf.at[j, sub], dst_ref=rbuf.at[j, sub], send_sem=up_send.at[sub % 4], recv_sem=up_recv.at[sub],
                                         device_id=(across,), device_id_type=MESH).start()

    def unpack(ref, j, sub):
        return pltpu.einshape("abc->bac", ref[j, sub])

    def load_rows(q_ref, q_j, g_ref, g_j, sub, start, turned):
        rows = slice(start, start + HALF)
        p = sub // SLOTS
        q2 = unpack(q_ref, q_j, sub)
        u = u_buf[2 * col + p].astype(F32)
        w = w_buf[2 * col + p].astype(F32)
        for hh in BOTH:
            q32 = q2[hh].astype(F32)
            a = (q32 + u[hh:hh + 1]).astype(BF16)
            c = (q32 + w[hh:hh + 1]).astype(BF16)
            a_s[hh, rows, :] = a
            c_s[hh, rows, :] = c
            at_s[hh, :, rows] = a.T
            if turned:
                ct_s[hh, :, rows] = flip8(c.astype(F32)).astype(BF16).T
        g2 = unpack(g_ref, g_j, sub)
        g_s[:, rows, :] = g2
        for hh in BOTH:
            gt_s[hh, :, rows] = g2[hh].T

    def load_keys(k_ref, k_j, v_ref, v_j, sub, start):
        rows = slice(start, start + HALF)
        k2 = unpack(k_ref, k_j, sub)
        v2 = unpack(v_ref, v_j, sub)
        k_s[:, rows, :] = k2
        v_s[:, rows, :] = v2
        for hh in BOTH:
            kt_s[hh, :, rows] = k2[hh].T
            vt_s[hh, :, rows] = v2[hh].T

    def row_block(hh, head, start, i0, lo, fresh, stats):
        width = i0 + QB
        rows = slice(start, start + QB)
        s_ref[:, :width] = dot(a_s[hh, rows, :], kt_s[hh, :, :width])
        e_ref[:, :width] = dot(c_s[hh, rows, :], rt_s[head, :, SEQ - width:])
        dp_ref[:, :width] = dot(g_s[hh, rows, :], vt_s[hh, :, :width])
        for r0 in range(0, QB, 16):
            group = slice(r0, r0 + 16)
            rel = pltpu.roll(e_ref[group, :width], i0 + 1 + r0, 1, stride=1, stride_axis=0)
            s = s_ref[group, :width] + rel
            ahead = lax.broadcasted_iota(jnp.int32, (16, width), 1) - lax.broadcasted_iota(jnp.int32, (16, width), 0)
            s = jnp.where(ahead <= i0 + r0, s, -jnp.inf)
            top = jnp.max(s, axis=1, keepdims=True)
            p = jnp.exp2((s - top) * (scale * LOG2E))
            total = jnp.sum(p, axis=1, keepdims=True)
            p = p * (1.0 / total)
            pb_ref[group, :width] = p.astype(BF16)
            dp = dp_ref[group, :width]
            row_dot = jnp.sum(p * dp, axis=1, keepdims=True)
            ds = (p * (dp - row_dot) * scale).astype(BF16)
            ds_ref[group, :width] = ds
            flipped = flip8(ds.astype(F32))
            half = [pltpu.roll(flipped[8 * j:8 * j + 8], QB - 8 - r0 - 8 * j, 1, stride=1, stride_axis=0) for j in range(2)]
            dd_ref[group, :width] = jnp.concatenate(half, axis=0).astype(BF16)
            if stats:
                lane = lax.broadcasted_iota(jnp.int32, (16, HEAD), 1)
                st_ref[group, :] = jnp.where(lane == 0, top * (scale * LOG2E) + jnp.log2(total), row_dot)
        pb = pb_ref[:, :width]
        ds = ds_ref[:, :width]
        dd = dd_ref[:, :width]
        stage[0, hh, rows, :] = dot(pb, v_s[hh, :width, :]).astype(BF16)
        dqc = dot(ds, k_s[hh, :width, :])
        dqr = flip8(dot(dd, rev_s[head, SEQ - width:, :]))
        stage[1, hh, rows, :] = (dqc + dqr).astype(BF16)
        dr_acc[head, 1, HEAD:HEAD + 1, HALF - HEAD:] += jnp.sum(dqc, axis=0, keepdims=True)
        dr_acc[head, 1, HEAD + 1:HEAD + 2, HALF - HEAD:] += jnp.sum(dqr, axis=0, keepdims=True)
        dk_new = dot(at_s[hh, :, rows], ds_ref[:, lo:width])
        dv_new = dot(gt_s[hh, :, rows], pb_ref[:, lo:width])
        if fresh:
            dkt[hh] = dk_new
            dvt[hh] = dv_new
        else:
            dkt[hh, :, :width - lo] += dk_new
            dvt[hh, :, :width - lo] += dv_new
        dr_new = dot(ct_s[hh, :, rows], dd)
        if width > HALF:
            dr_acc[head, 0, :HEAD, SEQ - width:] += dr_new[:, :width - HALF]
            dr_acc[head, 1, :HEAD, :] += dr_new[:, width - HALF:]
        else:
            dr_acc[head, 1, :HEAD, HALF - width:] += dr_new

    def col_block(hh, head, sub, i0):
        rows = slice(i0, i0 + QB)
        first = WIN - i0
        s_ref[:, :HALF] = dot(a_s[hh, rows, :], kt_s[hh, :, :HALF])
        e_ref[:, :WIN] = dot(c_s[hh, rows, :], rt_s[head, :, first:first + WIN])
        dp_ref[:, :HALF] = dot(g_s[hh, rows, :], vt_s[hh, :, :HALF])
        st_ref[:, :8] = st_rx[sub, hh, :, i0 - HALF:i0 - HALF + QB].T
        for r0 in range(0, QB, 16):
            group = slice(r0, r0 + 16)
            rel = pltpu.roll(e_ref[group, :WIN], HALF + 1 + r0, 1, stride=1, stride_axis=0)[:, :HALF]
            log_sum = st_ref[group, 0:1]
            row_dot = st_ref[group, 1:2]
            p = jnp.exp2((s_ref[group, :HALF] + rel) * (scale * LOG2E) - log_sum)
            pb_ref[group, :HALF] = p.astype(BF16)
            ds_ref[group, :HALF] = (p * (dp_ref[group, :HALF] - row_dot) * scale).astype(BF16)
        dkt[hh] += dot(at_s[hh, :, rows], ds_ref[:, :HALF])
        dvt[hh] += dot(gt_s[hh, :, rows], pb_ref[:, :HALF])

    def store_rows(sub):
        for t in BOTH:
            buf[2 + t, sub] = pltpu.einshape("abc->bac", stage[t])

    def store_keys(sub):
        for hh in BOTH:
            stage[2, hh] = dkt[hh].astype(BF16).T
            stage[3, hh] = dvt[hh].astype(BF16).T
        for t in BOTH:
            buf[t, sub] = pltpu.einshape("abc->bac", stage[2 + t])

    def wait_up(sub):
        wait_for(rbuf.at[:, sub], up_recv.at[sub])
        wait_for(rbuf.at[:, sub], up_send.at[sub % 4])

    def wait_in(sub):
        wait_for(buf.at[2:4, sub], in_recv.at[1, sub])

    def lower_rows(sub):
        wait_in(sub)
        load_rows(buf, 2, buf, 3, sub, 0, True)

    def lower_own(sub):
        load_keys(buf, 0, buf, 1, sub, 0)

        def own(hh, carry):
            head = 2 * (sub // SLOTS) + hh
            row_block(hh, head, QB, QB, 0, True, False)
            row_block(hh, head, 0, 0, 0, False, False)
            return carry

        lax.fori_loop(0, PAIR, own, 0)
        store_rows(sub)

    def lower_theirs(sub):
        wait_up(sub)
        load_rows(rbuf, 0, rbuf, 1, sub, HALF, False)
        wait_for(st_rx.at[sub], st_recv.at[sub % 4])

        def theirs(hh, carry):
            head = 2 * (sub // SLOTS) + hh
            col_block(hh, head, sub, HALF)
            col_block(hh, head, sub, HALF + QB)
            return carry

        lax.fori_loop(0, PAIR, theirs, 0)
        store_keys(sub)

    def upper_own(sub):
        wait_in(sub)
        wait_up(sub)
        load_rows(buf, 0, buf, 1, sub, 0, True)
        load_keys(rbuf, 0, rbuf, 1, sub, 0)
        load_keys(buf, 2, buf, 3, sub, HALF)

        def own(hh, carry):
            head = 2 * (sub // SLOTS) + hh
            for blk in (1, 0):
                row_block(hh, head, QB * blk, HALF + QB * blk, HALF, blk == 1, True)
                st_tx[sub, hh, :, QB * blk:QB * (blk + 1)] = st_ref[...].T[:8]
            pltpu.make_async_remote_copy(src_ref=st_tx.at[sub, hh], dst_ref=st_rx.at[sub, hh], send_sem=st_send, recv_sem=st_recv.at[sub % 4],
                                         device_id=(across,), device_id_type=MESH).start()
            place = 2 * (sub % 2 * PAIR + hh)
            row_id = lax.broadcasted_iota(jnp.int32, (8, TIP), 0)
            tile = tip_tx[sub // 2]
            for j in BOTH:
                tile = jnp.where(row_id == place + j, st_tx[sub, hh, j:j + 1, HALF - TIP:], tile)
            tip_tx[sub // 2] = tile
            return carry

        lax.fori_loop(0, PAIR, own, 0)

        @pl.when(jnp.logical_not(tip) & (sub % 2 == 1))
        def _():
            pltpu.make_async_remote_copy(src_ref=tip_tx.at[sub // 2], dst_ref=tip_st.at[col, sub // 2], send_sem=ts_send, recv_sem=ts_recv,
                                         device_id=(N_DEV - 2 + core,), device_id_type=MESH).start()
        store_rows(sub)
        store_keys(sub)

    side = 1 - core
    parts = (dr0_out, dr1_out, dr2_out, dr3_out, dr4_out, dr5_out)

    def swap_start(p):
        for n in BOTH:
            pltpu.make_async_remote_copy(src_ref=dr_acc.at[2 * p + n, side], dst_ref=dr_rx.at[p, n], send_sem=x_send, recv_sem=x_recv.at[p],
                                         device_id=(partner,), device_id_type=MESH).start()

    def swap_add(p):
        wait_for(dr_rx.at[p], x_recv.at[p])
        for n in BOTH:
            dr_rx[p, n] = dr_rx[p, n] + dr_acc[2 * p + n, core]

    def cross_start(p):
        pltpu.make_async_remote_copy(src_ref=dr_rx.at[p, 1 - z], dst_ref=dr_rz.at[p], send_sem=z_send, recv_sem=z_recv.at[p],
                                     device_id=(across,), device_id_type=MESH).start()

    def head_of(p, bits):
        other = chip ^ bits
        return 4 * (other % 4) + 2 * p + other // 4

    def block(p, m, bits):
        if bits == 0:
            return dr_fin.at[p, PART * m:PART * (m + 1)]
        return parts[m].at[side, :, head_of(p, bits)]

    def forward(p, m, bits):
        pltpu.make_async_remote_copy(src_ref=block(p, m, bits), dst_ref=parts[m].at[side, :, head_of(p, bits)], send_sem=fw_send,
                                     recv_sem=fw_recv, device_id=(partner,), device_id_type=MESH).start()

    def blocks(count):
        return parts[0].at[:, :, :N_PART // 2 * count]

    def pass_on(p, bits, hop, device):
        for m in range(N_PART):
            pltpu.make_async_remote_copy(
                src_ref=block(p, m, bits), dst_ref=parts[m].at[side, :, head_of(p, bits)], send_sem=ring_send,
                recv_sem=ring_recv.at[p, hop], device_id=(device,), device_id_type=MESH).start()

    def hand_over(p, bits):
        for m in range(N_PART):
            forward(p, m, bits)

    along_x, along_y = me ^ 2, me ^ 4

    def hop_start(p, hop):
        if hop == 0:
            for device in (along_x, along_y, across):
                pass_on(p, 0, 0, device)
        if hop == 1:
            @pl.when(even & loaded)
            def _():
                pass_on(p, 1, 1, along_y)

            @pl.when(jnp.logical_not(even) & loaded)
            def _():
                pass_on(p, 2, 1, along_x)

            pass_on(p, 1, 1, across)
            pass_on(p, 2, 1, across)
        if hop == 2:
            @pl.when(even & loaded)
            def _():
                pass_on(p, 5, 2, along_y)

            @pl.when(jnp.logical_not(even) & loaded)
            def _():
                pass_on(p, 6, 2, along_x)

            @pl.when(even)
            def _():
                pass_on(p, 3, 2, across)
        if hop == 3:
            @pl.when(even)
            def _():
                pass_on(p, 7, 3, across)

    def hop_wait(p, hop):
        if hop == 0:
            wait_for(blocks(3), ring_recv.at[p, 0])
            for bits in (1, 2, 4):
                hand_over(p, bits)
        if hop == 1:
            @pl.when(even)
            def _():
                wait_for(blocks(3), ring_recv.at[p, 1])
                hand_over(p, 3)

            @pl.when(jnp.logical_not(even))
            def _():
                wait_for(blocks(2), ring_recv.at[p, 1])
            for bits in (5, 6):
                hand_over(p, bits)
        if hop == 2:
            wait_for(blocks(1), ring_recv.at[p, 2])
            hand_over(p, 7)
        if hop == 3:
            @pl.when(jnp.logical_not(even))
            def _():
                wait_for(blocks(1), ring_recv.at[p, 3])
                hand_over(p, 3)

    def sent_wait():
        @pl.when(even & loaded)
        def _():
            wait_for(buf.at[:3, :, :FIN * 18 // 24], ring_send)

        @pl.when(even != loaded)
        def _():
            wait_for(buf.at[:3, :7, :FIN * 14 // 21], ring_send)

        @pl.when(jnp.logical_not(even | loaded))
        def _():
            wait_for(buf.at[:2, :6, :FIN * 10 // 12], ring_send)

    def cross_finish(p):
        wait_for(dr_rz.at[p], z_recv.at[p])
        total = dr_rx[p, z] + dr_rz[p]
        rev32 = eye_rev(F32)
        for m in range(HALF // HEAD):
            part = total[:HEAD, HALF - HEAD * (m + 1):HALF - HEAD * m]
            turned = lax.dot_general(rev32, part, (((1,), (1,)), ((), ())), precision=lax.Precision.HIGHEST, preferred_element_type=F32)
            dr_fin[p, HEAD * m:HEAD * (m + 1)] = turned.reshape(HEAD, 1, HEAD)
        dr_fin[p, HALF] = total[HEAD:HEAD + 1, HALF - HEAD:]
        dr_fin[p, HALF + 1] = total[HEAD + 1:HEAD + 2, HALF - HEAD:]
        dr_fin[p, HALF + 2:] = jnp.zeros((FIN - HALF - 2, 1, HEAD), F32)
        hop_start(p, 0)
        for m in range(N_PART):
            pltpu.make_async_copy(block(p, m, 0), parts[m].at[side, :, head_of(p, 0)], own_sem).start()
        hand_over(p, 0)

    def tip_load(unit):
        slot, row, far = unit % 2, unit // FAR, unit % FAR
        pair = far + tip_base
        for t, src in enumerate((q_in, k_in, v_in, g_in)):
            pltpu.make_async_copy(src.at[core * SLOTS + row, :, pair], r_buf.at[slot, pl.ds(TIP * t + ROWS * core, ROWS)], tip_sem.at[slot]).start()
            pltpu.make_async_copy(far_out.at[t, row, :, far], r_buf.at[slot, pl.ds(TIP * t + ROWS * (1 - core), ROWS)], tip_sem.at[slot]).start()
        pltpu.make_async_copy(r_in.at[:TIP, pair], r_buf.at[slot, 4 * TIP:5 * TIP], tip_sem.at[slot]).start()

    def tip_done(slot):
        wait_for(r_buf.at[slot, :TIP], tip_near.at[slot])
        wait_for(r_buf.at[slot, :TIP], tip_send.at[slot])

    def tip_group(hh, r0):
        group = slice(TIP * hh + r0, TIP * hh + r0 + 16)
        rel = pltpu.roll(e_ref[group, :TIP], 1 + r0, 1, stride=1, stride_axis=0)
        ahead = lax.broadcasted_iota(jnp.int32, (16, TIP), 1) - lax.broadcasted_iota(jnp.int32, (16, TIP), 0)
        return group, s_ref[group, :TIP] + rel, ahead <= r0

    def tip_rows(hh):
        for r0 in range(0, TIP, 16):
            group, s, seen = tip_group(hh, r0)
            s = jnp.where(seen, s, -jnp.inf)
            top = jnp.max(s, axis=1, keepdims=True)
            p = jnp.exp2((s - top) * (scale * LOG2E))
            p = p * (1.0 / jnp.sum(p, axis=1, keepdims=True))
            pb_ref[group, :TIP] = p.astype(BF16)
            dp = dp_ref[group, :TIP]
            row_dot = jnp.sum(p * dp, axis=1, keepdims=True)
            ds = (p * (dp - row_dot) * scale).astype(BF16)
            ds_ref[group, :TIP] = ds
            flipped = flip8(ds.astype(F32))
            half = [pltpu.roll(flipped[8 * j:8 * j + 8], TIP - 8 - r0 - 8 * j, 1, stride=1, stride_axis=0) for j in range(2)]
            dd_ref[group, :TIP] = jnp.concatenate(half, axis=0).astype(BF16)
        rows = slice(TIP * hh, TIP * (hh + 1))
        stage[0, hh, :TIP, :] = dot(pb_ref[rows, :TIP], v_s[hh, :TIP, :]).astype(BF16)
        dqc = dot(ds_ref[rows, :TIP], k_s[hh, :TIP, :])
        dqr = flip8(dot(dd_ref[rows, :TIP], c_s[hh, :TIP, :]))
        stage[1, hh, :TIP, :] = (dqc + dqr).astype(BF16)

    def tip_keys(hh, stats, odd):
        rows = slice(TIP * hh, TIP * (hh + 1))
        by_row = stats.T
        even_row, odd_row = [by_row[:, n:n + 2] for n in (2 * hh, 2 * (hh + PAIR))]
        st_ref[rows, :2] = jnp.where(odd == 1, odd_row, even_row)
        for r0 in range(0, TIP, 16):
            group, s, seen = tip_group(hh, r0)
            p = jnp.where(seen, jnp.exp2(s * (scale * LOG2E) - st_ref[group, 0:1]), 0.0)
            pb_ref[group, :TIP] = p.astype(BF16)
            ds_ref[group, :TIP] = (p * (dp_ref[group, :TIP] - st_ref[group, 1:2]) * scale).astype(BF16)
        over_rows = (((0,), (0,)), ((), ()))
        stage[0, hh, :TIP, :] = lax.dot_general(ds_ref[rows, :TIP], a_s[hh, :TIP, :], over_rows, preferred_element_type=F32).astype(BF16)
        stage[1, hh, :TIP, :] = lax.dot_general(pb_ref[rows, :TIP], g_s[hh, :TIP, :], over_rows, preferred_element_type=F32).astype(BF16)

    def tip_unit(unit, carry):
        slot, row, far = unit % 2, unit // FAR, unit % FAR
        pair = far + tip_base
        wait_for(r_buf.at[slot, :5 * TIP], tip_sem.at[slot])

        @pl.when(unit + 1 < UNITS)
        def _():
            tip_load(unit + 1)

        q2, k2, v2, g2, r2 = [pltpu.einshape("abc->bac", r_buf[slot, TIP * t:TIP * (t + 1)]) for t in range(5)]
        u = u_buf[pair].astype(F32)
        w = w_buf[pair].astype(F32)
        for hh in BOTH:
            rows = slice(TIP * hh, TIP * (hh + 1))
            q32 = q2[hh].astype(F32)
            a = (q32 + u[hh:hh + 1]).astype(BF16)
            c = (q32 + w[hh:hh + 1]).astype(BF16)
            falling = dot(eye_rev(BF16), r2[hh]).astype(BF16)
            s_ref[rows, :TIP] = dot(a, k2[hh].T)
            e_ref[rows, :TIP] = dot(c, falling.T)
            dp_ref[rows, :TIP] = dot(g2[hh], v2[hh].T)
            a_s[hh, :TIP, :] = a
            c_s[hh, :TIP, :] = falling
            g_s[hh, :TIP, :] = g2[hh]
            k_s[hh, :TIP, :] = k2[hh]
            v_s[hh, :TIP, :] = v2[hh]

        @pl.when(lower)
        def _():
            for hh in BOTH:
                tip_rows(hh)

        @pl.when(upper)
        def _():
            for hh in BOTH:
                tip_keys(hh, tip_st[far // 2, (far % 2 * SLOTS + row) // 2], row % 2)

        @pl.when(unit >= 2)
        def _():
            tip_done(slot)

        for n in BOTH:
            r_buf[slot, (5 + n) * TIP:(6 + n) * TIP] = pltpu.einshape("abc->bac", stage[n, :, :TIP, :])
        place = (core * SLOTS + row, slice(None), pair)

        def give(results):
            for n, dst in enumerate(results):
                pltpu.make_async_copy(r_buf.at[slot, pl.ds((5 + n) * TIP + ROWS * core, ROWS)], dst.at[place], tip_near.at[slot]).start()
                pltpu.make_async_remote_copy(
                    src_ref=r_buf.at[slot, pl.ds((5 + n) * TIP + ROWS * (1 - core), ROWS)], dst_ref=dst.at[place],
                    send_sem=tip_send.at[slot], recv_sem=out_recv, device_id=(partner,), device_id_type=MESH).start()

        @pl.when(lower)
        def _():
            give((o_out, dq_out))

        @pl.when(upper)
        def _():
            give((dk_out, dv_out))
        return carry

    def tips(third):
        @pl.when(tip)
        def _():
            if third == 0:
                wait_for(far_out, far_recv)

                @pl.when(upper)
                def _():
                    wait_for(tip_st, ts_recv)
                tip_load(0)
            lax.fori_loop(UNITS // 3 * third, UNITS // 3 * (third + 1), tip_unit, 0)
            if third == 2:
                tip_done(0)
                tip_done(1)

    send_up(0)

    def sub_body(sub, carry):
        @pl.when(sub < SUBS - 1)
        def _():
            send_up(sub + 1)

        @pl.when(sub == SLOTS)
        def _():
            swap_start(0)

        @pl.when(sub == SUBS - 1)
        def _():
            swap_add(0)
            cross_start(0)

        @pl.when(sub == SUBS)
        def _():
            swap_start(1)
            swap_add(1)
            cross_start(1)
            cross_finish(0)

        @pl.when(lower & (sub < SUBS))
        def _():
            lower_rows(sub)

        @pl.when(lower & (sub > 0))
        def _():
            lower_theirs(sub - 1)

        @pl.when(lower & (sub < SUBS))
        def _():
            lower_own(sub)

        @pl.when(upper & (sub < SUBS))
        def _():
            upper_own(sub)

        @pl.when(sub <= EARLY)
        def _():
            send_out(sub, (2, 3))

        @pl.when((sub > 0) & (sub <= EARLY))
        def _():
            send_out(sub - 1, (0, 1))
        return carry

    lax.fori_loop(0, SUBS + 1, sub_body, 0)

    cross_finish(1)
    send_out(EARLY, (0, 1))

    @pl.when(lone)
    def _():
        send_out(EARLY + 1, (2, 3))

    for p in BOTH:
        hop_wait(p, 0)
        hop_start(p, 1)

    @pl.when(lone)
    def _():
        send_out(EARLY + 1, BOTH)

    @pl.when(jnp.logical_not(lone))
    def _():
        send_out(EARLY + 1, range(4))

    for p in BOTH:
        if p:
            send_out(EARLY + 2, range(4))
        tips(p)
        hop_wait(p, 1)
        hop_start(p, 2)

    def send_late(sub, carry):
        send_out(sub, range(4), True)
        return carry

    lax.fori_loop(EARLY + 3, SUBS, send_late, 0)
    tips(2)
    for p in BOTH:
        hop_wait(p, 2)
        hop_start(p, 3)
    for p in BOTH:
        hop_wait(p, 3)

    wait_for(buf.at[:, :, :HALF - ROWS], in_send)

    @pl.when(tip)
    def _():
        wait_for(buf.at[:, :, :HALF - 3 * ROWS // 2], out_recv)
        wait_for(buf.at[:, :, :HALF - ROWS], out_send)
        wait_for(far_out, far_send)

    @pl.when(jnp.logical_not(tip))
    def _():
        wait_for(buf, out_recv)
        wait_for(buf.at[:, :, :HALF - 2 * ROWS], out_send)

    @pl.when(upper & jnp.logical_not(tip))
    def _():
        wait_for(tip_tx, ts_send)

    @pl.when(upper)
    def _():
        wait_for(st_tx, st_send)

    wait_for(dr_rx, x_send)
    wait_for(dr_rz, z_send)
    wait_for(blocks(2), own_sem)
    sent_wait()
    for sem in (fw_send, fw_recv):
        wait_for(buf.at[:3, :, :FIN * 16 // 24], sem)


def writer(*refs):
    ins, (o, dq, dk, dv, dr, du, dw, sem) = refs[:4 + N_PART], refs[4 + N_PART:]
    pairs = list(zip(ins[:4], (o, dq, dk, dv)))
    for m, part in enumerate(ins[4:]):
        rows = min(PART, HALF - PART * m)
        for side in BOTH:
            start = HALF * side + PART * m
            pairs.append((part.at[side, :rows], dr.at[start:start + rows]))
    last = HALF - PART * (N_PART - 1)
    pairs += [(ins[-1].at[0, last], du), (ins[-1].at[0, last + 1], dw)]
    copies = [pltpu.make_async_copy(src, dst, sem.at[j]) for j, (src, dst) in enumerate(pairs)]
    for copy in copies:
        copy.start()
    for copy in copies:
        copy.wait()


def solution(mesh):
    seq_spec = P(None, "cp", None, None)

    def local(query, key_in, value, bias_u, bias_w, rel_k, d_out):
        n_batch, rows, n_heads, head_dim = query.shape
        pairs = (n_batch, rows, N_PAIR, PAIR, head_dim)
        vm = pltpu.VMEM
        dma = pltpu.SemaphoreType.DMA
        whole = pl.BlockSpec(memory_space=pl.ANY)
        act = jax.ShapeDtypeStruct(pairs, BF16)
        vec = jax.ShapeDtypeStruct((n_heads, 1, head_dim), F32)
        tok = (PAIR, SEQ, HEAD)
        tok_t = (PAIR, HEAD, SEQ)
        acc = (HEAD + 8, HALF)
        outs = pl.pallas_call(
            kernel,
            name="rel_attn",
            out_shape=(act, act, act, act,
                       *[jax.ShapeDtypeStruct((2, PART, n_heads, 1, head_dim), F32)] * N_PART,
                       jax.ShapeDtypeStruct((4, SLOTS, ROWS, FAR, PAIR, HEAD), BF16)),
            in_specs=[pl.BlockSpec(memory_space=pltpu.HBM)] * 7,
            out_specs=[whole] * (5 + N_PART),
            scratch_shapes=[
                vm((4, SUBS, HALF, PAIR, HEAD), BF16), vm((2, SUBS, HALF, PAIR, HEAD), BF16),
                vm((2, SEQ, PAIR, HEAD), BF16), vm((N_PAIR, PAIR, HEAD), BF16), vm((N_PAIR, PAIR, HEAD), BF16),
                vm((SUBS, PAIR, 8, HALF), F32), vm((SUBS, PAIR, 8, HALF), F32), vm((SUBS // 2, 8, TIP), F32), vm((3, SUBS // 2, 8, TIP), F32), vm((QB, HEAD), F32),
                vm((2, 2) + acc, F32), vm((2,) + acc, F32), vm((2, FIN, 1, HEAD), F32), vm((4, 2) + acc, F32),
                vm((QB, SEQ), F32), vm((QB, SEQ), F32), vm((QB, SEQ), F32),
                vm((QB, SEQ), BF16), vm((QB, SEQ), BF16), vm((QB, SEQ), BF16),
                vm(tok, BF16), vm(tok, BF16), vm(tok, BF16), vm(tok, BF16), vm(tok, BF16),
                vm(tok_t, BF16), vm(tok_t, BF16), vm(tok_t, BF16), vm(tok_t, BF16), vm(tok_t, BF16),
                vm((4, SEQ, HEAD), BF16), vm((4, HEAD, SEQ), BF16),
                vm((PAIR, HEAD, HALF), F32), vm((PAIR, HEAD, HALF), F32), vm((4, PAIR, HALF, HEAD), BF16),
                dma, dma((2, SUBS)), dma, dma, dma, dma((4,)), dma((4,)), dma((SUBS,)), dma, dma((4,)),
                dma, dma((2,)), dma, dma((2,)), dma, dma((2, 4)), dma, dma,
                dma, dma, dma((2,)), dma((2,)), dma((2,)), dma, dma,
            ],
            compiler_params=pltpu.CompilerParams(collective_id=0, has_side_effects=True, vmem_limit_bytes=37 * 1024 * 1024),
        )(*[pltpu.with_memory_space_constraint(x, pltpu.HBM) for x in (
            query.reshape(pairs), key_in.reshape(pairs), value.reshape(pairs), d_out.reshape(pairs),
            rel_k.reshape(SEQ, N_PAIR, PAIR, head_dim), bias_u.reshape(N_PAIR, PAIR, head_dim), bias_w.reshape(N_PAIR, PAIR, head_dim))])
        o, dq, dk, dv, dr, du, dw = pl.pallas_call(
            writer,
            name="writer",
            out_shape=(act, act, act, act, jax.ShapeDtypeStruct((SEQ, n_heads, 1, head_dim), F32), vec, vec),
            in_specs=[whole] * (4 + N_PART),
            out_specs=[whole] * 7,
            scratch_shapes=[dma((6 + 2 * N_PART,))],
            compiler_params=pltpu.CompilerParams(vmem_limit_bytes=1024 * 1024),
        )(*outs[:-1])
        full = query.shape
        return (o.reshape(full), dq.reshape(full), dk.reshape(full), dv.reshape(full),
                du.reshape(bias_u.shape), dw.reshape(bias_w.shape), dr.reshape(rel_k.shape))

    return jax.shard_map(local, mesh=mesh,
                         in_specs=(seq_spec, seq_spec, seq_spec, P(), P(), P(), seq_spec),
                         out_specs=(seq_spec, seq_spec, seq_spec, seq_spec, P(), P(), P()),
                         check_vma=False)
```

```python
import jax
import jax.numpy as jnp
from jax import lax
from jax.experimental import pallas as pl
from jax.experimental.pallas import tpu as pltpu
from jax.sharding import PartitionSpec as P

MESH = pl.DeviceIdType.MESH
BF16, F32 = jnp.bfloat16, jnp.float32
LOG2E = 1.4426950408889634

N_DEV = 16
BOTH = range(2)
ALL = range(4)
PLANE = 8
PAIR = 2
N_PAIR = 8
SLOTS = 4
SUBS = 2 * SLOTS
EARLY = 3
ROWS = 64
HALF = PLANE * ROWS
SEQ = 2 * HALF
HEAD = 128
QB = 256
WIN = HALF + QB
N_PART = 6
PART = 86
FIN = N_PART * PART
TIP = 2 * ROWS
FAR = N_PAIR - 2
UNITS = FAR * SLOTS
TURNS = ((1, 3, 2), (3, 1, 2))


def dot(lhs, rhs):
    return jnp.dot(lhs, rhs, preferred_element_type=F32)


def flip8(x):
    rows, cols = x.shape
    idx = 7 - lax.broadcasted_iota(jnp.int32, (rows // 8, 8, cols), 1)
    return jnp.take_along_axis(x.reshape(rows // 8, 8, cols), idx, axis=1).reshape(rows, cols)


def eye_rev(dtype):
    total = lax.broadcasted_iota(jnp.int32, (HEAD, HEAD), 0) + lax.broadcasted_iota(jnp.int32, (HEAD, HEAD), 1)
    return jnp.where(total == HEAD - 1, 1.0, 0.0).astype(dtype)


def kernel(q_in, k_in, v_in, g_in, r_in, u_in, w_in,
           o_out, dq_out, dk_out, dv_out, dr0_out, dr1_out, dr2_out, dr3_out, dr4_out, dr5_out, far_out,
           buf, rbuf, r_buf, u_buf, w_buf, st_tx, st_rx, tip_tx, tip_st, st_ref, dr_rx, dr_rz, dr_fin, dr_acc,
           s_ref, e_ref, dp_ref, pb_ref, ds_ref, dd_ref,
           a_s, c_s, g_s, k_s, v_s, at_s, ct_s, gt_s, kt_s, vt_s, rev_s, rt_s, dkt, dvt, stage,
           in_send, in_recv, out_send, out_recv, own_sem, r_sem, up_send, up_recv, st_send, st_recv,
           x_recv, z_recv, ring_send, ring_recv, fw_send, fw_recv,
           far_send, far_recv, tip_sem, tip_send, ts_recv):
    me = lax.axis_index("cp")
    core = me % 2
    chip = me // 2
    col = chip % 4
    z = chip // 4
    partner = me + 1 - 2 * core
    across = me + PLANE * (1 - 2 * z)
    scale = HEAD ** -0.5

    def wait_for(ref, sem):
        pltpu.make_async_copy(ref, ref, sem).wait()

    y = col // 2
    lower, upper = z == 0, z == 1
    tip = chip == 7 * z
    tip_base = 2 - 2 * z

    tables = [pltpu.make_async_copy(src, dst, r_sem.at[j]) for j, (src, dst) in enumerate(
        ((r_in.at[:, 2 * col], r_buf.at[0]), (r_in.at[:, 2 * col + 1], r_buf.at[1]), (u_in, u_buf), (w_in, w_buf)))]
    for copy in tables:
        copy.start()

    barrier = pltpu.get_barrier_semaphore()

    for peer in [across] + [me ^ step for step in range(PLANE - 1, 0, -1)]:
        pl.semaphore_signal(barrier, inc=1, device_id=(peer,), device_id_type=MESH)
    pl.semaphore_wait(barrier, PLANE)

    my_rows = pl.ds(pl.multiple_of((me % PLANE) * ROWS, ROWS), ROWS)

    even = chip % 2 == z
    loaded = y != z
    lone = loaded & jnp.logical_not(even)

    def peers(late=False):
        near = core == 0
        if late:
            near = jnp.logical_not(near | lone)
        first, second, third = [jnp.where(near, near_turn, far_turn) for near_turn, far_turn in zip(*TURNS)]
        for turn, other in ((first, 0), (third, 0), (first, 1), (third, 1), (second, 0), (second, 1)):
            yield me ^ (2 * turn + other)
        yield partner

    def send_in(ins, sub):
        pair, row = sub // SLOTS, sub % SLOTS
        for first in (0, 2):
            for t in (first, first + 1):
                pltpu.make_async_copy(ins[t].at[core * SLOTS + row, :, 2 * col + pair], buf.at[t, sub, my_rows], in_recv.at[first // 2, sub]).start()
            for peer in peers():
                for t in (first, first + 1):
                    pltpu.make_async_remote_copy(
                        src_ref=ins[t].at[(peer % 2) * SLOTS + row, :, 2 * ((peer // 2) % 4) + pair], dst_ref=buf.at[t, sub, my_rows],
                        send_sem=in_send, recv_sem=in_recv.at[first // 2, sub], device_id=(peer,), device_id_type=MESH).start()

    def send_all(ins):
        def send_sub(sub, carry):
            send_in(ins, sub)
            return carry
        lax.fori_loop(0, SUBS, send_sub, 0)

    @pl.when(lower)
    def _():
        send_all((k_in, v_in, q_in, g_in))

    @pl.when(upper)
    def _():
        send_all((q_in, g_in, k_in, v_in))

    @pl.when(tip)
    def _():
        for t, src in enumerate((q_in, k_in, v_in, g_in)):
            for row in range(SLOTS):
                pltpu.make_async_remote_copy(
                    src_ref=src.at[(1 - core) * SLOTS + row, :, pl.ds(tip_base, FAR)], dst_ref=far_out.at[t, row],
                    send_sem=far_send, recv_sem=far_recv, device_id=(partner,), device_id_type=MESH).start()

    for copy in tables:
        copy.wait()
    rev = eye_rev(BF16)
    for p in BOTH:
        pair_tab = pltpu.einshape("abc->bac", r_buf[p])
        for hh in BOTH:
            for blk in range(SEQ // HEAD):
                part = pair_tab[hh, SEQ - HEAD * (blk + 1):SEQ - HEAD * blk]
                flipped = dot(rev, part).astype(BF16)
                rev_s[2 * p + hh, HEAD * blk:HEAD * (blk + 1), :] = flipped
                rt_s[2 * p + hh, :, HEAD * blk:HEAD * (blk + 1)] = flipped.T
    dr_acc[...] = jnp.zeros_like(dr_acc)

    acts = (dk_out, dv_out, o_out, dq_out)

    def send_out(sub, which, late=False):
        place = (core * SLOTS + sub % SLOTS, slice(None), 2 * col + sub // SLOTS)
        for t in which:
            pltpu.make_async_copy(buf.at[t, sub, my_rows], acts[t].at[place], out_recv).start()
        for peer in peers(late):
            peer_rows = pl.ds(pl.multiple_of((peer % PLANE) * ROWS, ROWS), ROWS)
            to_tip = (peer // 2 == 7 * z) & jnp.logical_not(tip)
            for t in which:
                @pl.when(jnp.logical_not(to_tip & (lower if t >= 2 else upper)))
                def _():
                    pltpu.make_async_remote_copy(
                        src_ref=buf.at[t, sub, peer_rows], dst_ref=acts[t].at[place],
                        send_sem=out_send, recv_sem=out_recv, device_id=(peer,), device_id_type=MESH).start()

    def send_up(sub):
        wait_for(buf.at[0:2, sub], in_recv.at[0, sub])
        for j in BOTH:
            pltpu.make_async_remote_copy(src_ref=buf.at[j, sub], dst_ref=rbuf.at[j, sub], send_sem=up_send.at[sub % 4], recv_sem=up_recv.at[sub],
                                         device_id=(across,), device_id_type=MESH).start()

    def unpack(ref, j, sub):
        return pltpu.einshape("abc->bac", ref[j, sub])

    def load_rows(q_ref, q_j, g_ref, g_j, sub, start, turned):
        rows = slice(start, start + HALF)
        p = sub // SLOTS
        q2 = unpack(q_ref, q_j, sub)
        u = u_buf[2 * col + p].astype(F32)
        w = w_buf[2 * col + p].astype(F32)
        for hh in BOTH:
            q32 = q2[hh].astype(F32)
            a = (q32 + u[hh:hh + 1]).astype(BF16)
            c = (q32 + w[hh:hh + 1]).astype(BF16)
            a_s[hh, rows, :] = a
            c_s[hh, rows, :] = c
            at_s[hh, :, rows] = a.T
            if turned:
                ct_s[hh, :, rows] = flip8(c.astype(F32)).astype(BF16).T
        g2 = unpack(g_ref, g_j, sub)
        g_s[:, rows, :] = g2
        for hh in BOTH:
            gt_s[hh, :, rows] = g2[hh].T

    def load_keys(k_ref, k_j, v_ref, v_j, sub, start):
        rows = slice(start, start + HALF)
        k2 = unpack(k_ref, k_j, sub)
        v2 = unpack(v_ref, v_j, sub)
        k_s[:, rows, :] = k2
        v_s[:, rows, :] = v2
        for hh in BOTH:
            kt_s[hh, :, rows] = k2[hh].T
            vt_s[hh, :, rows] = v2[hh].T

    def row_block(hh, head, start, i0, lo, fresh, stats):
        width = i0 + QB
        rows = slice(start, start + QB)
        s_ref[:, :width] = dot(a_s[hh, rows, :], kt_s[hh, :, :width])
        e_ref[:, :width] = dot(c_s[hh, rows, :], rt_s[head, :, SEQ - width:])
        dp_ref[:, :width] = dot(g_s[hh, rows, :], vt_s[hh, :, :width])
        for r0 in range(0, QB, 16):
            group = slice(r0, r0 + 16)
            rel = pltpu.roll(e_ref[group, :width], i0 + 1 + r0, 1, stride=1, stride_axis=0)
            s = s_ref[group, :width] + rel
            ahead = lax.broadcasted_iota(jnp.int32, (16, width), 1) - lax.broadcasted_iota(jnp.int32, (16, width), 0)
            s = jnp.where(ahead <= i0 + r0, s, -jnp.inf)
            top = jnp.max(s, axis=1, keepdims=True)
            p = jnp.exp2((s - top) * (scale * LOG2E))
            total = jnp.sum(p, axis=1, keepdims=True)
            p = p * (1.0 / total)
            pb_ref[group, :width] = p.astype(BF16)
            dp = dp_ref[group, :width]
            row_dot = jnp.sum(p * dp, axis=1, keepdims=True)
            ds = (p * (dp - row_dot) * scale).astype(BF16)
            ds_ref[group, :width] = ds
            flipped = flip8(ds.astype(F32))
            half = [pltpu.roll(flipped[8 * j:8 * j + 8], QB - 8 - r0 - 8 * j, 1, stride=1, stride_axis=0) for j in range(2)]
            dd_ref[group, :width] = jnp.concatenate(half, axis=0).astype(BF16)
            if stats:
                lane = lax.broadcasted_iota(jnp.int32, (16, HEAD), 1)
                st_ref[group, :] = jnp.where(lane == 0, top * (scale * LOG2E) + jnp.log2(total), row_dot)
        pb = pb_ref[:, :width]
        ds = ds_ref[:, :width]
        dd = dd_ref[:, :width]
        stage[0, hh, rows, :] = dot(pb, v_s[hh, :width, :]).astype(BF16)
        dqc = dot(ds, k_s[hh, :width, :])
        dqr = flip8(dot(dd, rev_s[head, SEQ - width:, :]))
        stage[1, hh, rows, :] = (dqc + dqr).astype(BF16)
        dr_acc[head, 1, HEAD:HEAD + 1, HALF - HEAD:] += jnp.sum(dqc, axis=0, keepdims=True)
        dr_acc[head, 1, HEAD + 1:HEAD + 2, HALF - HEAD:] += jnp.sum(dqr, axis=0, keepdims=True)
        dk_new = dot(at_s[hh, :, rows], ds_ref[:, lo:width])
        dv_new = dot(gt_s[hh, :, rows], pb_ref[:, lo:width])
        if fresh:
            dkt[hh] = dk_new
            dvt[hh] = dv_new
        else:
            dkt[hh, :, :width - lo] += dk_new
            dvt[hh, :, :width - lo] += dv_new
        dr_new = dot(ct_s[hh, :, rows], dd)
        if width > HALF:
            dr_acc[head, 0, :HEAD, SEQ - width:] += dr_new[:, :width - HALF]
            dr_acc[head, 1, :HEAD, :] += dr_new[:, width - HALF:]
        else:
            dr_acc[head, 1, :HEAD, HALF - width:] += dr_new

    def col_block(hh, head, sub, i0):
        rows = slice(i0, i0 + QB)
        first = WIN - i0
        s_ref[:, :HALF] = dot(a_s[hh, rows, :], kt_s[hh, :, :HALF])
        e_ref[:, :WIN] = dot(c_s[hh, rows, :], rt_s[head, :, first:first + WIN])
        dp_ref[:, :HALF] = dot(g_s[hh, rows, :], vt_s[hh, :, :HALF])
        st_ref[:, :8] = st_rx[sub, hh, :, i0 - HALF:i0 - HALF + QB].T
        for r0 in range(0, QB, 16):
            group = slice(r0, r0 + 16)
            rel = pltpu.roll(e_ref[group, :WIN], HALF + 1 + r0, 1, stride=1, stride_axis=0)[:, :HALF]
            log_sum = st_ref[group, 0:1]
            row_dot = st_ref[group, 1:2]
            p = jnp.exp2((s_ref[group, :HALF] + rel) * (scale * LOG2E) - log_sum)
            pb_ref[group, :HALF] = p.astype(BF16)
            ds_ref[group, :HALF] = (p * (dp_ref[group, :HALF] - row_dot) * scale).astype(BF16)
        dkt[hh] += dot(at_s[hh, :, rows], ds_ref[:, :HALF])
        dvt[hh] += dot(gt_s[hh, :, rows], pb_ref[:, :HALF])

    def store_rows(sub):
        for t in BOTH:
            buf[2 + t, sub] = pltpu.einshape("abc->bac", stage[t])

    def store_keys(sub):
        for hh in BOTH:
            stage[2, hh] = dkt[hh].astype(BF16).T
            stage[3, hh] = dvt[hh].astype(BF16).T
        for t in BOTH:
            buf[t, sub] = pltpu.einshape("abc->bac", stage[2 + t])

    def wait_up(sub):
        wait_for(rbuf.at[:, sub], up_recv.at[sub])
        wait_for(rbuf.at[:, sub], up_send.at[sub % 4])

    def wait_in(sub):
        wait_for(buf.at[2:4, sub], in_recv.at[1, sub])

    def lower_rows(sub):
        wait_in(sub)
        load_rows(buf, 2, buf, 3, sub, 0, True)

    def lower_own(sub):
        load_keys(buf, 0, buf, 1, sub, 0)

        def own(hh, carry):
            head = 2 * (sub // SLOTS) + hh
            row_block(hh, head, QB, QB, 0, True, False)
            row_block(hh, head, 0, 0, 0, False, False)
            return carry

        lax.fori_loop(0, PAIR, own, 0)
        store_rows(sub)

    def lower_theirs(sub):
        wait_up(sub)
        load_rows(rbuf, 0, rbuf, 1, sub, HALF, False)
        wait_for(st_rx.at[sub], st_recv.at[sub % 4])

        def theirs(hh, carry):
            head = 2 * (sub // SLOTS) + hh
            col_block(hh, head, sub, HALF)
            col_block(hh, head, sub, HALF + QB)
            return carry

        lax.fori_loop(0, PAIR, theirs, 0)
        store_keys(sub)

    def upper_own(sub):
        wait_in(sub)
        wait_up(sub)
        load_rows(buf, 0, buf, 1, sub, 0, True)
        load_keys(rbuf, 0, rbuf, 1, sub, 0)
        load_keys(buf, 2, buf, 3, sub, HALF)

        def own(hh, carry):
            head = 2 * (sub // SLOTS) + hh
            for blk in (1, 0):
                row_block(hh, head, QB * blk, HALF + QB * blk, HALF, blk == 1, True)
                st_tx[sub, hh, :, QB * blk:QB * (blk + 1)] = st_ref[...].T[:8]
            pltpu.make_async_remote_copy(src_ref=st_tx.at[sub, hh], dst_ref=st_rx.at[sub, hh], send_sem=st_send, recv_sem=st_recv.at[sub % 4],
                                         device_id=(across,), device_id_type=MESH).start()
            place = 2 * (sub % 2 * PAIR + hh)
            row_id = lax.broadcasted_iota(jnp.int32, (8, TIP), 0)
            tile = tip_tx[sub // 2]
            for j in BOTH:
                tile = jnp.where(row_id == place + j, st_tx[sub, hh, j:j + 1, HALF - TIP:], tile)
            tip_tx[sub // 2] = tile
            return carry

        lax.fori_loop(0, PAIR, own, 0)

        @pl.when(jnp.logical_not(tip) & (sub % 2 == 1))
        def _():
            pltpu.make_async_remote_copy(src_ref=tip_tx.at[sub // 2], dst_ref=tip_st.at[col, sub // 2], send_sem=st_send, recv_sem=ts_recv,
                                         device_id=(N_DEV - 2 + core,), device_id_type=MESH).start()
        store_rows(sub)
        store_keys(sub)

    side = 1 - core
    parts = (dr0_out, dr1_out, dr2_out, dr3_out, dr4_out, dr5_out)

    def swap_start(p):
        for n in BOTH:
            pltpu.make_async_remote_copy(src_ref=dr_acc.at[2 * p + n, side], dst_ref=dr_rx.at[p, n], send_sem=fw_send, recv_sem=x_recv.at[p],
                                         device_id=(partner,), device_id_type=MESH).start()

    def swap_add(p):
        wait_for(dr_rx.at[p], x_recv.at[p])
        for n in BOTH:
            dr_rx[p, n] = dr_rx[p, n] + dr_acc[2 * p + n, core]

    def cross_start(p):
        pltpu.make_async_remote_copy(src_ref=dr_rx.at[p, 1 - z], dst_ref=dr_rz.at[p], send_sem=fw_send, recv_sem=z_recv.at[p],
                                     device_id=(across,), device_id_type=MESH).start()

    def head_of(p, bits):
        other = chip ^ bits
        return 4 * (other % 4) + 2 * p + other // 4

    def block(p, m, bits):
        if bits == 0:
            return dr_fin.at[p, PART * m:PART * (m + 1)]
        return parts[m].at[side, :, head_of(p, bits)]

    def forward(p, m, bits):
        pltpu.make_async_remote_copy(src_ref=block(p, m, bits), dst_ref=parts[m].at[side, :, head_of(p, bits)], send_sem=fw_send,
                                     recv_sem=fw_recv, device_id=(partner,), device_id_type=MESH).start()

    def blocks(count):
        return parts[0].at[:, :, :N_PART // 2 * count]

    def pass_on(p, bits, hop, device):
        for m in range(N_PART):
            pltpu.make_async_remote_copy(
                src_ref=block(p, m, bits), dst_ref=parts[m].at[side, :, head_of(p, bits)], send_sem=ring_send,
                recv_sem=ring_recv.at[p, hop], device_id=(device,), device_id_type=MESH).start()

    def hand_over(p, bits):
        for m in range(N_PART):
            forward(p, m, bits)

    along_x, along_y = me ^ 2, me ^ 4

    def hop_start(p, hop):
        if hop == 0:
            for device in (along_x, along_y, across):
                pass_on(p, 0, 0, device)
        if hop == 1:
            @pl.when(even & loaded)
            def _():
                pass_on(p, 1, 1, along_y)

            @pl.when(jnp.logical_not(even) & loaded)
            def _():
                pass_on(p, 2, 1, along_x)

            pass_on(p, 1, 1, across)
            pass_on(p, 2, 1, across)
        if hop == 2:
            @pl.when(even & loaded)
            def _():
                pass_on(p, 5, 2, along_y)

            @pl.when(jnp.logical_not(even) & loaded)
            def _():
                pass_on(p, 6, 2, along_x)

            @pl.when(even)
            def _():
                pass_on(p, 3, 2, across)
        if hop == 3:
            @pl.when(even)
            def _():
                pass_on(p, 7, 3, across)

    def hop_wait(p, hop):
        if hop == 0:
            wait_for(blocks(3), ring_recv.at[p, 0])
            for bits in (1, 2, 4):
                hand_over(p, bits)
        if hop == 1:
            @pl.when(even)
            def _():
                wait_for(blocks(3), ring_recv.at[p, 1])
                hand_over(p, 3)

            @pl.when(jnp.logical_not(even))
            def _():
                wait_for(blocks(2), ring_recv.at[p, 1])
            for bits in (5, 6):
                hand_over(p, bits)
        if hop == 2:
            wait_for(blocks(1), ring_recv.at[p, 2])
            hand_over(p, 7)
        if hop == 3:
            @pl.when(jnp.logical_not(even))
            def _():
                wait_for(blocks(1), ring_recv.at[p, 3])
                hand_over(p, 3)

    def sent_wait():
        @pl.when(even & loaded)
        def _():
            wait_for(buf.at[:3, :, :FIN * 18 // 24], ring_send)

        @pl.when(even != loaded)
        def _():
            wait_for(buf.at[:3, :7, :FIN * 14 // 21], ring_send)

        @pl.when(jnp.logical_not(even | loaded))
        def _():
            wait_for(buf.at[:2, :6, :FIN * 10 // 12], ring_send)

    def cross_finish(p):
        wait_for(dr_rz.at[p], z_recv.at[p])
        total = dr_rx[p, z] + dr_rz[p]
        rev32 = eye_rev(F32)
        for m in range(HALF // HEAD):
            part = total[:HEAD, HALF - HEAD * (m + 1):HALF - HEAD * m]
            turned = lax.dot_general(rev32, part, (((1,), (1,)), ((), ())), precision=lax.Precision.HIGHEST, preferred_element_type=F32)
            dr_fin[p, HEAD * m:HEAD * (m + 1)] = turned.reshape(HEAD, 1, HEAD)
        dr_fin[p, HALF] = total[HEAD:HEAD + 1, HALF - HEAD:]
        dr_fin[p, HALF + 1] = total[HEAD + 1:HEAD + 2, HALF - HEAD:]
        dr_fin[p, HALF + 2:] = jnp.zeros((FIN - HALF - 2, 1, HEAD), F32)
        hop_start(p, 0)
        for m in range(N_PART):
            pltpu.make_async_copy(block(p, m, 0), parts[m].at[side, :, head_of(p, 0)], own_sem).start()
        hand_over(p, 0)

    def tip_load(unit):
        slot, row, far = unit % 2, unit // FAR, unit % FAR
        pair = far + tip_base
        for t, src in enumerate((q_in, k_in, v_in, g_in)):
            pltpu.make_async_copy(src.at[core * SLOTS + row, :, pair], r_buf.at[slot, pl.ds(TIP * t + ROWS * core, ROWS)], tip_sem.at[slot]).start()
            pltpu.make_async_copy(far_out.at[t, row, :, far], r_buf.at[slot, pl.ds(TIP * t + ROWS * (1 - core), ROWS)], tip_sem.at[slot]).start()
        pltpu.make_async_copy(r_in.at[:TIP, pair], r_buf.at[slot, 4 * TIP:5 * TIP], tip_sem.at[slot]).start()

    def tip_done(slot):
        wait_for(r_buf.at[slot, :2 * TIP], tip_send.at[slot])

    def tip_group(hh, r0):
        group = slice(TIP * hh + r0, TIP * hh + r0 + 16)
        rel = pltpu.roll(e_ref[group, :TIP], 1 + r0, 1, stride=1, stride_axis=0)
        ahead = lax.broadcasted_iota(jnp.int32, (16, TIP), 1) - lax.broadcasted_iota(jnp.int32, (16, TIP), 0)
        return group, s_ref[group, :TIP] + rel, ahead <= r0

    def tip_rows(hh):
        for r0 in range(0, TIP, 16):
            group, s, seen = tip_group(hh, r0)
            s = jnp.where(seen, s, -jnp.inf)
            top = jnp.max(s, axis=1, keepdims=True)
            p = jnp.exp2((s - top) * (scale * LOG2E))
            p = p * (1.0 / jnp.sum(p, axis=1, keepdims=True))
            pb_ref[group, :TIP] = p.astype(BF16)
            dp = dp_ref[group, :TIP]
            row_dot = jnp.sum(p * dp, axis=1, keepdims=True)
            ds = (p * (dp - row_dot) * scale).astype(BF16)
            ds_ref[group, :TIP] = ds
            flipped = flip8(ds.astype(F32))
            half = [pltpu.roll(flipped[8 * j:8 * j + 8], TIP - 8 - r0 - 8 * j, 1, stride=1, stride_axis=0) for j in range(2)]
            dd_ref[group, :TIP] = jnp.concatenate(half, axis=0).astype(BF16)
        rows = slice(TIP * hh, TIP * (hh + 1))
        stage[0, hh, :TIP, :] = dot(pb_ref[rows, :TIP], v_s[hh, :TIP, :]).astype(BF16)
        dqc = dot(ds_ref[rows, :TIP], k_s[hh, :TIP, :])
        dqr = flip8(dot(dd_ref[rows, :TIP], c_s[hh, :TIP, :]))
        stage[1, hh, :TIP, :] = (dqc + dqr).astype(BF16)

    def tip_keys(hh, stats, odd):
        rows = slice(TIP * hh, TIP * (hh + 1))
        by_row = stats.T
        even_row, odd_row = [by_row[:, n:n + 2] for n in (2 * hh, 2 * (hh + PAIR))]
        st_ref[rows, :2] = jnp.where(odd == 1, odd_row, even_row)
        for r0 in range(0, TIP, 16):
            group, s, seen = tip_group(hh, r0)
            p = jnp.where(seen, jnp.exp2(s * (scale * LOG2E) - st_ref[group, 0:1]), 0.0)
            pb_ref[group, :TIP] = p.astype(BF16)
            ds_ref[group, :TIP] = (p * (dp_ref[group, :TIP] - st_ref[group, 1:2]) * scale).astype(BF16)
        over_rows = (((0,), (0,)), ((), ()))
        stage[0, hh, :TIP, :] = lax.dot_general(ds_ref[rows, :TIP], a_s[hh, :TIP, :], over_rows, preferred_element_type=F32).astype(BF16)
        stage[1, hh, :TIP, :] = lax.dot_general(pb_ref[rows, :TIP], g_s[hh, :TIP, :], over_rows, preferred_element_type=F32).astype(BF16)

    def tip_unit(unit, carry):
        slot, row, far = unit % 2, unit // FAR, unit % FAR
        pair = far + tip_base
        wait_for(r_buf.at[slot, :5 * TIP], tip_sem.at[slot])

        @pl.when(unit + 1 < UNITS)
        def _():
            tip_load(unit + 1)

        q2, k2, v2, g2, r2 = [pltpu.einshape("abc->bac", r_buf[slot, TIP * t:TIP * (t + 1)]) for t in range(5)]
        u = u_buf[pair].astype(F32)
        w = w_buf[pair].astype(F32)
        for hh in BOTH:
            rows = slice(TIP * hh, TIP * (hh + 1))
            q32 = q2[hh].astype(F32)
            a = (q32 + u[hh:hh + 1]).astype(BF16)
            c = (q32 + w[hh:hh + 1]).astype(BF16)
            falling = dot(eye_rev(BF16), r2[hh]).astype(BF16)
            s_ref[rows, :TIP] = dot(a, k2[hh].T)
            e_ref[rows, :TIP] = dot(c, falling.T)
            dp_ref[rows, :TIP] = dot(g2[hh], v2[hh].T)
            a_s[hh, :TIP, :] = a
            c_s[hh, :TIP, :] = falling
            g_s[hh, :TIP, :] = g2[hh]
            k_s[hh, :TIP, :] = k2[hh]
            v_s[hh, :TIP, :] = v2[hh]

        @pl.when(lower)
        def _():
            for hh in BOTH:
                tip_rows(hh)

        @pl.when(upper)
        def _():
            for hh in BOTH:
                tip_keys(hh, tip_st[far // 2, (far % 2 * SLOTS + row) // 2], row % 2)

        @pl.when(unit >= 2)
        def _():
            tip_done(slot)

        for n in BOTH:
            r_buf[slot, (5 + n) * TIP:(6 + n) * TIP] = pltpu.einshape("abc->bac", stage[n, :, :TIP, :])
        place = (core * SLOTS + row, slice(None), pair)

        def give(results):
            for n, dst in enumerate(results):
                pltpu.make_async_copy(r_buf.at[slot, pl.ds((5 + n) * TIP + ROWS * core, ROWS)], dst.at[place], tip_send.at[slot]).start()
                pltpu.make_async_remote_copy(
                    src_ref=r_buf.at[slot, pl.ds((5 + n) * TIP + ROWS * (1 - core), ROWS)], dst_ref=dst.at[place],
                    send_sem=tip_send.at[slot], recv_sem=out_recv, device_id=(partner,), device_id_type=MESH).start()

        @pl.when(lower)
        def _():
            give((o_out, dq_out))

        @pl.when(upper)
        def _():
            give((dk_out, dv_out))
        return carry

    def tips(third):
        @pl.when(tip)
        def _():
            if third == 0:
                wait_for(far_out, far_recv)

                @pl.when(upper)
                def _():
                    wait_for(tip_st, ts_recv)
                tip_load(0)
            lax.fori_loop(UNITS // 3 * third, UNITS // 3 * (third + 1), tip_unit, 0)
            if third == 2:
                tip_done(0)
                tip_done(1)

    send_up(0)

    def sub_body(sub, carry):
        @pl.when(sub < SUBS - 1)
        def _():
            send_up(sub + 1)

        @pl.when(sub == SLOTS)
        def _():
            swap_start(0)

        @pl.when(sub == SUBS - 1)
        def _():
            swap_add(0)
            cross_start(0)

        @pl.when(sub == SUBS)
        def _():
            swap_start(1)
            swap_add(1)
            cross_start(1)
            cross_finish(0)

        @pl.when(lower & (sub < SUBS))
        def _():
            lower_rows(sub)

        @pl.when(lower & (sub > 0))
        def _():
            lower_theirs(sub - 1)

        @pl.when(lower & (sub < SUBS))
        def _():
            lower_own(sub)

        @pl.when(upper & (sub < SUBS))
        def _():
            upper_own(sub)

        @pl.when(sub <= EARLY)
        def _():
            send_out(sub, (2, 3))

        @pl.when((sub > 0) & (sub <= EARLY))
        def _():
            send_out(sub - 1, (0, 1))
        return carry

    lax.fori_loop(0, SUBS + 1, sub_body, 0)

    cross_finish(1)
    send_out(EARLY, (0, 1))

    @pl.when(lone)
    def _():
        send_out(EARLY + 1, (2, 3))

    for p in BOTH:
        hop_wait(p, 0)
        hop_start(p, 1)

    @pl.when(lone)
    def _():
        send_out(EARLY + 1, BOTH)

    @pl.when(jnp.logical_not(lone))
    def _():
        send_out(EARLY + 1, ALL)

    for p in BOTH:
        if p:
            send_out(EARLY + 2, ALL)
        tips(p)
        hop_wait(p, 1)
        hop_start(p, 2)

    def send_late(sub, carry):
        send_out(sub, ALL, True)
        return carry

    lax.fori_loop(EARLY + 3, SUBS, send_late, 0)
    tips(2)
    for p in BOTH:
        hop_wait(p, 2)
        hop_start(p, 3)
    for p in BOTH:
        hop_wait(p, 3)

    wait_for(buf.at[:, :, :HALF - ROWS], in_send)

    @pl.when(tip)
    def _():
        wait_for(buf.at[:, :, :HALF - 3 * ROWS // 2], out_recv)
        wait_for(buf.at[:, :, :HALF - ROWS], out_send)
        wait_for(far_out, far_send)

    @pl.when(jnp.logical_not(tip))
    def _():
        wait_for(buf, out_recv)
        wait_for(buf.at[:, :, :HALF - 2 * ROWS], out_send)

    @pl.when(upper & tip)
    def _():
        wait_for(st_tx, st_send)

    @pl.when(upper & jnp.logical_not(tip))
    def _():
        wait_for(buf.at[0, :2, :272], st_send)

    wait_for(blocks(2), own_sem)
    sent_wait()
    wait_for(buf.at[:3, :, :480], fw_send)
    wait_for(buf.at[:3, :, :FIN * 16 // 24], fw_recv)


def writer(*refs):
    ins, (o, dq, dk, dv, dr, du, dw, sem) = refs[:4 + N_PART], refs[4 + N_PART:]
    pairs = list(zip(ins[:4], (o, dq, dk, dv)))
    for m, part in enumerate(ins[4:]):
        rows = min(PART, HALF - PART * m)
        for side in BOTH:
            start = HALF * side + PART * m
            pairs.append((part.at[side, :rows], dr.at[start:start + rows]))
    last = HALF - PART * (N_PART - 1)
    pairs += [(ins[-1].at[0, last], du), (ins[-1].at[0, last + 1], dw)]
    copies = [pltpu.make_async_copy(src, dst, sem.at[j]) for j, (src, dst) in enumerate(pairs)]
    for copy in copies:
        copy.start()
    for copy in copies:
        copy.wait()


def solution(mesh):
    seq_spec = P(None, "cp", None, None)

    def local(query, key_in, value, bias_u, bias_w, rel_k, d_out):
        n_batch, rows, n_heads, head_dim = query.shape
        pairs = (n_batch, rows, N_PAIR, PAIR, head_dim)
        vm = pltpu.VMEM
        dma = pltpu.SemaphoreType.DMA
        whole = pl.BlockSpec(memory_space=pl.ANY)
        act = jax.ShapeDtypeStruct(pairs, BF16)
        vec = jax.ShapeDtypeStruct((n_heads, 1, head_dim), F32)
        tok = (PAIR, SEQ, HEAD)
        tok_t = (PAIR, HEAD, SEQ)
        acc = (HEAD + 8, HALF)
        outs = pl.pallas_call(
            kernel,
            name="rel_attn",
            out_shape=(act, act, act, act,
                       *[jax.ShapeDtypeStruct((2, PART, n_heads, 1, head_dim), F32)] * N_PART,
                       jax.ShapeDtypeStruct((4, SLOTS, ROWS, FAR, PAIR, HEAD), BF16)),
            in_specs=[pl.BlockSpec(memory_space=pltpu.HBM)] * 7,
            out_specs=[whole] * (5 + N_PART),
            scratch_shapes=[
                vm((4, SUBS, HALF, PAIR, HEAD), BF16), vm((2, SUBS, HALF, PAIR, HEAD), BF16),
                vm((2, SEQ, PAIR, HEAD), BF16), vm((N_PAIR, PAIR, HEAD), BF16), vm((N_PAIR, PAIR, HEAD), BF16),
                vm((SUBS, PAIR, 8, HALF), F32), vm((SUBS, PAIR, 8, HALF), F32), vm((SUBS // 2, 8, TIP), F32), vm((3, SUBS // 2, 8, TIP), F32), vm((QB, HEAD), F32),
                vm((2, 2) + acc, F32), vm((2,) + acc, F32), vm((2, FIN, 1, HEAD), F32), vm((4, 2) + acc, F32),
                vm((QB, SEQ), F32), vm((QB, SEQ), F32), vm((QB, SEQ), F32),
                vm((QB, SEQ), BF16), vm((QB, SEQ), BF16), vm((QB, SEQ), BF16),
                vm(tok, BF16), vm(tok, BF16), vm(tok, BF16), vm(tok, BF16), vm(tok, BF16),
                vm(tok_t, BF16), vm(tok_t, BF16), vm(tok_t, BF16), vm(tok_t, BF16), vm(tok_t, BF16),
                vm((4, SEQ, HEAD), BF16), vm((4, HEAD, SEQ), BF16),
                vm((PAIR, HEAD, HALF), F32), vm((PAIR, HEAD, HALF), F32), vm((4, PAIR, HALF, HEAD), BF16),
                dma, dma((2, SUBS)), dma, dma, dma, dma((4,)), dma((4,)), dma((SUBS,)), dma, dma((4,)),
                dma((2,)), dma((2,)), dma, dma((2, 4)), dma, dma,
                dma, dma, dma((2,)), dma((2,)), dma,
            ],
            compiler_params=pltpu.CompilerParams(collective_id=0, has_side_effects=True, vmem_limit_bytes=37 * 1024 * 1024),
        )(*[pltpu.with_memory_space_constraint(x, pltpu.HBM) for x in (
            query.reshape(pairs), key_in.reshape(pairs), value.reshape(pairs), d_out.reshape(pairs),
            rel_k.reshape(SEQ, N_PAIR, PAIR, head_dim), bias_u.reshape(N_PAIR, PAIR, head_dim), bias_w.reshape(N_PAIR, PAIR, head_dim))])
        o, dq, dk, dv, dr, du, dw = pl.pallas_call(
            writer,
            name="writer",
            out_shape=(act, act, act, act, jax.ShapeDtypeStruct((SEQ, n_heads, 1, head_dim), F32), vec, vec),
            in_specs=[whole] * (4 + N_PART),
            out_specs=[whole] * 7,
            scratch_shapes=[dma((6 + 2 * N_PART,))],
            compiler_params=pltpu.CompilerParams(vmem_limit_bytes=1024 * 1024),
        )(*outs[:-1])
        full = query.shape
        return (o.reshape(full), dq.reshape(full), dk.reshape(full), dv.reshape(full),
                du.reshape(bias_u.shape), dw.reshape(bias_w.shape), dr.reshape(rel_k.shape))

    return jax.shard_map(local, mesh=mesh,
                         in_specs=(seq_spec, seq_spec, seq_spec, P(), P(), P(), seq_spec),
                         out_specs=(seq_spec, seq_spec, seq_spec, seq_spec, P(), P(), P()),
                         check_vma=False)
```

```python
import jax
import jax.numpy as jnp
from jax import lax
from jax.experimental import pallas as pl
from jax.experimental.pallas import tpu as pltpu
from jax.sharding import PartitionSpec as P

MESH = pl.DeviceIdType.MESH
BF16, F32 = jnp.bfloat16, jnp.float32
LOG2E = 1.4426950408889634

N_DEV = 16
BOTH = range(2)
ALL = range(4)
PLANE = 8
PAIR = 2
N_PAIR = 8
SLOTS = 4
SUBS = 2 * SLOTS
EARLY = 3
ROWS = 64
HALF = PLANE * ROWS
SEQ = 2 * HALF
HEAD = 128
QB = 256
WIN = HALF + QB
N_PART = 6
PART = 86
FIN = N_PART * PART
TIP = 2 * ROWS
FAR = N_PAIR - 2
UNITS = FAR * SLOTS
TURNS = ((1, 3, 2), (3, 1, 2))


def dot(lhs, rhs):
    return jnp.dot(lhs, rhs, preferred_element_type=F32)


def flip8(x):
    rows, cols = x.shape
    idx = 7 - lax.broadcasted_iota(jnp.int32, (rows // 8, 8, cols), 1)
    return jnp.take_along_axis(x.reshape(rows // 8, 8, cols), idx, axis=1).reshape(rows, cols)


def eye_rev(dtype):
    total = lax.broadcasted_iota(jnp.int32, (HEAD, HEAD), 0) + lax.broadcasted_iota(jnp.int32, (HEAD, HEAD), 1)
    return jnp.where(total == HEAD - 1, 1.0, 0.0).astype(dtype)


def kernel(q_in, k_in, v_in, g_in, r_in, u_in, w_in,
           o_out, dq_out, dk_out, dv_out, dr0_out, dr1_out, dr2_out, dr3_out, dr4_out, dr5_out, far_out,
           buf, rbuf, r_buf, u_buf, w_buf, st_tx, st_rx, tip_tx, tip_st, st_ref, dr_rx, dr_rz, dr_fin, dr_acc,
           s_ref, e_ref, dp_ref, pb_ref, ds_ref, dd_ref,
           a_s, c_s, g_s, k_s, v_s, at_s, ct_s, gt_s, kt_s, vt_s, rev_s, rt_s, dkt, dvt, stage,
           in_send, in_recv, out_send, out_recv, own_sem, r_sem, up_send, up_recv, st_send, st_recv,
           x_recv, z_recv, ring_send, ring_recv, fw_send, fw_recv,
           far_send, far_recv, tip_sem, tip_send, ts_recv):
    me = lax.axis_index("cp")
    core = me % 2
    chip = me // 2
    col = chip % 4
    z = chip // 4
    partner = me + 1 - 2 * core
    across = me + PLANE * (1 - 2 * z)
    scale = HEAD ** -0.5

    def wait_for(ref, sem):
        pltpu.make_async_copy(ref, ref, sem).wait()

    y = col // 2
    lower, upper = z == 0, z == 1
    tip = chip == 7 * z
    tip_base = 2 - 2 * z

    tables = [pltpu.make_async_copy(src, dst, r_sem.at[j]) for j, (src, dst) in enumerate(
        ((r_in.at[:, 2 * col], r_buf.at[0]), (r_in.at[:, 2 * col + 1], r_buf.at[1]), (u_in, u_buf), (w_in, w_buf)))]
    for copy in tables:
        copy.start()

    barrier = pltpu.get_barrier_semaphore()

    for peer in [across] + [me ^ step for step in range(PLANE - 1, 0, -1)]:
        pl.semaphore_signal(barrier, inc=1, device_id=(peer,), device_id_type=MESH)
    pl.semaphore_wait(barrier, PLANE)

    my_rows = pl.ds(pl.multiple_of((me % PLANE) * ROWS, ROWS), ROWS)

    even = chip % 2 == z
    loaded = y != z
    lone = loaded & jnp.logical_not(even)

    def peers(late=False):
        near = core == 0
        if late:
            near = jnp.logical_not(near | lone)
        first, second, third = [jnp.where(near, near_turn, far_turn) for near_turn, far_turn in zip(*TURNS)]
        for turn, other in ((first, 0), (third, 0), (first, 1), (third, 1), (second, 0), (second, 1)):
            yield me ^ (2 * turn + other)
        yield partner

    def send_in(ins, sub):
        pair, row = sub // SLOTS, sub % SLOTS
        for first in (0, 2):
            for t in (first, first + 1):
                pltpu.make_async_copy(ins[t].at[core * SLOTS + row, :, 2 * col + pair], buf.at[t, sub, my_rows], in_recv.at[first // 2, sub]).start()
            for peer in peers():
                for t in (first, first + 1):
                    pltpu.make_async_remote_copy(
                        src_ref=ins[t].at[(peer % 2) * SLOTS + row, :, 2 * ((peer // 2) % 4) + pair], dst_ref=buf.at[t, sub, my_rows],
                        send_sem=in_send, recv_sem=in_recv.at[first // 2, sub], device_id=(peer,), device_id_type=MESH).start()

    def send_all(ins):
        def send_sub(sub, carry):
            send_in(ins, sub)
            return carry
        lax.fori_loop(0, SUBS, send_sub, 0)

    @pl.when(lower)
    def _():
        send_all((k_in, v_in, q_in, g_in))

    @pl.when(upper)
    def _():
        send_all((q_in, g_in, k_in, v_in))

    @pl.when(tip)
    def _():
        for t, src in enumerate((q_in, k_in, v_in, g_in)):
            for row in range(SLOTS):
                pltpu.make_async_remote_copy(
                    src_ref=src.at[(1 - core) * SLOTS + row, :, pl.ds(tip_base, FAR)], dst_ref=far_out.at[t, row],
                    send_sem=far_send, recv_sem=far_recv, device_id=(partner,), device_id_type=MESH).start()

    for copy in tables:
        copy.wait()
    rev = eye_rev(BF16)
    for p in BOTH:
        pair_tab = pltpu.einshape("abc->bac", r_buf[p])
        for hh in BOTH:
            for blk in range(SEQ // HEAD):
                part = pair_tab[hh, SEQ - HEAD * (blk + 1):SEQ - HEAD * blk]
                flipped = dot(rev, part).astype(BF16)
                rev_s[2 * p + hh, HEAD * blk:HEAD * (blk + 1), :] = flipped
                rt_s[2 * p + hh, :, HEAD * blk:HEAD * (blk + 1)] = flipped.T
    dr_acc[...] = jnp.zeros_like(dr_acc)

    acts = (dk_out, dv_out, o_out, dq_out)

    def send_out(sub, which, late=False):
        place = (core * SLOTS + sub % SLOTS, slice(None), 2 * col + sub // SLOTS)
        for t in which:
            pltpu.make_async_copy(buf.at[t, sub, my_rows], acts[t].at[place], out_recv).start()
        for peer in peers(late):
            peer_rows = pl.ds(pl.multiple_of((peer % PLANE) * ROWS, ROWS), ROWS)
            to_tip = (peer // 2 == 7 * z) & jnp.logical_not(tip)
            for t in which:
                @pl.when(jnp.logical_not(to_tip & (lower if t >= 2 else upper)))
                def _():
                    pltpu.make_async_remote_copy(
                        src_ref=buf.at[t, sub, peer_rows], dst_ref=acts[t].at[place],
                        send_sem=out_send, recv_sem=out_recv, device_id=(peer,), device_id_type=MESH).start()

    def send_up(sub):
        wait_for(buf.at[0:2, sub], in_recv.at[0, sub])
        for j in BOTH:
            pltpu.make_async_remote_copy(src_ref=buf.at[j, sub], dst_ref=rbuf.at[j, sub], send_sem=up_send.at[sub % 3], recv_sem=up_recv.at[sub],
                                         device_id=(across,), device_id_type=MESH).start()

    def unpack(ref, j, sub):
        return pltpu.einshape("abc->bac", ref[j, sub])

    def load_rows(q_ref, q_j, g_ref, g_j, sub, start, turned):
        rows = slice(start, start + HALF)
        p = sub // SLOTS
        q2 = unpack(q_ref, q_j, sub)
        u = u_buf[2 * col + p].astype(F32)
        w = w_buf[2 * col + p].astype(F32)
        for hh in BOTH:
            q32 = q2[hh].astype(F32)
            a = (q32 + u[hh:hh + 1]).astype(BF16)
            c = (q32 + w[hh:hh + 1]).astype(BF16)
            a_s[hh, rows, :] = a
            c_s[hh, rows, :] = c
            at_s[hh, :, rows] = a.T
            if turned:
                ct_s[hh, :, rows] = flip8(c.astype(F32)).astype(BF16).T
        g2 = unpack(g_ref, g_j, sub)
        g_s[:, rows, :] = g2
        for hh in BOTH:
            gt_s[hh, :, rows] = g2[hh].T

    def load_keys(k_ref, k_j, v_ref, v_j, sub, start):
        rows = slice(start, start + HALF)
        k2 = unpack(k_ref, k_j, sub)
        v2 = unpack(v_ref, v_j, sub)
        k_s[:, rows, :] = k2
        v_s[:, rows, :] = v2
        for hh in BOTH:
            kt_s[hh, :, rows] = k2[hh].T
            vt_s[hh, :, rows] = v2[hh].T

    def row_block(hh, head, start, i0, lo, fresh, stats):
        width = i0 + QB
        rows = slice(start, start + QB)
        s_ref[:, :width] = dot(a_s[hh, rows, :], kt_s[hh, :, :width])
        e_ref[:, :width] = dot(c_s[hh, rows, :], rt_s[head, :, SEQ - width:])
        dp_ref[:, :width] = dot(g_s[hh, rows, :], vt_s[hh, :, :width])
        for r0 in range(0, QB, 16):
            group = slice(r0, r0 + 16)
            rel = pltpu.roll(e_ref[group, :width], i0 + 1 + r0, 1, stride=1, stride_axis=0)
            s = s_ref[group, :width] + rel
            ahead = lax.broadcasted_iota(jnp.int32, (16, width), 1) - lax.broadcasted_iota(jnp.int32, (16, width), 0)
            s = jnp.where(ahead <= i0 + r0, s, -jnp.inf)
            top = jnp.max(s, axis=1, keepdims=True)
            p = jnp.exp2((s - top) * (scale * LOG2E))
            total = jnp.sum(p, axis=1, keepdims=True)
            p = p * (1.0 / total)
            pb_ref[group, :width] = p.astype(BF16)
            dp = dp_ref[group, :width]
            row_dot = jnp.sum(p * dp, axis=1, keepdims=True)
            ds = (p * (dp - row_dot) * scale).astype(BF16)
            ds_ref[group, :width] = ds
            flipped = flip8(ds.astype(F32))
            half = [pltpu.roll(flipped[8 * j:8 * j + 8], QB - 8 - r0 - 8 * j, 1, stride=1, stride_axis=0) for j in range(2)]
            dd_ref[group, :width] = jnp.concatenate(half, axis=0).astype(BF16)
            if stats:
                lane = lax.broadcasted_iota(jnp.int32, (16, HEAD), 1)
                st_ref[group, :] = jnp.where(lane == 0, top * (scale * LOG2E) + jnp.log2(total), row_dot)
        pb = pb_ref[:, :width]
        ds = ds_ref[:, :width]
        dd = dd_ref[:, :width]
        stage[0, hh, rows, :] = dot(pb, v_s[hh, :width, :]).astype(BF16)
        dqc = dot(ds, k_s[hh, :width, :])
        dqr = flip8(dot(dd, rev_s[head, SEQ - width:, :]))
        stage[1, hh, rows, :] = (dqc + dqr).astype(BF16)
        dr_acc[head, 1, HEAD:HEAD + 1, HALF - HEAD:] += jnp.sum(dqc, axis=0, keepdims=True)
        dr_acc[head, 1, HEAD + 1:HEAD + 2, HALF - HEAD:] += jnp.sum(dqr, axis=0, keepdims=True)
        dk_new = dot(at_s[hh, :, rows], ds_ref[:, lo:width])
        dv_new = dot(gt_s[hh, :, rows], pb_ref[:, lo:width])
        if fresh:
            dkt[hh] = dk_new
            dvt[hh] = dv_new
        else:
            dkt[hh, :, :width - lo] += dk_new
            dvt[hh, :, :width - lo] += dv_new
        dr_new = dot(ct_s[hh, :, rows], dd)
        if width > HALF:
            dr_acc[head, 0, :HEAD, SEQ - width:] += dr_new[:, :width - HALF]
            dr_acc[head, 1, :HEAD, :] += dr_new[:, width - HALF:]
        else:
            dr_acc[head, 1, :HEAD, HALF - width:] += dr_new

    def col_block(hh, head, sub, i0):
        rows = slice(i0, i0 + QB)
        first = WIN - i0
        s_ref[:, :HALF] = dot(a_s[hh, rows, :], kt_s[hh, :, :HALF])
        e_ref[:, :WIN] = dot(c_s[hh, rows, :], rt_s[head, :, first:first + WIN])
        dp_ref[:, :HALF] = dot(g_s[hh, rows, :], vt_s[hh, :, :HALF])
        st_ref[:, :8] = st_rx[sub, hh, :, i0 - HALF:i0 - HALF + QB].T
        for r0 in range(0, QB, 16):
            group = slice(r0, r0 + 16)
            rel = pltpu.roll(e_ref[group, :WIN], HALF + 1 + r0, 1, stride=1, stride_axis=0)[:, :HALF]
            log_sum = st_ref[group, 0:1]
            row_dot = st_ref[group, 1:2]
            p = jnp.exp2((s_ref[group, :HALF] + rel) * (scale * LOG2E) - log_sum)
            pb_ref[group, :HALF] = p.astype(BF16)
            ds_ref[group, :HALF] = (p * (dp_ref[group, :HALF] - row_dot) * scale).astype(BF16)
        dkt[hh] += dot(at_s[hh, :, rows], ds_ref[:, :HALF])
        dvt[hh] += dot(gt_s[hh, :, rows], pb_ref[:, :HALF])

    def store_rows(sub):
        for t in BOTH:
            buf[2 + t, sub] = pltpu.einshape("abc->bac", stage[t])

    def store_keys(sub):
        for hh in BOTH:
            stage[2, hh] = dkt[hh].astype(BF16).T
            stage[3, hh] = dvt[hh].astype(BF16).T
        for t in BOTH:
            buf[t, sub] = pltpu.einshape("abc->bac", stage[2 + t])

    def wait_up(sub):
        wait_for(rbuf.at[:, sub], up_recv.at[sub])
        wait_for(rbuf.at[:, sub], up_send.at[sub % 3])

    def wait_in(sub):
        wait_for(buf.at[2:4, sub], in_recv.at[1, sub])

    def lower_rows(sub):
        wait_in(sub)
        load_rows(buf, 2, buf, 3, sub, 0, True)

    def lower_own(sub):
        load_keys(buf, 0, buf, 1, sub, 0)

        def own(hh, carry):
            head = 2 * (sub // SLOTS) + hh
            row_block(hh, head, QB, QB, 0, True, False)
            row_block(hh, head, 0, 0, 0, False, False)
            return carry

        lax.fori_loop(0, PAIR, own, 0)
        store_rows(sub)

    def lower_theirs(sub):
        wait_up(sub)
        load_rows(rbuf, 0, rbuf, 1, sub, HALF, False)
        wait_for(st_rx.at[sub], st_recv.at[sub % 3])

        def theirs(hh, carry):
            head = 2 * (sub // SLOTS) + hh
            col_block(hh, head, sub, HALF)
            col_block(hh, head, sub, HALF + QB)
            return carry

        lax.fori_loop(0, PAIR, theirs, 0)
        store_keys(sub)

    def upper_own(sub):
        wait_in(sub)
        wait_up(sub)
        load_rows(buf, 0, buf, 1, sub, 0, True)
        load_keys(rbuf, 0, rbuf, 1, sub, 0)
        load_keys(buf, 2, buf, 3, sub, HALF)

        def own(hh, carry):
            head = 2 * (sub // SLOTS) + hh
            for blk in (1, 0):
                row_block(hh, head, QB * blk, HALF + QB * blk, HALF, blk == 1, True)
                st_tx[sub, hh, :, QB * blk:QB * (blk + 1)] = st_ref[...].T[:8]
            pltpu.make_async_remote_copy(src_ref=st_tx.at[sub, hh], dst_ref=st_rx.at[sub, hh], send_sem=st_send, recv_sem=st_recv.at[sub % 3],
                                         device_id=(across,), device_id_type=MESH).start()
            place = 2 * (sub % 2 * PAIR + hh)
            row_id = lax.broadcasted_iota(jnp.int32, (8, TIP), 0)
            tile = tip_tx[sub // 2]
            for j in BOTH:
                tile = jnp.where(row_id == place + j, st_tx[sub, hh, j:j + 1, HALF - TIP:], tile)
            tip_tx[sub // 2] = tile
            return carry

        lax.fori_loop(0, PAIR, own, 0)

        @pl.when(jnp.logical_not(tip) & (sub % 2 == 1))
        def _():
            pltpu.make_async_remote_copy(src_ref=tip_tx.at[sub // 2], dst_ref=tip_st.at[col, sub // 2], send_sem=st_send, recv_sem=ts_recv,
                                         device_id=(N_DEV - 2 + core,), device_id_type=MESH).start()
        store_rows(sub)
        store_keys(sub)

    side = 1 - core
    parts = (dr0_out, dr1_out, dr2_out, dr3_out, dr4_out, dr5_out)

    def swap_start(p):
        for n in BOTH:
            pltpu.make_async_remote_copy(src_ref=dr_acc.at[2 * p + n, side], dst_ref=dr_rx.at[p, n], send_sem=fw_send, recv_sem=x_recv.at[p],
                                         device_id=(partner,), device_id_type=MESH).start()

    def swap_add(p):
        wait_for(dr_rx.at[p], x_recv.at[p])
        for n in BOTH:
            dr_rx[p, n] = dr_rx[p, n] + dr_acc[2 * p + n, core]

    def cross_start(p):
        pltpu.make_async_remote_copy(src_ref=dr_rx.at[p, 1 - z], dst_ref=dr_rz.at[p], send_sem=fw_send, recv_sem=z_recv.at[p],
                                     device_id=(across,), device_id_type=MESH).start()

    def head_of(p, bits):
        other = chip ^ bits
        return 4 * (other % 4) + 2 * p + other // 4

    def block(p, m, bits):
        if bits == 0:
            return dr_fin.at[p, PART * m:PART * (m + 1)]
        return parts[m].at[side, :, head_of(p, bits)]

    def forward(p, m, bits):
        pltpu.make_async_remote_copy(src_ref=block(p, m, bits), dst_ref=parts[m].at[side, :, head_of(p, bits)], send_sem=fw_send,
                                     recv_sem=fw_recv, device_id=(partner,), device_id_type=MESH).start()

    def blocks(count):
        return parts[0].at[:, :, :N_PART // 2 * count]

    def pass_on(p, bits, hop, device):
        for m in range(N_PART):
            pltpu.make_async_remote_copy(
                src_ref=block(p, m, bits), dst_ref=parts[m].at[side, :, head_of(p, bits)], send_sem=ring_send,
                recv_sem=ring_recv.at[p, hop], device_id=(device,), device_id_type=MESH).start()

    def hand_over(p, bits):
        for m in range(N_PART):
            forward(p, m, bits)

    along_x, along_y = me ^ 2, me ^ 4

    def hop_start(p, hop):
        if hop == 0:
            for device in (along_x, along_y, across):
                pass_on(p, 0, 0, device)
        if hop == 1:
            @pl.when(even & loaded)
            def _():
                pass_on(p, 1, 1, along_y)

            @pl.when(jnp.logical_not(even) & loaded)
            def _():
                pass_on(p, 2, 1, along_x)

            pass_on(p, 1, 1, across)
            pass_on(p, 2, 1, across)
        if hop == 2:
            @pl.when(even & loaded)
            def _():
                pass_on(p, 5, 2, along_y)

            @pl.when(jnp.logical_not(even) & loaded)
            def _():
                pass_on(p, 6, 2, along_x)

            @pl.when(even)
            def _():
                pass_on(p, 3, 2, across)
        if hop == 3:
            @pl.when(even)
            def _():
                pass_on(p, 7, 3, across)

    def hop_wait(p, hop):
        if hop == 0:
            wait_for(blocks(3), ring_recv.at[p, 0])
            for bits in (1, 2, 4):
                hand_over(p, bits)
        if hop == 1:
            @pl.when(even)
            def _():
                wait_for(blocks(3), ring_recv.at[p, 1])
                hand_over(p, 3)

            @pl.when(jnp.logical_not(even))
            def _():
                wait_for(blocks(2), ring_recv.at[p, 1])
            for bits in (5, 6):
                hand_over(p, bits)
        if hop == 2:
            wait_for(blocks(1), ring_recv.at[p, 2])
            hand_over(p, 7)
        if hop == 3:
            @pl.when(jnp.logical_not(even))
            def _():
                wait_for(blocks(1), ring_recv.at[p, 3])
                hand_over(p, 3)

    def sent_wait():
        @pl.when(even & loaded)
        def _():
            wait_for(buf.at[:3, :, :FIN * 18 // 24], ring_send)

        @pl.when(even != loaded)
        def _():
            wait_for(buf.at[:3, :7, :FIN * 14 // 21], ring_send)

        @pl.when(jnp.logical_not(even | loaded))
        def _():
            wait_for(buf.at[:2, :6, :FIN * 10 // 12], ring_send)

    def cross_finish(p):
        wait_for(dr_rz.at[p], z_recv.at[p])
        total = dr_rx[p, z] + dr_rz[p]
        rev32 = eye_rev(F32)
        for m in range(HALF // HEAD):
            part = total[:HEAD, HALF - HEAD * (m + 1):HALF - HEAD * m]
            turned = lax.dot_general(rev32, part, (((1,), (1,)), ((), ())), precision=lax.Precision.HIGHEST, preferred_element_type=F32)
            dr_fin[p, HEAD * m:HEAD * (m + 1)] = turned.reshape(HEAD, 1, HEAD)
        dr_fin[p, HALF] = total[HEAD:HEAD + 1, HALF - HEAD:]
        dr_fin[p, HALF + 1] = total[HEAD + 1:HEAD + 2, HALF - HEAD:]
        dr_fin[p, HALF + 2:] = jnp.zeros((FIN - HALF - 2, 1, HEAD), F32)
        hop_start(p, 0)
        for m in range(N_PART):
            pltpu.make_async_copy(block(p, m, 0), parts[m].at[side, :, head_of(p, 0)], own_sem).start()
        hand_over(p, 0)

    def tip_load(unit):
        slot, row, far = unit % 2, unit // FAR, unit % FAR
        pair = far + tip_base
        for t, src in enumerate((q_in, k_in, v_in, g_in)):
            pltpu.make_async_copy(src.at[core * SLOTS + row, :, pair], r_buf.at[slot, pl.ds(TIP * t + ROWS * core, ROWS)], tip_sem.at[slot]).start()
            pltpu.make_async_copy(far_out.at[t, row, :, far], r_buf.at[slot, pl.ds(TIP * t + ROWS * (1 - core), ROWS)], tip_sem.at[slot]).start()
        pltpu.make_async_copy(r_in.at[:TIP, pair], r_buf.at[slot, 4 * TIP:5 * TIP], tip_sem.at[slot]).start()

    def tip_done(slot):
        wait_for(r_buf.at[slot, :2 * TIP], tip_send.at[slot])

    def tip_group(hh, r0):
        group = slice(TIP * hh + r0, TIP * hh + r0 + 16)
        rel = pltpu.roll(e_ref[group, :TIP], 1 + r0, 1, stride=1, stride_axis=0)
        ahead = lax.broadcasted_iota(jnp.int32, (16, TIP), 1) - lax.broadcasted_iota(jnp.int32, (16, TIP), 0)
        return group, s_ref[group, :TIP] + rel, ahead <= r0

    def tip_rows(hh):
        for r0 in range(0, TIP, 16):
            group, s, seen = tip_group(hh, r0)
            s = jnp.where(seen, s, -jnp.inf)
            top = jnp.max(s, axis=1, keepdims=True)
            p = jnp.exp2((s - top) * (scale * LOG2E))
            p = p * (1.0 / jnp.sum(p, axis=1, keepdims=True))
            pb_ref[group, :TIP] = p.astype(BF16)
            dp = dp_ref[group, :TIP]
            row_dot = jnp.sum(p * dp, axis=1, keepdims=True)
            ds = (p * (dp - row_dot) * scale).astype(BF16)
            ds_ref[group, :TIP] = ds
            flipped = flip8(ds.astype(F32))
            half = [pltpu.roll(flipped[8 * j:8 * j + 8], TIP - 8 - r0 - 8 * j, 1, stride=1, stride_axis=0) for j in range(2)]
            dd_ref[group, :TIP] = jnp.concatenate(half, axis=0).astype(BF16)
        rows = slice(TIP * hh, TIP * (hh + 1))
        stage[0, hh, :TIP, :] = dot(pb_ref[rows, :TIP], v_s[hh, :TIP, :]).astype(BF16)
        dqc = dot(ds_ref[rows, :TIP], k_s[hh, :TIP, :])
        dqr = flip8(dot(dd_ref[rows, :TIP], c_s[hh, :TIP, :]))
        stage[1, hh, :TIP, :] = (dqc + dqr).astype(BF16)

    def tip_keys(hh, stats, odd):
        rows = slice(TIP * hh, TIP * (hh + 1))
        by_row = stats.T
        even_row, odd_row = [by_row[:, n:n + 2] for n in (2 * hh, 2 * (hh + PAIR))]
        st_ref[rows, :2] = jnp.where(odd == 1, odd_row, even_row)
        for r0 in range(0, TIP, 16):
            group, s, seen = tip_group(hh, r0)
            p = jnp.where(seen, jnp.exp2(s * (scale * LOG2E) - st_ref[group, 0:1]), 0.0)
            pb_ref[group, :TIP] = p.astype(BF16)
            ds_ref[group, :TIP] = (p * (dp_ref[group, :TIP] - st_ref[group, 1:2]) * scale).astype(BF16)
        over_rows = (((0,), (0,)), ((), ()))
        stage[0, hh, :TIP, :] = lax.dot_general(ds_ref[rows, :TIP], a_s[hh, :TIP, :], over_rows, preferred_element_type=F32).astype(BF16)
        stage[1, hh, :TIP, :] = lax.dot_general(pb_ref[rows, :TIP], g_s[hh, :TIP, :], over_rows, preferred_element_type=F32).astype(BF16)

    def tip_unit(unit, carry):
        slot, row, far = unit % 2, unit // FAR, unit % FAR
        pair = far + tip_base
        wait_for(r_buf.at[slot, :5 * TIP], tip_sem.at[slot])

        @pl.when(unit + 1 < UNITS)
        def _():
            tip_load(unit + 1)

        q2, k2, v2, g2, r2 = [pltpu.einshape("abc->bac", r_buf[slot, TIP * t:TIP * (t + 1)]) for t in range(5)]
        u = u_buf[pair].astype(F32)
        w = w_buf[pair].astype(F32)
        for hh in BOTH:
            rows = slice(TIP * hh, TIP * (hh + 1))
            q32 = q2[hh].astype(F32)
            a = (q32 + u[hh:hh + 1]).astype(BF16)
            c = (q32 + w[hh:hh + 1]).astype(BF16)
            falling = dot(eye_rev(BF16), r2[hh]).astype(BF16)
            s_ref[rows, :TIP] = dot(a, k2[hh].T)
            e_ref[rows, :TIP] = dot(c, falling.T)
            dp_ref[rows, :TIP] = dot(g2[hh], v2[hh].T)
            a_s[hh, :TIP, :] = a
            c_s[hh, :TIP, :] = falling
            g_s[hh, :TIP, :] = g2[hh]
            k_s[hh, :TIP, :] = k2[hh]
            v_s[hh, :TIP, :] = v2[hh]

        @pl.when(lower)
        def _():
            for hh in BOTH:
                tip_rows(hh)

        @pl.when(upper)
        def _():
            for hh in BOTH:
                tip_keys(hh, tip_st[far // 2, (far % 2 * SLOTS + row) // 2], row % 2)

        @pl.when(unit >= 2)
        def _():
            tip_done(slot)

        for n in BOTH:
            r_buf[slot, (5 + n) * TIP:(6 + n) * TIP] = pltpu.einshape("abc->bac", stage[n, :, :TIP, :])
        place = (core * SLOTS + row, slice(None), pair)

        def give(results):
            for n, dst in enumerate(results):
                pltpu.make_async_copy(r_buf.at[slot, pl.ds((5 + n) * TIP + ROWS * core, ROWS)], dst.at[place], tip_send.at[slot]).start()
                pltpu.make_async_remote_copy(
                    src_ref=r_buf.at[slot, pl.ds((5 + n) * TIP + ROWS * (1 - core), ROWS)], dst_ref=dst.at[place],
                    send_sem=tip_send.at[slot], recv_sem=out_recv, device_id=(partner,), device_id_type=MESH).start()

        @pl.when(lower)
        def _():
            give((o_out, dq_out))

        @pl.when(upper)
        def _():
            give((dk_out, dv_out))
        return carry

    def tips(third):
        @pl.when(tip)
        def _():
            if third == 0:
                wait_for(far_out, far_recv)

                @pl.when(upper)
                def _():
                    wait_for(tip_st, ts_recv)
                tip_load(0)
            lax.fori_loop(UNITS // 3 * third, UNITS // 3 * (third + 1), tip_unit, 0)
            if third == 2:
                tip_done(0)
                tip_done(1)

    send_up(0)

    def sub_body(sub, carry):
        @pl.when(sub < SUBS - 1)
        def _():
            send_up(sub + 1)

        @pl.when(sub == SLOTS)
        def _():
            swap_start(0)

        @pl.when(sub == SUBS - 1)
        def _():
            swap_add(0)
            cross_start(0)

        @pl.when(sub == SUBS)
        def _():
            swap_start(1)
            swap_add(1)
            cross_start(1)
            cross_finish(0)

        @pl.when(lower & (sub < SUBS))
        def _():
            lower_rows(sub)

        @pl.when(lower & (sub > 0))
        def _():
            lower_theirs(sub - 1)

        @pl.when(lower & (sub < SUBS))
        def _():
            lower_own(sub)

        @pl.when(upper & (sub < SUBS))
        def _():
            upper_own(sub)

        @pl.when(sub <= EARLY)
        def _():
            send_out(sub, (2, 3))

        @pl.when((sub > 0) & (sub <= EARLY))
        def _():
            send_out(sub - 1, (0, 1))
        return carry

    lax.fori_loop(0, SUBS + 1, sub_body, 0)

    cross_finish(1)
    send_out(EARLY, (0, 1))

    @pl.when(lone)
    def _():
        send_out(EARLY + 1, (2, 3))

    for p in BOTH:
        hop_wait(p, 0)
        hop_start(p, 1)

    @pl.when(lone)
    def _():
        send_out(EARLY + 1, BOTH)

    @pl.when(jnp.logical_not(lone))
    def _():
        send_out(EARLY + 1, ALL)

    for p in BOTH:
        if p:
            send_out(EARLY + 2, ALL)
        tips(p)
        hop_wait(p, 1)
        hop_start(p, 2)

    def send_late(sub, carry):
        send_out(sub, ALL, True)
        return carry

    lax.fori_loop(EARLY + 3, SUBS, send_late, 0)
    tips(2)
    for p in BOTH:
        hop_wait(p, 2)
        hop_start(p, 3)
    for p in BOTH:
        hop_wait(p, 3)

    wait_for(buf.at[:, :, :HALF - ROWS], in_send)

    @pl.when(tip)
    def _():
        wait_for(buf.at[:, :, :HALF - 3 * ROWS // 2], out_recv)
        wait_for(buf.at[:, :, :HALF - ROWS], out_send)
        wait_for(far_out, far_send)

    @pl.when(jnp.logical_not(tip))
    def _():
        wait_for(buf, out_recv)
        wait_for(buf.at[:, :, :HALF - 2 * ROWS], out_send)

    @pl.when(upper & tip)
    def _():
        wait_for(st_tx, st_send)

    @pl.when(upper & jnp.logical_not(tip))
    def _():
        wait_for(buf.at[0, :2, :272], st_send)

    wait_for(blocks(2), own_sem)
    sent_wait()
    wait_for(buf.at[:3, :, :480], fw_send)
    wait_for(buf.at[:3, :, :FIN * 16 // 24], fw_recv)


def writer(*refs):
    ins, (o, dq, dk, dv, dr, du, dw, sem) = refs[:4 + N_PART], refs[4 + N_PART:]
    pairs = list(zip(ins[:4], (o, dq, dk, dv)))
    for m, part in enumerate(ins[4:]):
        rows = min(PART, HALF - PART * m)
        for side in BOTH:
            start = HALF * side + PART * m
            pairs.append((part.at[side, :rows], dr.at[start:start + rows]))
    last = HALF - PART * (N_PART - 1)
    pairs += [(ins[-1].at[0, last], du), (ins[-1].at[0, last + 1], dw)]
    copies = [pltpu.make_async_copy(src, dst, sem.at[j]) for j, (src, dst) in enumerate(pairs)]
    for copy in copies:
        copy.start()
    for copy in copies:
        copy.wait()


def solution(mesh):
    seq_spec = P(None, "cp", None, None)

    def local(query, key_in, value, bias_u, bias_w, rel_k, d_out):
        n_batch, rows, n_heads, head_dim = query.shape
        pairs = (n_batch, rows, N_PAIR, PAIR, head_dim)
        vm = pltpu.VMEM
        dma = pltpu.SemaphoreType.DMA
        whole = pl.BlockSpec(memory_space=pl.ANY)
        act = jax.ShapeDtypeStruct(pairs, BF16)
        vec = jax.ShapeDtypeStruct((n_heads, 1, head_dim), F32)
        tok = (PAIR, SEQ, HEAD)
        tok_t = (PAIR, HEAD, SEQ)
        acc = (HEAD + 8, HALF)
        outs = pl.pallas_call(
            kernel,
            name="rel_attn",
            out_shape=(act, act, act, act,
                       *[jax.ShapeDtypeStruct((2, PART, n_heads, 1, head_dim), F32)] * N_PART,
                       jax.ShapeDtypeStruct((4, SLOTS, ROWS, FAR, PAIR, HEAD), BF16)),
            in_specs=[pl.BlockSpec(memory_space=pltpu.HBM)] * 7,
            out_specs=[whole] * (5 + N_PART),
            scratch_shapes=[
                vm((4, SUBS, HALF, PAIR, HEAD), BF16), vm((2, SUBS, HALF, PAIR, HEAD), BF16),
                vm((2, SEQ, PAIR, HEAD), BF16), vm((N_PAIR, PAIR, HEAD), BF16), vm((N_PAIR, PAIR, HEAD), BF16),
                vm((SUBS, PAIR, 8, HALF), F32), vm((SUBS, PAIR, 8, HALF), F32), vm((SUBS // 2, 8, TIP), F32), vm((3, SUBS // 2, 8, TIP), F32), vm((QB, HEAD), F32),
                vm((2, 2) + acc, F32), vm((2,) + acc, F32), vm((2, FIN, 1, HEAD), F32), vm((4, 2) + acc, F32),
                vm((QB, SEQ), F32), vm((QB, SEQ), F32), vm((QB, SEQ), F32),
                vm((QB, SEQ), BF16), vm((QB, SEQ), BF16), vm((QB, SEQ), BF16),
                vm(tok, BF16), vm(tok, BF16), vm(tok, BF16), vm(tok, BF16), vm(tok, BF16),
                vm(tok_t, BF16), vm(tok_t, BF16), vm(tok_t, BF16), vm(tok_t, BF16), vm(tok_t, BF16),
                vm((4, SEQ, HEAD), BF16), vm((4, HEAD, SEQ), BF16),
                vm((PAIR, HEAD, HALF), F32), vm((PAIR, HEAD, HALF), F32), vm((4, PAIR, HALF, HEAD), BF16),
                dma, dma((2, SUBS)), dma, dma, dma, dma((4,)), dma((3,)), dma((SUBS,)), dma, dma((3,)),
                dma((2,)), dma((2,)), dma, dma((2, 4)), dma, dma,
                dma, dma, dma((2,)), dma((2,)), dma,
            ],
            compiler_params=pltpu.CompilerParams(collective_id=0, has_side_effects=True, vmem_limit_bytes=37 * 1024 * 1024),
        )(*[pltpu.with_memory_space_constraint(x, pltpu.HBM) for x in (
            query.reshape(pairs), key_in.reshape(pairs), value.reshape(pairs), d_out.reshape(pairs),
            rel_k.reshape(SEQ, N_PAIR, PAIR, head_dim), bias_u.reshape(N_PAIR, PAIR, head_dim), bias_w.reshape(N_PAIR, PAIR, head_dim))])
        o, dq, dk, dv, dr, du, dw = pl.pallas_call(
            writer,
            name="writer",
            out_shape=(act, act, act, act, jax.ShapeDtypeStruct((SEQ, n_heads, 1, head_dim), F32), vec, vec),
            in_specs=[whole] * (4 + N_PART),
            out_specs=[whole] * 7,
            scratch_shapes=[dma((6 + 2 * N_PART,))],
            compiler_params=pltpu.CompilerParams(vmem_limit_bytes=1024 * 1024),
        )(*outs[:-1])
        full = query.shape
        return (o.reshape(full), dq.reshape(full), dk.reshape(full), dv.reshape(full),
                du.reshape(bias_u.shape), dw.reshape(bias_w.shape), dr.reshape(rel_k.shape))

    return jax.shard_map(local, mesh=mesh,
                         in_specs=(seq_spec, seq_spec, seq_spec, P(), P(), P(), seq_spec),
                         out_specs=(seq_spec, seq_spec, seq_spec, seq_spec, P(), P(), P()),
                         check_vma=False)
```
